32 devices in a mesh: dp: 8 (over y, x, core), tensor: 4 (over z).
Axes of the slice: x: 2, y: 2, z: 4, core: 2. Of those that a mesh axis runs over, the one named last changes fastest.
Arguments:
- hidden_in: bfloat16 [4096, 2048], P(('dp', 'tensor')), may hold values from -6 to 6
- out_cotangent: bfloat16 [4096, 2048], P(('dp', 'tensor')), may hold values from -6 to 6
- doc_ids: int32 [4096], P('dp'), may hold values from 0 to 7, as said below
- attn_gain: bfloat16 [2048], P('dp'), may hold values from 0.5 to 1.5
- query_weight: bfloat16 [2048, 2048], P('dp', 'tensor')
- key_weight: bfloat16 [2048, 2048], P('dp', 'tensor')
- value_weight: bfloat16 [2048, 2048], P('dp', 'tensor'), may hold values from -0.125 to 0.125
- out_weight: bfloat16 [2048, 2048], P('tensor', 'dp'), may hold values from -1 to 1
- mlp_gain: bfloat16 [2048], P('dp'), may hold values from 0.5 to 1.5
- gate_weight: bfloat16 [2048, 8192], P('dp', 'tensor'), may hold values from -0.125 to 0.125
- up_weight: bfloat16 [2048, 8192], P('dp', 'tensor'), may hold values from -0.125 to 0.125
- down_weight: bfloat16 [8192, 2048], P('tensor', 'dp'), may hold values from -0.0625 to 0.0625
Outputs:
- layer_out: bfloat16 [4096, 2048], P(('dp', 'tensor'))
- input_grad: float32 [4096, 2048], P(('dp', 'tensor'))
- attn_gain_grad: float32 [2048], P(('dp', 'tensor'))
- query_grad: float32 [2048, 2048], P('dp', 'tensor')
- key_grad: float32 [2048, 2048], P('dp', 'tensor')
- value_grad: float32 [2048, 2048], P('dp', 'tensor')
- out_proj_grad: float32 [2048, 2048], P('tensor', 'dp')
- mlp_gain_grad: float32 [2048], P(('dp', 'tensor'))
- gate_grad: float32 [2048, 8192], P('dp', 'tensor')
- up_grad: float32 [2048, 8192], P('dp', 'tensor')
- down_grad: float32 [8192, 2048], P('tensor', 'dp')
The draws below stay inside these ranges and needn't reach their ends.
Inputs may be any that keep to these rules, and one draw needn't show every extreme that they name: `doc_ids`: within each aligned block of 512 tokens (the tokens of one index of dp) the ids start at 0 and never fall. In some block all ids are 0.
All inputs are finite; a program needn't handle non-finite values.
Results may differ from the reference program's by a relative error of at most 0.017.
Values may be sent and summed in bfloat16 or wider, within the bound.
A program may use at most 320 MiB of HBM per device.

```python
import math
import jax
import jax.numpy as jnp
from jax import lax

D = 2048
HEAD_DIM = 64
FF = 8192
TOK_DEV = 512
TOKENS = 4096


def projection(key, offset):
    own_key = jax.random.fold_in(key, offset)
    entries = jax.random.normal(own_key, (D, D), jnp.float32)
    return (entries / math.sqrt(D)).astype(jnp.bfloat16)


def draw_query_weight(key, part):
    return projection(key, 211)


def draw_key_weight(key, part):
    return projection(key, 223)


def draw_doc_ids(key, part):
    blocks = TOKENS // TOK_DEV
    cut_points = jax.random.randint(jax.random.fold_in(key, 1), (blocks, 7), 1, TOK_DEV)
    active = jax.random.randint(jax.random.fold_in(key, 2), (blocks,), 0, 8)
    whole_block = jax.random.randint(jax.random.fold_in(key, 3), (), 0, blocks)
    number = jnp.arange(blocks)
    active = jnp.where(number == whole_block, 0, active)
    active = jnp.where(number == (whole_block + blocks // 2) % blocks, 7, active)
    in_use = jnp.arange(7)[None, :] < active[:, None]
    position = jnp.arange(TOK_DEV)
    passed = (position[None, :, None] >= cut_points[:, None, :]) & in_use[:, None, :]
    return jnp.sum(passed.astype(jnp.int32), axis=2).astype(jnp.int32).reshape(TOKENS)


def raised(values, key, source, target, blocks, factor):
    def block_of(dim):
        return (jnp.arange(values.shape[dim]) // (values.shape[dim] // blocks)).reshape((-1,) + (1,) * (values.ndim - 1 - dim))

    near = jax.random.permutation(key, blocks)[block_of(target)]
    far = (block_of(target) + blocks // 2) % blocks
    return jnp.where((block_of(source) == near) | (block_of(source) == far), factor * values, values)


def steps_of(key, dims, cuts, low, top_value):
    gain, own = 1.0, jax.random.fold_in(key, 6)
    for dim, parts in cuts:
        draws = jnp.exp(jax.random.uniform(jax.random.fold_in(own, dim), (parts,), jnp.float32, low / len(cuts), top_value / len(cuts)))
        gain = gain * jnp.repeat(draws, dims[dim] // parts).reshape([-1 if axis == dim else 1 for axis in range(len(dims))])
    return gain


def centred(key, shape, width, most, shards=(), kind=jnp.bfloat16):
    values = width * jax.random.normal(key, shape, jnp.float32)
    if shards:
        values = values * steps_of(key, shape, shards, -0.22, 0.18)
    return jnp.clip(values, -most, most).astype(kind)


def gaussian_with(rng, dims, deviation, most, split, heavy, kind=jnp.bfloat16):
    values = deviation * jax.random.normal(rng, dims, jnp.float32)
    if split:
        values = values * steps_of(rng, dims, split, -0.22, 0.18)
    return jnp.clip(raised(values, jax.random.fold_in(rng, 3), *heavy), -most, most).astype(kind)


def setup_inputs(seed: int = 0) -> dict:
    key_list = jax.random.split(jax.random.key(seed), 13)
    hidden_in = centred(key_list[0], (TOKENS, D), 1.0, 6.0, ((0, 32),))
    out_cotangent = gaussian_with(key_list[1], (TOKENS, D), 1.0, 6.0, ((0, 32),), (0, 1, 32, 2.75))
    doc_ids = draw_doc_ids(jax.random.fold_in(key_list[12], 71), 0)
    attn_gain = jnp.clip(1.0 + 0.1 * jax.random.normal(key_list[3], (D,), jnp.float32), 0.5, 1.5).astype(jnp.bfloat16)
    query_weight = draw_query_weight(jax.random.fold_in(key_list[12], 71), 0)
    key_weight = draw_key_weight(jax.random.fold_in(key_list[12], 71), 0)
    value_weight = centred(key_list[6], (D, D), D ** -0.5, 0.125, ((0, 8), (1, 4)))
    out_weight = centred(key_list[7], (D, D), (D // 64) ** -0.5, 1.0, ((0, 4), (1, 8)))
    mlp_gain = jnp.clip(1.0 + 0.1 * jax.random.normal(key_list[8], (D,), jnp.float32), 0.5, 1.5).astype(jnp.bfloat16)
    gate_weight = centred(key_list[9], (D, FF), D ** -0.5, 0.125, ((0, 8), (1, 4)))
    up_weight = centred(key_list[10], (D, FF), D ** -0.5, 0.125, ((0, 8), (1, 4)))
    down_weight = centred(key_list[11], (FF, D), FF ** -0.5, 0.0625, ((0, 4), (1, 8)))
    return dict(hidden_in=hidden_in, out_cotangent=out_cotangent, doc_ids=doc_ids, attn_gain=attn_gain, query_weight=query_weight, key_weight=key_weight, value_weight=value_weight, out_weight=out_weight, mlp_gain=mlp_gain, gate_weight=gate_weight, up_weight=up_weight, down_weight=down_weight)


EPSILON = 1e-05
ROPE_BASE = 130000.0
NEGATIVE = -1e+30
HIGHEST_PRECISION = lax.Precision.HIGHEST

@jax.custom_vjp
def low(v):
    return lax.optimization_barrier(v.astype(jnp.bfloat16)).astype(jnp.float32)

@jax.custom_vjp
def low_back(v):
    return v

def low_keep(v):
    return (low(v), None)

def low_pass(kept, grad):
    return (grad,)

def back_keep(v):
    return (v, None)

def back_low(kept, grad):
    return (low(grad),)
low.defvjp(low_keep, low_pass)
low_back.defvjp(back_keep, back_low)

def rope_tables(doc_ids):
    length = doc_ids.shape[0]
    token_index = jnp.arange(length, dtype=jnp.int32)
    before = jnp.concatenate([doc_ids[:1] - 1, doc_ids[:-1]])
    doc_start = lax.cummax(jnp.where(doc_ids != before, token_index, 0), axis=0)
    offset_in_doc = (token_index - doc_start).astype(jnp.float32)
    half_size = HEAD_DIM // 2
    frequency = ROPE_BASE ** (-jnp.arange(half_size, dtype=jnp.float32) / half_size)
    angles = offset_in_doc[:, None] * frequency[None, :]
    return (jnp.cos(angles)[:, None, :], jnp.sin(angles)[:, None, :])

def rotate(values, cosine_table, sine_table):
    half_size = values.shape[-1] // 2
    leading = values[..., :half_size]
    trailing = values[..., half_size:]
    return jnp.concatenate([leading * cosine_table - trailing * sine_table, trailing * cosine_table + leading * sine_table], axis=-1)

def attend(query_rot, key_rot, value_rows, doc_ids):
    length = doc_ids.shape[0]
    token_index = jnp.arange(length, dtype=jnp.int32)
    allowed = (doc_ids[:, None] == doc_ids[None, :]) & (token_index[:, None] >= token_index[None, :])
    scores = low_back(jnp.einsum('qhd,khd->hqk', query_rot, key_rot, precision=HIGHEST_PRECISION) * HEAD_DIM ** (-0.5))
    scores = jnp.where(allowed[None], scores, NEGATIVE)
    shifted = scores - lax.optimization_barrier(jnp.max(scores, axis=-1, keepdims=True))
    weights = jnp.exp(shifted)
    probabilities = weights / lax.optimization_barrier(jnp.sum(weights, axis=-1, keepdims=True))
    return jnp.einsum('hqk,khd->qhd', low(probabilities), value_rows, precision=HIGHEST_PRECISION)

def layer(block_rows, weights, cosine_table, sine_table, doc_ids):
    attn_gain, query_weight, key_weight, value_weight, out_weight, mlp_gain, gate_weight, up_weight, down_weight = weights
    length = block_rows.shape[0]
    head_count = query_weight.shape[1] // HEAD_DIM
    inverse_one = lax.rsqrt(lax.optimization_barrier(jnp.mean(block_rows * block_rows, axis=-1, keepdims=True)) + EPSILON)
    normed = low(block_rows * inverse_one * attn_gain)
    query_pre = low_back(jnp.dot(normed, query_weight, precision=HIGHEST_PRECISION)).reshape(length, head_count, HEAD_DIM)
    key_pre = low_back(jnp.dot(normed, key_weight, precision=HIGHEST_PRECISION)).reshape(length, head_count, HEAD_DIM)
    value_rows = low(low_back(jnp.dot(normed, value_weight, precision=HIGHEST_PRECISION))).reshape(length, head_count, HEAD_DIM)
    query_rot = low(rotate(query_pre, cosine_table, sine_table))
    key_rot = low(rotate(key_pre, cosine_table, sine_table))
    attended = jax.checkpoint(attend)(query_rot, key_rot, value_rows, doc_ids)
    attended = low(low_back(attended.reshape(length, head_count * HEAD_DIM)))
    branch = low_back(jnp.dot(attended, out_weight, precision=HIGHEST_PRECISION))
    middle = block_rows + branch
    sent = low(middle)
    inverse_two = lax.rsqrt(lax.optimization_barrier(jnp.mean(sent * sent, axis=-1, keepdims=True)) + EPSILON)
    normed_two = low(sent * inverse_two * mlp_gain)
    gate = low_back(jnp.dot(normed_two, gate_weight, precision=HIGHEST_PRECISION))
    upward = low_back(jnp.dot(normed_two, up_weight, precision=HIGHEST_PRECISION))
    hidden = low(gate * jax.nn.sigmoid(gate) * upward)
    return middle + low_back(jnp.dot(hidden, down_weight, precision=HIGHEST_PRECISION))

def reference(hidden_in, out_cotangent, doc_ids, attn_gain, query_weight, key_weight, value_weight, out_weight, mlp_gain, gate_weight, up_weight, down_weight):
    params = tuple((weight.astype(jnp.float32) for weight in (attn_gain, query_weight, key_weight, value_weight, out_weight, mlp_gain, gate_weight, up_weight, down_weight)))
    block_total = TOKENS // TOK_DEV
    inputs = hidden_in.astype(jnp.float32).reshape(block_total, TOK_DEV, D)
    cotangents = out_cotangent.astype(jnp.float32).reshape(block_total, TOK_DEV, D)
    id_blocks = doc_ids.reshape(block_total, TOK_DEV)

    def one_block(summed, pieces):
        block_in, cot_block, block_ids = pieces
        cosine_table, sine_table = rope_tables(block_ids)

        def forward(block_rows, *weights):
            return layer(block_rows, weights, cosine_table, sine_table, block_ids)
        result, pullback = jax.vjp(forward, block_in, *params)
        gradients = pullback(cot_block)
        summed = tuple((earlier + fresh for earlier, fresh in zip(summed, gradients[1:])))
        return (summed, (result.astype(jnp.bfloat16), gradients[0]))
    initial = tuple((jnp.zeros_like(weight) for weight in params))
    summed, (outputs, input_grads) = lax.scan(one_block, initial, (inputs, cotangents, id_blocks))
    return (outputs.reshape(TOKENS, D), input_grads.reshape(TOKENS, D), summed[0], summed[1], summed[2], summed[3], summed[4], summed[5], summed[6], summed[7], summed[8])
```

```python
from functools import partial

import jax
import jax.numpy as jnp
from jax import lax
from jax.experimental import pallas as pl
from jax.experimental.pallas import tpu as pltpu
from jax.sharding import PartitionSpec as P

HEAD_DIM = 64
EPSILON = 1e-05
ROPE_BASE = 130000.0
NEGATIVE = -1e30
VMEM_LIMIT = 63 * 1024 * 1024
BF = jnp.bfloat16
F32 = jnp.float32


def dot(left, right):
    return jnp.dot(left, right, preferred_element_type=F32)


def dot_rows(left, right):
    return lax.dot_general(left, right, (((1,), (1,)), ((), ())), preferred_element_type=F32)


def dot_cols(left, right):
    return lax.dot_general(left, right, (((0,), (0,)), ((), ())), preferred_element_type=F32)


def vmem():
    return pl.BlockSpec(memory_space=pltpu.VMEM)


def anyspace():
    return pl.BlockSpec(memory_space=pl.ANY)


def params():
    return pltpu.CompilerParams(vmem_limit_bytes=VMEM_LIMIT)


def cost(flops, nbytes):
    return pl.CostEstimate(flops=int(flops), bytes_accessed=int(nbytes), transcendentals=0)


def shape(dims, kind):
    return jax.ShapeDtypeStruct(dims, kind)


def place_copies(tags, pieces, target, sem, axis, width):
    own = lax.axis_index("dp")
    copies = []
    for slot, (tag, piece) in enumerate(zip(tags, pieces)):
        if tag is None:
            where = target
        else:
            start = pl.multiple_of((own ^ tag) * width, width)
            where = target.at[pl.ds(start, width), :] if axis == 0 else target.at[:, pl.ds(start, width)]
        copies.append(pltpu.make_async_copy(piece, where, sem.at[slot]))
    return copies


def row_copies(pieces, target, sem):
    copies = []
    for slot, piece in enumerate(pieces):
        rows = piece.shape[0]
        copies.append(pltpu.make_async_copy(piece, target.at[pl.ds(slot * rows, rows), :], sem.at[slot]))
    return copies


def start_all(copies):
    for copy in copies:
        copy.start()


def wait_all(copies):
    for copy in copies:
        copy.wait()


def turn(values, cosine, sine):
    width = values.shape[1]
    lane = lax.broadcasted_iota(jnp.int32, values.shape, 1)
    partner = jnp.where(
        lax.rem(lane, HEAD_DIM) < HEAD_DIM // 2,
        pltpu.roll(values, width - HEAD_DIM // 2, 1),
        pltpu.roll(values, HEAD_DIM // 2, 1),
    )
    return values * cosine + partner * sine


def norm_rows(source, target, inverses, gain, tile):
    @pl.loop(0, source.shape[0] // tile)
    def _(step):
        rows = pl.ds(pl.multiple_of(step * tile, tile), tile)
        values = source[rows, :].astype(F32)
        inverse = lax.rsqrt(jnp.mean(values * values, axis=-1, keepdims=True) + EPSILON)
        inverses[rows, :] = inverse
        target[rows, :] = (values * inverse * gain[...]).astype(BF)


def fill_bias(bias, first, last, key_index):
    keys = key_index[...]
    bias[...] = jnp.where((keys >= first[...]) & (keys <= last[...]), 0.0, NEGATIVE)


def head_lanes(width, half):
    lane = lax.broadcasted_iota(jnp.int32, (1, width), 1)
    return (lax.div(lane, HEAD_DIM) == half).astype(F32)


def probabilities(query, key, bias):
    scores = dot_rows(query, key) + bias
    weights = jnp.exp(scores - jnp.max(scores, axis=-1, keepdims=True))
    return weights * (1.0 / jnp.sum(weights, axis=-1, keepdims=True))


def attn_fwd_kernel(tags, width, nrow, *refs):
    npiece = len(tags)
    rows_in = refs[:nrow]
    gain, cosine, sine, first, last, key_index = refs[nrow : nrow + 6]
    rest = refs[nrow + 6 :]
    qkv_in, out_in = rest[:npiece], rest[npiece : 2 * npiece]
    rest = rest[2 * npiece :]
    normed, qkv, attended, inverses = rest[:4]
    parts = rest[4 : 4 + nrow]
    hidden, qkv_w, out_w, bias, sem_rows, sem_qkv, sem_out = rest[4 + nrow :]
    load_rows = row_copies(rows_in, hidden, sem_rows)
    load_qkv = place_copies(tags, qkv_in, qkv_w, sem_qkv, 0, width)
    load_out = place_copies(tags, out_in, out_w, sem_out, 1, width)
    start_all(load_rows + load_qkv + load_out)
    fill_bias(bias, first, last, key_index)
    wait_all(load_rows)
    norm_rows(hidden, normed, inverses, gain, 64)
    wait_all(load_qkv)
    heads = attended.shape[1]
    step_cols = 256

    @pl.loop(0, 2 * heads // step_cols)
    def _(step):
        cols = pl.ds(pl.multiple_of(step * step_cols, step_cols), step_cols)
        qkv[:, cols] = turn(dot(normed[...], qkv_w[:, cols]), cosine[...], sine[...]).astype(BF)

    @pl.loop(2 * heads // step_cols, 3 * heads // step_cols)
    def _(step):
        cols = pl.ds(pl.multiple_of(step * step_cols, step_cols), step_cols)
        qkv[:, cols] = dot(normed[...], qkv_w[:, cols]).astype(BF)

    @pl.loop(0, heads // 128)
    def _(pair):
        base = pl.multiple_of(pair * 128, 128)
        query = qkv[:, pl.ds(base, 128)]
        key = qkv[:, pl.ds(heads + base, 128)]
        value = qkv[:, pl.ds(2 * heads + base, 128)]
        total = None
        for half in range(2):
            lanes = head_lanes(128, half).astype(BF)
            probs = probabilities(query * (lanes * HEAD_DIM ** (-0.5)), key, bias[...])
            term = dot(probs.astype(BF), value * lanes)
            total = term if total is None else total + term
        attended[:, pl.ds(base, 128)] = total.astype(BF)

    wait_all(load_out)
    tile = parts[0].shape[0]

    @pl.loop(0, out_w.shape[1] // step_cols)
    def _(step):
        cols = pl.ds(pl.multiple_of(step * step_cols, step_cols), step_cols)
        product = dot(attended[...], out_w[:, cols])
        for slot, part in enumerate(parts):
            part[:, cols] = product[slot * tile : (slot + 1) * tile, :].astype(part.dtype)


def attn_fwd(rows, gain, tables, tags, width, qkv_pieces, out_pieces):
    nrow, (tile, dim) = len(rows), rows[0].shape
    tokens = nrow * tile
    heads = out_pieces[0].shape[0]
    npiece = len(tags)
    return pl.pallas_call(
        partial(attn_fwd_kernel, tags, width, nrow),
        out_shape=[
            shape((tokens, dim), BF),
            shape((tokens, 3 * heads), BF),
            shape((tokens, heads), BF),
            shape((tokens, 1), F32),
        ]
        + [shape((tile, dim), F32 if slot == 0 else BF) for slot in range(nrow)],
        in_specs=[anyspace()] * nrow + [vmem()] * 6 + [anyspace()] * (2 * npiece),
        out_specs=[vmem()] * (4 + nrow),
        scratch_shapes=[
            pltpu.VMEM((tokens, dim), BF),
            pltpu.VMEM((dim, 3 * heads), BF),
            pltpu.VMEM((heads, dim), BF),
            pltpu.VMEM((tokens, tokens), F32),
            pltpu.SemaphoreType.DMA((nrow,)),
            pltpu.SemaphoreType.DMA((npiece,)),
            pltpu.SemaphoreType.DMA((npiece,)),
        ],
        compiler_params=params(),
        cost_estimate=cost(2 * tokens * dim * 4 * heads * 3, 20e6),
        name="attn_fwd",
    )(*rows, gain, *tables, *qkv_pieces, *out_pieces)


def attn_bwd_kernel(tags, width, nrow, *refs):
    npiece = len(tags)
    rows_in, hidden_in = refs[:nrow], refs[nrow : 2 * nrow]
    qkv, inverses, cosine, sine, first, last, key_index = refs[2 * nrow : 2 * nrow + 7]
    rest = refs[2 * nrow + 7 :]
    qkv_in, out_in = rest[:npiece], rest[npiece : 2 * npiece]
    rest = rest[2 * npiece :]
    branch, d_qkv, gain_grad = rest[:3]
    parts = rest[3 : 3 + nrow]
    hidden, d_attended, qkv_w, out_w, bias, sem_rows, sem_x, sem_qkv, sem_out = rest[3 + nrow :]
    load_rows = row_copies(rows_in, branch, sem_rows)
    load_x = row_copies(hidden_in, hidden, sem_x)
    load_out = place_copies(tags, out_in, out_w, sem_out, 1, width)
    load_qkv = place_copies(tags, qkv_in, qkv_w, sem_qkv, 0, width)
    start_all(load_rows + load_out + load_qkv + load_x)
    fill_bias(bias, first, last, key_index)
    wait_all(load_rows)
    wait_all(load_out)
    heads = out_w.shape[0]
    step_cols = 256

    @pl.loop(0, heads // step_cols)
    def _(step):
        cols = pl.ds(pl.multiple_of(step * step_cols, step_cols), step_cols)
        d_attended[:, cols] = dot_rows(branch[...], out_w[cols, :]).astype(BF)

    score_scale = HEAD_DIM ** (-0.5)

    @pl.loop(0, heads // 128)
    def _(pair):
        base = pl.multiple_of(pair * 128, 128)
        query = qkv[:, pl.ds(base, 128)]
        key = qkv[:, pl.ds(heads + base, 128)]
        value = qkv[:, pl.ds(2 * heads + base, 128)]
        grad = d_attended[:, pl.ds(base, 128)]
        sums = [0.0, 0.0, 0.0]
        for half in range(2):
            lanes = head_lanes(128, half).astype(BF)
            own_query = query * (lanes * score_scale)
            own_grad = grad * lanes
            probs = probabilities(own_query, key, bias[...])
            d_value = dot_cols(probs.astype(BF), own_grad)
            d_probs = dot_rows(own_grad, value)
            delta = jnp.sum(probs * d_probs, axis=-1, keepdims=True)
            d_scores = (probs * (d_probs - delta)).astype(BF)
            d_query = dot(d_scores, key * lanes) * score_scale
            d_key = dot_cols(d_scores, own_query)
            sums = [sums[0] + d_query, sums[1] + d_key, sums[2] + d_value]
        back = -sine[:, :128]
        d_qkv[:, pl.ds(base, 128)] = turn(sums[0], cosine[:, :128], back).astype(BF)
        d_qkv[:, pl.ds(heads + base, 128)] = turn(sums[1], cosine[:, :128], back).astype(BF)
        d_qkv[:, pl.ds(2 * heads + base, 128)] = sums[2].astype(BF)

    wait_all(load_qkv)
    wait_all(load_x)
    tile = parts[0].shape[0]

    @pl.loop(0, qkv_w.shape[0] // step_cols)
    def _(step):
        cols = pl.ds(pl.multiple_of(step * step_cols, step_cols), step_cols)
        product = dot_rows(d_qkv[...], qkv_w[cols, :])
        gain_grad[:, cols] = jnp.sum(product * (hidden[:, cols].astype(F32) * inverses[...]), axis=0, keepdims=True)
        for slot, part in enumerate(parts):
            part[:, cols] = product[slot * tile : (slot + 1) * tile, :].astype(part.dtype)


def attn_bwd(rows, hidden, qkv, inverses, tables, tags, width, qkv_pieces, out_pieces):
    nrow, (tile, dim) = len(rows), rows[0].shape
    tokens = nrow * tile
    heads = out_pieces[0].shape[0]
    npiece = len(tags)
    return pl.pallas_call(
        partial(attn_bwd_kernel, tags, width, nrow),
        out_shape=[shape((tokens, dim), BF), shape((tokens, 3 * heads), BF), shape((1, dim), F32)]
        + [shape((tile, dim), F32 if slot == 0 else BF) for slot in range(nrow)],
        in_specs=[anyspace()] * (2 * nrow) + [vmem()] * 7 + [anyspace()] * (2 * npiece),
        out_specs=[vmem()] * (3 + nrow),
        scratch_shapes=[
            pltpu.VMEM((tokens, dim), BF),
            pltpu.VMEM((tokens, heads), BF),
            pltpu.VMEM((dim, 3 * heads), BF),
            pltpu.VMEM((heads, dim), BF),
            pltpu.VMEM((tokens, tokens), F32),
            pltpu.SemaphoreType.DMA((nrow,)),
            pltpu.SemaphoreType.DMA((nrow,)),
            pltpu.SemaphoreType.DMA((npiece,)),
            pltpu.SemaphoreType.DMA((npiece,)),
        ],
        compiler_params=params(),
        cost_estimate=cost(2 * tokens * dim * 4 * heads * 6, 30e6),
        name="attn_bwd",
    )(*rows, *hidden, qkv, inverses, *tables, *qkv_pieces, *out_pieces)


def mlp_kernel(tags, width, nrow, *refs):
    npiece = len(tags)
    sent_in, cot_in = refs[:nrow], refs[nrow : 2 * nrow]
    gain = refs[2 * nrow]
    rest = refs[2 * nrow + 1 :]
    gate_in, up_in, down_in = rest[:npiece], rest[npiece : 2 * npiece], rest[2 * npiece : 3 * npiece]
    rest = rest[3 * npiece :]
    normed, hidden, d_gate, d_up, gain_grad = rest[:5]
    parts = rest[5 : 5 + nrow]
    sent, cot, inverses, gate_w, up_w, down_w, sem_sent, sem_cot, sem_gate, sem_up, sem_down = rest[5 + nrow :]
    load_sent = row_copies(sent_in, sent, sem_sent)
    load_cot = row_copies(cot_in, cot, sem_cot)
    load_gate = place_copies(tags, gate_in, gate_w, sem_gate, 0, width)
    load_up = place_copies(tags, up_in, up_w, sem_up, 0, width)
    load_down = place_copies(tags, down_in, down_w, sem_down, 1, width)
    start_all(load_sent + load_cot + load_gate + load_up + load_down)
    wait_all(load_sent)
    norm_rows(sent, normed, inverses, gain, 64)
    wait_all(load_cot)
    wait_all(load_gate)
    wait_all(load_up)
    wait_all(load_down)
    step_cols = 256

    @pl.loop(0, gate_w.shape[1] // step_cols)
    def _(step):
        cols = pl.ds(pl.multiple_of(step * step_cols, step_cols), step_cols)
        gate = dot(normed[...], gate_w[:, cols])
        up = dot(normed[...], up_w[:, cols])
        d_hidden = dot_rows(cot[...], down_w[cols, :])
        s = jax.nn.sigmoid(gate)
        activated = gate * s
        hidden[:, cols] = (activated * up).astype(BF)
        d_gate[:, cols] = (d_hidden * up * (s + activated * (1.0 - s))).astype(BF)
        d_up[:, cols] = (d_hidden * activated).astype(BF)

    tile = parts[0].shape[0]

    @pl.loop(0, gate_w.shape[0] // step_cols)
    def _(step):
        cols = pl.ds(pl.multiple_of(step * step_cols, step_cols), step_cols)
        product = dot_rows(d_gate[...], gate_w[cols, :]) + dot_rows(d_up[...], up_w[cols, :])
        gain_grad[:, cols] = jnp.sum(product * (sent[:, cols].astype(F32) * inverses[...]), axis=0, keepdims=True)
        for slot, part in enumerate(parts):
            part[:, cols] = product[slot * tile : (slot + 1) * tile, :].astype(part.dtype)


def mlp(sent, cot, gain, tags, width, gate_pieces, up_pieces, down_pieces):
    nrow, (tile, dim) = len(sent), sent[0].shape
    tokens = nrow * tile
    units = gate_pieces[0].shape[1]
    npiece = len(tags)
    return pl.pallas_call(
        partial(mlp_kernel, tags, width, nrow),
        out_shape=[shape((tokens, dim), BF)]
        + [shape((tokens, units), BF)] * 3
        + [shape((1, dim), F32)]
        + [shape((tile, dim), F32 if slot == 0 else BF) for slot in range(nrow)],
        in_specs=[anyspace()] * (2 * nrow) + [vmem()] + [anyspace()] * (3 * npiece),
        out_specs=[vmem()] * (5 + nrow),
        scratch_shapes=[
            pltpu.VMEM((tokens, dim), BF),
            pltpu.VMEM((tokens, dim), BF),
            pltpu.VMEM((tokens, 1), F32),
            pltpu.VMEM((dim, units), BF),
            pltpu.VMEM((dim, units), BF),
            pltpu.VMEM((units, dim), BF),
            pltpu.SemaphoreType.DMA((nrow,)),
            pltpu.SemaphoreType.DMA((nrow,)),
            pltpu.SemaphoreType.DMA((npiece,)),
            pltpu.SemaphoreType.DMA((npiece,)),
            pltpu.SemaphoreType.DMA((npiece,)),
        ],
        compiler_params=params(),
        cost_estimate=cost(2 * tokens * dim * units * 5, 40e6),
        name="mlp",
    )(*sent, *cot, gain, *gate_pieces, *up_pieces, *down_pieces)


def mlp_out_kernel(tags, width, *refs):
    npiece = len(tags)
    hidden, down_in = refs[0], refs[1 : 1 + npiece]
    *parts, down_w, sem_down = refs[1 + npiece :]
    load_down = place_copies(tags, down_in, down_w, sem_down, 1, width)
    start_all(load_down)
    wait_all(load_down)
    tile, step_cols = parts[0].shape[0], 256

    @pl.loop(0, down_w.shape[1] // step_cols)
    def _(step):
        cols = pl.ds(pl.multiple_of(step * step_cols, step_cols), step_cols)
        product = dot(hidden[...], down_w[:, cols])
        for slot, part in enumerate(parts):
            part[:, cols] = product[slot * tile : (slot + 1) * tile, :].astype(part.dtype)


def mlp_out(hidden, nrow, dim, tags, width, down_pieces):
    tokens, units = hidden.shape
    tile, npiece = tokens // nrow, len(tags)
    return pl.pallas_call(
        partial(mlp_out_kernel, tags, width),
        out_shape=[shape((tile, dim), F32 if slot == 0 else BF) for slot in range(nrow)],
        in_specs=[vmem()] + [anyspace()] * npiece,
        out_specs=[vmem()] * nrow,
        scratch_shapes=[pltpu.VMEM((units, dim), BF), pltpu.SemaphoreType.DMA((npiece,))],
        compiler_params=params(),
        cost_estimate=cost(2 * tokens * dim * units, 14e6),
        name="mlp_out",
    )(hidden, *down_pieces)


def slice_of(slot, width, own):
    index = lax.axis_index("dp")
    owner = index ^ (2 * slot)
    return pl.ds(pl.multiple_of((owner if own else lax.div(owner, 2)) * width, width), width)


def grad_rows_kernel(width, left, left_pair, right, right_pair, *parts):
    step_cols = 512
    for slot, part in enumerate(parts):
        own, pair = slice_of(slot, width, True), slice_of(slot, width, False)

        @pl.loop(0, right.shape[1] // step_cols)
        def _(step):
            cols = pl.ds(pl.multiple_of(step * step_cols, step_cols), step_cols)
            total = dot_cols(left[:, own], right[:, cols]) + dot_cols(left_pair[:, pair], right_pair[:, cols])
            part[:, cols] = total.astype(part.dtype)


def grad_rows(left, left_pair, right, right_pair, width):
    tokens, columns = right.shape
    count = left_pair.shape[1] // width
    return pl.pallas_call(
        partial(grad_rows_kernel, width),
        out_shape=[shape((width, columns), F32 if slot == 0 else BF) for slot in range(count)],
        in_specs=[vmem()] * 4,
        out_specs=[vmem()] * count,
        compiler_params=params(),
        cost_estimate=cost(4 * tokens * count * width * columns, 10e6),
        name="grad_rows",
    )(left, left_pair, right, right_pair)


def grad_cols_kernel(width, left, left_pair, right, right_pair, *parts):
    step_rows = 512
    for slot, part in enumerate(parts):
        own, pair = slice_of(slot, width, True), slice_of(slot, width, False)

        @pl.loop(0, left.shape[1] // step_rows)
        def _(step):
            rows = pl.ds(pl.multiple_of(step * step_rows, step_rows), step_rows)
            total = dot_cols(left[:, rows], right[:, own]) + dot_cols(left_pair[:, rows], right_pair[:, pair])
            part[rows, :] = total.astype(part.dtype)


def grad_cols(left, left_pair, right, right_pair, width):
    tokens, rows = left.shape
    count = right_pair.shape[1] // width
    return pl.pallas_call(
        partial(grad_cols_kernel, width),
        out_shape=[shape((rows, width), F32 if slot == 0 else BF) for slot in range(count)],
        in_specs=[vmem()] * 4,
        out_specs=[vmem()] * count,
        compiler_params=params(),
        cost_estimate=cost(4 * tokens * count * width * rows, 10e6),
        name="grad_cols",
    )(left, left_pair, right, right_pair)


def swap(values, flip):
    size = lax.axis_size("dp")
    return lax.ppermute(values, "dp", [(index, index ^ flip) for index in range(size)])


def shift(values, step):
    size = lax.axis_size("tensor")
    return lax.ppermute(values, "tensor", [(index, (index + step) % size) for index in range(size)])


def gather_rows(values):
    return [values] + [shift(values, step) for step in range(1, lax.axis_size("tensor"))]


def scatter_rows(parts):
    total = parts[0].astype(F32)
    for step in range(1, len(parts)):
        total = total + shift(parts[step], -step).astype(F32)
    return total


def gather_weight(values, axis, paired):
    if not paired:
        return [None], [lax.all_gather(values, "dp", axis=axis, tiled=True)]
    size = lax.axis_size("dp")
    near = [values] + [swap(values, flip) for flip in range(2, size, 2)]
    far = [swap(piece, 1) for piece in near]
    return list(range(0, size, 2)) + list(range(1, size, 2)), near + far


def pick(values, core, width):
    tokens, dim = values.shape
    split = values.reshape(tokens, dim // (2 * width), 2, width)
    return lax.dynamic_index_in_dim(split, core, axis=2, keepdims=False).reshape(tokens, dim // 2)


def gather_grads(parts):
    total = parts[0]
    for slot in range(1, len(parts)):
        total = total + swap(parts[slot], 2 * slot).astype(F32)
    return total


def scatter_full(left, right, axis):
    full = dot_cols(left, right).astype(BF)
    return lax.psum_scatter(full, "dp", scatter_dimension=axis, tiled=True).astype(F32)


def scatter_gains(gains, paired):
    if not paired:
        return lax.psum_scatter(gains, ("dp", "tensor"), scatter_dimension=1, tiled=True)
    groups, ranks = lax.axis_size("dp"), lax.axis_size("tensor")
    group, rank = lax.axis_index("dp"), lax.axis_index("tensor")
    split = gains.reshape(gains.shape[0], groups, ranks, -1)
    take = lambda step: lax.dynamic_index_in_dim(split, (rank - step) % ranks, axis=2, keepdims=False)
    total = take(0)
    for step in range(1, ranks):
        total = total + shift(take(step), -step)
    pull = lambda flip: lax.dynamic_index_in_dim(total, group ^ flip, axis=1, keepdims=False)
    result = pull(0)
    for flip in range(1, groups):
        result = result + swap(pull(flip), flip)
    return result


def position_tables(doc_ids, ranks):
    length = doc_ids.shape[0]
    token_index = jnp.arange(length, dtype=jnp.int32)
    before = jnp.concatenate([doc_ids[:1] - 1, doc_ids[:-1]])
    doc_start = lax.cummax(jnp.where(doc_ids != before, token_index, 0), axis=0)
    order = (lax.axis_index("tensor") - jnp.arange(ranks)) % ranks
    last = token_index.reshape(ranks, -1)[order].reshape(length)
    first = doc_start.reshape(ranks, -1)[order].reshape(length)
    half_size = HEAD_DIM // 2
    frequency = ROPE_BASE ** (-jnp.arange(half_size, dtype=F32) / half_size)
    angles = (last - first).astype(F32)[:, None] * frequency[None, :]
    cosine, sine = jnp.cos(angles), jnp.sin(angles)
    cosine = jnp.tile(cosine, (1, 8))
    sine = jnp.tile(jnp.concatenate([-sine, sine], axis=1), (1, 4))
    return cosine, sine, first[:, None], last[:, None], last[None, :]


def rms_back(grad_rows_, values, gain):
    inverse = lax.rsqrt(jnp.mean(values * values, axis=-1, keepdims=True) + EPSILON)
    scaled = grad_rows_ * gain
    return inverse * (scaled - values * inverse * inverse * jnp.mean(scaled * values, axis=-1, keepdims=True))


def body(
    hidden_in,
    out_cotangent,
    doc_ids,
    attn_gain,
    query_weight,
    key_weight,
    value_weight,
    out_weight,
    mlp_gain,
    gate_weight,
    up_weight,
    down_weight,
):
    ranks, groups = lax.axis_size("tensor"), lax.axis_size("dp")
    paired = groups == 8
    core = lax.axis_index("dp") % 2
    width, heads = query_weight.shape
    dim = hidden_in.shape[1]

    hidden_rows = gather_rows(hidden_in)
    gains = lax.all_gather(jnp.stack([attn_gain, mlp_gain]), "dp", axis=1, tiled=True).astype(F32)
    attn_scale, mlp_scale = gains[:1], gains[1:]
    qkv_weight = jnp.concatenate([query_weight, key_weight, value_weight], axis=1)
    tags, qkv_pieces = gather_weight(qkv_weight, 0, paired)
    tags, out_pieces = gather_weight(out_weight, 1, paired)
    cot_rows = gather_rows(out_cotangent)
    tags, down_pieces = gather_weight(down_weight, 1, paired)
    tags, gate_pieces = gather_weight(gate_weight, 0, paired)
    tags, up_pieces = gather_weight(up_weight, 0, paired)

    tables = position_tables(doc_ids, ranks)
    normed, qkv, attended, inverses, *branch_parts = attn_fwd(
        hidden_rows, attn_scale, tables, tags, width, qkv_pieces, out_pieces
    )
    input_local = hidden_in.astype(F32)
    middle = input_local + scatter_rows(branch_parts)
    sent = middle.astype(BF)
    sent_rows = gather_rows(sent)
    normed_two, hidden, d_gate, d_up, mlp_gain_part, *two_parts = mlp(
        sent_rows, cot_rows, mlp_scale, tags, width, gate_pieces, up_pieces, down_pieces
    )
    grad_two_rows = scatter_rows(two_parts)
    grad_middle = out_cotangent.astype(F32) + rms_back(grad_two_rows, sent.astype(F32), mlp_scale)
    branch_rows = gather_rows(grad_middle.astype(BF))

    cot_full = jnp.concatenate(cot_rows, axis=0)
    if paired:
        hidden_pair, d_gate_pair, d_up_pair = swap(hidden, 1), swap(d_gate, 1), swap(d_up, 1)
        cot_pair = swap(pick(cot_full, 1 - core, width), 1)
        two_pair = swap(pick(normed_two, 1 - core, width), 1)
        down_grad = gather_grads(grad_cols(hidden, hidden_pair, cot_full, cot_pair, width))
        gate_grad = gather_grads(grad_rows(normed_two, two_pair, d_gate, d_gate_pair, width))
        up_grad = gather_grads(grad_rows(normed_two, two_pair, d_up, d_up_pair, width))
    else:
        down_grad = scatter_full(hidden, cot_full, 1)
        gate_grad = scatter_full(normed_two, d_gate, 0)
        up_grad = scatter_full(normed_two, d_up, 0)
    mlp_rows = scatter_rows(mlp_out(hidden, ranks, dim, tags, width, down_pieces))
    layer_out = (middle + mlp_rows).astype(BF)

    branch_full, d_qkv, attn_gain_part, *one_parts = attn_bwd(
        branch_rows, hidden_rows, qkv, inverses, tables, tags, width, qkv_pieces, out_pieces
    )
    if paired:
        d_qkv_pair, attended_pair = swap(d_qkv, 1), swap(attended, 1)
        normed_pair = swap(pick(normed, 1 - core, width), 1)
        branch_pair = swap(pick(branch_full, 1 - core, width), 1)
        out_proj_grad = gather_grads(grad_cols(attended, attended_pair, branch_full, branch_pair, width))
        qkv_grad = gather_grads(grad_rows(normed, normed_pair, d_qkv, d_qkv_pair, width))
    else:
        out_proj_grad = scatter_full(attended, branch_full, 1)
        qkv_grad = scatter_full(normed, d_qkv, 0)
    grad_one_rows = scatter_rows(one_parts)
    input_grad = grad_middle + rms_back(grad_one_rows, input_local, attn_scale)
    gain_grads = scatter_gains(jnp.concatenate([attn_gain_part, mlp_gain_part], axis=0), paired)
    return (
        layer_out,
        input_grad,
        gain_grads[0],
        qkv_grad[:, :heads],
        qkv_grad[:, heads : 2 * heads],
        qkv_grad[:, 2 * heads :],
        out_proj_grad,
        gain_grads[1],
        gate_grad,
        up_grad,
        down_grad,
    )


def solution(mesh):
    return jax.shard_map(
        body,
        mesh=mesh,
        in_specs=(
            P(("dp", "tensor"), None),
            P(("dp", "tensor"), None),
            P("dp"),
            P("dp"),
            P("dp", "tensor"),
            P("dp", "tensor"),
            P("dp", "tensor"),
            P("tensor", "dp"),
            P("dp"),
            P("dp", "tensor"),
            P("dp", "tensor"),
            P("tensor", "dp"),
        ),
        out_specs=(
            P(("dp", "tensor"), None),
            P(("dp", "tensor"), None),
            P(("dp", "tensor")),
            P("dp", "tensor"),
            P("dp", "tensor"),
            P("dp", "tensor"),
            P("tensor", "dp"),
            P(("dp", "tensor")),
            P("dp", "tensor"),
            P("dp", "tensor"),
            P("tensor", "dp"),
        ),
        check_vma=False,
    )
```

```python
from functools import partial

import jax
import jax.numpy as jnp
from jax import lax
from jax.experimental import pallas as pl
from jax.experimental.pallas import tpu as pltpu
from jax.sharding import PartitionSpec as P

HEAD_DIM = 64
EPSILON = 1e-05
ROPE_BASE = 130000.0
NEGATIVE = -1e30
VMEM_LIMIT = 63 * 1024 * 1024
BF = jnp.bfloat16
F32 = jnp.float32


def dot(left, right):
    return jnp.dot(left, right, preferred_element_type=F32)


def dot_rows(left, right):
    return lax.dot_general(left, right, (((1,), (1,)), ((), ())), preferred_element_type=F32)


def dot_cols(left, right):
    return lax.dot_general(left, right, (((0,), (0,)), ((), ())), preferred_element_type=F32)


def vmem():
    return pl.BlockSpec(memory_space=pltpu.VMEM)


def anyspace():
    return pl.BlockSpec(memory_space=pl.ANY)


def params():
    return pltpu.CompilerParams(vmem_limit_bytes=VMEM_LIMIT)


def cost(flops, nbytes):
    return pl.CostEstimate(flops=int(flops), bytes_accessed=int(nbytes), transcendentals=0)


def shape(dims, kind):
    return jax.ShapeDtypeStruct(dims, kind)


def place_copies(tags, pieces, target, sem, axis, width):
    own = lax.axis_index("dp")
    copies = []
    for slot, (tag, piece) in enumerate(zip(tags, pieces)):
        if tag is None:
            where = target
        else:
            start = pl.multiple_of((own ^ tag) * width, width)
            where = target.at[pl.ds(start, width), :] if axis == 0 else target.at[:, pl.ds(start, width)]
        copies.append(pltpu.make_async_copy(piece, where, sem.at[slot]))
    return copies


def row_copies(pieces, target, sem):
    copies = []
    for slot, piece in enumerate(pieces):
        rows = piece.shape[0]
        copies.append(pltpu.make_async_copy(piece, target.at[pl.ds(slot * rows, rows), :], sem.at[slot]))
    return copies


def start_all(copies):
    for copy in copies:
        copy.start()


def wait_all(copies):
    for copy in copies:
        copy.wait()


def turn(values, cosine, sine):
    width = values.shape[1]
    lane = lax.broadcasted_iota(jnp.int32, values.shape, 1)
    partner = jnp.where(
        lax.rem(lane, HEAD_DIM) < HEAD_DIM // 2,
        pltpu.roll(values, width - HEAD_DIM // 2, 1),
        pltpu.roll(values, HEAD_DIM // 2, 1),
    )
    return values * cosine + partner * sine


def norm_rows(source, target, inverses, gain, tile):
    @pl.loop(0, source.shape[0] // tile)
    def _(step):
        rows = pl.ds(pl.multiple_of(step * tile, tile), tile)
        values = source[rows, :].astype(F32)
        inverse = lax.rsqrt(jnp.mean(values * values, axis=-1, keepdims=True) + EPSILON)
        inverses[rows, :] = inverse
        target[rows, :] = (values * inverse * gain[...]).astype(BF)


def fill_bias(bias, first, last, key_index):
    keys = key_index[...]
    bias[...] = jnp.where((keys >= first[...]) & (keys <= last[...]), 0.0, NEGATIVE)


def head_lanes(width, half):
    lane = lax.broadcasted_iota(jnp.int32, (1, width), 1)
    return (lax.div(lane, HEAD_DIM) == half).astype(F32)


def probabilities(query, key, bias):
    scores = dot_rows(query, key) + bias
    weights = jnp.exp(scores - jnp.max(scores, axis=-1, keepdims=True))
    return weights * (1.0 / jnp.sum(weights, axis=-1, keepdims=True))


def attend(qkv, attended, bias, heads):
    @pl.loop(0, heads // 128)
    def _(pair):
        base = pl.multiple_of(pair * 128, 128)
        query = qkv[:, pl.ds(base, 128)]
        key = qkv[:, pl.ds(heads + base, 128)]
        value = qkv[:, pl.ds(2 * heads + base, 128)]
        total = None
        for half in range(2):
            lanes = head_lanes(128, half).astype(BF)
            probs = probabilities(query * (lanes * HEAD_DIM ** (-0.5)), key, bias[...])
            term = dot(probs.astype(BF), value * lanes)
            total = term if total is None else total + term
        attended[:, pl.ds(base, 128)] = total.astype(BF)


def attn_fwd_kernel(tags, width, nrow, *refs):
    npiece = len(tags)
    rows_in = refs[:nrow]
    gain, cosine, sine, first, last, key_index = refs[nrow : nrow + 6]
    rest = refs[nrow + 6 :]
    qkv_in, out_in = rest[:npiece], rest[npiece : 2 * npiece]
    rest = rest[2 * npiece :]
    normed, qkv, attended, inverses = rest[:4]
    parts = rest[4 : 4 + nrow]
    hidden, qkv_w, out_w, bias, sem_rows, sem_qkv, sem_out = rest[4 + nrow :]
    load_rows = row_copies(rows_in, hidden, sem_rows)
    load_qkv = place_copies(tags, qkv_in, qkv_w, sem_qkv, 0, width)
    load_out = place_copies(tags, out_in, out_w, sem_out, 1, width)
    start_all(load_rows + load_qkv + load_out)
    fill_bias(bias, first, last, key_index)
    wait_all(load_rows)
    norm_rows(hidden, normed, inverses, gain, 64)
    wait_all(load_qkv)
    heads = attended.shape[1]
    step_cols = 256

    @pl.loop(0, 2 * heads // step_cols)
    def _(step):
        cols = pl.ds(pl.multiple_of(step * step_cols, step_cols), step_cols)
        qkv[:, cols] = turn(dot(normed[...], qkv_w[:, cols]), cosine[...], sine[...]).astype(BF)

    @pl.loop(2 * heads // step_cols, 3 * heads // step_cols)
    def _(step):
        cols = pl.ds(pl.multiple_of(step * step_cols, step_cols), step_cols)
        qkv[:, cols] = dot(normed[...], qkv_w[:, cols]).astype(BF)

    attend(qkv, attended, bias, heads)
    wait_all(load_out)
    tile = parts[0].shape[0]

    @pl.loop(0, out_w.shape[1] // step_cols)
    def _(step):
        cols = pl.ds(pl.multiple_of(step * step_cols, step_cols), step_cols)
        product = dot(attended[...], out_w[:, cols])
        for slot, part in enumerate(parts):
            part[:, cols] = product[slot * tile : (slot + 1) * tile, :].astype(part.dtype)


def attn_fwd(rows, gain, tables, tags, width, qkv_pieces, out_pieces):
    nrow, (tile, dim) = len(rows), rows[0].shape
    tokens = nrow * tile
    heads = out_pieces[0].shape[0]
    npiece = len(tags)
    return pl.pallas_call(
        partial(attn_fwd_kernel, tags, width, nrow),
        out_shape=[
            shape((tokens, dim), BF),
            shape((tokens, 3 * heads), BF),
            shape((tokens, heads), BF),
            shape((tokens, 1), F32),
        ]
        + [shape((tile, dim), F32 if slot == 0 else BF) for slot in range(nrow)],
        in_specs=[anyspace()] * nrow + [vmem()] * 6 + [anyspace()] * (2 * npiece),
        out_specs=[vmem()] * (4 + nrow),
        scratch_shapes=[
            pltpu.VMEM((tokens, dim), BF),
            pltpu.VMEM((dim, 3 * heads), BF),
            pltpu.VMEM((heads, dim), BF),
            pltpu.VMEM((tokens, tokens), F32),
            pltpu.SemaphoreType.DMA((nrow,)),
            pltpu.SemaphoreType.DMA((npiece,)),
            pltpu.SemaphoreType.DMA((npiece,)),
        ],
        compiler_params=params(),
        cost_estimate=cost(2 * tokens * dim * 4 * heads * 3, 20e6),
        name="attn_fwd",
    )(*rows, gain, *tables, *qkv_pieces, *out_pieces)


def attn_bwd_kernel(tags, width, nrow, npart, *refs):
    npiece = len(tags)
    nhid, nrow = nrow[1], nrow[0]
    rows_in, hidden_in = refs[:nrow], refs[nrow : nrow + nhid]
    refs = refs[nrow + nhid :]
    qkv, inverses, cosine, sine, first, last, key_index = refs[:7]
    rest = refs[7:]
    qkv_in, out_in = rest[:npiece], rest[npiece : 2 * npiece]
    rest = rest[2 * npiece :]
    branch, d_qkv, gain_grad = rest[:3]
    parts = rest[3 : 3 + npart]
    hidden, d_attended, qkv_w, out_w, bias, sem_rows, sem_x, sem_qkv, sem_out = rest[3 + npart :]
    load_rows = row_copies(rows_in, branch, sem_rows)
    load_x = row_copies(hidden_in, hidden, sem_x)
    load_out = place_copies(tags, out_in, out_w, sem_out, 1, width)
    load_qkv = place_copies(tags, qkv_in, qkv_w, sem_qkv, 0, width)
    start_all(load_rows + load_out + load_qkv + load_x)
    fill_bias(bias, first, last, key_index)
    wait_all(load_rows)
    wait_all(load_out)
    heads = out_w.shape[0]
    step_cols = 256

    @pl.loop(0, heads // step_cols)
    def _(step):
        cols = pl.ds(pl.multiple_of(step * step_cols, step_cols), step_cols)
        d_attended[:, cols] = dot_rows(branch[...], out_w[cols, :]).astype(BF)

    score_scale = HEAD_DIM ** (-0.5)

    @pl.loop(0, heads // 128)
    def _(pair):
        base = pl.multiple_of(pair * 128, 128)
        query = qkv[:, pl.ds(base, 128)]
        key = qkv[:, pl.ds(heads + base, 128)]
        value = qkv[:, pl.ds(2 * heads + base, 128)]
        grad = d_attended[:, pl.ds(base, 128)]
        sums = [0.0, 0.0, 0.0]
        for half in range(2):
            lanes = head_lanes(128, half).astype(BF)
            own_query = query * (lanes * score_scale)
            own_grad = grad * lanes
            probs = probabilities(own_query, key, bias[...])
            d_value = dot_cols(probs.astype(BF), own_grad)
            d_probs = dot_rows(own_grad, value)
            delta = jnp.sum(probs * d_probs, axis=-1, keepdims=True)
            d_scores = (probs * (d_probs - delta)).astype(BF)
            d_query = dot(d_scores, key * lanes) * score_scale
            d_key = dot_cols(d_scores, own_query)
            sums = [sums[0] + d_query, sums[1] + d_key, sums[2] + d_value]
        back = -sine[:, :128]
        d_qkv[:, pl.ds(base, 128)] = turn(sums[0], cosine[:, :128], back).astype(BF)
        d_qkv[:, pl.ds(heads + base, 128)] = turn(sums[1], cosine[:, :128], back).astype(BF)
        d_qkv[:, pl.ds(2 * heads + base, 128)] = sums[2].astype(BF)

    wait_all(load_qkv)
    wait_all(load_x)
    tile = parts[0].shape[0]

    @pl.loop(0, qkv_w.shape[0] // step_cols)
    def _(step):
        cols = pl.ds(pl.multiple_of(step * step_cols, step_cols), step_cols)
        product = dot_rows(d_qkv[...], qkv_w[cols, :])
        gain_grad[:, cols] = jnp.sum(product * (hidden[:, cols].astype(F32) * inverses[...]), axis=0, keepdims=True)
        for slot, part in enumerate(parts):
            part[:, cols] = product[slot * tile : (slot + 1) * tile, :].astype(part.dtype)


def attn_bwd(rows, hidden, qkv, inverses, tables, tags, width, qkv_pieces, out_pieces, npart):
    nrow, nhid, dim = len(rows), len(hidden), rows[0].shape[1]
    tokens = qkv.shape[0]
    tile = tokens // npart
    heads = out_pieces[0].shape[0]
    npiece = len(tags)
    return pl.pallas_call(
        partial(attn_bwd_kernel, tags, width, (nrow, nhid), npart),
        out_shape=[shape((tokens, dim), BF), shape((tokens, 3 * heads), BF), shape((1, dim), F32)]
        + [shape((tile, dim), F32 if slot == 0 else BF) for slot in range(npart)],
        in_specs=[anyspace()] * (nrow + nhid) + [vmem()] * 7 + [anyspace()] * (2 * npiece),
        out_specs=[vmem()] * (3 + npart),
        scratch_shapes=[
            pltpu.VMEM((tokens, dim), BF),
            pltpu.VMEM((tokens, heads), BF),
            pltpu.VMEM((dim, 3 * heads), BF),
            pltpu.VMEM((heads, dim), BF),
            pltpu.VMEM((tokens, tokens), F32),
            pltpu.SemaphoreType.DMA((nrow,)),
            pltpu.SemaphoreType.DMA((nhid,)),
            pltpu.SemaphoreType.DMA((npiece,)),
            pltpu.SemaphoreType.DMA((npiece,)),
        ],
        compiler_params=params(),
        cost_estimate=cost(2 * tokens * dim * 4 * heads * 6, 30e6),
        name="attn_bwd",
    )(*rows, *hidden, qkv, inverses, *tables, *qkv_pieces, *out_pieces)


def mlp_kernel(tags, width, nrow, npart, *refs):
    npiece = len(tags)
    sent_in, cot_in = refs[:nrow], refs[nrow : 2 * nrow]
    gain = refs[2 * nrow]
    rest = refs[2 * nrow + 1 :]
    gate_in, up_in, down_in = rest[:npiece], rest[npiece : 2 * npiece], rest[2 * npiece : 3 * npiece]
    rest = rest[3 * npiece :]
    normed, hidden, d_gate, d_up, gain_grad = rest[:5]
    parts = rest[5 : 5 + npart]
    sent, cot, inverses, gate_w, up_w, down_w, sem_sent, sem_cot, sem_gate, sem_up, sem_down = rest[5 + npart :]
    load_sent = row_copies(sent_in, sent, sem_sent)
    load_cot = row_copies(cot_in, cot, sem_cot)
    load_gate = place_copies(tags, gate_in, gate_w, sem_gate, 0, width)
    load_up = place_copies(tags, up_in, up_w, sem_up, 0, width)
    load_down = place_copies(tags, down_in, down_w, sem_down, 1, width)
    start_all(load_sent + load_cot + load_gate + load_up + load_down)
    wait_all(load_sent)
    norm_rows(sent, normed, inverses, gain, 64)
    wait_all(load_cot)
    wait_all(load_gate)
    wait_all(load_up)
    wait_all(load_down)
    step_cols = 256

    @pl.loop(0, gate_w.shape[1] // step_cols)
    def _(step):
        cols = pl.ds(pl.multiple_of(step * step_cols, step_cols), step_cols)
        gate = dot(normed[...], gate_w[:, cols])
        up = dot(normed[...], up_w[:, cols])
        d_hidden = dot_rows(cot[...], down_w[cols, :])
        s = jax.nn.sigmoid(gate)
        activated = gate * s
        hidden[:, cols] = (activated * up).astype(BF)
        d_gate[:, cols] = (d_hidden * up * (s + activated * (1.0 - s))).astype(BF)
        d_up[:, cols] = (d_hidden * activated).astype(BF)

    tile = parts[0].shape[0]

    @pl.loop(0, gate_w.shape[0] // step_cols)
    def _(step):
        cols = pl.ds(pl.multiple_of(step * step_cols, step_cols), step_cols)
        product = dot_rows(d_gate[...], gate_w[cols, :]) + dot_rows(d_up[...], up_w[cols, :])
        gain_grad[:, cols] = jnp.sum(product * (sent[:, cols].astype(F32) * inverses[...]), axis=0, keepdims=True)
        for slot, part in enumerate(parts):
            part[:, cols] = product[slot * tile : (slot + 1) * tile, :].astype(part.dtype)


def mlp(sent, cot, gain, tags, width, gate_pieces, up_pieces, down_pieces, npart):
    nrow, dim = len(sent), sent[0].shape[1]
    tokens = nrow * sent[0].shape[0]
    tile = tokens // npart
    units = gate_pieces[0].shape[1]
    npiece = len(tags)
    return pl.pallas_call(
        partial(mlp_kernel, tags, width, nrow, npart),
        out_shape=[shape((tokens, dim), BF)]
        + [shape((tokens, units), BF)] * 3
        + [shape((1, dim), F32)]
        + [shape((tile, dim), F32 if slot == 0 else BF) for slot in range(npart)],
        in_specs=[anyspace()] * (2 * nrow) + [vmem()] + [anyspace()] * (3 * npiece),
        out_specs=[vmem()] * (5 + npart),
        scratch_shapes=[
            pltpu.VMEM((tokens, dim), BF),
            pltpu.VMEM((tokens, dim), BF),
            pltpu.VMEM((tokens, 1), F32),
            pltpu.VMEM((dim, units), BF),
            pltpu.VMEM((dim, units), BF),
            pltpu.VMEM((units, dim), BF),
            pltpu.SemaphoreType.DMA((nrow,)),
            pltpu.SemaphoreType.DMA((nrow,)),
            pltpu.SemaphoreType.DMA((npiece,)),
            pltpu.SemaphoreType.DMA((npiece,)),
            pltpu.SemaphoreType.DMA((npiece,)),
        ],
        compiler_params=params(),
        cost_estimate=cost(2 * tokens * dim * units * 5, 40e6),
        name="mlp",
    )(*sent, *cot, gain, *gate_pieces, *up_pieces, *down_pieces)


def mlp_out_kernel(tags, width, *refs):
    npiece = len(tags)
    hidden, down_in = refs[0], refs[1 : 1 + npiece]
    *parts, down_w, sem_down = refs[1 + npiece :]
    load_down = place_copies(tags, down_in, down_w, sem_down, 1, width)
    start_all(load_down)
    wait_all(load_down)
    tile, step_cols = parts[0].shape[0], 256

    @pl.loop(0, down_w.shape[1] // step_cols)
    def _(step):
        cols = pl.ds(pl.multiple_of(step * step_cols, step_cols), step_cols)
        product = dot(hidden[...], down_w[:, cols])
        for slot, part in enumerate(parts):
            part[:, cols] = product[slot * tile : (slot + 1) * tile, :].astype(part.dtype)


def mlp_out(hidden, nrow, dim, tags, width, down_pieces):
    tokens, units = hidden.shape
    tile, npiece = tokens // nrow, len(tags)
    return pl.pallas_call(
        partial(mlp_out_kernel, tags, width),
        out_shape=[shape((tile, dim), F32 if slot == 0 else BF) for slot in range(nrow)],
        in_specs=[vmem()] + [anyspace()] * npiece,
        out_specs=[vmem()] * nrow,
        scratch_shapes=[pltpu.VMEM((units, dim), BF), pltpu.SemaphoreType.DMA((npiece,))],
        compiler_params=params(),
        cost_estimate=cost(2 * tokens * dim * units, 14e6),
        name="mlp_out",
    )(hidden, *down_pieces)


def slice_of(slot, width, own):
    index = lax.axis_index("dp")
    owner = index ^ (2 * slot)
    return pl.ds(pl.multiple_of((owner if own else lax.div(owner, 2)) * width, width), width)


def grad_rows_kernel(width, left, left_pair, right, right_pair, *parts):
    step_cols = 512
    for slot, part in enumerate(parts):
        own, pair = slice_of(slot, width, True), slice_of(slot, width, False)

        @pl.loop(0, right.shape[1] // step_cols)
        def _(step):
            cols = pl.ds(pl.multiple_of(step * step_cols, step_cols), step_cols)
            total = dot_cols(left[:, own], right[:, cols]) + dot_cols(left_pair[:, pair], right_pair[:, cols])
            part[:, cols] = total.astype(part.dtype)


def grad_rows(left, left_pair, right, right_pair, width):
    tokens, columns = right.shape
    count = left_pair.shape[1] // width
    return pl.pallas_call(
        partial(grad_rows_kernel, width),
        out_shape=[shape((width, columns), F32 if slot == 0 else BF) for slot in range(count)],
        in_specs=[vmem()] * 4,
        out_specs=[vmem()] * count,
        compiler_params=params(),
        cost_estimate=cost(4 * tokens * count * width * columns, 10e6),
        name="grad_rows",
    )(left, left_pair, right, right_pair)


def grad_cols_kernel(width, left, left_pair, right, right_pair, *parts):
    step_rows = 512
    for slot, part in enumerate(parts):
        own, pair = slice_of(slot, width, True), slice_of(slot, width, False)

        @pl.loop(0, left.shape[1] // step_rows)
        def _(step):
            rows = pl.ds(pl.multiple_of(step * step_rows, step_rows), step_rows)
            total = dot_cols(left[:, rows], right[:, own]) + dot_cols(left_pair[:, rows], right_pair[:, pair])
            part[rows, :] = total.astype(part.dtype)


def grad_cols(left, left_pair, right, right_pair, width):
    tokens, rows = left.shape
    count = right_pair.shape[1] // width
    return pl.pallas_call(
        partial(grad_cols_kernel, width),
        out_shape=[shape((rows, width), F32 if slot == 0 else BF) for slot in range(count)],
        in_specs=[vmem()] * 4,
        out_specs=[vmem()] * count,
        compiler_params=params(),
        cost_estimate=cost(4 * tokens * count * width * rows, 10e6),
        name="grad_cols",
    )(left, left_pair, right, right_pair)


MESH = pl.DeviceIdType.MESH
NEAR = (2, 4, 6)


def remote(source, target, send_sem, recv_sem, axis, peer):
    return pltpu.make_async_remote_copy(
        src_ref=source,
        dst_ref=target,
        send_sem=send_sem,
        recv_sem=recv_sem,
        device_id={axis: peer},
        device_id_type=MESH,
    )


def meet(ranks):
    own, rank = lax.axis_index("dp"), lax.axis_index("tensor")
    barrier = pltpu.get_barrier_semaphore()
    for flip in range(1, 8):
        pl.semaphore_signal(barrier, inc=1, device_id={"dp": own ^ flip}, device_id_type=MESH)
    for step in range(1, ranks):
        pl.semaphore_signal(barrier, inc=1, device_id={"tensor": lax.rem(rank + step, ranks)}, device_id_type=MESH)
    pl.semaphore_wait(barrier, ranks + 6)


def at_cols(ref, index, width):
    return ref.at[:, pl.ds(pl.multiple_of(index * width, width), width)]


def at_rows(ref, index, width):
    return ref.at[pl.ds(pl.multiple_of(index * width, width), width), :]


def fill_mask(bias, docs, ranks):
    rank = lax.axis_index("tensor")
    tile = docs.shape[1]
    blocks = [lax.rem(rank - slot + ranks, ranks) for slot in range(ranks)]
    own_docs = [jnp.broadcast_to(docs[pl.ds(block, 1), :].astype(F32), (tile, tile)) for block in blocks]
    turned = [jnp.transpose(values) for values in own_docs]
    row = lax.broadcasted_iota(jnp.int32, (tile, tile), 0)
    lane = lax.broadcasted_iota(jnp.int32, (tile, tile), 1)
    for q in range(ranks):
        for k in range(ranks):
            same = turned[q] == own_docs[k]
            before = row + blocks[q] * tile >= lane + blocks[k] * tile
            bias[q * tile : (q + 1) * tile, k * tile : (k + 1) * tile] = jnp.where(same & before, 0.0, NEGATIVE)


def front_kernel(ranks, *refs):
    hidden_in, cot_in, gains_in = refs[:3]
    weights_in = refs[3:10]
    cosine_in, sine_in, docs = refs[10:13]
    qkv_full, out_full, down_full, gate_full, up_full, hidden_rows, cot_rows, sent_rows = refs[13:21]
    normed, qkv, attended, inverses, middle, gains = refs[21:27]
    hidden, qkv_w, out_w, cosine, sine, bias, part, send_part, recv_part, sent = refs[27:37]
    stage = refs[37:44]
    (w_send, w_recv, z_send, z_recv, p_send, p_recv, g_send, g_recv, load, keep) = refs[44:]
    own, rank = lax.axis_index("dp"), lax.axis_index("tensor")
    tile, dim = hidden_in.shape
    width = weights_in[0].shape[0]
    heads = weights_in[0].shape[1]
    step_cols = 256
    count = dim // step_cols

    def slot_of(index, owner):
        if index < 3:
            rows = pl.ds(pl.multiple_of(owner * width, width), width)
            return qkv_full.at[rows, pl.ds(index * heads, heads)]
        if index == 3:
            return at_cols(out_full, owner, width)
        if index == 4:
            return at_cols(down_full, owner, width)
        return at_rows((gate_full, up_full)[index - 5], owner, width)

    def send_weight(index, flip):
        return remote(
            weights_in[index], slot_of(index, own), w_send.at[index, flip], w_recv.at[index, flip], "dp", own ^ flip
        )

    def pass_weight(index, flip):
        place = slot_of(index, own ^ flip)
        return remote(place, place, w_send.at[index, flip + 1], w_recv.at[index, flip + 1], "dp", own ^ 1)

    def pass_on(indices):
        for index in indices:
            for flip in NEAR:
                send_weight(index, flip).wait_recv()
                pass_weight(index, flip).start()

    def finish(indices):
        for index in indices:
            send_weight(index, 1).wait_recv()
            for flip in NEAR:
                pass_weight(index, flip).wait_recv()

    def send_gain(flip):
        return remote(gains_in, at_cols(gains, own, width), g_send.at[flip], g_recv.at[flip], "dp", own ^ flip)

    def send_z(kind, source, target, step, start, size):
        place = target.at[pl.ds(step * tile + start, size), :]
        peer = lax.rem(rank + step, ranks)
        return remote(
            source.at[pl.ds(start, size), :], place, z_send.at[kind, step], z_recv.at[kind, step], "tensor", peer
        )

    half = tile // 2
    steps = list(range(1, ranks))
    send_hidden = [send_z(0, hidden_in, hidden_rows, step, 0, tile) for step in steps]
    send_cot = [[send_z(1 + h, cot_in, cot_rows, step, h * half, half) for step in steps] for h in range(2)]
    send_sent = [send_z(3, sent, sent_rows, step, 0, tile) for step in steps]

    meet(ranks)
    for copy in send_hidden:
        copy.start()
    for flip in range(1, 8):
        send_gain(flip).start()
    for index in range(4):
        for flip in NEAR + (1,):
            send_weight(index, flip).start()
    for copy in send_cot[0]:
        copy.start()
    for index in range(4, 7):
        for flip in NEAR + (1,):
            send_weight(index, flip).start()

    stage_in = [pltpu.make_async_copy(weights_in[index], stage[index], load.at[index]) for index in range(7)]
    stage_out = [pltpu.make_async_copy(stage[index], slot_of(index, own), keep.at[index]) for index in range(7)]
    own_hidden = pltpu.make_async_copy(hidden_in, hidden.at[pl.ds(0, tile), :], load.at[7])
    own_cot = pltpu.make_async_copy(cot_in, sent, load.at[8])
    own_gain = pltpu.make_async_copy(gains_in, at_cols(gains, own, width), load.at[9])
    tables = []
    for slot in range(ranks):
        block = lax.rem(rank - slot + ranks, ranks)
        for which, (source, target) in enumerate(((cosine_in, cosine), (sine_in, sine))):
            tables.append(
                pltpu.make_async_copy(
                    at_rows(source, block, tile), at_rows(target, slot, tile), load.at[10 + 2 * slot + which]
                )
            )
    start_all(stage_in + [own_hidden, own_cot, own_gain] + tables)
    wait_all(stage_in)
    start_all(stage_out)
    wait_all([own_hidden, own_cot, own_gain])
    keep_hidden = pltpu.make_async_copy(hidden.at[pl.ds(0, tile), :], hidden_rows.at[pl.ds(0, tile), :], keep.at[7])
    keep_cot = pltpu.make_async_copy(sent, cot_rows.at[pl.ds(0, tile), :], keep.at[8])
    start_all([keep_hidden, keep_cot])
    fill_mask(bias, docs, ranks)
    wait_all(tables + stage_out + [keep_hidden, keep_cot])

    pass_on(range(4))
    for flip in range(1, 8):
        send_gain(flip).wait_recv()
    for copy in send_hidden:
        copy.wait_recv()
    load_rows = pltpu.make_async_copy(
        hidden_rows.at[pl.ds(tile, (ranks - 1) * tile), :], hidden.at[pl.ds(tile, (ranks - 1) * tile), :], load.at[0]
    )
    load_rows.start()
    load_rows.wait()
    norm_rows(hidden, normed, inverses, gains.at[pl.ds(0, 1), :], 64)
    finish(range(4))
    load_qkv = pltpu.make_async_copy(qkv_full, qkv_w, load.at[1])
    load_out = pltpu.make_async_copy(out_full, out_w, load.at[2])
    load_qkv.start()
    load_out.start()
    load_qkv.wait()

    @pl.loop(0, 2 * heads // step_cols)
    def _(step):
        cols = pl.ds(pl.multiple_of(step * step_cols, step_cols), step_cols)
        qkv[:, cols] = turn(dot(normed[...], qkv_w[:, cols]), cosine[...], sine[...]).astype(BF)

    @pl.loop(2 * heads // step_cols, 3 * heads // step_cols)
    def _(step):
        cols = pl.ds(pl.multiple_of(step * step_cols, step_cols), step_cols)
        qkv[:, cols] = dot(normed[...], qkv_w[:, cols]).astype(BF)

    attend(qkv, attended, bias, heads)
    load_out.wait()

    def send_branch(step, k):
        cols = pl.ds(pl.multiple_of(step * step_cols, step_cols), step_cols)
        rows = pl.ds((k - 1) * tile, tile)
        peer = lax.rem(rank - k + ranks, ranks)
        return remote(
            send_part.at[rows, cols], recv_part.at[rows, cols], p_send.at[step, k], p_recv.at[step, k], "tensor", peer
        )

    @pl.loop(0, count)
    def _(step):
        cols = pl.ds(pl.multiple_of(step * step_cols, step_cols), step_cols)
        product = dot(attended[...], out_w[:, cols])
        part[:, cols] = product[:tile, :]
        send_part[:, cols] = product[tile:, :].astype(BF)
        for k in steps:
            send_branch(step, k).start()

    pass_on([4])

    @pl.loop(0, count)
    def _(step):
        cols = pl.ds(pl.multiple_of(step * step_cols, step_cols), step_cols)
        for k in steps:
            send_branch(step, k).wait_recv()
        total = hidden[pl.ds(0, tile), cols].astype(F32) + part[:, cols]
        for k in steps:
            total = total + recv_part[pl.ds((k - 1) * tile, tile), cols].astype(F32)
        middle[:, cols] = total
        sent[:, cols] = total.astype(BF)

    for copy in send_sent + send_cot[1]:
        copy.start()
    keep_sent = pltpu.make_async_copy(sent, sent_rows.at[pl.ds(0, tile), :], keep.at[0])
    keep_sent.start()
    pass_on([5, 6])
    finish([4, 5, 6])
    for copy in send_sent + send_cot[0] + send_cot[1]:
        copy.wait_recv()
    keep_sent.wait()
    for copy in send_hidden + send_sent + send_cot[0] + send_cot[1]:
        copy.wait_send()
    for index in range(7):
        send_weight(index, 1).wait_send()
        for flip in NEAR:
            send_weight(index, flip).wait_send()
            pass_weight(index, flip).wait_send()
    for flip in range(1, 8):
        send_gain(flip).wait_send()

    @pl.loop(0, count)
    def _(step):
        for k in steps:
            send_branch(step, k).wait_send()


def front(hidden_in, cot, gains, weights, cosine, sine, docs, ranks):
    tile, dim = hidden_in.shape
    tokens = tile * ranks
    width, heads = weights[0].shape
    units = weights[5].shape[1]
    dma = pltpu.SemaphoreType.DMA
    return pl.pallas_call(
        partial(front_kernel, ranks),
        out_shape=[
            shape((dim, 3 * heads), BF),
            shape((heads, dim), BF),
            shape((units, dim), BF),
            shape((dim, units), BF),
            shape((dim, units), BF),
            shape((tokens, dim), BF),
            shape((tokens, dim), BF),
            shape((tokens, dim), BF),
            shape((tokens, dim), BF),
            shape((tokens, 3 * heads), BF),
            shape((tokens, heads), BF),
            shape((tokens, 1), F32),
            shape((tile, dim), F32),
            shape((8, dim), F32),
        ],
        in_specs=[anyspace()] * 12 + [vmem()],
        out_specs=[anyspace()] * 8 + [vmem()] * 6,
        scratch_shapes=[
            pltpu.VMEM((tokens, dim), BF),
            pltpu.VMEM((dim, 3 * heads), BF),
            pltpu.VMEM((heads, dim), BF),
            pltpu.VMEM((tokens, 256), F32),
            pltpu.VMEM((tokens, 256), F32),
            pltpu.VMEM((tokens, tokens), F32),
            pltpu.VMEM((tile, dim), F32),
            pltpu.VMEM((tokens - tile, dim), BF),
            pltpu.VMEM((tokens - tile, dim), BF),
            pltpu.VMEM((tile, dim), BF),
        ]
        + [pltpu.VMEM(weight.shape, BF) for weight in weights]
        + [
            dma((7, 8)),
            dma((7, 8)),
            dma((4, ranks)),
            dma((4, ranks)),
            dma((dim // 256, ranks)),
            dma((dim // 256, ranks)),
            dma((8,)),
            dma((8,)),
            dma((10 + 2 * ranks,)),
            dma((9,)),
        ],
        compiler_params=pltpu.CompilerParams(vmem_limit_bytes=VMEM_LIMIT, collective_id=0, has_side_effects=True),
        cost_estimate=cost(2 * tokens * dim * 4 * heads * 3, 20e6),
        name="front",
    )(hidden_in, cot, gains, *weights, cosine, sine, docs)


def swap(values, flip):
    size = lax.axis_size("dp")
    return lax.ppermute(values, "dp", [(index, index ^ flip) for index in range(size)])


def shift(values, step):
    size = lax.axis_size("tensor")
    return lax.ppermute(values, "tensor", [(index, (index + step) % size) for index in range(size)])


def gather_rows(values):
    return [values] + [shift(values, step) for step in range(1, lax.axis_size("tensor"))]


def scatter_rows(parts):
    total = parts[0].astype(F32)
    for step in range(1, len(parts)):
        total = total + shift(parts[step], -step).astype(F32)
    return total


def gather_weight(values, axis):
    return [None], [lax.all_gather(values, "dp", axis=axis, tiled=True)]


def pick(values, core, width):
    tokens, dim = values.shape
    split = values.reshape(tokens, dim // (2 * width), 2, width)
    return lax.dynamic_index_in_dim(split, core, axis=2, keepdims=False).reshape(tokens, dim // 2)


def gather_grads(parts):
    total = parts[0]
    for slot in range(1, len(parts)):
        total = total + swap(parts[slot], 2 * slot).astype(F32)
    return total


def scatter_full(left, right, axis):
    full = dot_cols(left, right).astype(BF)
    return lax.psum_scatter(full, "dp", scatter_dimension=axis, tiled=True).astype(F32)


def scatter_gains(gains, paired):
    if not paired:
        return lax.psum_scatter(gains, ("dp", "tensor"), scatter_dimension=1, tiled=True)
    groups, ranks = lax.axis_size("dp"), lax.axis_size("tensor")
    group, rank = lax.axis_index("dp"), lax.axis_index("tensor")
    split = gains.reshape(gains.shape[0], groups, ranks, -1)
    take = lambda step: lax.dynamic_index_in_dim(split, (rank - step) % ranks, axis=2, keepdims=False)
    total = take(0)
    for step in range(1, ranks):
        total = total + shift(take(step), -step)
    pull = lambda flip: lax.dynamic_index_in_dim(total, group ^ flip, axis=1, keepdims=False)
    result = pull(0)
    for flip in range(1, groups):
        result = result + swap(pull(flip), flip)
    return result


def rotary(length):
    half_size = HEAD_DIM // 2
    frequency = ROPE_BASE ** (-jnp.arange(half_size, dtype=F32) / half_size)
    angles = jnp.arange(length).astype(F32)[:, None] * frequency[None, :]
    cosine, sine = jnp.cos(angles), jnp.sin(angles)
    cosine = jnp.tile(cosine, (1, 8))
    sine = jnp.tile(jnp.concatenate([-sine, sine], axis=1), (1, 4))
    return cosine, sine


def position_tables(doc_ids, ranks):
    length = doc_ids.shape[0]
    token_index = jnp.arange(length, dtype=jnp.int32)
    before = jnp.concatenate([doc_ids[:1] - 1, doc_ids[:-1]])
    doc_start = lax.cummax(jnp.where(doc_ids != before, token_index, 0), axis=0)
    order = (lax.axis_index("tensor") - jnp.arange(ranks)) % ranks
    last = token_index.reshape(ranks, -1)[order].reshape(length)
    first = doc_start.reshape(ranks, -1)[order].reshape(length)
    cosine, sine = (table.reshape(ranks, -1, 256)[order].reshape(length, 256) for table in rotary(length))
    return cosine, sine, first[:, None], last[:, None], last[None, :]


def rms_back(grad_rows_, values, gain):
    inverse = lax.rsqrt(jnp.mean(values * values, axis=-1, keepdims=True) + EPSILON)
    scaled = grad_rows_ * gain
    return inverse * (scaled - values * inverse * inverse * jnp.mean(scaled * values, axis=-1, keepdims=True))


def body(
    hidden_in,
    out_cotangent,
    doc_ids,
    attn_gain,
    query_weight,
    key_weight,
    value_weight,
    out_weight,
    mlp_gain,
    gate_weight,
    up_weight,
    down_weight,
):
    ranks, groups = lax.axis_size("tensor"), lax.axis_size("dp")
    paired = groups == 8
    core = lax.axis_index("dp") % 2
    width, heads = query_weight.shape
    dim = hidden_in.shape[1]

    tables = position_tables(doc_ids, ranks)
    input_local = hidden_in.astype(F32)
    if paired:
        pad = jnp.zeros((6, width), F32)
        own_gains = jnp.concatenate([attn_gain[None].astype(F32), mlp_gain[None].astype(F32), pad], axis=0)
        weights = (query_weight, key_weight, value_weight, out_weight, down_weight, gate_weight, up_weight)
        docs = doc_ids.reshape(ranks, -1)
        front_out = front(hidden_in, out_cotangent, own_gains, weights, *rotary(doc_ids.shape[0]), docs, ranks)
        qkv_full, out_full, down_full, gate_full, up_full, hidden_all, cot_full, sent_all = front_out[:8]
        normed, qkv, attended, inverses, middle, gains = front_out[8:]
        tags, qkv_pieces, out_pieces = [None], [qkv_full], [out_full]
        down_pieces, gate_pieces, up_pieces = [down_full], [gate_full], [up_full]
        hidden_rows, cot_rows, sent_rows = [hidden_all], [cot_full], [sent_all]
        attn_scale, mlp_scale = gains[:1], gains[1:2]
        sent = middle.astype(BF)
    else:
        hidden_rows = gather_rows(hidden_in)
        gains = lax.all_gather(jnp.stack([attn_gain, mlp_gain]), "dp", axis=1, tiled=True).astype(F32)
        attn_scale, mlp_scale = gains[:1], gains[1:]
        qkv_weight = jnp.concatenate([query_weight, key_weight, value_weight], axis=1)
        tags, qkv_pieces = gather_weight(qkv_weight, 0)
        tags, out_pieces = gather_weight(out_weight, 1)
        cot_rows = gather_rows(out_cotangent)
        tags, down_pieces = gather_weight(down_weight, 1)
        tags, gate_pieces = gather_weight(gate_weight, 0)
        tags, up_pieces = gather_weight(up_weight, 0)
        normed, qkv, attended, inverses, *branch_parts = attn_fwd(
            hidden_rows, attn_scale, tables, tags, width, qkv_pieces, out_pieces
        )
        middle = input_local + scatter_rows(branch_parts)
        sent = middle.astype(BF)
        sent_rows = gather_rows(sent)
        cot_full = jnp.concatenate(cot_rows, axis=0)
    normed_two, hidden, d_gate, d_up, mlp_gain_part, *two_parts = mlp(
        sent_rows, cot_rows, mlp_scale, tags, width, gate_pieces, up_pieces, down_pieces, ranks
    )
    grad_two_rows = scatter_rows(two_parts)
    grad_middle = out_cotangent.astype(F32) + rms_back(grad_two_rows, sent.astype(F32), mlp_scale)
    branch_rows = gather_rows(grad_middle.astype(BF))

    if paired:
        hidden_pair, d_gate_pair, d_up_pair = swap(hidden, 1), swap(d_gate, 1), swap(d_up, 1)
        cot_pair = swap(pick(cot_full, 1 - core, width), 1)
        two_pair = swap(pick(normed_two, 1 - core, width), 1)
        down_grad = gather_grads(grad_cols(hidden, hidden_pair, cot_full, cot_pair, width))
        gate_grad = gather_grads(grad_rows(normed_two, two_pair, d_gate, d_gate_pair, width))
        up_grad = gather_grads(grad_rows(normed_two, two_pair, d_up, d_up_pair, width))
    else:
        down_grad = scatter_full(hidden, cot_full, 1)
        gate_grad = scatter_full(normed_two, d_gate, 0)
        up_grad = scatter_full(normed_two, d_up, 0)
    mlp_rows = scatter_rows(mlp_out(hidden, ranks, dim, tags, width, down_pieces))
    layer_out = (middle + mlp_rows).astype(BF)

    branch_full, d_qkv, attn_gain_part, *one_parts = attn_bwd(
        branch_rows, hidden_rows, qkv, inverses, tables, tags, width, qkv_pieces, out_pieces, ranks
    )
    if paired:
        d_qkv_pair, attended_pair = swap(d_qkv, 1), swap(attended, 1)
        normed_pair = swap(pick(normed, 1 - core, width), 1)
        branch_pair = swap(pick(branch_full, 1 - core, width), 1)
        out_proj_grad = gather_grads(grad_cols(attended, attended_pair, branch_full, branch_pair, width))
        qkv_grad = gather_grads(grad_rows(normed, normed_pair, d_qkv, d_qkv_pair, width))
    else:
        out_proj_grad = scatter_full(attended, branch_full, 1)
        qkv_grad = scatter_full(normed, d_qkv, 0)
    grad_one_rows = scatter_rows(one_parts)
    input_grad = grad_middle + rms_back(grad_one_rows, input_local, attn_scale)
    gain_grads = scatter_gains(jnp.concatenate([attn_gain_part, mlp_gain_part], axis=0), paired)
    return (
        layer_out,
        input_grad,
        gain_grads[0],
        qkv_grad[:, :heads],
        qkv_grad[:, heads : 2 * heads],
        qkv_grad[:, 2 * heads :],
        out_proj_grad,
        gain_grads[1],
        gate_grad,
        up_grad,
        down_grad,
    )


def solution(mesh):
    return jax.shard_map(
        body,
        mesh=mesh,
        in_specs=(
            P(("dp", "tensor"), None),
            P(("dp", "tensor"), None),
            P("dp"),
            P("dp"),
            P("dp", "tensor"),
            P("dp", "tensor"),
            P("dp", "tensor"),
            P("tensor", "dp"),
            P("dp"),
            P("dp", "tensor"),
            P("dp", "tensor"),
            P("tensor", "dp"),
        ),
        out_specs=(
            P(("dp", "tensor"), None),
            P(("dp", "tensor"), None),
            P(("dp", "tensor")),
            P("dp", "tensor"),
            P("dp", "tensor"),
            P("dp", "tensor"),
            P("tensor", "dp"),
            P(("dp", "tensor")),
            P("dp", "tensor"),
            P("dp", "tensor"),
            P("tensor", "dp"),
        ),
        check_vma=False,
    )
```

```python
from functools import partial

import jax
import jax.numpy as jnp
from jax import lax
from jax.experimental import pallas as pl
from jax.experimental.pallas import tpu as pltpu
from jax.sharding import PartitionSpec as P

HEAD_DIM = 64
EPSILON = 1e-05
ROPE_BASE = 130000.0
NEGATIVE = -1e30
VMEM_LIMIT = 63 * 1024 * 1024
BF = jnp.bfloat16
F32 = jnp.float32


def dot(left, right):
    return jnp.dot(left, right, preferred_element_type=F32)


def dot_rows(left, right):
    return lax.dot_general(left, right, (((1,), (1,)), ((), ())), preferred_element_type=F32)


def dot_cols(left, right):
    return lax.dot_general(left, right, (((0,), (0,)), ((), ())), preferred_element_type=F32)


def vmem():
    return pl.BlockSpec(memory_space=pltpu.VMEM)


def anyspace():
    return pl.BlockSpec(memory_space=pl.ANY)


def params():
    return pltpu.CompilerParams(vmem_limit_bytes=VMEM_LIMIT)


def cost(flops, nbytes):
    return pl.CostEstimate(flops=int(flops), bytes_accessed=int(nbytes), transcendentals=0)


def shape(dims, kind):
    return jax.ShapeDtypeStruct(dims, kind)


def place_copies(tags, pieces, target, sem, axis, width):
    own = lax.axis_index("dp")
    copies = []
    for slot, (tag, piece) in enumerate(zip(tags, pieces)):
        if tag is None:
            where = target
        else:
            start = pl.multiple_of((own ^ tag) * width, width)
            where = target.at[pl.ds(start, width), :] if axis == 0 else target.at[:, pl.ds(start, width)]
        copies.append(pltpu.make_async_copy(piece, where, sem.at[slot]))
    return copies


def row_copies(pieces, target, sem):
    copies = []
    for slot, piece in enumerate(pieces):
        rows = piece.shape[0]
        copies.append(pltpu.make_async_copy(piece, target.at[pl.ds(slot * rows, rows), :], sem.at[slot]))
    return copies


def start_all(copies):
    for copy in copies:
        copy.start()


def wait_all(copies):
    for copy in copies:
        copy.wait()


def turn(values, cosine, sine):
    width = values.shape[1]
    lane = lax.broadcasted_iota(jnp.int32, values.shape, 1)
    partner = jnp.where(
        lax.rem(lane, HEAD_DIM) < HEAD_DIM // 2,
        pltpu.roll(values, width - HEAD_DIM // 2, 1),
        pltpu.roll(values, HEAD_DIM // 2, 1),
    )
    return values * cosine + partner * sine


def norm_rows(source, target, inverses, gain, tile):
    @pl.loop(0, source.shape[0] // tile)
    def _(step):
        rows = pl.ds(pl.multiple_of(step * tile, tile), tile)
        values = source[rows, :].astype(F32)
        inverse = lax.rsqrt(jnp.mean(values * values, axis=-1, keepdims=True) + EPSILON)
        inverses[rows, :] = inverse
        target[rows, :] = (values * inverse * gain[...]).astype(BF)


def fill_bias(bias, first, last, key_index):
    keys = key_index[...]
    bias[...] = jnp.where((keys >= first[...]) & (keys <= last[...]), 0.0, NEGATIVE)


def head_lanes(width, half):
    lane = lax.broadcasted_iota(jnp.int32, (1, width), 1)
    return (lax.div(lane, HEAD_DIM) == half).astype(F32)


def probabilities(query, key, bias):
    scores = dot_rows(query, key) + bias
    weights = jnp.exp(scores - jnp.max(scores, axis=-1, keepdims=True))
    return weights * (1.0 / jnp.sum(weights, axis=-1, keepdims=True))


def attend(qkv, attended, bias, heads):
    @pl.loop(0, heads // 128)
    def _(pair):
        base = pl.multiple_of(pair * 128, 128)
        query = qkv[:, pl.ds(base, 128)]
        key = qkv[:, pl.ds(heads + base, 128)]
        value = qkv[:, pl.ds(2 * heads + base, 128)]
        total = None
        for half in range(2):
            lanes = head_lanes(128, half).astype(BF)
            probs = probabilities(query * (lanes * HEAD_DIM ** (-0.5)), key, bias[...])
            term = dot(probs.astype(BF), value * lanes)
            total = term if total is None else total + term
        attended[:, pl.ds(base, 128)] = total.astype(BF)


def attn_fwd_kernel(tags, width, nrow, *refs):
    npiece = len(tags)
    rows_in = refs[:nrow]
    gain, cosine, sine, first, last, key_index = refs[nrow : nrow + 6]
    rest = refs[nrow + 6 :]
    qkv_in, out_in = rest[:npiece], rest[npiece : 2 * npiece]
    rest = rest[2 * npiece :]
    normed, qkv, attended, inverses = rest[:4]
    parts = rest[4 : 4 + nrow]
    hidden, qkv_w, out_w, bias, sem_rows, sem_qkv, sem_out = rest[4 + nrow :]
    load_rows = row_copies(rows_in, hidden, sem_rows)
    load_qkv = place_copies(tags, qkv_in, qkv_w, sem_qkv, 0, width)
    load_out = place_copies(tags, out_in, out_w, sem_out, 1, width)
    start_all(load_rows + load_qkv + load_out)
    fill_bias(bias, first, last, key_index)
    wait_all(load_rows)
    norm_rows(hidden, normed, inverses, gain, 64)
    wait_all(load_qkv)
    heads = attended.shape[1]
    step_cols = 256

    @pl.loop(0, 2 * heads // step_cols)
    def _(step):
        cols = pl.ds(pl.multiple_of(step * step_cols, step_cols), step_cols)
        qkv[:, cols] = turn(dot(normed[...], qkv_w[:, cols]), cosine[...], sine[...]).astype(BF)

    @pl.loop(2 * heads // step_cols, 3 * heads // step_cols)
    def _(step):
        cols = pl.ds(pl.multiple_of(step * step_cols, step_cols), step_cols)
        qkv[:, cols] = dot(normed[...], qkv_w[:, cols]).astype(BF)

    attend(qkv, attended, bias, heads)
    wait_all(load_out)
    tile = parts[0].shape[0]

    @pl.loop(0, out_w.shape[1] // step_cols)
    def _(step):
        cols = pl.ds(pl.multiple_of(step * step_cols, step_cols), step_cols)
        product = dot(attended[...], out_w[:, cols])
        for slot, part in enumerate(parts):
            part[:, cols] = product[slot * tile : (slot + 1) * tile, :].astype(part.dtype)


def attn_fwd(rows, gain, tables, tags, width, qkv_pieces, out_pieces):
    nrow, (tile, dim) = len(rows), rows[0].shape
    tokens = nrow * tile
    heads = out_pieces[0].shape[0]
    npiece = len(tags)
    return pl.pallas_call(
        partial(attn_fwd_kernel, tags, width, nrow),
        out_shape=[
            shape((tokens, dim), BF),
            shape((tokens, 3 * heads), BF),
            shape((tokens, heads), BF),
            shape((tokens, 1), F32),
        ]
        + [shape((tile, dim), F32 if slot == 0 else BF) for slot in range(nrow)],
        in_specs=[anyspace()] * nrow + [vmem()] * 6 + [anyspace()] * (2 * npiece),
        out_specs=[vmem()] * (4 + nrow),
        scratch_shapes=[
            pltpu.VMEM((tokens, dim), BF),
            pltpu.VMEM((dim, 3 * heads), BF),
            pltpu.VMEM((heads, dim), BF),
            pltpu.VMEM((tokens, tokens), F32),
            pltpu.SemaphoreType.DMA((nrow,)),
            pltpu.SemaphoreType.DMA((npiece,)),
            pltpu.SemaphoreType.DMA((npiece,)),
        ],
        compiler_params=params(),
        cost_estimate=cost(2 * tokens * dim * 4 * heads * 3, 20e6),
        name="attn_fwd",
    )(*rows, gain, *tables, *qkv_pieces, *out_pieces)


def attend_back(qkv, d_attended, d_qkv, bias, cosine, sine, heads):
    score_scale = HEAD_DIM ** (-0.5)

    @pl.loop(0, heads // 128)
    def _(pair):
        base = pl.multiple_of(pair * 128, 128)
        query = qkv[:, pl.ds(base, 128)]
        key = qkv[:, pl.ds(heads + base, 128)]
        value = qkv[:, pl.ds(2 * heads + base, 128)]
        grad = d_attended[:, pl.ds(base, 128)]
        sums = [0.0, 0.0, 0.0]
        for half in range(2):
            lanes = head_lanes(128, half).astype(BF)
            own_query = query * (lanes * score_scale)
            own_grad = grad * lanes
            probs = probabilities(own_query, key, bias[...])
            d_value = dot_cols(probs.astype(BF), own_grad)
            d_probs = dot_rows(own_grad, value)
            delta = jnp.sum(probs * d_probs, axis=-1, keepdims=True)
            d_scores = (probs * (d_probs - delta)).astype(BF)
            d_query = dot(d_scores, key * lanes) * score_scale
            d_key = dot_cols(d_scores, own_query)
            sums = [sums[0] + d_query, sums[1] + d_key, sums[2] + d_value]
        back = -sine[:, :128]
        d_qkv[:, pl.ds(base, 128)] = turn(sums[0], cosine[:, :128], back).astype(BF)
        d_qkv[:, pl.ds(heads + base, 128)] = turn(sums[1], cosine[:, :128], back).astype(BF)
        d_qkv[:, pl.ds(2 * heads + base, 128)] = sums[2].astype(BF)


def attn_bwd_kernel(tags, width, nrow, npart, *refs):
    npiece = len(tags)
    nhid, nrow = nrow[1], nrow[0]
    rows_in, hidden_in = refs[:nrow], refs[nrow : nrow + nhid]
    refs = refs[nrow + nhid :]
    qkv, inverses, cosine, sine, first, last, key_index = refs[:7]
    rest = refs[7:]
    qkv_in, out_in = rest[:npiece], rest[npiece : 2 * npiece]
    rest = rest[2 * npiece :]
    branch, d_qkv, gain_grad = rest[:3]
    parts = rest[3 : 3 + npart]
    hidden, d_attended, qkv_w, out_w, bias, sem_rows, sem_x, sem_qkv, sem_out = rest[3 + npart :]
    load_rows = row_copies(rows_in, branch, sem_rows)
    load_x = row_copies(hidden_in, hidden, sem_x)
    load_out = place_copies(tags, out_in, out_w, sem_out, 1, width)
    load_qkv = place_copies(tags, qkv_in, qkv_w, sem_qkv, 0, width)
    start_all(load_rows + load_out + load_qkv + load_x)
    fill_bias(bias, first, last, key_index)
    wait_all(load_rows)
    wait_all(load_out)
    heads = out_w.shape[0]
    step_cols = 256

    @pl.loop(0, heads // step_cols)
    def _(step):
        cols = pl.ds(pl.multiple_of(step * step_cols, step_cols), step_cols)
        d_attended[:, cols] = dot_rows(branch[...], out_w[cols, :]).astype(BF)

    attend_back(qkv, d_attended, d_qkv, bias, cosine, sine, heads)
    wait_all(load_qkv)
    wait_all(load_x)
    tile = parts[0].shape[0]

    @pl.loop(0, qkv_w.shape[0] // step_cols)
    def _(step):
        cols = pl.ds(pl.multiple_of(step * step_cols, step_cols), step_cols)
        product = dot_rows(d_qkv[...], qkv_w[cols, :])
        gain_grad[:, cols] = jnp.sum(product * (hidden[:, cols].astype(F32) * inverses[...]), axis=0, keepdims=True)
        for slot, part in enumerate(parts):
            part[:, cols] = product[slot * tile : (slot + 1) * tile, :].astype(part.dtype)


def attn_bwd(rows, hidden, qkv, inverses, tables, tags, width, qkv_pieces, out_pieces, npart):
    nrow, nhid, dim = len(rows), len(hidden), rows[0].shape[1]
    tokens = qkv.shape[0]
    tile = tokens // npart
    heads = out_pieces[0].shape[0]
    npiece = len(tags)
    return pl.pallas_call(
        partial(attn_bwd_kernel, tags, width, (nrow, nhid), npart),
        out_shape=[shape((tokens, dim), BF), shape((tokens, 3 * heads), BF), shape((1, dim), F32)]
        + [shape((tile, dim), F32 if slot == 0 else BF) for slot in range(npart)],
        in_specs=[anyspace()] * (nrow + nhid) + [vmem()] * 7 + [anyspace()] * (2 * npiece),
        out_specs=[vmem()] * (3 + npart),
        scratch_shapes=[
            pltpu.VMEM((tokens, dim), BF),
            pltpu.VMEM((tokens, heads), BF),
            pltpu.VMEM((dim, 3 * heads), BF),
            pltpu.VMEM((heads, dim), BF),
            pltpu.VMEM((tokens, tokens), F32),
            pltpu.SemaphoreType.DMA((nrow,)),
            pltpu.SemaphoreType.DMA((nhid,)),
            pltpu.SemaphoreType.DMA((npiece,)),
            pltpu.SemaphoreType.DMA((npiece,)),
        ],
        compiler_params=params(),
        cost_estimate=cost(2 * tokens * dim * 4 * heads * 6, 30e6),
        name="attn_bwd",
    )(*rows, *hidden, qkv, inverses, *tables, *qkv_pieces, *out_pieces)


def mlp_kernel(tags, width, nrow, npart, *refs):
    npiece = len(tags)
    sent_in, cot_in = refs[:nrow], refs[nrow : 2 * nrow]
    gain = refs[2 * nrow]
    rest = refs[2 * nrow + 1 :]
    gate_in, up_in, down_in = rest[:npiece], rest[npiece : 2 * npiece], rest[2 * npiece : 3 * npiece]
    rest = rest[3 * npiece :]
    normed, hidden, d_gate, d_up, gain_grad = rest[:5]
    parts = rest[5 : 5 + npart]
    sent, cot, inverses, gate_w, up_w, down_w, sem_sent, sem_cot, sem_gate, sem_up, sem_down = rest[5 + npart :]
    load_sent = row_copies(sent_in, sent, sem_sent)
    load_cot = row_copies(cot_in, cot, sem_cot)
    load_gate = place_copies(tags, gate_in, gate_w, sem_gate, 0, width)
    load_up = place_copies(tags, up_in, up_w, sem_up, 0, width)
    load_down = place_copies(tags, down_in, down_w, sem_down, 1, width)
    start_all(load_sent + load_cot + load_gate + load_up + load_down)
    wait_all(load_sent)
    norm_rows(sent, normed, inverses, gain, 64)
    wait_all(load_cot)
    wait_all(load_gate)
    wait_all(load_up)
    wait_all(load_down)
    step_cols = 256

    @pl.loop(0, gate_w.shape[1] // step_cols)
    def _(step):
        cols = pl.ds(pl.multiple_of(step * step_cols, step_cols), step_cols)
        gate = dot(normed[...], gate_w[:, cols])
        up = dot(normed[...], up_w[:, cols])
        d_hidden = dot_rows(cot[...], down_w[cols, :])
        s = jax.nn.sigmoid(gate)
        activated = gate * s
        hidden[:, cols] = (activated * up).astype(BF)
        d_gate[:, cols] = (d_hidden * up * (s + activated * (1.0 - s))).astype(BF)
        d_up[:, cols] = (d_hidden * activated).astype(BF)

    tile = parts[0].shape[0]

    @pl.loop(0, gate_w.shape[0] // step_cols)
    def _(step):
        cols = pl.ds(pl.multiple_of(step * step_cols, step_cols), step_cols)
        product = dot_rows(d_gate[...], gate_w[cols, :]) + dot_rows(d_up[...], up_w[cols, :])
        gain_grad[:, cols] = jnp.sum(product * (sent[:, cols].astype(F32) * inverses[...]), axis=0, keepdims=True)
        for slot, part in enumerate(parts):
            part[:, cols] = product[slot * tile : (slot + 1) * tile, :].astype(part.dtype)


def mlp(sent, cot, gain, tags, width, gate_pieces, up_pieces, down_pieces, npart):
    nrow, dim = len(sent), sent[0].shape[1]
    tokens = nrow * sent[0].shape[0]
    tile = tokens // npart
    units = gate_pieces[0].shape[1]
    npiece = len(tags)
    return pl.pallas_call(
        partial(mlp_kernel, tags, width, nrow, npart),
        out_shape=[shape((tokens, dim), BF)]
        + [shape((tokens, units), BF)] * 3
        + [shape((1, dim), F32)]
        + [shape((tile, dim), F32 if slot == 0 else BF) for slot in range(npart)],
        in_specs=[anyspace()] * (2 * nrow) + [vmem()] + [anyspace()] * (3 * npiece),
        out_specs=[vmem()] * (5 + npart),
        scratch_shapes=[
            pltpu.VMEM((tokens, dim), BF),
            pltpu.VMEM((tokens, dim), BF),
            pltpu.VMEM((tokens, 1), F32),
            pltpu.VMEM((dim, units), BF),
            pltpu.VMEM((dim, units), BF),
            pltpu.VMEM((units, dim), BF),
            pltpu.SemaphoreType.DMA((nrow,)),
            pltpu.SemaphoreType.DMA((nrow,)),
            pltpu.SemaphoreType.DMA((npiece,)),
            pltpu.SemaphoreType.DMA((npiece,)),
            pltpu.SemaphoreType.DMA((npiece,)),
        ],
        compiler_params=params(),
        cost_estimate=cost(2 * tokens * dim * units * 5, 40e6),
        name="mlp",
    )(*sent, *cot, gain, *gate_pieces, *up_pieces, *down_pieces)


def mlp_out_kernel(tags, width, *refs):
    npiece = len(tags)
    hidden, down_in = refs[0], refs[1 : 1 + npiece]
    *parts, down_w, sem_down = refs[1 + npiece :]
    load_down = place_copies(tags, down_in, down_w, sem_down, 1, width)
    start_all(load_down)
    wait_all(load_down)
    tile, step_cols = parts[0].shape[0], 256

    @pl.loop(0, down_w.shape[1] // step_cols)
    def _(step):
        cols = pl.ds(pl.multiple_of(step * step_cols, step_cols), step_cols)
        product = dot(hidden[...], down_w[:, cols])
        for slot, part in enumerate(parts):
            part[:, cols] = product[slot * tile : (slot + 1) * tile, :].astype(part.dtype)


def mlp_out(hidden, nrow, dim, tags, width, down_pieces):
    tokens, units = hidden.shape
    tile, npiece = tokens // nrow, len(tags)
    return pl.pallas_call(
        partial(mlp_out_kernel, tags, width),
        out_shape=[shape((tile, dim), F32 if slot == 0 else BF) for slot in range(nrow)],
        in_specs=[vmem()] + [anyspace()] * npiece,
        out_specs=[vmem()] * nrow,
        scratch_shapes=[pltpu.VMEM((units, dim), BF), pltpu.SemaphoreType.DMA((npiece,))],
        compiler_params=params(),
        cost_estimate=cost(2 * tokens * dim * units, 14e6),
        name="mlp_out",
    )(hidden, *down_pieces)


def slice_of(slot, width, own):
    index = lax.axis_index("dp")
    owner = index ^ (2 * slot)
    return pl.ds(pl.multiple_of((owner if own else lax.div(owner, 2)) * width, width), width)


MESH = pl.DeviceIdType.MESH
NEAR = (2, 4, 6)


def remote(source, target, send_sem, recv_sem, axis, peer):
    return pltpu.make_async_remote_copy(
        src_ref=source,
        dst_ref=target,
        send_sem=send_sem,
        recv_sem=recv_sem,
        device_id={axis: peer},
        device_id_type=MESH,
    )


def meet(ranks):
    own, rank = lax.axis_index("dp"), lax.axis_index("tensor")
    barrier = pltpu.get_barrier_semaphore()
    for flip in range(1, 8):
        pl.semaphore_signal(barrier, inc=1, device_id={"dp": own ^ flip}, device_id_type=MESH)
    for step in range(1, ranks):
        pl.semaphore_signal(barrier, inc=1, device_id={"tensor": lax.rem(rank + step, ranks)}, device_id_type=MESH)
    pl.semaphore_wait(barrier, ranks + 6)


def at_cols(ref, index, width):
    return ref.at[:, pl.ds(pl.multiple_of(index * width, width), width)]


def at_rows(ref, index, width):
    return ref.at[pl.ds(pl.multiple_of(index * width, width), width), :]


def fill_mask(bias, docs, ranks):
    rank = lax.axis_index("tensor")
    tile = docs.shape[1]
    blocks = [lax.rem(rank - slot + ranks, ranks) for slot in range(ranks)]
    own_docs = [jnp.broadcast_to(docs[pl.ds(block, 1), :].astype(F32), (tile, tile)) for block in blocks]
    turned = [jnp.transpose(values) for values in own_docs]
    row = lax.broadcasted_iota(jnp.int32, (tile, tile), 0)
    lane = lax.broadcasted_iota(jnp.int32, (tile, tile), 1)
    for q in range(ranks):
        for k in range(ranks):
            same = turned[q] == own_docs[k]
            before = row + blocks[q] * tile >= lane + blocks[k] * tile
            bias[q * tile : (q + 1) * tile, k * tile : (k + 1) * tile] = jnp.where(same & before, 0.0, NEGATIVE)


def front_kernel(ranks, *refs):
    hidden_in, cot_in, gains_in = refs[:3]
    weights_in = refs[3:10]
    cosine_in, sine_in, docs = refs[10:13]
    qkv_full, out_full, down_full, gate_full, up_full, hidden_rows, cot_rows, sent_rows = refs[13:21]
    normed, qkv, attended, inverses, middle, gains = refs[21:27]
    hidden, qkv_w, out_w, cosine, sine, bias, part, send_part, recv_part, sent = refs[27:37]
    stage = refs[37:44]
    (w_send, w_recv, z_send, z_recv, p_send, p_recv, g_send, g_recv, load, keep) = refs[44:]
    own, rank = lax.axis_index("dp"), lax.axis_index("tensor")
    tile, dim = hidden_in.shape
    width = weights_in[0].shape[0]
    heads = weights_in[0].shape[1]
    step_cols = 256
    count = dim // step_cols

    def slot_of(index, owner):
        if index < 3:
            rows = pl.ds(pl.multiple_of(owner * width, width), width)
            return qkv_full.at[rows, pl.ds(index * heads, heads)]
        if index == 3:
            return at_cols(out_full, owner, width)
        if index == 4:
            return at_cols(down_full, owner, width)
        return at_rows((gate_full, up_full)[index - 5], owner, width)

    def send_weight(index, flip):
        return remote(
            weights_in[index], slot_of(index, own), w_send.at[index, flip], w_recv.at[index, flip], "dp", own ^ flip
        )

    def pass_weight(index, flip):
        place = slot_of(index, own ^ flip)
        return remote(place, place, w_send.at[index, flip + 1], w_recv.at[index, flip + 1], "dp", own ^ 1)

    def pass_on(indices):
        for index in indices:
            for flip in NEAR:
                send_weight(index, flip).wait_recv()
                pass_weight(index, flip).start()

    def finish(indices):
        for index in indices:
            send_weight(index, 1).wait_recv()
            for flip in NEAR:
                pass_weight(index, flip).wait_recv()

    def send_gain(flip):
        return remote(gains_in, at_cols(gains, own, width), g_send.at[flip], g_recv.at[flip], "dp", own ^ flip)

    def send_z(kind, source, target, step, start, size):
        place = target.at[pl.ds(step * tile + start, size), :]
        peer = lax.rem(rank + step, ranks)
        return remote(
            source.at[pl.ds(start, size), :], place, z_send.at[kind, step], z_recv.at[kind, step], "tensor", peer
        )

    half = tile // 2
    steps = list(range(1, ranks))
    send_hidden = [send_z(0, hidden_in, hidden_rows, step, 0, tile) for step in steps]
    send_cot = [[send_z(1 + h, cot_in, cot_rows, step, h * half, half) for step in steps] for h in range(2)]
    send_sent = [send_z(3, sent, sent_rows, step, 0, tile) for step in steps]

    meet(ranks)
    for copy in send_hidden:
        copy.start()
    for flip in range(1, 8):
        send_gain(flip).start()
    for index in range(4):
        for flip in NEAR + (1,):
            send_weight(index, flip).start()
    for copy in send_cot[0]:
        copy.start()
    for index in range(4, 7):
        for flip in NEAR + (1,):
            send_weight(index, flip).start()

    stage_in = [pltpu.make_async_copy(weights_in[index], stage[index], load.at[index]) for index in range(7)]
    stage_out = [pltpu.make_async_copy(stage[index], slot_of(index, own), keep.at[index]) for index in range(7)]
    own_hidden = pltpu.make_async_copy(hidden_in, hidden.at[pl.ds(0, tile), :], load.at[7])
    own_cot = pltpu.make_async_copy(cot_in, sent, load.at[8])
    own_gain = pltpu.make_async_copy(gains_in, at_cols(gains, own, width), load.at[9])
    tables = []
    for slot in range(ranks):
        block = lax.rem(rank - slot + ranks, ranks)
        for which, (source, target) in enumerate(((cosine_in, cosine), (sine_in, sine))):
            tables.append(
                pltpu.make_async_copy(
                    at_rows(source, block, tile), at_rows(target, slot, tile), load.at[10 + 2 * slot + which]
                )
            )
    start_all(stage_in + [own_hidden, own_cot, own_gain] + tables)
    wait_all(stage_in)
    start_all(stage_out)
    wait_all([own_hidden, own_cot, own_gain])
    keep_hidden = pltpu.make_async_copy(hidden.at[pl.ds(0, tile), :], hidden_rows.at[pl.ds(0, tile), :], keep.at[7])
    keep_cot = pltpu.make_async_copy(sent, cot_rows.at[pl.ds(0, tile), :], keep.at[8])
    start_all([keep_hidden, keep_cot])
    fill_mask(bias, docs, ranks)
    wait_all(tables + stage_out + [keep_hidden, keep_cot])

    pass_on(range(4))
    for flip in range(1, 8):
        send_gain(flip).wait_recv()
    for copy in send_hidden:
        copy.wait_recv()
    load_rows = pltpu.make_async_copy(
        hidden_rows.at[pl.ds(tile, (ranks - 1) * tile), :], hidden.at[pl.ds(tile, (ranks - 1) * tile), :], load.at[0]
    )
    load_rows.start()
    load_rows.wait()
    norm_rows(hidden, normed, inverses, gains.at[pl.ds(0, 1), :], 64)
    finish(range(4))
    load_qkv = pltpu.make_async_copy(qkv_full, qkv_w, load.at[1])
    load_out = pltpu.make_async_copy(out_full, out_w, load.at[2])
    load_qkv.start()
    load_out.start()
    load_qkv.wait()

    @pl.loop(0, 2 * heads // step_cols)
    def _(step):
        cols = pl.ds(pl.multiple_of(step * step_cols, step_cols), step_cols)
        qkv[:, cols] = turn(dot(normed[...], qkv_w[:, cols]), cosine[...], sine[...]).astype(BF)

    @pl.loop(2 * heads // step_cols, 3 * heads // step_cols)
    def _(step):
        cols = pl.ds(pl.multiple_of(step * step_cols, step_cols), step_cols)
        qkv[:, cols] = dot(normed[...], qkv_w[:, cols]).astype(BF)

    attend(qkv, attended, bias, heads)
    load_out.wait()

    def send_branch(step, k):
        cols = pl.ds(pl.multiple_of(step * step_cols, step_cols), step_cols)
        rows = pl.ds((k - 1) * tile, tile)
        peer = lax.rem(rank - k + ranks, ranks)
        return remote(
            send_part.at[rows, cols], recv_part.at[rows, cols], p_send.at[step, k], p_recv.at[step, k], "tensor", peer
        )

    @pl.loop(0, count)
    def _(step):
        cols = pl.ds(pl.multiple_of(step * step_cols, step_cols), step_cols)
        product = dot(attended[...], out_w[:, cols])
        part[:, cols] = product[:tile, :]
        send_part[:, cols] = product[tile:, :].astype(BF)
        for k in steps:
            send_branch(step, k).start()

    pass_on([4])

    @pl.loop(0, count)
    def _(step):
        cols = pl.ds(pl.multiple_of(step * step_cols, step_cols), step_cols)
        for k in steps:
            send_branch(step, k).wait_recv()
        total = hidden[pl.ds(0, tile), cols].astype(F32) + part[:, cols]
        for k in steps:
            total = total + recv_part[pl.ds((k - 1) * tile, tile), cols].astype(F32)
        middle[:, cols] = total
        sent[:, cols] = total.astype(BF)

    for copy in send_sent + send_cot[1]:
        copy.start()
    keep_sent = pltpu.make_async_copy(sent, sent_rows.at[pl.ds(0, tile), :], keep.at[0])
    keep_sent.start()
    pass_on([5, 6])
    finish([4, 5, 6])
    for copy in send_sent + send_cot[0] + send_cot[1]:
        copy.wait_recv()
    keep_sent.wait()
    for copy in send_hidden + send_sent + send_cot[0] + send_cot[1]:
        copy.wait_send()
    for index in range(7):
        send_weight(index, 1).wait_send()
        for flip in NEAR:
            send_weight(index, flip).wait_send()
            pass_weight(index, flip).wait_send()
    for flip in range(1, 8):
        send_gain(flip).wait_send()

    @pl.loop(0, count)
    def _(step):
        for k in steps:
            send_branch(step, k).wait_send()


def front(hidden_in, cot, gains, weights, cosine, sine, docs, ranks):
    tile, dim = hidden_in.shape
    tokens = tile * ranks
    width, heads = weights[0].shape
    units = weights[5].shape[1]
    dma = pltpu.SemaphoreType.DMA
    return pl.pallas_call(
        partial(front_kernel, ranks),
        out_shape=[
            shape((dim, 3 * heads), BF),
            shape((heads, dim), BF),
            shape((units, dim), BF),
            shape((dim, units), BF),
            shape((dim, units), BF),
            shape((tokens, dim), BF),
            shape((tokens, dim), BF),
            shape((tokens, dim), BF),
            shape((tokens, dim), BF),
            shape((tokens, 3 * heads), BF),
            shape((tokens, heads), BF),
            shape((tokens, 1), F32),
            shape((tile, dim), F32),
            shape((8, dim), F32),
        ],
        in_specs=[anyspace()] * 12 + [vmem()],
        out_specs=[anyspace()] * 8 + [vmem()] * 6,
        scratch_shapes=[
            pltpu.VMEM((tokens, dim), BF),
            pltpu.VMEM((dim, 3 * heads), BF),
            pltpu.VMEM((heads, dim), BF),
            pltpu.VMEM((tokens, 256), F32),
            pltpu.VMEM((tokens, 256), F32),
            pltpu.VMEM((tokens, tokens), F32),
            pltpu.VMEM((tile, dim), F32),
            pltpu.VMEM((tokens - tile, dim), BF),
            pltpu.VMEM((tokens - tile, dim), BF),
            pltpu.VMEM((tile, dim), BF),
        ]
        + [pltpu.VMEM(weight.shape, BF) for weight in weights]
        + [
            dma((7, 8)),
            dma((7, 8)),
            dma((4, ranks)),
            dma((4, ranks)),
            dma((dim // 256, ranks)),
            dma((dim // 256, ranks)),
            dma((8,)),
            dma((8,)),
            dma((10 + 2 * ranks,)),
            dma((9,)),
        ],
        compiler_params=pltpu.CompilerParams(vmem_limit_bytes=VMEM_LIMIT, collective_id=0, has_side_effects=True),
        cost_estimate=cost(2 * tokens * dim * 4 * heads * 3, 20e6),
        name="front",
    )(hidden_in, cot, gains, *weights, cosine, sine, docs)


def back_kernel(ranks, *refs):
    (
        sent_in,
        cot_in,
        hidden_in,
        qkv_full,
        out_full,
        down_full,
        gate_full,
        up_full,
        normed_in,
        qkv_in,
        attended_in,
        middle_in,
        cosine_in,
        sine_in,
        docs,
        inverses_one,
        gains,
    ) = refs[:17]
    gate_parts, up_parts, down_parts, qkv_parts, out_parts = refs[17:22]
    pair_ff = refs[22:25]
    pair_two, pair_cot, pair_qkv, pair_attended, pair_normed, pair_branch = refs[25:31]
    two_recv, mlp_recv, one_recv, branch_rows = refs[31:35]
    layer_out, input_grad, gain_total = refs[35:38]
    gate_w, up_w, down_w, sent, cot, normed, hidden, d_gate, d_up = refs[38:47]
    two_half, cot_half, buffer_a, buffer_b, buffer_c, out_w = refs[47:53]
    qkv, d_qkv, attended, d_attended, bias, cosine, sine, inverses = refs[53:61]
    own_mlp, grad_middle, send_part, recv_part, gain_part, gain_recv, gain_z = refs[61:68]
    f_send, f_recv, h_send, h_recv, z_send, z_recv, b_send, b_recv, w_send, w_recv, g_send, g_recv, load, keep = refs[68:]

    own, rank = lax.axis_index("dp"), lax.axis_index("tensor")
    core = lax.rem(own, 2)
    tokens, dim = sent.shape
    units = gate_w.shape[1]
    tile = tokens // ranks
    heads = attended.shape[1]
    width = out_parts.shape[1] // 4
    half = dim // (2 * width)
    step_cols = 256
    count = dim // step_cols
    steps = list(range(1, ranks))
    rest = tokens - tile
    branch, send_mlp = sent.at[pl.ds(0, tile), :], sent.at[pl.ds(tile, rest), :]

    def tile_cols(step, size=step_cols):
        return pl.ds(pl.multiple_of(step * size, size), size)

    def local(source, target, sem):
        return pltpu.make_async_copy(source, target, sem)

    def to_pair(source, target, row, slot):
        return remote(source, target, h_send.at[row, slot], h_recv.at[row, slot], "dp", own ^ 1)

    def halves(source, target, row):
        return [
            to_pair(at_cols(source, 2 * slot + 1 - core, width), at_cols(target, slot, width), row, slot)
            for slot in range(half)
        ]

    def send_ff(step, which):
        cols = tile_cols(step)
        source = (hidden, d_gate, d_up)[which].at[:, cols]
        return remote(
            source, pair_ff[which].at[:, cols], f_send.at[step, which], f_recv.at[step, which], "dp", own ^ 1
        )

    def send_z(kind, source, target, step, k):
        cols = tile_cols(step)
        rows = pl.ds((k - 1) * tile, tile)
        peer = lax.rem(rank - k + ranks, ranks)
        return remote(
            source.at[rows, cols], target.at[rows, cols], z_send.at[kind, step, k], z_recv.at[kind, step, k], "tensor", peer
        )

    def send_branch(k):
        peer = lax.rem(rank + k, ranks)
        return remote(branch, at_rows(branch_rows, k, tile), b_send.at[k], b_recv.at[k], "tensor", peer)

    def piece(index, slot):
        if index == 0:
            return at_cols(up_w, slot, width)
        if index < 3:
            return at_rows(gate_w, (index - 1) * 4 + slot, width)
        if index == 3:
            return (hidden, d_gate)[slot // 2].at[pl.ds((slot % 2) * width, width), pl.ds(0, 3 * heads)]
        return at_cols(d_up, slot, width)

    def landing(index, slot):
        ref = (down_parts, gate_parts, up_parts, qkv_parts, out_parts)[index]
        return at_cols(ref, slot, width) if index in (0, 4) else at_rows(ref, slot, width)

    def send_grad(index, slot):
        return remote(
            piece(index, slot),
            landing(index, slot),
            w_send.at[index, slot],
            w_recv.at[index, slot],
            "dp",
            own ^ (2 * slot),
        )

    def keep_grad(index):
        return local(piece(index, 0), landing(index, 0), keep.at[index])

    def row_grads(index, left, left_pair, right, right_pair, columns):
        for slot in (3, 1, 2, 0):
            mine, theirs = slice_of(slot, width, True), slice_of(slot, width, False)
            target = piece(index, slot)

            @pl.loop(0, columns // 512)
            def _(step):
                cols = tile_cols(step, 512)
                total = dot_cols(left[:, mine], right[:, cols]) + dot_cols(left_pair[:, theirs], right_pair[:, cols])
                target[:, cols] = total.astype(BF)

            (send_grad(index, slot) if slot else keep_grad(index)).start()

    def col_grads(index, left, left_pair, right, right_pair, columns):
        for slot in (3, 1, 2, 0):
            mine, theirs = slice_of(slot, width, True), slice_of(slot, width, False)
            target = piece(index, slot)

            @pl.loop(0, columns // 512)
            def _(step):
                rows = tile_cols(step, 512)
                total = dot_cols(left[:, rows], right[:, mine]) + dot_cols(left_pair[:, rows], right_pair[:, theirs])
                target[rows, :] = total.astype(BF)

            (send_grad(index, slot) if slot else keep_grad(index)).start()

    def take(kind, source, target):
        @pl.loop(0, count)
        def _(step):
            for k in steps:
                send_z(kind, send_part, target, step, k).wait_recv()

        copy = local(target, recv_part, load.at[0])
        copy.start()
        copy.wait()

    def received(rows_start, size, base):
        total = base
        for k in steps:
            total = total + recv_part[pl.ds(pl.multiple_of((k - 1) * tile + rows_start, size), size), :].astype(F32)
        return total

    def norm_back(total, values, gain):
        inverse = lax.rsqrt(jnp.mean(values * values, axis=-1, keepdims=True) + EPSILON)
        scaled = total * gain
        return inverse * (scaled - values * inverse * inverse * jnp.mean(scaled * values, axis=-1, keepdims=True))

    load_sent = local(sent_in, sent, load.at[1])
    load_cot = local(cot_in, cot, load.at[2])
    load_gate = local(gate_full, gate_w, load.at[3])
    load_up = local(up_full, up_w, load.at[4])
    load_down = local(down_full, down_w, load.at[5])
    load_out = local(out_full, out_w, load.at[6])
    load_qkv = local(qkv_in, qkv, load.at[7])
    load_attended = local(attended_in, attended, load.at[8])
    load_middle = local(middle_in, own_mlp, load.at[9])
    load_tables = []
    for slot in range(ranks):
        block = lax.rem(rank - slot + ranks, ranks)
        for which, (source, target) in enumerate(((cosine_in, cosine), (sine_in, sine))):
            rows = pl.ds(pl.multiple_of(block * tile, tile), tile)
            load_tables.append(
                local(
                    source.at[rows, pl.ds(0, 128)], at_rows(target, slot, tile), load.at[10 + 2 * slot + which]
                )
            )
    start_all([load_sent, load_gate, load_up, load_cot, load_down])
    start_all([load_out, load_qkv, load_attended, load_middle] + load_tables)
    meet(ranks)
    send_cot, send_normed = halves(cot_in, pair_cot, 0), halves(normed_in, pair_normed, 1)
    send_attended = to_pair(attended_in, pair_attended, 2, 0)
    start_all(send_cot + send_normed + [send_attended])
    load_sent.wait()
    norm_rows(sent, normed, inverses, gains.at[pl.ds(1, 1), :], 64)
    send_two = halves(normed, pair_two, 3)
    start_all(send_two)
    wait_all([load_gate, load_up, load_cot, load_down])

    @pl.loop(0, units // step_cols)
    def _(step):
        cols = tile_cols(step)
        gate = dot(normed[...], gate_w[:, cols])
        up = dot(normed[...], up_w[:, cols])
        d_hidden = dot_rows(cot[...], down_w[cols, :])
        s = jax.nn.sigmoid(gate)
        activated = gate * s
        hidden[:, cols] = (activated * up).astype(BF)
        d_gate[:, cols] = (d_hidden * up * (s + activated * (1.0 - s))).astype(BF)
        d_up[:, cols] = (d_hidden * activated).astype(BF)
        for which in range(3):
            send_ff(step, which).start()

    gain_part[...] = jnp.zeros(gain_part.shape, F32)

    @pl.loop(0, count)
    def _(step):
        cols = tile_cols(step)
        product = dot_rows(d_gate[...], gate_w[cols, :]) + dot_rows(d_up[...], up_w[cols, :])
        gain_part[pl.ds(1, 1), cols] = jnp.sum(product * (sent[:, cols].astype(F32) * inverses[...]), axis=0, keepdims=True)
        grad_middle[:, cols] = product[:tile, :]
        send_part[:, cols] = product[tile:, :].astype(BF)
        for k in steps:
            send_z(0, send_part, two_recv, step, k).start()

    @pl.loop(0, units // step_cols)
    def _(step):
        for which in range(3):
            send_ff(step, which).wait_recv()

    for copy in send_cot + send_two:
        copy.wait_recv()
    pair_loads = [
        local(pair_ff[0], buffer_a, load.at[0]),
        local(pair_cot, cot_half, load.at[1]),
        local(pair_ff[1], buffer_b, load.at[2]),
        local(pair_two, two_half, load.at[3]),
        local(pair_ff[2], buffer_c, load.at[4]),
    ]
    start_all(pair_loads)
    wait_all(pair_loads)
    col_grads(0, hidden, buffer_a, cot, cot_half, units)
    row_grads(1, normed, two_half, d_gate, buffer_b, units)
    row_grads(2, normed, two_half, d_up, buffer_c, units)

    take(0, send_part, two_recv)

    @pl.loop(0, tile // 32)
    def _(step):
        rows = pl.ds(pl.multiple_of(step * 32, 32), 32)
        total = received(step * 32, 32, grad_middle[rows, :])
        result = cot[rows, :].astype(F32) + norm_back(total, sent[rows, :].astype(F32), gains[1:2, :])
        grad_middle[rows, :] = result
        branch[rows, :] = result.astype(BF)

    for k in steps:
        send_branch(k).start()
    keep_branch = local(branch, at_rows(branch_rows, 0, tile), keep.at[5])
    keep_branch.start()
    wait_all([load_middle, load_attended, load_qkv, load_out] + load_tables)
    fill_mask(bias, docs, ranks)

    @pl.loop(0, count)
    def _(step):
        cols = tile_cols(step)
        product = dot(hidden[...], down_w[:, cols])
        own_mlp[:, cols] = own_mlp[:, cols] + product[:tile, :]
        send_mlp[:, cols] = product[tile:, :].astype(BF)
        for k in steps:
            send_z(1, send_mlp, mlp_recv, step, k).start()

    load_weight = local(qkv_full, down_w.at[:, pl.ds(0, 3 * heads)], load.at[0])
    load_hidden = local(hidden_in, buffer_b, load.at[1])
    load_normed = local(normed_in, buffer_c, load.at[2])
    start_all([load_weight, load_hidden, load_normed])

    @pl.loop(0, count)
    def _(step):
        for k in steps:
            send_z(0, send_part, two_recv, step, k).wait_send()

    for k in steps:
        send_branch(k).wait_recv()
    keep_branch.wait()
    load_branch = local(branch_rows, buffer_a, load.at[3])
    load_branch.start()
    send_half = halves(branch_rows, pair_branch, 4)
    start_all(send_half)
    load_branch.wait()

    @pl.loop(0, heads // step_cols)
    def _(step):
        cols = tile_cols(step)
        d_attended[:, cols] = dot_rows(buffer_a[...], out_w[cols, :]).astype(BF)

    attend_back(qkv, d_attended, d_qkv, bias, cosine, sine, heads)
    send_qkv = to_pair(d_qkv, pair_qkv, 5, 0)
    send_qkv.start()
    wait_all([load_weight, load_hidden, load_normed])

    @pl.loop(0, count)
    def _(step):
        cols = tile_cols(step)
        product = dot_rows(d_qkv[...], down_w[cols, pl.ds(0, 3 * heads)])
        gain_part[pl.ds(0, 1), cols] = jnp.sum(
            product * (buffer_b[:, cols].astype(F32) * inverses_one[...]), axis=0, keepdims=True
        )
        input_grad[:, cols] = product[:tile, :]
        send_part[:, cols] = product[tile:, :].astype(BF)
        for k in steps:
            send_z(2, send_part, one_recv, step, k).start()

    def send_gain(flip):
        return remote(
            at_cols(gain_part, own ^ flip, width), at_rows(gain_recv, flip, 8), g_send.at[flip], g_recv.at[flip], "dp", own ^ flip
        )

    for flip in range(1, 8):
        send_gain(flip).start()

    for index in range(3):
        keep_grad(index).wait()
    send_qkv.wait_recv()
    for copy in send_half + send_normed + [send_attended]:
        copy.wait_recv()

    @pl.loop(0, units // step_cols)
    def _(step):
        for which in range(3):
            send_ff(step, which).wait_send()

    for copy in send_two:
        copy.wait_send()
    last_loads = [
        local(pair_qkv, normed.at[:, pl.ds(0, 3 * heads)], load.at[0]),
        local(pair_attended, cot.at[:, pl.ds(0, heads)], load.at[1]),
        local(pair_normed, two_half, load.at[2]),
        local(pair_branch, cot_half, load.at[3]),
    ]
    start_all(last_loads)
    wait_all(last_loads)
    row_grads(3, buffer_c, two_half, d_qkv, normed, 3 * heads)
    col_grads(4, attended, cot, buffer_a, cot_half, heads)

    for flip in range(1, 8):
        send_gain(flip).wait_recv()
    gain_sum = gain_part[:, pl.ds(pl.multiple_of(own * width, width), width)]
    for flip in range(1, 8):
        gain_sum = gain_sum + gain_recv[pl.ds(flip * 8, 8), :]
    gain_z[pl.ds(0, 8), :] = gain_sum

    def send_gain_z(k):
        peer = lax.rem(rank + k, ranks)
        return remote(
            gain_z.at[pl.ds(0, 8), :], gain_z.at[pl.ds(8 * k, 8), :], b_send.at[ranks + k], b_recv.at[ranks + k], "tensor", peer
        )

    for k in steps:
        send_gain_z(k).start()

    take(1, send_mlp, mlp_recv)

    @pl.loop(0, tile // 32)
    def _(step):
        rows = pl.ds(pl.multiple_of(step * 32, 32), 32)
        layer_out[rows, :] = received(step * 32, 32, own_mlp[rows, :]).astype(BF)

    take(2, send_part, one_recv)
    load_own = local(hidden_in.at[pl.ds(0, tile), :], branch, load.at[1])
    for k in steps:
        send_branch(k).wait_send()
    load_own.start()
    load_own.wait()

    @pl.loop(0, tile // 32)
    def _(step):
        rows = pl.ds(pl.multiple_of(step * 32, 32), 32)
        total = received(step * 32, 32, input_grad[rows, :])
        input_grad[rows, :] = grad_middle[rows, :] + norm_back(total, branch[rows, :].astype(F32), gains[0:1, :])

    for k in steps:
        send_gain_z(k).wait_recv()
    gain_all = gain_z[pl.ds(0, 8), :]
    for k in steps:
        gain_all = gain_all + gain_z[pl.ds(8 * k, 8), :]
    gain_total[...] = gain_all

    for index in range(5):
        for slot in range(1, 4):
            send_grad(index, slot).wait_recv()
    for index in range(3, 5):
        keep_grad(index).wait()
    for index in range(5):
        for slot in range(1, 4):
            send_grad(index, slot).wait_send()
    for flip in range(1, 8):
        send_gain(flip).wait_send()
    for k in steps:
        send_gain_z(k).wait_send()
    for copy in send_cot + send_normed + send_half + [send_attended, send_qkv]:
        copy.wait_send()

    @pl.loop(0, count)
    def _(step):
        for k in steps:
            send_z(1, send_mlp, mlp_recv, step, k).wait_send()
            send_z(2, send_part, one_recv, step, k).wait_send()


def back(sent, cot, hidden, weights, normed, qkv, attended, middle, cosine, sine, docs, inverses, gains, ranks):
    tokens, dim = sent.shape
    tile, heads, units = tokens // ranks, attended.shape[1], weights[2].shape[0]
    width, rest = gains.shape[1] // 8, tokens - tile
    dma = pltpu.SemaphoreType.DMA
    count = dim // 256
    return pl.pallas_call(
        partial(back_kernel, ranks),
        out_shape=[
            shape((4 * width, units), BF),
            shape((4 * width, units), BF),
            shape((units, 4 * width), BF),
            shape((4 * width, 3 * heads), BF),
            shape((heads, 4 * width), BF),
        ]
        + [shape((tokens, units), BF)] * 3
        + [
            shape((tokens, dim // 2), BF),
            shape((tokens, dim // 2), BF),
            shape((tokens, 3 * heads), BF),
            shape((tokens, heads), BF),
            shape((tokens, dim // 2), BF),
            shape((tokens, dim // 2), BF),
        ]
        + [shape((rest, dim), BF)] * 3
        + [
            shape((tokens, dim), BF),
            shape((tile, dim), BF),
            shape((tile, dim), F32),
            shape((8, width), F32),
        ],
        in_specs=[anyspace()] * 14 + [vmem()] * 3,
        out_specs=[anyspace()] * 18 + [vmem()] * 3,
        scratch_shapes=[
            pltpu.VMEM((dim, units), BF),
            pltpu.VMEM((dim, units), BF),
            pltpu.VMEM((units, dim), BF),
            pltpu.VMEM((tokens, dim), BF),
            pltpu.VMEM((tokens, dim), BF),
            pltpu.VMEM((tokens, dim), BF),
            pltpu.VMEM((tokens, units), BF),
            pltpu.VMEM((tokens, units), BF),
            pltpu.VMEM((tokens, units), BF),
            pltpu.VMEM((tokens, dim // 2), BF),
            pltpu.VMEM((tokens, dim // 2), BF),
            pltpu.VMEM((tokens, units), BF),
            pltpu.VMEM((tokens, units), BF),
            pltpu.VMEM((tokens, units), BF),
            pltpu.VMEM((heads, dim), BF),
            pltpu.VMEM((tokens, 3 * heads), BF),
            pltpu.VMEM((tokens, 3 * heads), BF),
            pltpu.VMEM((tokens, heads), BF),
            pltpu.VMEM((tokens, heads), BF),
            pltpu.VMEM((tokens, tokens), F32),
            pltpu.VMEM((tokens, 128), F32),
            pltpu.VMEM((tokens, 128), F32),
            pltpu.VMEM((tokens, 1), F32),
            pltpu.VMEM((tile, dim), F32),
            pltpu.VMEM((tile, dim), F32),
            pltpu.VMEM((rest, dim), BF),
            pltpu.VMEM((rest, dim), BF),
            pltpu.VMEM((8, dim), F32),
            pltpu.VMEM((64, width), F32),
            pltpu.VMEM((8 * ranks, width), F32),
            dma((units // 256, 3)),
            dma((units // 256, 3)),
            dma((6, 4)),
            dma((6, 4)),
            dma((3, count, ranks)),
            dma((3, count, ranks)),
            dma((2 * ranks,)),
            dma((2 * ranks,)),
            dma((5, 4)),
            dma((5, 4)),
            dma((8,)),
            dma((8,)),
            dma((10 + 2 * ranks,)),
            dma((6,)),
        ],
        compiler_params=pltpu.CompilerParams(vmem_limit_bytes=67000000, collective_id=1, has_side_effects=True),
        cost_estimate=cost(2 * tokens * dim * units * 9, 100e6),
        name="back",
    )(sent, cot, hidden, *weights, normed, qkv, attended, middle, cosine, sine, docs, inverses, gains)


def shift(values, step):
    size = lax.axis_size("tensor")
    return lax.ppermute(values, "tensor", [(index, (index + step) % size) for index in range(size)])


def gather_rows(values):
    return [values] + [shift(values, step) for step in range(1, lax.axis_size("tensor"))]


def scatter_rows(parts):
    total = parts[0].astype(F32)
    for step in range(1, len(parts)):
        total = total + shift(parts[step], -step).astype(F32)
    return total


def gather_weight(values, axis):
    return [None], [lax.all_gather(values, "dp", axis=axis, tiled=True)]


def scatter_full(left, right, axis):
    full = dot_cols(left, right).astype(BF)
    return lax.psum_scatter(full, "dp", scatter_dimension=axis, tiled=True).astype(F32)


def sum_parts(parts, width, axis):
    pieces = jnp.split(parts, 4, axis=axis)
    return sum(piece.astype(F32) for piece in pieces)


def rotary(length):
    half_size = HEAD_DIM // 2
    frequency = ROPE_BASE ** (-jnp.arange(half_size, dtype=F32) / half_size)
    angles = jnp.arange(length).astype(F32)[:, None] * frequency[None, :]
    cosine, sine = jnp.cos(angles), jnp.sin(angles)
    cosine = jnp.tile(cosine, (1, 8))
    sine = jnp.tile(jnp.concatenate([-sine, sine], axis=1), (1, 4))
    return cosine, sine


def position_tables(doc_ids, ranks):
    length = doc_ids.shape[0]
    token_index = jnp.arange(length, dtype=jnp.int32)
    before = jnp.concatenate([doc_ids[:1] - 1, doc_ids[:-1]])
    doc_start = lax.cummax(jnp.where(doc_ids != before, token_index, 0), axis=0)
    order = (lax.axis_index("tensor") - jnp.arange(ranks)) % ranks
    last = token_index.reshape(ranks, -1)[order].reshape(length)
    first = doc_start.reshape(ranks, -1)[order].reshape(length)
    cosine, sine = (table.reshape(ranks, -1, 256)[order].reshape(length, 256) for table in rotary(length))
    return cosine, sine, first[:, None], last[:, None], last[None, :]


def rms_back(grad_rows_, values, gain):
    inverse = lax.rsqrt(jnp.mean(values * values, axis=-1, keepdims=True) + EPSILON)
    scaled = grad_rows_ * gain
    return inverse * (scaled - values * inverse * inverse * jnp.mean(scaled * values, axis=-1, keepdims=True))


def body(
    hidden_in,
    out_cotangent,
    doc_ids,
    attn_gain,
    query_weight,
    key_weight,
    value_weight,
    out_weight,
    mlp_gain,
    gate_weight,
    up_weight,
    down_weight,
):
    ranks, groups = lax.axis_size("tensor"), lax.axis_size("dp")
    paired = groups == 8
    width, heads = query_weight.shape
    dim = hidden_in.shape[1]

    if paired:
        pad = jnp.zeros((6, width), F32)
        own_gains = jnp.concatenate([attn_gain[None].astype(F32), mlp_gain[None].astype(F32), pad], axis=0)
        weights = (query_weight, key_weight, value_weight, out_weight, down_weight, gate_weight, up_weight)
        docs, turns = doc_ids.reshape(ranks, -1), rotary(doc_ids.shape[0])
        front_out = front(hidden_in, out_cotangent, own_gains, weights, *turns, docs, ranks)
        full, (hidden_rows, cot_rows, sent_rows) = front_out[:5], front_out[5:8]
        normed, qkv, attended, inverses, middle, gains = front_out[8:]
        back_out = back(
            sent_rows, cot_rows, hidden_rows, full, normed, qkv, attended, middle, *turns, docs, inverses, gains, ranks
        )
        gate_grad, up_grad, down_grad, qkv_grad, out_proj_grad = (
            sum_parts(part, width, axis) for part, axis in zip(back_out[:5], (0, 0, 1, 0, 1))
        )
        layer_out, input_grad, gain_total = back_out[18:]
        share = width // ranks
        gain_grads = lax.dynamic_slice_in_dim(gain_total, lax.axis_index("tensor") * share, share, axis=1)
    else:
        tables = position_tables(doc_ids, ranks)
        input_local = hidden_in.astype(F32)
        hidden_rows = gather_rows(hidden_in)
        gains = lax.all_gather(jnp.stack([attn_gain, mlp_gain]), "dp", axis=1, tiled=True).astype(F32)
        attn_scale, mlp_scale = gains[:1], gains[1:]
        qkv_weight = jnp.concatenate([query_weight, key_weight, value_weight], axis=1)
        tags, qkv_pieces = gather_weight(qkv_weight, 0)
        tags, out_pieces = gather_weight(out_weight, 1)
        cot_rows = gather_rows(out_cotangent)
        tags, down_pieces = gather_weight(down_weight, 1)
        tags, gate_pieces = gather_weight(gate_weight, 0)
        tags, up_pieces = gather_weight(up_weight, 0)
        normed, qkv, attended, inverses, *branch_parts = attn_fwd(
            hidden_rows, attn_scale, tables, tags, width, qkv_pieces, out_pieces
        )
        middle = input_local + scatter_rows(branch_parts)
        sent = middle.astype(BF)
        sent_rows = gather_rows(sent)
        cot_full = jnp.concatenate(cot_rows, axis=0)
        normed_two, hidden, d_gate, d_up, mlp_gain_part, *two_parts = mlp(
            sent_rows, cot_rows, mlp_scale, tags, width, gate_pieces, up_pieces, down_pieces, ranks
        )
        grad_two_rows = scatter_rows(two_parts)
        grad_middle = out_cotangent.astype(F32) + rms_back(grad_two_rows, sent.astype(F32), mlp_scale)
        branch_rows = gather_rows(grad_middle.astype(BF))
        down_grad = scatter_full(hidden, cot_full, 1)
        gate_grad = scatter_full(normed_two, d_gate, 0)
        up_grad = scatter_full(normed_two, d_up, 0)
        mlp_rows = scatter_rows(mlp_out(hidden, ranks, dim, tags, width, down_pieces))
        layer_out = (middle + mlp_rows).astype(BF)
        branch_full, d_qkv, attn_gain_part, *one_parts = attn_bwd(
            branch_rows, hidden_rows, qkv, inverses, tables, tags, width, qkv_pieces, out_pieces, ranks
        )
        out_proj_grad = scatter_full(attended, branch_full, 1)
        qkv_grad = scatter_full(normed, d_qkv, 0)
        grad_one_rows = scatter_rows(one_parts)
        input_grad = grad_middle + rms_back(grad_one_rows, input_local, attn_scale)
        gain_parts = jnp.concatenate([attn_gain_part, mlp_gain_part], axis=0)
        gain_grads = lax.psum_scatter(gain_parts, ("dp", "tensor"), scatter_dimension=1, tiled=True)
    return (
        layer_out,
        input_grad,
        gain_grads[0],
        qkv_grad[:, :heads],
        qkv_grad[:, heads : 2 * heads],
        qkv_grad[:, 2 * heads :],
        out_proj_grad,
        gain_grads[1],
        gate_grad,
        up_grad,
        down_grad,
    )


def solution(mesh):
    return jax.shard_map(
        body,
        mesh=mesh,
        in_specs=(
            P(("dp", "tensor"), None),
            P(("dp", "tensor"), None),
            P("dp"),
            P("dp"),
            P("dp", "tensor"),
            P("dp", "tensor"),
            P("dp", "tensor"),
            P("tensor", "dp"),
            P("dp"),
            P("dp", "tensor"),
            P("dp", "tensor"),
            P("tensor", "dp"),
        ),
        out_specs=(
            P(("dp", "tensor"), None),
            P(("dp", "tensor"), None),
            P(("dp", "tensor")),
            P("dp", "tensor"),
            P("dp", "tensor"),
            P("dp", "tensor"),
            P("tensor", "dp"),
            P(("dp", "tensor")),
            P("dp", "tensor"),
            P("dp", "tensor"),
            P("tensor", "dp"),
        ),
        check_vma=False,
    )
```

```python
from functools import partial

import jax
import jax.numpy as jnp
from jax import lax
from jax.experimental import pallas as pl
from jax.experimental.pallas import tpu as pltpu
from jax.sharding import PartitionSpec as P

HEAD_DIM = 64
EPSILON = 1e-05
ROPE_BASE = 130000.0
NEGATIVE = -1e30
VMEM_LIMIT = 63 * 1024 * 1024
BF = jnp.bfloat16
F32 = jnp.float32


def dot(left, right):
    return jnp.dot(left, right, preferred_element_type=F32)


def dot_rows(left, right):
    return lax.dot_general(left, right, (((1,), (1,)), ((), ())), preferred_element_type=F32)


def dot_cols(left, right):
    return lax.dot_general(left, right, (((0,), (0,)), ((), ())), preferred_element_type=F32)


def vmem():
    return pl.BlockSpec(memory_space=pltpu.VMEM)


def anyspace():
    return pl.BlockSpec(memory_space=pl.ANY)


def params():
    return pltpu.CompilerParams(vmem_limit_bytes=VMEM_LIMIT)


def cost(flops, nbytes):
    return pl.CostEstimate(flops=int(flops), bytes_accessed=int(nbytes), transcendentals=0)


def shape(dims, kind):
    return jax.ShapeDtypeStruct(dims, kind)


def place_copies(tags, pieces, target, sem, axis, width):
    own = lax.axis_index("dp")
    copies = []
    for slot, (tag, piece) in enumerate(zip(tags, pieces)):
        if tag is None:
            where = target
        else:
            start = pl.multiple_of((own ^ tag) * width, width)
            where = target.at[pl.ds(start, width), :] if axis == 0 else target.at[:, pl.ds(start, width)]
        copies.append(pltpu.make_async_copy(piece, where, sem.at[slot]))
    return copies


def row_copies(pieces, target, sem):
    copies = []
    for slot, piece in enumerate(pieces):
        rows = piece.shape[0]
        copies.append(pltpu.make_async_copy(piece, target.at[pl.ds(slot * rows, rows), :], sem.at[slot]))
    return copies


def start_all(copies):
    for copy in copies:
        copy.start()


def wait_all(copies):
    for copy in copies:
        copy.wait()


def turn(values, cosine, sine):
    width = values.shape[1]
    lane = lax.broadcasted_iota(jnp.int32, values.shape, 1)
    partner = jnp.where(
        lax.rem(lane, HEAD_DIM) < HEAD_DIM // 2,
        pltpu.roll(values, width - HEAD_DIM // 2, 1),
        pltpu.roll(values, HEAD_DIM // 2, 1),
    )
    return values * cosine + partner * sine


def norm_rows(source, target, inverses, gain, tile):
    @pl.loop(0, source.shape[0] // tile)
    def _(step):
        rows = pl.ds(pl.multiple_of(step * tile, tile), tile)
        values = source[rows, :].astype(F32)
        inverse = lax.rsqrt(jnp.mean(values * values, axis=-1, keepdims=True) + EPSILON)
        inverses[rows, :] = inverse
        target[rows, :] = (values * inverse * gain[...]).astype(BF)


def fill_bias(bias, first, last, key_index):
    keys = key_index[...]
    bias[...] = jnp.where((keys >= first[...]) & (keys <= last[...]), 0.0, NEGATIVE)


def head_lanes(width, half):
    lane = lax.broadcasted_iota(jnp.int32, (1, width), 1)
    return (lax.div(lane, HEAD_DIM) == half).astype(F32)


def probabilities(query, key, bias):
    scores = dot_rows(query, key) + bias
    weights = jnp.exp(scores - jnp.max(scores, axis=-1, keepdims=True))
    return weights * (1.0 / jnp.sum(weights, axis=-1, keepdims=True))


def attend(qkv, attended, bias, heads):
    @pl.loop(0, heads // 128)
    def _(pair):
        base = pl.multiple_of(pair * 128, 128)
        query = qkv[:, pl.ds(base, 128)]
        key = qkv[:, pl.ds(heads + base, 128)]
        value = qkv[:, pl.ds(2 * heads + base, 128)]
        total = None
        for half in range(2):
            lanes = head_lanes(128, half).astype(BF)
            probs = probabilities(query * (lanes * HEAD_DIM ** (-0.5)), key, bias[...])
            term = dot(probs.astype(BF), value * lanes)
            total = term if total is None else total + term
        attended[:, pl.ds(base, 128)] = total.astype(BF)


def attn_fwd_kernel(tags, width, nrow, *refs):
    npiece = len(tags)
    rows_in = refs[:nrow]
    gain, cosine, sine, first, last, key_index = refs[nrow : nrow + 6]
    rest = refs[nrow + 6 :]
    qkv_in, out_in = rest[:npiece], rest[npiece : 2 * npiece]
    rest = rest[2 * npiece :]
    normed, qkv, attended, inverses = rest[:4]
    parts = rest[4 : 4 + nrow]
    hidden, qkv_w, out_w, bias, sem_rows, sem_qkv, sem_out = rest[4 + nrow :]
    load_rows = row_copies(rows_in, hidden, sem_rows)
    load_qkv = place_copies(tags, qkv_in, qkv_w, sem_qkv, 0, width)
    load_out = place_copies(tags, out_in, out_w, sem_out, 1, width)
    start_all(load_rows + load_qkv + load_out)
    fill_bias(bias, first, last, key_index)
    wait_all(load_rows)
    norm_rows(hidden, normed, inverses, gain, 64)
    wait_all(load_qkv)
    heads = attended.shape[1]
    step_cols = 256

    @pl.loop(0, 2 * heads // step_cols)
    def _(step):
        cols = pl.ds(pl.multiple_of(step * step_cols, step_cols), step_cols)
        qkv[:, cols] = turn(dot(normed[...], qkv_w[:, cols]), cosine[...], sine[...]).astype(BF)

    @pl.loop(2 * heads // step_cols, 3 * heads // step_cols)
    def _(step):
        cols = pl.ds(pl.multiple_of(step * step_cols, step_cols), step_cols)
        qkv[:, cols] = dot(normed[...], qkv_w[:, cols]).astype(BF)

    attend(qkv, attended, bias, heads)
    wait_all(load_out)
    tile = parts[0].shape[0]

    @pl.loop(0, out_w.shape[1] // step_cols)
    def _(step):
        cols = pl.ds(pl.multiple_of(step * step_cols, step_cols), step_cols)
        product = dot(attended[...], out_w[:, cols])
        for slot, part in enumerate(parts):
            part[:, cols] = product[slot * tile : (slot + 1) * tile, :].astype(part.dtype)


def attn_fwd(rows, gain, tables, tags, width, qkv_pieces, out_pieces):
    nrow, (tile, dim) = len(rows), rows[0].shape
    tokens = nrow * tile
    heads = out_pieces[0].shape[0]
    npiece = len(tags)
    return pl.pallas_call(
        partial(attn_fwd_kernel, tags, width, nrow),
        out_shape=[
            shape((tokens, dim), BF),
            shape((tokens, 3 * heads), BF),
            shape((tokens, heads), BF),
            shape((tokens, 1), F32),
        ]
        + [shape((tile, dim), F32 if slot == 0 else BF) for slot in range(nrow)],
        in_specs=[anyspace()] * nrow + [vmem()] * 6 + [anyspace()] * (2 * npiece),
        out_specs=[vmem()] * (4 + nrow),
        scratch_shapes=[
            pltpu.VMEM((tokens, dim), BF),
            pltpu.VMEM((dim, 3 * heads), BF),
            pltpu.VMEM((heads, dim), BF),
            pltpu.VMEM((tokens, tokens), F32),
            pltpu.SemaphoreType.DMA((nrow,)),
            pltpu.SemaphoreType.DMA((npiece,)),
            pltpu.SemaphoreType.DMA((npiece,)),
        ],
        compiler_params=params(),
        cost_estimate=cost(2 * tokens * dim * 4 * heads * 3, 20e6),
        name="attn_fwd",
    )(*rows, gain, *tables, *qkv_pieces, *out_pieces)


def attend_back(qkv, d_attended, d_qkv, bias, cosine, sine, heads):
    score_scale = HEAD_DIM ** (-0.5)

    @pl.loop(0, heads // 128)
    def _(pair):
        base = pl.multiple_of(pair * 128, 128)
        query = qkv[:, pl.ds(base, 128)]
        key = qkv[:, pl.ds(heads + base, 128)]
        value = qkv[:, pl.ds(2 * heads + base, 128)]
        grad = d_attended[:, pl.ds(base, 128)]
        sums = [0.0, 0.0, 0.0]
        for half in range(2):
            lanes = head_lanes(128, half).astype(BF)
            own_query = query * (lanes * score_scale)
            own_grad = grad * lanes
            probs = probabilities(own_query, key, bias[...])
            d_value = dot_cols(probs.astype(BF), own_grad)
            d_probs = dot_rows(own_grad, value)
            delta = jnp.sum(probs * d_probs, axis=-1, keepdims=True)
            d_scores = (probs * (d_probs - delta)).astype(BF)
            d_query = dot(d_scores, key * lanes) * score_scale
            d_key = dot_cols(d_scores, own_query)
            sums = [sums[0] + d_query, sums[1] + d_key, sums[2] + d_value]
        back = -sine[:, :128]
        d_qkv[:, pl.ds(base, 128)] = turn(sums[0], cosine[:, :128], back).astype(BF)
        d_qkv[:, pl.ds(heads + base, 128)] = turn(sums[1], cosine[:, :128], back).astype(BF)
        d_qkv[:, pl.ds(2 * heads + base, 128)] = sums[2].astype(BF)


def attn_bwd_kernel(tags, width, nrow, npart, *refs):
    npiece = len(tags)
    nhid, nrow = nrow[1], nrow[0]
    rows_in, hidden_in = refs[:nrow], refs[nrow : nrow + nhid]
    refs = refs[nrow + nhid :]
    qkv, inverses, cosine, sine, first, last, key_index = refs[:7]
    rest = refs[7:]
    qkv_in, out_in = rest[:npiece], rest[npiece : 2 * npiece]
    rest = rest[2 * npiece :]
    branch, d_qkv, gain_grad = rest[:3]
    parts = rest[3 : 3 + npart]
    hidden, d_attended, qkv_w, out_w, bias, sem_rows, sem_x, sem_qkv, sem_out = rest[3 + npart :]
    load_rows = row_copies(rows_in, branch, sem_rows)
    load_x = row_copies(hidden_in, hidden, sem_x)
    load_out = place_copies(tags, out_in, out_w, sem_out, 1, width)
    load_qkv = place_copies(tags, qkv_in, qkv_w, sem_qkv, 0, width)
    start_all(load_rows + load_out + load_qkv + load_x)
    fill_bias(bias, first, last, key_index)
    wait_all(load_rows)
    wait_all(load_out)
    heads = out_w.shape[0]
    step_cols = 256

    @pl.loop(0, heads // step_cols)
    def _(step):
        cols = pl.ds(pl.multiple_of(step * step_cols, step_cols), step_cols)
        d_attended[:, cols] = dot_rows(branch[...], out_w[cols, :]).astype(BF)

    attend_back(qkv, d_attended, d_qkv, bias, cosine, sine, heads)
    wait_all(load_qkv)
    wait_all(load_x)
    tile = parts[0].shape[0]

    @pl.loop(0, qkv_w.shape[0] // step_cols)
    def _(step):
        cols = pl.ds(pl.multiple_of(step * step_cols, step_cols), step_cols)
        product = dot_rows(d_qkv[...], qkv_w[cols, :])
        gain_grad[:, cols] = jnp.sum(product * (hidden[:, cols].astype(F32) * inverses[...]), axis=0, keepdims=True)
        for slot, part in enumerate(parts):
            part[:, cols] = product[slot * tile : (slot + 1) * tile, :].astype(part.dtype)


def attn_bwd(rows, hidden, qkv, inverses, tables, tags, width, qkv_pieces, out_pieces, npart):
    nrow, nhid, dim = len(rows), len(hidden), rows[0].shape[1]
    tokens = qkv.shape[0]
    tile = tokens // npart
    heads = out_pieces[0].shape[0]
    npiece = len(tags)
    return pl.pallas_call(
        partial(attn_bwd_kernel, tags, width, (nrow, nhid), npart),
        out_shape=[shape((tokens, dim), BF), shape((tokens, 3 * heads), BF), shape((1, dim), F32)]
        + [shape((tile, dim), F32 if slot == 0 else BF) for slot in range(npart)],
        in_specs=[anyspace()] * (nrow + nhid) + [vmem()] * 7 + [anyspace()] * (2 * npiece),
        out_specs=[vmem()] * (3 + npart),
        scratch_shapes=[
            pltpu.VMEM((tokens, dim), BF),
            pltpu.VMEM((tokens, heads), BF),
            pltpu.VMEM((dim, 3 * heads), BF),
            pltpu.VMEM((heads, dim), BF),
            pltpu.VMEM((tokens, tokens), F32),
            pltpu.SemaphoreType.DMA((nrow,)),
            pltpu.SemaphoreType.DMA((nhid,)),
            pltpu.SemaphoreType.DMA((npiece,)),
            pltpu.SemaphoreType.DMA((npiece,)),
        ],
        compiler_params=params(),
        cost_estimate=cost(2 * tokens * dim * 4 * heads * 6, 30e6),
        name="attn_bwd",
    )(*rows, *hidden, qkv, inverses, *tables, *qkv_pieces, *out_pieces)


def mlp_kernel(tags, width, nrow, npart, *refs):
    npiece = len(tags)
    sent_in, cot_in = refs[:nrow], refs[nrow : 2 * nrow]
    gain = refs[2 * nrow]
    rest = refs[2 * nrow + 1 :]
    gate_in, up_in, down_in = rest[:npiece], rest[npiece : 2 * npiece], rest[2 * npiece : 3 * npiece]
    rest = rest[3 * npiece :]
    normed, hidden, d_gate, d_up, gain_grad = rest[:5]
    parts = rest[5 : 5 + npart]
    sent, cot, inverses, gate_w, up_w, down_w, sem_sent, sem_cot, sem_gate, sem_up, sem_down = rest[5 + npart :]
    load_sent = row_copies(sent_in, sent, sem_sent)
    load_cot = row_copies(cot_in, cot, sem_cot)
    load_gate = place_copies(tags, gate_in, gate_w, sem_gate, 0, width)
    load_up = place_copies(tags, up_in, up_w, sem_up, 0, width)
    load_down = place_copies(tags, down_in, down_w, sem_down, 1, width)
    start_all(load_sent + load_cot + load_gate + load_up + load_down)
    wait_all(load_sent)
    norm_rows(sent, normed, inverses, gain, 64)
    wait_all(load_cot)
    wait_all(load_gate)
    wait_all(load_up)
    wait_all(load_down)
    step_cols = 256

    @pl.loop(0, gate_w.shape[1] // step_cols)
    def _(step):
        cols = pl.ds(pl.multiple_of(step * step_cols, step_cols), step_cols)
        gate = dot(normed[...], gate_w[:, cols])
        up = dot(normed[...], up_w[:, cols])
        d_hidden = dot_rows(cot[...], down_w[cols, :])
        s = jax.nn.sigmoid(gate)
        activated = gate * s
        hidden[:, cols] = (activated * up).astype(BF)
        d_gate[:, cols] = (d_hidden * up * (s + activated * (1.0 - s))).astype(BF)
        d_up[:, cols] = (d_hidden * activated).astype(BF)

    tile = parts[0].shape[0]

    @pl.loop(0, gate_w.shape[0] // step_cols)
    def _(step):
        cols = pl.ds(pl.multiple_of(step * step_cols, step_cols), step_cols)
        product = dot_rows(d_gate[...], gate_w[cols, :]) + dot_rows(d_up[...], up_w[cols, :])
        gain_grad[:, cols] = jnp.sum(product * (sent[:, cols].astype(F32) * inverses[...]), axis=0, keepdims=True)
        for slot, part in enumerate(parts):
            part[:, cols] = product[slot * tile : (slot + 1) * tile, :].astype(part.dtype)


def mlp(sent, cot, gain, tags, width, gate_pieces, up_pieces, down_pieces, npart):
    nrow, dim = len(sent), sent[0].shape[1]
    tokens = nrow * sent[0].shape[0]
    tile = tokens // npart
    units = gate_pieces[0].shape[1]
    npiece = len(tags)
    return pl.pallas_call(
        partial(mlp_kernel, tags, width, nrow, npart),
        out_shape=[shape((tokens, dim), BF)]
        + [shape((tokens, units), BF)] * 3
        + [shape((1, dim), F32)]
        + [shape((tile, dim), F32 if slot == 0 else BF) for slot in range(npart)],
        in_specs=[anyspace()] * (2 * nrow) + [vmem()] + [anyspace()] * (3 * npiece),
        out_specs=[vmem()] * (5 + npart),
        scratch_shapes=[
            pltpu.VMEM((tokens, dim), BF),
            pltpu.VMEM((tokens, dim), BF),
            pltpu.VMEM((tokens, 1), F32),
            pltpu.VMEM((dim, units), BF),
            pltpu.VMEM((dim, units), BF),
            pltpu.VMEM((units, dim), BF),
            pltpu.SemaphoreType.DMA((nrow,)),
            pltpu.SemaphoreType.DMA((nrow,)),
            pltpu.SemaphoreType.DMA((npiece,)),
            pltpu.SemaphoreType.DMA((npiece,)),
            pltpu.SemaphoreType.DMA((npiece,)),
        ],
        compiler_params=params(),
        cost_estimate=cost(2 * tokens * dim * units * 5, 40e6),
        name="mlp",
    )(*sent, *cot, gain, *gate_pieces, *up_pieces, *down_pieces)


def mlp_out_kernel(tags, width, *refs):
    npiece = len(tags)
    hidden, down_in = refs[0], refs[1 : 1 + npiece]
    *parts, down_w, sem_down = refs[1 + npiece :]
    load_down = place_copies(tags, down_in, down_w, sem_down, 1, width)
    start_all(load_down)
    wait_all(load_down)
    tile, step_cols = parts[0].shape[0], 256

    @pl.loop(0, down_w.shape[1] // step_cols)
    def _(step):
        cols = pl.ds(pl.multiple_of(step * step_cols, step_cols), step_cols)
        product = dot(hidden[...], down_w[:, cols])
        for slot, part in enumerate(parts):
            part[:, cols] = product[slot * tile : (slot + 1) * tile, :].astype(part.dtype)


def mlp_out(hidden, nrow, dim, tags, width, down_pieces):
    tokens, units = hidden.shape
    tile, npiece = tokens // nrow, len(tags)
    return pl.pallas_call(
        partial(mlp_out_kernel, tags, width),
        out_shape=[shape((tile, dim), F32 if slot == 0 else BF) for slot in range(nrow)],
        in_specs=[vmem()] + [anyspace()] * npiece,
        out_specs=[vmem()] * nrow,
        scratch_shapes=[pltpu.VMEM((units, dim), BF), pltpu.SemaphoreType.DMA((npiece,))],
        compiler_params=params(),
        cost_estimate=cost(2 * tokens * dim * units, 14e6),
        name="mlp_out",
    )(hidden, *down_pieces)


def slice_of(slot, width, own):
    index = lax.axis_index("dp")
    owner = index ^ (2 * slot)
    return pl.ds(pl.multiple_of((owner if own else lax.div(owner, 2)) * width, width), width)


MESH = pl.DeviceIdType.MESH
NEAR = (2, 4, 6)


def remote(source, target, send_sem, recv_sem, axis, peer):
    return pltpu.make_async_remote_copy(
        src_ref=source,
        dst_ref=target,
        send_sem=send_sem,
        recv_sem=recv_sem,
        device_id={axis: peer},
        device_id_type=MESH,
    )


def meet(ranks):
    own, rank = lax.axis_index("dp"), lax.axis_index("tensor")
    barrier = pltpu.get_barrier_semaphore()
    for flip in range(1, 8):
        pl.semaphore_signal(barrier, inc=1, device_id={"dp": own ^ flip}, device_id_type=MESH)
    for step in range(1, ranks):
        pl.semaphore_signal(barrier, inc=1, device_id={"tensor": lax.rem(rank + step, ranks)}, device_id_type=MESH)
    pl.semaphore_wait(barrier, ranks + 6)


def at_cols(ref, index, width):
    return ref.at[:, pl.ds(pl.multiple_of(index * width, width), width)]


def at_rows(ref, index, width):
    return ref.at[pl.ds(pl.multiple_of(index * width, width), width), :]


def fill_mask(bias, docs, ranks):
    rank = lax.axis_index("tensor")
    tile = docs.shape[1]
    blocks = [lax.rem(rank - slot + ranks, ranks) for slot in range(ranks)]
    own_docs = [jnp.broadcast_to(docs[pl.ds(block, 1), :].astype(F32), (tile, tile)) for block in blocks]
    turned = [jnp.transpose(values) for values in own_docs]
    row = lax.broadcasted_iota(jnp.int32, (tile, tile), 0)
    lane = lax.broadcasted_iota(jnp.int32, (tile, tile), 1)
    for q in range(ranks):
        for k in range(ranks):
            same = turned[q] == own_docs[k]
            before = row + blocks[q] * tile >= lane + blocks[k] * tile
            bias[q * tile : (q + 1) * tile, k * tile : (k + 1) * tile] = jnp.where(same & before, 0.0, NEGATIVE)


def either(rank, *choices):
    result = rank == choices[0]
    for choice in choices[1:]:
        result = result | (rank == choice)
    return result


class RowGather:
    def __init__(self, rank, source, landing, tile, send, recv, kind):
        self.rank = rank

        def copy(origin, slot, target, step, sem):
            peer = lax.rem(rank + step + 4, 4)
            return remote(origin, at_rows(landing, target, tile), send.at[kind, sem], recv.at[kind, target], "tensor", peer)

        self.direct = [None] + [copy(source, 0, step, step, step) for step in (1, 2, 3)]
        self.up = copy(at_rows(landing, 2, tile), 2, 3, 1, 0)
        self.down = copy(at_rows(landing, 2, tile), 2, 1, -1, 0)

    def start(self):
        self.direct[2].start()
        pl.when(self.rank < 3)(self.direct[1].start)
        pl.when(self.rank > 0)(self.direct[3].start)

    def relay(self):
        @pl.when(self.rank == 2)
        def _():
            self.direct[2].wait_recv()
            self.up.start()

        @pl.when(self.rank == 1)
        def _():
            self.direct[2].wait_recv()
            self.down.start()

    def wait(self):
        pl.when(either(self.rank, 0, 3))(self.direct[2].wait_recv)
        self.direct[1].wait_recv()
        self.direct[3].wait_recv()

    def finish(self):
        self.direct[2].wait_send()
        pl.when(self.rank < 3)(self.direct[1].wait_send)
        pl.when(self.rank > 0)(self.direct[3].wait_send)
        pl.when(self.rank == 2)(self.up.wait_send)
        pl.when(self.rank == 1)(self.down.wait_send)


class RowScatter:
    def __init__(self, rank, source, landing, merge, tile, step_cols, send, recv):
        self.rank, self.tile, self.source = rank, tile, source
        self.merge_in = merge
        self.count = source.shape[1] // step_cols
        self.cols = lambda step: pl.ds(pl.multiple_of(step * step_cols, step_cols), step_cols)

        def copy(step, k):
            rows, cols = pl.ds((k - 1) * tile, tile), self.cols(step)
            return remote(
                source.at[rows, cols],
                landing.at[rows, cols],
                send.at[step, k],
                recv.at[step, k],
                "tensor",
                lax.rem(rank - k + 4, 4),
            )

        def far(step, k, peer):
            rows, cols = pl.ds((k - 1) * tile, tile), self.cols(step)
            return remote(
                source.at[rows, cols], merge.at[:, cols], send.at[step, k], recv.at[step, 0], "tensor", peer
            )

        self.copy, self.far = copy, far

    def start_first(self, step):
        pl.when(self.rank == 0)(self.far(step, 1, 1).start)
        pl.when(self.rank == 3)(self.far(step, 3, 2).start)

        @pl.when(either(self.rank, 1, 2))
        def _():
            self.copy(step, 1).start()
            self.copy(step, 3).start()

    def start_rest(self):
        @pl.when(either(self.rank, 0, 3))
        def _():
            @pl.loop(0, self.count)
            def _(step):
                self.copy(step, 2).start()

        @pl.when(self.rank == 0)
        def _():
            @pl.loop(0, self.count)
            def _(step):
                self.copy(step, 3).start()

        @pl.when(self.rank == 3)
        def _():
            @pl.loop(0, self.count)
            def _(step):
                self.copy(step, 1).start()

    def merge(self, staged=None, sem=None):
        @pl.when(either(self.rank, 1, 2))
        def _():
            rows = pl.ds(self.tile, self.tile)
            other = self.merge_in if staged is None else staged
            if staged is not None:

                @pl.loop(0, self.count)
                def _(step):
                    self.far(step, 1, 1).wait_recv()

                load = pltpu.make_async_copy(self.merge_in, staged, sem)
                load.start()
                load.wait()

            @pl.loop(0, self.count)
            def _(step):
                cols = self.cols(step)
                if staged is None:
                    self.far(step, 1, 1).wait_recv()
                total = self.source[rows, cols].astype(F32) + other[:, cols].astype(F32)
                self.source[rows, cols] = total.astype(BF)
                self.copy(step, 2).start()

    def wait(self):
        @pl.loop(0, self.count)
        def _(step):
            self.copy(step, 2).wait_recv()

        @pl.when(self.rank != 3)
        def _():
            @pl.loop(0, self.count)
            def _(step):
                self.copy(step, 1).wait_recv()

        @pl.when(self.rank != 0)
        def _():
            @pl.loop(0, self.count)
            def _(step):
                self.copy(step, 3).wait_recv()

    def clear(self, target):
        rows = self.tile

        @pl.when(self.rank == 3)
        def _():
            target[:rows, :] = jnp.zeros((rows, target.shape[1]), target.dtype)

        @pl.when(self.rank == 0)
        def _():
            target[2 * rows :, :] = jnp.zeros((rows, target.shape[1]), target.dtype)

    def finish(self):
        @pl.loop(0, self.count)
        def _(step):
            for k in (1, 2, 3):
                self.copy(step, k).wait_send()


def front_kernel(ranks, *refs):
    hidden_in, cot_in, gains_in = refs[:3]
    weights_in = refs[3:10]
    cosine_in, sine_in, docs = refs[10:13]
    qkv_full, out_full, down_full, gate_full, up_full, hidden_rows, cot_rows, sent_rows = refs[13:21]
    normed, qkv, attended, inverses, middle, gains = refs[21:27]
    hidden, qkv_w, out_w, cosine, sine, bias, part, send_part, recv_part, merge_part, sent = refs[27:38]
    stage = refs[38:45]
    (w_send, w_recv, z_send, z_recv, p_send, p_recv, g_send, g_recv, load, keep) = refs[45:]
    own, rank = lax.axis_index("dp"), lax.axis_index("tensor")
    tile, dim = hidden_in.shape
    width = weights_in[0].shape[0]
    heads = weights_in[0].shape[1]
    step_cols = 256
    count = dim // step_cols

    def slot_of(index, owner, part=None):
        ref = (qkv_full, qkv_full, qkv_full, out_full, down_full, gate_full, up_full)[index]
        rows = weights_in[index].shape[0]
        size = rows if part is None else rows // 2
        start = 0 if part is None else part * size
        if index in (3, 4):
            return ref.at[pl.ds(start, size), pl.ds(pl.multiple_of(owner * width, width), width)]
        rows = pl.ds(pl.multiple_of(owner * width + start, size), size)
        return ref.at[rows, pl.ds(index * heads, heads)] if index < 3 else ref.at[rows, :]

    def send_weight(index, flip):
        return remote(
            weights_in[index], slot_of(index, own), w_send.at[index, flip], w_recv.at[index, flip], "dp", own ^ flip
        )

    def relay_weight(index, part):
        place = slot_of(index, own ^ (4 - 2 * part), part)
        tag = 6 + part
        return remote(place, place, w_send.at[index, tag], w_recv.at[index, tag], "dp", own ^ (2 + 2 * part))

    def pass_weight(index, flip):
        place = slot_of(index, own ^ flip)
        tag = {2: 3, 4: 5, 6: 8}[flip]
        return remote(place, place, w_send.at[index, tag], w_recv.at[index, tag], "dp", own ^ 1)

    def relay_weights(indices):
        for index in indices:
            send_weight(index, 4).wait_recv()
            relay_weight(index, 0).start()
            send_weight(index, 2).wait_recv()
            relay_weight(index, 1).start()
            pass_weight(index, 4).start()
            pass_weight(index, 2).start()

    def pass_weights(indices):
        for index in indices:
            relay_weight(index, 0).wait_recv()
            relay_weight(index, 1).wait_recv()
            pass_weight(index, 6).start()

    def finish(indices):
        for index in indices:
            send_weight(index, 1).wait_recv()
            for flip in NEAR:
                pass_weight(index, flip).wait_recv()

    def send_gain(flip):
        return remote(gains_in, at_cols(gains, own, width), g_send.at[flip], g_recv.at[flip], "dp", own ^ flip)

    gather_hidden = RowGather(rank, hidden_in, hidden_rows, tile, z_send, z_recv, 0)
    gather_cot = RowGather(rank, cot_in, cot_rows, tile, z_send, z_recv, 1)
    gather_sent = RowGather(rank, sent, sent_rows, tile, z_send, z_recv, 2)
    branch = RowScatter(rank, send_part, recv_part, merge_part, tile, step_cols, p_send, p_recv)
    steps = list(range(1, ranks))

    meet(ranks)
    gather_hidden.start()
    for flip in range(1, 8):
        send_gain(flip).start()
    for index in range(4):
        for flip in (2, 4, 1):
            send_weight(index, flip).start()
    gather_cot.start()

    stage_in = [pltpu.make_async_copy(weights_in[index], stage[index], load.at[index]) for index in range(7)]
    stage_out = [pltpu.make_async_copy(stage[index], slot_of(index, own), keep.at[index]) for index in range(7)]
    own_hidden = pltpu.make_async_copy(hidden_in, hidden.at[pl.ds(0, tile), :], load.at[7])
    own_cot = pltpu.make_async_copy(cot_in, sent, load.at[8])
    own_gain = pltpu.make_async_copy(gains_in, at_cols(gains, own, width), load.at[9])
    tables = []
    for slot in range(ranks):
        block = lax.rem(rank - slot + ranks, ranks)
        for which, (source, target) in enumerate(((cosine_in, cosine), (sine_in, sine))):
            tables.append(
                pltpu.make_async_copy(
                    at_rows(source, block, tile), at_rows(target, slot, tile), load.at[10 + 2 * slot + which]
                )
            )
    start_all(stage_in + [own_hidden, own_cot, own_gain] + tables)
    relay_weights(range(4))
    for index in range(4, 7):
        for flip in (2, 4, 1):
            send_weight(index, flip).start()
    gather_hidden.relay()
    wait_all(stage_in)
    start_all(stage_out)
    wait_all([own_hidden, own_cot, own_gain])
    keep_hidden = pltpu.make_async_copy(hidden.at[pl.ds(0, tile), :], hidden_rows.at[pl.ds(0, tile), :], keep.at[7])
    keep_cot = pltpu.make_async_copy(sent, cot_rows.at[pl.ds(0, tile), :], keep.at[8])
    start_all([keep_hidden, keep_cot])
    fill_mask(bias, docs, ranks)
    wait_all(tables + stage_out + [keep_hidden, keep_cot])

    pass_weights(range(4))
    for flip in range(1, 8):
        send_gain(flip).wait_recv()
    gather_hidden.wait()
    load_rows = pltpu.make_async_copy(
        hidden_rows.at[pl.ds(tile, (ranks - 1) * tile), :], hidden.at[pl.ds(tile, (ranks - 1) * tile), :], load.at[0]
    )
    load_rows.start()
    load_rows.wait()
    norm_rows(hidden, normed, inverses, gains.at[pl.ds(0, 1), :], 64)
    finish(range(4))
    load_qkv = pltpu.make_async_copy(qkv_full, qkv_w, load.at[1])
    load_out = pltpu.make_async_copy(out_full, out_w, load.at[2])
    load_qkv.start()
    load_out.start()
    load_qkv.wait()

    @pl.loop(0, 2 * heads // step_cols)
    def _(step):
        cols = pl.ds(pl.multiple_of(step * step_cols, step_cols), step_cols)
        qkv[:, cols] = turn(dot(normed[...], qkv_w[:, cols]), cosine[...], sine[...]).astype(BF)

    @pl.loop(2 * heads // step_cols, 3 * heads // step_cols)
    def _(step):
        cols = pl.ds(pl.multiple_of(step * step_cols, step_cols), step_cols)
        qkv[:, cols] = dot(normed[...], qkv_w[:, cols]).astype(BF)

    attend(qkv, attended, bias, heads)
    load_out.wait()

    gather_cot.relay()

    @pl.loop(0, count)
    def _(step):
        cols = pl.ds(pl.multiple_of(step * step_cols, step_cols), step_cols)
        product = dot(attended[...], out_w[:, cols])
        part[:, cols] = product[:tile, :]
        send_part[:, cols] = product[tile:, :].astype(BF)
        branch.start_first(step)

    branch.start_rest()
    branch.clear(recv_part)
    branch.merge()
    relay_weights([4, 5, 6])
    branch.wait()

    @pl.loop(0, count)
    def _(step):
        cols = pl.ds(pl.multiple_of(step * step_cols, step_cols), step_cols)
        total = hidden[pl.ds(0, tile), cols].astype(F32) + part[:, cols]
        for k in steps:
            total = total + recv_part[pl.ds((k - 1) * tile, tile), cols].astype(F32)
        middle[:, cols] = total
        sent[:, cols] = total.astype(BF)

    gather_sent.start()
    keep_sent = pltpu.make_async_copy(sent, sent_rows.at[pl.ds(0, tile), :], keep.at[0])
    keep_sent.start()
    pass_weights([4, 5])
    gather_sent.relay()
    pass_weights([6])
    finish([4, 5, 6])
    gather_cot.wait()
    gather_sent.wait()
    keep_sent.wait()
    for gather in (gather_hidden, gather_cot, gather_sent):
        gather.finish()
    for index in range(7):
        for flip in (1, 2, 4):
            send_weight(index, flip).wait_send()
        for flip in NEAR:
            pass_weight(index, flip).wait_send()
        for part_index in range(2):
            relay_weight(index, part_index).wait_send()
    for flip in range(1, 8):
        send_gain(flip).wait_send()
    branch.finish()


def front(hidden_in, cot, gains, weights, cosine, sine, docs, ranks):
    tile, dim = hidden_in.shape
    tokens = tile * ranks
    width, heads = weights[0].shape
    units = weights[5].shape[1]
    dma = pltpu.SemaphoreType.DMA
    return pl.pallas_call(
        partial(front_kernel, ranks),
        out_shape=[
            shape((dim, 3 * heads), BF),
            shape((heads, dim), BF),
            shape((units, dim), BF),
            shape((dim, units), BF),
            shape((dim, units), BF),
            shape((tokens, dim), BF),
            shape((tokens, dim), BF),
            shape((tokens, dim), BF),
            shape((tokens, dim), BF),
            shape((tokens, 3 * heads), BF),
            shape((tokens, heads), BF),
            shape((tokens, 1), F32),
            shape((tile, dim), F32),
            shape((8, dim), F32),
        ],
        in_specs=[anyspace()] * 12 + [vmem()],
        out_specs=[anyspace()] * 8 + [vmem()] * 6,
        scratch_shapes=[
            pltpu.VMEM((tokens, dim), BF),
            pltpu.VMEM((dim, 3 * heads), BF),
            pltpu.VMEM((heads, dim), BF),
            pltpu.VMEM((tokens, 256), F32),
            pltpu.VMEM((tokens, 256), F32),
            pltpu.VMEM((tokens, tokens), F32),
            pltpu.VMEM((tile, dim), F32),
            pltpu.VMEM((tokens - tile, dim), BF),
            pltpu.VMEM((tokens - tile, dim), BF),
            pltpu.VMEM((tile, dim), BF),
            pltpu.VMEM((tile, dim), BF),
        ]
        + [pltpu.VMEM(weight.shape, BF) for weight in weights]
        + [
            dma((7, 9)),
            dma((7, 9)),
            dma((3, ranks)),
            dma((3, ranks)),
            dma((dim // 256, ranks)),
            dma((dim // 256, ranks)),
            dma((8,)),
            dma((8,)),
            dma((10 + 2 * ranks,)),
            dma((9,)),
        ],
        compiler_params=pltpu.CompilerParams(vmem_limit_bytes=VMEM_LIMIT, collective_id=0, has_side_effects=True),
        cost_estimate=cost(2 * tokens * dim * 4 * heads * 3, 20e6),
        name="front",
    )(hidden_in, cot, gains, *weights, cosine, sine, docs)


def back_kernel(ranks, *refs):
    (
        sent_in,
        cot_in,
        hidden_in,
        qkv_full,
        out_full,
        down_full,
        gate_full,
        up_full,
        normed_in,
        qkv_in,
        attended_in,
        middle_in,
        cosine_in,
        sine_in,
        docs,
        inverses_one,
        gains,
    ) = refs[:17]
    gate_parts, up_parts, down_parts, qkv_parts, out_parts = refs[17:22]
    pair_ff = refs[22:25]
    pair_two, pair_cot, pair_qkv, pair_attended, pair_normed, pair_branch = refs[25:31]
    two_recv, mlp_recv, one_recv, branch_rows = refs[31:35]
    layer_out, input_grad, gain_total = refs[35:38]
    gate_w, up_w, down_w, sent, cot, normed, hidden, d_gate, d_up = refs[38:47]
    two_half, cot_half, buffer_a, buffer_b, buffer_c, out_w = refs[47:53]
    qkv, d_qkv, attended, d_attended, bias, cosine, sine, inverses = refs[53:61]
    own_mlp, grad_middle, send_part, recv_part, gain_part, gain_recv, gain_z = refs[61:68]
    f_send, f_recv, h_send, h_recv, z_send, z_recv, b_send, b_recv, w_send, w_recv, g_send, g_recv, load, keep = refs[68:]

    own, rank = lax.axis_index("dp"), lax.axis_index("tensor")
    core = lax.rem(own, 2)
    tokens, dim = sent.shape
    units = gate_w.shape[1]
    tile = tokens // ranks
    heads = attended.shape[1]
    width = out_parts.shape[1] // 4
    half = dim // (2 * width)
    step_cols = 256
    count = dim // step_cols
    steps = list(range(1, ranks))
    rest = tokens - tile
    branch, send_mlp = sent.at[pl.ds(0, tile), :], sent.at[pl.ds(tile, rest), :]

    def tile_cols(step, size=step_cols):
        return pl.ds(pl.multiple_of(step * size, size), size)

    def local(source, target, sem):
        return pltpu.make_async_copy(source, target, sem)

    def to_pair(source, target, row, slot):
        return remote(source, target, h_send.at[row, slot], h_recv.at[row, slot], "dp", own ^ 1)

    def halves(source, target, row):
        return [
            to_pair(at_cols(source, 2 * slot + 1 - core, width), at_cols(target, slot, width), row, slot)
            for slot in range(half)
        ]

    def send_ff(step, which):
        cols = tile_cols(step)
        source = (hidden, d_gate, d_up)[which].at[:, cols]
        return remote(
            source, pair_ff[which].at[:, cols], f_send.at[step, which], f_recv.at[step, which], "dp", own ^ 1
        )

    def send_z(kind, source, target, step, k):
        cols = tile_cols(step)
        rows = pl.ds((k - 1) * tile, tile)
        peer = lax.rem(rank - k + ranks, ranks)
        return remote(
            source.at[rows, cols], target.at[rows, cols], z_send.at[kind, step, k], z_recv.at[kind, step, k], "tensor", peer
        )

    def send_branch(k):
        peer = lax.rem(rank + k, ranks)
        return remote(branch, at_rows(branch_rows, k, tile), b_send.at[k], b_recv.at[k], "tensor", peer)

    def piece(index, slot):
        if index == 0:
            return at_cols(up_w, slot, width)
        if index < 3:
            return at_rows(gate_w, (index - 1) * 4 + slot, width)
        if index == 3:
            return (hidden, d_gate)[slot // 2].at[pl.ds((slot % 2) * width, width), pl.ds(0, 3 * heads)]
        return at_cols(d_up, slot, width)

    def landing(index, slot):
        ref = (down_parts, gate_parts, up_parts, qkv_parts, out_parts)[index]
        return at_cols(ref, slot, width) if index in (0, 4) else at_rows(ref, slot, width)

    def send_grad(index, slot):
        return remote(
            piece(index, slot),
            landing(index, slot),
            w_send.at[index, slot],
            w_recv.at[index, slot],
            "dp",
            own ^ (2 * slot),
        )

    def keep_grad(index):
        return local(piece(index, 0), landing(index, 0), keep.at[index])

    def row_grads(index, left, left_pair, right, right_pair, columns):
        for slot in (3, 1, 2, 0):
            mine, theirs = slice_of(slot, width, True), slice_of(slot, width, False)
            target = piece(index, slot)

            @pl.loop(0, columns // 512)
            def _(step):
                cols = tile_cols(step, 512)
                total = dot_cols(left[:, mine], right[:, cols]) + dot_cols(left_pair[:, theirs], right_pair[:, cols])
                target[:, cols] = total.astype(BF)

            (send_grad(index, slot) if slot else keep_grad(index)).start()

    def col_grads(index, left, left_pair, right, right_pair, columns):
        for slot in (3, 1, 2, 0):
            mine, theirs = slice_of(slot, width, True), slice_of(slot, width, False)
            target = piece(index, slot)

            @pl.loop(0, columns // 512)
            def _(step):
                rows = tile_cols(step, 512)
                total = dot_cols(left[:, rows], right[:, mine]) + dot_cols(left_pair[:, rows], right_pair[:, theirs])
                target[rows, :] = total.astype(BF)

            (send_grad(index, slot) if slot else keep_grad(index)).start()

    def take(kind, source, target):
        @pl.loop(0, count)
        def _(step):
            for k in steps:
                send_z(kind, send_part, target, step, k).wait_recv()

        copy = local(target, recv_part, load.at[0])
        copy.start()
        copy.wait()

    def received(rows_start, size, base):
        total = base
        for k in steps:
            total = total + recv_part[pl.ds(pl.multiple_of((k - 1) * tile + rows_start, size), size), :].astype(F32)
        return total

    def norm_back(total, values, gain):
        inverse = lax.rsqrt(jnp.mean(values * values, axis=-1, keepdims=True) + EPSILON)
        scaled = total * gain
        return inverse * (scaled - values * inverse * inverse * jnp.mean(scaled * values, axis=-1, keepdims=True))

    load_sent = local(sent_in, sent, load.at[1])
    load_cot = local(cot_in, cot, load.at[2])
    load_gate = local(gate_full, gate_w, load.at[3])
    load_up = local(up_full, up_w, load.at[4])
    load_down = local(down_full, down_w, load.at[5])
    load_out = local(out_full, out_w, load.at[6])
    load_qkv = local(qkv_in, qkv, load.at[7])
    load_attended = local(attended_in, attended, load.at[8])
    load_middle = local(middle_in, own_mlp, load.at[9])
    load_tables = []
    for slot in range(ranks):
        block = lax.rem(rank - slot + ranks, ranks)
        for which, (source, target) in enumerate(((cosine_in, cosine), (sine_in, sine))):
            rows = pl.ds(pl.multiple_of(block * tile, tile), tile)
            load_tables.append(
                local(
                    source.at[rows, pl.ds(0, 128)], at_rows(target, slot, tile), load.at[10 + 2 * slot + which]
                )
            )
    start_all([load_sent, load_gate, load_up, load_cot, load_down])
    start_all([load_out, load_qkv, load_attended, load_middle] + load_tables)
    meet(ranks)
    send_cot, send_normed = halves(cot_in, pair_cot, 0), halves(normed_in, pair_normed, 1)
    send_attended = to_pair(attended_in, pair_attended, 2, 0)
    start_all(send_cot + send_normed + [send_attended])
    load_sent.wait()
    norm_rows(sent, normed, inverses, gains.at[pl.ds(1, 1), :], 64)
    send_two = halves(normed, pair_two, 3)
    start_all(send_two)
    wait_all([load_gate, load_up, load_cot, load_down])

    @pl.loop(0, units // step_cols)
    def _(step):
        cols = tile_cols(step)
        gate = dot(normed[...], gate_w[:, cols])
        up = dot(normed[...], up_w[:, cols])
        d_hidden = dot_rows(cot[...], down_w[cols, :])
        s = jax.nn.sigmoid(gate)
        activated = gate * s
        hidden[:, cols] = (activated * up).astype(BF)
        d_gate[:, cols] = (d_hidden * up * (s + activated * (1.0 - s))).astype(BF)
        d_up[:, cols] = (d_hidden * activated).astype(BF)
        for which in range(3):
            send_ff(step, which).start()

    gain_part[...] = jnp.zeros(gain_part.shape, F32)

    @pl.loop(0, count)
    def _(step):
        cols = tile_cols(step)
        product = dot_rows(d_gate[...], gate_w[cols, :]) + dot_rows(d_up[...], up_w[cols, :])
        gain_part[pl.ds(1, 1), cols] = jnp.sum(product * (sent[:, cols].astype(F32) * inverses[...]), axis=0, keepdims=True)
        grad_middle[:, cols] = product[:tile, :]
        send_part[:, cols] = product[tile:, :].astype(BF)
        for k in steps:
            send_z(0, send_part, two_recv, step, k).start()

    @pl.loop(0, units // step_cols)
    def _(step):
        for which in range(3):
            send_ff(step, which).wait_recv()

    for copy in send_cot + send_two:
        copy.wait_recv()
    pair_loads = [
        local(pair_ff[0], buffer_a, load.at[0]),
        local(pair_cot, cot_half, load.at[1]),
        local(pair_ff[1], buffer_b, load.at[2]),
        local(pair_two, two_half, load.at[3]),
        local(pair_ff[2], buffer_c, load.at[4]),
    ]
    start_all(pair_loads)
    wait_all(pair_loads)
    col_grads(0, hidden, buffer_a, cot, cot_half, units)
    row_grads(1, normed, two_half, d_gate, buffer_b, units)
    row_grads(2, normed, two_half, d_up, buffer_c, units)

    take(0, send_part, two_recv)

    @pl.loop(0, tile // 32)
    def _(step):
        rows = pl.ds(pl.multiple_of(step * 32, 32), 32)
        total = received(step * 32, 32, grad_middle[rows, :])
        result = cot[rows, :].astype(F32) + norm_back(total, sent[rows, :].astype(F32), gains[1:2, :])
        grad_middle[rows, :] = result
        branch[rows, :] = result.astype(BF)

    for k in steps:
        send_branch(k).start()
    keep_branch = local(branch, at_rows(branch_rows, 0, tile), keep.at[5])
    keep_branch.start()
    wait_all([load_middle, load_attended, load_qkv, load_out] + load_tables)
    fill_mask(bias, docs, ranks)

    @pl.loop(0, count)
    def _(step):
        cols = tile_cols(step)
        product = dot(hidden[...], down_w[:, cols])
        own_mlp[:, cols] = own_mlp[:, cols] + product[:tile, :]
        send_mlp[:, cols] = product[tile:, :].astype(BF)
        for k in steps:
            send_z(1, send_mlp, mlp_recv, step, k).start()

    load_weight = local(qkv_full, down_w.at[:, pl.ds(0, 3 * heads)], load.at[0])
    load_hidden = local(hidden_in, buffer_b, load.at[1])
    load_normed = local(normed_in, buffer_c, load.at[2])
    start_all([load_weight, load_hidden, load_normed])

    @pl.loop(0, count)
    def _(step):
        for k in steps:
            send_z(0, send_part, two_recv, step, k).wait_send()

    for k in steps:
        send_branch(k).wait_recv()
    keep_branch.wait()
    load_branch = local(branch_rows, buffer_a, load.at[3])
    load_branch.start()
    send_half = halves(branch_rows, pair_branch, 4)
    start_all(send_half)
    load_branch.wait()

    @pl.loop(0, heads // step_cols)
    def _(step):
        cols = tile_cols(step)
        d_attended[:, cols] = dot_rows(buffer_a[...], out_w[cols, :]).astype(BF)

    attend_back(qkv, d_attended, d_qkv, bias, cosine, sine, heads)
    send_qkv = to_pair(d_qkv, pair_qkv, 5, 0)
    send_qkv.start()
    wait_all([load_weight, load_hidden, load_normed])

    @pl.loop(0, count)
    def _(step):
        cols = tile_cols(step)
        product = dot_rows(d_qkv[...], down_w[cols, pl.ds(0, 3 * heads)])
        gain_part[pl.ds(0, 1), cols] = jnp.sum(
            product * (buffer_b[:, cols].astype(F32) * inverses_one[...]), axis=0, keepdims=True
        )
        input_grad[:, cols] = product[:tile, :]
        send_part[:, cols] = product[tile:, :].astype(BF)
        for k in steps:
            send_z(2, send_part, one_recv, step, k).start()

    def send_gain(flip):
        return remote(
            at_cols(gain_part, own ^ flip, width), at_rows(gain_recv, flip, 8), g_send.at[flip], g_recv.at[flip], "dp", own ^ flip
        )

    for flip in range(1, 8):
        send_gain(flip).start()

    for index in range(3):
        keep_grad(index).wait()
    send_qkv.wait_recv()
    for copy in send_half + send_normed + [send_attended]:
        copy.wait_recv()

    @pl.loop(0, units // step_cols)
    def _(step):
        for which in range(3):
            send_ff(step, which).wait_send()

    for copy in send_two:
        copy.wait_send()
    last_loads = [
        local(pair_qkv, normed.at[:, pl.ds(0, 3 * heads)], load.at[0]),
        local(pair_attended, cot.at[:, pl.ds(0, heads)], load.at[1]),
        local(pair_normed, two_half, load.at[2]),
        local(pair_branch, cot_half, load.at[3]),
    ]
    start_all(last_loads)
    wait_all(last_loads)
    row_grads(3, buffer_c, two_half, d_qkv, normed, 3 * heads)
    col_grads(4, attended, cot, buffer_a, cot_half, heads)

    for flip in range(1, 8):
        send_gain(flip).wait_recv()
    gain_sum = gain_part[:, pl.ds(pl.multiple_of(own * width, width), width)]
    for flip in range(1, 8):
        gain_sum = gain_sum + gain_recv[pl.ds(flip * 8, 8), :]
    gain_z[pl.ds(0, 8), :] = gain_sum

    def send_gain_z(k):
        peer = lax.rem(rank + k, ranks)
        return remote(
            gain_z.at[pl.ds(0, 8), :], gain_z.at[pl.ds(8 * k, 8), :], b_send.at[ranks + k], b_recv.at[ranks + k], "tensor", peer
        )

    for k in steps:
        send_gain_z(k).start()

    take(1, send_mlp, mlp_recv)

    @pl.loop(0, tile // 32)
    def _(step):
        rows = pl.ds(pl.multiple_of(step * 32, 32), 32)
        layer_out[rows, :] = received(step * 32, 32, own_mlp[rows, :]).astype(BF)

    take(2, send_part, one_recv)
    load_own = local(hidden_in.at[pl.ds(0, tile), :], branch, load.at[1])
    for k in steps:
        send_branch(k).wait_send()
    load_own.start()
    load_own.wait()

    @pl.loop(0, tile // 32)
    def _(step):
        rows = pl.ds(pl.multiple_of(step * 32, 32), 32)
        total = received(step * 32, 32, input_grad[rows, :])
        input_grad[rows, :] = grad_middle[rows, :] + norm_back(total, branch[rows, :].astype(F32), gains[0:1, :])

    for k in steps:
        send_gain_z(k).wait_recv()
    gain_all = gain_z[pl.ds(0, 8), :]
    for k in steps:
        gain_all = gain_all + gain_z[pl.ds(8 * k, 8), :]
    gain_total[...] = gain_all

    for index in range(5):
        for slot in range(1, 4):
            send_grad(index, slot).wait_recv()
    for index in range(3, 5):
        keep_grad(index).wait()
    for index in range(5):
        for slot in range(1, 4):
            send_grad(index, slot).wait_send()
    for flip in range(1, 8):
        send_gain(flip).wait_send()
    for k in steps:
        send_gain_z(k).wait_send()
    for copy in send_cot + send_normed + send_half + [send_attended, send_qkv]:
        copy.wait_send()

    @pl.loop(0, count)
    def _(step):
        for k in steps:
            send_z(1, send_mlp, mlp_recv, step, k).wait_send()
            send_z(2, send_part, one_recv, step, k).wait_send()


def back(sent, cot, hidden, weights, normed, qkv, attended, middle, cosine, sine, docs, inverses, gains, ranks):
    tokens, dim = sent.shape
    tile, heads, units = tokens // ranks, attended.shape[1], weights[2].shape[0]
    width, rest = gains.shape[1] // 8, tokens - tile
    dma = pltpu.SemaphoreType.DMA
    count = dim // 256
    return pl.pallas_call(
        partial(back_kernel, ranks),
        out_shape=[
            shape((4 * width, units), BF),
            shape((4 * width, units), BF),
            shape((units, 4 * width), BF),
            shape((4 * width, 3 * heads), BF),
            shape((heads, 4 * width), BF),
        ]
        + [shape((tokens, units), BF)] * 3
        + [
            shape((tokens, dim // 2), BF),
            shape((tokens, dim // 2), BF),
            shape((tokens, 3 * heads), BF),
            shape((tokens, heads), BF),
            shape((tokens, dim // 2), BF),
            shape((tokens, dim // 2), BF),
        ]
        + [shape((rest, dim), BF)] * 3
        + [
            shape((tokens, dim), BF),
            shape((tile, dim), BF),
            shape((tile, dim), F32),
            shape((8, width), F32),
        ],
        in_specs=[anyspace()] * 14 + [vmem()] * 3,
        out_specs=[anyspace()] * 18 + [vmem()] * 3,
        scratch_shapes=[
            pltpu.VMEM((dim, units), BF),
            pltpu.VMEM((dim, units), BF),
            pltpu.VMEM((units, dim), BF),
            pltpu.VMEM((tokens, dim), BF),
            pltpu.VMEM((tokens, dim), BF),
            pltpu.VMEM((tokens, dim), BF),
            pltpu.VMEM((tokens, units), BF),
            pltpu.VMEM((tokens, units), BF),
            pltpu.VMEM((tokens, units), BF),
            pltpu.VMEM((tokens, dim // 2), BF),
            pltpu.VMEM((tokens, dim // 2), BF),
            pltpu.VMEM((tokens, units), BF),
            pltpu.VMEM((tokens, units), BF),
            pltpu.VMEM((tokens, units), BF),
            pltpu.VMEM((heads, dim), BF),
            pltpu.VMEM((tokens, 3 * heads), BF),
            pltpu.VMEM((tokens, 3 * heads), BF),
            pltpu.VMEM((tokens, heads), BF),
            pltpu.VMEM((tokens, heads), BF),
            pltpu.VMEM((tokens, tokens), F32),
            pltpu.VMEM((tokens, 128), F32),
            pltpu.VMEM((tokens, 128), F32),
            pltpu.VMEM((tokens, 1), F32),
            pltpu.VMEM((tile, dim), F32),
            pltpu.VMEM((tile, dim), F32),
            pltpu.VMEM((rest, dim), BF),
            pltpu.VMEM((rest, dim), BF),
            pltpu.VMEM((8, dim), F32),
            pltpu.VMEM((64, width), F32),
            pltpu.VMEM((8 * ranks, width), F32),
            dma((units // 256, 3)),
            dma((units // 256, 3)),
            dma((6, 4)),
            dma((6, 4)),
            dma((3, count, ranks)),
            dma((3, count, ranks)),
            dma((2 * ranks,)),
            dma((2 * ranks,)),
            dma((5, 4)),
            dma((5, 4)),
            dma((8,)),
            dma((8,)),
            dma((10 + 2 * ranks,)),
            dma((6,)),
        ],
        compiler_params=pltpu.CompilerParams(vmem_limit_bytes=67000000, collective_id=1, has_side_effects=True),
        cost_estimate=cost(2 * tokens * dim * units * 9, 100e6),
        name="back",
    )(sent, cot, hidden, *weights, normed, qkv, attended, middle, cosine, sine, docs, inverses, gains)


def shift(values, step):
    size = lax.axis_size("tensor")
    return lax.ppermute(values, "tensor", [(index, (index + step) % size) for index in range(size)])


def gather_rows(values):
    return [values] + [shift(values, step) for step in range(1, lax.axis_size("tensor"))]


def scatter_rows(parts):
    total = parts[0].astype(F32)
    for step in range(1, len(parts)):
        total = total + shift(parts[step], -step).astype(F32)
    return total


def gather_weight(values, axis):
    return [None], [lax.all_gather(values, "dp", axis=axis, tiled=True)]


def scatter_full(left, right, axis):
    full = dot_cols(left, right).astype(BF)
    return lax.psum_scatter(full, "dp", scatter_dimension=axis, tiled=True).astype(F32)


def sum_parts(parts, width, axis):
    pieces = jnp.split(parts, 4, axis=axis)
    return sum(piece.astype(F32) for piece in pieces)


def rotary(length):
    half_size = HEAD_DIM // 2
    frequency = ROPE_BASE ** (-jnp.arange(half_size, dtype=F32) / half_size)
    angles = jnp.arange(length).astype(F32)[:, None] * frequency[None, :]
    cosine, sine = jnp.cos(angles), jnp.sin(angles)
    cosine = jnp.tile(cosine, (1, 8))
    sine = jnp.tile(jnp.concatenate([-sine, sine], axis=1), (1, 4))
    return cosine, sine


def position_tables(doc_ids, ranks):
    length = doc_ids.shape[0]
    token_index = jnp.arange(length, dtype=jnp.int32)
    before = jnp.concatenate([doc_ids[:1] - 1, doc_ids[:-1]])
    doc_start = lax.cummax(jnp.where(doc_ids != before, token_index, 0), axis=0)
    order = (lax.axis_index("tensor") - jnp.arange(ranks)) % ranks
    last = token_index.reshape(ranks, -1)[order].reshape(length)
    first = doc_start.reshape(ranks, -1)[order].reshape(length)
    cosine, sine = (table.reshape(ranks, -1, 256)[order].reshape(length, 256) for table in rotary(length))
    return cosine, sine, first[:, None], last[:, None], last[None, :]


def rms_back(grad_rows_, values, gain):
    inverse = lax.rsqrt(jnp.mean(values * values, axis=-1, keepdims=True) + EPSILON)
    scaled = grad_rows_ * gain
    return inverse * (scaled - values * inverse * inverse * jnp.mean(scaled * values, axis=-1, keepdims=True))


def body(
    hidden_in,
    out_cotangent,
    doc_ids,
    attn_gain,
    query_weight,
    key_weight,
    value_weight,
    out_weight,
    mlp_gain,
    gate_weight,
    up_weight,
    down_weight,
):
    ranks, groups = lax.axis_size("tensor"), lax.axis_size("dp")
    paired = (groups, ranks) == (8, 4)
    width, heads = query_weight.shape
    dim = hidden_in.shape[1]

    if paired:
        pad = jnp.zeros((6, width), F32)
        own_gains = jnp.concatenate([attn_gain[None].astype(F32), mlp_gain[None].astype(F32), pad], axis=0)
        weights = (query_weight, key_weight, value_weight, out_weight, down_weight, gate_weight, up_weight)
        docs, turns = doc_ids.reshape(ranks, -1), rotary(doc_ids.shape[0])
        front_out = front(hidden_in, out_cotangent, own_gains, weights, *turns, docs, ranks)
        full, (hidden_rows, cot_rows, sent_rows) = front_out[:5], front_out[5:8]
        normed, qkv, attended, inverses, middle, gains = front_out[8:]
        back_out = back(
            sent_rows, cot_rows, hidden_rows, full, normed, qkv, attended, middle, *turns, docs, inverses, gains, ranks
        )
        gate_grad, up_grad, down_grad, qkv_grad, out_proj_grad = (
            sum_parts(part, width, axis) for part, axis in zip(back_out[:5], (0, 0, 1, 0, 1))
        )
        layer_out, input_grad, gain_total = back_out[18:]
        share = width // ranks
        gain_grads = lax.dynamic_slice_in_dim(gain_total, lax.axis_index("tensor") * share, share, axis=1)
    else:
        tables = position_tables(doc_ids, ranks)
        input_local = hidden_in.astype(F32)
        hidden_rows = gather_rows(hidden_in)
        gains = lax.all_gather(jnp.stack([attn_gain, mlp_gain]), "dp", axis=1, tiled=True).astype(F32)
        attn_scale, mlp_scale = gains[:1], gains[1:]
        qkv_weight = jnp.concatenate([query_weight, key_weight, value_weight], axis=1)
        tags, qkv_pieces = gather_weight(qkv_weight, 0)
        tags, out_pieces = gather_weight(out_weight, 1)
        cot_rows = gather_rows(out_cotangent)
        tags, down_pieces = gather_weight(down_weight, 1)
        tags, gate_pieces = gather_weight(gate_weight, 0)
        tags, up_pieces = gather_weight(up_weight, 0)
        normed, qkv, attended, inverses, *branch_parts = attn_fwd(
            hidden_rows, attn_scale, tables, tags, width, qkv_pieces, out_pieces
        )
        middle = input_local + scatter_rows(branch_parts)
        sent = middle.astype(BF)
        sent_rows = gather_rows(sent)
        cot_full = jnp.concatenate(cot_rows, axis=0)
        normed_two, hidden, d_gate, d_up, mlp_gain_part, *two_parts = mlp(
            sent_rows, cot_rows, mlp_scale, tags, width, gate_pieces, up_pieces, down_pieces, ranks
        )
        grad_two_rows = scatter_rows(two_parts)
        grad_middle = out_cotangent.astype(F32) + rms_back(grad_two_rows, sent.astype(F32), mlp_scale)
        branch_rows = gather_rows(grad_middle.astype(BF))
        down_grad = scatter_full(hidden, cot_full, 1)
        gate_grad = scatter_full(normed_two, d_gate, 0)
        up_grad = scatter_full(normed_two, d_up, 0)
        mlp_rows = scatter_rows(mlp_out(hidden, ranks, dim, tags, width, down_pieces))
        layer_out = (middle + mlp_rows).astype(BF)
        branch_full, d_qkv, attn_gain_part, *one_parts = attn_bwd(
            branch_rows, hidden_rows, qkv, inverses, tables, tags, width, qkv_pieces, out_pieces, ranks
        )
        out_proj_grad = scatter_full(attended, branch_full, 1)
        qkv_grad = scatter_full(normed, d_qkv, 0)
        grad_one_rows = scatter_rows(one_parts)
        input_grad = grad_middle + rms_back(grad_one_rows, input_local, attn_scale)
        gain_parts = jnp.concatenate([attn_gain_part, mlp_gain_part], axis=0)
        gain_grads = lax.psum_scatter(gain_parts, ("dp", "tensor"), scatter_dimension=1, tiled=True)
    return (
        layer_out,
        input_grad,
        gain_grads[0],
        qkv_grad[:, :heads],
        qkv_grad[:, heads : 2 * heads],
        qkv_grad[:, 2 * heads :],
        out_proj_grad,
        gain_grads[1],
        gate_grad,
        up_grad,
        down_grad,
    )


def solution(mesh):
    return jax.shard_map(
        body,
        mesh=mesh,
        in_specs=(
            P(("dp", "tensor"), None),
            P(("dp", "tensor"), None),
            P("dp"),
            P("dp"),
            P("dp", "tensor"),
            P("dp", "tensor"),
            P("dp", "tensor"),
            P("tensor", "dp"),
            P("dp"),
            P("dp", "tensor"),
            P("dp", "tensor"),
            P("tensor", "dp"),
        ),
        out_specs=(
            P(("dp", "tensor"), None),
            P(("dp", "tensor"), None),
            P(("dp", "tensor")),
            P("dp", "tensor"),
            P("dp", "tensor"),
            P("dp", "tensor"),
            P("tensor", "dp"),
            P(("dp", "tensor")),
            P("dp", "tensor"),
            P("dp", "tensor"),
            P("tensor", "dp"),
        ),
        check_vma=False,
    )
```

```python
from functools import partial

import jax
import jax.numpy as jnp
from jax import lax
from jax.experimental import pallas as pl
from jax.experimental.pallas import tpu as pltpu
from jax.sharding import PartitionSpec as P

HEAD_DIM = 64
EPSILON = 1e-05
ROPE_BASE = 130000.0
NEGATIVE = -1e30
VMEM_LIMIT = 63 * 1024 * 1024
BF = jnp.bfloat16
F32 = jnp.float32


def dot(left, right):
    return jnp.dot(left, right, preferred_element_type=F32)


def dot_rows(left, right):
    return lax.dot_general(left, right, (((1,), (1,)), ((), ())), preferred_element_type=F32)


def dot_cols(left, right):
    return lax.dot_general(left, right, (((0,), (0,)), ((), ())), preferred_element_type=F32)


def vmem():
    return pl.BlockSpec(memory_space=pltpu.VMEM)


def anyspace():
    return pl.BlockSpec(memory_space=pl.ANY)


def params():
    return pltpu.CompilerParams(vmem_limit_bytes=VMEM_LIMIT)


def cost(flops, nbytes):
    return pl.CostEstimate(flops=int(flops), bytes_accessed=int(nbytes), transcendentals=0)


def shape(dims, kind):
    return jax.ShapeDtypeStruct(dims, kind)


def place_copies(tags, pieces, target, sem, axis, width):
    own = lax.axis_index("dp")
    copies = []
    for slot, (tag, piece) in enumerate(zip(tags, pieces)):
        if tag is None:
            where = target
        else:
            start = pl.multiple_of((own ^ tag) * width, width)
            where = target.at[pl.ds(start, width), :] if axis == 0 else target.at[:, pl.ds(start, width)]
        copies.append(pltpu.make_async_copy(piece, where, sem.at[slot]))
    return copies


def row_copies(pieces, target, sem):
    copies = []
    for slot, piece in enumerate(pieces):
        rows = piece.shape[0]
        copies.append(pltpu.make_async_copy(piece, target.at[pl.ds(slot * rows, rows), :], sem.at[slot]))
    return copies


def start_all(copies):
    for copy in copies:
        copy.start()


def wait_all(copies):
    for copy in copies:
        copy.wait()


def turn(values, cosine, sine):
    width = values.shape[1]
    lane = lax.broadcasted_iota(jnp.int32, values.shape, 1)
    partner = jnp.where(
        lax.rem(lane, HEAD_DIM) < HEAD_DIM // 2,
        pltpu.roll(values, width - HEAD_DIM // 2, 1),
        pltpu.roll(values, HEAD_DIM // 2, 1),
    )
    return values * cosine + partner * sine


def norm_rows(source, target, inverses, gain, tile):
    @pl.loop(0, source.shape[0] // tile)
    def _(step):
        rows = pl.ds(pl.multiple_of(step * tile, tile), tile)
        values = source[rows, :].astype(F32)
        inverse = lax.rsqrt(jnp.mean(values * values, axis=-1, keepdims=True) + EPSILON)
        inverses[rows, :] = inverse
        target[rows, :] = (values * inverse * gain[...]).astype(BF)


def fill_bias(bias, first, last, key_index):
    keys = key_index[...]
    bias[...] = jnp.where((keys >= first[...]) & (keys <= last[...]), 0.0, NEGATIVE)


def head_lanes(width, half):
    lane = lax.broadcasted_iota(jnp.int32, (1, width), 1)
    return (lax.div(lane, HEAD_DIM) == half).astype(F32)


def probabilities(query, key, bias):
    scores = dot_rows(query, key) + bias
    weights = jnp.exp(scores - jnp.max(scores, axis=-1, keepdims=True))
    return weights * (1.0 / jnp.sum(weights, axis=-1, keepdims=True))


def attend(qkv, attended, bias, heads):
    @pl.loop(0, heads // 128)
    def _(pair):
        base = pl.multiple_of(pair * 128, 128)
        query = qkv[:, pl.ds(base, 128)]
        key = qkv[:, pl.ds(heads + base, 128)]
        value = qkv[:, pl.ds(2 * heads + base, 128)]
        total = None
        for half in range(2):
            lanes = head_lanes(128, half).astype(BF)
            probs = probabilities(query * (lanes * HEAD_DIM ** (-0.5)), key, bias[...])
            term = dot(probs.astype(BF), value * lanes)
            total = term if total is None else total + term
        attended[:, pl.ds(base, 128)] = total.astype(BF)


def attn_fwd_kernel(tags, width, nrow, *refs):
    npiece = len(tags)
    rows_in = refs[:nrow]
    gain, cosine, sine, first, last, key_index = refs[nrow : nrow + 6]
    rest = refs[nrow + 6 :]
    qkv_in, out_in = rest[:npiece], rest[npiece : 2 * npiece]
    rest = rest[2 * npiece :]
    normed, qkv, attended, inverses = rest[:4]
    parts = rest[4 : 4 + nrow]
    hidden, qkv_w, out_w, bias, sem_rows, sem_qkv, sem_out = rest[4 + nrow :]
    load_rows = row_copies(rows_in, hidden, sem_rows)
    load_qkv = place_copies(tags, qkv_in, qkv_w, sem_qkv, 0, width)
    load_out = place_copies(tags, out_in, out_w, sem_out, 1, width)
    start_all(load_rows + load_qkv + load_out)
    fill_bias(bias, first, last, key_index)
    wait_all(load_rows)
    norm_rows(hidden, normed, inverses, gain, 64)
    wait_all(load_qkv)
    heads = attended.shape[1]
    step_cols = 256

    @pl.loop(0, 2 * heads // step_cols)
    def _(step):
        cols = pl.ds(pl.multiple_of(step * step_cols, step_cols), step_cols)
        qkv[:, cols] = turn(dot(normed[...], qkv_w[:, cols]), cosine[...], sine[...]).astype(BF)

    @pl.loop(2 * heads // step_cols, 3 * heads // step_cols)
    def _(step):
        cols = pl.ds(pl.multiple_of(step * step_cols, step_cols), step_cols)
        qkv[:, cols] = dot(normed[...], qkv_w[:, cols]).astype(BF)

    attend(qkv, attended, bias, heads)
    wait_all(load_out)
    tile = parts[0].shape[0]

    @pl.loop(0, out_w.shape[1] // step_cols)
    def _(step):
        cols = pl.ds(pl.multiple_of(step * step_cols, step_cols), step_cols)
        product = dot(attended[...], out_w[:, cols])
        for slot, part in enumerate(parts):
            part[:, cols] = product[slot * tile : (slot + 1) * tile, :].astype(part.dtype)


def attn_fwd(rows, gain, tables, tags, width, qkv_pieces, out_pieces):
    nrow, (tile, dim) = len(rows), rows[0].shape
    tokens = nrow * tile
    heads = out_pieces[0].shape[0]
    npiece = len(tags)
    return pl.pallas_call(
        partial(attn_fwd_kernel, tags, width, nrow),
        out_shape=[
            shape((tokens, dim), BF),
            shape((tokens, 3 * heads), BF),
            shape((tokens, heads), BF),
            shape((tokens, 1), F32),
        ]
        + [shape((tile, dim), F32 if slot == 0 else BF) for slot in range(nrow)],
        in_specs=[anyspace()] * nrow + [vmem()] * 6 + [anyspace()] * (2 * npiece),
        out_specs=[vmem()] * (4 + nrow),
        scratch_shapes=[
            pltpu.VMEM((tokens, dim), BF),
            pltpu.VMEM((dim, 3 * heads), BF),
            pltpu.VMEM((heads, dim), BF),
            pltpu.VMEM((tokens, tokens), F32),
            pltpu.SemaphoreType.DMA((nrow,)),
            pltpu.SemaphoreType.DMA((npiece,)),
            pltpu.SemaphoreType.DMA((npiece,)),
        ],
        compiler_params=params(),
        cost_estimate=cost(2 * tokens * dim * 4 * heads * 3, 20e6),
        name="attn_fwd",
    )(*rows, gain, *tables, *qkv_pieces, *out_pieces)


def attend_back(qkv, d_attended, d_qkv, bias, cosine, sine, heads):
    score_scale = HEAD_DIM ** (-0.5)

    @pl.loop(0, heads // 128)
    def _(pair):
        base = pl.multiple_of(pair * 128, 128)
        query = qkv[:, pl.ds(base, 128)]
        key = qkv[:, pl.ds(heads + base, 128)]
        value = qkv[:, pl.ds(2 * heads + base, 128)]
        grad = d_attended[:, pl.ds(base, 128)]
        sums = [0.0, 0.0, 0.0]
        for half in range(2):
            lanes = head_lanes(128, half).astype(BF)
            own_query = query * (lanes * score_scale)
            own_grad = grad * lanes
            probs = probabilities(own_query, key, bias[...])
            d_value = dot_cols(probs.astype(BF), own_grad)
            d_probs = dot_rows(own_grad, value)
            delta = jnp.sum(probs * d_probs, axis=-1, keepdims=True)
            d_scores = (probs * (d_probs - delta)).astype(BF)
            d_query = dot(d_scores, key * lanes) * score_scale
            d_key = dot_cols(d_scores, own_query)
            sums = [sums[0] + d_query, sums[1] + d_key, sums[2] + d_value]
        back = -sine[:, :128]
        d_qkv[:, pl.ds(base, 128)] = turn(sums[0], cosine[:, :128], back).astype(BF)
        d_qkv[:, pl.ds(heads + base, 128)] = turn(sums[1], cosine[:, :128], back).astype(BF)
        d_qkv[:, pl.ds(2 * heads + base, 128)] = sums[2].astype(BF)


def attn_bwd_kernel(tags, width, nrow, npart, *refs):
    npiece = len(tags)
    nhid, nrow = nrow[1], nrow[0]
    rows_in, hidden_in = refs[:nrow], refs[nrow : nrow + nhid]
    refs = refs[nrow + nhid :]
    qkv, inverses, cosine, sine, first, last, key_index = refs[:7]
    rest = refs[7:]
    qkv_in, out_in = rest[:npiece], rest[npiece : 2 * npiece]
    rest = rest[2 * npiece :]
    branch, d_qkv, gain_grad = rest[:3]
    parts = rest[3 : 3 + npart]
    hidden, d_attended, qkv_w, out_w, bias, sem_rows, sem_x, sem_qkv, sem_out = rest[3 + npart :]
    load_rows = row_copies(rows_in, branch, sem_rows)
    load_x = row_copies(hidden_in, hidden, sem_x)
    load_out = place_copies(tags, out_in, out_w, sem_out, 1, width)
    load_qkv = place_copies(tags, qkv_in, qkv_w, sem_qkv, 0, width)
    start_all(load_rows + load_out + load_qkv + load_x)
    fill_bias(bias, first, last, key_index)
    wait_all(load_rows)
    wait_all(load_out)
    heads = out_w.shape[0]
    step_cols = 256

    @pl.loop(0, heads // step_cols)
    def _(step):
        cols = pl.ds(pl.multiple_of(step * step_cols, step_cols), step_cols)
        d_attended[:, cols] = dot_rows(branch[...], out_w[cols, :]).astype(BF)

    attend_back(qkv, d_attended, d_qkv, bias, cosine, sine, heads)
    wait_all(load_qkv)
    wait_all(load_x)
    tile = parts[0].shape[0]

    @pl.loop(0, qkv_w.shape[0] // step_cols)
    def _(step):
        cols = pl.ds(pl.multiple_of(step * step_cols, step_cols), step_cols)
        product = dot_rows(d_qkv[...], qkv_w[cols, :])
        gain_grad[:, cols] = jnp.sum(product * (hidden[:, cols].astype(F32) * inverses[...]), axis=0, keepdims=True)
        for slot, part in enumerate(parts):
            part[:, cols] = product[slot * tile : (slot + 1) * tile, :].astype(part.dtype)


def attn_bwd(rows, hidden, qkv, inverses, tables, tags, width, qkv_pieces, out_pieces, npart):
    nrow, nhid, dim = len(rows), len(hidden), rows[0].shape[1]
    tokens = qkv.shape[0]
    tile = tokens // npart
    heads = out_pieces[0].shape[0]
    npiece = len(tags)
    return pl.pallas_call(
        partial(attn_bwd_kernel, tags, width, (nrow, nhid), npart),
        out_shape=[shape((tokens, dim), BF), shape((tokens, 3 * heads), BF), shape((1, dim), F32)]
        + [shape((tile, dim), F32 if slot == 0 else BF) for slot in range(npart)],
        in_specs=[anyspace()] * (nrow + nhid) + [vmem()] * 7 + [anyspace()] * (2 * npiece),
        out_specs=[vmem()] * (3 + npart),
        scratch_shapes=[
            pltpu.VMEM((tokens, dim), BF),
            pltpu.VMEM((tokens, heads), BF),
            pltpu.VMEM((dim, 3 * heads), BF),
            pltpu.VMEM((heads, dim), BF),
            pltpu.VMEM((tokens, tokens), F32),
            pltpu.SemaphoreType.DMA((nrow,)),
            pltpu.SemaphoreType.DMA((nhid,)),
            pltpu.SemaphoreType.DMA((npiece,)),
            pltpu.SemaphoreType.DMA((npiece,)),
        ],
        compiler_params=params(),
        cost_estimate=cost(2 * tokens * dim * 4 * heads * 6, 30e6),
        name="attn_bwd",
    )(*rows, *hidden, qkv, inverses, *tables, *qkv_pieces, *out_pieces)


def mlp_kernel(tags, width, nrow, npart, *refs):
    npiece = len(tags)
    sent_in, cot_in = refs[:nrow], refs[nrow : 2 * nrow]
    gain = refs[2 * nrow]
    rest = refs[2 * nrow + 1 :]
    gate_in, up_in, down_in = rest[:npiece], rest[npiece : 2 * npiece], rest[2 * npiece : 3 * npiece]
    rest = rest[3 * npiece :]
    normed, hidden, d_gate, d_up, gain_grad = rest[:5]
    parts = rest[5 : 5 + npart]
    sent, cot, inverses, gate_w, up_w, down_w, sem_sent, sem_cot, sem_gate, sem_up, sem_down = rest[5 + npart :]
    load_sent = row_copies(sent_in, sent, sem_sent)
    load_cot = row_copies(cot_in, cot, sem_cot)
    load_gate = place_copies(tags, gate_in, gate_w, sem_gate, 0, width)
    load_up = place_copies(tags, up_in, up_w, sem_up, 0, width)
    load_down = place_copies(tags, down_in, down_w, sem_down, 1, width)
    start_all(load_sent + load_cot + load_gate + load_up + load_down)
    wait_all(load_sent)
    norm_rows(sent, normed, inverses, gain, 64)
    wait_all(load_cot)
    wait_all(load_gate)
    wait_all(load_up)
    wait_all(load_down)
    step_cols = 256

    @pl.loop(0, gate_w.shape[1] // step_cols)
    def _(step):
        cols = pl.ds(pl.multiple_of(step * step_cols, step_cols), step_cols)
        gate = dot(normed[...], gate_w[:, cols])
        up = dot(normed[...], up_w[:, cols])
        d_hidden = dot_rows(cot[...], down_w[cols, :])
        s = jax.nn.sigmoid(gate)
        activated = gate * s
        hidden[:, cols] = (activated * up).astype(BF)
        d_gate[:, cols] = (d_hidden * up * (s + activated * (1.0 - s))).astype(BF)
        d_up[:, cols] = (d_hidden * activated).astype(BF)

    tile = parts[0].shape[0]

    @pl.loop(0, gate_w.shape[0] // step_cols)
    def _(step):
        cols = pl.ds(pl.multiple_of(step * step_cols, step_cols), step_cols)
        product = dot_rows(d_gate[...], gate_w[cols, :]) + dot_rows(d_up[...], up_w[cols, :])
        gain_grad[:, cols] = jnp.sum(product * (sent[:, cols].astype(F32) * inverses[...]), axis=0, keepdims=True)
        for slot, part in enumerate(parts):
            part[:, cols] = product[slot * tile : (slot + 1) * tile, :].astype(part.dtype)


def mlp(sent, cot, gain, tags, width, gate_pieces, up_pieces, down_pieces, npart):
    nrow, dim = len(sent), sent[0].shape[1]
    tokens = nrow * sent[0].shape[0]
    tile = tokens // npart
    units = gate_pieces[0].shape[1]
    npiece = len(tags)
    return pl.pallas_call(
        partial(mlp_kernel, tags, width, nrow, npart),
        out_shape=[shape((tokens, dim), BF)]
        + [shape((tokens, units), BF)] * 3
        + [shape((1, dim), F32)]
        + [shape((tile, dim), F32 if slot == 0 else BF) for slot in range(npart)],
        in_specs=[anyspace()] * (2 * nrow) + [vmem()] + [anyspace()] * (3 * npiece),
        out_specs=[vmem()] * (5 + npart),
        scratch_shapes=[
            pltpu.VMEM((tokens, dim), BF),
            pltpu.VMEM((tokens, dim), BF),
            pltpu.VMEM((tokens, 1), F32),
            pltpu.VMEM((dim, units), BF),
            pltpu.VMEM((dim, units), BF),
            pltpu.VMEM((units, dim), BF),
            pltpu.SemaphoreType.DMA((nrow,)),
            pltpu.SemaphoreType.DMA((nrow,)),
            pltpu.SemaphoreType.DMA((npiece,)),
            pltpu.SemaphoreType.DMA((npiece,)),
            pltpu.SemaphoreType.DMA((npiece,)),
        ],
        compiler_params=params(),
        cost_estimate=cost(2 * tokens * dim * units * 5, 40e6),
        name="mlp",
    )(*sent, *cot, gain, *gate_pieces, *up_pieces, *down_pieces)


def mlp_out_kernel(tags, width, *refs):
    npiece = len(tags)
    hidden, down_in = refs[0], refs[1 : 1 + npiece]
    *parts, down_w, sem_down = refs[1 + npiece :]
    load_down = place_copies(tags, down_in, down_w, sem_down, 1, width)
    start_all(load_down)
    wait_all(load_down)
    tile, step_cols = parts[0].shape[0], 256

    @pl.loop(0, down_w.shape[1] // step_cols)
    def _(step):
        cols = pl.ds(pl.multiple_of(step * step_cols, step_cols), step_cols)
        product = dot(hidden[...], down_w[:, cols])
        for slot, part in enumerate(parts):
            part[:, cols] = product[slot * tile : (slot + 1) * tile, :].astype(part.dtype)


def mlp_out(hidden, nrow, dim, tags, width, down_pieces):
    tokens, units = hidden.shape
    tile, npiece = tokens // nrow, len(tags)
    return pl.pallas_call(
        partial(mlp_out_kernel, tags, width),
        out_shape=[shape((tile, dim), F32 if slot == 0 else BF) for slot in range(nrow)],
        in_specs=[vmem()] + [anyspace()] * npiece,
        out_specs=[vmem()] * nrow,
        scratch_shapes=[pltpu.VMEM((units, dim), BF), pltpu.SemaphoreType.DMA((npiece,))],
        compiler_params=params(),
        cost_estimate=cost(2 * tokens * dim * units, 14e6),
        name="mlp_out",
    )(hidden, *down_pieces)


def slice_of(slot, width, own):
    index = lax.axis_index("dp")
    owner = index ^ (2 * slot)
    return pl.ds(pl.multiple_of((owner if own else lax.div(owner, 2)) * width, width), width)


MESH = pl.DeviceIdType.MESH
NEAR = (2, 4, 6)


def remote(source, target, send_sem, recv_sem, axis, peer):
    return pltpu.make_async_remote_copy(
        src_ref=source,
        dst_ref=target,
        send_sem=send_sem,
        recv_sem=recv_sem,
        device_id={axis: peer},
        device_id_type=MESH,
    )


def meet(ranks):
    own, rank = lax.axis_index("dp"), lax.axis_index("tensor")
    barrier = pltpu.get_barrier_semaphore()
    for flip in range(1, 8):
        pl.semaphore_signal(barrier, inc=1, device_id={"dp": own ^ flip}, device_id_type=MESH)
    for step in range(1, ranks):
        pl.semaphore_signal(barrier, inc=1, device_id={"tensor": lax.rem(rank + step, ranks)}, device_id_type=MESH)
    pl.semaphore_wait(barrier, ranks + 6)


def at_cols(ref, index, width):
    return ref.at[:, pl.ds(pl.multiple_of(index * width, width), width)]


def at_rows(ref, index, width):
    return ref.at[pl.ds(pl.multiple_of(index * width, width), width), :]


def fill_mask(bias, docs, ranks):
    rank = lax.axis_index("tensor")
    tile = docs.shape[1]
    blocks = [lax.rem(rank - slot + ranks, ranks) for slot in range(ranks)]
    own_docs = [jnp.broadcast_to(docs[pl.ds(block, 1), :].astype(F32), (tile, tile)) for block in blocks]
    turned = [jnp.transpose(values) for values in own_docs]
    row = lax.broadcasted_iota(jnp.int32, (tile, tile), 0)
    lane = lax.broadcasted_iota(jnp.int32, (tile, tile), 1)
    for q in range(ranks):
        for k in range(ranks):
            same = turned[q] == own_docs[k]
            before = row + blocks[q] * tile >= lane + blocks[k] * tile
            bias[q * tile : (q + 1) * tile, k * tile : (k + 1) * tile] = jnp.where(same & before, 0.0, NEGATIVE)


def either(rank, *choices):
    result = rank == choices[0]
    for choice in choices[1:]:
        result = result | (rank == choice)
    return result


class RowGather:
    def __init__(self, rank, source, landing, tile, send, recv, kind):
        self.rank = rank

        def copy(origin, slot, target, step, sem):
            peer = lax.rem(rank + step + 4, 4)
            return remote(origin, at_rows(landing, target, tile), send.at[kind, sem], recv.at[kind, target], "tensor", peer)

        self.direct = [None] + [copy(source, 0, step, step, step) for step in (1, 2, 3)]
        self.up = copy(at_rows(landing, 2, tile), 2, 3, 1, 0)
        self.down = copy(at_rows(landing, 2, tile), 2, 1, -1, 0)

    def start(self):
        self.direct[2].start()
        pl.when(self.rank < 3)(self.direct[1].start)
        pl.when(self.rank > 0)(self.direct[3].start)

    def relay(self):
        @pl.when(self.rank == 2)
        def _():
            self.direct[2].wait_recv()
            self.up.start()

        @pl.when(self.rank == 1)
        def _():
            self.direct[2].wait_recv()
            self.down.start()

    def wait(self):
        pl.when(either(self.rank, 0, 3))(self.direct[2].wait_recv)
        self.direct[1].wait_recv()
        self.direct[3].wait_recv()

    def finish(self):
        self.direct[2].wait_send()
        pl.when(self.rank < 3)(self.direct[1].wait_send)
        pl.when(self.rank > 0)(self.direct[3].wait_send)
        pl.when(self.rank == 2)(self.up.wait_send)
        pl.when(self.rank == 1)(self.down.wait_send)


class RowScatter:
    def __init__(self, rank, source, landing, merge, tile, step_cols, send, recv):
        self.rank, self.tile, self.source = rank, tile, source
        self.merge_in = merge
        self.count = source.shape[1] // step_cols
        self.cols = lambda step: pl.ds(pl.multiple_of(step * step_cols, step_cols), step_cols)

        def copy(step, k):
            rows, cols = pl.ds((k - 1) * tile, tile), self.cols(step)
            return remote(
                source.at[rows, cols],
                landing.at[rows, cols],
                send.at[step, k],
                recv.at[step, k],
                "tensor",
                lax.rem(rank - k + 4, 4),
            )

        def far(step, k, peer):
            rows, cols = pl.ds((k - 1) * tile, tile), self.cols(step)
            return remote(
                source.at[rows, cols], merge.at[:, cols], send.at[step, k], recv.at[step, 0], "tensor", peer
            )

        self.copy, self.far = copy, far

    def start_first(self, step):
        pl.when(self.rank == 0)(self.far(step, 1, 1).start)
        pl.when(self.rank == 3)(self.far(step, 3, 2).start)

        @pl.when(either(self.rank, 1, 2))
        def _():
            self.copy(step, 1).start()
            self.copy(step, 3).start()

    def start_rest(self):
        @pl.when(either(self.rank, 0, 3))
        def _():
            @pl.loop(0, self.count)
            def _(step):
                self.copy(step, 2).start()

        @pl.when(self.rank == 0)
        def _():
            @pl.loop(0, self.count)
            def _(step):
                self.copy(step, 3).start()

        @pl.when(self.rank == 3)
        def _():
            @pl.loop(0, self.count)
            def _(step):
                self.copy(step, 1).start()

    def merge(self, staged=None, sem=None):
        @pl.when(either(self.rank, 1, 2))
        def _():
            rows = pl.ds(self.tile, self.tile)
            other = self.merge_in if staged is None else staged
            if staged is not None:

                @pl.loop(0, self.count)
                def _(step):
                    self.far(step, 1, 1).wait_recv()

                load = pltpu.make_async_copy(self.merge_in, staged, sem)
                load.start()
                load.wait()

            @pl.loop(0, self.count)
            def _(step):
                cols = self.cols(step)
                if staged is None:
                    self.far(step, 1, 1).wait_recv()
                total = self.source[rows, cols].astype(F32) + other[:, cols].astype(F32)
                self.source[rows, cols] = total.astype(BF)
                self.copy(step, 2).start()

    def wait(self):
        @pl.loop(0, self.count)
        def _(step):
            self.copy(step, 2).wait_recv()

        @pl.when(self.rank != 3)
        def _():
            @pl.loop(0, self.count)
            def _(step):
                self.copy(step, 1).wait_recv()

        @pl.when(self.rank != 0)
        def _():
            @pl.loop(0, self.count)
            def _(step):
                self.copy(step, 3).wait_recv()

    def clear(self, target):
        rows = self.tile

        @pl.when(self.rank == 3)
        def _():
            target[:rows, :] = jnp.zeros((rows, target.shape[1]), target.dtype)

        @pl.when(self.rank == 0)
        def _():
            target[2 * rows :, :] = jnp.zeros((rows, target.shape[1]), target.dtype)

    def finish(self):
        @pl.loop(0, self.count)
        def _(step):
            for k in (1, 2, 3):
                self.copy(step, k).wait_send()


def front_kernel(ranks, *refs):
    hidden_in, cot_in, gains_in = refs[:3]
    weights_in = refs[3:10]
    cosine_in, sine_in, docs = refs[10:13]
    qkv_full, out_full, down_full, gate_full, up_full, hidden_rows, cot_rows, sent_rows = refs[13:21]
    normed, qkv, attended, inverses, middle, gains = refs[21:27]
    hidden, qkv_w, out_w, cosine, sine, bias, part, send_part, recv_part, merge_part, sent = refs[27:38]
    stage = refs[38:45]
    (w_send, w_recv, z_send, z_recv, p_send, p_recv, g_send, g_recv, load, keep) = refs[45:]
    own, rank = lax.axis_index("dp"), lax.axis_index("tensor")
    tile, dim = hidden_in.shape
    width = weights_in[0].shape[0]
    heads = weights_in[0].shape[1]
    step_cols = 256
    count = dim // step_cols

    def slot_of(index, owner, part=None):
        ref = (qkv_full, qkv_full, qkv_full, out_full, down_full, gate_full, up_full)[index]
        rows = weights_in[index].shape[0]
        size = rows if part is None else rows // 2
        start = 0 if part is None else part * size
        if index in (3, 4):
            return ref.at[pl.ds(start, size), pl.ds(pl.multiple_of(owner * width, width), width)]
        rows = pl.ds(pl.multiple_of(owner * width + start, size), size)
        return ref.at[rows, pl.ds(index * heads, heads)] if index < 3 else ref.at[rows, :]

    def send_weight(index, flip):
        return remote(
            weights_in[index], slot_of(index, own), w_send.at[index, flip], w_recv.at[index, flip], "dp", own ^ flip
        )

    def relay_weight(index, part):
        place = slot_of(index, own ^ (4 - 2 * part), part)
        tag = 6 + part
        return remote(place, place, w_send.at[index, tag], w_recv.at[index, tag], "dp", own ^ (2 + 2 * part))

    def pass_weight(index, flip):
        place = slot_of(index, own ^ flip)
        tag = {2: 3, 4: 5, 6: 8}[flip]
        return remote(place, place, w_send.at[index, tag], w_recv.at[index, tag], "dp", own ^ 1)

    def relay_weights(indices):
        for index in indices:
            send_weight(index, 4).wait_recv()
            relay_weight(index, 0).start()
            send_weight(index, 2).wait_recv()
            relay_weight(index, 1).start()
            pass_weight(index, 4).start()
            pass_weight(index, 2).start()

    def pass_weights(indices):
        for index in indices:
            relay_weight(index, 0).wait_recv()
            relay_weight(index, 1).wait_recv()
            pass_weight(index, 6).start()

    def finish(indices):
        for index in indices:
            send_weight(index, 1).wait_recv()
            for flip in NEAR:
                pass_weight(index, flip).wait_recv()

    def send_gain(flip):
        return remote(gains_in, at_cols(gains, own, width), g_send.at[flip], g_recv.at[flip], "dp", own ^ flip)

    gather_hidden = RowGather(rank, hidden_in, hidden_rows, tile, z_send, z_recv, 0)
    gather_cot = RowGather(rank, cot_in, cot_rows, tile, z_send, z_recv, 1)
    gather_sent = RowGather(rank, sent, sent_rows, tile, z_send, z_recv, 2)
    branch = RowScatter(rank, send_part, recv_part, merge_part, tile, step_cols, p_send, p_recv)
    steps = list(range(1, ranks))

    meet(ranks)
    gather_hidden.start()
    for flip in range(1, 8):
        send_gain(flip).start()
    for index in range(4):
        for flip in (2, 4, 1):
            send_weight(index, flip).start()
    gather_cot.start()

    stage_in = [pltpu.make_async_copy(weights_in[index], stage[index], load.at[index]) for index in range(7)]
    stage_out = [pltpu.make_async_copy(stage[index], slot_of(index, own), keep.at[index]) for index in range(7)]
    own_hidden = pltpu.make_async_copy(hidden_in, hidden.at[pl.ds(0, tile), :], load.at[7])
    own_cot = pltpu.make_async_copy(cot_in, sent, load.at[8])
    own_gain = pltpu.make_async_copy(gains_in, at_cols(gains, own, width), load.at[9])
    tables = []
    for slot in range(ranks):
        block = lax.rem(rank - slot + ranks, ranks)
        for which, (source, target) in enumerate(((cosine_in, cosine), (sine_in, sine))):
            tables.append(
                pltpu.make_async_copy(
                    at_rows(source, block, tile), at_rows(target, slot, tile), load.at[10 + 2 * slot + which]
                )
            )
    start_all(stage_in + [own_hidden, own_cot, own_gain] + tables)
    relay_weights(range(4))
    for index in range(4, 7):
        for flip in (2, 4, 1):
            send_weight(index, flip).start()
    gather_hidden.relay()
    wait_all(stage_in)
    start_all(stage_out)
    wait_all([own_hidden, own_cot, own_gain])
    keep_hidden = pltpu.make_async_copy(hidden.at[pl.ds(0, tile), :], hidden_rows.at[pl.ds(0, tile), :], keep.at[7])
    keep_cot = pltpu.make_async_copy(sent, cot_rows.at[pl.ds(0, tile), :], keep.at[8])
    start_all([keep_hidden, keep_cot])
    fill_mask(bias, docs, ranks)
    wait_all(tables + stage_out + [keep_hidden, keep_cot])

    pass_weights(range(4))
    for flip in range(1, 8):
        send_gain(flip).wait_recv()
    gather_hidden.wait()
    load_rows = pltpu.make_async_copy(
        hidden_rows.at[pl.ds(tile, (ranks - 1) * tile), :], hidden.at[pl.ds(tile, (ranks - 1) * tile), :], load.at[0]
    )
    load_rows.start()
    load_rows.wait()
    norm_rows(hidden, normed, inverses, gains.at[pl.ds(0, 1), :], 64)
    finish(range(4))
    load_qkv = pltpu.make_async_copy(qkv_full, qkv_w, load.at[1])
    load_out = pltpu.make_async_copy(out_full, out_w, load.at[2])
    load_qkv.start()
    load_out.start()
    load_qkv.wait()

    @pl.loop(0, 2 * heads // step_cols)
    def _(step):
        cols = pl.ds(pl.multiple_of(step * step_cols, step_cols), step_cols)
        qkv[:, cols] = turn(dot(normed[...], qkv_w[:, cols]), cosine[...], sine[...]).astype(BF)

    @pl.loop(2 * heads // step_cols, 3 * heads // step_cols)
    def _(step):
        cols = pl.ds(pl.multiple_of(step * step_cols, step_cols), step_cols)
        qkv[:, cols] = dot(normed[...], qkv_w[:, cols]).astype(BF)

    attend(qkv, attended, bias, heads)
    load_out.wait()

    gather_cot.relay()

    @pl.loop(0, count)
    def _(step):
        cols = pl.ds(pl.multiple_of(step * step_cols, step_cols), step_cols)
        product = dot(attended[...], out_w[:, cols])
        part[:, cols] = product[:tile, :]
        send_part[:, cols] = product[tile:, :].astype(BF)
        branch.start_first(step)

    branch.start_rest()
    branch.clear(recv_part)
    branch.merge()
    relay_weights([4, 5, 6])
    branch.wait()

    @pl.loop(0, count)
    def _(step):
        cols = pl.ds(pl.multiple_of(step * step_cols, step_cols), step_cols)
        total = hidden[pl.ds(0, tile), cols].astype(F32) + part[:, cols]
        for k in steps:
            total = total + recv_part[pl.ds((k - 1) * tile, tile), cols].astype(F32)
        middle[:, cols] = total
        sent[:, cols] = total.astype(BF)

    gather_sent.start()
    keep_sent = pltpu.make_async_copy(sent, sent_rows.at[pl.ds(0, tile), :], keep.at[0])
    keep_sent.start()
    pass_weights([4, 5])
    gather_sent.relay()
    pass_weights([6])
    finish([4, 5, 6])
    gather_cot.wait()
    gather_sent.wait()
    keep_sent.wait()
    for gather in (gather_hidden, gather_cot, gather_sent):
        gather.finish()
    for index in range(7):
        for flip in (1, 2, 4):
            send_weight(index, flip).wait_send()
        for flip in NEAR:
            pass_weight(index, flip).wait_send()
        for part_index in range(2):
            relay_weight(index, part_index).wait_send()
    for flip in range(1, 8):
        send_gain(flip).wait_send()
    branch.finish()


def front(hidden_in, cot, gains, weights, cosine, sine, docs, ranks):
    tile, dim = hidden_in.shape
    tokens = tile * ranks
    width, heads = weights[0].shape
    units = weights[5].shape[1]
    dma = pltpu.SemaphoreType.DMA
    return pl.pallas_call(
        partial(front_kernel, ranks),
        out_shape=[
            shape((dim, 3 * heads), BF),
            shape((heads, dim), BF),
            shape((units, dim), BF),
            shape((dim, units), BF),
            shape((dim, units), BF),
            shape((tokens, dim), BF),
            shape((tokens, dim), BF),
            shape((tokens, dim), BF),
            shape((tokens, dim), BF),
            shape((tokens, 3 * heads), BF),
            shape((tokens, heads), BF),
            shape((tokens, 1), F32),
            shape((tile, dim), F32),
            shape((8, dim), F32),
        ],
        in_specs=[anyspace()] * 12 + [vmem()],
        out_specs=[anyspace()] * 8 + [vmem()] * 6,
        scratch_shapes=[
            pltpu.VMEM((tokens, dim), BF),
            pltpu.VMEM((dim, 3 * heads), BF),
            pltpu.VMEM((heads, dim), BF),
            pltpu.VMEM((tokens, 256), F32),
            pltpu.VMEM((tokens, 256), F32),
            pltpu.VMEM((tokens, tokens), F32),
            pltpu.VMEM((tile, dim), F32),
            pltpu.VMEM((tokens - tile, dim), BF),
            pltpu.VMEM((tokens - tile, dim), BF),
            pltpu.VMEM((tile, dim), BF),
            pltpu.VMEM((tile, dim), BF),
        ]
        + [pltpu.VMEM(weight.shape, BF) for weight in weights]
        + [
            dma((7, 9)),
            dma((7, 9)),
            dma((3, ranks)),
            dma((3, ranks)),
            dma((dim // 256, ranks)),
            dma((dim // 256, ranks)),
            dma((8,)),
            dma((8,)),
            dma((10 + 2 * ranks,)),
            dma((9,)),
        ],
        compiler_params=pltpu.CompilerParams(vmem_limit_bytes=VMEM_LIMIT, collective_id=0, has_side_effects=True),
        cost_estimate=cost(2 * tokens * dim * 4 * heads * 3, 20e6),
        name="front",
    )(hidden_in, cot, gains, *weights, cosine, sine, docs)


def back_kernel(ranks, *refs):
    (
        sent_in,
        cot_in,
        hidden_in,
        qkv_full,
        out_full,
        down_full,
        gate_full,
        up_full,
        normed_in,
        qkv_in,
        attended_in,
        middle_in,
        cosine_in,
        sine_in,
        docs,
        inverses_one,
        gains,
    ) = refs[:17]
    gate_parts, up_parts, down_parts, qkv_parts, out_parts = refs[17:22]
    pair_ff = refs[22:25]
    pair_two, pair_cot, pair_qkv, pair_attended, pair_normed, pair_branch = refs[25:31]
    two_recv, mlp_recv, one_recv, branch_rows = refs[31:35]
    two_merge, mlp_merge, one_merge = refs[35:38]
    grad_merge = refs[38:43]
    layer_out, input_grad, gain_total = refs[43:46]
    gate_w, up_w, down_w, sent, cot, normed, hidden, d_gate, d_up = refs[46:55]
    two_half, cot_half, buffer_a, buffer_b, buffer_c, out_w = refs[55:61]
    qkv, d_qkv, attended, d_attended, bias, cosine, sine, inverses = refs[61:69]
    own_mlp, grad_middle, send_part, recv_part, gain_part, gain_recv, gain_z = refs[69:76]
    f_send, f_recv, h_send, h_recv, z_send, z_recv, b_send, b_recv, w_send, w_recv, g_send, g_recv = refs[76:88]
    load, keep, tile_load = refs[88:]

    own, rank = lax.axis_index("dp"), lax.axis_index("tensor")
    core = lax.rem(own, 2)
    tokens, dim = sent.shape
    units = gate_w.shape[1]
    tile = tokens // ranks
    heads = attended.shape[1]
    width = out_parts.shape[1] // 3
    half = dim // (2 * width)
    step_cols = 256
    count = dim // step_cols
    steps = list(range(1, ranks))
    rest = tokens - tile
    branch, send_mlp = sent.at[pl.ds(0, tile), :], sent.at[pl.ds(tile, rest), :]

    def tile_cols(step, size=step_cols):
        return pl.ds(pl.multiple_of(step * size, size), size)

    def local(source, target, sem):
        return pltpu.make_async_copy(source, target, sem)

    def to_pair(source, target, row, slot):
        return remote(source, target, h_send.at[row, slot], h_recv.at[row, slot], "dp", own ^ 1)

    def halves(source, target, row):
        return [
            to_pair(at_cols(source, 2 * slot + 1 - core, width), at_cols(target, slot, width), row, slot)
            for slot in range(half)
        ]

    def send_ff(step, which):
        cols = tile_cols(step)
        source = (hidden, d_gate, d_up)[which].at[:, cols]
        return remote(
            source, pair_ff[which].at[:, cols], f_send.at[step, which], f_recv.at[step, which], "dp", own ^ 1
        )

    def scatter(kind, source, target, merge):
        return RowScatter(rank, source, target, merge, tile, step_cols, z_send.at[kind], z_recv.at[kind])

    two = scatter(0, send_part, two_recv, two_merge)
    mlp_scatter = scatter(1, send_mlp, mlp_recv, mlp_merge)
    one = scatter(2, send_part, one_recv, one_merge)
    gather_branch = RowGather(rank, branch, branch_rows, tile, b_send, b_recv, 0)

    def piece(index, slot):
        if index == 0:
            return at_cols(up_w, slot, width)
        if index < 3:
            return at_rows(gate_w, (index - 1) * 4 + slot, width)
        if index == 3:
            return (hidden, d_gate)[slot // 2].at[pl.ds((slot % 2) * width, width), pl.ds(0, 3 * heads)]
        return at_cols(d_up, slot, width)

    def landing(index, slot):
        ref = (down_parts, gate_parts, up_parts, qkv_parts, out_parts)[index]
        return at_cols(ref, slot, width) if index in (0, 4) else at_rows(ref, slot, width)

    def half_of(ref, index, part):
        rows, cols = ref.shape
        if index in (0, 4):
            return ref.at[pl.ds(part * (rows // 2), rows // 2), :]
        return ref.at[:, pl.ds(part * (cols // 2), cols // 2)]

    def stage_of(index, part):
        if index == 0:
            return up_w.at[pl.ds(0, units // 2), pl.ds((4 + part) * width, width)]
        if index == 4:
            return up_w.at[pl.ds(0, heads // 2), pl.ds((4 + part) * width, width)]
        size = (0, units // 2, units // 2, 3 * heads // 2)[index]
        return up_w.at[pl.ds((4 + part + 2 * (index == 2)) * width, width), pl.ds(4 * width, size)]

    def send_far(index, part):
        return remote(
            half_of(piece(index, 3), index, part),
            half_of(grad_merge[index], index, part),
            w_send.at[index, part],
            w_recv.at[index, part],
            "dp",
            own ^ (2 + 2 * part),
        )

    def send_near(index, slot, part):
        tag = 2 * slot + part
        return remote(
            half_of(piece(index, slot), index, part),
            half_of(landing(index, slot), index, part),
            w_send.at[index, tag],
            w_recv.at[index, tag],
            "dp",
            own ^ (2 * slot),
        )

    def keep_grad(index):
        return local(piece(index, 0), landing(index, 0), keep.at[index])

    def send_slot(index, slot):
        if slot == 3:
            send_far(index, 0).start()
            send_far(index, 1).start()
        elif slot == 0:
            keep_grad(index).start()
        else:
            send_near(index, slot, slot - 1).start()

    def merge_grads(index):
        loads = [local(half_of(grad_merge[index], index, part), stage_of(index, part), load.at[part]) for part in range(2)]
        for part in range(2):
            send_far(index, part).wait_recv()
            loads[part].start()
        for part in range(2):
            loads[part].wait()
            target, source = half_of(piece(index, 2 - part), index, part), stage_of(index, part)
            size = source.shape[0] // 4

            @pl.loop(0, 4)
            def _(step):
                rows = tile_cols(step, size)
                target[rows, :] = (target[rows, :].astype(F32) + source[rows, :].astype(F32)).astype(BF)

            send_near(index, 2 - part, part).start()

    def row_grads(index, left, left_pair, right, right_pair, columns):
        for slot in (3, 1, 2, 0):
            mine, theirs = slice_of(slot, width, True), slice_of(slot, width, False)
            turned, turned_pair = jnp.transpose(left[:, mine]), jnp.transpose(left_pair[:, theirs])
            target = piece(index, slot)

            @pl.loop(0, columns // 512)
            def _(step):
                cols = tile_cols(step, 512)
                total = dot(turned, right[:, cols]) + dot(turned_pair, right_pair[:, cols])
                target[:, cols] = total.astype(BF)

            send_slot(index, slot)

    def col_grads(index, left, left_pair, right, right_pair, columns):
        @pl.loop(0, columns // 256)
        def _(step):
            rows = tile_cols(step, 256)
            turned, turned_pair = jnp.transpose(left[:, rows]), jnp.transpose(left_pair[:, rows])
            for slot in range(4):
                mine, theirs = slice_of(slot, width, True), slice_of(slot, width, False)
                total = dot(turned, right[:, mine]) + dot(turned_pair, right_pair[:, theirs])
                piece(index, slot)[rows, :] = total.astype(BF)

        for slot in (3, 1, 2, 0):
            send_slot(index, slot)

    def take(rows, target):
        rows.wait()
        copy = local(target, recv_part, load.at[0])
        copy.start()
        copy.wait()
        rows.clear(recv_part)

    def received(rows_start, size, base):
        total = base
        for k in steps:
            total = total + recv_part[pl.ds(pl.multiple_of((k - 1) * tile + rows_start, size), size), :].astype(F32)
        return total

    def norm_back(total, values, gain):
        inverse = lax.rsqrt(jnp.mean(values * values, axis=-1, keepdims=True) + EPSILON)
        scaled = total * gain
        return inverse * (scaled - values * inverse * inverse * jnp.mean(scaled * values, axis=-1, keepdims=True))

    load_sent = local(sent_in, sent, load.at[1])
    load_cot = local(cot_in, cot, load.at[2])

    def load_tile(step):
        cols = tile_cols(step)
        return [
            local(gate_full.at[:, cols], gate_w.at[:, cols], tile_load.at[step, 0]),
            local(up_full.at[:, cols], up_w.at[:, cols], tile_load.at[step, 1]),
            local(down_full.at[cols, :], down_w.at[cols, :], tile_load.at[step, 2]),
        ]

    load_out = local(out_full, out_w, load.at[6])
    load_qkv = local(qkv_in, qkv, load.at[7])
    load_attended = local(attended_in, attended, load.at[8])
    load_middle = local(middle_in, own_mlp, load.at[9])
    load_tables = []
    for slot in range(ranks):
        block = lax.rem(rank - slot + ranks, ranks)
        for which, (source, target) in enumerate(((cosine_in, cosine), (sine_in, sine))):
            rows = pl.ds(pl.multiple_of(block * tile, tile), tile)
            load_tables.append(
                local(
                    source.at[rows, pl.ds(0, 128)], at_rows(target, slot, tile), load.at[10 + 2 * slot + which]
                )
            )
    start_all([load_sent, load_cot])

    @pl.loop(0, units // step_cols)
    def _(step):
        start_all(load_tile(step))

    start_all([load_out, load_qkv, load_attended, load_middle] + load_tables)
    meet(ranks)
    send_cot, send_normed = halves(cot_in, pair_cot, 0), halves(normed_in, pair_normed, 1)
    send_attended = to_pair(attended_in, pair_attended, 2, 0)
    start_all(send_cot + send_normed + [send_attended])
    load_sent.wait()
    norm_rows(sent, normed, inverses, gains.at[pl.ds(1, 1), :], 64)
    send_two = halves(normed, pair_two, 3)
    start_all(send_two)
    load_cot.wait()

    @pl.loop(0, units // step_cols)
    def _(step):
        cols = tile_cols(step)
        wait_all(load_tile(step))
        gate = dot(normed[...], gate_w[:, cols])
        up = dot(normed[...], up_w[:, cols])
        d_hidden = dot_rows(cot[...], down_w[cols, :])
        s = jax.nn.sigmoid(gate)
        activated = gate * s
        hidden[:, cols] = (activated * up).astype(BF)
        d_gate[:, cols] = (d_hidden * up * (s + activated * (1.0 - s))).astype(BF)
        d_up[:, cols] = (d_hidden * activated).astype(BF)
        for which in range(3):
            send_ff(step, which).start()

    gain_part[...] = jnp.zeros(gain_part.shape, F32)

    @pl.loop(0, count)
    def _(step):
        cols = tile_cols(step)
        product = dot_rows(d_gate[...], gate_w[cols, :]) + dot_rows(d_up[...], up_w[cols, :])
        gain_part[pl.ds(1, 1), cols] = jnp.sum(product * (sent[:, cols].astype(F32) * inverses[...]), axis=0, keepdims=True)
        grad_middle[:, cols] = product[:tile, :]
        send_part[:, cols] = product[tile:, :].astype(BF)
        two.start_first(step)

    two.start_rest()
    two.merge(recv_part.at[pl.ds(0, tile), :], load.at[0])

    @pl.loop(0, units // step_cols)
    def _(step):
        for which in range(3):
            send_ff(step, which).wait_recv()

    for copy in send_cot + send_two:
        copy.wait_recv()
    pair_loads = [
        local(pair_ff[0], buffer_a, load.at[0]),
        local(pair_cot, cot_half, load.at[1]),
        local(pair_ff[1], buffer_b, load.at[2]),
        local(pair_two, two_half, load.at[3]),
        local(pair_ff[2], buffer_c, load.at[4]),
    ]
    start_all(pair_loads)
    wait_all(pair_loads)
    col_grads(0, hidden, buffer_a, cot, cot_half, units)
    row_grads(1, normed, two_half, d_gate, buffer_b, units)
    merge_grads(0)
    row_grads(2, normed, two_half, d_up, buffer_c, units)
    take(two, two_recv)

    @pl.loop(0, tile // 32)
    def _(step):
        rows = pl.ds(pl.multiple_of(step * 32, 32), 32)
        total = received(step * 32, 32, grad_middle[rows, :])
        result = cot[rows, :].astype(F32) + norm_back(total, sent[rows, :].astype(F32), gains[1:2, :])
        grad_middle[rows, :] = result
        branch[rows, :] = result.astype(BF)

    gather_branch.start()
    keep_branch = local(branch, at_rows(branch_rows, 0, tile), keep.at[5])
    keep_branch.start()
    wait_all([load_middle, load_attended, load_qkv, load_out] + load_tables)
    fill_mask(bias, docs, ranks)

    @pl.loop(0, count)
    def _(step):
        cols = tile_cols(step)
        product = dot(hidden[...], down_w[:, cols])
        own_mlp[:, cols] = own_mlp[:, cols] + product[:tile, :]
        send_mlp[:, cols] = product[tile:, :].astype(BF)

    merge_grads(1)
    gather_branch.relay()

    @pl.loop(0, count)
    def _(step):
        mlp_scatter.start_first(step)

    mlp_scatter.start_rest()
    merge_grads(2)
    load_weight = local(qkv_full, down_w.at[:, pl.ds(0, 3 * heads)], load.at[0])
    load_hidden = local(hidden_in, buffer_b, load.at[1])
    load_normed = local(normed_in, buffer_c, load.at[2])
    start_all([load_weight, load_hidden, load_normed])

    two.finish()
    mlp_scatter.merge(recv_part.at[pl.ds(0, tile), :], load.at[3])
    gather_branch.wait()
    keep_branch.wait()
    load_branch = local(branch_rows, buffer_a, load.at[3])
    load_branch.start()
    send_half = halves(branch_rows, pair_branch, 4)
    start_all(send_half)
    load_branch.wait()

    @pl.loop(0, heads // step_cols)
    def _(step):
        cols = tile_cols(step)
        d_attended[:, cols] = dot_rows(buffer_a[...], out_w[cols, :]).astype(BF)

    attend_back(qkv, d_attended, d_qkv, bias, cosine, sine, heads)
    send_qkv = to_pair(d_qkv, pair_qkv, 5, 0)
    send_qkv.start()
    wait_all([load_weight, load_hidden, load_normed])

    @pl.loop(0, count)
    def _(step):
        cols = tile_cols(step)
        product = dot_rows(d_qkv[...], down_w[cols, pl.ds(0, 3 * heads)])
        gain_part[pl.ds(0, 1), cols] = jnp.sum(
            product * (buffer_b[:, cols].astype(F32) * inverses_one[...]), axis=0, keepdims=True
        )
        input_grad[:, cols] = product[:tile, :]
        send_part[:, cols] = product[tile:, :].astype(BF)
        one.start_first(step)

    one.start_rest()

    def send_gain(flip):
        return remote(
            at_cols(gain_part, own ^ flip, width), at_rows(gain_recv, flip, 8), g_send.at[flip], g_recv.at[flip], "dp", own ^ flip
        )

    for flip in range(1, 8):
        send_gain(flip).start()

    for index in range(3):
        keep_grad(index).wait()
    send_qkv.wait_recv()
    for copy in send_half + send_normed + [send_attended]:
        copy.wait_recv()

    @pl.loop(0, units // step_cols)
    def _(step):
        for which in range(3):
            send_ff(step, which).wait_send()

    for copy in send_two:
        copy.wait_send()
    last_loads = [
        local(pair_qkv, normed.at[:, pl.ds(0, 3 * heads)], load.at[0]),
        local(pair_attended, cot.at[:, pl.ds(0, heads)], load.at[1]),
        local(pair_normed, two_half, load.at[2]),
        local(pair_branch, cot_half, load.at[3]),
    ]
    start_all(last_loads)
    wait_all(last_loads)
    col_grads(4, attended, cot, buffer_a, cot_half, heads)
    row_grads(3, buffer_c, two_half, d_qkv, normed, 3 * heads)
    one.merge(recv_part.at[pl.ds(0, tile), :], load.at[0])
    merge_grads(4)
    merge_grads(3)

    for flip in range(1, 8):
        send_gain(flip).wait_recv()
    gain_sum = gain_part[:, pl.ds(pl.multiple_of(own * width, width), width)]
    for flip in range(1, 8):
        gain_sum = gain_sum + gain_recv[pl.ds(flip * 8, 8), :]
    gain_z[pl.ds(0, 8), :] = gain_sum

    def send_gain_z(k):
        peer = lax.rem(rank + k, ranks)
        return remote(
            gain_z.at[pl.ds(0, 8), :], gain_z.at[pl.ds(8 * k, 8), :], b_send.at[1, k], b_recv.at[1, k], "tensor", peer
        )

    for k in steps:
        send_gain_z(k).start()

    take(mlp_scatter, mlp_recv)

    @pl.loop(0, tile // 32)
    def _(step):
        rows = pl.ds(pl.multiple_of(step * 32, 32), 32)
        layer_out[rows, :] = received(step * 32, 32, own_mlp[rows, :]).astype(BF)

    take(one, one_recv)
    load_own = local(hidden_in.at[pl.ds(0, tile), :], branch, load.at[1])
    gather_branch.finish()
    load_own.start()
    load_own.wait()

    @pl.loop(0, tile // 32)
    def _(step):
        rows = pl.ds(pl.multiple_of(step * 32, 32), 32)
        total = received(step * 32, 32, input_grad[rows, :])
        input_grad[rows, :] = grad_middle[rows, :] + norm_back(total, branch[rows, :].astype(F32), gains[0:1, :])

    for k in steps:
        send_gain_z(k).wait_recv()
    gain_all = gain_z[pl.ds(0, 8), :]
    for k in steps:
        gain_all = gain_all + gain_z[pl.ds(8 * k, 8), :]
    gain_total[...] = gain_all

    for index in range(5):
        for slot in range(1, 3):
            for part in range(2):
                send_near(index, slot, part).wait_recv()
    for index in range(3, 5):
        keep_grad(index).wait()
    for index in range(5):
        for part in range(2):
            send_far(index, part).wait_send()
            for slot in range(1, 3):
                send_near(index, slot, part).wait_send()
    for flip in range(1, 8):
        send_gain(flip).wait_send()
    for k in steps:
        send_gain_z(k).wait_send()
    for copy in send_cot + send_normed + send_half + [send_attended, send_qkv]:
        copy.wait_send()

    mlp_scatter.finish()
    one.finish()


def back(sent, cot, hidden, weights, normed, qkv, attended, middle, cosine, sine, docs, inverses, gains, ranks):
    tokens, dim = sent.shape
    tile, heads, units = tokens // ranks, attended.shape[1], weights[2].shape[0]
    width, rest = gains.shape[1] // 8, tokens - tile
    dma = pltpu.SemaphoreType.DMA
    count = dim // 256
    return pl.pallas_call(
        partial(back_kernel, ranks),
        out_shape=[
            shape((3 * width, units), BF),
            shape((3 * width, units), BF),
            shape((units, 3 * width), BF),
            shape((3 * width, 3 * heads), BF),
            shape((heads, 3 * width), BF),
        ]
        + [shape((tokens, units), BF)] * 3
        + [
            shape((tokens, dim // 2), BF),
            shape((tokens, dim // 2), BF),
            shape((tokens, 3 * heads), BF),
            shape((tokens, heads), BF),
            shape((tokens, dim // 2), BF),
            shape((tokens, dim // 2), BF),
        ]
        + [shape((rest, dim), BF)] * 3
        + [
            shape((tokens, dim), BF),
        ]
        + [shape((tile, dim), BF)] * 3
        + [
            shape((units, width), BF),
            shape((width, units), BF),
            shape((width, units), BF),
            shape((width, 3 * heads), BF),
            shape((heads, width), BF),
            shape((tile, dim), BF),
            shape((tile, dim), F32),
            shape((8, width), F32),
        ],
        in_specs=[anyspace()] * 14 + [vmem()] * 3,
        out_specs=[anyspace()] * 26 + [vmem()] * 3,
        scratch_shapes=[
            pltpu.VMEM((dim, units), BF),
            pltpu.VMEM((dim, units), BF),
            pltpu.VMEM((units, dim), BF),
            pltpu.VMEM((tokens, dim), BF),
            pltpu.VMEM((tokens, dim), BF),
            pltpu.VMEM((tokens, dim), BF),
            pltpu.VMEM((tokens, units), BF),
            pltpu.VMEM((tokens, units), BF),
            pltpu.VMEM((tokens, units), BF),
            pltpu.VMEM((tokens, dim // 2), BF),
            pltpu.VMEM((tokens, dim // 2), BF),
            pltpu.VMEM((tokens, units), BF),
            pltpu.VMEM((tokens, units), BF),
            pltpu.VMEM((tokens, units), BF),
            pltpu.VMEM((heads, dim), BF),
            pltpu.VMEM((tokens, 3 * heads), BF),
            pltpu.VMEM((tokens, 3 * heads), BF),
            pltpu.VMEM((tokens, heads), BF),
            pltpu.VMEM((tokens, heads), BF),
            pltpu.VMEM((tokens, tokens), F32),
            pltpu.VMEM((tokens, 128), F32),
            pltpu.VMEM((tokens, 128), F32),
            pltpu.VMEM((tokens, 1), F32),
            pltpu.VMEM((tile, dim), F32),
            pltpu.VMEM((tile, dim), F32),
            pltpu.VMEM((rest, dim), BF),
            pltpu.VMEM((rest, dim), BF),
            pltpu.VMEM((8, dim), F32),
            pltpu.VMEM((64, width), F32),
            pltpu.VMEM((8 * ranks, width), F32),
            dma((units // 256, 3)),
            dma((units // 256, 3)),
            dma((6, 4)),
            dma((6, 4)),
            dma((3, count, ranks)),
            dma((3, count, ranks)),
            dma((2, ranks)),
            dma((2, ranks)),
            dma((5, 6)),
            dma((5, 6)),
            dma((8,)),
            dma((8,)),
            dma((10 + 2 * ranks,)),
            dma((6,)),
            dma((units // 256, 3)),
        ],
        compiler_params=pltpu.CompilerParams(vmem_limit_bytes=67000000, collective_id=1, has_side_effects=True),
        cost_estimate=cost(2 * tokens * dim * units * 9, 100e6),
        name="back",
    )(sent, cot, hidden, *weights, normed, qkv, attended, middle, cosine, sine, docs, inverses, gains)


def shift(values, step):
    size = lax.axis_size("tensor")
    return lax.ppermute(values, "tensor", [(index, (index + step) % size) for index in range(size)])


def gather_rows(values):
    return [values] + [shift(values, step) for step in range(1, lax.axis_size("tensor"))]


def scatter_rows(parts):
    total = parts[0].astype(F32)
    for step in range(1, len(parts)):
        total = total + shift(parts[step], -step).astype(F32)
    return total


def gather_weight(values, axis):
    return [None], [lax.all_gather(values, "dp", axis=axis, tiled=True)]


def scatter_full(left, right, axis):
    full = dot_cols(left, right).astype(BF)
    return lax.psum_scatter(full, "dp", scatter_dimension=axis, tiled=True).astype(F32)


def sum_parts(parts, width, axis):
    pieces = jnp.split(parts, 3, axis=axis)
    return sum(piece.astype(F32) for piece in pieces)


def rotary(length):
    half_size = HEAD_DIM // 2
    frequency = ROPE_BASE ** (-jnp.arange(half_size, dtype=F32) / half_size)
    angles = jnp.arange(length).astype(F32)[:, None] * frequency[None, :]
    cosine, sine = jnp.cos(angles), jnp.sin(angles)
    cosine = jnp.tile(cosine, (1, 8))
    sine = jnp.tile(jnp.concatenate([-sine, sine], axis=1), (1, 4))
    return cosine, sine


def position_tables(doc_ids, ranks):
    length = doc_ids.shape[0]
    token_index = jnp.arange(length, dtype=jnp.int32)
    before = jnp.concatenate([doc_ids[:1] - 1, doc_ids[:-1]])
    doc_start = lax.cummax(jnp.where(doc_ids != before, token_index, 0), axis=0)
    order = (lax.axis_index("tensor") - jnp.arange(ranks)) % ranks
    last = token_index.reshape(ranks, -1)[order].reshape(length)
    first = doc_start.reshape(ranks, -1)[order].reshape(length)
    cosine, sine = (table.reshape(ranks, -1, 256)[order].reshape(length, 256) for table in rotary(length))
    return cosine, sine, first[:, None], last[:, None], last[None, :]


def rms_back(grad_rows_, values, gain):
    inverse = lax.rsqrt(jnp.mean(values * values, axis=-1, keepdims=True) + EPSILON)
    scaled = grad_rows_ * gain
    return inverse * (scaled - values * inverse * inverse * jnp.mean(scaled * values, axis=-1, keepdims=True))


def body(
    hidden_in,
    out_cotangent,
    doc_ids,
    attn_gain,
    query_weight,
    key_weight,
    value_weight,
    out_weight,
    mlp_gain,
    gate_weight,
    up_weight,
    down_weight,
):
    ranks, groups = lax.axis_size("tensor"), lax.axis_size("dp")
    paired = (groups, ranks) == (8, 4)
    width, heads = query_weight.shape
    dim = hidden_in.shape[1]

    if paired:
        pad = jnp.zeros((6, width), F32)
        own_gains = jnp.concatenate([attn_gain[None].astype(F32), mlp_gain[None].astype(F32), pad], axis=0)
        weights = (query_weight, key_weight, value_weight, out_weight, down_weight, gate_weight, up_weight)
        docs, turns = doc_ids.reshape(ranks, -1), rotary(doc_ids.shape[0])
        front_out = front(hidden_in, out_cotangent, own_gains, weights, *turns, docs, ranks)
        full, (hidden_rows, cot_rows, sent_rows) = front_out[:5], front_out[5:8]
        normed, qkv, attended, inverses, middle, gains = front_out[8:]
        back_out = back(
            sent_rows, cot_rows, hidden_rows, full, normed, qkv, attended, middle, *turns, docs, inverses, gains, ranks
        )
        gate_grad, up_grad, down_grad, qkv_grad, out_proj_grad = (
            sum_parts(part, width, axis) for part, axis in zip(back_out[:5], (0, 0, 1, 0, 1))
        )
        layer_out, input_grad, gain_total = back_out[26:]
        share = width // ranks
        gain_grads = lax.dynamic_slice_in_dim(gain_total, lax.axis_index("tensor") * share, share, axis=1)
    else:
        tables = position_tables(doc_ids, ranks)
        input_local = hidden_in.astype(F32)
        hidden_rows = gather_rows(hidden_in)
        gains = lax.all_gather(jnp.stack([attn_gain, mlp_gain]), "dp", axis=1, tiled=True).astype(F32)
        attn_scale, mlp_scale = gains[:1], gains[1:]
        qkv_weight = jnp.concatenate([query_weight, key_weight, value_weight], axis=1)
        tags, qkv_pieces = gather_weight(qkv_weight, 0)
        tags, out_pieces = gather_weight(out_weight, 1)
        cot_rows = gather_rows(out_cotangent)
        tags, down_pieces = gather_weight(down_weight, 1)
        tags, gate_pieces = gather_weight(gate_weight, 0)
        tags, up_pieces = gather_weight(up_weight, 0)
        normed, qkv, attended, inverses, *branch_parts = attn_fwd(
            hidden_rows, attn_scale, tables, tags, width, qkv_pieces, out_pieces
        )
        middle = input_local + scatter_rows(branch_parts)
        sent = middle.astype(BF)
        sent_rows = gather_rows(sent)
        cot_full = jnp.concatenate(cot_rows, axis=0)
        normed_two, hidden, d_gate, d_up, mlp_gain_part, *two_parts = mlp(
            sent_rows, cot_rows, mlp_scale, tags, width, gate_pieces, up_pieces, down_pieces, ranks
        )
        grad_two_rows = scatter_rows(two_parts)
        grad_middle = out_cotangent.astype(F32) + rms_back(grad_two_rows, sent.astype(F32), mlp_scale)
        branch_rows = gather_rows(grad_middle.astype(BF))
        down_grad = scatter_full(hidden, cot_full, 1)
        gate_grad = scatter_full(normed_two, d_gate, 0)
        up_grad = scatter_full(normed_two, d_up, 0)
        mlp_rows = scatter_rows(mlp_out(hidden, ranks, dim, tags, width, down_pieces))
        layer_out = (middle + mlp_rows).astype(BF)
        branch_full, d_qkv, attn_gain_part, *one_parts = attn_bwd(
            branch_rows, hidden_rows, qkv, inverses, tables, tags, width, qkv_pieces, out_pieces, ranks
        )
        out_proj_grad = scatter_full(attended, branch_full, 1)
        qkv_grad = scatter_full(normed, d_qkv, 0)
        grad_one_rows = scatter_rows(one_parts)
        input_grad = grad_middle + rms_back(grad_one_rows, input_local, attn_scale)
        gain_parts = jnp.concatenate([attn_gain_part, mlp_gain_part], axis=0)
        gain_grads = lax.psum_scatter(gain_parts, ("dp", "tensor"), scatter_dimension=1, tiled=True)
    return (
        layer_out,
        input_grad,
        gain_grads[0],
        qkv_grad[:, :heads],
        qkv_grad[:, heads : 2 * heads],
        qkv_grad[:, 2 * heads :],
        out_proj_grad,
        gain_grads[1],
        gate_grad,
        up_grad,
        down_grad,
    )


def solution(mesh):
    return jax.shard_map(
        body,
        mesh=mesh,
        in_specs=(
            P(("dp", "tensor"), None),
            P(("dp", "tensor"), None),
            P("dp"),
            P("dp"),
            P("dp", "tensor"),
            P("dp", "tensor"),
            P("dp", "tensor"),
            P("tensor", "dp"),
            P("dp"),
            P("dp", "tensor"),
            P("dp", "tensor"),
            P("tensor", "dp"),
        ),
        out_specs=(
            P(("dp", "tensor"), None),
            P(("dp", "tensor"), None),
            P(("dp", "tensor")),
            P("dp", "tensor"),
            P("dp", "tensor"),
            P("dp", "tensor"),
            P("tensor", "dp"),
            P(("dp", "tensor")),
            P("dp", "tensor"),
            P("dp", "tensor"),
            P("tensor", "dp"),
        ),
        check_vma=False,
    )
```

```python
from functools import partial

import jax
import jax.numpy as jnp
from jax import lax
from jax.experimental import pallas as pl
from jax.experimental.pallas import tpu as pltpu
from jax.sharding import PartitionSpec as P

HEAD_DIM = 64
EPSILON = 1e-05
ROPE_BASE = 130000.0
NEGATIVE = -1e30
VMEM_LIMIT = 63 * 1024 * 1024
BF = jnp.bfloat16
F32 = jnp.float32


def dot(left, right):
    return jnp.dot(left, right, preferred_element_type=F32)


def dot_rows(left, right):
    return lax.dot_general(left, right, (((1,), (1,)), ((), ())), preferred_element_type=F32)


def dot_cols(left, right):
    return lax.dot_general(left, right, (((0,), (0,)), ((), ())), preferred_element_type=F32)


def vmem():
    return pl.BlockSpec(memory_space=pltpu.VMEM)


def anyspace():
    return pl.BlockSpec(memory_space=pl.ANY)


def params():
    return pltpu.CompilerParams(vmem_limit_bytes=VMEM_LIMIT)


def cost(flops, nbytes):
    return pl.CostEstimate(flops=int(flops), bytes_accessed=int(nbytes), transcendentals=0)


def shape(dims, kind):
    return jax.ShapeDtypeStruct(dims, kind)


def place_copies(tags, pieces, target, sem, axis, width):
    own = lax.axis_index("dp")
    copies = []
    for slot, (tag, piece) in enumerate(zip(tags, pieces)):
        if tag is None:
            where = target
        else:
            start = pl.multiple_of((own ^ tag) * width, width)
            where = target.at[pl.ds(start, width), :] if axis == 0 else target.at[:, pl.ds(start, width)]
        copies.append(pltpu.make_async_copy(piece, where, sem.at[slot]))
    return copies


def row_copies(pieces, target, sem):
    copies = []
    for slot, piece in enumerate(pieces):
        rows = piece.shape[0]
        copies.append(pltpu.make_async_copy(piece, target.at[pl.ds(slot * rows, rows), :], sem.at[slot]))
    return copies


def start_all(copies):
    for copy in copies:
        copy.start()


def wait_all(copies):
    for copy in copies:
        copy.wait()


def turn(values, cosine, sine):
    width = values.shape[1]
    lane = lax.broadcasted_iota(jnp.int32, values.shape, 1)
    partner = jnp.where(
        lax.rem(lane, HEAD_DIM) < HEAD_DIM // 2,
        pltpu.roll(values, width - HEAD_DIM // 2, 1),
        pltpu.roll(values, HEAD_DIM // 2, 1),
    )
    return values * cosine + partner * sine


def norm_rows(source, target, inverses, gain, tile):
    @pl.loop(0, source.shape[0] // tile)
    def _(step):
        rows = pl.ds(pl.multiple_of(step * tile, tile), tile)
        values = source[rows, :].astype(F32)
        inverse = lax.rsqrt(jnp.mean(values * values, axis=-1, keepdims=True) + EPSILON)
        inverses[rows, :] = inverse
        target[rows, :] = (values * inverse * gain[...]).astype(BF)


def fill_bias(bias, first, last, key_index):
    keys = key_index[...]
    bias[...] = jnp.where((keys >= first[...]) & (keys <= last[...]), 0.0, NEGATIVE)


def head_lanes(width, half):
    lane = lax.broadcasted_iota(jnp.int32, (1, width), 1)
    return (lax.div(lane, HEAD_DIM) == half).astype(F32)


def probabilities(query, key, bias):
    scores = dot_rows(query, key) + bias
    weights = jnp.exp(scores - jnp.max(scores, axis=-1, keepdims=True))
    return weights * (1.0 / jnp.sum(weights, axis=-1, keepdims=True))


def attend(qkv, attended, bias, heads):
    @pl.loop(0, heads // 128)
    def _(pair):
        base = pl.multiple_of(pair * 128, 128)
        query = qkv[:, pl.ds(base, 128)]
        key = qkv[:, pl.ds(heads + base, 128)]
        value = qkv[:, pl.ds(2 * heads + base, 128)]
        total = None
        for half in range(2):
            lanes = head_lanes(128, half).astype(BF)
            probs = probabilities(query * (lanes * HEAD_DIM ** (-0.5)), key, bias[...])
            term = dot(probs.astype(BF), value * lanes)
            total = term if total is None else total + term
        attended[:, pl.ds(base, 128)] = total.astype(BF)


def attn_fwd_kernel(tags, width, nrow, *refs):
    npiece = len(tags)
    rows_in = refs[:nrow]
    gain, cosine, sine, first, last, key_index = refs[nrow : nrow + 6]
    rest = refs[nrow + 6 :]
    qkv_in, out_in = rest[:npiece], rest[npiece : 2 * npiece]
    rest = rest[2 * npiece :]
    normed, qkv, attended, inverses = rest[:4]
    parts = rest[4 : 4 + nrow]
    hidden, qkv_w, out_w, bias, sem_rows, sem_qkv, sem_out = rest[4 + nrow :]
    load_rows = row_copies(rows_in, hidden, sem_rows)
    load_qkv = place_copies(tags, qkv_in, qkv_w, sem_qkv, 0, width)
    load_out = place_copies(tags, out_in, out_w, sem_out, 1, width)
    start_all(load_rows + load_qkv + load_out)
    fill_bias(bias, first, last, key_index)
    wait_all(load_rows)
    norm_rows(hidden, normed, inverses, gain, 64)
    wait_all(load_qkv)
    heads = attended.shape[1]
    step_cols = 256

    @pl.loop(0, 2 * heads // step_cols)
    def _(step):
        cols = pl.ds(pl.multiple_of(step * step_cols, step_cols), step_cols)
        qkv[:, cols] = turn(dot(normed[...], qkv_w[:, cols]), cosine[...], sine[...]).astype(BF)

    @pl.loop(2 * heads // step_cols, 3 * heads // step_cols)
    def _(step):
        cols = pl.ds(pl.multiple_of(step * step_cols, step_cols), step_cols)
        qkv[:, cols] = dot(normed[...], qkv_w[:, cols]).astype(BF)

    attend(qkv, attended, bias, heads)
    wait_all(load_out)
    tile = parts[0].shape[0]

    @pl.loop(0, out_w.shape[1] // step_cols)
    def _(step):
        cols = pl.ds(pl.multiple_of(step * step_cols, step_cols), step_cols)
        product = dot(attended[...], out_w[:, cols])
        for slot, part in enumerate(parts):
            part[:, cols] = product[slot * tile : (slot + 1) * tile, :].astype(part.dtype)


def attn_fwd(rows, gain, tables, tags, width, qkv_pieces, out_pieces):
    nrow, (tile, dim) = len(rows), rows[0].shape
    tokens = nrow * tile
    heads = out_pieces[0].shape[0]
    npiece = len(tags)
    return pl.pallas_call(
        partial(attn_fwd_kernel, tags, width, nrow),
        out_shape=[
            shape((tokens, dim), BF),
            shape((tokens, 3 * heads), BF),
            shape((tokens, heads), BF),
            shape((tokens, 1), F32),
        ]
        + [shape((tile, dim), F32 if slot == 0 else BF) for slot in range(nrow)],
        in_specs=[anyspace()] * nrow + [vmem()] * 6 + [anyspace()] * (2 * npiece),
        out_specs=[vmem()] * (4 + nrow),
        scratch_shapes=[
            pltpu.VMEM((tokens, dim), BF),
            pltpu.VMEM((dim, 3 * heads), BF),
            pltpu.VMEM((heads, dim), BF),
            pltpu.VMEM((tokens, tokens), F32),
            pltpu.SemaphoreType.DMA((nrow,)),
            pltpu.SemaphoreType.DMA((npiece,)),
            pltpu.SemaphoreType.DMA((npiece,)),
        ],
        compiler_params=params(),
        cost_estimate=cost(2 * tokens * dim * 4 * heads * 3, 20e6),
        name="attn_fwd",
    )(*rows, gain, *tables, *qkv_pieces, *out_pieces)


def attend_back(qkv, d_attended, d_qkv, bias, cosine, sine, heads):
    score_scale = HEAD_DIM ** (-0.5)

    @pl.loop(0, heads // 128)
    def _(pair):
        base = pl.multiple_of(pair * 128, 128)
        query = qkv[:, pl.ds(base, 128)]
        key = qkv[:, pl.ds(heads + base, 128)]
        value = qkv[:, pl.ds(2 * heads + base, 128)]
        grad = d_attended[:, pl.ds(base, 128)]
        sums = [0.0, 0.0, 0.0]
        for half in range(2):
            lanes = head_lanes(128, half).astype(BF)
            own_query = query * (lanes * score_scale)
            own_grad = grad * lanes
            probs = probabilities(own_query, key, bias[...])
            d_value = dot_cols(probs.astype(BF), own_grad)
            d_probs = dot_rows(own_grad, value)
            delta = jnp.sum(probs * d_probs, axis=-1, keepdims=True)
            d_scores = (probs * (d_probs - delta)).astype(BF)
            d_query = dot(d_scores, key * lanes) * score_scale
            d_key = dot_cols(d_scores, own_query)
            sums = [sums[0] + d_query, sums[1] + d_key, sums[2] + d_value]
        back = -sine[:, :128]
        d_qkv[:, pl.ds(base, 128)] = turn(sums[0], cosine[:, :128], back).astype(BF)
        d_qkv[:, pl.ds(heads + base, 128)] = turn(sums[1], cosine[:, :128], back).astype(BF)
        d_qkv[:, pl.ds(2 * heads + base, 128)] = sums[2].astype(BF)


def attn_bwd_kernel(tags, width, nrow, npart, *refs):
    npiece = len(tags)
    nhid, nrow = nrow[1], nrow[0]
    rows_in, hidden_in = refs[:nrow], refs[nrow : nrow + nhid]
    refs = refs[nrow + nhid :]
    qkv, inverses, cosine, sine, first, last, key_index = refs[:7]
    rest = refs[7:]
    qkv_in, out_in = rest[:npiece], rest[npiece : 2 * npiece]
    rest = rest[2 * npiece :]
    branch, d_qkv, gain_grad = rest[:3]
    parts = rest[3 : 3 + npart]
    hidden, d_attended, qkv_w, out_w, bias, sem_rows, sem_x, sem_qkv, sem_out = rest[3 + npart :]
    load_rows = row_copies(rows_in, branch, sem_rows)
    load_x = row_copies(hidden_in, hidden, sem_x)
    load_out = place_copies(tags, out_in, out_w, sem_out, 1, width)
    load_qkv = place_copies(tags, qkv_in, qkv_w, sem_qkv, 0, width)
    start_all(load_rows + load_out + load_qkv + load_x)
    fill_bias(bias, first, last, key_index)
    wait_all(load_rows)
    wait_all(load_out)
    heads = out_w.shape[0]
    step_cols = 256

    @pl.loop(0, heads // step_cols)
    def _(step):
        cols = pl.ds(pl.multiple_of(step * step_cols, step_cols), step_cols)
        d_attended[:, cols] = dot_rows(branch[...], out_w[cols, :]).astype(BF)

    attend_back(qkv, d_attended, d_qkv, bias, cosine, sine, heads)
    wait_all(load_qkv)
    wait_all(load_x)
    tile = parts[0].shape[0]

    @pl.loop(0, qkv_w.shape[0] // step_cols)
    def _(step):
        cols = pl.ds(pl.multiple_of(step * step_cols, step_cols), step_cols)
        product = dot_rows(d_qkv[...], qkv_w[cols, :])
        gain_grad[:, cols] = jnp.sum(product * (hidden[:, cols].astype(F32) * inverses[...]), axis=0, keepdims=True)
        for slot, part in enumerate(parts):
            part[:, cols] = product[slot * tile : (slot + 1) * tile, :].astype(part.dtype)


def attn_bwd(rows, hidden, qkv, inverses, tables, tags, width, qkv_pieces, out_pieces, npart):
    nrow, nhid, dim = len(rows), len(hidden), rows[0].shape[1]
    tokens = qkv.shape[0]
    tile = tokens // npart
    heads = out_pieces[0].shape[0]
    npiece = len(tags)
    return pl.pallas_call(
        partial(attn_bwd_kernel, tags, width, (nrow, nhid), npart),
        out_shape=[shape((tokens, dim), BF), shape((tokens, 3 * heads), BF), shape((1, dim), F32)]
        + [shape((tile, dim), F32 if slot == 0 else BF) for slot in range(npart)],
        in_specs=[anyspace()] * (nrow + nhid) + [vmem()] * 7 + [anyspace()] * (2 * npiece),
        out_specs=[vmem()] * (3 + npart),
        scratch_shapes=[
            pltpu.VMEM((tokens, dim), BF),
            pltpu.VMEM((tokens, heads), BF),
            pltpu.VMEM((dim, 3 * heads), BF),
            pltpu.VMEM((heads, dim), BF),
            pltpu.VMEM((tokens, tokens), F32),
            pltpu.SemaphoreType.DMA((nrow,)),
            pltpu.SemaphoreType.DMA((nhid,)),
            pltpu.SemaphoreType.DMA((npiece,)),
            pltpu.SemaphoreType.DMA((npiece,)),
        ],
        compiler_params=params(),
        cost_estimate=cost(2 * tokens * dim * 4 * heads * 6, 30e6),
        name="attn_bwd",
    )(*rows, *hidden, qkv, inverses, *tables, *qkv_pieces, *out_pieces)


def mlp_kernel(tags, width, nrow, npart, *refs):
    npiece = len(tags)
    sent_in, cot_in = refs[:nrow], refs[nrow : 2 * nrow]
    gain = refs[2 * nrow]
    rest = refs[2 * nrow + 1 :]
    gate_in, up_in, down_in = rest[:npiece], rest[npiece : 2 * npiece], rest[2 * npiece : 3 * npiece]
    rest = rest[3 * npiece :]
    normed, hidden, d_gate, d_up, gain_grad = rest[:5]
    parts = rest[5 : 5 + npart]
    sent, cot, inverses, gate_w, up_w, down_w, sem_sent, sem_cot, sem_gate, sem_up, sem_down = rest[5 + npart :]
    load_sent = row_copies(sent_in, sent, sem_sent)
    load_cot = row_copies(cot_in, cot, sem_cot)
    load_gate = place_copies(tags, gate_in, gate_w, sem_gate, 0, width)
    load_up = place_copies(tags, up_in, up_w, sem_up, 0, width)
    load_down = place_copies(tags, down_in, down_w, sem_down, 1, width)
    start_all(load_sent + load_cot + load_gate + load_up + load_down)
    wait_all(load_sent)
    norm_rows(sent, normed, inverses, gain, 64)
    wait_all(load_cot)
    wait_all(load_gate)
    wait_all(load_up)
    wait_all(load_down)
    step_cols = 256

    @pl.loop(0, gate_w.shape[1] // step_cols)
    def _(step):
        cols = pl.ds(pl.multiple_of(step * step_cols, step_cols), step_cols)
        gate = dot(normed[...], gate_w[:, cols])
        up = dot(normed[...], up_w[:, cols])
        d_hidden = dot_rows(cot[...], down_w[cols, :])
        s = jax.nn.sigmoid(gate)
        activated = gate * s
        hidden[:, cols] = (activated * up).astype(BF)
        d_gate[:, cols] = (d_hidden * up * (s + activated * (1.0 - s))).astype(BF)
        d_up[:, cols] = (d_hidden * activated).astype(BF)

    tile = parts[0].shape[0]

    @pl.loop(0, gate_w.shape[0] // step_cols)
    def _(step):
        cols = pl.ds(pl.multiple_of(step * step_cols, step_cols), step_cols)
        product = dot_rows(d_gate[...], gate_w[cols, :]) + dot_rows(d_up[...], up_w[cols, :])
        gain_grad[:, cols] = jnp.sum(product * (sent[:, cols].astype(F32) * inverses[...]), axis=0, keepdims=True)
        for slot, part in enumerate(parts):
            part[:, cols] = product[slot * tile : (slot + 1) * tile, :].astype(part.dtype)


def mlp(sent, cot, gain, tags, width, gate_pieces, up_pieces, down_pieces, npart):
    nrow, dim = len(sent), sent[0].shape[1]
    tokens = nrow * sent[0].shape[0]
    tile = tokens // npart
    units = gate_pieces[0].shape[1]
    npiece = len(tags)
    return pl.pallas_call(
        partial(mlp_kernel, tags, width, nrow, npart),
        out_shape=[shape((tokens, dim), BF)]
        + [shape((tokens, units), BF)] * 3
        + [shape((1, dim), F32)]
        + [shape((tile, dim), F32 if slot == 0 else BF) for slot in range(npart)],
        in_specs=[anyspace()] * (2 * nrow) + [vmem()] + [anyspace()] * (3 * npiece),
        out_specs=[vmem()] * (5 + npart),
        scratch_shapes=[
            pltpu.VMEM((tokens, dim), BF),
            pltpu.VMEM((tokens, dim), BF),
            pltpu.VMEM((tokens, 1), F32),
            pltpu.VMEM((dim, units), BF),
            pltpu.VMEM((dim, units), BF),
            pltpu.VMEM((units, dim), BF),
            pltpu.SemaphoreType.DMA((nrow,)),
            pltpu.SemaphoreType.DMA((nrow,)),
            pltpu.SemaphoreType.DMA((npiece,)),
            pltpu.SemaphoreType.DMA((npiece,)),
            pltpu.SemaphoreType.DMA((npiece,)),
        ],
        compiler_params=params(),
        cost_estimate=cost(2 * tokens * dim * units * 5, 40e6),
        name="mlp",
    )(*sent, *cot, gain, *gate_pieces, *up_pieces, *down_pieces)


def mlp_out_kernel(tags, width, *refs):
    npiece = len(tags)
    hidden, down_in = refs[0], refs[1 : 1 + npiece]
    *parts, down_w, sem_down = refs[1 + npiece :]
    load_down = place_copies(tags, down_in, down_w, sem_down, 1, width)
    start_all(load_down)
    wait_all(load_down)
    tile, step_cols = parts[0].shape[0], 256

    @pl.loop(0, down_w.shape[1] // step_cols)
    def _(step):
        cols = pl.ds(pl.multiple_of(step * step_cols, step_cols), step_cols)
        product = dot(hidden[...], down_w[:, cols])
        for slot, part in enumerate(parts):
            part[:, cols] = product[slot * tile : (slot + 1) * tile, :].astype(part.dtype)


def mlp_out(hidden, nrow, dim, tags, width, down_pieces):
    tokens, units = hidden.shape
    tile, npiece = tokens // nrow, len(tags)
    return pl.pallas_call(
        partial(mlp_out_kernel, tags, width),
        out_shape=[shape((tile, dim), F32 if slot == 0 else BF) for slot in range(nrow)],
        in_specs=[vmem()] + [anyspace()] * npiece,
        out_specs=[vmem()] * nrow,
        scratch_shapes=[pltpu.VMEM((units, dim), BF), pltpu.SemaphoreType.DMA((npiece,))],
        compiler_params=params(),
        cost_estimate=cost(2 * tokens * dim * units, 14e6),
        name="mlp_out",
    )(hidden, *down_pieces)


def slice_of(slot, width, own):
    index = lax.axis_index("dp")
    owner = index ^ (2 * slot)
    return pl.ds(pl.multiple_of((owner if own else lax.div(owner, 2)) * width, width), width)

MESH = pl.DeviceIdType.MESH
NEAR = (2, 4, 6)
PARTS = 2
GROUPS = 4


def remote(source, target, send_sem, recv_sem, axis, peer):
    return pltpu.make_async_remote_copy(
        src_ref=source,
        dst_ref=target,
        send_sem=send_sem,
        recv_sem=recv_sem,
        device_id={axis: peer},
        device_id_type=MESH,
    )


def meet():
    own, rank = lax.axis_index("dp"), lax.axis_index("tensor")
    barrier = pltpu.get_barrier_semaphore()
    for flip in range(1, 8):
        pl.semaphore_signal(barrier, inc=1, device_id={"dp": own ^ flip}, device_id_type=MESH)
    for step in range(1, 4):
        pl.semaphore_signal(barrier, inc=1, device_id={"tensor": lax.rem(rank + step, 4)}, device_id_type=MESH)
    pl.semaphore_wait(barrier, 10)


def at_cols(ref, index, width):
    return ref.at[:, pl.ds(pl.multiple_of(index * width, width), width)]


def at_rows(ref, index, width):
    return ref.at[pl.ds(pl.multiple_of(index * width, width), width), :]


def either(rank, *choices):
    result = rank == choices[0]
    for choice in choices[1:]:
        result = result | (rank == choice)
    return result


class RowGather:
    def __init__(self, rank, source, landing, part, size, send, recv):
        self.rank = rank

        def place(slot):
            return landing.at[pl.ds((4 * part + slot) * size, size), :]

        def copy(origin, target, step, sem):
            peer = lax.rem(rank + step + 4, 4)
            return remote(origin, place(target), send.at[part, sem], recv.at[part, target], "tensor", peer)

        self.direct = [None] + [copy(source, step, step, step) for step in (1, 2, 3)]
        self.up = copy(place(2), 3, 1, 0)
        self.down = copy(place(2), 1, -1, 0)

    def start(self):
        self.direct[2].start()
        pl.when(self.rank < 3)(self.direct[1].start)
        pl.when(self.rank > 0)(self.direct[3].start)

    def relay(self):
        @pl.when(self.rank == 2)
        def _():
            self.direct[2].wait_recv()
            self.up.start()

        @pl.when(self.rank == 1)
        def _():
            self.direct[2].wait_recv()
            self.down.start()

    def wait(self):
        pl.when(either(self.rank, 0, 3))(self.direct[2].wait_recv)
        self.direct[1].wait_recv()
        self.direct[3].wait_recv()

    def finish(self):
        self.direct[2].wait_send()
        pl.when(self.rank < 3)(self.direct[1].wait_send)
        pl.when(self.rank > 0)(self.direct[3].wait_send)
        pl.when(self.rank == 2)(self.up.wait_send)
        pl.when(self.rank == 1)(self.down.wait_send)


class RowScatter:
    def __init__(self, rank, source, landing, merge, part, size, send, recv):
        self.rank, self.source, self.merge_in, self.size = rank, source, merge, size
        self.place = lambda k: pl.ds((4 * part + k) * size, size)
        self.merge_at = merge.at[pl.ds(part * size, size), :]

        def copy(k):
            peer = lax.rem(rank - k + 4, 4)
            return remote(
                source.at[self.place(k), :], landing.at[self.place(k), :], send.at[part, k], recv.at[part, k], "tensor", peer
            )

        def far(k, peer):
            return remote(source.at[self.place(k), :], self.merge_at, send.at[part, k], recv.at[part, 0], "tensor", peer)

        self.copy = [None] + [copy(k) for k in (1, 2, 3)]
        self.far_up, self.far_down = far(1, 1), far(3, 2)

    def start(self):
        @pl.when(self.rank == 0)
        def _():
            self.far_up.start()
            self.copy[2].start()
            self.copy[3].start()

        @pl.when(self.rank == 3)
        def _():
            self.far_down.start()
            self.copy[2].start()
            self.copy[1].start()

        @pl.when(either(self.rank, 1, 2))
        def _():
            self.copy[1].start()
            self.copy[3].start()

    def merge(self, staged=None, sem=None):
        @pl.when(either(self.rank, 1, 2))
        def _():
            self.far_up.wait_recv()
            other = self.merge_at
            if staged is not None:
                load = pltpu.make_async_copy(self.merge_at, staged, sem)
                load.start()
                load.wait()
                other = staged
            target = self.source.at[self.place(2), :]

            @pl.loop(0, self.size // 16)
            def _(step):
                rows = pl.ds(pl.multiple_of(step * 16, 16), 16)
                target[rows, :] = (target[rows, :].astype(F32) + other[rows, :].astype(F32)).astype(BF)

            self.copy[2].start()

    def wait(self):
        self.copy[2].wait_recv()
        pl.when(self.rank != 3)(self.copy[1].wait_recv)
        pl.when(self.rank != 0)(self.copy[3].wait_recv)

    def clear(self, target):
        def zero(k):
            target[self.place(k), :] = jnp.zeros((self.size, target.shape[1]), target.dtype)

        pl.when(self.rank == 3)(lambda: zero(1))
        pl.when(self.rank == 0)(lambda: zero(3))

    def finish(self):
        for k in (1, 2, 3):
            self.copy[k].wait_send()


def fill_mask(bias, docs, size):
    rank = lax.axis_index("tensor")
    tokens = bias.shape[0]
    values = docs[...]
    starts = [jnp.sum(jnp.where(values < number, 1, 0), keepdims=True) for number in range(1, 8)]

    def document(position):
        return sum(jnp.where(position >= start, 1, 0) for start in starts)

    lane = lax.broadcasted_iota(jnp.int32, (1, tokens), 1)
    slot = lax.rem(lax.div(lane, size), 4)
    part = lax.div(lane, 4 * size)
    keys = lax.rem(rank - slot + 4, 4) * (2 * size) + part * size + lax.rem(lane, size)
    key_docs = document(keys)

    @pl.loop(0, tokens // size)
    def _(block):
        base = lax.rem(rank - lax.rem(block, 4) + 4, 4) * (2 * size) + lax.div(block, 4) * size
        queries = base + lax.broadcasted_iota(jnp.int32, (size, 1), 0)
        allowed = (document(queries) == key_docs) & (queries >= keys)
        bias[pl.ds(pl.multiple_of(block * size, size), size), :] = jnp.where(allowed, 0.0, NEGATIVE)


def slice_of(slot, width, own):
    index = lax.axis_index("dp")
    owner = index ^ (2 * slot)
    return pl.ds(pl.multiple_of((owner if own else lax.div(owner, 2)) * width, width), width)


def layer_kernel(*refs):
    hidden_in, cot_in, gains_in = refs[:3]
    weights_in = refs[3:10]
    cosine_in, sine_in, docs = refs[10:13]
    down_parts, gate_parts, up_parts, qkv_parts, out_parts = refs[13:18]
    grad_merge = refs[18:23]
    pair_ff = refs[23:26]
    pair_two, pair_cot, pair_qkv, pair_attended, pair_normed, pair_branch = refs[26:32]
    branch_rows, hidden_rows, normed_rows, mlp_recv, mlp_merge, qkv_full, down_full = refs[32:39]
    layer_out, input_grad, gain_total = refs[39:42]
    gate_w, up_w, down_w, sent, cot, normed, hidden, d_gate, d_up = refs[42:51]
    two_half, cot_half, buffer_a, buffer_b, buffer_c, out_w = refs[51:57]
    qkv, attended, d_attended, bias, cosine, sine = refs[57:63]
    inverses_one, inverses, middle, grad_middle, send_part, recv_part, merge_part = refs[63:70]
    gains, gain_part, gain_recv, gain_z = refs[70:74]
    a_send, a_recv, f_send, f_recv, h_send, h_recv, z_send, z_recv, r_send, r_recv = refs[74:84]
    w_send, w_recv, g_send, g_recv, y_send, y_recv, load, keep, down_load = refs[84:]

    own, rank = lax.axis_index("dp"), lax.axis_index("tensor")
    core = lax.rem(own, 2)
    tokens, dim = sent.shape
    units = gate_w.shape[1]
    tile = hidden_in.shape[0]
    size = tile // PARTS
    span = 4 * size
    heads = attended.shape[1]
    width = weights_in[0].shape[0]
    half = dim // (2 * width)
    d_qkv = cot.at[:, pl.ds(heads, 3 * heads)]
    group = units // GROUPS
    step_cols = 256
    count = dim // step_cols

    def cols_of(step, length=step_cols):
        return pl.ds(pl.multiple_of(step * length, length), length)

    def local(source, target, sem):
        return pltpu.make_async_copy(source, target, sem)

    def own_rows(part):
        return pl.ds(part * span, size)

    def part_rows(part):
        return pl.ds(part * size, size)

    def source_of(item):
        if item < 4:
            return weights_in[item]
        which, start = (item - 4) % 3, ((item - 4) // 3) * group
        if which == 2:
            return weights_in[4].at[pl.ds(start, group), :]
        return weights_in[5 + which].at[:, pl.ds(start, group)]

    def view(item, owner, part=None):
        rows = heads if item == 3 else group if item > 3 and (item - 4) % 3 == 2 else width
        length = rows if part is None else rows // 2
        start = 0 if part is None else part * length
        if item < 3:
            place = pl.ds(pl.multiple_of(owner * width + start, length), length)
            return down_w.at[place, pl.ds(item * heads, heads)]
        if item == 3:
            return out_w.at[pl.ds(start, length), pl.ds(pl.multiple_of(owner * width, width), width)]
        which, offset = (item - 4) % 3, ((item - 4) // 3) * group
        if which == 2:
            return down_full.at[pl.ds(offset + start, length), pl.ds(pl.multiple_of(owner * width, width), width)]
        place = pl.ds(pl.multiple_of(owner * width + start, length), length)
        return (gate_w, up_w)[which].at[place, pl.ds(offset, group)]

    def send_weight(item, flip):
        return remote(source_of(item), view(item, own), a_send.at[item, flip], a_recv.at[item, flip], "dp", own ^ flip)

    def relay_weight(item, part):
        place = view(item, own ^ (4 - 2 * part), part)
        return remote(place, place, a_send.at[item, 6 + part], a_recv.at[item, 6 + part], "dp", own ^ (2 + 2 * part))

    def pass_weight(item, flip):
        place = view(item, own ^ flip)
        tag = {2: 3, 4: 5, 6: 8}[flip]
        return remote(place, place, a_send.at[item, tag], a_recv.at[item, tag], "dp", own ^ 1)

    def send_weights(items):
        for item in items:
            for flip in (2, 4, 1):
                send_weight(item, flip).start()

    def relay_weights(items):
        for item in items:
            send_weight(item, 4).wait_recv()
            relay_weight(item, 0).start()
            send_weight(item, 2).wait_recv()
            relay_weight(item, 1).start()
            pass_weight(item, 4).start()
            pass_weight(item, 2).start()

    def pass_weights(items):
        for item in items:
            relay_weight(item, 0).wait_recv()
            relay_weight(item, 1).wait_recv()
            pass_weight(item, 6).start()

    def have_weights(items):
        for item in items:
            send_weight(item, 1).wait_recv()
            for flip in NEAR:
                pass_weight(item, flip).wait_recv()

    def sent_weights(items):
        for item in items:
            for flip in (1, 2, 4):
                send_weight(item, flip).wait_send()
            for flip in NEAR:
                pass_weight(item, flip).wait_send()
            for part in range(2):
                relay_weight(item, part).wait_send()

    def items_of(index):
        return list(range(4 + 3 * index, 7 + 3 * index))

    def send_gain(flip):
        return remote(gains_in, at_cols(gains, own, width), y_send.at[0, flip], y_recv.at[0, flip], "dp", own ^ flip)

    def gathers(kind, source, landing):
        return [
            RowGather(rank, source(part), landing, part, size, z_send.at[kind], z_recv.at[kind]) for part in range(PARTS)
        ]

    gather_hidden = gathers(0, lambda part: hidden_in.at[part_rows(part), :], buffer_b)
    gather_cot = gathers(1, lambda part: cot_in.at[part_rows(part), :], cot)
    gather_sent = gathers(2, lambda part: sent.at[own_rows(part), :], sent)
    gather_branch = gathers(3, lambda part: sent.at[own_rows(part), :], branch_rows)

    def scatters(kind, source, landing, merge):
        return [
            RowScatter(rank, source, landing, merge, part, size, r_send.at[kind], r_recv.at[kind]) for part in range(PARTS)
        ]

    out_scatter = scatters(0, send_part, recv_part, merge_part)
    two_scatter = scatters(1, send_part, recv_part, merge_part)
    mlp_scatter = scatters(2, sent, mlp_recv, mlp_merge)
    one_scatter = scatters(3, send_part, recv_part, merge_part)

    def received(part, start, length, base):
        total = base
        for k in (1, 2, 3):
            rows = pl.ds(pl.multiple_of(part * span + k * size + start, length), length)
            total = total + recv_part[rows, :].astype(F32)
        return total

    def to_pair(source, target, row, slot):
        return remote(source, target, h_send.at[row, slot], h_recv.at[row, slot], "dp", own ^ 1)

    def halves(source, target, row):
        return [
            to_pair(at_cols(source, 2 * slot + 1 - core, width), at_cols(target, slot, width), row, slot)
            for slot in range(half)
        ]

    def send_ff(step, which):
        cols = cols_of(step)
        source = (hidden, d_gate, d_up)[which].at[:, cols]
        return remote(source, pair_ff[which].at[:, cols], f_send.at[step, which], f_recv.at[step, which], "dp", own ^ 1)

    def piece(index, slot):
        if index == 0:
            return at_cols(up_w, slot, width)
        if index < 3:
            return at_rows(gate_w, (index - 1) * 4 + slot, width)
        if index == 3:
            return (hidden, d_gate)[slot // 2].at[pl.ds((slot % 2) * width, width), pl.ds(0, 3 * heads)]
        return at_cols(d_up, slot, width)

    def landing_of(index, slot):
        ref = (down_parts, gate_parts, up_parts, qkv_parts, out_parts)[index]
        return at_cols(ref, slot, width) if index in (0, 4) else at_rows(ref, slot, width)

    def half_of(ref, index, part):
        rows, cols = ref.shape
        if index in (0, 4):
            return ref.at[pl.ds(part * (rows // 2), rows // 2), :]
        return ref.at[:, pl.ds(part * (cols // 2), cols // 2)]

    def stage_of(index, part):
        if index == 0:
            return up_w.at[pl.ds(0, units // 2), pl.ds((4 + part) * width, width)]
        if index == 4:
            return up_w.at[pl.ds(0, heads // 2), pl.ds((4 + part) * width, width)]
        length = (0, units // 2, units // 2, 3 * heads // 2)[index]
        return up_w.at[pl.ds((4 + part + 2 * (index == 2)) * width, width), pl.ds(4 * width, length)]

    def send_far(index, part):
        return remote(
            half_of(piece(index, 3), index, part),
            half_of(grad_merge[index], index, part),
            w_send.at[index, part],
            w_recv.at[index, part],
            "dp",
            own ^ (2 + 2 * part),
        )

    def send_near(index, slot, part):
        tag = 2 * slot + part
        return remote(
            half_of(piece(index, slot), index, part),
            half_of(landing_of(index, slot), index, part),
            w_send.at[index, tag],
            w_recv.at[index, tag],
            "dp",
            own ^ (2 * slot),
        )

    def keep_grad(index):
        return local(piece(index, 0), landing_of(index, 0), keep.at[index])

    def merge_grads(index):
        loads = [local(half_of(grad_merge[index], index, part), stage_of(index, part), load.at[part]) for part in range(2)]
        for part in range(2):
            send_far(index, part).wait_recv()
            loads[part].start()
        for part in range(2):
            loads[part].wait()
            target, source = half_of(piece(index, 2 - part), index, part), stage_of(index, part)
            length = source.shape[0] // 4

            @pl.loop(0, 4)
            def _(step):
                rows = cols_of(step, length)
                target[rows, :] = (target[rows, :].astype(F32) + source[rows, :].astype(F32)).astype(BF)

            send_near(index, 2 - part, part).start()

    def row_grads(index, left, left_pair, right, right_pair, columns):
        for slot in (3, 1, 2, 0):
            mine, theirs = slice_of(slot, width, True), slice_of(slot, width, False)
            turned, turned_pair = jnp.transpose(left[:, mine]), jnp.transpose(left_pair[:, theirs])
            target = piece(index, slot)

            @pl.loop(0, columns // 512)
            def _(step):
                cols = cols_of(step, 512)
                total = dot(turned, right[:, cols]) + dot(turned_pair, right_pair[:, cols])
                target[:, cols] = total.astype(BF)

            if slot == 3:
                send_far(index, 0).start()
                send_far(index, 1).start()
            elif slot == 0:
                keep_grad(index).start()
            else:
                send_near(index, slot, slot - 1).start()

    def col_grads(index, left, left_pair, right, right_pair, columns):
        for part in range(2):

            @pl.loop(part * columns // 512, (part + 1) * columns // 512)
            def _(step):
                rows = cols_of(step, 256)
                turned, turned_pair = jnp.transpose(left[:, rows]), jnp.transpose(left_pair[:, rows])
                for slot in range(4):
                    mine, theirs = slice_of(slot, width, True), slice_of(slot, width, False)
                    total = dot(turned, right[:, mine]) + dot(turned_pair, right_pair[:, theirs])
                    piece(index, slot)[rows, :] = total.astype(BF)

            send_far(index, part).start()
            send_near(index, part + 1, part).start()
        keep_grad(index).start()

    def norm_back(total, values, gain):
        inverse = lax.rsqrt(jnp.mean(values * values, axis=-1, keepdims=True) + EPSILON)
        scaled = total * gain
        return inverse * (scaled - values * inverse * inverse * jnp.mean(scaled * values, axis=-1, keepdims=True))

    meet()
    for gather in gather_hidden:
        gather.start()
    for flip in range(1, 8):
        send_gain(flip).start()
    send_weights(range(4))
    stage_down = down_w.at[:, pl.ds(3 * heads, width)]
    stage_in = local(weights_in[4], stage_down, load.at[0])
    own_loads = [local(gains_in, at_cols(gains, own, width), load.at[1])]
    own_loads += [local(weights_in[item], view(item, own), load.at[2 + item]) for item in range(4)]
    own_loads += [local(weights_in[5], at_rows(gate_w, own, width), load.at[6])]
    own_loads += [local(weights_in[6], at_rows(up_w, own, width), load.at[7])]
    for part in range(PARTS):
        own_loads.append(local(hidden_in.at[part_rows(part), :], buffer_b.at[own_rows(part), :], load.at[8 + part]))
        own_loads.append(local(cot_in.at[part_rows(part), :], cot.at[own_rows(part), :], load.at[10 + part]))
    for block in range(4 * PARTS):
        start = lax.rem(rank - block % 4 + 4, 4) * tile + (block // 4) * size
        for which, (source, target) in enumerate(((cosine_in, cosine), (sine_in, sine))):
            rows = pl.ds(pl.multiple_of(start, size), size)
            own_loads.append(
                local(source.at[rows, :], target.at[pl.ds(block * size, size), :], load.at[12 + 2 * block + which])
            )
    start_all([stage_in] + own_loads)
    fill_mask(bias, docs, size)
    relay_weights(range(4))
    for index in range(GROUPS):
        send_weights(items_of(index))
    for gather in gather_hidden:
        gather.relay()
    for gather in gather_cot:
        gather.start()
    stage_in.wait()
    stage_out = local(stage_down, at_cols(down_full, own, width), keep.at[5])
    stage_out.start()
    pass_weights(range(4))
    wait_all(own_loads)
    for flip in range(1, 8):
        send_gain(flip).wait_recv()
    for gather in gather_hidden:
        gather.wait()

    norm_rows(buffer_b, buffer_c, inverses_one, gains.at[pl.ds(0, 1), :], 64)
    keep_hidden = local(buffer_b, hidden_rows, keep.at[0])
    keep_normed = local(buffer_c, normed_rows, keep.at[1])
    start_all([keep_hidden, keep_normed])
    have_weights(range(4))
    qkv_w = down_w.at[:, pl.ds(0, 3 * heads)]
    keep_qkv = local(qkv_w, qkv_full, keep.at[2])
    keep_qkv.start()

    @pl.loop(0, 2 * heads // step_cols)
    def _(step):
        cols = cols_of(step)
        product = dot(buffer_c[...], down_w[:, cols])
        turns = [jnp.concatenate([table[...]] * (step_cols // 128), axis=1) for table in (cosine, sine)]
        qkv[:, cols] = turn(product, *turns).astype(BF)

    @pl.loop(2 * heads // step_cols, 3 * heads // step_cols)
    def _(step):
        cols = cols_of(step)
        qkv[:, cols] = dot(buffer_c[...], down_w[:, cols]).astype(BF)

    attend(qkv, attended, bias, heads)
    for gather in gather_cot:
        gather.relay()
    for part in range(PARTS):

        @pl.loop(0, count)
        def _(step):
            cols = cols_of(step)
            product = dot(attended[part * span : (part + 1) * span, :], out_w[:, cols])
            middle[part_rows(part), cols] = product[:size, :]
            send_part[pl.ds(part * span + size, span - size), cols] = product[size:, :].astype(BF)

        out_scatter[part].start()
    wait_all([keep_hidden, keep_normed, keep_qkv, stage_out])
    send_normed = halves(normed_rows, pair_normed, 1)
    send_attended = to_pair(attended, pair_attended, 2, 0)
    start_all(send_normed + [send_attended])
    relay_weights(items_of(0))
    for part in range(PARTS):
        out_scatter[part].clear(recv_part)
    out_scatter[0].merge()
    relay_weights(items_of(1))
    out_scatter[1].merge()

    def make_sent(part):
        out_scatter[part].wait()

        @pl.loop(0, size // 32)
        def _(step):
            rows = pl.ds(pl.multiple_of(part * size + step * 32, 32), 32)
            place = pl.ds(pl.multiple_of(part * span + step * 32, 32), 32)
            total = received(part, step * 32, 32, hidden_of(place) + middle[rows, :])
            middle[rows, :] = total
            sent[place, :] = total.astype(BF)

        gather_sent[part].start()

    def hidden_of(place):
        return buffer_b[place, :].astype(F32)

    make_sent(0)
    relay_weights(items_of(2))
    gather_sent[0].relay()
    make_sent(1)
    for gather in gather_cot:
        gather.wait()
    send_cot = halves(cot, pair_cot, 0)
    start_all(send_cot)
    relay_weights(items_of(3))
    gather_sent[1].relay()
    pass_weights(items_of(0))

    def load_down(index):
        rows = pl.ds(index * group, group)
        return local(down_full.at[rows, :], down_w.at[rows, :], down_load.at[index])

    pass_weights(items_of(1))
    have_weights(items_of(0))
    sent_weights(range(4))
    load_down(0).start()
    for gather in gather_sent:
        gather.wait()
    norm_rows(sent, normed, inverses, gains.at[pl.ds(1, 1), :], 64)
    send_two = halves(normed, pair_two, 3)
    start_all(send_two)
    for index in range(GROUPS):
        if index + 1 < GROUPS:
            if index + 1 > 1:
                pass_weights(items_of(index + 1))
            have_weights(items_of(index + 1))
            load_down(index + 1).start()
        load_down(index).wait()

        @pl.loop(index * group // step_cols, (index + 1) * group // step_cols)
        def _(step):
            cols = cols_of(step)
            gate = dot(normed[...], gate_w[:, cols])
            up = dot(normed[...], up_w[:, cols])
            d_hidden = dot_rows(cot[...], down_w[cols, :])
            s = jax.nn.sigmoid(gate)
            activated = gate * s
            hidden[:, cols] = (activated * up).astype(BF)
            d_gate[:, cols] = (d_hidden * up * (s + activated * (1.0 - s))).astype(BF)
            d_up[:, cols] = (d_hidden * activated).astype(BF)
            for which in range(3):
                send_ff(step, which).start()

    gain_part[...] = jnp.zeros(gain_part.shape, F32)
    for part in range(PARTS):
        out_scatter[part].finish()

    def make_two(part):
        block = slice(part * span, (part + 1) * span)

        @pl.loop(0, count)
        def _(step):
            cols = cols_of(step)
            product = dot_rows(d_gate[block, :], gate_w[cols, :]) + dot_rows(d_up[block, :], up_w[cols, :])
            gain_part[pl.ds(1, 1), cols] += jnp.sum(
                product * (sent[block, cols].astype(F32) * inverses[block, :]), axis=0, keepdims=True
            )
            grad_middle[part_rows(part), cols] = product[:size, :]
            send_part[pl.ds(part * span + size, span - size), cols] = product[size:, :].astype(BF)

        two_scatter[part].start()

    def pair_ready(which):
        @pl.loop(0, units // step_cols)
        def _(step):
            send_ff(step, which).wait_recv()

    make_two(0)
    make_two(1)
    for which in range(3):
        pair_ready(which)
    for copy in send_cot + send_two:
        copy.wait_recv()
    pair_loads = [
        local(pair_ff[0], buffer_a, load.at[0]),
        local(pair_cot, cot_half, load.at[1]),
        local(pair_ff[1], buffer_b, load.at[2]),
        local(pair_two, two_half, load.at[3]),
        local(pair_ff[2], buffer_c, load.at[4]),
    ]
    for gather in gather_hidden + gather_cot:
        gather.finish()
    start_all(pair_loads)
    sent_weights(range(4, 4 + 3 * GROUPS))
    two_scatter[0].merge()
    wait_all(pair_loads)
    col_grads(0, hidden, buffer_a, cot, cot_half, units)
    two_scatter[1].merge()
    row_grads(1, normed, two_half, d_gate, buffer_b, units)

    def make_branch(part):
        two_scatter[part].wait()

        @pl.loop(0, size // 32)
        def _(step):
            rows = pl.ds(pl.multiple_of(part * size + step * 32, 32), 32)
            place = pl.ds(pl.multiple_of(part * span + step * 32, 32), 32)
            total = received(part, step * 32, 32, grad_middle[rows, :])
            result = cot[place, :].astype(F32) + norm_back(total, sent[place, :].astype(F32), gains[1:2, :])
            grad_middle[rows, :] = result
            sent[place, :] = result.astype(BF)

        gather_branch[part].start()
        keep_branch[part].start()

    keep_branch = [
        local(sent.at[own_rows(part), :], branch_rows.at[own_rows(part), :], keep.at[6 + part]) for part in range(PARTS)
    ]
    for part in range(PARTS):
        gather_sent[part].finish()
    make_branch(0)
    row_grads(2, normed, two_half, d_up, buffer_c, units)
    gather_branch[0].relay()
    make_branch(1)
    merge_grads(0)

    @pl.loop(0, count)
    def _(step):
        cols = cols_of(step)
        product = dot(hidden[...], down_w[:, cols])
        for part in range(PARTS):
            start = part * span
            middle[part_rows(part), cols] = middle[part_rows(part), cols] + product[start : start + size, :]
            sent[pl.ds(start + size, span - size), cols] = product[start + size : start + span, :].astype(BF)

    merge_grads(1)
    gather_branch[1].relay()
    for scatter in mlp_scatter:
        scatter.start()
    merge_grads(2)
    load_weight = local(qkv_full, qkv_w, load.at[0])
    load_hidden = local(hidden_rows, buffer_b, load.at[1])
    load_normed = local(normed_rows, buffer_c, load.at[2])
    start_all([load_weight, load_hidden, load_normed])
    for part in range(PARTS):
        two_scatter[part].finish()
        gather_branch[part].wait()
        keep_branch[part].wait()

    load_branch = local(branch_rows, buffer_a, load.at[3])
    load_branch.start()
    send_half = halves(branch_rows, pair_branch, 4)
    start_all(send_half)
    load_branch.wait()

    @pl.loop(0, heads // step_cols)
    def _(step):
        cols = cols_of(step)
        d_attended[:, cols] = dot_rows(buffer_a[...], out_w[cols, :]).astype(BF)

    for copy in send_cot:
        copy.wait_send()
    attend_back(qkv, d_attended, d_qkv, bias, cosine, sine, heads)
    send_qkv = to_pair(d_qkv, pair_qkv, 5, 0)
    send_qkv.start()
    @pl.loop(0, units // step_cols)
    def _(step):
        for which in range(3):
            send_ff(step, which).wait_send()

    for part in range(PARTS):
        mlp_scatter[part].merge(d_up.at[part_rows(part), :], load.at[3])
    wait_all([load_weight, load_hidden, load_normed])
    for part in range(PARTS):
        block = slice(part * span, (part + 1) * span)

        @pl.loop(0, count)
        def _(step):
            cols = cols_of(step)
            product = dot_rows(d_qkv[block, :], down_w[cols, pl.ds(0, 3 * heads)])
            gain_part[pl.ds(0, 1), cols] += jnp.sum(
                product * (buffer_b[block, cols].astype(F32) * inverses_one[block, :]), axis=0, keepdims=True
            )
            input_grad[part_rows(part), cols] = product[:size, :]
            send_part[pl.ds(part * span + size, span - size), cols] = product[size:, :].astype(BF)

        one_scatter[part].start()

    def share_gain(flip):
        source = at_cols(gain_part, own ^ flip, width)
        return remote(source, at_rows(gain_recv, flip, 8), g_send.at[flip], g_recv.at[flip], "dp", own ^ flip)

    for flip in range(1, 8):
        share_gain(flip).start()

    for index in range(3):
        keep_grad(index).wait()
    send_qkv.wait_recv()
    for copy in send_half + send_normed + [send_attended]:
        copy.wait_recv()

    for copy in send_two:
        copy.wait_send()
    last_loads = [
        local(pair_qkv, normed.at[:, pl.ds(0, 3 * heads)], load.at[0]),
        local(pair_attended, cot.at[:, pl.ds(0, heads)], load.at[1]),
        local(pair_normed, two_half, load.at[2]),
        local(pair_branch, cot_half, load.at[3]),
    ]
    start_all(last_loads)
    wait_all(last_loads)
    col_grads(4, attended, cot, buffer_a, cot_half, heads)
    row_grads(3, buffer_c, two_half, d_qkv, normed, 3 * heads)
    for part in range(PARTS):
        one_scatter[part].merge()
    merge_grads(4)
    merge_grads(3)

    for flip in range(1, 8):
        share_gain(flip).wait_recv()
    gain_sum = gain_part[:, pl.ds(pl.multiple_of(own * width, width), width)]
    for flip in range(1, 8):
        gain_sum = gain_sum + gain_recv[pl.ds(flip * 8, 8), :]
    gain_z[pl.ds(0, 8), :] = gain_sum

    def share_gain_z(k):
        target = gain_z.at[pl.ds(8 * k, 8), :]
        return remote(gain_z.at[pl.ds(0, 8), :], target, y_send.at[1, k], y_recv.at[1, k], "tensor", lax.rem(rank + k, 4))

    for k in (1, 2, 3):
        share_gain_z(k).start()

    load_own = [
        local(hidden_in.at[part_rows(part), :], sent.at[own_rows(part), :], load.at[4 + part]) for part in range(PARTS)
    ]
    for part in range(PARTS):
        gather_branch[part].finish()
    start_all(load_own)
    wait_all(load_own)
    for part in range(PARTS):
        one_scatter[part].wait()

        @pl.loop(0, size // 32)
        def _(step):
            rows = pl.ds(pl.multiple_of(part * size + step * 32, 32), 32)
            place = pl.ds(pl.multiple_of(part * span + step * 32, 32), 32)
            total = received(part, step * 32, 32, input_grad[rows, :])
            input_grad[rows, :] = grad_middle[rows, :] + norm_back(total, sent[place, :].astype(F32), gains[0:1, :])

    for scatter in mlp_scatter:
        scatter.wait()
    load_mlp = local(mlp_recv, recv_part, load.at[0])
    load_mlp.start()
    load_mlp.wait()
    for part in range(PARTS):
        mlp_scatter[part].clear(recv_part)

        @pl.loop(0, size // 32)
        def _(step):
            rows = pl.ds(pl.multiple_of(part * size + step * 32, 32), 32)
            layer_out[rows, :] = received(part, step * 32, 32, middle[rows, :]).astype(BF)

    for k in (1, 2, 3):
        share_gain_z(k).wait_recv()
    gain_all = gain_z[pl.ds(0, 8), :]
    for k in (1, 2, 3):
        gain_all = gain_all + gain_z[pl.ds(8 * k, 8), :]
    gain_total[...] = gain_all

    for scatter in mlp_scatter + one_scatter:
        scatter.finish()
    for flip in range(1, 8):
        send_gain(flip).wait_send()
        share_gain(flip).wait_send()
    for k in (1, 2, 3):
        share_gain_z(k).wait_send()
    for copy in send_normed + send_half + [send_attended, send_qkv]:
        copy.wait_send()
    for index in range(5):
        for slot in range(1, 3):
            for part in range(2):
                send_near(index, slot, part).wait_recv()
    for index in range(3, 5):
        keep_grad(index).wait()
    for index in range(5):
        for part in range(2):
            send_far(index, part).wait_send()
            for slot in range(1, 3):
                send_near(index, slot, part).wait_send()


def layer(hidden_in, cot, gains, weights, cosine, sine, docs):
    tile, dim = hidden_in.shape
    tokens = 4 * tile
    width, heads = weights[0].shape
    units = weights[5].shape[1]
    dma = pltpu.SemaphoreType.DMA
    rows, narrow, ff = shape((tokens, dim), BF), shape((tokens, dim // 2), BF), shape((tokens, units), BF)
    weights_shape = [(units, width), (width, units), (width, units), (width, 3 * heads), (heads, width)]
    parts_shape = [(units, 3 * width), (3 * width, units), (3 * width, units), (3 * width, 3 * heads), (heads, 3 * width)]
    outs = [shape(dims, BF) for dims in parts_shape + weights_shape]
    outs += [ff] * 3 + [narrow, narrow, shape((tokens, 3 * heads), BF), shape((tokens, heads), BF), narrow, narrow]
    outs += [rows] * 4 + [shape((tile, dim), BF), shape((dim, 3 * heads), BF), shape((units, dim), BF)]
    in_hbm = len(outs)
    outs += [shape((tile, dim), BF), shape((tile, dim), F32), shape((8, width), F32)]
    items = 4 + 3 * GROUPS
    scratch = [((dim, units), BF), ((dim, units), BF), ((units, dim), BF)]
    scratch += [((tokens, dim), BF)] * 3 + [((tokens, units), BF)] * 3
    scratch += [((tokens, dim // 2), BF)] * 2 + [((tokens, dim), BF)] * 3 + [((heads, dim), BF)]
    scratch += [((tokens, 3 * heads), BF)] + [((tokens, heads), BF)] * 2
    scratch += [((tokens, tokens), F32), ((tokens, 128), F32), ((tokens, 128), F32)]
    scratch += [((tokens, 1), F32), ((tokens, 1), F32), ((tile, dim), F32), ((tile, dim), F32)]
    scratch += [((tokens, dim), BF), ((tokens, dim), BF), ((tile, dim), BF)]
    scratch += [((8, dim), F32), ((8, dim), F32), ((64, width), F32), ((32, width), F32)]
    sems = [(items, 9)] * 2 + [(units // 256, 3)] * 2 + [(6, 4)] * 2 + [(4, PARTS, 4)] * 4 + [(5, 6)] * 2
    sems += [(8,)] * 2 + [(2, 8)] * 2 + [(12 + 8 * PARTS,), (6 + PARTS,), (GROUPS,)]
    return pl.pallas_call(
        layer_kernel,
        out_shape=outs,
        in_specs=[anyspace()] * 12 + [vmem()],
        out_specs=[anyspace()] * in_hbm + [vmem()] * 3,
        scratch_shapes=[pltpu.VMEM(*entry) for entry in scratch] + [dma(entry) for entry in sems],
        compiler_params=pltpu.CompilerParams(vmem_limit_bytes=67000000, collective_id=0, has_side_effects=True),
        cost_estimate=cost(2 * tokens * dim * units * 12, 100e6),
        name="layer",
    )(hidden_in, cot, gains, *weights, cosine, sine, docs)


def shift(values, step):
    size = lax.axis_size("tensor")
    return lax.ppermute(values, "tensor", [(index, (index + step) % size) for index in range(size)])


def gather_rows(values):
    return [values] + [shift(values, step) for step in range(1, lax.axis_size("tensor"))]


def scatter_rows(parts):
    total = parts[0].astype(F32)
    for step in range(1, len(parts)):
        total = total + shift(parts[step], -step).astype(F32)
    return total


def gather_weight(values, axis):
    return [None], [lax.all_gather(values, "dp", axis=axis, tiled=True)]


def scatter_full(left, right, axis):
    full = dot_cols(left, right).astype(BF)
    return lax.psum_scatter(full, "dp", scatter_dimension=axis, tiled=True).astype(F32)


def sum_parts(parts, axis):
    pieces = jnp.split(parts, 3, axis=axis)
    return sum(piece.astype(F32) for piece in pieces)


def rotary(length):
    half_size = HEAD_DIM // 2
    frequency = ROPE_BASE ** (-jnp.arange(half_size, dtype=F32) / half_size)
    angles = jnp.arange(length).astype(F32)[:, None] * frequency[None, :]
    cosine, sine = jnp.cos(angles), jnp.sin(angles)
    cosine = jnp.tile(cosine, (1, 8))
    sine = jnp.tile(jnp.concatenate([-sine, sine], axis=1), (1, 4))
    return cosine, sine


def position_tables(doc_ids, ranks):
    length = doc_ids.shape[0]
    token_index = jnp.arange(length, dtype=jnp.int32)
    before = jnp.concatenate([doc_ids[:1] - 1, doc_ids[:-1]])
    doc_start = lax.cummax(jnp.where(doc_ids != before, token_index, 0), axis=0)
    order = (lax.axis_index("tensor") - jnp.arange(ranks)) % ranks
    last = token_index.reshape(ranks, -1)[order].reshape(length)
    first = doc_start.reshape(ranks, -1)[order].reshape(length)
    cosine, sine = (table.reshape(ranks, -1, 256)[order].reshape(length, 256) for table in rotary(length))
    return cosine, sine, first[:, None], last[:, None], last[None, :]


def rms_back(grad_rows_, values, gain):
    inverse = lax.rsqrt(jnp.mean(values * values, axis=-1, keepdims=True) + EPSILON)
    scaled = grad_rows_ * gain
    return inverse * (scaled - values * inverse * inverse * jnp.mean(scaled * values, axis=-1, keepdims=True))


def body(
    hidden_in,
    out_cotangent,
    doc_ids,
    attn_gain,
    query_weight,
    key_weight,
    value_weight,
    out_weight,
    mlp_gain,
    gate_weight,
    up_weight,
    down_weight,
):
    ranks, groups = lax.axis_size("tensor"), lax.axis_size("dp")
    paired = (groups, ranks) == (8, 4)
    width, heads = query_weight.shape
    dim = hidden_in.shape[1]

    if paired:
        pad = jnp.zeros((6, width), F32)
        own_gains = jnp.concatenate([attn_gain[None].astype(F32), mlp_gain[None].astype(F32), pad], axis=0)
        weights = (query_weight, key_weight, value_weight, out_weight, down_weight, gate_weight, up_weight)
        turns = [table[:, :128] for table in rotary(doc_ids.shape[0])]
        outs = layer(hidden_in, out_cotangent, own_gains, weights, *turns, doc_ids.reshape(ranks, -1))
        down_grad, gate_grad, up_grad, qkv_grad, out_proj_grad = (
            sum_parts(part, axis) for part, axis in zip(outs[:5], (1, 0, 0, 0, 1))
        )
        layer_out, input_grad, gain_total = outs[-3:]
        share = width // ranks
        gain_grads = lax.dynamic_slice_in_dim(gain_total, lax.axis_index("tensor") * share, share, axis=1)
    else:
        tables = position_tables(doc_ids, ranks)
        input_local = hidden_in.astype(F32)
        hidden_rows = gather_rows(hidden_in)
        gains = lax.all_gather(jnp.stack([attn_gain, mlp_gain]), "dp", axis=1, tiled=True).astype(F32)
        attn_scale, mlp_scale = gains[:1], gains[1:]
        qkv_weight = jnp.concatenate([query_weight, key_weight, value_weight], axis=1)
        tags, qkv_pieces = gather_weight(qkv_weight, 0)
        tags, out_pieces = gather_weight(out_weight, 1)
        cot_rows = gather_rows(out_cotangent)
        tags, down_pieces = gather_weight(down_weight, 1)
        tags, gate_pieces = gather_weight(gate_weight, 0)
        tags, up_pieces = gather_weight(up_weight, 0)
        normed, qkv, attended, inverses, *branch_parts = attn_fwd(
            hidden_rows, attn_scale, tables, tags, width, qkv_pieces, out_pieces
        )
        middle = input_local + scatter_rows(branch_parts)
        sent = middle.astype(BF)
        sent_rows = gather_rows(sent)
        cot_full = jnp.concatenate(cot_rows, axis=0)
        normed_two, hidden, d_gate, d_up, mlp_gain_part, *two_parts = mlp(
            sent_rows, cot_rows, mlp_scale, tags, width, gate_pieces, up_pieces, down_pieces, ranks
        )
        grad_two_rows = scatter_rows(two_parts)
        grad_middle = out_cotangent.astype(F32) + rms_back(grad_two_rows, sent.astype(F32), mlp_scale)
        branch_rows = gather_rows(grad_middle.astype(BF))
        down_grad = scatter_full(hidden, cot_full, 1)
        gate_grad = scatter_full(normed_two, d_gate, 0)
        up_grad = scatter_full(normed_two, d_up, 0)
        mlp_rows = scatter_rows(mlp_out(hidden, ranks, dim, tags, width, down_pieces))
        layer_out = (middle + mlp_rows).astype(BF)
        branch_full, d_qkv, attn_gain_part, *one_parts = attn_bwd(
            branch_rows, hidden_rows, qkv, inverses, tables, tags, width, qkv_pieces, out_pieces, ranks
        )
        out_proj_grad = scatter_full(attended, branch_full, 1)
        qkv_grad = scatter_full(normed, d_qkv, 0)
        grad_one_rows = scatter_rows(one_parts)
        input_grad = grad_middle + rms_back(grad_one_rows, input_local, attn_scale)
        gain_parts = jnp.concatenate([attn_gain_part, mlp_gain_part], axis=0)
        gain_grads = lax.psum_scatter(gain_parts, ("dp", "tensor"), scatter_dimension=1, tiled=True)
    return (
        layer_out,
        input_grad,
        gain_grads[0],
        qkv_grad[:, :heads],
        qkv_grad[:, heads : 2 * heads],
        qkv_grad[:, 2 * heads :],
        out_proj_grad,
        gain_grads[1],
        gate_grad,
        up_grad,
        down_grad,
    )


def solution(mesh):
    return jax.shard_map(
        body,
        mesh=mesh,
        in_specs=(
            P(("dp", "tensor"), None),
            P(("dp", "tensor"), None),
            P("dp"),
            P("dp"),
            P("dp", "tensor"),
            P("dp", "tensor"),
            P("dp", "tensor"),
            P("tensor", "dp"),
            P("dp"),
            P("dp", "tensor"),
            P("dp", "tensor"),
            P("tensor", "dp"),
        ),
        out_specs=(
            P(("dp", "tensor"), None),
            P(("dp", "tensor"), None),
            P(("dp", "tensor")),
            P("dp", "tensor"),
            P("dp", "tensor"),
            P("dp", "tensor"),
            P("tensor", "dp"),
            P(("dp", "tensor")),
            P("dp", "tensor"),
            P("dp", "tensor"),
            P("tensor", "dp"),
        ),
        check_vma=False,
    )
```

```python
from functools import partial

import jax
import jax.numpy as jnp
from jax import lax
from jax.experimental import pallas as pl
from jax.experimental.pallas import tpu as pltpu
from jax.sharding import PartitionSpec as P

HEAD_DIM = 64
EPSILON = 1e-05
ROPE_BASE = 130000.0
NEGATIVE = -1e30
VMEM_LIMIT = 63 * 1024 * 1024
BF = jnp.bfloat16
F32 = jnp.float32


def dot(left, right):
    return jnp.dot(left, right, preferred_element_type=F32)


def dot_rows(left, right):
    return lax.dot_general(left, right, (((1,), (1,)), ((), ())), preferred_element_type=F32)


def dot_cols(left, right):
    return lax.dot_general(left, right, (((0,), (0,)), ((), ())), preferred_element_type=F32)


def vmem():
    return pl.BlockSpec(memory_space=pltpu.VMEM)


def anyspace():
    return pl.BlockSpec(memory_space=pl.ANY)


def params():
    return pltpu.CompilerParams(vmem_limit_bytes=VMEM_LIMIT)


def cost(flops, nbytes):
    return pl.CostEstimate(flops=int(flops), bytes_accessed=int(nbytes), transcendentals=0)


def shape(dims, kind):
    return jax.ShapeDtypeStruct(dims, kind)


def place_copies(tags, pieces, target, sem, axis, width):
    own = lax.axis_index("dp")
    copies = []
    for slot, (tag, piece) in enumerate(zip(tags, pieces)):
        if tag is None:
            where = target
        else:
            start = pl.multiple_of((own ^ tag) * width, width)
            where = target.at[pl.ds(start, width), :] if axis == 0 else target.at[:, pl.ds(start, width)]
        copies.append(pltpu.make_async_copy(piece, where, sem.at[slot]))
    return copies


def row_copies(pieces, target, sem):
    copies = []
    for slot, piece in enumerate(pieces):
        rows = piece.shape[0]
        copies.append(pltpu.make_async_copy(piece, target.at[pl.ds(slot * rows, rows), :], sem.at[slot]))
    return copies


def start_all(copies):
    for copy in copies:
        copy.start()


def wait_all(copies):
    for copy in copies:
        copy.wait()


def turn(values, cosine, sine):
    width = values.shape[1]
    lane = lax.broadcasted_iota(jnp.int32, values.shape, 1)
    partner = jnp.where(
        lax.rem(lane, HEAD_DIM) < HEAD_DIM // 2,
        pltpu.roll(values, width - HEAD_DIM // 2, 1),
        pltpu.roll(values, HEAD_DIM // 2, 1),
    )
    return values * cosine + partner * sine


def norm_rows(source, target, inverses, gain, tile):
    @pl.loop(0, source.shape[0] // tile)
    def _(step):
        rows = pl.ds(pl.multiple_of(step * tile, tile), tile)
        values = source[rows, :].astype(F32)
        inverse = lax.rsqrt(jnp.mean(values * values, axis=-1, keepdims=True) + EPSILON)
        inverses[rows, :] = inverse
        target[rows, :] = (values * inverse * gain[...]).astype(BF)


def fill_bias(bias, first, last, key_index):
    keys = key_index[...]
    bias[...] = jnp.where((keys >= first[...]) & (keys <= last[...]), 0.0, NEGATIVE)


def head_lanes(width, half):
    lane = lax.broadcasted_iota(jnp.int32, (1, width), 1)
    return (lax.div(lane, HEAD_DIM) == half).astype(F32)


def probabilities(query, key, bias):
    scores = dot_rows(query, key) + bias
    weights = jnp.exp(scores - jnp.max(scores, axis=-1, keepdims=True))
    return weights * (1.0 / jnp.sum(weights, axis=-1, keepdims=True))


def attend(qkv, attended, bias, heads):
    @pl.loop(0, heads // 128)
    def _(pair):
        base = pl.multiple_of(pair * 128, 128)
        query = qkv[:, pl.ds(base, 128)]
        key = qkv[:, pl.ds(heads + base, 128)]
        value = qkv[:, pl.ds(2 * heads + base, 128)]
        total = None
        for half in range(2):
            lanes = head_lanes(128, half).astype(BF)
            probs = probabilities(query * (lanes * HEAD_DIM ** (-0.5)), key, bias[...])
            term = dot(probs.astype(BF), value * lanes)
            total = term if total is None else total + term
        attended[:, pl.ds(base, 128)] = total.astype(BF)


def attn_fwd_kernel(tags, width, nrow, *refs):
    npiece = len(tags)
    rows_in = refs[:nrow]
    gain, cosine, sine, first, last, key_index = refs[nrow : nrow + 6]
    rest = refs[nrow + 6 :]
    qkv_in, out_in = rest[:npiece], rest[npiece : 2 * npiece]
    rest = rest[2 * npiece :]
    normed, qkv, attended, inverses = rest[:4]
    parts = rest[4 : 4 + nrow]
    hidden, qkv_w, out_w, bias, sem_rows, sem_qkv, sem_out = rest[4 + nrow :]
    load_rows = row_copies(rows_in, hidden, sem_rows)
    load_qkv = place_copies(tags, qkv_in, qkv_w, sem_qkv, 0, width)
    load_out = place_copies(tags, out_in, out_w, sem_out, 1, width)
    start_all(load_rows + load_qkv + load_out)
    fill_bias(bias, first, last, key_index)
    wait_all(load_rows)
    norm_rows(hidden, normed, inverses, gain, 64)
    wait_all(load_qkv)
    heads = attended.shape[1]
    step_cols = 256

    @pl.loop(0, 2 * heads // step_cols)
    def _(step):
        cols = pl.ds(pl.multiple_of(step * step_cols, step_cols), step_cols)
        qkv[:, cols] = turn(dot(normed[...], qkv_w[:, cols]), cosine[...], sine[...]).astype(BF)

    @pl.loop(2 * heads // step_cols, 3 * heads // step_cols)
    def _(step):
        cols = pl.ds(pl.multiple_of(step * step_cols, step_cols), step_cols)
        qkv[:, cols] = dot(normed[...], qkv_w[:, cols]).astype(BF)

    attend(qkv, attended, bias, heads)
    wait_all(load_out)
    tile = parts[0].shape[0]

    @pl.loop(0, out_w.shape[1] // step_cols)
    def _(step):
        cols = pl.ds(pl.multiple_of(step * step_cols, step_cols), step_cols)
        product = dot(attended[...], out_w[:, cols])
        for slot, part in enumerate(parts):
            part[:, cols] = product[slot * tile : (slot + 1) * tile, :].astype(part.dtype)


def attn_fwd(rows, gain, tables, tags, width, qkv_pieces, out_pieces):
    nrow, (tile, dim) = len(rows), rows[0].shape
    tokens = nrow * tile
    heads = out_pieces[0].shape[0]
    npiece = len(tags)
    return pl.pallas_call(
        partial(attn_fwd_kernel, tags, width, nrow),
        out_shape=[
            shape((tokens, dim), BF),
            shape((tokens, 3 * heads), BF),
            shape((tokens, heads), BF),
            shape((tokens, 1), F32),
        ]
        + [shape((tile, dim), F32 if slot == 0 else BF) for slot in range(nrow)],
        in_specs=[anyspace()] * nrow + [vmem()] * 6 + [anyspace()] * (2 * npiece),
        out_specs=[vmem()] * (4 + nrow),
        scratch_shapes=[
            pltpu.VMEM((tokens, dim), BF),
            pltpu.VMEM((dim, 3 * heads), BF),
            pltpu.VMEM((heads, dim), BF),
            pltpu.VMEM((tokens, tokens), F32),
            pltpu.SemaphoreType.DMA((nrow,)),
            pltpu.SemaphoreType.DMA((npiece,)),
            pltpu.SemaphoreType.DMA((npiece,)),
        ],
        compiler_params=params(),
        cost_estimate=cost(2 * tokens * dim * 4 * heads * 3, 20e6),
        name="attn_fwd",
    )(*rows, gain, *tables, *qkv_pieces, *out_pieces)


def attend_back(qkv, d_attended, d_qkv, bias, cosine, sine, heads):
    score_scale = HEAD_DIM ** (-0.5)

    @pl.loop(0, heads // 128)
    def _(pair):
        base = pl.multiple_of(pair * 128, 128)
        query = qkv[:, pl.ds(base, 128)]
        key = qkv[:, pl.ds(heads + base, 128)]
        value = qkv[:, pl.ds(2 * heads + base, 128)]
        grad = d_attended[:, pl.ds(base, 128)]
        sums = [0.0, 0.0, 0.0]
        for half in range(2):
            lanes = head_lanes(128, half).astype(BF)
            own_query = query * (lanes * score_scale)
            own_grad = grad * lanes
            probs = probabilities(own_query, key, bias[...])
            d_value = dot_cols(probs.astype(BF), own_grad)
            d_probs = dot_rows(own_grad, value)
            delta = jnp.sum(probs * d_probs, axis=-1, keepdims=True)
            d_scores = (probs * (d_probs - delta)).astype(BF)
            d_query = dot(d_scores, key * lanes) * score_scale
            d_key = dot_cols(d_scores, own_query)
            sums = [sums[0] + d_query, sums[1] + d_key, sums[2] + d_value]
        back = -sine[:, :128]
        d_qkv[:, pl.ds(base, 128)] = turn(sums[0], cosine[:, :128], back).astype(BF)
        d_qkv[:, pl.ds(heads + base, 128)] = turn(sums[1], cosine[:, :128], back).astype(BF)
        d_qkv[:, pl.ds(2 * heads + base, 128)] = sums[2].astype(BF)


def attn_bwd_kernel(tags, width, nrow, npart, *refs):
    npiece = len(tags)
    nhid, nrow = nrow[1], nrow[0]
    rows_in, hidden_in = refs[:nrow], refs[nrow : nrow + nhid]
    refs = refs[nrow + nhid :]
    qkv, inverses, cosine, sine, first, last, key_index = refs[:7]
    rest = refs[7:]
    qkv_in, out_in = rest[:npiece], rest[npiece : 2 * npiece]
    rest = rest[2 * npiece :]
    branch, d_qkv, gain_grad = rest[:3]
    parts = rest[3 : 3 + npart]
    hidden, d_attended, qkv_w, out_w, bias, sem_rows, sem_x, sem_qkv, sem_out = rest[3 + npart :]
    load_rows = row_copies(rows_in, branch, sem_rows)
    load_x = row_copies(hidden_in, hidden, sem_x)
    load_out = place_copies(tags, out_in, out_w, sem_out, 1, width)
    load_qkv = place_copies(tags, qkv_in, qkv_w, sem_qkv, 0, width)
    start_all(load_rows + load_out + load_qkv + load_x)
    fill_bias(bias, first, last, key_index)
    wait_all(load_rows)
    wait_all(load_out)
    heads = out_w.shape[0]
    step_cols = 256

    @pl.loop(0, heads // step_cols)
    def _(step):
        cols = pl.ds(pl.multiple_of(step * step_cols, step_cols), step_cols)
        d_attended[:, cols] = dot_rows(branch[...], out_w[cols, :]).astype(BF)

    attend_back(qkv, d_attended, d_qkv, bias, cosine, sine, heads)
    wait_all(load_qkv)
    wait_all(load_x)
    tile = parts[0].shape[0]

    @pl.loop(0, qkv_w.shape[0] // step_cols)
    def _(step):
        cols = pl.ds(pl.multiple_of(step * step_cols, step_cols), step_cols)
        product = dot_rows(d_qkv[...], qkv_w[cols, :])
        gain_grad[:, cols] = jnp.sum(product * (hidden[:, cols].astype(F32) * inverses[...]), axis=0, keepdims=True)
        for slot, part in enumerate(parts):
            part[:, cols] = product[slot * tile : (slot + 1) * tile, :].astype(part.dtype)


def attn_bwd(rows, hidden, qkv, inverses, tables, tags, width, qkv_pieces, out_pieces, npart):
    nrow, nhid, dim = len(rows), len(hidden), rows[0].shape[1]
    tokens = qkv.shape[0]
    tile = tokens // npart
    heads = out_pieces[0].shape[0]
    npiece = len(tags)
    return pl.pallas_call(
        partial(attn_bwd_kernel, tags, width, (nrow, nhid), npart),
        out_shape=[shape((tokens, dim), BF), shape((tokens, 3 * heads), BF), shape((1, dim), F32)]
        + [shape((tile, dim), F32 if slot == 0 else BF) for slot in range(npart)],
        in_specs=[anyspace()] * (nrow + nhid) + [vmem()] * 7 + [anyspace()] * (2 * npiece),
        out_specs=[vmem()] * (3 + npart),
        scratch_shapes=[
            pltpu.VMEM((tokens, dim), BF),
            pltpu.VMEM((tokens, heads), BF),
            pltpu.VMEM((dim, 3 * heads), BF),
            pltpu.VMEM((heads, dim), BF),
            pltpu.VMEM((tokens, tokens), F32),
            pltpu.SemaphoreType.DMA((nrow,)),
            pltpu.SemaphoreType.DMA((nhid,)),
            pltpu.SemaphoreType.DMA((npiece,)),
            pltpu.SemaphoreType.DMA((npiece,)),
        ],
        compiler_params=params(),
        cost_estimate=cost(2 * tokens * dim * 4 * heads * 6, 30e6),
        name="attn_bwd",
    )(*rows, *hidden, qkv, inverses, *tables, *qkv_pieces, *out_pieces)


def mlp_kernel(tags, width, nrow, npart, *refs):
    npiece = len(tags)
    sent_in, cot_in = refs[:nrow], refs[nrow : 2 * nrow]
    gain = refs[2 * nrow]
    rest = refs[2 * nrow + 1 :]
    gate_in, up_in, down_in = rest[:npiece], rest[npiece : 2 * npiece], rest[2 * npiece : 3 * npiece]
    rest = rest[3 * npiece :]
    normed, hidden, d_gate, d_up, gain_grad = rest[:5]
    parts = rest[5 : 5 + npart]
    sent, cot, inverses, gate_w, up_w, down_w, sem_sent, sem_cot, sem_gate, sem_up, sem_down = rest[5 + npart :]
    load_sent = row_copies(sent_in, sent, sem_sent)
    load_cot = row_copies(cot_in, cot, sem_cot)
    load_gate = place_copies(tags, gate_in, gate_w, sem_gate, 0, width)
    load_up = place_copies(tags, up_in, up_w, sem_up, 0, width)
    load_down = place_copies(tags, down_in, down_w, sem_down, 1, width)
    start_all(load_sent + load_cot + load_gate + load_up + load_down)
    wait_all(load_sent)
    norm_rows(sent, normed, inverses, gain, 64)
    wait_all(load_cot)
    wait_all(load_gate)
    wait_all(load_up)
    wait_all(load_down)
    step_cols = 256

    @pl.loop(0, gate_w.shape[1] // step_cols)
    def _(step):
        cols = pl.ds(pl.multiple_of(step * step_cols, step_cols), step_cols)
        gate = dot(normed[...], gate_w[:, cols])
        up = dot(normed[...], up_w[:, cols])
        d_hidden = dot_rows(cot[...], down_w[cols, :])
        s = jax.nn.sigmoid(gate)
        activated = gate * s
        hidden[:, cols] = (activated * up).astype(BF)
        d_gate[:, cols] = (d_hidden * up * (s + activated * (1.0 - s))).astype(BF)
        d_up[:, cols] = (d_hidden * activated).astype(BF)

    tile = parts[0].shape[0]

    @pl.loop(0, gate_w.shape[0] // step_cols)
    def _(step):
        cols = pl.ds(pl.multiple_of(step * step_cols, step_cols), step_cols)
        product = dot_rows(d_gate[...], gate_w[cols, :]) + dot_rows(d_up[...], up_w[cols, :])
        gain_grad[:, cols] = jnp.sum(product * (sent[:, cols].astype(F32) * inverses[...]), axis=0, keepdims=True)
        for slot, part in enumerate(parts):
            part[:, cols] = product[slot * tile : (slot + 1) * tile, :].astype(part.dtype)


def mlp(sent, cot, gain, tags, width, gate_pieces, up_pieces, down_pieces, npart):
    nrow, dim = len(sent), sent[0].shape[1]
    tokens = nrow * sent[0].shape[0]
    tile = tokens // npart
    units = gate_pieces[0].shape[1]
    npiece = len(tags)
    return pl.pallas_call(
        partial(mlp_kernel, tags, width, nrow, npart),
        out_shape=[shape((tokens, dim), BF)]
        + [shape((tokens, units), BF)] * 3
        + [shape((1, dim), F32)]
        + [shape((tile, dim), F32 if slot == 0 else BF) for slot in range(npart)],
        in_specs=[anyspace()] * (2 * nrow) + [vmem()] + [anyspace()] * (3 * npiece),
        out_specs=[vmem()] * (5 + npart),
        scratch_shapes=[
            pltpu.VMEM((tokens, dim), BF),
            pltpu.VMEM((tokens, dim), BF),
            pltpu.VMEM((tokens, 1), F32),
            pltpu.VMEM((dim, units), BF),
            pltpu.VMEM((dim, units), BF),
            pltpu.VMEM((units, dim), BF),
            pltpu.SemaphoreType.DMA((nrow,)),
            pltpu.SemaphoreType.DMA((nrow,)),
            pltpu.SemaphoreType.DMA((npiece,)),
            pltpu.SemaphoreType.DMA((npiece,)),
            pltpu.SemaphoreType.DMA((npiece,)),
        ],
        compiler_params=params(),
        cost_estimate=cost(2 * tokens * dim * units * 5, 40e6),
        name="mlp",
    )(*sent, *cot, gain, *gate_pieces, *up_pieces, *down_pieces)


def mlp_out_kernel(tags, width, *refs):
    npiece = len(tags)
    hidden, down_in = refs[0], refs[1 : 1 + npiece]
    *parts, down_w, sem_down = refs[1 + npiece :]
    load_down = place_copies(tags, down_in, down_w, sem_down, 1, width)
    start_all(load_down)
    wait_all(load_down)
    tile, step_cols = parts[0].shape[0], 256

    @pl.loop(0, down_w.shape[1] // step_cols)
    def _(step):
        cols = pl.ds(pl.multiple_of(step * step_cols, step_cols), step_cols)
        product = dot(hidden[...], down_w[:, cols])
        for slot, part in enumerate(parts):
            part[:, cols] = product[slot * tile : (slot + 1) * tile, :].astype(part.dtype)


def mlp_out(hidden, nrow, dim, tags, width, down_pieces):
    tokens, units = hidden.shape
    tile, npiece = tokens // nrow, len(tags)
    return pl.pallas_call(
        partial(mlp_out_kernel, tags, width),
        out_shape=[shape((tile, dim), F32 if slot == 0 else BF) for slot in range(nrow)],
        in_specs=[vmem()] + [anyspace()] * npiece,
        out_specs=[vmem()] * nrow,
        scratch_shapes=[pltpu.VMEM((units, dim), BF), pltpu.SemaphoreType.DMA((npiece,))],
        compiler_params=params(),
        cost_estimate=cost(2 * tokens * dim * units, 14e6),
        name="mlp_out",
    )(hidden, *down_pieces)


def slice_of(slot, width, own):
    index = lax.axis_index("dp")
    owner = index ^ (2 * slot)
    return pl.ds(pl.multiple_of((owner if own else lax.div(owner, 2)) * width, width), width)

MESH = pl.DeviceIdType.MESH
NEAR = (2, 4, 6)
PARTS = 2
GROUPS = 4


def remote(source, target, send_sem, recv_sem, axis, peer):
    return pltpu.make_async_remote_copy(
        src_ref=source,
        dst_ref=target,
        send_sem=send_sem,
        recv_sem=recv_sem,
        device_id={axis: peer},
        device_id_type=MESH,
    )


def meet():
    own, rank = lax.axis_index("dp"), lax.axis_index("tensor")
    barrier = pltpu.get_barrier_semaphore()
    for flip in range(1, 8):
        pl.semaphore_signal(barrier, inc=1, device_id={"dp": own ^ flip}, device_id_type=MESH)
    for step in range(1, 4):
        pl.semaphore_signal(barrier, inc=1, device_id={"tensor": lax.rem(rank + step, 4)}, device_id_type=MESH)
    pl.semaphore_wait(barrier, 10)


def at_cols(ref, index, width):
    return ref.at[:, pl.ds(pl.multiple_of(index * width, width), width)]


def at_rows(ref, index, width):
    return ref.at[pl.ds(pl.multiple_of(index * width, width), width), :]


def either(rank, *choices):
    result = rank == choices[0]
    for choice in choices[1:]:
        result = result | (rank == choice)
    return result


class RowGather:
    def __init__(self, rank, source, landing, part, size, send, recv):
        self.rank = rank

        def place(slot):
            return landing.at[pl.ds((4 * part + slot) * size, size), :]

        def copy(origin, target, step, sem):
            peer = lax.rem(rank + step + 4, 4)
            return remote(origin, place(target), send.at[part, sem], recv.at[part, target], "tensor", peer)

        self.direct = [None] + [copy(source, step, step, step) for step in (1, 2, 3)]
        self.up = copy(place(2), 3, 1, 0)
        self.down = copy(place(2), 1, -1, 0)

    def start(self):
        self.direct[2].start()
        pl.when(self.rank < 3)(self.direct[1].start)
        pl.when(self.rank > 0)(self.direct[3].start)

    def relay(self):
        @pl.when(self.rank == 2)
        def _():
            self.direct[2].wait_recv()
            self.up.start()

        @pl.when(self.rank == 1)
        def _():
            self.direct[2].wait_recv()
            self.down.start()

    def wait(self):
        pl.when(either(self.rank, 0, 3))(self.direct[2].wait_recv)
        self.direct[1].wait_recv()
        self.direct[3].wait_recv()

    def finish(self):
        self.direct[2].wait_send()
        pl.when(self.rank < 3)(self.direct[1].wait_send)
        pl.when(self.rank > 0)(self.direct[3].wait_send)
        pl.when(self.rank == 2)(self.up.wait_send)
        pl.when(self.rank == 1)(self.down.wait_send)


class RowScatter:
    def __init__(self, rank, source, landing, merge, part, size, send, recv):
        self.rank, self.source, self.merge_in, self.size = rank, source, merge, size
        self.place = lambda k: pl.ds((4 * part + k) * size, size)
        self.merge_at = merge.at[pl.ds(part * size, size), :]

        def copy(k):
            peer = lax.rem(rank - k + 4, 4)
            return remote(
                source.at[self.place(k), :], landing.at[self.place(k), :], send.at[part, k], recv.at[part, k], "tensor", peer
            )

        def far(k, peer):
            return remote(source.at[self.place(k), :], self.merge_at, send.at[part, k], recv.at[part, 0], "tensor", peer)

        self.copy = [None] + [copy(k) for k in (1, 2, 3)]
        self.far_up, self.far_down = far(1, 1), far(3, 2)

    def start(self):
        @pl.when(self.rank == 0)
        def _():
            self.far_up.start()
            self.copy[2].start()
            self.copy[3].start()

        @pl.when(self.rank == 3)
        def _():
            self.far_down.start()
            self.copy[2].start()
            self.copy[1].start()

        @pl.when(either(self.rank, 1, 2))
        def _():
            self.copy[1].start()
            self.copy[3].start()

    def merge(self, staged=None, sem=None):
        @pl.when(either(self.rank, 1, 2))
        def _():
            self.far_up.wait_recv()
            other = self.merge_at
            if staged is not None:
                load = pltpu.make_async_copy(self.merge_at, staged, sem)
                load.start()
                load.wait()
                other = staged
            target = self.source.at[self.place(2), :]

            @pl.loop(0, self.size // 16)
            def _(step):
                rows = pl.ds(pl.multiple_of(step * 16, 16), 16)
                target[rows, :] = (target[rows, :].astype(F32) + other[rows, :].astype(F32)).astype(BF)

            self.copy[2].start()

    def wait(self):
        self.copy[2].wait_recv()
        pl.when(self.rank != 3)(self.copy[1].wait_recv)
        pl.when(self.rank != 0)(self.copy[3].wait_recv)

    def clear(self, target):
        def zero(k):
            target[self.place(k), :] = jnp.zeros((self.size, target.shape[1]), target.dtype)

        pl.when(self.rank == 3)(lambda: zero(1))
        pl.when(self.rank == 0)(lambda: zero(3))

    def finish(self):
        for k in (1, 2, 3):
            self.copy[k].wait_send()


def fill_mask(bias, docs, size):
    rank = lax.axis_index("tensor")
    tokens = bias.shape[0]
    values = docs[...]
    starts = [jnp.sum(jnp.where(values < number, 1, 0), keepdims=True) for number in range(1, 8)]

    def document(position):
        return sum(jnp.where(position >= start, 1, 0) for start in starts)

    lane = lax.broadcasted_iota(jnp.int32, (1, tokens), 1)
    slot = lax.rem(lax.div(lane, size), 4)
    part = lax.div(lane, 4 * size)
    keys = lax.rem(rank - slot + 4, 4) * (2 * size) + part * size + lax.rem(lane, size)
    key_docs = document(keys)

    @pl.loop(0, tokens // size)
    def _(block):
        base = lax.rem(rank - lax.rem(block, 4) + 4, 4) * (2 * size) + lax.div(block, 4) * size
        queries = base + lax.broadcasted_iota(jnp.int32, (size, 1), 0)
        allowed = (document(queries) == key_docs) & (queries >= keys)
        bias[pl.ds(pl.multiple_of(block * size, size), size), :] = jnp.where(allowed, 0.0, NEGATIVE)


def fill_turns(cosine, sine, tables, size):
    rank = lax.axis_index("tensor")
    near_cos, near_sin = tables[:size, :], tables[size : 2 * size, :]
    lane = lax.broadcasted_iota(jnp.int32, (1, tables.shape[1]), 1)
    sign = jnp.where(lax.rem(lane, HEAD_DIM) < HEAD_DIM // 2, -1.0, 1.0)
    count = cosine.shape[0] // size
    for block in range(count):
        index = lax.rem(rank - block % 4 + 4, 4) * PARTS + block // 4
        far_cos = tables[pl.ds(2 * size + index, 1), :]
        far_sin = tables[pl.ds(2 * size + count + index, 1), :]
        rows = slice(block * size, (block + 1) * size)
        cosine[rows, :] = near_cos * far_cos - near_sin * far_sin
        sine[rows, :] = (near_sin * far_cos + near_cos * far_sin) * sign


def slice_of(slot, width, own):
    index = lax.axis_index("dp")
    owner = index ^ (2 * slot)
    return pl.ds(pl.multiple_of((owner if own else lax.div(owner, 2)) * width, width), width)


def layer_kernel(*refs):
    hidden_in, cot_in, gains_in = refs[:3]
    weights_in = refs[3:10]
    tables, docs = refs[10:12]
    down_parts, gate_parts, up_parts, qkv_parts, out_parts = refs[12:17]
    grad_merge = refs[17:22]
    pair_gate, pair_up, pair_qkv, pair_attended, pair_normed, pair_branch = refs[22:28]
    branch_rows, hidden_rows, normed_rows, mlp_recv, mlp_merge, qkv_full, down_full = refs[28:35]
    layer_out, input_grad, gain_total = refs[35:38]
    gate_w, up_w, down_w, sent, cot, normed, hidden, d_gate, d_up = refs[38:47]
    two_half, cot_half, buffer_a, buffer_b, buffer_c, out_w = refs[47:53]
    qkv, attended, d_attended, bias, cosine, sine = refs[53:59]
    inverses_one, inverses, middle, grad_middle, send_part, recv_part, merge_part = refs[59:66]
    gains, gain_part, gain_recv, gain_z = refs[66:70]
    a_send, a_recv, f_send, f_recv, h_send, h_recv, z_send, z_recv, r_send, r_recv = refs[70:80]
    w_send, w_recv, d_send, d_recv, g_send, g_recv, y_send, y_recv, load, keep, down_load = refs[80:]

    own, rank = lax.axis_index("dp"), lax.axis_index("tensor")
    core = lax.rem(own, 2)
    tokens, dim = sent.shape
    units = gate_w.shape[1]
    tile = hidden_in.shape[0]
    size = tile // PARTS
    span = 4 * size
    heads = attended.shape[1]
    width = weights_in[0].shape[0]
    half = dim // (2 * width)
    d_qkv = cot.at[:, pl.ds(heads, 3 * heads)]
    group = units // GROUPS
    step_cols = 256
    count = dim // step_cols

    def cols_of(step, length=step_cols):
        return pl.ds(pl.multiple_of(step * length, length), length)

    def local(source, target, sem):
        return pltpu.make_async_copy(source, target, sem)

    def own_rows(part):
        return pl.ds(part * span, size)

    def part_rows(part):
        return pl.ds(part * size, size)

    def source_of(item):
        if item < 4:
            return weights_in[item]
        which, start = (item - 4) % 3, ((item - 4) // 3) * group
        if which == 2:
            return weights_in[4].at[pl.ds(start, group), :]
        return weights_in[5 + which].at[:, pl.ds(start, group)]

    def view(item, owner, part=None):
        rows = heads if item == 3 else group if item > 3 and (item - 4) % 3 == 2 else width
        length = rows if part is None else rows // 2
        start = 0 if part is None else part * length
        if item < 3:
            place = pl.ds(pl.multiple_of(owner * width + start, length), length)
            return down_w.at[place, pl.ds(item * heads, heads)]
        if item == 3:
            return out_w.at[pl.ds(start, length), pl.ds(pl.multiple_of(owner * width, width), width)]
        which, offset = (item - 4) % 3, ((item - 4) // 3) * group
        if which == 2:
            return down_full.at[pl.ds(offset + start, length), pl.ds(pl.multiple_of(owner * width, width), width)]
        place = pl.ds(pl.multiple_of(owner * width + start, length), length)
        return (gate_w, up_w)[which].at[place, pl.ds(offset, group)]

    def send_weight(item, flip):
        return remote(source_of(item), view(item, own), a_send.at[item, flip], a_recv.at[item, flip], "dp", own ^ flip)

    def relay_weight(item, part):
        place = view(item, own ^ (4 - 2 * part), part)
        return remote(place, place, a_send.at[item, 6 + part], a_recv.at[item, 6 + part], "dp", own ^ (2 + 2 * part))

    def pass_weight(item, flip):
        place = view(item, own ^ flip)
        tag = {2: 3, 4: 5, 6: 8}[flip]
        return remote(place, place, a_send.at[item, tag], a_recv.at[item, tag], "dp", own ^ 1)

    def send_weights(items):
        for item in items:
            for flip in (2, 4, 1):
                send_weight(item, flip).start()

    def relay_weights(items):
        for item in items:
            send_weight(item, 4).wait_recv()
            relay_weight(item, 0).start()
            send_weight(item, 2).wait_recv()
            relay_weight(item, 1).start()
            pass_weight(item, 4).start()
            pass_weight(item, 2).start()

    def pass_weights(items):
        for item in items:
            relay_weight(item, 0).wait_recv()
            relay_weight(item, 1).wait_recv()
            pass_weight(item, 6).start()

    def have_weights(items):
        for item in items:
            send_weight(item, 1).wait_recv()
            for flip in NEAR:
                pass_weight(item, flip).wait_recv()

    def sent_weights(items):
        for item in items:
            for flip in (1, 2, 4):
                send_weight(item, flip).wait_send()
            for flip in NEAR:
                pass_weight(item, flip).wait_send()
            for part in range(2):
                relay_weight(item, part).wait_send()

    def items_of(index):
        return list(range(4 + 3 * index, 7 + 3 * index))

    def send_gain(flip):
        return remote(gains_in, at_cols(gains, own, width), y_send.at[0, flip], y_recv.at[0, flip], "dp", own ^ flip)

    def gathers(kind, source, landing):
        return [
            RowGather(rank, source(part), landing, part, size, z_send.at[kind], z_recv.at[kind]) for part in range(PARTS)
        ]

    gather_hidden = gathers(0, lambda part: hidden_in.at[part_rows(part), :], buffer_b)
    gather_cot = gathers(1, lambda part: cot_in.at[part_rows(part), :], cot)
    gather_sent = gathers(2, lambda part: sent.at[own_rows(part), :], sent)
    gather_branch = gathers(3, lambda part: sent.at[own_rows(part), :], branch_rows)

    def scatters(kind, source, landing, merge):
        return [
            RowScatter(rank, source, landing, merge, part, size, r_send.at[kind], r_recv.at[kind]) for part in range(PARTS)
        ]

    out_scatter = scatters(0, send_part, recv_part, merge_part)
    two_scatter = scatters(1, send_part, recv_part, merge_part)
    mlp_scatter = scatters(2, sent, mlp_recv, mlp_merge)
    one_scatter = scatters(3, send_part, recv_part, merge_part)

    def received(part, start, length, base):
        total = base
        for k in (1, 2, 3):
            rows = pl.ds(pl.multiple_of(part * span + k * size + start, length), length)
            total = total + recv_part[rows, :].astype(F32)
        return total

    def to_pair(source, target, row, slot):
        return remote(source, target, h_send.at[row, slot], h_recv.at[row, slot], "dp", own ^ 1)

    def halves(source, target, row):
        return [
            to_pair(at_cols(source, 2 * slot + 1 - core, width), at_cols(target, slot, width), row, slot)
            for slot in range(half)
        ]

    def send_ff(step, which):
        cols = cols_of(step)
        source = (hidden, d_gate, d_up)[which].at[:, cols]
        target = (buffer_a, pair_gate, pair_up)[which].at[:, cols]
        return remote(source, target, f_send.at[step, which], f_recv.at[step, which], "dp", own ^ 1)

    def piece(index, slot):
        if index < 3:
            return at_rows(gate_w, (index - 1) * 4 + slot, width)
        if index == 3:
            return (hidden, d_gate)[slot // 2].at[pl.ds((slot % 2) * width, width), pl.ds(0, 3 * heads)]
        return at_cols(d_up, slot, width)

    def landing_of(index, slot):
        ref = (down_parts, gate_parts, up_parts, qkv_parts, out_parts)[index]
        return at_cols(ref, slot, width) if index == 4 else at_rows(ref, slot, width)

    def half_of(ref, index, part):
        rows, cols = ref.shape
        if index == 4:
            return ref.at[pl.ds(part * (rows // 2), rows // 2), :]
        return ref.at[:, pl.ds(part * (cols // 2), cols // 2)]

    def stage_of(index, part):
        if index == 4:
            return up_w.at[pl.ds(7 * width, heads // 2), pl.ds(part * width, width)]
        length = units // 2 if index < 3 else 3 * heads // 2
        return up_w.at[pl.ds((3 + index) * width, width), pl.ds(part * (units // 2), length)]

    def send_far(index, part):
        return remote(
            half_of(piece(index, 3), index, part),
            half_of(grad_merge[index], index, part),
            w_send.at[index, part],
            w_recv.at[index, part],
            "dp",
            own ^ (2 + 2 * part),
        )

    def send_near(index, slot, part):
        tag = 2 * slot + part
        return remote(
            half_of(piece(index, slot), index, part),
            half_of(landing_of(index, slot), index, part),
            w_send.at[index, tag],
            w_recv.at[index, tag],
            "dp",
            own ^ (2 * slot),
        )

    def keep_grad(index):
        return local(piece(index, 0), landing_of(index, 0), keep.at[index])

    def merge_grads(index):
        loads = [local(half_of(grad_merge[index], index, part), stage_of(index, part), load.at[part]) for part in range(2)]
        for part in range(2):
            send_far(index, part).wait_recv()
            loads[part].start()
        for part in range(2):
            loads[part].wait()
            target, source = half_of(piece(index, 2 - part), index, part), stage_of(index, part)
            length = source.shape[0] // 4

            @pl.loop(0, 4)
            def _(step):
                rows = cols_of(step, length)
                target[rows, :] = (target[rows, :].astype(F32) + source[rows, :].astype(F32)).astype(BF)

            send_near(index, 2 - part, part).start()

    def row_grads(index, slot, left, left_pair, right, right_pair, columns):
        mine, theirs = slice_of(slot, width, True), slice_of(slot, width, False)
        turned, turned_pair = jnp.transpose(left[:, mine]), jnp.transpose(left_pair[:, theirs])
        target = piece(index, slot)

        @pl.loop(0, columns // 512)
        def _(step):
            cols = cols_of(step, 512)
            total = dot(turned, right[:, cols]) + dot(turned_pair, right_pair[:, cols])
            target[:, cols] = total.astype(BF)

        if slot == 3:
            send_far(index, 0).start()
            send_far(index, 1).start()
        elif slot == 0:
            keep_grad(index).start()
        else:
            send_near(index, slot, slot - 1).start()

    def out_grads():
        for part in range(2):
            rows = pl.ds(part * (heads // 2), heads // 2)
            turned, turned_pair = jnp.transpose(attended[:, rows]), jnp.transpose(cot[:, rows])
            for slot in range(4):
                mine, theirs = slice_of(slot, width, True), slice_of(slot, width, False)
                total = dot(turned, buffer_a[:, mine]) + dot(turned_pair, cot_half[:, theirs])
                piece(4, slot)[rows, :] = total.astype(BF)
            send_far(4, part).start()
            send_near(4, part + 1, part).start()
        keep_grad(4).start()

    def down_piece(slot, index):
        return (buffer_b, buffer_c)[slot // 2].at[:, pl.ds(((slot % 2) * GROUPS + index) * width, width)]

    def down_rows(ref, index, slot):
        return ref.at[pl.ds(index * group, group), pl.ds(slot * width, width)]

    def send_down(kind, index):
        if kind == 0:
            target, source = down_rows(grad_merge[0], index, 0), down_piece(3, index)
            peer = own ^ (2 + 2 * (index // 2))
        else:
            target, source, peer = down_rows(down_parts, index, kind), down_piece(kind, index), own ^ (2 * kind)
        return remote(source, target, d_send.at[kind, index], d_recv.at[kind, index], "dp", peer)

    def keep_down(index):
        return local(down_piece(0, index), down_rows(down_parts, index, 0), keep.at[8 + index])

    def down_grads(index):
        @pl.loop(0, group // 256)
        def _(step):
            send_ff(index * (group // 256) + step, 0).wait_recv()

        @pl.loop(0, group // 256)
        def _(step):
            cols = pl.ds(pl.multiple_of(index * group + step * 256, 256), 256)
            rows = pl.ds(pl.multiple_of(step * 256, 256), 256)
            turned, turned_pair = jnp.transpose(hidden[:, cols]), jnp.transpose(buffer_a[:, cols])
            for slot in range(4):
                mine, theirs = slice_of(slot, width, True), slice_of(slot, width, False)
                total = dot(turned, cot[:, mine]) + dot(turned_pair, cot_half[:, theirs])
                down_piece(slot, index)[rows, :] = total.astype(BF)

        send_down(0, index).start()
        send_down(1 + index // 2, index).start()
        keep_down(index).start()

    def merge_down():
        stages = [up_w.at[pl.ds(6 * width, group), pl.ds(index * width, width)] for index in range(GROUPS)]
        loads = [local(down_rows(grad_merge[0], index, 0), stages[index], load.at[index]) for index in range(GROUPS)]
        for index in range(GROUPS):
            send_down(0, index).wait_recv()
            loads[index].start()
        for index in range(GROUPS):
            loads[index].wait()
            kind = 2 - index // 2
            target, source = down_piece(kind, index), stages[index]

            @pl.loop(0, 4)
            def _(step):
                rows = cols_of(step, group // 4)
                target[rows, :] = (target[rows, :].astype(F32) + source[rows, :].astype(F32)).astype(BF)

            send_down(kind, index).start()

    def norm_back(total, values, gain):
        inverse = lax.rsqrt(jnp.mean(values * values, axis=-1, keepdims=True) + EPSILON)
        scaled = total * gain
        return inverse * (scaled - values * inverse * inverse * jnp.mean(scaled * values, axis=-1, keepdims=True))

    meet()
    for gather in gather_hidden:
        gather.start()
    for flip in range(1, 8):
        send_gain(flip).start()
    send_weights(range(3))
    stage_down = down_w.at[:, pl.ds(3 * heads, width)]
    stage_in = local(weights_in[4], stage_down, load.at[0])
    own_loads = [local(gains_in, at_cols(gains, own, width), load.at[1])]
    own_loads += [local(weights_in[item], view(item, own), load.at[2 + item]) for item in range(4)]
    own_loads += [local(weights_in[5], at_rows(gate_w, own, width), load.at[6])]
    own_loads += [local(weights_in[6], at_rows(up_w, own, width), load.at[7])]
    for part in range(PARTS):
        own_loads.append(local(hidden_in.at[part_rows(part), :], buffer_b.at[own_rows(part), :], load.at[8 + part]))
        own_loads.append(local(cot_in.at[part_rows(part), :], cot.at[own_rows(part), :], load.at[10 + part]))
    start_all([stage_in] + own_loads)
    fill_mask(bias, docs, size)
    fill_turns(cosine, sine, tables, size)
    relay_weights([0, 1])
    gather_hidden[0].relay()
    relay_weights([2])
    send_weights([3, 4])
    gather_hidden[1].relay()
    gather_cot[0].start()
    stage_in.wait()
    stage_out = local(stage_down, at_cols(down_full, own, width), keep.at[5])
    stage_out.start()
    wait_all(own_loads)
    for flip in range(1, 8):
        send_gain(flip).wait_recv()
    pass_weights(range(3))
    relay_weights([3])
    send_weights(range(5, 4 + 3 * GROUPS))
    for gather in gather_hidden:
        gather.wait()

    norm_rows(buffer_b, buffer_c, inverses_one, gains.at[pl.ds(0, 1), :], 64)
    keep_hidden = local(buffer_b, hidden_rows, keep.at[0])
    keep_normed = local(buffer_c, normed_rows, keep.at[1])
    start_all([keep_hidden, keep_normed])
    have_weights(range(3))
    qkv_w = down_w.at[:, pl.ds(0, 3 * heads)]
    keep_qkv = local(qkv_w, qkv_full, keep.at[2])
    keep_qkv.start()

    @pl.loop(0, 2 * heads // step_cols)
    def _(step):
        cols = cols_of(step)
        product = dot(buffer_c[...], down_w[:, cols])
        turns = [jnp.concatenate([table[...]] * (step_cols // 128), axis=1) for table in (cosine, sine)]
        qkv[:, cols] = turn(product, *turns).astype(BF)

    @pl.loop(2 * heads // step_cols, 3 * heads // step_cols)
    def _(step):
        cols = cols_of(step)
        qkv[:, cols] = dot(buffer_c[...], down_w[:, cols]).astype(BF)

    attend(qkv, attended, bias, heads)
    gather_cot[0].relay()
    pass_weights([3])
    have_weights([3])

    def make_out(part):
        @pl.loop(0, count)
        def _(step):
            cols = cols_of(step)
            product = dot(attended[part * span : (part + 1) * span, :], out_w[:, cols])
            middle[part_rows(part), cols] = product[:size, :]
            send_part[pl.ds(part * span + size, span - size), cols] = product[size:, :].astype(BF)

    make_out(0)
    out_scatter[0].start()
    make_out(1)
    out_scatter[0].merge()
    out_scatter[1].start()
    wait_all([keep_hidden, keep_normed, keep_qkv, stage_out])
    send_normed = halves(normed_rows, pair_normed, 1)
    send_attended = to_pair(attended, pair_attended, 2, 0)
    start_all(send_normed + [send_attended])
    for part in range(PARTS):
        out_scatter[part].clear(recv_part)
    relay_weights(items_of(0))

    def make_sent(part):
        out_scatter[part].wait()

        @pl.loop(0, size // 32)
        def _(step):
            rows = pl.ds(pl.multiple_of(part * size + step * 32, 32), 32)
            place = pl.ds(pl.multiple_of(part * span + step * 32, 32), 32)
            total = received(part, step * 32, 32, hidden_of(place) + middle[rows, :])
            middle[rows, :] = total
            sent[place, :] = total.astype(BF)

        gather_sent[part].start()

    def hidden_of(place):
        return buffer_b[place, :].astype(F32)

    make_sent(0)
    out_scatter[1].merge()
    relay_weights(items_of(1))
    gather_sent[0].relay()
    make_sent(1)
    gather_cot[1].start()
    relay_weights(items_of(2))
    gather_sent[1].relay()
    relay_weights(items_of(3))
    gather_cot[1].relay()

    def load_down(index):
        rows = pl.ds(index * group, group)
        return local(down_full.at[rows, :], down_w.at[rows, :], down_load.at[index])

    for gather in gather_sent:
        gather.wait()
    norm_rows(sent, normed, inverses, gains.at[pl.ds(1, 1), :], 64)
    send_two = halves(normed, two_half, 3)
    start_all(send_two)
    for gather in gather_cot:
        gather.wait()
    send_cot = halves(cot, cot_half, 0)
    start_all(send_cot)
    pass_weights(items_of(0))
    have_weights(items_of(0))
    sent_weights(range(4))
    for gather in gather_hidden:
        gather.finish()
    load_down(0).start()
    for index in range(GROUPS):
        if index:
            pass_weights(items_of(index))
            have_weights(items_of(index))
            load_down(index).start()
        load_down(index).wait()

        @pl.loop(index * group // step_cols, (index + 1) * group // step_cols)
        def _(step):
            cols = cols_of(step)
            gate = dot(normed[...], gate_w[:, cols])
            up = dot(normed[...], up_w[:, cols])
            d_hidden = dot_rows(cot[...], down_w[cols, :])
            s = jax.nn.sigmoid(gate)
            activated = gate * s
            hidden[:, cols] = (activated * up).astype(BF)
            d_gate[:, cols] = (d_hidden * up * (s + activated * (1.0 - s))).astype(BF)
            d_up[:, cols] = (d_hidden * activated).astype(BF)
            for which in range(3):
                send_ff(step, which).start()

        if index == 0:
            for copy in send_cot:
                copy.wait_recv()
        else:
            down_grads(index - 1)

    gain_part[...] = jnp.zeros(gain_part.shape, F32)
    for part in range(PARTS):
        out_scatter[part].finish()

    def make_two(part):
        block = slice(part * span, (part + 1) * span)

        @pl.loop(0, count)
        def _(step):
            cols = cols_of(step)
            product = dot_rows(d_gate[block, :], gate_w[cols, :]) + dot_rows(d_up[block, :], up_w[cols, :])
            gain_part[pl.ds(1, 1), cols] += jnp.sum(
                product * (sent[block, cols].astype(F32) * inverses[block, :]), axis=0, keepdims=True
            )
            grad_middle[part_rows(part), cols] = product[:size, :]
            send_part[pl.ds(part * span + size, span - size), cols] = product[size:, :].astype(BF)

    def pair_ready(which):
        @pl.loop(0, units // step_cols)
        def _(step):
            send_ff(step, which).wait_recv()

    make_two(0)
    two_scatter[0].start()
    down_grads(GROUPS - 1)
    make_two(1)
    two_scatter[0].merge()
    two_scatter[1].start()
    sent_weights(range(4, 4 + 3 * GROUPS))
    pair_ready(1)
    pair_ready(2)
    gate_pair, up_pair = up_w.at[pl.ds(0, tokens), :], up_w.at[pl.ds(tokens, tokens), :]
    pair_loads = [local(pair_gate, gate_pair, load.at[0]), local(pair_up, up_pair, load.at[1])]
    start_all(pair_loads)
    for copy in send_two:
        copy.wait_recv()
    wait_all(pair_loads)
    gate_grads = lambda slot: row_grads(1, slot, normed, two_half, d_gate, gate_pair, units)
    up_grads = lambda slot: row_grads(2, slot, normed, two_half, d_up, up_pair, units)
    for slot in (3, 1, 2, 0):
        gate_grads(slot)

    def make_branch(part):
        two_scatter[part].wait()

        @pl.loop(0, size // 32)
        def _(step):
            rows = pl.ds(pl.multiple_of(part * size + step * 32, 32), 32)
            place = pl.ds(pl.multiple_of(part * span + step * 32, 32), 32)
            total = received(part, step * 32, 32, grad_middle[rows, :])
            result = cot[place, :].astype(F32) + norm_back(total, sent[place, :].astype(F32), gains[1:2, :])
            grad_middle[rows, :] = result
            sent[place, :] = result.astype(BF)

        gather_branch[part].start()
        keep_branch[part].start()

    keep_branch = [
        local(sent.at[own_rows(part), :], branch_rows.at[own_rows(part), :], keep.at[6 + part]) for part in range(PARTS)
    ]
    for part in range(PARTS):
        gather_sent[part].finish()
    make_branch(0)
    up_grads(3)
    up_grads(1)
    two_scatter[1].merge()
    up_grads(2)
    up_grads(0)
    merge_down()
    gather_branch[0].relay()

    @pl.loop(0, count)
    def _(step):
        cols = cols_of(step)
        product = dot(hidden[...], down_w[:, cols])
        for part in range(PARTS):
            start = part * span
            middle[part_rows(part), cols] = middle[part_rows(part), cols] + product[start : start + size, :]
            sent[pl.ds(start + size, span - size), cols] = product[start + size : start + span, :].astype(BF)

    make_branch(1)
    load_weight = local(qkv_full, qkv_w, load.at[4])
    load_hidden = local(hidden_rows, gate_pair, load.at[5])
    load_normed = local(normed_rows, up_pair, load.at[6])
    start_all([load_weight, load_hidden, load_normed])
    merge_grads(1)
    gather_branch[1].relay()
    for scatter in mlp_scatter:
        scatter.start()
    merge_grads(2)
    for part in range(PARTS):
        two_scatter[part].finish()
        gather_branch[part].wait()
        keep_branch[part].wait()

    load_branch = local(branch_rows, buffer_a, load.at[3])
    load_branch.start()
    send_half = halves(branch_rows, pair_branch, 4)
    start_all(send_half)
    load_branch.wait()

    @pl.loop(0, heads // step_cols)
    def _(step):
        cols = cols_of(step)
        d_attended[:, cols] = dot_rows(buffer_a[...], out_w[cols, :]).astype(BF)

    for copy in send_cot:
        copy.wait_send()
    for gather in gather_cot:
        gather.finish()
    attend_back(qkv, d_attended, d_qkv, bias, cosine, sine, heads)
    send_qkv = to_pair(d_qkv, pair_qkv, 5, 0)
    send_qkv.start()
    @pl.loop(0, units // step_cols)
    def _(step):
        for which in range(3):
            send_ff(step, which).wait_send()

    for part in range(PARTS):
        mlp_scatter[part].merge(d_up.at[part_rows(part), :], load.at[3])
    wait_all([load_weight, load_hidden, load_normed])
    for part in range(PARTS):
        block = slice(part * span, (part + 1) * span)

        @pl.loop(0, count)
        def _(step):
            cols = cols_of(step)
            product = dot_rows(d_qkv[block, :], down_w[cols, pl.ds(0, 3 * heads)])
            gain_part[pl.ds(0, 1), cols] += jnp.sum(
                product * (gate_pair[block, cols].astype(F32) * inverses_one[block, :]), axis=0, keepdims=True
            )
            input_grad[part_rows(part), cols] = product[:size, :]
            send_part[pl.ds(part * span + size, span - size), cols] = product[size:, :].astype(BF)

        if part:
            one_scatter[0].merge()
        one_scatter[part].start()

    def share_gain(flip):
        source = at_cols(gain_part, own ^ flip, width)
        return remote(source, at_rows(gain_recv, flip, 8), g_send.at[flip], g_recv.at[flip], "dp", own ^ flip)

    for flip in range(1, 8):
        share_gain(flip).start()

    for index in range(1, 3):
        keep_grad(index).wait()
    send_qkv.wait_recv()
    for copy in send_half + send_normed + [send_attended]:
        copy.wait_recv()

    for copy in send_two:
        copy.wait_send()
    last_loads = [
        local(pair_qkv, normed.at[:, pl.ds(0, 3 * heads)], load.at[0]),
        local(pair_attended, cot.at[:, pl.ds(0, heads)], load.at[1]),
        local(pair_normed, two_half, load.at[2]),
        local(pair_branch, cot_half, load.at[3]),
    ]
    start_all(last_loads)
    wait_all(last_loads)
    out_grads()
    for slot in (3, 1, 2, 0):
        row_grads(3, slot, up_pair, two_half, d_qkv, normed, 3 * heads)
    one_scatter[1].merge()
    merge_grads(4)
    merge_grads(3)

    for flip in range(1, 8):
        share_gain(flip).wait_recv()
    gain_sum = gain_part[:, pl.ds(pl.multiple_of(own * width, width), width)]
    for flip in range(1, 8):
        gain_sum = gain_sum + gain_recv[pl.ds(flip * 8, 8), :]
    gain_z[pl.ds(0, 8), :] = gain_sum

    def share_gain_z(k):
        target = gain_z.at[pl.ds(8 * k, 8), :]
        return remote(gain_z.at[pl.ds(0, 8), :], target, y_send.at[1, k], y_recv.at[1, k], "tensor", lax.rem(rank + k, 4))

    for k in (1, 2, 3):
        share_gain_z(k).start()

    load_own = [
        local(hidden_in.at[part_rows(part), :], sent.at[own_rows(part), :], load.at[4 + part]) for part in range(PARTS)
    ]
    for part in range(PARTS):
        gather_branch[part].finish()
    start_all(load_own)
    wait_all(load_own)
    for part in range(PARTS):
        one_scatter[part].wait()

        @pl.loop(0, size // 32)
        def _(step):
            rows = pl.ds(pl.multiple_of(part * size + step * 32, 32), 32)
            place = pl.ds(pl.multiple_of(part * span + step * 32, 32), 32)
            total = received(part, step * 32, 32, input_grad[rows, :])
            input_grad[rows, :] = grad_middle[rows, :] + norm_back(total, sent[place, :].astype(F32), gains[0:1, :])

    for scatter in mlp_scatter:
        scatter.wait()
    load_mlp = local(mlp_recv, recv_part, load.at[0])
    load_mlp.start()
    load_mlp.wait()
    for part in range(PARTS):
        mlp_scatter[part].clear(recv_part)

        @pl.loop(0, size // 32)
        def _(step):
            rows = pl.ds(pl.multiple_of(part * size + step * 32, 32), 32)
            layer_out[rows, :] = received(part, step * 32, 32, middle[rows, :]).astype(BF)

    for k in (1, 2, 3):
        share_gain_z(k).wait_recv()
    gain_all = gain_z[pl.ds(0, 8), :]
    for k in (1, 2, 3):
        gain_all = gain_all + gain_z[pl.ds(8 * k, 8), :]
    gain_total[...] = gain_all

    for scatter in mlp_scatter + one_scatter:
        scatter.finish()
    for index in range(GROUPS):
        keep_down(index).wait()
        for kind in range(3):
            if kind:
                send_down(kind, index).wait_recv()
            send_down(kind, index).wait_send()
    for flip in range(1, 8):
        send_gain(flip).wait_send()
        share_gain(flip).wait_send()
    for k in (1, 2, 3):
        share_gain_z(k).wait_send()
    for copy in send_normed + send_half + [send_attended, send_qkv]:
        copy.wait_send()
    for index in range(1, 5):
        for slot in range(1, 3):
            for part in range(2):
                send_near(index, slot, part).wait_recv()
    for index in range(3, 5):
        keep_grad(index).wait()
    for index in range(1, 5):
        for part in range(2):
            send_far(index, part).wait_send()
            for slot in range(1, 3):
                send_near(index, slot, part).wait_send()


def layer(hidden_in, cot, gains, weights, tables, docs):
    tile, dim = hidden_in.shape
    tokens = 4 * tile
    width, heads = weights[0].shape
    units = weights[5].shape[1]
    dma = pltpu.SemaphoreType.DMA
    rows, narrow, ff = shape((tokens, dim), BF), shape((tokens, dim // 2), BF), shape((tokens, units), BF)
    weights_shape = [(units, width), (width, units), (width, units), (width, 3 * heads), (heads, width)]
    parts_shape = [(units, 3 * width), (3 * width, units), (3 * width, units), (3 * width, 3 * heads), (heads, 3 * width)]
    outs = [shape(dims, BF) for dims in parts_shape + weights_shape]
    outs += [ff] * 2 + [shape((tokens, 3 * heads), BF), shape((tokens, heads), BF), narrow, narrow]
    outs += [rows] * 4 + [shape((tile, dim), BF), shape((dim, 3 * heads), BF), shape((units, dim), BF)]
    in_hbm = len(outs)
    outs += [shape((tile, dim), BF), shape((tile, dim), F32), shape((8, width), F32)]
    items = 4 + 3 * GROUPS
    scratch = [((dim, units), BF), ((dim, units), BF), ((units, dim), BF)]
    scratch += [((tokens, dim), BF)] * 3 + [((tokens, units), BF)] * 3
    scratch += [((tokens, dim // 2), BF)] * 2 + [((tokens, dim), BF)] * 3 + [((heads, dim), BF)]
    scratch += [((tokens, 3 * heads), BF)] + [((tokens, heads), BF)] * 2
    scratch += [((tokens, tokens), F32), ((tokens, 128), F32), ((tokens, 128), F32)]
    scratch += [((tokens, 1), F32), ((tokens, 1), F32), ((tile, dim), F32), ((tile, dim), F32)]
    scratch += [((tokens, dim), BF), ((tokens, dim), BF), ((tile, dim), BF)]
    scratch += [((8, dim), F32), ((8, dim), F32), ((64, width), F32), ((32, width), F32)]
    sems = [(items, 9)] * 2 + [(units // 256, 3)] * 2 + [(6, 4)] * 2 + [(4, PARTS, 4)] * 4 + [(5, 6)] * 2 + [(3, GROUPS)] * 2
    sems += [(8,)] * 2 + [(2, 8)] * 2 + [(12,), (8 + GROUPS,), (GROUPS,)]
    return pl.pallas_call(
        layer_kernel,
        out_shape=outs,
        in_specs=[anyspace()] * 10 + [vmem()] * 2,
        out_specs=[anyspace()] * in_hbm + [vmem()] * 3,
        scratch_shapes=[pltpu.VMEM(*entry) for entry in scratch] + [dma(entry) for entry in sems],
        compiler_params=pltpu.CompilerParams(vmem_limit_bytes=67000000, collective_id=0, has_side_effects=True),
        cost_estimate=cost(2 * tokens * dim * units * 12, 100e6),
        name="layer",
    )(hidden_in, cot, gains, *weights, tables, docs)


def sum_kernel(count, *refs):
    parts, plain_in = refs[:5], refs[5:7]
    down, gate, up, query, key, value, out, *plain_out = refs[7:16]
    staged, totals, plain, load, store = refs[16:21], refs[21:26], refs[26:28], refs[28], refs[29]
    loads = [pltpu.make_async_copy(parts[index], staged[index], load.at[index]) for index in range(5)]
    loads += [pltpu.make_async_copy(plain_in[index], plain[index], load.at[5 + index]) for index in range(2)]
    start_all(loads)
    heads = query.shape[1]
    stores = [pltpu.make_async_copy(totals[index], ref, store.at[index]) for index, ref in enumerate((down, gate, up))]
    qkv_stores = [
        pltpu.make_async_copy(totals[3].at[:, pl.ds(index * heads, heads)], ref, store.at[3 + index])
        for index, ref in enumerate((query, key, value))
    ]
    out_store = pltpu.make_async_copy(totals[4], out, store.at[6])
    plain_stores = [pltpu.make_async_copy(plain[index], plain_out[index], store.at[7 + index]) for index in range(2)]
    groups = [[stores[0]], [stores[1]], [stores[2]], qkv_stores, [out_store]]
    for index in range(5):
        loads[index].wait()
        rows_first = index in (1, 2, 3)
        rows, cols = totals[index].shape
        step_rows = 32 if rows_first else 256

        @pl.loop(0, rows // step_rows)
        def _(step):
            start = pl.multiple_of(step * step_rows, step_rows)
            total = None
            for slot in range(count):
                if rows_first:
                    term = staged[index][pl.ds(pl.multiple_of(start + slot * rows, step_rows), step_rows), :]
                else:
                    term = staged[index][pl.ds(start, step_rows), slot * cols : (slot + 1) * cols]
                term = term.astype(F32)
                total = term if total is None else total + term
            totals[index][pl.ds(start, step_rows), :] = total

        start_all(groups[index])
    for index in range(2):
        loads[5 + index].wait()
        plain_stores[index].start()
    for entry in groups + [plain_stores]:
        wait_all(entry)


def sum_grads(parts, plain, heads, count):
    dims = [part.shape for part in parts]
    sums = [
        (rows // count, cols) if index in (1, 2, 3) else (rows, cols // count) for index, (rows, cols) in enumerate(dims)
    ]
    outs = sums[:3] + [(sums[3][0], heads)] * 3 + [sums[4]]
    dma = pltpu.SemaphoreType.DMA
    return pl.pallas_call(
        partial(sum_kernel, count),
        out_shape=[shape(dim, F32) for dim in outs] + [shape(entry.shape, entry.dtype) for entry in plain],
        in_specs=[anyspace()] * 7,
        out_specs=[anyspace()] * 9,
        scratch_shapes=[pltpu.VMEM(dim, BF) for dim in dims]
        + [pltpu.VMEM(dim, F32) for dim in sums]
        + [pltpu.VMEM(entry.shape, entry.dtype) for entry in plain]
        + [dma((7,)), dma((9,))],
        compiler_params=params(),
        cost_estimate=cost(1e6, 22e6),
        name="sum_grads",
    )(*parts, *plain)


def shift(values, step):
    size = lax.axis_size("tensor")
    return lax.ppermute(values, "tensor", [(index, (index + step) % size) for index in range(size)])


def gather_rows(values):
    return [values] + [shift(values, step) for step in range(1, lax.axis_size("tensor"))]


def scatter_rows(parts):
    total = parts[0].astype(F32)
    for step in range(1, len(parts)):
        total = total + shift(parts[step], -step).astype(F32)
    return total


def gather_weight(values, axis):
    return [None], [lax.all_gather(values, "dp", axis=axis, tiled=True)]


def scatter_full(left, right, axis):
    full = dot_cols(left, right).astype(BF)
    return lax.psum_scatter(full, "dp", scatter_dimension=axis, tiled=True).astype(F32)


def frequencies():
    half_size = HEAD_DIM // 2
    return ROPE_BASE ** (-jnp.arange(half_size, dtype=F32) / half_size)


def turn_tables(size, count):
    near = jnp.arange(size).astype(F32)[:, None] * frequencies()[None, :]
    far = (jnp.arange(count) * size).astype(F32)[:, None] * frequencies()[None, :]
    return jnp.tile(jnp.concatenate([jnp.cos(near), jnp.sin(near), jnp.cos(far), jnp.sin(far)], axis=0), (1, 4))


def rotary(length):
    angles = jnp.arange(length).astype(F32)[:, None] * frequencies()[None, :]
    cosine, sine = jnp.cos(angles), jnp.sin(angles)
    cosine = jnp.tile(cosine, (1, 8))
    sine = jnp.tile(jnp.concatenate([-sine, sine], axis=1), (1, 4))
    return cosine, sine


def position_tables(doc_ids, ranks):
    length = doc_ids.shape[0]
    token_index = jnp.arange(length, dtype=jnp.int32)
    before = jnp.concatenate([doc_ids[:1] - 1, doc_ids[:-1]])
    doc_start = lax.cummax(jnp.where(doc_ids != before, token_index, 0), axis=0)
    order = (lax.axis_index("tensor") - jnp.arange(ranks)) % ranks
    last = token_index.reshape(ranks, -1)[order].reshape(length)
    first = doc_start.reshape(ranks, -1)[order].reshape(length)
    cosine, sine = (table.reshape(ranks, -1, 256)[order].reshape(length, 256) for table in rotary(length))
    return cosine, sine, first[:, None], last[:, None], last[None, :]


def rms_back(grad_rows_, values, gain):
    inverse = lax.rsqrt(jnp.mean(values * values, axis=-1, keepdims=True) + EPSILON)
    scaled = grad_rows_ * gain
    return inverse * (scaled - values * inverse * inverse * jnp.mean(scaled * values, axis=-1, keepdims=True))


def body(
    hidden_in,
    out_cotangent,
    doc_ids,
    attn_gain,
    query_weight,
    key_weight,
    value_weight,
    out_weight,
    mlp_gain,
    gate_weight,
    up_weight,
    down_weight,
):
    ranks, groups = lax.axis_size("tensor"), lax.axis_size("dp")
    paired = (groups, ranks) == (8, 4)
    width, heads = query_weight.shape
    dim = hidden_in.shape[1]

    if paired:
        pad = jnp.zeros((6, width), F32)
        own_gains = jnp.concatenate([attn_gain[None].astype(F32), mlp_gain[None].astype(F32), pad], axis=0)
        weights = (query_weight, key_weight, value_weight, out_weight, down_weight, gate_weight, up_weight)
        tables = turn_tables(hidden_in.shape[0] // PARTS, ranks * PARTS)
        outs = layer(hidden_in, out_cotangent, own_gains, weights, tables, doc_ids.reshape(ranks, -1))
        sums = sum_grads(outs[:5], outs[-3:-1], heads, 3)
        down_grad, gate_grad, up_grad, query_grad, key_grad, value_grad, out_proj_grad, layer_out, input_grad = sums
        gain_total = outs[-1]
        share = width // ranks
        gain_grads = lax.dynamic_slice_in_dim(gain_total, lax.axis_index("tensor") * share, share, axis=1)
    else:
        tables = position_tables(doc_ids, ranks)
        input_local = hidden_in.astype(F32)
        hidden_rows = gather_rows(hidden_in)
        gains = lax.all_gather(jnp.stack([attn_gain, mlp_gain]), "dp", axis=1, tiled=True).astype(F32)
        attn_scale, mlp_scale = gains[:1], gains[1:]
        qkv_weight = jnp.concatenate([query_weight, key_weight, value_weight], axis=1)
        tags, qkv_pieces = gather_weight(qkv_weight, 0)
        tags, out_pieces = gather_weight(out_weight, 1)
        cot_rows = gather_rows(out_cotangent)
        tags, down_pieces = gather_weight(down_weight, 1)
        tags, gate_pieces = gather_weight(gate_weight, 0)
        tags, up_pieces = gather_weight(up_weight, 0)
        normed, qkv, attended, inverses, *branch_parts = attn_fwd(
            hidden_rows, attn_scale, tables, tags, width, qkv_pieces, out_pieces
        )
        middle = input_local + scatter_rows(branch_parts)
        sent = middle.astype(BF)
        sent_rows = gather_rows(sent)
        cot_full = jnp.concatenate(cot_rows, axis=0)
        normed_two, hidden, d_gate, d_up, mlp_gain_part, *two_parts = mlp(
            sent_rows, cot_rows, mlp_scale, tags, width, gate_pieces, up_pieces, down_pieces, ranks
        )
        grad_two_rows = scatter_rows(two_parts)
        grad_middle = out_cotangent.astype(F32) + rms_back(grad_two_rows, sent.astype(F32), mlp_scale)
        branch_rows = gather_rows(grad_middle.astype(BF))
        down_grad = scatter_full(hidden, cot_full, 1)
        gate_grad = scatter_full(normed_two, d_gate, 0)
        up_grad = scatter_full(normed_two, d_up, 0)
        mlp_rows = scatter_rows(mlp_out(hidden, ranks, dim, tags, width, down_pieces))
        layer_out = (middle + mlp_rows).astype(BF)
        branch_full, d_qkv, attn_gain_part, *one_parts = attn_bwd(
            branch_rows, hidden_rows, qkv, inverses, tables, tags, width, qkv_pieces, out_pieces, ranks
        )
        out_proj_grad = scatter_full(attended, branch_full, 1)
        query_grad, key_grad, value_grad = jnp.split(scatter_full(normed, d_qkv, 0), 3, axis=1)
        grad_one_rows = scatter_rows(one_parts)
        input_grad = grad_middle + rms_back(grad_one_rows, input_local, attn_scale)
        gain_parts = jnp.concatenate([attn_gain_part, mlp_gain_part], axis=0)
        gain_grads = lax.psum_scatter(gain_parts, ("dp", "tensor"), scatter_dimension=1, tiled=True)
    return (
        layer_out,
        input_grad,
        gain_grads[0],
        query_grad,
        key_grad,
        value_grad,
        out_proj_grad,
        gain_grads[1],
        gate_grad,
        up_grad,
        down_grad,
    )


def solution(mesh):
    return jax.shard_map(
        body,
        mesh=mesh,
        in_specs=(
            P(("dp", "tensor"), None),
            P(("dp", "tensor"), None),
            P("dp"),
            P("dp"),
            P("dp", "tensor"),
            P("dp", "tensor"),
            P("dp", "tensor"),
            P("tensor", "dp"),
            P("dp"),
            P("dp", "tensor"),
            P("dp", "tensor"),
            P("tensor", "dp"),
        ),
        out_specs=(
            P(("dp", "tensor"), None),
            P(("dp", "tensor"), None),
            P(("dp", "tensor")),
            P("dp", "tensor"),
            P("dp", "tensor"),
            P("dp", "tensor"),
            P("tensor", "dp"),
            P(("dp", "tensor")),
            P("dp", "tensor"),
            P("dp", "tensor"),
            P("tensor", "dp"),
        ),
        check_vma=False,
    )
```

```python
import math
from functools import partial

import jax
import jax.numpy as jnp
from jax import lax
from jax.experimental import pallas as pl
from jax.experimental.pallas import tpu as pltpu
from jax.sharding import PartitionSpec as P

HEAD_DIM = 64
EPSILON = 1e-05
ROPE_BASE = 130000.0
NEGATIVE = -1e30
VMEM_LIMIT = 63 * 1024 * 1024
BF = jnp.bfloat16
F32 = jnp.float32


def dot(left, right):
    return jnp.dot(left, right, preferred_element_type=F32)


def dot_rows(left, right):
    return lax.dot_general(left, right, (((1,), (1,)), ((), ())), preferred_element_type=F32)


def dot_cols(left, right):
    return lax.dot_general(left, right, (((0,), (0,)), ((), ())), preferred_element_type=F32)


def vmem():
    return pl.BlockSpec(memory_space=pltpu.VMEM)


def anyspace():
    return pl.BlockSpec(memory_space=pl.ANY)


def params():
    return pltpu.CompilerParams(vmem_limit_bytes=VMEM_LIMIT)


def cost(flops, nbytes):
    return pl.CostEstimate(flops=int(flops), bytes_accessed=int(nbytes), transcendentals=0)


def shape(dims, kind):
    return jax.ShapeDtypeStruct(dims, kind)


def place_copies(tags, pieces, target, sem, axis, width):
    own = lax.axis_index("dp")
    copies = []
    for slot, (tag, piece) in enumerate(zip(tags, pieces)):
        if tag is None:
            where = target
        else:
            start = pl.multiple_of((own ^ tag) * width, width)
            where = target.at[pl.ds(start, width), :] if axis == 0 else target.at[:, pl.ds(start, width)]
        copies.append(pltpu.make_async_copy(piece, where, sem.at[slot]))
    return copies


def row_copies(pieces, target, sem):
    copies = []
    for slot, piece in enumerate(pieces):
        rows = piece.shape[0]
        copies.append(pltpu.make_async_copy(piece, target.at[pl.ds(slot * rows, rows), :], sem.at[slot]))
    return copies


def start_all(copies):
    for copy in copies:
        copy.start()


def wait_all(copies):
    for copy in copies:
        copy.wait()


def turn(values, cosine, sine):
    width = values.shape[1]
    lane = lax.broadcasted_iota(jnp.int32, values.shape, 1)
    partner = jnp.where(
        lax.rem(lane, HEAD_DIM) < HEAD_DIM // 2,
        pltpu.roll(values, width - HEAD_DIM // 2, 1),
        pltpu.roll(values, HEAD_DIM // 2, 1),
    )
    return values * cosine + partner * sine


def norm_rows(source, target, inverses, gain, tile):
    @pl.loop(0, source.shape[0] // tile)
    def _(step):
        rows = pl.ds(pl.multiple_of(step * tile, tile), tile)
        values = source[rows, :].astype(F32)
        inverse = lax.rsqrt(jnp.mean(values * values, axis=-1, keepdims=True) + EPSILON)
        inverses[rows, :] = inverse
        target[rows, :] = (values * inverse * gain[...]).astype(BF)


def fill_bias(bias, first, last, key_index):
    keys = key_index[...]
    bias[...] = jnp.where((keys >= first[...]) & (keys <= last[...]), 0.0, NEGATIVE)


def head_lanes(width, half):
    lane = lax.broadcasted_iota(jnp.int32, (1, width), 1)
    return (lax.div(lane, HEAD_DIM) == half).astype(F32)


def probabilities(query, key, bias):
    scores = dot_rows(query, key) + bias
    weights = jnp.exp(scores - jnp.max(scores, axis=-1, keepdims=True))
    return weights * (1.0 / jnp.sum(weights, axis=-1, keepdims=True))


def attend(qkv, attended, bias, heads):
    @pl.loop(0, heads // 128)
    def _(pair):
        base = pl.multiple_of(pair * 128, 128)
        query = qkv[:, pl.ds(base, 128)]
        key = qkv[:, pl.ds(heads + base, 128)]
        value = qkv[:, pl.ds(2 * heads + base, 128)]
        total = None
        for half in range(2):
            lanes = head_lanes(128, half).astype(BF)
            probs = probabilities(query * (lanes * HEAD_DIM ** (-0.5)), key, bias[...])
            term = dot(probs.astype(BF), value * lanes)
            total = term if total is None else total + term
        attended[:, pl.ds(base, 128)] = total.astype(BF)


def attn_fwd_kernel(tags, width, nrow, *refs):
    npiece = len(tags)
    rows_in = refs[:nrow]
    gain, cosine, sine, first, last, key_index = refs[nrow : nrow + 6]
    rest = refs[nrow + 6 :]
    qkv_in, out_in = rest[:npiece], rest[npiece : 2 * npiece]
    rest = rest[2 * npiece :]
    normed, qkv, attended, inverses = rest[:4]
    parts = rest[4 : 4 + nrow]
    hidden, qkv_w, out_w, bias, sem_rows, sem_qkv, sem_out = rest[4 + nrow :]
    load_rows = row_copies(rows_in, hidden, sem_rows)
    load_qkv = place_copies(tags, qkv_in, qkv_w, sem_qkv, 0, width)
    load_out = place_copies(tags, out_in, out_w, sem_out, 1, width)
    start_all(load_rows + load_qkv + load_out)
    fill_bias(bias, first, last, key_index)
    wait_all(load_rows)
    norm_rows(hidden, normed, inverses, gain, 64)
    wait_all(load_qkv)
    heads = attended.shape[1]
    step_cols = 256

    @pl.loop(0, 2 * heads // step_cols)
    def _(step):
        cols = pl.ds(pl.multiple_of(step * step_cols, step_cols), step_cols)
        qkv[:, cols] = turn(dot(normed[...], qkv_w[:, cols]), cosine[...], sine[...]).astype(BF)

    @pl.loop(2 * heads // step_cols, 3 * heads // step_cols)
    def _(step):
        cols = pl.ds(pl.multiple_of(step * step_cols, step_cols), step_cols)
        qkv[:, cols] = dot(normed[...], qkv_w[:, cols]).astype(BF)

    attend(qkv, attended, bias, heads)
    wait_all(load_out)
    tile = parts[0].shape[0]

    @pl.loop(0, out_w.shape[1] // step_cols)
    def _(step):
        cols = pl.ds(pl.multiple_of(step * step_cols, step_cols), step_cols)
        product = dot(attended[...], out_w[:, cols])
        for slot, part in enumerate(parts):
            part[:, cols] = product[slot * tile : (slot + 1) * tile, :].astype(part.dtype)


def attn_fwd(rows, gain, tables, tags, width, qkv_pieces, out_pieces):
    nrow, (tile, dim) = len(rows), rows[0].shape
    tokens = nrow * tile
    heads = out_pieces[0].shape[0]
    npiece = len(tags)
    return pl.pallas_call(
        partial(attn_fwd_kernel, tags, width, nrow),
        out_shape=[
            shape((tokens, dim), BF),
            shape((tokens, 3 * heads), BF),
            shape((tokens, heads), BF),
            shape((tokens, 1), F32),
        ]
        + [shape((tile, dim), F32 if slot == 0 else BF) for slot in range(nrow)],
        in_specs=[anyspace()] * nrow + [vmem()] * 6 + [anyspace()] * (2 * npiece),
        out_specs=[vmem()] * (4 + nrow),
        scratch_shapes=[
            pltpu.VMEM((tokens, dim), BF),
            pltpu.VMEM((dim, 3 * heads), BF),
            pltpu.VMEM((heads, dim), BF),
            pltpu.VMEM((tokens, tokens), F32),
            pltpu.SemaphoreType.DMA((nrow,)),
            pltpu.SemaphoreType.DMA((npiece,)),
            pltpu.SemaphoreType.DMA((npiece,)),
        ],
        compiler_params=params(),
        cost_estimate=cost(2 * tokens * dim * 4 * heads * 3, 20e6),
        name="attn_fwd",
    )(*rows, gain, *tables, *qkv_pieces, *out_pieces)


def attend_back(qkv, d_attended, d_qkv, bias, cosine, sine, heads):
    score_scale = HEAD_DIM ** (-0.5)

    @pl.loop(0, heads // 128)
    def _(pair):
        base = pl.multiple_of(pair * 128, 128)
        query = qkv[:, pl.ds(base, 128)]
        key = qkv[:, pl.ds(heads + base, 128)]
        value = qkv[:, pl.ds(2 * heads + base, 128)]
        grad = d_attended[:, pl.ds(base, 128)]
        sums = [0.0, 0.0, 0.0]
        for half in range(2):
            lanes = head_lanes(128, half).astype(BF)
            own_query = query * (lanes * score_scale)
            own_grad = grad * lanes
            probs = probabilities(own_query, key, bias[...])
            d_value = dot_cols(probs.astype(BF), own_grad)
            d_probs = dot_rows(own_grad, value)
            delta = jnp.sum(probs * d_probs, axis=-1, keepdims=True)
            d_scores = (probs * (d_probs - delta)).astype(BF)
            d_query = dot(d_scores, key * lanes) * score_scale
            d_key = dot_cols(d_scores, own_query)
            sums = [sums[0] + d_query, sums[1] + d_key, sums[2] + d_value]
        back = -sine[:, :128]
        d_qkv[:, pl.ds(base, 128)] = turn(sums[0], cosine[:, :128], back).astype(BF)
        d_qkv[:, pl.ds(heads + base, 128)] = turn(sums[1], cosine[:, :128], back).astype(BF)
        d_qkv[:, pl.ds(2 * heads + base, 128)] = sums[2].astype(BF)


def attn_bwd_kernel(tags, width, nrow, npart, *refs):
    npiece = len(tags)
    nhid, nrow = nrow[1], nrow[0]
    rows_in, hidden_in = refs[:nrow], refs[nrow : nrow + nhid]
    refs = refs[nrow + nhid :]
    qkv, inverses, cosine, sine, first, last, key_index = refs[:7]
    rest = refs[7:]
    qkv_in, out_in = rest[:npiece], rest[npiece : 2 * npiece]
    rest = rest[2 * npiece :]
    branch, d_qkv, gain_grad = rest[:3]
    parts = rest[3 : 3 + npart]
    hidden, d_attended, qkv_w, out_w, bias, sem_rows, sem_x, sem_qkv, sem_out = rest[3 + npart :]
    load_rows = row_copies(rows_in, branch, sem_rows)
    load_x = row_copies(hidden_in, hidden, sem_x)
    load_out = place_copies(tags, out_in, out_w, sem_out, 1, width)
    load_qkv = place_copies(tags, qkv_in, qkv_w, sem_qkv, 0, width)
    start_all(load_rows + load_out + load_qkv + load_x)
    fill_bias(bias, first, last, key_index)
    wait_all(load_rows)
    wait_all(load_out)
    heads = out_w.shape[0]
    step_cols = 256

    @pl.loop(0, heads // step_cols)
    def _(step):
        cols = pl.ds(pl.multiple_of(step * step_cols, step_cols), step_cols)
        d_attended[:, cols] = dot_rows(branch[...], out_w[cols, :]).astype(BF)

    attend_back(qkv, d_attended, d_qkv, bias, cosine, sine, heads)
    wait_all(load_qkv)
    wait_all(load_x)
    tile = parts[0].shape[0]

    @pl.loop(0, qkv_w.shape[0] // step_cols)
    def _(step):
        cols = pl.ds(pl.multiple_of(step * step_cols, step_cols), step_cols)
        product = dot_rows(d_qkv[...], qkv_w[cols, :])
        gain_grad[:, cols] = jnp.sum(product * (hidden[:, cols].astype(F32) * inverses[...]), axis=0, keepdims=True)
        for slot, part in enumerate(parts):
            part[:, cols] = product[slot * tile : (slot + 1) * tile, :].astype(part.dtype)


def attn_bwd(rows, hidden, qkv, inverses, tables, tags, width, qkv_pieces, out_pieces, npart):
    nrow, nhid, dim = len(rows), len(hidden), rows[0].shape[1]
    tokens = qkv.shape[0]
    tile = tokens // npart
    heads = out_pieces[0].shape[0]
    npiece = len(tags)
    return pl.pallas_call(
        partial(attn_bwd_kernel, tags, width, (nrow, nhid), npart),
        out_shape=[shape((tokens, dim), BF), shape((tokens, 3 * heads), BF), shape((1, dim), F32)]
        + [shape((tile, dim), F32 if slot == 0 else BF) for slot in range(npart)],
        in_specs=[anyspace()] * (nrow + nhid) + [vmem()] * 7 + [anyspace()] * (2 * npiece),
        out_specs=[vmem()] * (3 + npart),
        scratch_shapes=[
            pltpu.VMEM((tokens, dim), BF),
            pltpu.VMEM((tokens, heads), BF),
            pltpu.VMEM((dim, 3 * heads), BF),
            pltpu.VMEM((heads, dim), BF),
            pltpu.VMEM((tokens, tokens), F32),
            pltpu.SemaphoreType.DMA((nrow,)),
            pltpu.SemaphoreType.DMA((nhid,)),
            pltpu.SemaphoreType.DMA((npiece,)),
            pltpu.SemaphoreType.DMA((npiece,)),
        ],
        compiler_params=params(),
        cost_estimate=cost(2 * tokens * dim * 4 * heads * 6, 30e6),
        name="attn_bwd",
    )(*rows, *hidden, qkv, inverses, *tables, *qkv_pieces, *out_pieces)


def mlp_kernel(tags, width, nrow, npart, *refs):
    npiece = len(tags)
    sent_in, cot_in = refs[:nrow], refs[nrow : 2 * nrow]
    gain = refs[2 * nrow]
    rest = refs[2 * nrow + 1 :]
    gate_in, up_in, down_in = rest[:npiece], rest[npiece : 2 * npiece], rest[2 * npiece : 3 * npiece]
    rest = rest[3 * npiece :]
    normed, hidden, d_gate, d_up, gain_grad = rest[:5]
    parts = rest[5 : 5 + npart]
    sent, cot, inverses, gate_w, up_w, down_w, sem_sent, sem_cot, sem_gate, sem_up, sem_down = rest[5 + npart :]
    load_sent = row_copies(sent_in, sent, sem_sent)
    load_cot = row_copies(cot_in, cot, sem_cot)
    load_gate = place_copies(tags, gate_in, gate_w, sem_gate, 0, width)
    load_up = place_copies(tags, up_in, up_w, sem_up, 0, width)
    load_down = place_copies(tags, down_in, down_w, sem_down, 1, width)
    start_all(load_sent + load_cot + load_gate + load_up + load_down)
    wait_all(load_sent)
    norm_rows(sent, normed, inverses, gain, 64)
    wait_all(load_cot)
    wait_all(load_gate)
    wait_all(load_up)
    wait_all(load_down)
    step_cols = 256

    @pl.loop(0, gate_w.shape[1] // step_cols)
    def _(step):
        cols = pl.ds(pl.multiple_of(step * step_cols, step_cols), step_cols)
        gate = dot(normed[...], gate_w[:, cols])
        up = dot(normed[...], up_w[:, cols])
        d_hidden = dot_rows(cot[...], down_w[cols, :])
        s = jax.nn.sigmoid(gate)
        activated = gate * s
        hidden[:, cols] = (activated * up).astype(BF)
        d_gate[:, cols] = (d_hidden * up * (s + activated * (1.0 - s))).astype(BF)
        d_up[:, cols] = (d_hidden * activated).astype(BF)

    tile = parts[0].shape[0]

    @pl.loop(0, gate_w.shape[0] // step_cols)
    def _(step):
        cols = pl.ds(pl.multiple_of(step * step_cols, step_cols), step_cols)
        product = dot_rows(d_gate[...], gate_w[cols, :]) + dot_rows(d_up[...], up_w[cols, :])
        gain_grad[:, cols] = jnp.sum(product * (sent[:, cols].astype(F32) * inverses[...]), axis=0, keepdims=True)
        for slot, part in enumerate(parts):
            part[:, cols] = product[slot * tile : (slot + 1) * tile, :].astype(part.dtype)


def mlp(sent, cot, gain, tags, width, gate_pieces, up_pieces, down_pieces, npart):
    nrow, dim = len(sent), sent[0].shape[1]
    tokens = nrow * sent[0].shape[0]
    tile = tokens // npart
    units = gate_pieces[0].shape[1]
    npiece = len(tags)
    return pl.pallas_call(
        partial(mlp_kernel, tags, width, nrow, npart),
        out_shape=[shape((tokens, dim), BF)]
        + [shape((tokens, units), BF)] * 3
        + [shape((1, dim), F32)]
        + [shape((tile, dim), F32 if slot == 0 else BF) for slot in range(npart)],
        in_specs=[anyspace()] * (2 * nrow) + [vmem()] + [anyspace()] * (3 * npiece),
        out_specs=[vmem()] * (5 + npart),
        scratch_shapes=[
            pltpu.VMEM((tokens, dim), BF),
            pltpu.VMEM((tokens, dim), BF),
            pltpu.VMEM((tokens, 1), F32),
            pltpu.VMEM((dim, units), BF),
            pltpu.VMEM((dim, units), BF),
            pltpu.VMEM((units, dim), BF),
            pltpu.SemaphoreType.DMA((nrow,)),
            pltpu.SemaphoreType.DMA((nrow,)),
            pltpu.SemaphoreType.DMA((npiece,)),
            pltpu.SemaphoreType.DMA((npiece,)),
            pltpu.SemaphoreType.DMA((npiece,)),
        ],
        compiler_params=params(),
        cost_estimate=cost(2 * tokens * dim * units * 5, 40e6),
        name="mlp",
    )(*sent, *cot, gain, *gate_pieces, *up_pieces, *down_pieces)


def mlp_out_kernel(tags, width, *refs):
    npiece = len(tags)
    hidden, down_in = refs[0], refs[1 : 1 + npiece]
    *parts, down_w, sem_down = refs[1 + npiece :]
    load_down = place_copies(tags, down_in, down_w, sem_down, 1, width)
    start_all(load_down)
    wait_all(load_down)
    tile, step_cols = parts[0].shape[0], 256

    @pl.loop(0, down_w.shape[1] // step_cols)
    def _(step):
        cols = pl.ds(pl.multiple_of(step * step_cols, step_cols), step_cols)
        product = dot(hidden[...], down_w[:, cols])
        for slot, part in enumerate(parts):
            part[:, cols] = product[slot * tile : (slot + 1) * tile, :].astype(part.dtype)


def mlp_out(hidden, nrow, dim, tags, width, down_pieces):
    tokens, units = hidden.shape
    tile, npiece = tokens // nrow, len(tags)
    return pl.pallas_call(
        partial(mlp_out_kernel, tags, width),
        out_shape=[shape((tile, dim), F32 if slot == 0 else BF) for slot in range(nrow)],
        in_specs=[vmem()] + [anyspace()] * npiece,
        out_specs=[vmem()] * nrow,
        scratch_shapes=[pltpu.VMEM((units, dim), BF), pltpu.SemaphoreType.DMA((npiece,))],
        compiler_params=params(),
        cost_estimate=cost(2 * tokens * dim * units, 14e6),
        name="mlp_out",
    )(hidden, *down_pieces)


def slice_of(slot, width, own):
    index = lax.axis_index("dp")
    owner = index ^ (2 * slot)
    return pl.ds(pl.multiple_of((owner if own else lax.div(owner, 2)) * width, width), width)

MESH = pl.DeviceIdType.MESH
NEAR = (2, 4, 6)
PARTS = 2
GROUPS = 4


def remote(source, target, send_sem, recv_sem, axis, peer):
    return pltpu.make_async_remote_copy(
        src_ref=source,
        dst_ref=target,
        send_sem=send_sem,
        recv_sem=recv_sem,
        device_id={axis: peer},
        device_id_type=MESH,
    )


def drain(ref, sem):
    pltpu.make_async_copy(ref, ref, sem).wait()


def meet():
    own, rank = lax.axis_index("dp"), lax.axis_index("tensor")
    barrier = pltpu.get_barrier_semaphore()
    for flip in range(1, 8):
        pl.semaphore_signal(barrier, inc=1, device_id={"dp": own ^ flip}, device_id_type=MESH)
    for step in range(1, 4):
        pl.semaphore_signal(barrier, inc=1, device_id={"tensor": lax.rem(rank + step, 4)}, device_id_type=MESH)
    pl.semaphore_wait(barrier, 10)


def at_cols(ref, index, width):
    return ref.at[:, pl.ds(pl.multiple_of(index * width, width), width)]


def at_rows(ref, index, width):
    return ref.at[pl.ds(pl.multiple_of(index * width, width), width), :]


def either(rank, *choices):
    result = rank == choices[0]
    for choice in choices[1:]:
        result = result | (rank == choice)
    return result


def ends(rank):
    return either(rank, 0, 3)


def inner(rank):
    return either(rank, 1, 2)


class RowGather:
    def __init__(self, rank, source, landing, part, size, send, recv):
        self.rank = rank

        def place(slot):
            return landing.at[pl.ds(pl.multiple_of((4 * part + slot) * size, size), size), :]

        def copy(origin, slot, peer):
            return remote(origin, place(slot), send.at[part], recv.at[part, slot - 1], "tensor", peer)

        def forward(slot, target, peer):
            return copy(place(slot), target, peer)

        outward, inward = (rank - 1) * 3, 3 - rank
        near, far = 5 - 2 * rank, 2 * rank - 1
        self.up, self.down = copy(source, 1, rank + 1), copy(source, 3, rank - 1)
        self.hops = [forward(near, 2, outward), forward(far, 2, inward), forward(2, far, outward)]
        self.slots = [near, far, 2]
        self.arrival = lambda slot: copy(source, slot, lax.rem(rank + 1, 4))
        self.sent = lambda count: drain(landing.at[pl.ds(0, count * size), :], send.at[part])

    def start(self):
        pl.when(self.rank < 3)(self.up.start)
        pl.when(self.rank > 0)(self.down.start)

    def hop(self, index):
        @pl.when(inner(self.rank))
        def _():
            self.arrival(self.slots[index]).wait_recv()
            self.hops[index].start()

    def wait(self):
        @pl.when(ends(self.rank))
        def _():
            for slot in (1, 2, 3):
                self.arrival(slot).wait_recv()

    def finish(self):
        pl.when(ends(self.rank))(lambda: self.sent(1))
        pl.when(inner(self.rank))(lambda: self.sent(5))


class RowScatter:
    def __init__(self, rank, source, landing, part, size, send, recv, staged=None, sem=None):
        self.rank, self.source, self.size, self.staged, self.sem = rank, source, size, staged, sem
        self.place = lambda k: pl.ds(pl.multiple_of((4 * part + k) * size, size), size)
        self.land = lambda slot: landing.at[pl.ds((5 * part + slot) * size, size), :]

        def copy(k, slot, peer):
            return remote(source.at[self.place(k), :], self.land(slot), send.at[part], recv.at[part, slot], "tensor", peer)

        end = lax.div(rank, 3)
        self.first = [copy(index + 1 + end * (2 - 2 * index), index, 1 + end) for index in range(3)]
        self.keys = [2, 5 - 2 * rank, 2 * rank - 1]
        self.later = [
            copy(self.keys[0], 3, 3 - rank),
            copy(self.keys[1], 4, 3 - rank),
            copy(self.keys[2], 4, (rank - 1) * 3),
        ]
        self.arrival = lambda slot: copy(1, slot, lax.rem(rank + 1, 4))
        self.finish = lambda: drain(source.at[pl.ds(0, 3 * size), :], send.at[part])

    def start(self, indices=(0, 1, 2)):
        @pl.when(ends(self.rank))
        def _():
            for index in indices:
                self.first[index].start()

    def hop(self, index):
        @pl.when(inner(self.rank))
        def _():
            slot = (0, 1, 3)[index]
            self.arrival(slot).wait_recv()
            other = self.land(slot)
            if self.staged is not None:
                load = pltpu.make_async_copy(other, self.staged, self.sem)
                load.start()
                load.wait()
                other = self.staged
            target = self.source.at[self.place(self.keys[index]), :]

            @pl.loop(0, self.size // 16)
            def _(step):
                rows = pl.ds(pl.multiple_of(step * 16, 16), 16)
                target[rows, :] = (target[rows, :].astype(F32) + other[rows, :].astype(F32)).astype(BF)

            self.later[index].start()

    def wait(self):
        pl.when(inner(self.rank))(self.arrival(2).wait_recv)
        self.arrival(4).wait_recv()


def fill_mask(bias, docs, size):
    rank = lax.axis_index("tensor")
    tokens = bias.shape[0]
    values = docs[...]
    starts = [jnp.sum(jnp.where(values < number, 1, 0), keepdims=True) for number in range(1, 8)]

    def document(position):
        return sum(jnp.where(position >= start, 1, 0) for start in starts)

    lane = lax.broadcasted_iota(jnp.int32, (1, tokens), 1)
    slot = lax.rem(lax.div(lane, size), 4)
    part = lax.div(lane, 4 * size)
    keys = lax.rem(rank - slot + 4, 4) * (2 * size) + part * size + lax.rem(lane, size)
    key_docs = document(keys)

    @pl.loop(0, tokens // size)
    def _(block):
        base = lax.rem(rank - lax.rem(block, 4) + 4, 4) * (2 * size) + lax.div(block, 4) * size
        queries = base + lax.broadcasted_iota(jnp.int32, (size, 1), 0)
        allowed = (document(queries) == key_docs) & (queries >= keys)
        bias[pl.ds(pl.multiple_of(block * size, size), size), :] = jnp.where(allowed, 0.0, NEGATIVE)


def fill_turns(cosine, sine, size):
    rank = lax.axis_index("tensor")
    half_size = HEAD_DIM // 2
    dims = (size, cosine.shape[1])
    lane = lax.broadcasted_iota(jnp.int32, dims, 1)
    row = lax.broadcasted_iota(jnp.int32, dims, 0)
    frequency = jnp.exp(lax.rem(lane, half_size).astype(F32) * (-math.log(ROPE_BASE) / half_size))
    sign = jnp.where(lax.rem(lane, HEAD_DIM) < half_size, -1.0, 1.0)

    @pl.loop(0, cosine.shape[0] // size)
    def _(block):
        start = (lax.rem(rank - lax.rem(block, 4) + 4, 4) * PARTS + lax.div(block, 4)) * size
        angles = (row + start).astype(F32) * frequency
        rows = pl.ds(pl.multiple_of(block * size, size), size)
        cosine[rows, :] = jnp.cos(angles)
        sine[rows, :] = jnp.sin(angles) * sign


def slice_of(slot, width, own):
    index = lax.axis_index("dp")
    owner = index ^ (2 * slot)
    return pl.ds(pl.multiple_of((owner if own else lax.div(owner, 2)) * width, width), width)


def layer_kernel(*refs):
    hidden_in, cot_in, plain_gains = refs[:3]
    weights_in = refs[3:10]
    docs = refs[10]
    down_parts, gate_parts, up_parts, qkv_parts, out_parts = refs[11:16]
    grad_merge = refs[16:21]
    pair_gate, pair_up, pair_qkv, pair_attended, pair_normed, pair_branch = refs[21:27]
    branch_rows, hidden_rows, normed_rows, mlp_recv, qkv_full, down_full = refs[27:33]
    layer_out, input_grad, gain_total = refs[33:36]
    gate_w, up_w, down_w, sent, cot, normed, hidden, d_gate, d_up = refs[36:45]
    two_half, cot_half, buffer_a, buffer_b, buffer_c, out_w = refs[45:51]
    qkv, attended, d_attended, bias, cosine, sine = refs[51:57]
    inverses_one, inverses, middle, grad_middle, send_part, recv_part = refs[57:63]
    gains_in, gains, gain_part, gain_recv, gain_z = refs[63:68]
    a_send, a_recv, f_send, f_recv, h_send, h_recv, z_send, z_recv, r_send, r_recv = refs[68:78]
    w_send, w_recv, d_send, d_recv, g_send, g_recv, y_send, y_recv, load, keep, down_load, s_recv, n_recv = refs[78:]

    own, rank = lax.axis_index("dp"), lax.axis_index("tensor")
    core = lax.rem(own, 2)
    tokens, dim = sent.shape
    units = gate_w.shape[1]
    tile = hidden_in.shape[0]
    size = tile // PARTS
    span = 4 * size
    heads = attended.shape[1]
    width = weights_in[0].shape[0]
    half = dim // (2 * width)
    d_qkv = cot.at[:, pl.ds(heads, 3 * heads)]
    group = units // GROUPS
    step_cols = 256
    count = dim // step_cols

    def cols_of(step, length=step_cols):
        return pl.ds(pl.multiple_of(step * length, length), length)

    def local(source, target, sem):
        return pltpu.make_async_copy(source, target, sem)

    def own_rows(part):
        return pl.ds(part * span, size)

    def part_rows(part):
        return pl.ds(part * size, size)

    def source_of(item):
        if item < 4:
            return weights_in[item]
        which, start = (item - 4) % 3, ((item - 4) // 3) * group
        if which == 2:
            return weights_in[4].at[pl.ds(start, group), :]
        return weights_in[5 + which].at[:, pl.ds(start, group)]

    def view(item, owner, part=None):
        rows = heads if item == 3 else group if item > 3 and (item - 4) % 3 == 2 else width
        length = rows if part is None else rows // 2
        start = 0 if part is None else part * length
        if item < 3:
            place = pl.ds(pl.multiple_of(owner * width + start, length), length)
            return down_w.at[place, pl.ds(item * heads, heads)]
        if item == 3:
            return out_w.at[pl.ds(start, length), pl.ds(pl.multiple_of(owner * width, width), width)]
        which, offset = (item - 4) % 3, ((item - 4) // 3) * group
        if which == 2:
            return down_full.at[pl.ds(offset + start, length), pl.ds(pl.multiple_of(owner * width, width), width)]
        place = pl.ds(pl.multiple_of(owner * width + start, length), length)
        return (gate_w, up_w)[which].at[place, pl.ds(offset, group)]

    def phase_of(item):
        return 0 if item < 3 else 1 if item == 3 else 2 + (item - 4) // 3

    def send_weight(item, flip):
        sem = s_recv.at[phase_of(item)] if flip == 1 else a_recv.at[item, flip // 2 - 1]
        return remote(source_of(item), view(item, own), a_send.at[phase_of(item)], sem, "dp", own ^ flip)

    def relay_weight(item, part):
        place = view(item, own ^ (4 - 2 * part), part)
        return remote(place, place, a_send.at[phase_of(item)], a_recv.at[item, 2], "dp", own ^ (2 + 2 * part))

    def pass_weight(item, flip):
        place = view(item, own ^ flip)
        return remote(place, place, a_send.at[phase_of(item)], s_recv.at[phase_of(item)], "dp", own ^ 1)

    def send_weights(items):
        for item in items:
            for flip in (2, 4, 1):
                send_weight(item, flip).start()

    def relay_weights(items):
        for item in items:
            send_weight(item, 4).wait_recv()
            relay_weight(item, 0).start()
            send_weight(item, 2).wait_recv()
            relay_weight(item, 1).start()
            pass_weight(item, 4).start()
            pass_weight(item, 2).start()

    def pass_weights(items):
        for item in items:
            drain(view(item, own ^ 6), a_recv.at[item, 2])
            pass_weight(item, 6).start()

    def have_weights(phase):
        drain(gate_w.at[pl.ds(0, width if phase == 1 else 3 * width), :], s_recv.at[phase])

    def sent_weights(phase):
        length = 7 * width // 4
        drain(gate_w.at[pl.ds(0, length if phase == 1 else 3 * length), :], a_send.at[phase])

    def items_of(index):
        return list(range(4 + 3 * index, 7 + 3 * index))

    def send_gain(flip):
        return remote(gains_in, at_cols(gains, own, width), y_send.at[0], y_recv.at[0], "dp", own ^ flip)

    def gathers(kind, source, landing):
        return [
            RowGather(rank, source(part), landing, part, size, z_send.at[kind], z_recv.at[kind]) for part in range(PARTS)
        ]

    gather_hidden = gathers(0, lambda part: hidden_in.at[part_rows(part), :], buffer_b)
    gather_cot = gathers(1, lambda part: cot_in.at[part_rows(part), :], cot)
    gather_sent = gathers(2, lambda part: sent.at[own_rows(part), :], sent)
    gather_branch = gathers(3, lambda part: sent.at[own_rows(part), :], branch_rows)

    def scatters(kind, source, landing, staged=None, sem=None):
        return [
            RowScatter(rank, source, landing, part, size, r_send.at[kind], r_recv.at[kind], staged, sem)
            for part in range(PARTS)
        ]

    gate_stage = up_w.at[pl.ds(4 * width, size), :]
    out_scatter = scatters(0, send_part, recv_part)
    two_scatter = scatters(1, send_part, recv_part)
    mlp_scatter = scatters(2, sent, mlp_recv, gate_stage, load.at[3])
    one_scatter = scatters(3, send_part, recv_part)

    def arrived(part, slot):
        return pl.ds((5 * part + slot) * size, size)

    def clear(part):
        @pl.when(ends(rank))
        def _():
            recv_part[arrived(part, 2), :] = jnp.zeros((size, dim), BF)

    def received(part, start, length, base):
        total = base
        for slot in (2, 4):
            rows = pl.ds(pl.multiple_of((5 * part + slot) * size + start, length), length)
            total = total + recv_part[rows, :].astype(F32)
        return total

    def to_pair(source, target, row, slot):
        return remote(source, target, h_send.at[row], h_recv.at[row], "dp", own ^ 1)

    def halves(source, target, row):
        return [
            to_pair(at_cols(source, 2 * slot + 1 - core, width), at_cols(target, slot, width), row, slot)
            for slot in range(half)
        ]

    def send_ff(step, which):
        cols = cols_of(step)
        source = (hidden, d_gate, d_up)[which].at[:, cols]
        target = (buffer_a, pair_gate, pair_up)[which].at[:, cols]
        arrival = lax.div(step, group // step_cols) if which == 0 else GROUPS - 1 + which
        return remote(source, target, f_send.at[which], f_recv.at[arrival], "dp", own ^ 1)

    def piece(index, slot):
        if index < 3:
            return at_rows(gate_w, (index - 1) * 4 + slot, width)
        if index == 3:
            return (hidden, d_gate)[slot // 2].at[pl.ds((slot % 2) * width, width), pl.ds(0, 3 * heads)]
        return at_cols(d_up, slot, width)

    def landing_of(index, slot):
        ref = (down_parts, gate_parts, up_parts, qkv_parts, out_parts)[index]
        return at_cols(ref, slot, width) if index == 4 else at_rows(ref, slot, width)

    def half_of(ref, index, part):
        rows, cols = ref.shape
        if index == 4:
            return ref.at[pl.ds(part * (rows // 2), rows // 2), :]
        return ref.at[:, pl.ds(part * (cols // 2), cols // 2)]

    def stage_of(index, part):
        if index == 4:
            return up_w.at[pl.ds(7 * width, heads // 2), pl.ds(part * width, width)]
        length = units // 2 if index < 3 else 3 * heads // 2
        return up_w.at[pl.ds((3 + index) * width, width), pl.ds(part * (units // 2), length)]

    def send_far(index, part):
        return remote(
            half_of(piece(index, 3), index, part),
            half_of(grad_merge[index], index, part),
            w_send.at[index - 1],
            w_recv.at[index - 1, part],
            "dp",
            own ^ (2 + 2 * part),
        )

    def send_near(index, slot, part):
        return remote(
            half_of(piece(index, slot), index, part),
            half_of(landing_of(index, slot), index, part),
            w_send.at[index - 1],
            n_recv.at[index - 1],
            "dp",
            own ^ (2 * slot),
        )

    def keep_grad(index):
        return local(piece(index, 0), landing_of(index, 0), keep.at[index])

    def merge_grads(index):
        loads = [local(half_of(grad_merge[index], index, part), stage_of(index, part), load.at[part]) for part in range(2)]
        for part in range(2):
            send_far(index, part).wait_recv()
            loads[part].start()
        for part in range(2):
            loads[part].wait()
            target, source = half_of(piece(index, 2 - part), index, part), stage_of(index, part)
            length = source.shape[0] // 4

            @pl.loop(0, 4)
            def _(step):
                rows = cols_of(step, length)
                target[rows, :] = (target[rows, :].astype(F32) + source[rows, :].astype(F32)).astype(BF)

            send_near(index, 2 - part, part).start()

    def row_grads(index, slot, left, left_pair, right, right_pair, columns):
        mine, theirs = slice_of(slot, width, True), slice_of(slot, width, False)
        turned, turned_pair = jnp.transpose(left[:, mine]), jnp.transpose(left_pair[:, theirs])
        target = piece(index, slot)

        @pl.loop(0, columns // 512)
        def _(step):
            cols = cols_of(step, 512)
            total = dot(turned, right[:, cols]) + dot(turned_pair, right_pair[:, cols])
            target[:, cols] = total.astype(BF)

        if slot == 3:
            send_far(index, 0).start()
            send_far(index, 1).start()
        elif slot == 0:
            keep_grad(index).start()
        else:
            send_near(index, slot, slot - 1).start()

    def out_grads():
        for part in range(2):
            rows = pl.ds(part * (heads // 2), heads // 2)
            turned, turned_pair = jnp.transpose(attended[:, rows]), jnp.transpose(cot[:, rows])
            for slot in range(4):
                mine, theirs = slice_of(slot, width, True), slice_of(slot, width, False)
                total = dot(turned, buffer_a[:, mine]) + dot(turned_pair, cot_half[:, theirs])
                piece(4, slot)[rows, :] = total.astype(BF)
            send_far(4, part).start()
            send_near(4, part + 1, part).start()
        keep_grad(4).start()

    def down_piece(slot, index, part=None):
        cols = pl.ds(((slot % 2) * GROUPS + index) * width, width)
        rows = pl.ds(0, group) if part is None else pl.ds(part * (group // 2), group // 2)
        return (buffer_b, buffer_c)[slot // 2].at[rows, cols]

    def down_rows(ref, index, slot, part=None):
        rows = pl.ds(index * group, group) if part is None else pl.ds(index * group + part * (group // 2), group // 2)
        return ref.at[rows, pl.ds(slot * width, width)]

    def send_down(kind, index, part):
        if kind == 0:
            target, source = down_rows(grad_merge[0], index, 0, part), down_piece(3, index, part)
            peer = own ^ (2 + 2 * part)
        else:
            target, source = down_rows(down_parts, index, kind, part), down_piece(kind, index, part)
            peer = own ^ (2 * kind)
        return remote(source, target, d_send.at[0], d_recv.at[GROUPS if kind else index], "dp", peer)

    def keep_down(index):
        return local(down_piece(0, index), down_rows(down_parts, index, 0), keep.at[8 + index])

    def down_grads(index):
        drain(buffer_a.at[:, pl.ds(index * group, group)], f_recv.at[index])

        @pl.loop(0, group // 256)
        def _(step):
            cols = pl.ds(pl.multiple_of(index * group + step * 256, 256), 256)
            rows = pl.ds(pl.multiple_of(step * 256, 256), 256)
            turned, turned_pair = jnp.transpose(hidden[:, cols]), jnp.transpose(buffer_a[:, cols])
            for slot in range(4):
                mine, theirs = slice_of(slot, width, True), slice_of(slot, width, False)
                total = dot(turned, cot[:, mine]) + dot(turned_pair, cot_half[:, theirs])
                down_piece(slot, index)[rows, :] = total.astype(BF)

        for part in range(2):
            send_down(0, index, part).start()
        for part in range(2):
            send_down(1 + part, index, part).start()
        keep_down(index).start()

    def merge_down(indices):
        entries = [(index, part) for index in indices for part in range(2)]

        def stage(index, part):
            rows = pl.ds(part * (group // 2), group // 2)
            return d_attended.at[rows, pl.ds((index % 2) * width, width)]

        loads = [
            local(down_rows(grad_merge[0], index, 0, part), stage(index, part), load.at[2 * (index % 2) + part])
            for index, part in entries
        ]
        for index in indices:
            drain(down_rows(grad_merge[0], index, 0), d_recv.at[index])
        start_all(loads)
        for copy, (index, part) in zip(loads, entries):
            copy.wait()
            target, source = down_piece(2 - part, index, part), stage(index, part)

            @pl.loop(0, 2)
            def _(step):
                rows = cols_of(step, group // 4)
                target[rows, :] = (target[rows, :].astype(F32) + source[rows, :].astype(F32)).astype(BF)

            send_down(2 - part, index, part).start()

    def norm_back(total, values, gain):
        inverse = lax.rsqrt(jnp.mean(values * values, axis=-1, keepdims=True) + EPSILON)
        scaled = total * gain
        return inverse * (scaled - values * inverse * inverse * jnp.mean(scaled * values, axis=-1, keepdims=True))

    gains_in[...] = jnp.zeros(gains_in.shape, F32)
    gains_in[:2, :] = plain_gains[...].astype(F32)
    meet()
    for gather in gather_hidden:
        gather.start()
    for flip in range(1, 8):
        send_gain(flip).start()
    send_weights(range(3))
    stage_down = down_w.at[:, pl.ds(3 * heads, width)]
    stage_in = local(weights_in[4], stage_down, load.at[0])
    own_loads = [local(gains_in, at_cols(gains, own, width), load.at[1])]
    own_loads += [local(weights_in[item], view(item, own), load.at[2 + item]) for item in range(4)]
    own_loads += [local(weights_in[5], at_rows(gate_w, own, width), load.at[6])]
    own_loads += [local(weights_in[6], at_rows(up_w, own, width), load.at[7])]
    for part in range(PARTS):
        own_loads.append(local(hidden_in.at[part_rows(part), :], buffer_b.at[own_rows(part), :], load.at[8 + part]))
        own_loads.append(local(cot_in.at[part_rows(part), :], cot.at[own_rows(part), :], load.at[10 + part]))
    start_all([stage_in] + own_loads)
    fill_mask(bias, docs, size)
    fill_turns(cosine, sine, size)
    for part in range(PARTS):
        clear(part)
    relay_weights([0])
    gather_hidden[0].hop(0)
    gather_hidden[0].hop(1)
    relay_weights([1])
    gather_hidden[1].hop(0)
    gather_hidden[1].hop(1)
    gather_hidden[0].hop(2)
    relay_weights([2])
    send_weights([3, 4])
    gather_hidden[1].hop(2)
    for gather in gather_cot:
        gather.start()
    stage_in.wait()
    stage_out = local(stage_down, at_cols(down_full, own, width), keep.at[5])
    stage_out.start()
    wait_all(own_loads)
    drain(gain_recv.at[pl.ds(0, 56), :], y_recv.at[0])
    gather_cot[0].hop(1)
    gather_cot[0].hop(0)
    pass_weights(range(3))
    relay_weights([3])
    send_weights(range(5, 4 + 3 * GROUPS))
    for gather in gather_hidden:
        gather.wait()

    norm_rows(buffer_b, buffer_c, inverses_one, gains.at[pl.ds(0, 1), :], 64)
    keep_hidden = local(buffer_b, hidden_rows, keep.at[0])
    keep_normed = local(buffer_c, normed_rows, keep.at[1])
    start_all([keep_hidden, keep_normed])
    have_weights(0)
    qkv_w = down_w.at[:, pl.ds(0, 3 * heads)]
    keep_qkv = local(qkv_w, qkv_full, keep.at[2])
    keep_qkv.start()

    @pl.loop(0, 2 * heads // step_cols)
    def _(step):
        cols = cols_of(step)
        product = dot(buffer_c[...], down_w[:, cols])
        turns = [jnp.concatenate([table[...]] * (step_cols // 128), axis=1) for table in (cosine, sine)]
        qkv[:, cols] = turn(product, *turns).astype(BF)

    @pl.loop(2 * heads // step_cols, 3 * heads // step_cols)
    def _(step):
        cols = cols_of(step)
        qkv[:, cols] = dot(buffer_c[...], down_w[:, cols]).astype(BF)

    attend(qkv, attended, bias, heads)
    gather_cot[0].hop(2)
    gather_cot[1].hop(1)
    gather_cot[1].hop(0)
    pass_weights([3])
    have_weights(1)

    def make_out(part):
        @pl.loop(0, count)
        def _(step):
            cols = cols_of(step)
            product = dot(attended[part * span : (part + 1) * span, :], out_w[:, cols])
            middle[part_rows(part), cols] = product[:size, :]
            send_part[pl.ds(part * span + size, span - size), cols] = product[size:, :].astype(BF)

    make_out(0)
    out_scatter[0].start()
    make_out(1)
    out_scatter[1].start()
    gather_cot[1].hop(2)
    wait_all([keep_hidden, keep_normed, keep_qkv, stage_out])
    send_normed = halves(normed_rows, pair_normed, 1)
    send_attended = to_pair(attended, pair_attended, 2, 0)
    start_all(send_normed + [send_attended])
    for index in range(3):
        out_scatter[0].hop(index)
    relay_weights(items_of(0))

    def make_sent(part):
        out_scatter[part].wait()

        @pl.loop(0, size // 32)
        def _(step):
            rows = pl.ds(pl.multiple_of(part * size + step * 32, 32), 32)
            place = pl.ds(pl.multiple_of(part * span + step * 32, 32), 32)
            total = received(part, step * 32, 32, hidden_of(place) + middle[rows, :])
            middle[rows, :] = total
            sent[place, :] = total.astype(BF)

        gather_sent[part].start()

    def hidden_of(place):
        return buffer_b[place, :].astype(F32)

    make_sent(0)
    out_scatter[1].hop(0)
    relay_weights(items_of(1))
    gather_sent[0].hop(0)
    out_scatter[1].hop(1)
    out_scatter[1].hop(2)
    make_sent(1)
    gather_sent[0].hop(1)
    relay_weights(items_of(2))
    gather_sent[1].hop(0)
    gather_sent[1].hop(1)
    gather_sent[0].hop(2)
    gather_sent[1].hop(2)
    relay_weights(items_of(3))

    def load_down(index):
        rows = pl.ds(index * group, group)
        return local(down_full.at[rows, :], down_w.at[rows, :], down_load.at[index])

    for gather in gather_cot:
        gather.wait()
    send_cot = halves(cot, cot_half, 0)
    start_all(send_cot)
    for gather in gather_sent:
        gather.wait()
    norm_rows(sent, normed, inverses, gains.at[pl.ds(1, 1), :], 64)
    pass_weights(items_of(0))
    send_two = halves(normed, two_half, 3)
    start_all(send_two)
    have_weights(2)
    for phase in range(2):
        sent_weights(phase)
    for gather in gather_hidden:
        gather.finish()
    load_down(0).start()
    for index in range(GROUPS):
        load_down(index).wait()
        if index + 1 < GROUPS:
            pass_weights(items_of(index + 1))

        @pl.loop(index * group // step_cols, (index + 1) * group // step_cols)
        def _(step):
            cols = cols_of(step)
            gate = dot(normed[...], gate_w[:, cols])
            up = dot(normed[...], up_w[:, cols])
            d_hidden = dot_rows(cot[...], down_w[cols, :])
            s = jax.nn.sigmoid(gate)
            activated = gate * s
            hidden[:, cols] = (activated * up).astype(BF)
            d_gate[:, cols] = (d_hidden * up * (s + activated * (1.0 - s))).astype(BF)
            d_up[:, cols] = (d_hidden * activated).astype(BF)
            for which in range(3):
                send_ff(step, which).start()

        if index + 1 < GROUPS:
            have_weights(3 + index)
            load_down(index + 1).start()
        if index == 0:
            drain(cot_half, h_recv.at[0])
        else:
            down_grads(index - 1)

    gain_part[...] = jnp.zeros(gain_part.shape, F32)
    for part in range(PARTS):
        out_scatter[part].finish()

    def make_two(part):
        block = slice(part * span, (part + 1) * span)

        @pl.loop(0, count)
        def _(step):
            cols = cols_of(step)
            product = dot_rows(d_gate[block, :], gate_w[cols, :]) + dot_rows(d_up[block, :], up_w[cols, :])
            gain_part[pl.ds(1, 1), cols] += jnp.sum(
                product * (sent[block, cols].astype(F32) * inverses[block, :]), axis=0, keepdims=True
            )
            grad_middle[part_rows(part), cols] = product[:size, :]
            send_part[pl.ds(part * span + size, span - size), cols] = product[size:, :].astype(BF)

    make_two(0)
    two_scatter[0].start()
    down_grads(GROUPS - 1)
    merge_down((0, 1))
    make_two(1)
    two_scatter[0].hop(0)
    two_scatter[1].start()
    for phase in range(2, 2 + GROUPS):
        sent_weights(phase)
    for which in (1, 2):
        drain((d_gate, d_up)[which - 1], f_recv.at[GROUPS - 1 + which])
    gate_pair, up_pair = up_w.at[pl.ds(0, tokens), :], up_w.at[pl.ds(tokens, tokens), :]
    pair_loads = [local(pair_gate, gate_pair, load.at[0]), local(pair_up, up_pair, load.at[1])]
    start_all(pair_loads)
    drain(two_half, h_recv.at[3])
    wait_all(pair_loads)
    gate_grads = lambda slot: row_grads(1, slot, normed, two_half, d_gate, gate_pair, units)
    up_grads = lambda slot: row_grads(2, slot, normed, two_half, d_up, up_pair, units)
    gate_grads(3)
    merge_down((2, 3))
    two_scatter[0].hop(1)
    two_scatter[0].hop(2)
    for slot in (1, 2, 0):
        gate_grads(slot)

    def make_branch(part):
        two_scatter[part].wait()

        @pl.loop(0, size // 32)
        def _(step):
            rows = pl.ds(pl.multiple_of(part * size + step * 32, 32), 32)
            place = pl.ds(pl.multiple_of(part * span + step * 32, 32), 32)
            total = received(part, step * 32, 32, grad_middle[rows, :])
            result = cot[place, :].astype(F32) + norm_back(total, sent[place, :].astype(F32), gains[1:2, :])
            grad_middle[rows, :] = result
            sent[place, :] = result.astype(BF)

        gather_branch[part].start()
        keep_branch[part].start()

    keep_branch = [
        local(sent.at[own_rows(part), :], branch_rows.at[own_rows(part), :], keep.at[6 + part]) for part in range(PARTS)
    ]
    for part in range(PARTS):
        gather_sent[part].finish()
    make_branch(0)
    up_grads(3)
    two_scatter[1].hop(0)
    up_grads(1)
    gather_branch[0].hop(0)
    two_scatter[1].hop(1)
    two_scatter[1].hop(2)
    up_grads(2)
    up_grads(0)
    def project(first, last):
        @pl.loop(first, last)
        def _(step):
            cols = cols_of(step)
            product = dot(hidden[...], down_w[:, cols])
            for part in range(PARTS):
                start = part * span
                middle[part_rows(part), cols] = middle[part_rows(part), cols] + product[start : start + size, :]
                sent[pl.ds(start + size, span - size), cols] = product[start + size : start + span, :].astype(BF)

    pl.when(ends(rank))(lambda: project(0, count))
    mlp_scatter[0].start((0,))
    make_branch(1)
    mlp_scatter[0].start((1, 2))
    mlp_scatter[1].start()
    pl.when(inner(rank))(lambda: project(0, count // 4))
    gather_branch[0].hop(1)
    merge_grads(1)
    pl.when(inner(rank))(lambda: project(count // 4, count // 2))
    gather_branch[1].hop(0)
    pl.when(inner(rank))(lambda: project(count // 2, count))
    gather_branch[1].hop(1)
    gather_branch[0].hop(2)
    gather_branch[1].hop(2)
    load_weight = local(qkv_full, qkv_w, load.at[4])
    load_hidden = local(hidden_rows, gate_pair, load.at[5])
    load_normed = local(normed_rows, up_pair, load.at[6])
    start_all([load_hidden, load_normed])
    mlp_scatter[0].hop(0)
    merge_grads(2)
    for part in range(PARTS):
        two_scatter[part].finish()
        gather_branch[part].wait()
        keep_branch[part].wait()

    load_branch = local(branch_rows, buffer_a, load.at[7])
    load_branch.start()
    load_weight.start()
    send_half = halves(branch_rows, pair_branch, 4)
    start_all(send_half)
    mlp_scatter[0].hop(1)
    load_branch.wait()

    @pl.loop(0, heads // step_cols)
    def _(step):
        cols = cols_of(step)
        d_attended[:, cols] = dot_rows(buffer_a[...], out_w[cols, :]).astype(BF)

    drain(cot_half, h_send.at[0])
    for gather in gather_cot:
        gather.finish()
    drain(two_half, h_recv.at[1])
    send_attended.wait_recv()
    early_loads = [
        local(pair_attended, cot.at[:, pl.ds(0, heads)], load.at[8]),
        local(pair_normed, two_half, load.at[9]),
    ]
    start_all(early_loads)
    attend_back(qkv, d_attended, d_qkv, bias, cosine, sine, heads)
    send_qkv = to_pair(d_qkv, pair_qkv, 5, 0)
    send_qkv.start()
    for which in range(3):
        drain((hidden, d_gate, d_up)[which], f_send.at[which])

    drain(cot_half, h_recv.at[4])
    load_half = local(pair_branch, cot_half, load.at[10])
    load_half.start()
    mlp_scatter[0].hop(2)
    mlp_scatter[1].hop(0)
    wait_all([load_weight, load_hidden, load_normed])

    def make_one(part):
        block = slice(part * span, (part + 1) * span)

        @pl.loop(0, count)
        def _(step):
            cols = cols_of(step)
            product = dot_rows(d_qkv[block, :], down_w[cols, pl.ds(0, 3 * heads)])
            gain_part[pl.ds(0, 1), cols] += jnp.sum(
                product * (gate_pair[block, cols].astype(F32) * inverses_one[block, :]), axis=0, keepdims=True
            )
            input_grad[part_rows(part), cols] = product[:size, :]
            send_part[pl.ds(part * span + size, span - size), cols] = product[size:, :].astype(BF)

        one_scatter[part].start()

    def share_gain(flip):
        source = at_cols(gain_part, own ^ flip, width)
        return remote(source, at_rows(gain_recv, flip, 8), g_send.at[0], g_recv.at[0], "dp", own ^ flip)

    make_one(0)
    mlp_scatter[1].hop(1)

    send_qkv.wait_recv()
    drain(two_half, h_send.at[3])
    load_qkv = local(pair_qkv, normed.at[:, pl.ds(0, 3 * heads)], load.at[0])
    load_qkv.start()
    for index in range(1, 3):
        keep_grad(index).wait()
    wait_all(early_loads + [load_half])
    out_grads()
    mlp_scatter[1].hop(2)
    load_qkv.wait()
    for slot in (3, 1, 2, 0):
        row_grads(3, slot, up_pair, two_half, d_qkv, normed, 3 * heads)
        if slot == 2:
            one_scatter[0].hop(0)
            make_one(1)
    for flip in range(1, 8):
        share_gain(flip).start()
    one_scatter[0].hop(1)
    one_scatter[0].hop(2)
    merge_grads(4)
    one_scatter[1].hop(0)
    merge_grads(3)
    one_scatter[1].hop(1)
    one_scatter[1].hop(2)

    drain(gain_recv.at[pl.ds(8, 56), :], g_recv.at[0])
    gain_sum = gain_part[:, pl.ds(pl.multiple_of(own * width, width), width)]
    for flip in range(1, 8):
        gain_sum = gain_sum + gain_recv[pl.ds(flip * 8, 8), :]
    gain_z[pl.ds(0, 8), :] = gain_sum

    def share_gain_z(k):
        target = gain_z.at[pl.ds(8 * k, 8), :]
        return remote(gain_z.at[pl.ds(0, 8), :], target, y_send.at[1], y_recv.at[1], "tensor", lax.rem(rank + k, 4))

    for k in (1, 2, 3):
        share_gain_z(k).start()

    load_own = [
        local(hidden_in.at[part_rows(part), :], sent.at[own_rows(part), :], load.at[4 + part]) for part in range(PARTS)
    ]
    for part in range(PARTS):
        gather_branch[part].finish()
    start_all(load_own)
    wait_all(load_own)
    for part in range(PARTS):
        one_scatter[part].wait()

        @pl.loop(0, size // 32)
        def _(step):
            rows = pl.ds(pl.multiple_of(part * size + step * 32, 32), 32)
            place = pl.ds(pl.multiple_of(part * span + step * 32, 32), 32)
            total = received(part, step * 32, 32, input_grad[rows, :])
            input_grad[rows, :] = grad_middle[rows, :] + norm_back(total, sent[place, :].astype(F32), gains[0:1, :])

    for scatter in mlp_scatter:
        scatter.wait()
    load_mlp = [
        [local(mlp_recv.at[arrived(part, slot), :], recv_part.at[arrived(part, slot), :], load.at[2 * part + index])
         for index, slot in enumerate((4, 2))]
        for part in range(PARTS)
    ]
    for part in range(PARTS):
        load_mlp[part][0].start()
        pl.when(inner(rank))(load_mlp[part][1].start)
    for part in range(PARTS):
        load_mlp[part][0].wait()
        pl.when(inner(rank))(load_mlp[part][1].wait)

        @pl.loop(0, size // 32)
        def _(step):
            rows = pl.ds(pl.multiple_of(part * size + step * 32, 32), 32)
            layer_out[rows, :] = received(part, step * 32, 32, middle[rows, :]).astype(BF)

    drain(gain_z.at[pl.ds(8, 24), :], y_recv.at[1])
    gain_all = gain_z[pl.ds(0, 8), :]
    for k in (1, 2, 3):
        gain_all = gain_all + gain_z[pl.ds(8 * k, 8), :]
    gain_total[...] = gain_all

    for scatter in mlp_scatter + one_scatter:
        scatter.finish()
    for index in range(GROUPS):
        keep_down(index).wait()
    drain(gate_w.at[pl.ds(0, units // 4), :], d_recv.at[GROUPS])
    drain(gate_w.at[pl.ds(0, 3 * units // 8), :], d_send.at[0])
    drain(gain_recv.at[pl.ds(8, 56), :], y_send.at[0])
    drain(gain_recv.at[pl.ds(8, 56), :], g_send.at[0])
    drain(gain_z.at[pl.ds(8, 24), :], y_send.at[1])
    drain(two_half, h_send.at[1])
    drain(two_half, h_send.at[4])
    send_attended.wait_send()
    send_qkv.wait_send()
    def pieces(index, number):
        rows = number * width if index < 4 else number * heads * width // dim
        return gate_w.at[pl.ds(0, rows), pl.ds(0, 3 * heads if index == 3 else dim)]

    for index in range(1, 5):
        drain(pieces(index, 2), n_recv.at[index - 1])
        if index > 2:
            keep_grad(index).wait()
        drain(pieces(index, 3), w_send.at[index - 1])


def layer(hidden_in, cot, gains, weights, docs):
    tile, dim = hidden_in.shape
    tokens = 4 * tile
    width, heads = weights[0].shape
    units = weights[5].shape[1]
    dma = pltpu.SemaphoreType.DMA
    rows, narrow, ff = shape((tokens, dim), BF), shape((tokens, dim // 2), BF), shape((tokens, units), BF)
    weights_shape = [(units, width), (width, units), (width, units), (width, 3 * heads), (heads, width)]
    parts_shape = [(units, 3 * width), (3 * width, units), (3 * width, units), (3 * width, 3 * heads), (heads, 3 * width)]
    outs = [shape(dims, BF) for dims in parts_shape + weights_shape]
    outs += [ff] * 2 + [shape((tokens, 3 * heads), BF), shape((tokens, heads), BF), narrow, narrow]
    outs += [rows] * 3 + [shape((5 * tile, dim), BF), shape((dim, 3 * heads), BF), shape((units, dim), BF)]
    in_hbm = len(outs)
    outs += [shape((tile, dim), BF), shape((tile, dim), F32), shape((8, width), F32)]
    items = 4 + 3 * GROUPS
    scratch = [((dim, units), BF), ((dim, units), BF), ((units, dim), BF)]
    scratch += [((tokens, dim), BF)] * 3 + [((tokens, units), BF)] * 3
    scratch += [((tokens, dim // 2), BF)] * 2 + [((tokens, dim), BF)] * 3 + [((heads, dim), BF)]
    scratch += [((tokens, 3 * heads), BF)] + [((tokens, heads), BF)] * 2
    scratch += [((tokens, tokens), F32), ((tokens, 128), F32), ((tokens, 128), F32)]
    scratch += [((tokens, 1), F32), ((tokens, 1), F32), ((tile, dim), F32), ((tile, dim), F32)]
    scratch += [((tokens, dim), BF), ((5 * tile, dim), BF)]
    scratch += [((8, width), F32), ((8, dim), F32), ((8, dim), F32), ((64, width), F32), ((32, width), F32)]
    sems = [(2 + GROUPS,), (items, 3), (3,), (GROUPS + 2,), (6,), (6,)]
    sems += [(4, PARTS), (4, PARTS, 3), (4, PARTS), (4, PARTS, 5), (4,), (4, 2), (1,), (GROUPS + 1,)]
    sems += [(1,), (1,), (2,), (2,), (12,), (8 + GROUPS,), (GROUPS,), (2 + GROUPS,), (4,)]
    return pl.pallas_call(
        layer_kernel,
        out_shape=outs,
        in_specs=[anyspace()] * 2 + [vmem()] + [anyspace()] * 7 + [vmem()],
        out_specs=[anyspace()] * in_hbm + [vmem()] * 3,
        scratch_shapes=[pltpu.VMEM(*entry) for entry in scratch] + [dma(entry) for entry in sems],
        compiler_params=pltpu.CompilerParams(vmem_limit_bytes=67000000, collective_id=0, has_side_effects=True),
        cost_estimate=cost(2 * tokens * dim * units * 12, 100e6),
        name="layer",
    )(hidden_in, cot, gains, *weights, docs)


def sum_kernel(count, *refs):
    parts, plain_in = refs[:5], refs[5:7]
    down, gate, up, query, key, value, out, *plain_out = refs[7:16]
    staged, totals, plain, load, store = refs[16:21], refs[21:26], refs[26:28], refs[28], refs[29]
    loads = [pltpu.make_async_copy(parts[index], staged[index], load.at[index]) for index in range(5)]
    loads += [pltpu.make_async_copy(plain_in[index], plain[index], load.at[5 + index]) for index in range(2)]
    start_all(loads)
    heads = query.shape[1]
    stores = [pltpu.make_async_copy(totals[index], ref, store.at[index]) for index, ref in enumerate((down, gate, up))]
    qkv_stores = [
        pltpu.make_async_copy(totals[3].at[:, pl.ds(index * heads, heads)], ref, store.at[3 + index])
        for index, ref in enumerate((query, key, value))
    ]
    out_store = pltpu.make_async_copy(totals[4], out, store.at[6])
    plain_stores = [pltpu.make_async_copy(plain[index], plain_out[index], store.at[7 + index]) for index in range(2)]
    groups = [[stores[0]], [stores[1]], [stores[2]], qkv_stores, [out_store]]
    for index in range(5):
        loads[index].wait()
        rows_first = index in (1, 2, 3)
        rows, cols = totals[index].shape
        step_rows = 32 if rows_first else 256

        @pl.loop(0, rows // step_rows)
        def _(step):
            start = pl.multiple_of(step * step_rows, step_rows)
            total = None
            for slot in range(count):
                if rows_first:
                    term = staged[index][pl.ds(pl.multiple_of(start + slot * rows, step_rows), step_rows), :]
                else:
                    term = staged[index][pl.ds(start, step_rows), slot * cols : (slot + 1) * cols]
                term = term.astype(F32)
                total = term if total is None else total + term
            totals[index][pl.ds(start, step_rows), :] = total

        start_all(groups[index])
    for index in range(2):
        loads[5 + index].wait()
        plain_stores[index].start()
    for entry in groups + [plain_stores]:
        wait_all(entry)


def sum_grads(parts, plain, heads, count):
    dims = [part.shape for part in parts]
    sums = [
        (rows // count, cols) if index in (1, 2, 3) else (rows, cols // count) for index, (rows, cols) in enumerate(dims)
    ]
    outs = sums[:3] + [(sums[3][0], heads)] * 3 + [sums[4]]
    dma = pltpu.SemaphoreType.DMA
    return pl.pallas_call(
        partial(sum_kernel, count),
        out_shape=[shape(dim, F32) for dim in outs] + [shape(entry.shape, entry.dtype) for entry in plain],
        in_specs=[anyspace()] * 7,
        out_specs=[anyspace()] * 9,
        scratch_shapes=[pltpu.VMEM(dim, BF) for dim in dims]
        + [pltpu.VMEM(dim, F32) for dim in sums]
        + [pltpu.VMEM(entry.shape, entry.dtype) for entry in plain]
        + [dma((7,)), dma((9,))],
        compiler_params=params(),
        cost_estimate=cost(1e6, 22e6),
        name="sum_grads",
    )(*parts, *plain)


def shift(values, step):
    size = lax.axis_size("tensor")
    return lax.ppermute(values, "tensor", [(index, (index + step) % size) for index in range(size)])


def gather_rows(values):
    return [values] + [shift(values, step) for step in range(1, lax.axis_size("tensor"))]


def scatter_rows(parts):
    total = parts[0].astype(F32)
    for step in range(1, len(parts)):
        total = total + shift(parts[step], -step).astype(F32)
    return total


def gather_weight(values, axis):
    return [None], [lax.all_gather(values, "dp", axis=axis, tiled=True)]


def scatter_full(left, right, axis):
    full = dot_cols(left, right).astype(BF)
    return lax.psum_scatter(full, "dp", scatter_dimension=axis, tiled=True).astype(F32)


def frequencies():
    half_size = HEAD_DIM // 2
    return ROPE_BASE ** (-jnp.arange(half_size, dtype=F32) / half_size)


def rotary(length):
    angles = jnp.arange(length).astype(F32)[:, None] * frequencies()[None, :]
    cosine, sine = jnp.cos(angles), jnp.sin(angles)
    cosine = jnp.tile(cosine, (1, 8))
    sine = jnp.tile(jnp.concatenate([-sine, sine], axis=1), (1, 4))
    return cosine, sine


def position_tables(doc_ids, ranks):
    length = doc_ids.shape[0]
    token_index = jnp.arange(length, dtype=jnp.int32)
    before = jnp.concatenate([doc_ids[:1] - 1, doc_ids[:-1]])
    doc_start = lax.cummax(jnp.where(doc_ids != before, token_index, 0), axis=0)
    order = (lax.axis_index("tensor") - jnp.arange(ranks)) % ranks
    last = token_index.reshape(ranks, -1)[order].reshape(length)
    first = doc_start.reshape(ranks, -1)[order].reshape(length)
    cosine, sine = (table.reshape(ranks, -1, 256)[order].reshape(length, 256) for table in rotary(length))
    return cosine, sine, first[:, None], last[:, None], last[None, :]


def rms_back(grad_rows_, values, gain):
    inverse = lax.rsqrt(jnp.mean(values * values, axis=-1, keepdims=True) + EPSILON)
    scaled = grad_rows_ * gain
    return inverse * (scaled - values * inverse * inverse * jnp.mean(scaled * values, axis=-1, keepdims=True))


def body(
    hidden_in,
    out_cotangent,
    doc_ids,
    attn_gain,
    query_weight,
    key_weight,
    value_weight,
    out_weight,
    mlp_gain,
    gate_weight,
    up_weight,
    down_weight,
):
    ranks, groups = lax.axis_size("tensor"), lax.axis_size("dp")
    paired = (groups, ranks) == (8, 4)
    width, heads = query_weight.shape
    dim = hidden_in.shape[1]

    if paired:
        weights = (query_weight, key_weight, value_weight, out_weight, down_weight, gate_weight, up_weight)
        own_gains = jnp.stack([attn_gain, mlp_gain])
        outs = layer(hidden_in, out_cotangent, own_gains, weights, doc_ids.reshape(ranks, -1))
        sums = sum_grads(outs[:5], outs[-3:-1], heads, 3)
        down_grad, gate_grad, up_grad, query_grad, key_grad, value_grad, out_proj_grad, layer_out, input_grad = sums
        gain_total = outs[-1]
        share = width // ranks
        gain_grads = lax.dynamic_slice_in_dim(gain_total, lax.axis_index("tensor") * share, share, axis=1)
    else:
        tables = position_tables(doc_ids, ranks)
        input_local = hidden_in.astype(F32)
        hidden_rows = gather_rows(hidden_in)
        gains = lax.all_gather(jnp.stack([attn_gain, mlp_gain]), "dp", axis=1, tiled=True).astype(F32)
        attn_scale, mlp_scale = gains[:1], gains[1:]
        qkv_weight = jnp.concatenate([query_weight, key_weight, value_weight], axis=1)
        tags, qkv_pieces = gather_weight(qkv_weight, 0)
        tags, out_pieces = gather_weight(out_weight, 1)
        cot_rows = gather_rows(out_cotangent)
        tags, down_pieces = gather_weight(down_weight, 1)
        tags, gate_pieces = gather_weight(gate_weight, 0)
        tags, up_pieces = gather_weight(up_weight, 0)
        normed, qkv, attended, inverses, *branch_parts = attn_fwd(
            hidden_rows, attn_scale, tables, tags, width, qkv_pieces, out_pieces
        )
        middle = input_local + scatter_rows(branch_parts)
        sent = middle.astype(BF)
        sent_rows = gather_rows(sent)
        cot_full = jnp.concatenate(cot_rows, axis=0)
        normed_two, hidden, d_gate, d_up, mlp_gain_part, *two_parts = mlp(
            sent_rows, cot_rows, mlp_scale, tags, width, gate_pieces, up_pieces, down_pieces, ranks
        )
        grad_two_rows = scatter_rows(two_parts)
        grad_middle = out_cotangent.astype(F32) + rms_back(grad_two_rows, sent.astype(F32), mlp_scale)
        branch_rows = gather_rows(grad_middle.astype(BF))
        down_grad = scatter_full(hidden, cot_full, 1)
        gate_grad = scatter_full(normed_two, d_gate, 0)
        up_grad = scatter_full(normed_two, d_up, 0)
        mlp_rows = scatter_rows(mlp_out(hidden, ranks, dim, tags, width, down_pieces))
        layer_out = (middle + mlp_rows).astype(BF)
        branch_full, d_qkv, attn_gain_part, *one_parts = attn_bwd(
            branch_rows, hidden_rows, qkv, inverses, tables, tags, width, qkv_pieces, out_pieces, ranks
        )
        out_proj_grad = scatter_full(attended, branch_full, 1)
        query_grad, key_grad, value_grad = jnp.split(scatter_full(normed, d_qkv, 0), 3, axis=1)
        grad_one_rows = scatter_rows(one_parts)
        input_grad = grad_middle + rms_back(grad_one_rows, input_local, attn_scale)
        gain_parts = jnp.concatenate([attn_gain_part, mlp_gain_part], axis=0)
        gain_grads = lax.psum_scatter(gain_parts, ("dp", "tensor"), scatter_dimension=1, tiled=True)
    return (
        layer_out,
        input_grad,
        gain_grads[0],
        query_grad,
        key_grad,
        value_grad,
        out_proj_grad,
        gain_grads[1],
        gate_grad,
        up_grad,
        down_grad,
    )


def solution(mesh):
    return jax.shard_map(
        body,
        mesh=mesh,
        in_specs=(
            P(("dp", "tensor"), None),
            P(("dp", "tensor"), None),
            P("dp"),
            P("dp"),
            P("dp", "tensor"),
            P("dp", "tensor"),
            P("dp", "tensor"),
            P("tensor", "dp"),
            P("dp"),
            P("dp", "tensor"),
            P("dp", "tensor"),
            P("tensor", "dp"),
        ),
        out_specs=(
            P(("dp", "tensor"), None),
            P(("dp", "tensor"), None),
            P(("dp", "tensor")),
            P("dp", "tensor"),
            P("dp", "tensor"),
            P("dp", "tensor"),
            P("tensor", "dp"),
            P(("dp", "tensor")),
            P("dp", "tensor"),
            P("dp", "tensor"),
            P("tensor", "dp"),
        ),
        check_vma=False,
    )
```

```python
import math
from functools import partial

import jax
import jax.numpy as jnp
from jax import lax
from jax.experimental import pallas as pl
from jax.experimental.pallas import tpu as pltpu
from jax.sharding import PartitionSpec as P

HEAD_DIM = 64
EPSILON = 1e-05
ROPE_BASE = 130000.0
NEGATIVE = -1e30
VMEM_LIMIT = 63 * 1024 * 1024
BF = jnp.bfloat16
F32 = jnp.float32


def dot(left, right):
    return jnp.dot(left, right, preferred_element_type=F32)


def dot_rows(left, right):
    return lax.dot_general(left, right, (((1,), (1,)), ((), ())), preferred_element_type=F32)


def dot_cols(left, right):
    return lax.dot_general(left, right, (((0,), (0,)), ((), ())), preferred_element_type=F32)


def vmem():
    return pl.BlockSpec(memory_space=pltpu.VMEM)


def anyspace():
    return pl.BlockSpec(memory_space=pl.ANY)


def params():
    return pltpu.CompilerParams(vmem_limit_bytes=VMEM_LIMIT)


def cost(flops, nbytes):
    return pl.CostEstimate(flops=int(flops), bytes_accessed=int(nbytes), transcendentals=0)


def shape(dims, kind):
    return jax.ShapeDtypeStruct(dims, kind)


def place_copies(tags, pieces, target, sem, axis, width):
    own = lax.axis_index("dp")
    copies = []
    for slot, (tag, piece) in enumerate(zip(tags, pieces)):
        if tag is None:
            where = target
        else:
            start = pl.multiple_of((own ^ tag) * width, width)
            where = target.at[pl.ds(start, width), :] if axis == 0 else target.at[:, pl.ds(start, width)]
        copies.append(pltpu.make_async_copy(piece, where, sem.at[slot]))
    return copies


def row_copies(pieces, target, sem):
    copies = []
    for slot, piece in enumerate(pieces):
        rows = piece.shape[0]
        copies.append(pltpu.make_async_copy(piece, target.at[pl.ds(slot * rows, rows), :], sem.at[slot]))
    return copies


def start_all(copies):
    for copy in copies:
        copy.start()


def wait_all(copies):
    for copy in copies:
        copy.wait()


def turn(values, cosine, sine):
    width = values.shape[1]
    lane = lax.broadcasted_iota(jnp.int32, values.shape, 1)
    partner = jnp.where(
        lax.rem(lane, HEAD_DIM) < HEAD_DIM // 2,
        pltpu.roll(values, width - HEAD_DIM // 2, 1),
        pltpu.roll(values, HEAD_DIM // 2, 1),
    )
    return values * cosine + partner * sine


def norm_rows(source, target, inverses, gain, tile):
    @pl.loop(0, source.shape[0] // tile)
    def _(step):
        rows = pl.ds(pl.multiple_of(step * tile, tile), tile)
        values = source[rows, :].astype(F32)
        inverse = lax.rsqrt(jnp.mean(values * values, axis=-1, keepdims=True) + EPSILON)
        inverses[rows, :] = inverse
        target[rows, :] = (values * inverse * gain[...]).astype(BF)


def fill_bias(bias, first, last, key_index):
    keys = key_index[...]
    bias[...] = jnp.where((keys >= first[...]) & (keys <= last[...]), 0.0, NEGATIVE)


def head_lanes(width, half):
    lane = lax.broadcasted_iota(jnp.int32, (1, width), 1)
    return (lax.div(lane, HEAD_DIM) == half).astype(F32)


def probabilities(query, key, bias):
    scores = dot_rows(query, key) + bias
    weights = jnp.exp(scores - jnp.max(scores, axis=-1, keepdims=True))
    return weights * (1.0 / jnp.sum(weights, axis=-1, keepdims=True))


def attend(qkv, attended, bias, heads):
    @pl.loop(0, heads // 128)
    def _(pair):
        base = pl.multiple_of(pair * 128, 128)
        query = qkv[:, pl.ds(base, 128)]
        key = qkv[:, pl.ds(heads + base, 128)]
        value = qkv[:, pl.ds(2 * heads + base, 128)]
        total = None
        for half in range(2):
            lanes = head_lanes(128, half).astype(BF)
            probs = probabilities(query * (lanes * HEAD_DIM ** (-0.5)), key, bias[...])
            term = dot(probs.astype(BF), value * lanes)
            total = term if total is None else total + term
        attended[:, pl.ds(base, 128)] = total.astype(BF)


def attn_fwd_kernel(tags, width, nrow, *refs):
    npiece = len(tags)
    rows_in = refs[:nrow]
    gain, cosine, sine, first, last, key_index = refs[nrow : nrow + 6]
    rest = refs[nrow + 6 :]
    qkv_in, out_in = rest[:npiece], rest[npiece : 2 * npiece]
    rest = rest[2 * npiece :]
    normed, qkv, attended, inverses = rest[:4]
    parts = rest[4 : 4 + nrow]
    hidden, qkv_w, out_w, bias, sem_rows, sem_qkv, sem_out = rest[4 + nrow :]
    load_rows = row_copies(rows_in, hidden, sem_rows)
    load_qkv = place_copies(tags, qkv_in, qkv_w, sem_qkv, 0, width)
    load_out = place_copies(tags, out_in, out_w, sem_out, 1, width)
    start_all(load_rows + load_qkv + load_out)
    fill_bias(bias, first, last, key_index)
    wait_all(load_rows)
    norm_rows(hidden, normed, inverses, gain, 64)
    wait_all(load_qkv)
    heads = attended.shape[1]
    step_cols = 256

    @pl.loop(0, 2 * heads // step_cols)
    def _(step):
        cols = pl.ds(pl.multiple_of(step * step_cols, step_cols), step_cols)
        qkv[:, cols] = turn(dot(normed[...], qkv_w[:, cols]), cosine[...], sine[...]).astype(BF)

    @pl.loop(2 * heads // step_cols, 3 * heads // step_cols)
    def _(step):
        cols = pl.ds(pl.multiple_of(step * step_cols, step_cols), step_cols)
        qkv[:, cols] = dot(normed[...], qkv_w[:, cols]).astype(BF)

    attend(qkv, attended, bias, heads)
    wait_all(load_out)
    tile = parts[0].shape[0]

    @pl.loop(0, out_w.shape[1] // step_cols)
    def _(step):
        cols = pl.ds(pl.multiple_of(step * step_cols, step_cols), step_cols)
        product = dot(attended[...], out_w[:, cols])
        for slot, part in enumerate(parts):
            part[:, cols] = product[slot * tile : (slot + 1) * tile, :].astype(part.dtype)


def attn_fwd(rows, gain, tables, tags, width, qkv_pieces, out_pieces):
    nrow, (tile, dim) = len(rows), rows[0].shape
    tokens = nrow * tile
    heads = out_pieces[0].shape[0]
    npiece = len(tags)
    return pl.pallas_call(
        partial(attn_fwd_kernel, tags, width, nrow),
        out_shape=[
            shape((tokens, dim), BF),
            shape((tokens, 3 * heads), BF),
            shape((tokens, heads), BF),
            shape((tokens, 1), F32),
        ]
        + [shape((tile, dim), F32 if slot == 0 else BF) for slot in range(nrow)],
        in_specs=[anyspace()] * nrow + [vmem()] * 6 + [anyspace()] * (2 * npiece),
        out_specs=[vmem()] * (4 + nrow),
        scratch_shapes=[
            pltpu.VMEM((tokens, dim), BF),
            pltpu.VMEM((dim, 3 * heads), BF),
            pltpu.VMEM((heads, dim), BF),
            pltpu.VMEM((tokens, tokens), F32),
            pltpu.SemaphoreType.DMA((nrow,)),
            pltpu.SemaphoreType.DMA((npiece,)),
            pltpu.SemaphoreType.DMA((npiece,)),
        ],
        compiler_params=params(),
        cost_estimate=cost(2 * tokens * dim * 4 * heads * 3, 20e6),
        name="attn_fwd",
    )(*rows, gain, *tables, *qkv_pieces, *out_pieces)


def attend_back(qkv, d_attended, d_qkv, bias, cosine, sine, heads):
    score_scale = HEAD_DIM ** (-0.5)

    @pl.loop(0, heads // 128)
    def _(pair):
        base = pl.multiple_of(pair * 128, 128)
        query = qkv[:, pl.ds(base, 128)]
        key = qkv[:, pl.ds(heads + base, 128)]
        value = qkv[:, pl.ds(2 * heads + base, 128)]
        grad = d_attended[:, pl.ds(base, 128)]
        sums = [0.0, 0.0, 0.0]
        for half in range(2):
            lanes = head_lanes(128, half).astype(BF)
            own_query = query * (lanes * score_scale)
            own_grad = grad * lanes
            probs = probabilities(own_query, key, bias[...])
            d_value = dot_cols(probs.astype(BF), own_grad)
            d_probs = dot_rows(own_grad, value)
            delta = jnp.sum(probs * d_probs, axis=-1, keepdims=True)
            d_scores = (probs * (d_probs - delta)).astype(BF)
            d_query = dot(d_scores, key * lanes) * score_scale
            d_key = dot_cols(d_scores, own_query)
            sums = [sums[0] + d_query, sums[1] + d_key, sums[2] + d_value]
        back = -sine[:, :128]
        d_qkv[:, pl.ds(base, 128)] = turn(sums[0], cosine[:, :128], back).astype(BF)
        d_qkv[:, pl.ds(heads + base, 128)] = turn(sums[1], cosine[:, :128], back).astype(BF)
        d_qkv[:, pl.ds(2 * heads + base, 128)] = sums[2].astype(BF)


def attn_bwd_kernel(tags, width, nrow, npart, *refs):
    npiece = len(tags)
    nhid, nrow = nrow[1], nrow[0]
    rows_in, hidden_in = refs[:nrow], refs[nrow : nrow + nhid]
    refs = refs[nrow + nhid :]
    qkv, inverses, cosine, sine, first, last, key_index = refs[:7]
    rest = refs[7:]
    qkv_in, out_in = rest[:npiece], rest[npiece : 2 * npiece]
    rest = rest[2 * npiece :]
    branch, d_qkv, gain_grad = rest[:3]
    parts = rest[3 : 3 + npart]
    hidden, d_attended, qkv_w, out_w, bias, sem_rows, sem_x, sem_qkv, sem_out = rest[3 + npart :]
    load_rows = row_copies(rows_in, branch, sem_rows)
    load_x = row_copies(hidden_in, hidden, sem_x)
    load_out = place_copies(tags, out_in, out_w, sem_out, 1, width)
    load_qkv = place_copies(tags, qkv_in, qkv_w, sem_qkv, 0, width)
    start_all(load_rows + load_out + load_qkv + load_x)
    fill_bias(bias, first, last, key_index)
    wait_all(load_rows)
    wait_all(load_out)
    heads = out_w.shape[0]
    step_cols = 256

    @pl.loop(0, heads // step_cols)
    def _(step):
        cols = pl.ds(pl.multiple_of(step * step_cols, step_cols), step_cols)
        d_attended[:, cols] = dot_rows(branch[...], out_w[cols, :]).astype(BF)

    attend_back(qkv, d_attended, d_qkv, bias, cosine, sine, heads)
    wait_all(load_qkv)
    wait_all(load_x)
    tile = parts[0].shape[0]

    @pl.loop(0, qkv_w.shape[0] // step_cols)
    def _(step):
        cols = pl.ds(pl.multiple_of(step * step_cols, step_cols), step_cols)
        product = dot_rows(d_qkv[...], qkv_w[cols, :])
        gain_grad[:, cols] = jnp.sum(product * (hidden[:, cols].astype(F32) * inverses[...]), axis=0, keepdims=True)
        for slot, part in enumerate(parts):
            part[:, cols] = product[slot * tile : (slot + 1) * tile, :].astype(part.dtype)


def attn_bwd(rows, hidden, qkv, inverses, tables, tags, width, qkv_pieces, out_pieces, npart):
    nrow, nhid, dim = len(rows), len(hidden), rows[0].shape[1]
    tokens = qkv.shape[0]
    tile = tokens // npart
    heads = out_pieces[0].shape[0]
    npiece = len(tags)
    return pl.pallas_call(
        partial(attn_bwd_kernel, tags, width, (nrow, nhid), npart),
        out_shape=[shape((tokens, dim), BF), shape((tokens, 3 * heads), BF), shape((1, dim), F32)]
        + [shape((tile, dim), F32 if slot == 0 else BF) for slot in range(npart)],
        in_specs=[anyspace()] * (nrow + nhid) + [vmem()] * 7 + [anyspace()] * (2 * npiece),
        out_specs=[vmem()] * (3 + npart),
        scratch_shapes=[
            pltpu.VMEM((tokens, dim), BF),
            pltpu.VMEM((tokens, heads), BF),
            pltpu.VMEM((dim, 3 * heads), BF),
            pltpu.VMEM((heads, dim), BF),
            pltpu.VMEM((tokens, tokens), F32),
            pltpu.SemaphoreType.DMA((nrow,)),
            pltpu.SemaphoreType.DMA((nhid,)),
            pltpu.SemaphoreType.DMA((npiece,)),
            pltpu.SemaphoreType.DMA((npiece,)),
        ],
        compiler_params=params(),
        cost_estimate=cost(2 * tokens * dim * 4 * heads * 6, 30e6),
        name="attn_bwd",
    )(*rows, *hidden, qkv, inverses, *tables, *qkv_pieces, *out_pieces)


def mlp_kernel(tags, width, nrow, npart, *refs):
    npiece = len(tags)
    sent_in, cot_in = refs[:nrow], refs[nrow : 2 * nrow]
    gain = refs[2 * nrow]
    rest = refs[2 * nrow + 1 :]
    gate_in, up_in, down_in = rest[:npiece], rest[npiece : 2 * npiece], rest[2 * npiece : 3 * npiece]
    rest = rest[3 * npiece :]
    normed, hidden, d_gate, d_up, gain_grad = rest[:5]
    parts = rest[5 : 5 + npart]
    sent, cot, inverses, gate_w, up_w, down_w, sem_sent, sem_cot, sem_gate, sem_up, sem_down = rest[5 + npart :]
    load_sent = row_copies(sent_in, sent, sem_sent)
    load_cot = row_copies(cot_in, cot, sem_cot)
    load_gate = place_copies(tags, gate_in, gate_w, sem_gate, 0, width)
    load_up = place_copies(tags, up_in, up_w, sem_up, 0, width)
    load_down = place_copies(tags, down_in, down_w, sem_down, 1, width)
    start_all(load_sent + load_cot + load_gate + load_up + load_down)
    wait_all(load_sent)
    norm_rows(sent, normed, inverses, gain, 64)
    wait_all(load_cot)
    wait_all(load_gate)
    wait_all(load_up)
    wait_all(load_down)
    step_cols = 256

    @pl.loop(0, gate_w.shape[1] // step_cols)
    def _(step):
        cols = pl.ds(pl.multiple_of(step * step_cols, step_cols), step_cols)
        gate = dot(normed[...], gate_w[:, cols])
        up = dot(normed[...], up_w[:, cols])
        d_hidden = dot_rows(cot[...], down_w[cols, :])
        s = jax.nn.sigmoid(gate)
        activated = gate * s
        hidden[:, cols] = (activated * up).astype(BF)
        d_gate[:, cols] = (d_hidden * up * (s + activated * (1.0 - s))).astype(BF)
        d_up[:, cols] = (d_hidden * activated).astype(BF)

    tile = parts[0].shape[0]

    @pl.loop(0, gate_w.shape[0] // step_cols)
    def _(step):
        cols = pl.ds(pl.multiple_of(step * step_cols, step_cols), step_cols)
        product = dot_rows(d_gate[...], gate_w[cols, :]) + dot_rows(d_up[...], up_w[cols, :])
        gain_grad[:, cols] = jnp.sum(product * (sent[:, cols].astype(F32) * inverses[...]), axis=0, keepdims=True)
        for slot, part in enumerate(parts):
            part[:, cols] = product[slot * tile : (slot + 1) * tile, :].astype(part.dtype)


def mlp(sent, cot, gain, tags, width, gate_pieces, up_pieces, down_pieces, npart):
    nrow, dim = len(sent), sent[0].shape[1]
    tokens = nrow * sent[0].shape[0]
    tile = tokens // npart
    units = gate_pieces[0].shape[1]
    npiece = len(tags)
    return pl.pallas_call(
        partial(mlp_kernel, tags, width, nrow, npart),
        out_shape=[shape((tokens, dim), BF)]
        + [shape((tokens, units), BF)] * 3
        + [shape((1, dim), F32)]
        + [shape((tile, dim), F32 if slot == 0 else BF) for slot in range(npart)],
        in_specs=[anyspace()] * (2 * nrow) + [vmem()] + [anyspace()] * (3 * npiece),
        out_specs=[vmem()] * (5 + npart),
        scratch_shapes=[
            pltpu.VMEM((tokens, dim), BF),
            pltpu.VMEM((tokens, dim), BF),
            pltpu.VMEM((tokens, 1), F32),
            pltpu.VMEM((dim, units), BF),
            pltpu.VMEM((dim, units), BF),
            pltpu.VMEM((units, dim), BF),
            pltpu.SemaphoreType.DMA((nrow,)),
            pltpu.SemaphoreType.DMA((nrow,)),
            pltpu.SemaphoreType.DMA((npiece,)),
            pltpu.SemaphoreType.DMA((npiece,)),
            pltpu.SemaphoreType.DMA((npiece,)),
        ],
        compiler_params=params(),
        cost_estimate=cost(2 * tokens * dim * units * 5, 40e6),
        name="mlp",
    )(*sent, *cot, gain, *gate_pieces, *up_pieces, *down_pieces)


def mlp_out_kernel(tags, width, *refs):
    npiece = len(tags)
    hidden, down_in = refs[0], refs[1 : 1 + npiece]
    *parts, down_w, sem_down = refs[1 + npiece :]
    load_down = place_copies(tags, down_in, down_w, sem_down, 1, width)
    start_all(load_down)
    wait_all(load_down)
    tile, step_cols = parts[0].shape[0], 256

    @pl.loop(0, down_w.shape[1] // step_cols)
    def _(step):
        cols = pl.ds(pl.multiple_of(step * step_cols, step_cols), step_cols)
        product = dot(hidden[...], down_w[:, cols])
        for slot, part in enumerate(parts):
            part[:, cols] = product[slot * tile : (slot + 1) * tile, :].astype(part.dtype)


def mlp_out(hidden, nrow, dim, tags, width, down_pieces):
    tokens, units = hidden.shape
    tile, npiece = tokens // nrow, len(tags)
    return pl.pallas_call(
        partial(mlp_out_kernel, tags, width),
        out_shape=[shape((tile, dim), F32 if slot == 0 else BF) for slot in range(nrow)],
        in_specs=[vmem()] + [anyspace()] * npiece,
        out_specs=[vmem()] * nrow,
        scratch_shapes=[pltpu.VMEM((units, dim), BF), pltpu.SemaphoreType.DMA((npiece,))],
        compiler_params=params(),
        cost_estimate=cost(2 * tokens * dim * units, 14e6),
        name="mlp_out",
    )(hidden, *down_pieces)


def slice_of(slot, width, own):
    index = lax.axis_index("dp")
    owner = index ^ (2 * slot)
    return pl.ds(pl.multiple_of((owner if own else lax.div(owner, 2)) * width, width), width)

MESH = pl.DeviceIdType.MESH
NEAR = (2, 4, 6)
PARTS = 2
GROUPS = 4


def remote(source, target, send_sem, recv_sem, axis, peer):
    return pltpu.make_async_remote_copy(
        src_ref=source,
        dst_ref=target,
        send_sem=send_sem,
        recv_sem=recv_sem,
        device_id={axis: peer},
        device_id_type=MESH,
    )


def drain(ref, sem):
    pltpu.make_async_copy(ref, ref, sem).wait()


def meet():
    own, rank = lax.axis_index("dp"), lax.axis_index("tensor")
    barrier = pltpu.get_barrier_semaphore()
    for flip in range(1, 8):
        pl.semaphore_signal(barrier, inc=1, device_id={"dp": own ^ flip}, device_id_type=MESH)

    @pl.when(rank < 3)
    def _():
        pl.semaphore_signal(barrier, inc=1, device_id={"tensor": rank + 1}, device_id_type=MESH)

    @pl.when(rank > 0)
    def _():
        pl.semaphore_signal(barrier, inc=1, device_id={"tensor": rank - 1}, device_id_type=MESH)

    pl.semaphore_wait(barrier, 8 + lax.div(rank * (3 - rank), 2))


def at_cols(ref, index, width):
    return ref.at[:, pl.ds(pl.multiple_of(index * width, width), width)]


def at_rows(ref, index, width):
    return ref.at[pl.ds(pl.multiple_of(index * width, width), width), :]


def either(rank, *choices):
    result = rank == choices[0]
    for choice in choices[1:]:
        result = result | (rank == choice)
    return result


def ends(rank):
    return either(rank, 0, 3)


def inner(rank):
    return either(rank, 1, 2)


class RowGather:
    def __init__(self, rank, source, landing, part, size, send, recv):
        self.rank = rank

        def place(slot):
            return landing.at[pl.ds(pl.multiple_of((4 * part + slot) * size, size), size), :]

        def copy(origin, slot, peer):
            return remote(origin, place(slot), send.at[part], recv.at[part, slot - 1], "tensor", peer)

        def forward(slot, target, peer):
            return copy(place(slot), target, peer)

        outward, inward = (rank - 1) * 3, 3 - rank
        near, far = 5 - 2 * rank, 2 * rank - 1
        self.up, self.down = copy(source, 1, rank + 1), copy(source, 3, rank - 1)
        self.hops = [forward(near, 2, outward), forward(far, 2, inward), forward(2, far, outward)]
        self.slots = [near, far, 2]
        self.arrival = lambda slot: copy(source, slot, lax.rem(rank + 1, 4))
        self.sent = lambda count: drain(landing.at[pl.ds(0, count * size), :], send.at[part])

    def start(self):
        pl.when(self.rank < 3)(self.up.start)
        pl.when(self.rank > 0)(self.down.start)

    def hop(self, index):
        @pl.when(inner(self.rank))
        def _():
            self.arrival(self.slots[index]).wait_recv()
            self.hops[index].start()

    def wait(self):
        @pl.when(ends(self.rank))
        def _():
            for slot in (1, 2, 3):
                self.arrival(slot).wait_recv()

    def finish(self):
        pl.when(ends(self.rank))(lambda: self.sent(1))
        pl.when(inner(self.rank))(lambda: self.sent(5))


class RowScatter:
    def __init__(self, rank, source, landing, part, size, send, recv, staged=None, sem=None):
        self.rank, self.source, self.size, self.staged, self.sem = rank, source, size, staged, sem
        self.place = lambda k: pl.ds(pl.multiple_of((4 * part + k) * size, size), size)
        self.land = lambda slot: landing.at[pl.ds((5 * part + slot) * size, size), :]

        def copy(k, slot, peer):
            return remote(source.at[self.place(k), :], self.land(slot), send.at[part], recv.at[part, slot], "tensor", peer)

        end = lax.div(rank, 3)
        self.first = [copy(index + 1 + end * (2 - 2 * index), index, 1 + end) for index in range(3)]
        self.keys = [2, 5 - 2 * rank, 2 * rank - 1]
        self.later = [
            copy(self.keys[0], 3, 3 - rank),
            copy(self.keys[1], 4, 3 - rank),
            copy(self.keys[2], 4, (rank - 1) * 3),
        ]
        self.arrival = lambda slot: copy(1, slot, lax.rem(rank + 1, 4))
        self.finish = lambda: drain(source.at[pl.ds(0, 3 * size), :], send.at[part])

    def start(self, indices=(0, 1, 2)):
        @pl.when(ends(self.rank))
        def _():
            for index in indices:
                self.first[index].start()

    def hop(self, index):
        @pl.when(inner(self.rank))
        def _():
            slot = (0, 1, 3)[index]
            self.arrival(slot).wait_recv()
            other = self.land(slot)
            if self.staged is not None:
                load = pltpu.make_async_copy(other, self.staged, self.sem)
                load.start()
                load.wait()
                other = self.staged
            target = self.source.at[self.place(self.keys[index]), :]

            @pl.loop(0, self.size // 16)
            def _(step):
                rows = pl.ds(pl.multiple_of(step * 16, 16), 16)
                target[rows, :] = (target[rows, :].astype(F32) + other[rows, :].astype(F32)).astype(BF)

            self.later[index].start()

    def wait(self):
        pl.when(inner(self.rank))(self.arrival(2).wait_recv)
        self.arrival(4).wait_recv()


def fill_mask(bias, docs, size):
    rank = lax.axis_index("tensor")
    tokens = bias.shape[0]
    values = docs[...]
    starts = [jnp.sum(jnp.where(values < number, 1, 0), keepdims=True) for number in range(1, 8)]

    def document(position):
        return sum(jnp.where(position >= start, 1, 0) for start in starts)

    lane = lax.broadcasted_iota(jnp.int32, (1, tokens), 1)
    slot = lax.rem(lax.div(lane, size), 4)
    part = lax.div(lane, 4 * size)
    keys = lax.rem(rank - slot + 4, 4) * (2 * size) + part * size + lax.rem(lane, size)
    key_docs = document(keys)

    @pl.loop(0, tokens // size)
    def _(block):
        base = lax.rem(rank - lax.rem(block, 4) + 4, 4) * (2 * size) + lax.div(block, 4) * size
        queries = base + lax.broadcasted_iota(jnp.int32, (size, 1), 0)
        allowed = (document(queries) == key_docs) & (queries >= keys)
        bias[pl.ds(pl.multiple_of(block * size, size), size), :] = jnp.where(allowed, 0.0, NEGATIVE)


def fill_turns(cosine, sine, size):
    rank = lax.axis_index("tensor")
    half_size = HEAD_DIM // 2
    dims = (size, cosine.shape[1])
    lane = lax.broadcasted_iota(jnp.int32, dims, 1)
    row = lax.broadcasted_iota(jnp.int32, dims, 0)
    frequency = jnp.exp(lax.rem(lane, half_size).astype(F32) * (-math.log(ROPE_BASE) / half_size))
    sign = jnp.where(lax.rem(lane, HEAD_DIM) < half_size, -1.0, 1.0)

    @pl.loop(0, cosine.shape[0] // size)
    def _(block):
        start = (lax.rem(rank - lax.rem(block, 4) + 4, 4) * PARTS + lax.div(block, 4)) * size
        angles = (row + start).astype(F32) * frequency
        rows = pl.ds(pl.multiple_of(block * size, size), size)
        cosine[rows, :] = jnp.cos(angles)
        sine[rows, :] = jnp.sin(angles) * sign


def slice_of(slot, width, own):
    index = lax.axis_index("dp")
    owner = index ^ (2 * slot)
    return pl.ds(pl.multiple_of((owner if own else lax.div(owner, 2)) * width, width), width)


def layer_kernel(*refs):
    hidden_in, cot_in, *plain_gains = refs[:4]
    weights_in = refs[4:11]
    docs = refs[11]
    down_parts, gate_parts, up_parts, qkv_parts, out_parts = refs[12:17]
    grad_merge = refs[17:22]
    pair_gate, pair_up, pair_qkv, pair_attended, pair_normed, pair_branch = refs[22:28]
    branch_rows, hidden_rows, normed_rows, mlp_recv, qkv_full, down_full = refs[28:34]
    layer_out, input_grad, gain_total = refs[34:37]
    gate_w, up_w, down_w, sent, cot, normed, hidden, d_gate, d_up = refs[37:46]
    two_half, cot_half, buffer_a, buffer_b, buffer_c, out_w = refs[46:52]
    qkv, attended, d_attended, bias, cosine, sine = refs[52:58]
    inverses_one, inverses, middle, grad_middle, send_part, recv_part = refs[58:64]
    gains_in, gains, gain_part, gain_recv, gain_z = refs[64:69]
    a_send, a_recv, f_send, f_recv, h_send, h_recv, z_send, z_recv, r_send, r_recv = refs[69:79]
    w_send, w_recv, d_send, d_recv, g_send, g_recv, y_send, y_recv, load, keep, down_load, s_recv, n_recv = refs[79:]

    own, rank = lax.axis_index("dp"), lax.axis_index("tensor")
    core = lax.rem(own, 2)
    tokens, dim = sent.shape
    units = gate_w.shape[1]
    tile = hidden_in.shape[0]
    size = tile // PARTS
    span = 4 * size
    heads = attended.shape[1]
    width = weights_in[0].shape[0]
    half = dim // (2 * width)
    d_qkv = cot.at[:, pl.ds(heads, 3 * heads)]
    group = units // GROUPS
    step_cols = 256
    count = dim // step_cols

    def cols_of(step, length=step_cols):
        return pl.ds(pl.multiple_of(step * length, length), length)

    def local(source, target, sem):
        return pltpu.make_async_copy(source, target, sem)

    def own_rows(part):
        return pl.ds(part * span, size)

    def part_rows(part):
        return pl.ds(part * size, size)

    def source_of(item):
        if item < 4:
            return weights_in[item]
        which, start = (item - 4) % 3, ((item - 4) // 3) * group
        if which == 2:
            return weights_in[4].at[pl.ds(start, group), :]
        return weights_in[5 + which].at[:, pl.ds(start, group)]

    def view(item, owner, part=None):
        rows = heads if item == 3 else group if item > 3 and (item - 4) % 3 == 2 else width
        length = rows if part is None else rows // 2
        start = 0 if part is None else part * length
        if item < 3:
            place = pl.ds(pl.multiple_of(owner * width + start, length), length)
            return down_w.at[place, pl.ds(item * heads, heads)]
        if item == 3:
            return out_w.at[pl.ds(start, length), pl.ds(pl.multiple_of(owner * width, width), width)]
        which, offset = (item - 4) % 3, ((item - 4) // 3) * group
        if which == 2:
            return down_full.at[pl.ds(offset + start, length), pl.ds(pl.multiple_of(owner * width, width), width)]
        place = pl.ds(pl.multiple_of(owner * width + start, length), length)
        return (gate_w, up_w)[which].at[place, pl.ds(offset, group)]

    def phase_of(item):
        return 0 if item < 3 else 1 if item == 3 else 2 + (item - 4) // 3

    def send_weight(item, flip):
        sem = s_recv.at[phase_of(item)] if flip == 1 else a_recv.at[item, flip // 2 - 1]
        return remote(source_of(item), view(item, own), a_send.at[phase_of(item)], sem, "dp", own ^ flip)

    def relay_weight(item, part):
        place = view(item, own ^ (4 - 2 * part), part)
        return remote(place, place, a_send.at[phase_of(item)], a_recv.at[item, 2], "dp", own ^ (2 + 2 * part))

    def pass_weight(item, flip):
        place = view(item, own ^ flip)
        return remote(place, place, a_send.at[phase_of(item)], s_recv.at[phase_of(item)], "dp", own ^ 1)

    def send_weights(items):
        for item in items:
            for flip in (2, 4, 1):
                send_weight(item, flip).start()

    def relay_weights(items):
        for item in items:
            send_weight(item, 4).wait_recv()
            relay_weight(item, 0).start()
            send_weight(item, 2).wait_recv()
            relay_weight(item, 1).start()
            pass_weight(item, 4).start()
            pass_weight(item, 2).start()

    def pass_weights(items):
        for item in items:
            drain(view(item, own ^ 6), a_recv.at[item, 2])
            pass_weight(item, 6).start()

    def have_weights(phase):
        drain(gate_w.at[pl.ds(0, width if phase == 1 else 3 * width), :], s_recv.at[phase])

    def sent_weights(phase):
        length = 7 * width // 4
        drain(gate_w.at[pl.ds(0, length if phase == 1 else 3 * length), :], a_send.at[phase])

    def items_of(index):
        return list(range(4 + 3 * index, 7 + 3 * index))

    def send_gain(flip):
        return remote(gains_in, at_cols(gains, own, width), y_send.at[0], y_recv.at[0], "dp", own ^ flip)

    def gathers(kind, source, landing):
        return [
            RowGather(rank, source(part), landing, part, size, z_send.at[kind], z_recv.at[kind]) for part in range(PARTS)
        ]

    gather_hidden = gathers(0, lambda part: hidden_in.at[part_rows(part), :], buffer_b)
    gather_cot = gathers(1, lambda part: cot_in.at[part_rows(part), :], cot)
    gather_sent = gathers(2, lambda part: sent.at[own_rows(part), :], sent)
    gather_branch = gathers(3, lambda part: sent.at[own_rows(part), :], branch_rows)

    def scatters(kind, source, landing, staged=None, sem=None):
        return [
            RowScatter(rank, source, landing, part, size, r_send.at[kind], r_recv.at[kind], staged, sem)
            for part in range(PARTS)
        ]

    gate_stage = up_w.at[pl.ds(4 * width, size), :]
    out_scatter = scatters(0, send_part, recv_part)
    two_scatter = scatters(1, send_part, recv_part)
    mlp_scatter = scatters(2, sent, mlp_recv, gate_stage, load.at[3])
    one_scatter = scatters(3, send_part, recv_part)

    def arrived(part, slot):
        return pl.ds((5 * part + slot) * size, size)

    def clear(part):
        @pl.when(ends(rank))
        def _():
            recv_part[arrived(part, 2), :] = jnp.zeros((size, dim), BF)

    def received(part, start, length, base):
        total = base
        for slot in (2, 4):
            rows = pl.ds(pl.multiple_of((5 * part + slot) * size + start, length), length)
            total = total + recv_part[rows, :].astype(F32)
        return total

    def to_pair(source, target, row, slot):
        return remote(source, target, h_send.at[row], h_recv.at[row], "dp", own ^ 1)

    def halves(source, target, row):
        return [
            to_pair(at_cols(source, 2 * slot + 1 - core, width), at_cols(target, slot, width), row, slot)
            for slot in range(half)
        ]

    def send_ff(step, which):
        cols = cols_of(step)
        source = (hidden, d_gate, d_up)[which].at[:, cols]
        target = (buffer_a, pair_gate, pair_up)[which].at[:, cols]
        arrival = lax.div(step, group // step_cols) if which == 0 else GROUPS - 1 + which
        return remote(source, target, f_send.at[which], f_recv.at[arrival], "dp", own ^ 1)

    def piece(index, slot):
        if index < 3:
            return at_rows(gate_w, (index - 1) * 4 + slot, width)
        if index == 3:
            return (hidden, d_gate)[slot // 2].at[pl.ds((slot % 2) * width, width), pl.ds(0, 3 * heads)]
        return at_cols(d_up, slot, width)

    def landing_of(index, slot):
        ref = (down_parts, gate_parts, up_parts, qkv_parts, out_parts)[index]
        return at_cols(ref, slot, width) if index == 4 else at_rows(ref, slot, width)

    def half_of(ref, index, part):
        rows, cols = ref.shape
        if index == 4:
            return ref.at[pl.ds(part * (rows // 2), rows // 2), :]
        return ref.at[:, pl.ds(part * (cols // 2), cols // 2)]

    def stage_of(index, part):
        if index == 4:
            return up_w.at[pl.ds(7 * width, heads // 2), pl.ds(part * width, width)]
        length = units // 2 if index < 3 else 3 * heads // 2
        return up_w.at[pl.ds((3 + index) * width, width), pl.ds(part * (units // 2), length)]

    def send_far(index, part):
        return remote(
            half_of(piece(index, 3), index, part),
            half_of(grad_merge[index], index, part),
            w_send.at[index - 1],
            w_recv.at[index - 1, part],
            "dp",
            own ^ (2 + 2 * part),
        )

    def send_near(index, slot, part):
        return remote(
            half_of(piece(index, slot), index, part),
            half_of(landing_of(index, slot), index, part),
            w_send.at[index - 1],
            n_recv.at[index - 1],
            "dp",
            own ^ (2 * slot),
        )

    def keep_grad(index):
        return local(piece(index, 0), landing_of(index, 0), keep.at[index])

    def merge_grads(index):
        loads = [local(half_of(grad_merge[index], index, part), stage_of(index, part), load.at[part]) for part in range(2)]
        for part in range(2):
            send_far(index, part).wait_recv()
            loads[part].start()
        for part in range(2):
            loads[part].wait()
            target, source = half_of(piece(index, 2 - part), index, part), stage_of(index, part)
            length = source.shape[0] // 4

            @pl.loop(0, 4)
            def _(step):
                rows = cols_of(step, length)
                target[rows, :] = (target[rows, :].astype(F32) + source[rows, :].astype(F32)).astype(BF)

            send_near(index, 2 - part, part).start()

    def row_grads(index, slot, left, left_pair, right, right_pair, columns):
        mine, theirs = slice_of(slot, width, True), slice_of(slot, width, False)
        turned, turned_pair = jnp.transpose(left[:, mine]), jnp.transpose(left_pair[:, theirs])
        target = piece(index, slot)

        @pl.loop(0, columns // 512)
        def _(step):
            cols = cols_of(step, 512)
            total = dot(turned, right[:, cols]) + dot(turned_pair, right_pair[:, cols])
            target[:, cols] = total.astype(BF)

        if slot == 3:
            send_far(index, 0).start()
            send_far(index, 1).start()
        elif slot == 0:
            keep_grad(index).start()
        else:
            send_near(index, slot, slot - 1).start()

    def out_grads():
        for part in range(2):
            rows = pl.ds(part * (heads // 2), heads // 2)
            turned, turned_pair = jnp.transpose(attended[:, rows]), jnp.transpose(cot[:, rows])
            for slot in range(4):
                mine, theirs = slice_of(slot, width, True), slice_of(slot, width, False)
                total = dot(turned, buffer_a[:, mine]) + dot(turned_pair, cot_half[:, theirs])
                piece(4, slot)[rows, :] = total.astype(BF)
            send_far(4, part).start()
            send_near(4, part + 1, part).start()
        keep_grad(4).start()

    def down_piece(slot, index, part=None):
        cols = pl.ds(((slot % 2) * GROUPS + index) * width, width)
        rows = pl.ds(0, group) if part is None else pl.ds(part * (group // 2), group // 2)
        return (buffer_b, buffer_c)[slot // 2].at[rows, cols]

    def down_rows(ref, index, slot, part=None):
        rows = pl.ds(index * group, group) if part is None else pl.ds(index * group + part * (group // 2), group // 2)
        return ref.at[rows, pl.ds(slot * width, width)]

    def send_down(kind, index, part):
        if kind == 0:
            target, source = down_rows(grad_merge[0], index, 0, part), down_piece(3, index, part)
            peer = own ^ (2 + 2 * part)
        else:
            target, source = down_rows(down_parts, index, kind, part), down_piece(kind, index, part)
            peer = own ^ (2 * kind)
        return remote(source, target, d_send.at[0], d_recv.at[GROUPS if kind else index], "dp", peer)

    def keep_down(index):
        return local(down_piece(0, index), down_rows(down_parts, index, 0), keep.at[8 + index])

    def down_grads(index):
        drain(buffer_a.at[:, pl.ds(index * group, group)], f_recv.at[index])

        @pl.loop(0, group // 256)
        def _(step):
            cols = pl.ds(pl.multiple_of(index * group + step * 256, 256), 256)
            rows = pl.ds(pl.multiple_of(step * 256, 256), 256)
            turned, turned_pair = jnp.transpose(hidden[:, cols]), jnp.transpose(buffer_a[:, cols])
            for slot in range(4):
                mine, theirs = slice_of(slot, width, True), slice_of(slot, width, False)
                total = dot(turned, cot[:, mine]) + dot(turned_pair, cot_half[:, theirs])
                down_piece(slot, index)[rows, :] = total.astype(BF)

        for part in range(2):
            send_down(0, index, part).start()
        for part in range(2):
            send_down(1 + part, index, part).start()
        keep_down(index).start()

    def merge_down(indices):
        entries = [(index, part) for index in indices for part in range(2)]

        def stage(index, part):
            rows = pl.ds(part * (group // 2), group // 2)
            return d_attended.at[rows, pl.ds((index % 2) * width, width)]

        loads = [
            local(down_rows(grad_merge[0], index, 0, part), stage(index, part), load.at[2 * (index % 2) + part])
            for index, part in entries
        ]
        for index in indices:
            drain(down_rows(grad_merge[0], index, 0), d_recv.at[index])
        start_all(loads)
        for copy, (index, part) in zip(loads, entries):
            copy.wait()
            target, source = down_piece(2 - part, index, part), stage(index, part)

            @pl.loop(0, 2)
            def _(step):
                rows = cols_of(step, group // 4)
                target[rows, :] = (target[rows, :].astype(F32) + source[rows, :].astype(F32)).astype(BF)

            send_down(2 - part, index, part).start()

    def norm_back(total, values, gain):
        inverse = lax.rsqrt(jnp.mean(values * values, axis=-1, keepdims=True) + EPSILON)
        scaled = total * gain
        return inverse * (scaled - values * inverse * inverse * jnp.mean(scaled * values, axis=-1, keepdims=True))

    meet()
    for gather in gather_hidden:
        gather.start()
    gains_in[...] = jnp.zeros(gains_in.shape, F32)
    for index, plain in enumerate(plain_gains):
        gains_in[index : index + 1, :] = plain[...].astype(F32).reshape(1, width)
    send_weights(range(3))
    for flip in range(1, 8):
        send_gain(flip).start()
    stage_down = down_w.at[:, pl.ds(3 * heads, width)]
    stage_in = local(weights_in[4], stage_down, load.at[0])
    own_loads = [local(gains_in, at_cols(gains, own, width), load.at[1])]
    own_loads += [local(weights_in[item], view(item, own), load.at[2 + item]) for item in range(4)]
    own_loads += [local(weights_in[5], at_rows(gate_w, own, width), load.at[6])]
    own_loads += [local(weights_in[6], at_rows(up_w, own, width), load.at[7])]
    for part in range(PARTS):
        own_loads.append(local(hidden_in.at[part_rows(part), :], buffer_b.at[own_rows(part), :], load.at[8 + part]))
        own_loads.append(local(cot_in.at[part_rows(part), :], cot.at[own_rows(part), :], load.at[10 + part]))
    start_all([stage_in] + own_loads)
    fill_mask(bias, docs, size)
    fill_turns(cosine, sine, size)
    for part in range(PARTS):
        clear(part)
    relay_weights([0])
    gather_hidden[0].hop(0)
    gather_hidden[0].hop(1)
    relay_weights([1])
    gather_hidden[1].hop(0)
    gather_hidden[1].hop(1)
    gather_hidden[0].hop(2)
    relay_weights([2])
    send_weights([3, 4])
    gather_hidden[1].hop(2)
    for gather in gather_cot:
        gather.start()
    stage_in.wait()
    stage_out = local(stage_down, at_cols(down_full, own, width), keep.at[5])
    stage_out.start()
    wait_all(own_loads)
    drain(gain_recv.at[pl.ds(0, 56), :], y_recv.at[0])
    gather_cot[0].hop(1)
    gather_cot[0].hop(0)
    pass_weights(range(3))
    relay_weights([3])
    send_weights(range(5, 4 + 3 * GROUPS))
    for gather in gather_hidden:
        gather.wait()

    norm_rows(buffer_b, buffer_c, inverses_one, gains.at[pl.ds(0, 1), :], 64)
    keep_hidden = local(buffer_b, hidden_rows, keep.at[0])
    keep_normed = local(buffer_c, normed_rows, keep.at[1])
    start_all([keep_hidden, keep_normed])
    have_weights(0)
    qkv_w = down_w.at[:, pl.ds(0, 3 * heads)]
    keep_qkv = local(qkv_w, qkv_full, keep.at[2])
    keep_qkv.start()

    @pl.loop(0, 2 * heads // step_cols)
    def _(step):
        cols = cols_of(step)
        product = dot(buffer_c[...], down_w[:, cols])
        turns = [jnp.concatenate([table[...]] * (step_cols // 128), axis=1) for table in (cosine, sine)]
        qkv[:, cols] = turn(product, *turns).astype(BF)

    @pl.loop(2 * heads // step_cols, 3 * heads // step_cols)
    def _(step):
        cols = cols_of(step)
        qkv[:, cols] = dot(buffer_c[...], down_w[:, cols]).astype(BF)

    attend(qkv, attended, bias, heads)
    gather_cot[0].hop(2)
    gather_cot[1].hop(1)
    gather_cot[1].hop(0)
    pass_weights([3])
    have_weights(1)

    def make_out(part):
        @pl.loop(0, count)
        def _(step):
            cols = cols_of(step)
            product = dot(attended[part * span : (part + 1) * span, :], out_w[:, cols])
            middle[part_rows(part), cols] = product[:size, :]
            send_part[pl.ds(part * span + size, span - size), cols] = product[size:, :].astype(BF)

    make_out(0)
    out_scatter[0].start()
    make_out(1)
    out_scatter[1].start()
    gather_cot[1].hop(2)
    wait_all([keep_hidden, keep_normed, keep_qkv, stage_out])
    send_normed = halves(normed_rows, pair_normed, 1)
    send_attended = to_pair(attended, pair_attended, 2, 0)
    start_all(send_normed + [send_attended])
    for index in range(3):
        out_scatter[0].hop(index)
    relay_weights(items_of(0))

    def make_sent(part):
        out_scatter[part].wait()

        @pl.loop(0, size // 32)
        def _(step):
            rows = pl.ds(pl.multiple_of(part * size + step * 32, 32), 32)
            place = pl.ds(pl.multiple_of(part * span + step * 32, 32), 32)
            total = received(part, step * 32, 32, hidden_of(place) + middle[rows, :])
            middle[rows, :] = total
            sent[place, :] = total.astype(BF)

        gather_sent[part].start()

    def hidden_of(place):
        return buffer_b[place, :].astype(F32)

    make_sent(0)
    out_scatter[1].hop(0)
    relay_weights(items_of(1))
    gather_sent[0].hop(0)
    out_scatter[1].hop(1)
    out_scatter[1].hop(2)
    make_sent(1)
    gather_sent[0].hop(1)
    relay_weights(items_of(2))
    gather_sent[1].hop(0)
    gather_sent[1].hop(1)
    gather_sent[0].hop(2)
    gather_sent[1].hop(2)
    relay_weights(items_of(3))

    def load_down(index):
        rows = pl.ds(index * group, group)
        return local(down_full.at[rows, :], down_w.at[rows, :], down_load.at[index])

    for gather in gather_cot:
        gather.wait()
    send_cot = halves(cot, cot_half, 0)
    start_all(send_cot)
    for gather in gather_sent:
        gather.wait()
    norm_rows(sent, normed, inverses, gains.at[pl.ds(1, 1), :], 64)
    pass_weights(items_of(0))
    send_two = halves(normed, two_half, 3)
    start_all(send_two)
    have_weights(2)
    for phase in range(2):
        sent_weights(phase)
    for gather in gather_hidden:
        gather.finish()
    load_down(0).start()
    for index in range(GROUPS):
        load_down(index).wait()
        if index + 1 < GROUPS:
            pass_weights(items_of(index + 1))

        @pl.loop(index * group // step_cols, (index + 1) * group // step_cols)
        def _(step):
            cols = cols_of(step)
            gate = dot(normed[...], gate_w[:, cols])
            up = dot(normed[...], up_w[:, cols])
            d_hidden = dot_rows(cot[...], down_w[cols, :])
            s = jax.nn.sigmoid(gate)
            activated = gate * s
            hidden[:, cols] = (activated * up).astype(BF)
            d_gate[:, cols] = (d_hidden * up * (s + activated * (1.0 - s))).astype(BF)
            d_up[:, cols] = (d_hidden * activated).astype(BF)
            for which in range(3):
                send_ff(step, which).start()

        if index + 1 < GROUPS:
            have_weights(3 + index)
            load_down(index + 1).start()
        if index == 0:
            drain(cot_half, h_recv.at[0])
        else:
            down_grads(index - 1)

    gain_part[...] = jnp.zeros(gain_part.shape, F32)
    for part in range(PARTS):
        out_scatter[part].finish()

    def make_two(part):
        block = slice(part * span, (part + 1) * span)

        @pl.loop(0, count)
        def _(step):
            cols = cols_of(step)
            product = dot_rows(d_gate[block, :], gate_w[cols, :]) + dot_rows(d_up[block, :], up_w[cols, :])
            gain_part[pl.ds(1, 1), cols] += jnp.sum(
                product * (sent[block, cols].astype(F32) * inverses[block, :]), axis=0, keepdims=True
            )
            grad_middle[part_rows(part), cols] = product[:size, :]
            send_part[pl.ds(part * span + size, span - size), cols] = product[size:, :].astype(BF)

    make_two(0)
    two_scatter[0].start()
    down_grads(GROUPS - 1)
    merge_down((0, 1))
    make_two(1)
    two_scatter[0].hop(0)
    two_scatter[1].start()
    for phase in range(2, 2 + GROUPS):
        sent_weights(phase)
    for which in (1, 2):
        drain((d_gate, d_up)[which - 1], f_recv.at[GROUPS - 1 + which])
    gate_pair, up_pair = up_w.at[pl.ds(0, tokens), :], up_w.at[pl.ds(tokens, tokens), :]
    pair_loads = [local(pair_gate, gate_pair, load.at[0]), local(pair_up, up_pair, load.at[1])]
    start_all(pair_loads)
    drain(two_half, h_recv.at[3])
    wait_all(pair_loads)
    gate_grads = lambda slot: row_grads(1, slot, normed, two_half, d_gate, gate_pair, units)
    up_grads = lambda slot: row_grads(2, slot, normed, two_half, d_up, up_pair, units)
    gate_grads(3)
    merge_down((2, 3))
    two_scatter[0].hop(1)
    two_scatter[0].hop(2)
    for slot in (1, 2, 0):
        gate_grads(slot)

    def make_branch(part):
        two_scatter[part].wait()

        @pl.loop(0, size // 32)
        def _(step):
            rows = pl.ds(pl.multiple_of(part * size + step * 32, 32), 32)
            place = pl.ds(pl.multiple_of(part * span + step * 32, 32), 32)
            total = received(part, step * 32, 32, grad_middle[rows, :])
            result = cot[place, :].astype(F32) + norm_back(total, sent[place, :].astype(F32), gains[1:2, :])
            grad_middle[rows, :] = result
            sent[place, :] = result.astype(BF)

        gather_branch[part].start()
        keep_branch[part].start()

    keep_branch = [
        local(sent.at[own_rows(part), :], branch_rows.at[own_rows(part), :], keep.at[6 + part]) for part in range(PARTS)
    ]
    for part in range(PARTS):
        gather_sent[part].finish()
    make_branch(0)
    up_grads(3)
    two_scatter[1].hop(0)
    up_grads(1)
    gather_branch[0].hop(0)
    two_scatter[1].hop(1)
    two_scatter[1].hop(2)
    up_grads(2)
    up_grads(0)
    def project(first, last):
        @pl.loop(first, last)
        def _(step):
            cols = cols_of(step)
            product = dot(hidden[...], down_w[:, cols])
            for part in range(PARTS):
                start = part * span
                middle[part_rows(part), cols] = middle[part_rows(part), cols] + product[start : start + size, :]
                sent[pl.ds(start + size, span - size), cols] = product[start + size : start + span, :].astype(BF)

    pl.when(ends(rank))(lambda: project(0, count))
    mlp_scatter[0].start((0,))
    make_branch(1)
    mlp_scatter[0].start((1, 2))
    mlp_scatter[1].start()
    pl.when(inner(rank))(lambda: project(0, count // 4))
    gather_branch[0].hop(1)
    merge_grads(1)
    pl.when(inner(rank))(lambda: project(count // 4, count // 2))
    gather_branch[1].hop(0)
    pl.when(inner(rank))(lambda: project(count // 2, count))
    gather_branch[1].hop(1)
    gather_branch[0].hop(2)
    gather_branch[1].hop(2)
    load_weight = local(qkv_full, qkv_w, load.at[4])
    load_hidden = local(hidden_rows, gate_pair, load.at[5])
    load_normed = local(normed_rows, up_pair, load.at[6])
    start_all([load_hidden, load_normed])
    mlp_scatter[0].hop(0)
    merge_grads(2)
    for part in range(PARTS):
        two_scatter[part].finish()
        gather_branch[part].wait()
        keep_branch[part].wait()

    load_branch = local(branch_rows, buffer_a, load.at[7])
    load_branch.start()
    load_weight.start()
    send_half = halves(branch_rows, pair_branch, 4)
    start_all(send_half)
    mlp_scatter[0].hop(1)
    load_branch.wait()

    @pl.loop(0, heads // step_cols)
    def _(step):
        cols = cols_of(step)
        d_attended[:, cols] = dot_rows(buffer_a[...], out_w[cols, :]).astype(BF)

    drain(cot_half, h_send.at[0])
    for gather in gather_cot:
        gather.finish()
    drain(two_half, h_recv.at[1])
    send_attended.wait_recv()
    early_loads = [
        local(pair_attended, cot.at[:, pl.ds(0, heads)], load.at[8]),
        local(pair_normed, two_half, load.at[9]),
    ]
    start_all(early_loads)
    attend_back(qkv, d_attended, d_qkv, bias, cosine, sine, heads)
    send_qkv = to_pair(d_qkv, pair_qkv, 5, 0)
    send_qkv.start()
    for which in range(3):
        drain((hidden, d_gate, d_up)[which], f_send.at[which])

    drain(cot_half, h_recv.at[4])
    load_half = local(pair_branch, cot_half, load.at[10])
    load_half.start()
    mlp_scatter[0].hop(2)
    mlp_scatter[1].hop(0)
    wait_all([load_weight, load_hidden, load_normed])

    def make_one(part):
        block = slice(part * span, (part + 1) * span)

        @pl.loop(0, count)
        def _(step):
            cols = cols_of(step)
            product = dot_rows(d_qkv[block, :], down_w[cols, pl.ds(0, 3 * heads)])
            gain_part[pl.ds(0, 1), cols] += jnp.sum(
                product * (gate_pair[block, cols].astype(F32) * inverses_one[block, :]), axis=0, keepdims=True
            )
            input_grad[part_rows(part), cols] = product[:size, :]
            send_part[pl.ds(part * span + size, span - size), cols] = product[size:, :].astype(BF)

        one_scatter[part].start()

    def share_gain(flip):
        source = at_cols(gain_part, own ^ flip, width)
        return remote(source, at_rows(gain_recv, flip, 8), g_send.at[0], g_recv.at[0], "dp", own ^ flip)

    make_one(0)
    mlp_scatter[1].hop(1)

    send_qkv.wait_recv()
    drain(two_half, h_send.at[3])
    load_qkv = local(pair_qkv, normed.at[:, pl.ds(0, 3 * heads)], load.at[0])
    load_qkv.start()
    for index in range(1, 3):
        keep_grad(index).wait()
    wait_all(early_loads + [load_half])
    out_grads()
    mlp_scatter[1].hop(2)
    load_qkv.wait()
    for slot in (3, 1, 2, 0):
        row_grads(3, slot, up_pair, two_half, d_qkv, normed, 3 * heads)
        if slot == 2:
            one_scatter[0].hop(0)
            make_one(1)
    for flip in range(1, 8):
        share_gain(flip).start()
    one_scatter[0].hop(1)
    one_scatter[0].hop(2)
    merge_grads(4)
    one_scatter[1].hop(0)
    merge_grads(3)
    one_scatter[1].hop(1)
    one_scatter[1].hop(2)

    drain(gain_recv.at[pl.ds(8, 56), :], g_recv.at[0])
    gain_sum = gain_part[:, pl.ds(pl.multiple_of(own * width, width), width)]
    for flip in range(1, 8):
        gain_sum = gain_sum + gain_recv[pl.ds(flip * 8, 8), :]
    gain_z[pl.ds(0, 8), :] = gain_sum

    def share_gain_z(k):
        target = gain_z.at[pl.ds(8 * k, 8), :]
        return remote(gain_z.at[pl.ds(0, 8), :], target, y_send.at[1], y_recv.at[1], "tensor", lax.rem(rank + k, 4))

    for k in (1, 2, 3):
        share_gain_z(k).start()

    load_own = [
        local(hidden_in.at[part_rows(part), :], sent.at[own_rows(part), :], load.at[4 + part]) for part in range(PARTS)
    ]
    for part in range(PARTS):
        gather_branch[part].finish()
    start_all(load_own)
    wait_all(load_own)
    for part in range(PARTS):
        one_scatter[part].wait()

        @pl.loop(0, size // 32)
        def _(step):
            rows = pl.ds(pl.multiple_of(part * size + step * 32, 32), 32)
            place = pl.ds(pl.multiple_of(part * span + step * 32, 32), 32)
            total = received(part, step * 32, 32, input_grad[rows, :])
            input_grad[rows, :] = grad_middle[rows, :] + norm_back(total, sent[place, :].astype(F32), gains[0:1, :])

    for scatter in mlp_scatter:
        scatter.wait()
    load_mlp = [
        [local(mlp_recv.at[arrived(part, slot), :], recv_part.at[arrived(part, slot), :], load.at[2 * part + index])
         for index, slot in enumerate((4, 2))]
        for part in range(PARTS)
    ]
    for part in range(PARTS):
        load_mlp[part][0].start()
        pl.when(inner(rank))(load_mlp[part][1].start)
    for part in range(PARTS):
        load_mlp[part][0].wait()
        pl.when(inner(rank))(load_mlp[part][1].wait)

        @pl.loop(0, size // 32)
        def _(step):
            rows = pl.ds(pl.multiple_of(part * size + step * 32, 32), 32)
            layer_out[rows, :] = received(part, step * 32, 32, middle[rows, :]).astype(BF)

    drain(gain_z.at[pl.ds(8, 24), :], y_recv.at[1])
    gain_all = gain_z[pl.ds(0, 8), :]
    for k in (1, 2, 3):
        gain_all = gain_all + gain_z[pl.ds(8 * k, 8), :]
    gain_total[...] = gain_all

    for scatter in mlp_scatter + one_scatter:
        scatter.finish()
    for index in range(GROUPS):
        keep_down(index).wait()
    drain(gate_w.at[pl.ds(0, units // 4), :], d_recv.at[GROUPS])
    drain(gate_w.at[pl.ds(0, 3 * units // 8), :], d_send.at[0])
    drain(gain_recv.at[pl.ds(8, 56), :], y_send.at[0])
    drain(gain_recv.at[pl.ds(8, 56), :], g_send.at[0])
    drain(gain_z.at[pl.ds(8, 24), :], y_send.at[1])
    drain(two_half, h_send.at[1])
    drain(two_half, h_send.at[4])
    send_attended.wait_send()
    send_qkv.wait_send()
    def pieces(index, number):
        rows = number * width if index < 4 else number * heads * width // dim
        return gate_w.at[pl.ds(0, rows), pl.ds(0, 3 * heads if index == 3 else dim)]

    for index in range(1, 5):
        drain(pieces(index, 2), n_recv.at[index - 1])
        if index > 2:
            keep_grad(index).wait()
        drain(pieces(index, 3), w_send.at[index - 1])


def layer(hidden_in, cot, gains, weights, docs):
    tile, dim = hidden_in.shape
    tokens = 4 * tile
    width, heads = weights[0].shape
    units = weights[5].shape[1]
    dma = pltpu.SemaphoreType.DMA
    rows, narrow, ff = shape((tokens, dim), BF), shape((tokens, dim // 2), BF), shape((tokens, units), BF)
    weights_shape = [(units, width), (width, units), (width, units), (width, 3 * heads), (heads, width)]
    parts_shape = [(units, 3 * width), (3 * width, units), (3 * width, units), (3 * width, 3 * heads), (heads, 3 * width)]
    outs = [shape(dims, BF) for dims in parts_shape + weights_shape]
    outs += [ff] * 2 + [shape((tokens, 3 * heads), BF), shape((tokens, heads), BF), narrow, narrow]
    outs += [rows] * 3 + [shape((5 * tile, dim), BF), shape((dim, 3 * heads), BF), shape((units, dim), BF)]
    in_hbm = len(outs)
    outs += [shape((tile, dim), BF), shape((tile, dim), F32), shape((8, width), F32)]
    items = 4 + 3 * GROUPS
    scratch = [((dim, units), BF), ((dim, units), BF), ((units, dim), BF)]
    scratch += [((tokens, dim), BF)] * 3 + [((tokens, units), BF)] * 3
    scratch += [((tokens, dim // 2), BF)] * 2 + [((tokens, dim), BF)] * 3 + [((heads, dim), BF)]
    scratch += [((tokens, 3 * heads), BF)] + [((tokens, heads), BF)] * 2
    scratch += [((tokens, tokens), F32), ((tokens, 128), F32), ((tokens, 128), F32)]
    scratch += [((tokens, 1), F32), ((tokens, 1), F32), ((tile, dim), F32), ((tile, dim), F32)]
    scratch += [((tokens, dim), BF), ((5 * tile, dim), BF)]
    scratch += [((8, width), F32), ((8, dim), F32), ((8, dim), F32), ((64, width), F32), ((32, width), F32)]
    sems = [(2 + GROUPS,), (items, 3), (3,), (GROUPS + 2,), (6,), (6,)]
    sems += [(4, PARTS), (4, PARTS, 3), (4, PARTS), (4, PARTS, 5), (4,), (4, 2), (1,), (GROUPS + 1,)]
    sems += [(1,), (1,), (2,), (2,), (12,), (8 + GROUPS,), (GROUPS,), (2 + GROUPS,), (4,)]
    return pl.pallas_call(
        layer_kernel,
        out_shape=outs,
        in_specs=[anyspace()] * 2 + [vmem()] * 2 + [anyspace()] * 7 + [vmem()],
        out_specs=[anyspace()] * in_hbm + [vmem()] * 3,
        scratch_shapes=[pltpu.VMEM(*entry) for entry in scratch] + [dma(entry) for entry in sems],
        compiler_params=pltpu.CompilerParams(vmem_limit_bytes=67000000, collective_id=0, has_side_effects=True),
        cost_estimate=cost(2 * tokens * dim * units * 12, 100e6),
        name="layer",
    )(hidden_in, cot, *gains, *weights, docs)


def sum_kernel(count, *refs):
    parts, plain_in = refs[:5], refs[5:7]
    down, gate, up, query, key, value, out, *plain_out = refs[7:16]
    staged, totals, plain, load, store = refs[16:21], refs[21:26], refs[26:28], refs[28], refs[29]
    loads = [pltpu.make_async_copy(parts[index], staged[index], load.at[index]) for index in range(5)]
    loads += [pltpu.make_async_copy(plain_in[index], plain[index], load.at[5 + index]) for index in range(2)]
    start_all(loads)
    heads = query.shape[1]
    stores = [pltpu.make_async_copy(totals[index], ref, store.at[index]) for index, ref in enumerate((down, gate, up))]
    qkv_stores = [
        pltpu.make_async_copy(totals[3].at[:, pl.ds(index * heads, heads)], ref, store.at[3 + index])
        for index, ref in enumerate((query, key, value))
    ]
    out_store = pltpu.make_async_copy(totals[4], out, store.at[6])
    plain_stores = [pltpu.make_async_copy(plain[index], plain_out[index], store.at[7 + index]) for index in range(2)]
    groups = [[stores[0]], [stores[1]], [stores[2]], qkv_stores, [out_store]]
    for index in range(5):
        loads[index].wait()
        rows_first = index in (1, 2, 3)
        rows, cols = totals[index].shape
        step_rows = 32 if rows_first else 256

        @pl.loop(0, rows // step_rows)
        def _(step):
            start = pl.multiple_of(step * step_rows, step_rows)
            total = None
            for slot in range(count):
                if rows_first:
                    term = staged[index][pl.ds(pl.multiple_of(start + slot * rows, step_rows), step_rows), :]
                else:
                    term = staged[index][pl.ds(start, step_rows), slot * cols : (slot + 1) * cols]
                term = term.astype(F32)
                total = term if total is None else total + term
            totals[index][pl.ds(start, step_rows), :] = total

        start_all(groups[index])
    for index in range(2):
        loads[5 + index].wait()
        plain_stores[index].start()
    for entry in groups + [plain_stores]:
        wait_all(entry)


def sum_grads(parts, plain, heads, count):
    dims = [part.shape for part in parts]
    sums = [
        (rows // count, cols) if index in (1, 2, 3) else (rows, cols // count) for index, (rows, cols) in enumerate(dims)
    ]
    outs = sums[:3] + [(sums[3][0], heads)] * 3 + [sums[4]]
    dma = pltpu.SemaphoreType.DMA
    return pl.pallas_call(
        partial(sum_kernel, count),
        out_shape=[shape(dim, F32) for dim in outs] + [shape(entry.shape, entry.dtype) for entry in plain],
        in_specs=[anyspace()] * 7,
        out_specs=[anyspace()] * 9,
        scratch_shapes=[pltpu.VMEM(dim, BF) for dim in dims]
        + [pltpu.VMEM(dim, F32) for dim in sums]
        + [pltpu.VMEM(entry.shape, entry.dtype) for entry in plain]
        + [dma((7,)), dma((9,))],
        compiler_params=params(),
        cost_estimate=cost(1e6, 22e6),
        name="sum_grads",
    )(*parts, *plain)


def shift(values, step):
    size = lax.axis_size("tensor")
    return lax.ppermute(values, "tensor", [(index, (index + step) % size) for index in range(size)])


def gather_rows(values):
    return [values] + [shift(values, step) for step in range(1, lax.axis_size("tensor"))]


def scatter_rows(parts):
    total = parts[0].astype(F32)
    for step in range(1, len(parts)):
        total = total + shift(parts[step], -step).astype(F32)
    return total


def gather_weight(values, axis):
    return [None], [lax.all_gather(values, "dp", axis=axis, tiled=True)]


def scatter_full(left, right, axis):
    full = dot_cols(left, right).astype(BF)
    return lax.psum_scatter(full, "dp", scatter_dimension=axis, tiled=True).astype(F32)


def frequencies():
    half_size = HEAD_DIM // 2
    return ROPE_BASE ** (-jnp.arange(half_size, dtype=F32) / half_size)


def rotary(length):
    angles = jnp.arange(length).astype(F32)[:, None] * frequencies()[None, :]
    cosine, sine = jnp.cos(angles), jnp.sin(angles)
    cosine = jnp.tile(cosine, (1, 8))
    sine = jnp.tile(jnp.concatenate([-sine, sine], axis=1), (1, 4))
    return cosine, sine


def position_tables(doc_ids, ranks):
    length = doc_ids.shape[0]
    token_index = jnp.arange(length, dtype=jnp.int32)
    before = jnp.concatenate([doc_ids[:1] - 1, doc_ids[:-1]])
    doc_start = lax.cummax(jnp.where(doc_ids != before, token_index, 0), axis=0)
    order = (lax.axis_index("tensor") - jnp.arange(ranks)) % ranks
    last = token_index.reshape(ranks, -1)[order].reshape(length)
    first = doc_start.reshape(ranks, -1)[order].reshape(length)
    cosine, sine = (table.reshape(ranks, -1, 256)[order].reshape(length, 256) for table in rotary(length))
    return cosine, sine, first[:, None], last[:, None], last[None, :]


def rms_back(grad_rows_, values, gain):
    inverse = lax.rsqrt(jnp.mean(values * values, axis=-1, keepdims=True) + EPSILON)
    scaled = grad_rows_ * gain
    return inverse * (scaled - values * inverse * inverse * jnp.mean(scaled * values, axis=-1, keepdims=True))


def body(
    hidden_in,
    out_cotangent,
    doc_ids,
    attn_gain,
    query_weight,
    key_weight,
    value_weight,
    out_weight,
    mlp_gain,
    gate_weight,
    up_weight,
    down_weight,
):
    ranks, groups = lax.axis_size("tensor"), lax.axis_size("dp")
    paired = (groups, ranks) == (8, 4)
    width, heads = query_weight.shape
    dim = hidden_in.shape[1]

    if paired:
        weights = (query_weight, key_weight, value_weight, out_weight, down_weight, gate_weight, up_weight)
        outs = layer(hidden_in, out_cotangent, (attn_gain, mlp_gain), weights, doc_ids.reshape(ranks, -1))
        sums = sum_grads(outs[:5], outs[-3:-1], heads, 3)
        down_grad, gate_grad, up_grad, query_grad, key_grad, value_grad, out_proj_grad, layer_out, input_grad = sums
        gain_total = outs[-1]
        share = width // ranks
        gain_grads = lax.dynamic_slice_in_dim(gain_total, lax.axis_index("tensor") * share, share, axis=1)
    else:
        tables = position_tables(doc_ids, ranks)
        input_local = hidden_in.astype(F32)
        hidden_rows = gather_rows(hidden_in)
        gains = lax.all_gather(jnp.stack([attn_gain, mlp_gain]), "dp", axis=1, tiled=True).astype(F32)
        attn_scale, mlp_scale = gains[:1], gains[1:]
        qkv_weight = jnp.concatenate([query_weight, key_weight, value_weight], axis=1)
        tags, qkv_pieces = gather_weight(qkv_weight, 0)
        tags, out_pieces = gather_weight(out_weight, 1)
        cot_rows = gather_rows(out_cotangent)
        tags, down_pieces = gather_weight(down_weight, 1)
        tags, gate_pieces = gather_weight(gate_weight, 0)
        tags, up_pieces = gather_weight(up_weight, 0)
        normed, qkv, attended, inverses, *branch_parts = attn_fwd(
            hidden_rows, attn_scale, tables, tags, width, qkv_pieces, out_pieces
        )
        middle = input_local + scatter_rows(branch_parts)
        sent = middle.astype(BF)
        sent_rows = gather_rows(sent)
        cot_full = jnp.concatenate(cot_rows, axis=0)
        normed_two, hidden, d_gate, d_up, mlp_gain_part, *two_parts = mlp(
            sent_rows, cot_rows, mlp_scale, tags, width, gate_pieces, up_pieces, down_pieces, ranks
        )
        grad_two_rows = scatter_rows(two_parts)
        grad_middle = out_cotangent.astype(F32) + rms_back(grad_two_rows, sent.astype(F32), mlp_scale)
        branch_rows = gather_rows(grad_middle.astype(BF))
        down_grad = scatter_full(hidden, cot_full, 1)
        gate_grad = scatter_full(normed_two, d_gate, 0)
        up_grad = scatter_full(normed_two, d_up, 0)
        mlp_rows = scatter_rows(mlp_out(hidden, ranks, dim, tags, width, down_pieces))
        layer_out = (middle + mlp_rows).astype(BF)
        branch_full, d_qkv, attn_gain_part, *one_parts = attn_bwd(
            branch_rows, hidden_rows, qkv, inverses, tables, tags, width, qkv_pieces, out_pieces, ranks
        )
        out_proj_grad = scatter_full(attended, branch_full, 1)
        query_grad, key_grad, value_grad = jnp.split(scatter_full(normed, d_qkv, 0), 3, axis=1)
        grad_one_rows = scatter_rows(one_parts)
        input_grad = grad_middle + rms_back(grad_one_rows, input_local, attn_scale)
        gain_parts = jnp.concatenate([attn_gain_part, mlp_gain_part], axis=0)
        gain_grads = lax.psum_scatter(gain_parts, ("dp", "tensor"), scatter_dimension=1, tiled=True)
    return (
        layer_out,
        input_grad,
        gain_grads[0],
        query_grad,
        key_grad,
        value_grad,
        out_proj_grad,
        gain_grads[1],
        gate_grad,
        up_grad,
        down_grad,
    )


def solution(mesh):
    return jax.shard_map(
        body,
        mesh=mesh,
        in_specs=(
            P(("dp", "tensor"), None),
            P(("dp", "tensor"), None),
            P("dp"),
            P("dp"),
            P("dp", "tensor"),
            P("dp", "tensor"),
            P("dp", "tensor"),
            P("tensor", "dp"),
            P("dp"),
            P("dp", "tensor"),
            P("dp", "tensor"),
            P("tensor", "dp"),
        ),
        out_specs=(
            P(("dp", "tensor"), None),
            P(("dp", "tensor"), None),
            P(("dp", "tensor")),
            P("dp", "tensor"),
            P("dp", "tensor"),
            P("dp", "tensor"),
            P("tensor", "dp"),
            P(("dp", "tensor")),
            P("dp", "tensor"),
            P("dp", "tensor"),
            P("tensor", "dp"),
        ),
        check_vma=False,
    )
```

```python
import math
from functools import partial

import jax
import jax.numpy as jnp
from jax import lax
from jax.experimental import pallas as pl
from jax.experimental.pallas import tpu as pltpu
from jax.sharding import PartitionSpec as P

HEAD_DIM = 64
EPSILON = 1e-05
ROPE_BASE = 130000.0
NEGATIVE = -1e30
VMEM_LIMIT = 63 * 1024 * 1024
BF = jnp.bfloat16
F32 = jnp.float32


def dot(left, right):
    return jnp.dot(left, right, preferred_element_type=F32)


def dot_rows(left, right):
    return lax.dot_general(left, right, (((1,), (1,)), ((), ())), preferred_element_type=F32)


def dot_cols(left, right):
    return lax.dot_general(left, right, (((0,), (0,)), ((), ())), preferred_element_type=F32)


def vmem():
    return pl.BlockSpec(memory_space=pltpu.VMEM)


def anyspace():
    return pl.BlockSpec(memory_space=pl.ANY)


def params():
    return pltpu.CompilerParams(vmem_limit_bytes=VMEM_LIMIT)


def cost(flops, nbytes):
    return pl.CostEstimate(flops=int(flops), bytes_accessed=int(nbytes), transcendentals=0)


def shape(dims, kind):
    return jax.ShapeDtypeStruct(dims, kind)


def place_copies(tags, pieces, target, sem, axis, width):
    own = lax.axis_index("dp")
    copies = []
    for slot, (tag, piece) in enumerate(zip(tags, pieces)):
        if tag is None:
            where = target
        else:
            start = pl.multiple_of((own ^ tag) * width, width)
            where = target.at[pl.ds(start, width), :] if axis == 0 else target.at[:, pl.ds(start, width)]
        copies.append(pltpu.make_async_copy(piece, where, sem.at[slot]))
    return copies


def row_copies(pieces, target, sem):
    copies = []
    for slot, piece in enumerate(pieces):
        rows = piece.shape[0]
        copies.append(pltpu.make_async_copy(piece, target.at[pl.ds(slot * rows, rows), :], sem.at[slot]))
    return copies


def start_all(copies):
    for copy in copies:
        copy.start()


def wait_all(copies):
    for copy in copies:
        copy.wait()


def turn(values, cosine, sine):
    width = values.shape[1]
    lane = lax.broadcasted_iota(jnp.int32, values.shape, 1)
    partner = jnp.where(
        lax.rem(lane, HEAD_DIM) < HEAD_DIM // 2,
        pltpu.roll(values, width - HEAD_DIM // 2, 1),
        pltpu.roll(values, HEAD_DIM // 2, 1),
    )
    return values * cosine + partner * sine


def norm_rows(source, target, inverses, gain, tile):
    @pl.loop(0, source.shape[0] // tile)
    def _(step):
        rows = pl.ds(pl.multiple_of(step * tile, tile), tile)
        values = source[rows, :].astype(F32)
        inverse = lax.rsqrt(jnp.mean(values * values, axis=-1, keepdims=True) + EPSILON)
        inverses[rows, :] = inverse
        target[rows, :] = (values * inverse * gain[...]).astype(BF)


def fill_bias(bias, first, last, key_index):
    keys = key_index[...]
    bias[...] = jnp.where((keys >= first[...]) & (keys <= last[...]), 0.0, NEGATIVE)


def head_lanes(width, half):
    lane = lax.broadcasted_iota(jnp.int32, (1, width), 1)
    return (lax.div(lane, HEAD_DIM) == half).astype(F32)


def probabilities(query, key, bias):
    scores = dot_rows(query, key) + bias
    weights = jnp.exp(scores - jnp.max(scores, axis=-1, keepdims=True))
    return weights * (1.0 / jnp.sum(weights, axis=-1, keepdims=True))


def attend(qkv, attended, bias, heads):
    @pl.loop(0, heads // 128)
    def _(pair):
        base = pl.multiple_of(pair * 128, 128)
        query = qkv[:, pl.ds(base, 128)]
        key = qkv[:, pl.ds(heads + base, 128)]
        value = qkv[:, pl.ds(2 * heads + base, 128)]
        total = None
        for half in range(2):
            lanes = head_lanes(128, half).astype(BF)
            probs = probabilities(query * (lanes * HEAD_DIM ** (-0.5)), key, bias[...])
            term = dot(probs.astype(BF), value * lanes)
            total = term if total is None else total + term
        attended[:, pl.ds(base, 128)] = total.astype(BF)


def attn_fwd_kernel(tags, width, nrow, *refs):
    npiece = len(tags)
    rows_in = refs[:nrow]
    gain, cosine, sine, first, last, key_index = refs[nrow : nrow + 6]
    rest = refs[nrow + 6 :]
    qkv_in, out_in = rest[:npiece], rest[npiece : 2 * npiece]
    rest = rest[2 * npiece :]
    normed, qkv, attended, inverses = rest[:4]
    parts = rest[4 : 4 + nrow]
    hidden, qkv_w, out_w, bias, sem_rows, sem_qkv, sem_out = rest[4 + nrow :]
    load_rows = row_copies(rows_in, hidden, sem_rows)
    load_qkv = place_copies(tags, qkv_in, qkv_w, sem_qkv, 0, width)
    load_out = place_copies(tags, out_in, out_w, sem_out, 1, width)
    start_all(load_rows + load_qkv + load_out)
    fill_bias(bias, first, last, key_index)
    wait_all(load_rows)
    norm_rows(hidden, normed, inverses, gain, 64)
    wait_all(load_qkv)
    heads = attended.shape[1]
    step_cols = 256

    @pl.loop(0, 2 * heads // step_cols)
    def _(step):
        cols = pl.ds(pl.multiple_of(step * step_cols, step_cols), step_cols)
        qkv[:, cols] = turn(dot(normed[...], qkv_w[:, cols]), cosine[...], sine[...]).astype(BF)

    @pl.loop(2 * heads // step_cols, 3 * heads // step_cols)
    def _(step):
        cols = pl.ds(pl.multiple_of(step * step_cols, step_cols), step_cols)
        qkv[:, cols] = dot(normed[...], qkv_w[:, cols]).astype(BF)

    attend(qkv, attended, bias, heads)
    wait_all(load_out)
    tile = parts[0].shape[0]

    @pl.loop(0, out_w.shape[1] // step_cols)
    def _(step):
        cols = pl.ds(pl.multiple_of(step * step_cols, step_cols), step_cols)
        product = dot(attended[...], out_w[:, cols])
        for slot, part in enumerate(parts):
            part[:, cols] = product[slot * tile : (slot + 1) * tile, :].astype(part.dtype)


def attn_fwd(rows, gain, tables, tags, width, qkv_pieces, out_pieces):
    nrow, (tile, dim) = len(rows), rows[0].shape
    tokens = nrow * tile
    heads = out_pieces[0].shape[0]
    npiece = len(tags)
    return pl.pallas_call(
        partial(attn_fwd_kernel, tags, width, nrow),
        out_shape=[
            shape((tokens, dim), BF),
            shape((tokens, 3 * heads), BF),
            shape((tokens, heads), BF),
            shape((tokens, 1), F32),
        ]
        + [shape((tile, dim), F32 if slot == 0 else BF) for slot in range(nrow)],
        in_specs=[anyspace()] * nrow + [vmem()] * 6 + [anyspace()] * (2 * npiece),
        out_specs=[vmem()] * (4 + nrow),
        scratch_shapes=[
            pltpu.VMEM((tokens, dim), BF),
            pltpu.VMEM((dim, 3 * heads), BF),
            pltpu.VMEM((heads, dim), BF),
            pltpu.VMEM((tokens, tokens), F32),
            pltpu.SemaphoreType.DMA((nrow,)),
            pltpu.SemaphoreType.DMA((npiece,)),
            pltpu.SemaphoreType.DMA((npiece,)),
        ],
        compiler_params=params(),
        cost_estimate=cost(2 * tokens * dim * 4 * heads * 3, 20e6),
        name="attn_fwd",
    )(*rows, gain, *tables, *qkv_pieces, *out_pieces)


def attend_back(qkv, d_attended, d_qkv, bias, cosine, sine, heads):
    score_scale = HEAD_DIM ** (-0.5)

    @pl.loop(0, heads // 128)
    def _(pair):
        base = pl.multiple_of(pair * 128, 128)
        query = qkv[:, pl.ds(base, 128)]
        key = qkv[:, pl.ds(heads + base, 128)]
        value = qkv[:, pl.ds(2 * heads + base, 128)]
        grad = d_attended[:, pl.ds(base, 128)]
        sums = [0.0, 0.0, 0.0]
        for half in range(2):
            lanes = head_lanes(128, half).astype(BF)
            own_query = query * (lanes * score_scale)
            own_grad = grad * lanes
            probs = probabilities(own_query, key, bias[...])
            d_value = dot_cols(probs.astype(BF), own_grad)
            d_probs = dot_rows(own_grad, value)
            delta = jnp.sum(probs * d_probs, axis=-1, keepdims=True)
            d_scores = (probs * (d_probs - delta)).astype(BF)
            d_query = dot(d_scores, key * lanes) * score_scale
            d_key = dot_cols(d_scores, own_query)
            sums = [sums[0] + d_query, sums[1] + d_key, sums[2] + d_value]
        back = -sine[:, :128]
        d_qkv[:, pl.ds(base, 128)] = turn(sums[0], cosine[:, :128], back).astype(BF)
        d_qkv[:, pl.ds(heads + base, 128)] = turn(sums[1], cosine[:, :128], back).astype(BF)
        d_qkv[:, pl.ds(2 * heads + base, 128)] = sums[2].astype(BF)


def attn_bwd_kernel(tags, width, nrow, npart, *refs):
    npiece = len(tags)
    nhid, nrow = nrow[1], nrow[0]
    rows_in, hidden_in = refs[:nrow], refs[nrow : nrow + nhid]
    refs = refs[nrow + nhid :]
    qkv, inverses, cosine, sine, first, last, key_index = refs[:7]
    rest = refs[7:]
    qkv_in, out_in = rest[:npiece], rest[npiece : 2 * npiece]
    rest = rest[2 * npiece :]
    branch, d_qkv, gain_grad = rest[:3]
    parts = rest[3 : 3 + npart]
    hidden, d_attended, qkv_w, out_w, bias, sem_rows, sem_x, sem_qkv, sem_out = rest[3 + npart :]
    load_rows = row_copies(rows_in, branch, sem_rows)
    load_x = row_copies(hidden_in, hidden, sem_x)
    load_out = place_copies(tags, out_in, out_w, sem_out, 1, width)
    load_qkv = place_copies(tags, qkv_in, qkv_w, sem_qkv, 0, width)
    start_all(load_rows + load_out + load_qkv + load_x)
    fill_bias(bias, first, last, key_index)
    wait_all(load_rows)
    wait_all(load_out)
    heads = out_w.shape[0]
    step_cols = 256

    @pl.loop(0, heads // step_cols)
    def _(step):
        cols = pl.ds(pl.multiple_of(step * step_cols, step_cols), step_cols)
        d_attended[:, cols] = dot_rows(branch[...], out_w[cols, :]).astype(BF)

    attend_back(qkv, d_attended, d_qkv, bias, cosine, sine, heads)
    wait_all(load_qkv)
    wait_all(load_x)
    tile = parts[0].shape[0]

    @pl.loop(0, qkv_w.shape[0] // step_cols)
    def _(step):
        cols = pl.ds(pl.multiple_of(step * step_cols, step_cols), step_cols)
        product = dot_rows(d_qkv[...], qkv_w[cols, :])
        gain_grad[:, cols] = jnp.sum(product * (hidden[:, cols].astype(F32) * inverses[...]), axis=0, keepdims=True)
        for slot, part in enumerate(parts):
            part[:, cols] = product[slot * tile : (slot + 1) * tile, :].astype(part.dtype)


def attn_bwd(rows, hidden, qkv, inverses, tables, tags, width, qkv_pieces, out_pieces, npart):
    nrow, nhid, dim = len(rows), len(hidden), rows[0].shape[1]
    tokens = qkv.shape[0]
    tile = tokens // npart
    heads = out_pieces[0].shape[0]
    npiece = len(tags)
    return pl.pallas_call(
        partial(attn_bwd_kernel, tags, width, (nrow, nhid), npart),
        out_shape=[shape((tokens, dim), BF), shape((tokens, 3 * heads), BF), shape((1, dim), F32)]
        + [shape((tile, dim), F32 if slot == 0 else BF) for slot in range(npart)],
        in_specs=[anyspace()] * (nrow + nhid) + [vmem()] * 7 + [anyspace()] * (2 * npiece),
        out_specs=[vmem()] * (3 + npart),
        scratch_shapes=[
            pltpu.VMEM((tokens, dim), BF),
            pltpu.VMEM((tokens, heads), BF),
            pltpu.VMEM((dim, 3 * heads), BF),
            pltpu.VMEM((heads, dim), BF),
            pltpu.VMEM((tokens, tokens), F32),
            pltpu.SemaphoreType.DMA((nrow,)),
            pltpu.SemaphoreType.DMA((nhid,)),
            pltpu.SemaphoreType.DMA((npiece,)),
            pltpu.SemaphoreType.DMA((npiece,)),
        ],
        compiler_params=params(),
        cost_estimate=cost(2 * tokens * dim * 4 * heads * 6, 30e6),
        name="attn_bwd",
    )(*rows, *hidden, qkv, inverses, *tables, *qkv_pieces, *out_pieces)


def mlp_kernel(tags, width, nrow, npart, *refs):
    npiece = len(tags)
    sent_in, cot_in = refs[:nrow], refs[nrow : 2 * nrow]
    gain = refs[2 * nrow]
    rest = refs[2 * nrow + 1 :]
    gate_in, up_in, down_in = rest[:npiece], rest[npiece : 2 * npiece], rest[2 * npiece : 3 * npiece]
    rest = rest[3 * npiece :]
    normed, hidden, d_gate, d_up, gain_grad = rest[:5]
    parts = rest[5 : 5 + npart]
    sent, cot, inverses, gate_w, up_w, down_w, sem_sent, sem_cot, sem_gate, sem_up, sem_down = rest[5 + npart :]
    load_sent = row_copies(sent_in, sent, sem_sent)
    load_cot = row_copies(cot_in, cot, sem_cot)
    load_gate = place_copies(tags, gate_in, gate_w, sem_gate, 0, width)
    load_up = place_copies(tags, up_in, up_w, sem_up, 0, width)
    load_down = place_copies(tags, down_in, down_w, sem_down, 1, width)
    start_all(load_sent + load_cot + load_gate + load_up + load_down)
    wait_all(load_sent)
    norm_rows(sent, normed, inverses, gain, 64)
    wait_all(load_cot)
    wait_all(load_gate)
    wait_all(load_up)
    wait_all(load_down)
    step_cols = 256

    @pl.loop(0, gate_w.shape[1] // step_cols)
    def _(step):
        cols = pl.ds(pl.multiple_of(step * step_cols, step_cols), step_cols)
        gate = dot(normed[...], gate_w[:, cols])
        up = dot(normed[...], up_w[:, cols])
        d_hidden = dot_rows(cot[...], down_w[cols, :])
        s = jax.nn.sigmoid(gate)
        activated = gate * s
        hidden[:, cols] = (activated * up).astype(BF)
        d_gate[:, cols] = (d_hidden * up * (s + activated * (1.0 - s))).astype(BF)
        d_up[:, cols] = (d_hidden * activated).astype(BF)

    tile = parts[0].shape[0]

    @pl.loop(0, gate_w.shape[0] // step_cols)
    def _(step):
        cols = pl.ds(pl.multiple_of(step * step_cols, step_cols), step_cols)
        product = dot_rows(d_gate[...], gate_w[cols, :]) + dot_rows(d_up[...], up_w[cols, :])
        gain_grad[:, cols] = jnp.sum(product * (sent[:, cols].astype(F32) * inverses[...]), axis=0, keepdims=True)
        for slot, part in enumerate(parts):
            part[:, cols] = product[slot * tile : (slot + 1) * tile, :].astype(part.dtype)


def mlp(sent, cot, gain, tags, width, gate_pieces, up_pieces, down_pieces, npart):
    nrow, dim = len(sent), sent[0].shape[1]
    tokens = nrow * sent[0].shape[0]
    tile = tokens // npart
    units = gate_pieces[0].shape[1]
    npiece = len(tags)
    return pl.pallas_call(
        partial(mlp_kernel, tags, width, nrow, npart),
        out_shape=[shape((tokens, dim), BF)]
        + [shape((tokens, units), BF)] * 3
        + [shape((1, dim), F32)]
        + [shape((tile, dim), F32 if slot == 0 else BF) for slot in range(npart)],
        in_specs=[anyspace()] * (2 * nrow) + [vmem()] + [anyspace()] * (3 * npiece),
        out_specs=[vmem()] * (5 + npart),
        scratch_shapes=[
            pltpu.VMEM((tokens, dim), BF),
            pltpu.VMEM((tokens, dim), BF),
            pltpu.VMEM((tokens, 1), F32),
            pltpu.VMEM((dim, units), BF),
            pltpu.VMEM((dim, units), BF),
            pltpu.VMEM((units, dim), BF),
            pltpu.SemaphoreType.DMA((nrow,)),
            pltpu.SemaphoreType.DMA((nrow,)),
            pltpu.SemaphoreType.DMA((npiece,)),
            pltpu.SemaphoreType.DMA((npiece,)),
            pltpu.SemaphoreType.DMA((npiece,)),
        ],
        compiler_params=params(),
        cost_estimate=cost(2 * tokens * dim * units * 5, 40e6),
        name="mlp",
    )(*sent, *cot, gain, *gate_pieces, *up_pieces, *down_pieces)


def mlp_out_kernel(tags, width, *refs):
    npiece = len(tags)
    hidden, down_in = refs[0], refs[1 : 1 + npiece]
    *parts, down_w, sem_down = refs[1 + npiece :]
    load_down = place_copies(tags, down_in, down_w, sem_down, 1, width)
    start_all(load_down)
    wait_all(load_down)
    tile, step_cols = parts[0].shape[0], 256

    @pl.loop(0, down_w.shape[1] // step_cols)
    def _(step):
        cols = pl.ds(pl.multiple_of(step * step_cols, step_cols), step_cols)
        product = dot(hidden[...], down_w[:, cols])
        for slot, part in enumerate(parts):
            part[:, cols] = product[slot * tile : (slot + 1) * tile, :].astype(part.dtype)


def mlp_out(hidden, nrow, dim, tags, width, down_pieces):
    tokens, units = hidden.shape
    tile, npiece = tokens // nrow, len(tags)
    return pl.pallas_call(
        partial(mlp_out_kernel, tags, width),
        out_shape=[shape((tile, dim), F32 if slot == 0 else BF) for slot in range(nrow)],
        in_specs=[vmem()] + [anyspace()] * npiece,
        out_specs=[vmem()] * nrow,
        scratch_shapes=[pltpu.VMEM((units, dim), BF), pltpu.SemaphoreType.DMA((npiece,))],
        compiler_params=params(),
        cost_estimate=cost(2 * tokens * dim * units, 14e6),
        name="mlp_out",
    )(hidden, *down_pieces)


def slice_of(slot, width, own):
    index = lax.axis_index("dp")
    owner = index ^ (2 * slot)
    return pl.ds(pl.multiple_of((owner if own else lax.div(owner, 2)) * width, width), width)

MESH = pl.DeviceIdType.MESH
NEAR = (2, 4, 6)
PARTS = 2
GROUPS = 4


def remote(source, target, send_sem, recv_sem, axis, peer):
    return pltpu.make_async_remote_copy(
        src_ref=source,
        dst_ref=target,
        send_sem=send_sem,
        recv_sem=recv_sem,
        device_id={axis: peer},
        device_id_type=MESH,
    )


def drain(ref, sem):
    pltpu.make_async_copy(ref, ref, sem).wait()


def meet():
    own, rank = lax.axis_index("dp"), lax.axis_index("tensor")
    barrier = pltpu.get_barrier_semaphore()
    for flip in range(1, 8):
        pl.semaphore_signal(barrier, inc=1, device_id={"dp": own ^ flip}, device_id_type=MESH)

    @pl.when(rank < 3)
    def _():
        pl.semaphore_signal(barrier, inc=1, device_id={"tensor": rank + 1}, device_id_type=MESH)

    @pl.when(rank > 0)
    def _():
        pl.semaphore_signal(barrier, inc=1, device_id={"tensor": rank - 1}, device_id_type=MESH)

    pl.semaphore_wait(barrier, 8 + lax.div(rank * (3 - rank), 2))


def at_cols(ref, index, width):
    return ref.at[:, pl.ds(pl.multiple_of(index * width, width), width)]


def at_rows(ref, index, width):
    return ref.at[pl.ds(pl.multiple_of(index * width, width), width), :]


def either(rank, *choices):
    result = rank == choices[0]
    for choice in choices[1:]:
        result = result | (rank == choice)
    return result


def ends(rank):
    return either(rank, 0, 3)


def inner(rank):
    return either(rank, 1, 2)


class RowGather:
    def __init__(self, rank, source, landing, part, size, send, recv):
        self.rank = rank

        def place(slot):
            return landing.at[pl.ds(pl.multiple_of((4 * part + slot) * size, size), size), :]

        def copy(origin, slot, peer):
            return remote(origin, place(slot), send.at[part], recv.at[part, slot - 1], "tensor", peer)

        def forward(slot, target, peer):
            return copy(place(slot), target, peer)

        outward, inward = (rank - 1) * 3, 3 - rank
        near, far = 5 - 2 * rank, 2 * rank - 1
        self.up, self.down = copy(source, 1, rank + 1), copy(source, 3, rank - 1)
        self.hops = [forward(near, 2, outward), forward(far, 2, inward), forward(2, far, outward)]
        self.slots = [near, far, 2]
        self.arrival = lambda slot: copy(source, slot, lax.rem(rank + 1, 4))
        self.sent = lambda count: drain(landing.at[pl.ds(0, count * size), :], send.at[part])

    def start(self):
        pl.when(self.rank < 3)(self.up.start)
        pl.when(self.rank > 0)(self.down.start)

    def hop(self, index):
        @pl.when(inner(self.rank))
        def _():
            self.arrival(self.slots[index]).wait_recv()
            self.hops[index].start()

    def wait(self):
        @pl.when(ends(self.rank))
        def _():
            for slot in (1, 2, 3):
                self.arrival(slot).wait_recv()

    def finish(self):
        pl.when(ends(self.rank))(lambda: self.sent(1))
        pl.when(inner(self.rank))(lambda: self.sent(5))


class RowScatter:
    def __init__(self, rank, source, landing, part, size, send, recv, staged=None, sem=None):
        self.rank, self.source, self.size, self.staged, self.sem = rank, source, size, staged, sem
        self.place = lambda k: pl.ds(pl.multiple_of((4 * part + k) * size, size), size)
        self.land = lambda slot: landing.at[pl.ds((5 * part + slot) * size, size), :]

        def copy(k, slot, peer):
            return remote(source.at[self.place(k), :], self.land(slot), send.at[part], recv.at[part, slot], "tensor", peer)

        end = lax.div(rank, 3)
        self.first = [copy(index + 1 + end * (2 - 2 * index), index, 1 + end) for index in range(3)]
        self.keys = [2, 5 - 2 * rank, 2 * rank - 1]
        self.later = [
            copy(self.keys[0], 3, 3 - rank),
            copy(self.keys[1], 4, 3 - rank),
            copy(self.keys[2], 4, (rank - 1) * 3),
        ]
        self.arrival = lambda slot: copy(1, slot, lax.rem(rank + 1, 4))
        self.finish = lambda: drain(source.at[pl.ds(0, 3 * size), :], send.at[part])

    def start(self, indices=(0, 1, 2)):
        @pl.when(ends(self.rank))
        def _():
            for index in indices:
                self.first[index].start()

    def hop(self, index):
        @pl.when(inner(self.rank))
        def _():
            slot = (0, 1, 3)[index]
            self.arrival(slot).wait_recv()
            other = self.land(slot)
            if self.staged is not None:
                load = pltpu.make_async_copy(other, self.staged, self.sem)
                load.start()
                load.wait()
                other = self.staged
            target = self.source.at[self.place(self.keys[index]), :]

            @pl.loop(0, self.size // 16)
            def _(step):
                rows = pl.ds(pl.multiple_of(step * 16, 16), 16)
                target[rows, :] = (target[rows, :].astype(F32) + other[rows, :].astype(F32)).astype(BF)

            self.later[index].start()

    def wait(self):
        pl.when(inner(self.rank))(self.arrival(2).wait_recv)
        self.arrival(4).wait_recv()


def fill_mask(bias, docs, size):
    rank = lax.axis_index("tensor")
    tokens = bias.shape[0]
    values = docs[...]
    starts = [jnp.sum(jnp.where(values < number, 1, 0), keepdims=True) for number in range(1, 8)]

    def document(position):
        return sum(jnp.where(position >= start, 1, 0) for start in starts)

    lane = lax.broadcasted_iota(jnp.int32, (1, tokens), 1)
    slot = lax.rem(lax.div(lane, size), 4)
    part = lax.div(lane, 4 * size)
    keys = lax.rem(rank - slot + 4, 4) * (2 * size) + part * size + lax.rem(lane, size)
    key_docs = document(keys)

    @pl.loop(0, tokens // size)
    def _(block):
        base = lax.rem(rank - lax.rem(block, 4) + 4, 4) * (2 * size) + lax.div(block, 4) * size
        queries = base + lax.broadcasted_iota(jnp.int32, (size, 1), 0)
        allowed = (document(queries) == key_docs) & (queries >= keys)
        bias[pl.ds(pl.multiple_of(block * size, size), size), :] = jnp.where(allowed, 0.0, NEGATIVE)


def fill_turns(cosine, sine, size):
    rank = lax.axis_index("tensor")
    half_size = HEAD_DIM // 2
    dims = (size, cosine.shape[1])
    lane = lax.broadcasted_iota(jnp.int32, dims, 1)
    row = lax.broadcasted_iota(jnp.int32, dims, 0)
    frequency = jnp.exp(lax.rem(lane, half_size).astype(F32) * (-math.log(ROPE_BASE) / half_size))
    sign = jnp.where(lax.rem(lane, HEAD_DIM) < half_size, -1.0, 1.0)

    @pl.loop(0, cosine.shape[0] // size)
    def _(block):
        start = (lax.rem(rank - lax.rem(block, 4) + 4, 4) * PARTS + lax.div(block, 4)) * size
        angles = (row + start).astype(F32) * frequency
        rows = pl.ds(pl.multiple_of(block * size, size), size)
        cosine[rows, :] = jnp.cos(angles)
        sine[rows, :] = jnp.sin(angles) * sign


def slice_of(slot, width, own):
    index = lax.axis_index("dp")
    owner = index ^ (2 * slot)
    return pl.ds(pl.multiple_of((owner if own else lax.div(owner, 2)) * width, width), width)


def layer_kernel(*refs):
    hidden_in, cot_in, *plain_gains = refs[:4]
    weights_in = refs[4:11]
    docs = refs[11]
    down_sum, gate_sum, up_sum, qkv_parts, out_parts = refs[12:17]
    down_parts, gate_parts, up_parts = refs[17:20]
    grad_merge = refs[20:25]
    pair_gate, pair_up, pair_qkv, pair_attended, pair_normed, pair_branch = refs[25:31]
    branch_rows, hidden_rows, normed_rows, mlp_recv, qkv_full, down_full = refs[31:37]
    layer_out, input_grad, gain_total = refs[37:40]
    gate_w, up_w, down_w, sent, cot, normed, hidden, d_gate, d_up = refs[40:49]
    two_half, cot_half, buffer_a, buffer_b, buffer_c, out_w = refs[49:55]
    qkv, attended, d_attended, bias, cosine, sine = refs[55:61]
    inverses_one, inverses, middle, grad_middle, send_part, recv_part = refs[61:67]
    gains_in, gains, gain_part, gain_recv, gain_z = refs[67:72]
    a_send, a_recv, f_send, f_recv, h_send, h_recv, z_send, z_recv, r_send, r_recv = refs[72:82]
    w_send, w_recv, d_send, d_recv, g_send, g_recv, y_send, y_recv, load, keep, down_load, s_recv, n_recv = refs[82:]

    own, rank = lax.axis_index("dp"), lax.axis_index("tensor")
    core = lax.rem(own, 2)
    tokens, dim = sent.shape
    units = gate_w.shape[1]
    tile = hidden_in.shape[0]
    size = tile // PARTS
    span = 4 * size
    heads = attended.shape[1]
    width = weights_in[0].shape[0]
    half = dim // (2 * width)
    d_qkv = cot.at[:, pl.ds(heads, 3 * heads)]
    group = units // GROUPS
    step_cols = 256
    count = dim // step_cols

    def cols_of(step, length=step_cols):
        return pl.ds(pl.multiple_of(step * length, length), length)

    def local(source, target, sem):
        return pltpu.make_async_copy(source, target, sem)

    def own_rows(part):
        return pl.ds(part * span, size)

    def part_rows(part):
        return pl.ds(part * size, size)

    def source_of(item):
        if item < 4:
            return weights_in[item]
        which, start = (item - 4) % 3, ((item - 4) // 3) * group
        if which == 2:
            return weights_in[4].at[pl.ds(start, group), :]
        return weights_in[5 + which].at[:, pl.ds(start, group)]

    def view(item, owner, part=None):
        rows = heads if item == 3 else group if item > 3 and (item - 4) % 3 == 2 else width
        length = rows if part is None else rows // 2
        start = 0 if part is None else part * length
        if item < 3:
            place = pl.ds(pl.multiple_of(owner * width + start, length), length)
            return down_w.at[place, pl.ds(item * heads, heads)]
        if item == 3:
            return out_w.at[pl.ds(start, length), pl.ds(pl.multiple_of(owner * width, width), width)]
        which, offset = (item - 4) % 3, ((item - 4) // 3) * group
        if which == 2:
            return down_full.at[pl.ds(offset + start, length), pl.ds(pl.multiple_of(owner * width, width), width)]
        place = pl.ds(pl.multiple_of(owner * width + start, length), length)
        return (gate_w, up_w)[which].at[place, pl.ds(offset, group)]

    def phase_of(item):
        return 0 if item < 3 else 1 if item == 3 else 2 + (item - 4) // 3

    def send_weight(item, flip):
        sem = s_recv.at[phase_of(item)] if flip == 1 else a_recv.at[item, flip // 2 - 1]
        return remote(source_of(item), view(item, own), a_send.at[phase_of(item)], sem, "dp", own ^ flip)

    def relay_weight(item, part):
        place = view(item, own ^ (4 - 2 * part), part)
        return remote(place, place, a_send.at[phase_of(item)], a_recv.at[item, 2], "dp", own ^ (2 + 2 * part))

    def pass_weight(item, flip):
        place = view(item, own ^ flip)
        return remote(place, place, a_send.at[phase_of(item)], s_recv.at[phase_of(item)], "dp", own ^ 1)

    def send_weights(items):
        for item in items:
            for flip in (2, 4, 1):
                send_weight(item, flip).start()

    def relay_weights(items):
        for item in items:
            send_weight(item, 4).wait_recv()
            relay_weight(item, 0).start()
            send_weight(item, 2).wait_recv()
            relay_weight(item, 1).start()
            pass_weight(item, 4).start()
            pass_weight(item, 2).start()

    def pass_weights(items):
        for item in items:
            drain(view(item, own ^ 6), a_recv.at[item, 2])
            pass_weight(item, 6).start()

    def have_weights(phase):
        drain(gate_w.at[pl.ds(0, width if phase == 1 else 3 * width), :], s_recv.at[phase])

    def sent_weights(phase):
        length = 7 * width // 4
        drain(gate_w.at[pl.ds(0, length if phase == 1 else 3 * length), :], a_send.at[phase])

    def items_of(index):
        return list(range(4 + 3 * index, 7 + 3 * index))

    def send_gain(flip):
        return remote(gains_in, at_cols(gains, own, width), y_send.at[0], y_recv.at[0], "dp", own ^ flip)

    def gathers(kind, source, landing):
        return [
            RowGather(rank, source(part), landing, part, size, z_send.at[kind], z_recv.at[kind]) for part in range(PARTS)
        ]

    gather_hidden = gathers(0, lambda part: hidden_in.at[part_rows(part), :], buffer_b)
    gather_cot = gathers(1, lambda part: cot_in.at[part_rows(part), :], cot)
    gather_sent = gathers(2, lambda part: sent.at[own_rows(part), :], sent)
    gather_branch = gathers(3, lambda part: sent.at[own_rows(part), :], branch_rows)

    def scatters(kind, source, landing, staged=None, sem=None):
        return [
            RowScatter(rank, source, landing, part, size, r_send.at[kind], r_recv.at[kind], staged, sem)
            for part in range(PARTS)
        ]

    gate_stage = up_w.at[pl.ds(4 * width, size), :]
    out_scatter = scatters(0, send_part, recv_part)
    two_scatter = scatters(1, send_part, recv_part)
    mlp_scatter = scatters(2, sent, mlp_recv, gate_stage, load.at[3])
    one_scatter = scatters(3, send_part, recv_part)

    def arrived(part, slot):
        return pl.ds((5 * part + slot) * size, size)

    def clear(part):
        @pl.when(ends(rank))
        def _():
            recv_part[arrived(part, 2), :] = jnp.zeros((size, dim), BF)

    def received(part, start, length, base):
        total = base
        for slot in (2, 4):
            rows = pl.ds(pl.multiple_of((5 * part + slot) * size + start, length), length)
            total = total + recv_part[rows, :].astype(F32)
        return total

    def to_pair(source, target, row, slot):
        return remote(source, target, h_send.at[row], h_recv.at[row], "dp", own ^ 1)

    def halves(source, target, row):
        return [
            to_pair(at_cols(source, 2 * slot + 1 - core, width), at_cols(target, slot, width), row, slot)
            for slot in range(half)
        ]

    def send_ff(step, which):
        cols = cols_of(step)
        source = (hidden, d_gate, d_up)[which].at[:, cols]
        target = (buffer_a, pair_gate, pair_up)[which].at[:, cols]
        arrival = lax.div(step, group // step_cols) if which == 0 else GROUPS - 1 + which
        return remote(source, target, f_send.at[which], f_recv.at[arrival], "dp", own ^ 1)

    def piece(index, slot):
        if index < 3:
            return at_rows(gate_w, (index - 1) * 4 + slot, width)
        if index == 3:
            return (hidden, d_gate)[slot // 2].at[pl.ds((slot % 2) * width, width), pl.ds(0, 3 * heads)]
        return at_cols(d_up, slot, width)

    def landing_of(index, slot):
        ref = (down_parts, gate_parts, up_parts, qkv_parts, out_parts)[index]
        if index < 3:
            return at_rows(ref, slot - 1, width)
        return at_cols(ref, slot, width) if index == 4 else at_rows(ref, slot, width)

    def half_of(ref, index, part):
        rows, cols = ref.shape
        if index == 4:
            return ref.at[pl.ds(part * (rows // 2), rows // 2), :]
        return ref.at[:, pl.ds(part * (cols // 2), cols // 2)]

    def stage_of(index, part):
        if index == 4:
            return up_w.at[pl.ds(7 * width, heads // 2), pl.ds(part * width, width)]
        length = units // 2 if index < 3 else 3 * heads // 2
        return up_w.at[pl.ds((3 + index) * width, width), pl.ds(part * (units // 2), length)]

    def send_far(index, part):
        return remote(
            half_of(piece(index, 3), index, part),
            half_of(grad_merge[index], index, part),
            w_send.at[index - 1],
            w_recv.at[index - 1, part],
            "dp",
            own ^ (2 + 2 * part),
        )

    def send_near(index, slot, part):
        return remote(
            half_of(piece(index, slot), index, part),
            half_of(landing_of(index, slot), index, part),
            w_send.at[index - 1],
            n_recv.at[index - 1],
            "dp",
            own ^ (2 * slot),
        )

    def keep_grad(index):
        return local(piece(index, 0), landing_of(index, 0), keep.at[index])

    def merge_grads(index):
        loads = [local(half_of(grad_merge[index], index, part), stage_of(index, part), load.at[part]) for part in range(2)]
        for part in range(2):
            send_far(index, part).wait_recv()
            loads[part].start()
        for part in range(2):
            loads[part].wait()
            target, source = half_of(piece(index, 2 - part), index, part), stage_of(index, part)
            length = source.shape[0] // 4

            @pl.loop(0, 4)
            def _(step):
                rows = cols_of(step, length)
                target[rows, :] = (target[rows, :].astype(F32) + source[rows, :].astype(F32)).astype(BF)

            send_near(index, 2 - part, part).start()

    def row_grads(index, slot, left, left_pair, right, right_pair, columns):
        mine, theirs = slice_of(slot, width, True), slice_of(slot, width, False)
        turned, turned_pair = jnp.transpose(left[:, mine]), jnp.transpose(left_pair[:, theirs])
        target = piece(index, slot)

        @pl.loop(0, columns // 512)
        def _(step):
            cols = cols_of(step, 512)
            total = dot(turned, right[:, cols]) + dot(turned_pair, right_pair[:, cols])
            target[:, cols] = total.astype(BF)

        if slot == 3:
            send_far(index, 0).start()
            send_far(index, 1).start()
        elif slot:
            send_near(index, slot, slot - 1).start()
        elif index == 3:
            keep_grad(index).start()

    def out_grads():
        for part in range(2):
            rows = pl.ds(part * (heads // 2), heads // 2)
            turned, turned_pair = jnp.transpose(attended[:, rows]), jnp.transpose(cot[:, rows])
            for slot in range(4):
                mine, theirs = slice_of(slot, width, True), slice_of(slot, width, False)
                total = dot(turned, buffer_a[:, mine]) + dot(turned_pair, cot_half[:, theirs])
                piece(4, slot)[rows, :] = total.astype(BF)
            send_far(4, part).start()
            send_near(4, part + 1, part).start()
        keep_grad(4).start()

    def down_piece(slot, index, part=None):
        cols = pl.ds(((slot % 2) * GROUPS + index) * width, width)
        rows = pl.ds(0, group) if part is None else pl.ds(part * (group // 2), group // 2)
        return (buffer_b, buffer_c)[slot // 2].at[rows, cols]

    def down_rows(ref, index, slot, part=None):
        rows = pl.ds(index * group, group) if part is None else pl.ds(index * group + part * (group // 2), group // 2)
        return ref.at[rows, pl.ds(slot * width, width)]

    def send_down(kind, index, part):
        if kind == 0:
            target, source = down_rows(grad_merge[0], index, 0, part), down_piece(3, index, part)
            peer = own ^ (2 + 2 * part)
        else:
            target, source = down_rows(down_parts, index, kind - 1, part), down_piece(kind, index, part)
            peer = own ^ (2 * kind)
        return remote(source, target, d_send.at[0], d_recv.at[GROUPS if kind else index], "dp", peer)

    def down_grads(index):
        drain(buffer_a.at[:, pl.ds(index * group, group)], f_recv.at[index])

        @pl.loop(0, group // 256)
        def _(step):
            cols = pl.ds(pl.multiple_of(index * group + step * 256, 256), 256)
            rows = pl.ds(pl.multiple_of(step * 256, 256), 256)
            turned, turned_pair = jnp.transpose(hidden[:, cols]), jnp.transpose(buffer_a[:, cols])
            for slot in range(4):
                mine, theirs = slice_of(slot, width, True), slice_of(slot, width, False)
                total = dot(turned, cot[:, mine]) + dot(turned_pair, cot_half[:, theirs])
                down_piece(slot, index)[rows, :] = total.astype(BF)

        for part in range(2):
            send_down(0, index, part).start()
        for part in range(2):
            send_down(1 + part, index, part).start()

    def merge_down(indices):
        entries = [(index, part) for index in indices for part in range(2)]

        def stage(index, part):
            rows = pl.ds(part * (group // 2), group // 2)
            return d_attended.at[rows, pl.ds((index % 2) * width, width)]

        loads = [
            local(down_rows(grad_merge[0], index, 0, part), stage(index, part), load.at[2 * (index % 2) + part])
            for index, part in entries
        ]
        for index in indices:
            drain(down_rows(grad_merge[0], index, 0), d_recv.at[index])
        start_all(loads)
        for copy, (index, part) in zip(loads, entries):
            copy.wait()
            target, source = down_piece(2 - part, index, part), stage(index, part)

            @pl.loop(0, 2)
            def _(step):
                rows = cols_of(step, group // 4)
                target[rows, :] = (target[rows, :].astype(F32) + source[rows, :].astype(F32)).astype(BF)

            send_down(2 - part, index, part).start()

    def norm_back(total, values, gain):
        inverse = lax.rsqrt(jnp.mean(values * values, axis=-1, keepdims=True) + EPSILON)
        scaled = total * gain
        return inverse * (scaled - values * inverse * inverse * jnp.mean(scaled * values, axis=-1, keepdims=True))

    meet()
    for gather in gather_hidden:
        gather.start()
    gains_in[...] = jnp.zeros(gains_in.shape, F32)
    for index, plain in enumerate(plain_gains):
        gains_in[index : index + 1, :] = plain[...].astype(F32).reshape(1, width)
    send_weights(range(3))
    for flip in range(1, 8):
        send_gain(flip).start()
    stage_down = down_w.at[:, pl.ds(3 * heads, width)]
    stage_in = local(weights_in[4], stage_down, load.at[0])
    own_loads = [local(gains_in, at_cols(gains, own, width), load.at[1])]
    own_loads += [local(weights_in[item], view(item, own), load.at[2 + item]) for item in range(4)]
    own_loads += [local(weights_in[5], at_rows(gate_w, own, width), load.at[6])]
    own_loads += [local(weights_in[6], at_rows(up_w, own, width), load.at[7])]
    for part in range(PARTS):
        own_loads.append(local(hidden_in.at[part_rows(part), :], buffer_b.at[own_rows(part), :], load.at[8 + part]))
        own_loads.append(local(cot_in.at[part_rows(part), :], cot.at[own_rows(part), :], load.at[10 + part]))
    start_all([stage_in] + own_loads)
    fill_mask(bias, docs, size)
    fill_turns(cosine, sine, size)
    for part in range(PARTS):
        clear(part)
    relay_weights([0])
    gather_hidden[0].hop(0)
    gather_hidden[0].hop(1)
    relay_weights([1])
    gather_hidden[1].hop(0)
    gather_hidden[1].hop(1)
    gather_hidden[0].hop(2)
    relay_weights([2])
    send_weights([3, 4])
    gather_hidden[1].hop(2)
    for gather in gather_cot:
        gather.start()
    stage_in.wait()
    stage_out = local(stage_down, at_cols(down_full, own, width), keep.at[5])
    stage_out.start()
    wait_all(own_loads)
    drain(gain_recv.at[pl.ds(0, 56), :], y_recv.at[0])
    gather_cot[0].hop(1)
    gather_cot[0].hop(0)
    pass_weights(range(3))
    relay_weights([3])
    send_weights(range(5, 4 + 3 * GROUPS))
    for gather in gather_hidden:
        gather.wait()

    norm_rows(buffer_b, buffer_c, inverses_one, gains.at[pl.ds(0, 1), :], 64)
    keep_hidden = local(buffer_b, hidden_rows, keep.at[0])
    keep_normed = local(buffer_c, normed_rows, keep.at[1])
    start_all([keep_hidden, keep_normed])
    have_weights(0)
    qkv_w = down_w.at[:, pl.ds(0, 3 * heads)]
    keep_qkv = local(qkv_w, qkv_full, keep.at[2])
    keep_qkv.start()

    @pl.loop(0, 2 * heads // step_cols)
    def _(step):
        cols = cols_of(step)
        product = dot(buffer_c[...], down_w[:, cols])
        turns = [jnp.concatenate([table[...]] * (step_cols // 128), axis=1) for table in (cosine, sine)]
        qkv[:, cols] = turn(product, *turns).astype(BF)

    @pl.loop(2 * heads // step_cols, 3 * heads // step_cols)
    def _(step):
        cols = cols_of(step)
        qkv[:, cols] = dot(buffer_c[...], down_w[:, cols]).astype(BF)

    attend(qkv, attended, bias, heads)
    gather_cot[0].hop(2)
    gather_cot[1].hop(1)
    gather_cot[1].hop(0)
    pass_weights([3])
    have_weights(1)

    def make_out(part):
        @pl.loop(0, count)
        def _(step):
            cols = cols_of(step)
            product = dot(attended[part * span : (part + 1) * span, :], out_w[:, cols])
            middle[part_rows(part), cols] = product[:size, :]
            send_part[pl.ds(part * span + size, span - size), cols] = product[size:, :].astype(BF)

    make_out(0)
    out_scatter[0].start()
    make_out(1)
    out_scatter[1].start()
    gather_cot[1].hop(2)
    wait_all([keep_hidden, keep_normed, keep_qkv, stage_out])
    send_normed = halves(normed_rows, pair_normed, 1)
    send_attended = to_pair(attended, pair_attended, 2, 0)
    start_all(send_normed + [send_attended])
    for index in range(3):
        out_scatter[0].hop(index)
    relay_weights(items_of(0))

    def make_sent(part):
        out_scatter[part].wait()

        @pl.loop(0, size // 32)
        def _(step):
            rows = pl.ds(pl.multiple_of(part * size + step * 32, 32), 32)
            place = pl.ds(pl.multiple_of(part * span + step * 32, 32), 32)
            total = received(part, step * 32, 32, hidden_of(place) + middle[rows, :])
            middle[rows, :] = total
            sent[place, :] = total.astype(BF)

        gather_sent[part].start()

    def hidden_of(place):
        return buffer_b[place, :].astype(F32)

    make_sent(0)
    out_scatter[1].hop(0)
    relay_weights(items_of(1))
    gather_sent[0].hop(0)
    out_scatter[1].hop(1)
    out_scatter[1].hop(2)
    make_sent(1)
    gather_sent[0].hop(1)
    relay_weights(items_of(2))
    gather_sent[1].hop(0)
    gather_sent[1].hop(1)
    gather_sent[0].hop(2)
    gather_sent[1].hop(2)
    relay_weights(items_of(3))

    def load_down(index):
        rows = pl.ds(index * group, group)
        return local(down_full.at[rows, :], down_w.at[rows, :], down_load.at[index])

    for gather in gather_cot:
        gather.wait()
    send_cot = halves(cot, cot_half, 0)
    start_all(send_cot)
    for gather in gather_sent:
        gather.wait()
    norm_rows(sent, normed, inverses, gains.at[pl.ds(1, 1), :], 64)
    pass_weights(items_of(0))
    send_two = halves(normed, two_half, 3)
    start_all(send_two)
    have_weights(2)
    for phase in range(2):
        sent_weights(phase)
    for gather in gather_hidden:
        gather.finish()
    load_down(0).start()
    for index in range(GROUPS):
        load_down(index).wait()
        if index + 1 < GROUPS:
            pass_weights(items_of(index + 1))

        @pl.loop(index * group // step_cols, (index + 1) * group // step_cols)
        def _(step):
            cols = cols_of(step)
            gate = dot(normed[...], gate_w[:, cols])
            up = dot(normed[...], up_w[:, cols])
            d_hidden = dot_rows(cot[...], down_w[cols, :])
            s = jax.nn.sigmoid(gate)
            activated = gate * s
            hidden[:, cols] = (activated * up).astype(BF)
            d_gate[:, cols] = (d_hidden * up * (s + activated * (1.0 - s))).astype(BF)
            d_up[:, cols] = (d_hidden * activated).astype(BF)
            for which in range(3):
                send_ff(step, which).start()

        if index + 1 < GROUPS:
            have_weights(3 + index)
            load_down(index + 1).start()
        if index == 0:
            drain(cot_half, h_recv.at[0])
        else:
            down_grads(index - 1)

    gain_part[...] = jnp.zeros(gain_part.shape, F32)
    for part in range(PARTS):
        out_scatter[part].finish()

    def make_two(part):
        block = slice(part * span, (part + 1) * span)

        @pl.loop(0, count)
        def _(step):
            cols = cols_of(step)
            product = dot_rows(d_gate[block, :], gate_w[cols, :]) + dot_rows(d_up[block, :], up_w[cols, :])
            gain_part[pl.ds(1, 1), cols] += jnp.sum(
                product * (sent[block, cols].astype(F32) * inverses[block, :]), axis=0, keepdims=True
            )
            grad_middle[part_rows(part), cols] = product[:size, :]
            send_part[pl.ds(part * span + size, span - size), cols] = product[size:, :].astype(BF)

    make_two(0)
    two_scatter[0].start()
    down_grads(GROUPS - 1)
    merge_down((0, 1))
    make_two(1)
    two_scatter[0].hop(0)
    two_scatter[1].start()
    for phase in range(2, 2 + GROUPS):
        sent_weights(phase)
    for which in (1, 2):
        drain((d_gate, d_up)[which - 1], f_recv.at[GROUPS - 1 + which])
    gate_pair, up_pair = up_w.at[pl.ds(0, tokens), :], up_w.at[pl.ds(tokens, tokens), :]
    pair_loads = [local(pair_gate, gate_pair, load.at[0]), local(pair_up, up_pair, load.at[1])]
    start_all(pair_loads)
    drain(two_half, h_recv.at[3])
    wait_all(pair_loads)
    gate_grads = lambda slot: row_grads(1, slot, normed, two_half, d_gate, gate_pair, units)
    up_grads = lambda slot: row_grads(2, slot, normed, two_half, d_up, up_pair, units)
    gate_grads(3)
    merge_down((2, 3))
    two_scatter[0].hop(1)
    two_scatter[0].hop(2)
    for slot in (1, 2, 0):
        gate_grads(slot)

    def make_branch(part):
        two_scatter[part].wait()

        @pl.loop(0, size // 32)
        def _(step):
            rows = pl.ds(pl.multiple_of(part * size + step * 32, 32), 32)
            place = pl.ds(pl.multiple_of(part * span + step * 32, 32), 32)
            total = received(part, step * 32, 32, grad_middle[rows, :])
            result = cot[place, :].astype(F32) + norm_back(total, sent[place, :].astype(F32), gains[1:2, :])
            grad_middle[rows, :] = result
            sent[place, :] = result.astype(BF)

        gather_branch[part].start()
        keep_branch[part].start()

    keep_branch = [
        local(sent.at[own_rows(part), :], branch_rows.at[own_rows(part), :], keep.at[6 + part]) for part in range(PARTS)
    ]
    for part in range(PARTS):
        gather_sent[part].finish()
    make_branch(0)
    up_grads(3)
    two_scatter[1].hop(0)
    up_grads(1)
    gather_branch[0].hop(0)
    two_scatter[1].hop(1)
    two_scatter[1].hop(2)
    up_grads(2)
    up_grads(0)
    def project(first, last):
        @pl.loop(first, last)
        def _(step):
            cols = cols_of(step)
            product = dot(hidden[...], down_w[:, cols])
            for part in range(PARTS):
                start = part * span
                middle[part_rows(part), cols] = middle[part_rows(part), cols] + product[start : start + size, :]
                sent[pl.ds(start + size, span - size), cols] = product[start + size : start + span, :].astype(BF)

    pl.when(ends(rank))(lambda: project(0, count))
    mlp_scatter[0].start((0,))
    make_branch(1)
    mlp_scatter[0].start((1, 2))
    mlp_scatter[1].start()
    pl.when(inner(rank))(lambda: project(0, count // 4))
    gather_branch[0].hop(1)
    merge_grads(1)
    pl.when(inner(rank))(lambda: project(count // 4, count // 2))
    gather_branch[1].hop(0)
    pl.when(inner(rank))(lambda: project(count // 2, count))
    gather_branch[1].hop(1)
    gather_branch[0].hop(2)
    gather_branch[1].hop(2)
    load_weight = local(qkv_full, qkv_w, load.at[4])
    load_hidden = local(hidden_rows, gate_pair, load.at[5])
    load_normed = local(normed_rows, up_pair, load.at[6])
    start_all([load_hidden, load_normed])
    mlp_scatter[0].hop(0)
    merge_grads(2)
    for part in range(PARTS):
        two_scatter[part].finish()
        gather_branch[part].wait()
        keep_branch[part].wait()

    load_branch = local(branch_rows, buffer_a, load.at[7])
    load_branch.start()
    load_weight.start()
    send_half = halves(branch_rows, pair_branch, 4)
    start_all(send_half)
    mlp_scatter[0].hop(1)
    load_branch.wait()

    @pl.loop(0, heads // step_cols)
    def _(step):
        cols = cols_of(step)
        d_attended[:, cols] = dot_rows(buffer_a[...], out_w[cols, :]).astype(BF)

    drain(cot_half, h_send.at[0])
    for gather in gather_cot:
        gather.finish()
    drain(two_half, h_recv.at[1])
    send_attended.wait_recv()
    early_loads = [
        local(pair_attended, cot.at[:, pl.ds(0, heads)], load.at[8]),
        local(pair_normed, two_half, load.at[9]),
    ]
    start_all(early_loads)
    attend_back(qkv, d_attended, d_qkv, bias, cosine, sine, heads)
    send_qkv = to_pair(d_qkv, pair_qkv, 5, 0)
    send_qkv.start()
    for which in range(3):
        drain((hidden, d_gate, d_up)[which], f_send.at[which])

    drain(cot_half, h_recv.at[4])
    load_half = local(pair_branch, cot_half, load.at[10])
    load_half.start()
    mlp_scatter[0].hop(2)
    mlp_scatter[1].hop(0)
    wait_all([load_weight, load_hidden, load_normed])

    def make_one(part):
        block = slice(part * span, (part + 1) * span)

        @pl.loop(0, count)
        def _(step):
            cols = cols_of(step)
            product = dot_rows(d_qkv[block, :], down_w[cols, pl.ds(0, 3 * heads)])
            gain_part[pl.ds(0, 1), cols] += jnp.sum(
                product * (gate_pair[block, cols].astype(F32) * inverses_one[block, :]), axis=0, keepdims=True
            )
            input_grad[part_rows(part), cols] = product[:size, :]
            send_part[pl.ds(part * span + size, span - size), cols] = product[size:, :].astype(BF)

        one_scatter[part].start()

    def share_gain(flip):
        source = at_cols(gain_part, own ^ flip, width)
        return remote(source, at_rows(gain_recv, flip, 8), g_send.at[0], g_recv.at[0], "dp", own ^ flip)

    make_one(0)
    mlp_scatter[1].hop(1)

    send_qkv.wait_recv()
    drain(two_half, h_send.at[3])
    load_qkv = local(pair_qkv, normed.at[:, pl.ds(0, 3 * heads)], load.at[0])
    load_qkv.start()
    wait_all(early_loads + [load_half])
    out_grads()
    mlp_scatter[1].hop(2)
    load_qkv.wait()
    for slot in (3, 1, 2, 0):
        row_grads(3, slot, up_pair, two_half, d_qkv, normed, 3 * heads)
        if slot == 2:
            one_scatter[0].hop(0)
            make_one(1)
    for flip in range(1, 8):
        share_gain(flip).start()
    one_scatter[0].hop(1)
    one_scatter[0].hop(2)
    merge_grads(4)

    drain(gate_w.at[pl.ds(0, 2 * width), :], n_recv.at[0])
    drain(gate_w.at[pl.ds(0, 2 * width), :], n_recv.at[1])
    drain(gate_w.at[pl.ds(0, units // 4), :], d_recv.at[GROUPS])
    staged = [up_w.at[pl.ds(2 * index * width, 2 * width), :] for index in range(2)]
    sum_loads = [local(ref, staged[index], load.at[4 + index]) for index, ref in enumerate((gate_parts, up_parts))]
    for index in range(GROUPS):
        for slot in range(2):
            place = buffer_a.at[:, pl.ds((slot * GROUPS + index) * width, width)]
            sum_loads.append(local(down_rows(down_parts, index, slot), place, load.at[6]))
    start_all(sum_loads)

    def add_rows(index):
        total = piece(index, 0)
        sum_loads[index - 1].wait()

        @pl.loop(0, width // 32)
        def _(step):
            rows = cols_of(step, 32)
            near = pl.ds(pl.multiple_of(width + step * 32, 32), 32)
            terms = [total[rows, :], staged[index - 1][rows, :], staged[index - 1][near, :]]
            total[rows, :] = sum(term.astype(F32) for term in terms).astype(BF)

        local(total, (gate_sum, up_sum)[index - 1], keep.at[index]).start()

    def add_down():
        drain(buffer_a, load.at[6])

        @pl.loop(0, tokens // 64)
        def _(step):
            rows = cols_of(step, 64)
            for index in range(GROUPS):
                total = down_piece(0, index)
                terms = [total[rows, :]]
                terms += [buffer_a[rows, pl.ds((slot * GROUPS + index) * width, width)] for slot in range(2)]
                total[rows, :] = sum(term.astype(F32) for term in terms).astype(BF)

        for index in range(GROUPS):
            local(down_piece(0, index), down_rows(down_sum, index, 0), keep.at[8]).start()

    one_scatter[1].hop(0)
    add_rows(1)
    merge_grads(3)
    add_rows(2)
    one_scatter[1].hop(1)
    one_scatter[1].hop(2)
    add_down()

    drain(gain_recv.at[pl.ds(8, 56), :], g_recv.at[0])
    gain_sum = gain_part[:, pl.ds(pl.multiple_of(own * width, width), width)]
    for flip in range(1, 8):
        gain_sum = gain_sum + gain_recv[pl.ds(flip * 8, 8), :]
    gain_z[pl.ds(0, 8), :] = gain_sum

    def share_gain_z(k):
        target = gain_z.at[pl.ds(8 * k, 8), :]
        return remote(gain_z.at[pl.ds(0, 8), :], target, y_send.at[1], y_recv.at[1], "tensor", lax.rem(rank + k, 4))

    for k in (1, 2, 3):
        share_gain_z(k).start()

    load_own = [
        local(hidden_in.at[part_rows(part), :], sent.at[own_rows(part), :], load.at[4 + part]) for part in range(PARTS)
    ]
    for part in range(PARTS):
        gather_branch[part].finish()
    start_all(load_own)
    wait_all(load_own)
    for part in range(PARTS):
        one_scatter[part].wait()

        @pl.loop(0, size // 32)
        def _(step):
            rows = pl.ds(pl.multiple_of(part * size + step * 32, 32), 32)
            place = pl.ds(pl.multiple_of(part * span + step * 32, 32), 32)
            total = received(part, step * 32, 32, input_grad[rows, :])
            input_grad[rows, :] = grad_middle[rows, :] + norm_back(total, sent[place, :].astype(F32), gains[0:1, :])

    for scatter in mlp_scatter:
        scatter.wait()
    load_mlp = [
        [local(mlp_recv.at[arrived(part, slot), :], recv_part.at[arrived(part, slot), :], load.at[2 * part + index])
         for index, slot in enumerate((4, 2))]
        for part in range(PARTS)
    ]
    for part in range(PARTS):
        load_mlp[part][0].start()
        pl.when(inner(rank))(load_mlp[part][1].start)
    for part in range(PARTS):
        load_mlp[part][0].wait()
        pl.when(inner(rank))(load_mlp[part][1].wait)

        @pl.loop(0, size // 32)
        def _(step):
            rows = pl.ds(pl.multiple_of(part * size + step * 32, 32), 32)
            layer_out[rows, :] = received(part, step * 32, 32, middle[rows, :]).astype(BF)

    drain(gain_z.at[pl.ds(8, 24), :], y_recv.at[1])
    gain_all = gain_z[pl.ds(0, 8), :]
    for k in (1, 2, 3):
        gain_all = gain_all + gain_z[pl.ds(8 * k, 8), :]
    gain_total[...] = gain_all

    for scatter in mlp_scatter + one_scatter:
        scatter.finish()
    drain(gate_w.at[pl.ds(0, 3 * units // 8), :], d_send.at[0])
    drain(gain_recv.at[pl.ds(8, 56), :], y_send.at[0])
    drain(gain_recv.at[pl.ds(8, 56), :], g_send.at[0])
    drain(gain_z.at[pl.ds(8, 24), :], y_send.at[1])
    drain(two_half, h_send.at[1])
    drain(two_half, h_send.at[4])
    send_attended.wait_send()
    send_qkv.wait_send()
    def pieces(index, number):
        rows = number * width if index < 4 else number * heads * width // dim
        return gate_w.at[pl.ds(0, rows), pl.ds(0, 3 * heads if index == 3 else dim)]

    local(gate_w.at[pl.ds(0, width), :], gate_sum, keep.at[1]).wait()
    local(gate_w.at[pl.ds(0, width), :], up_sum, keep.at[2]).wait()
    drain(down_sum, keep.at[8])
    for index in range(1, 5):
        if index > 2:
            drain(pieces(index, 2), n_recv.at[index - 1])
            keep_grad(index).wait()
        drain(pieces(index, 3), w_send.at[index - 1])


def layer(hidden_in, cot, gains, weights, docs):
    tile, dim = hidden_in.shape
    tokens = 4 * tile
    width, heads = weights[0].shape
    units = weights[5].shape[1]
    dma = pltpu.SemaphoreType.DMA
    rows, narrow, ff = shape((tokens, dim), BF), shape((tokens, dim // 2), BF), shape((tokens, units), BF)
    weights_shape = [(units, width), (width, units), (width, units), (width, 3 * heads), (heads, width)]
    sums_shape = weights_shape[:3] + [(3 * width, 3 * heads), (heads, 3 * width)]
    parts_shape = [(units, 2 * width), (2 * width, units), (2 * width, units)]
    outs = [shape(dims, BF) for dims in sums_shape + parts_shape + weights_shape]
    outs += [ff] * 2 + [shape((tokens, 3 * heads), BF), shape((tokens, heads), BF), narrow, narrow]
    outs += [rows] * 3 + [shape((5 * tile, dim), BF), shape((dim, 3 * heads), BF), shape((units, dim), BF)]
    in_hbm = len(outs)
    outs += [shape((tile, dim), BF), shape((tile, dim), F32), shape((8, width), F32)]
    items = 4 + 3 * GROUPS
    scratch = [((dim, units), BF), ((dim, units), BF), ((units, dim), BF)]
    scratch += [((tokens, dim), BF)] * 3 + [((tokens, units), BF)] * 3
    scratch += [((tokens, dim // 2), BF)] * 2 + [((tokens, dim), BF)] * 3 + [((heads, dim), BF)]
    scratch += [((tokens, 3 * heads), BF)] + [((tokens, heads), BF)] * 2
    scratch += [((tokens, tokens), F32), ((tokens, 128), F32), ((tokens, 128), F32)]
    scratch += [((tokens, 1), F32), ((tokens, 1), F32), ((tile, dim), F32), ((tile, dim), F32)]
    scratch += [((tokens, dim), BF), ((5 * tile, dim), BF)]
    scratch += [((8, width), F32), ((8, dim), F32), ((8, dim), F32), ((64, width), F32), ((32, width), F32)]
    sems = [(2 + GROUPS,), (items, 3), (3,), (GROUPS + 2,), (6,), (6,)]
    sems += [(4, PARTS), (4, PARTS, 3), (4, PARTS), (4, PARTS, 5), (4,), (4, 2), (1,), (GROUPS + 1,)]
    sems += [(1,), (1,), (2,), (2,), (12,), (8 + GROUPS,), (GROUPS,), (2 + GROUPS,), (4,)]
    return pl.pallas_call(
        layer_kernel,
        out_shape=outs,
        in_specs=[anyspace()] * 2 + [vmem()] * 2 + [anyspace()] * 7 + [vmem()],
        out_specs=[anyspace()] * in_hbm + [vmem()] * 3,
        scratch_shapes=[pltpu.VMEM(*entry) for entry in scratch] + [dma(entry) for entry in sems],
        compiler_params=pltpu.CompilerParams(vmem_limit_bytes=67000000, collective_id=0, has_side_effects=True),
        cost_estimate=cost(2 * tokens * dim * units * 12, 100e6),
        name="layer",
    )(hidden_in, cot, *gains, *weights, docs)


def sum_kernel(counts, *refs):
    parts, plain_in = refs[:5], refs[5:7]
    down, gate, up, query, key, value, out, *plain_out = refs[7:16]
    staged, totals, plain, load, store = refs[16:21], refs[21:26], refs[26:28], refs[28], refs[29]
    loads = [pltpu.make_async_copy(parts[index], staged[index], load.at[index]) for index in range(5)]
    loads += [pltpu.make_async_copy(plain_in[index], plain[index], load.at[5 + index]) for index in range(2)]
    start_all(loads)
    heads = query.shape[1]
    stores = [pltpu.make_async_copy(totals[index], ref, store.at[index]) for index, ref in enumerate((down, gate, up))]
    qkv_stores = [
        pltpu.make_async_copy(totals[3].at[:, pl.ds(index * heads, heads)], ref, store.at[3 + index])
        for index, ref in enumerate((query, key, value))
    ]
    out_store = pltpu.make_async_copy(totals[4], out, store.at[6])
    plain_stores = [pltpu.make_async_copy(plain[index], plain_out[index], store.at[7 + index]) for index in range(2)]
    groups = [[stores[0]], [stores[1]], [stores[2]], qkv_stores, [out_store]]
    for index in range(5):
        loads[index].wait()
        rows_first = index in (1, 2, 3)
        rows, cols = totals[index].shape
        step_rows = 32 if rows_first else 256

        @pl.loop(0, rows // step_rows)
        def _(step):
            start = pl.multiple_of(step * step_rows, step_rows)
            total = None
            for slot in range(counts[index]):
                if rows_first:
                    term = staged[index][pl.ds(pl.multiple_of(start + slot * rows, step_rows), step_rows), :]
                else:
                    term = staged[index][pl.ds(start, step_rows), slot * cols : (slot + 1) * cols]
                term = term.astype(F32)
                total = term if total is None else total + term
            totals[index][pl.ds(start, step_rows), :] = total

        start_all(groups[index])
    for index in range(2):
        loads[5 + index].wait()
        plain_stores[index].start()
    for entry in groups + [plain_stores]:
        wait_all(entry)


def sum_grads(parts, plain, heads, counts):
    dims = [part.shape for part in parts]
    sums = [
        (rows // counts[index], cols) if index in (1, 2, 3) else (rows, cols // counts[index])
        for index, (rows, cols) in enumerate(dims)
    ]
    outs = sums[:3] + [(sums[3][0], heads)] * 3 + [sums[4]]
    dma = pltpu.SemaphoreType.DMA
    return pl.pallas_call(
        partial(sum_kernel, counts),
        out_shape=[shape(dim, F32) for dim in outs] + [shape(entry.shape, entry.dtype) for entry in plain],
        in_specs=[anyspace()] * 7,
        out_specs=[anyspace()] * 9,
        scratch_shapes=[pltpu.VMEM(dim, BF) for dim in dims]
        + [pltpu.VMEM(dim, F32) for dim in sums]
        + [pltpu.VMEM(entry.shape, entry.dtype) for entry in plain]
        + [dma((7,)), dma((9,))],
        compiler_params=params(),
        cost_estimate=cost(1e6, 22e6),
        name="sum_grads",
    )(*parts, *plain)


def shift(values, step):
    size = lax.axis_size("tensor")
    return lax.ppermute(values, "tensor", [(index, (index + step) % size) for index in range(size)])


def gather_rows(values):
    return [values] + [shift(values, step) for step in range(1, lax.axis_size("tensor"))]


def scatter_rows(parts):
    total = parts[0].astype(F32)
    for step in range(1, len(parts)):
        total = total + shift(parts[step], -step).astype(F32)
    return total


def gather_weight(values, axis):
    return [None], [lax.all_gather(values, "dp", axis=axis, tiled=True)]


def scatter_full(left, right, axis):
    full = dot_cols(left, right).astype(BF)
    return lax.psum_scatter(full, "dp", scatter_dimension=axis, tiled=True).astype(F32)


def frequencies():
    half_size = HEAD_DIM // 2
    return ROPE_BASE ** (-jnp.arange(half_size, dtype=F32) / half_size)


def rotary(length):
    angles = jnp.arange(length).astype(F32)[:, None] * frequencies()[None, :]
    cosine, sine = jnp.cos(angles), jnp.sin(angles)
    cosine = jnp.tile(cosine, (1, 8))
    sine = jnp.tile(jnp.concatenate([-sine, sine], axis=1), (1, 4))
    return cosine, sine


def position_tables(doc_ids, ranks):
    length = doc_ids.shape[0]
    token_index = jnp.arange(length, dtype=jnp.int32)
    before = jnp.concatenate([doc_ids[:1] - 1, doc_ids[:-1]])
    doc_start = lax.cummax(jnp.where(doc_ids != before, token_index, 0), axis=0)
    order = (lax.axis_index("tensor") - jnp.arange(ranks)) % ranks
    last = token_index.reshape(ranks, -1)[order].reshape(length)
    first = doc_start.reshape(ranks, -1)[order].reshape(length)
    cosine, sine = (table.reshape(ranks, -1, 256)[order].reshape(length, 256) for table in rotary(length))
    return cosine, sine, first[:, None], last[:, None], last[None, :]


def rms_back(grad_rows_, values, gain):
    inverse = lax.rsqrt(jnp.mean(values * values, axis=-1, keepdims=True) + EPSILON)
    scaled = grad_rows_ * gain
    return inverse * (scaled - values * inverse * inverse * jnp.mean(scaled * values, axis=-1, keepdims=True))


def body(
    hidden_in,
    out_cotangent,
    doc_ids,
    attn_gain,
    query_weight,
    key_weight,
    value_weight,
    out_weight,
    mlp_gain,
    gate_weight,
    up_weight,
    down_weight,
):
    ranks, groups = lax.axis_size("tensor"), lax.axis_size("dp")
    paired = (groups, ranks) == (8, 4)
    width, heads = query_weight.shape
    dim = hidden_in.shape[1]

    if paired:
        weights = (query_weight, key_weight, value_weight, out_weight, down_weight, gate_weight, up_weight)
        outs = layer(hidden_in, out_cotangent, (attn_gain, mlp_gain), weights, doc_ids.reshape(ranks, -1))
        sums = sum_grads(outs[:5], outs[-3:-1], heads, (1, 1, 1, 3, 3))
        down_grad, gate_grad, up_grad, query_grad, key_grad, value_grad, out_proj_grad, layer_out, input_grad = sums
        gain_total = outs[-1]
        share = width // ranks
        gain_grads = lax.dynamic_slice_in_dim(gain_total, lax.axis_index("tensor") * share, share, axis=1)
    else:
        tables = position_tables(doc_ids, ranks)
        input_local = hidden_in.astype(F32)
        hidden_rows = gather_rows(hidden_in)
        gains = lax.all_gather(jnp.stack([attn_gain, mlp_gain]), "dp", axis=1, tiled=True).astype(F32)
        attn_scale, mlp_scale = gains[:1], gains[1:]
        qkv_weight = jnp.concatenate([query_weight, key_weight, value_weight], axis=1)
        tags, qkv_pieces = gather_weight(qkv_weight, 0)
        tags, out_pieces = gather_weight(out_weight, 1)
        cot_rows = gather_rows(out_cotangent)
        tags, down_pieces = gather_weight(down_weight, 1)
        tags, gate_pieces = gather_weight(gate_weight, 0)
        tags, up_pieces = gather_weight(up_weight, 0)
        normed, qkv, attended, inverses, *branch_parts = attn_fwd(
            hidden_rows, attn_scale, tables, tags, width, qkv_pieces, out_pieces
        )
        middle = input_local + scatter_rows(branch_parts)
        sent = middle.astype(BF)
        sent_rows = gather_rows(sent)
        cot_full = jnp.concatenate(cot_rows, axis=0)
        normed_two, hidden, d_gate, d_up, mlp_gain_part, *two_parts = mlp(
            sent_rows, cot_rows, mlp_scale, tags, width, gate_pieces, up_pieces, down_pieces, ranks
        )
        grad_two_rows = scatter_rows(two_parts)
        grad_middle = out_cotangent.astype(F32) + rms_back(grad_two_rows, sent.astype(F32), mlp_scale)
        branch_rows = gather_rows(grad_middle.astype(BF))
        down_grad = scatter_full(hidden, cot_full, 1)
        gate_grad = scatter_full(normed_two, d_gate, 0)
        up_grad = scatter_full(normed_two, d_up, 0)
        mlp_rows = scatter_rows(mlp_out(hidden, ranks, dim, tags, width, down_pieces))
        layer_out = (middle + mlp_rows).astype(BF)
        branch_full, d_qkv, attn_gain_part, *one_parts = attn_bwd(
            branch_rows, hidden_rows, qkv, inverses, tables, tags, width, qkv_pieces, out_pieces, ranks
        )
        out_proj_grad = scatter_full(attended, branch_full, 1)
        query_grad, key_grad, value_grad = jnp.split(scatter_full(normed, d_qkv, 0), 3, axis=1)
        grad_one_rows = scatter_rows(one_parts)
        input_grad = grad_middle + rms_back(grad_one_rows, input_local, attn_scale)
        gain_parts = jnp.concatenate([attn_gain_part, mlp_gain_part], axis=0)
        gain_grads = lax.psum_scatter(gain_parts, ("dp", "tensor"), scatter_dimension=1, tiled=True)
    return (
        layer_out,
        input_grad,
        gain_grads[0],
        query_grad,
        key_grad,
        value_grad,
        out_proj_grad,
        gain_grads[1],
        gate_grad,
        up_grad,
        down_grad,
    )


def solution(mesh):
    return jax.shard_map(
        body,
        mesh=mesh,
        in_specs=(
            P(("dp", "tensor"), None),
            P(("dp", "tensor"), None),
            P("dp"),
            P("dp"),
            P("dp", "tensor"),
            P("dp", "tensor"),
            P("dp", "tensor"),
            P("tensor", "dp"),
            P("dp"),
            P("dp", "tensor"),
            P("dp", "tensor"),
            P("tensor", "dp"),
        ),
        out_specs=(
            P(("dp", "tensor"), None),
            P(("dp", "tensor"), None),
            P(("dp", "tensor")),
            P("dp", "tensor"),
            P("dp", "tensor"),
            P("dp", "tensor"),
            P("tensor", "dp"),
            P(("dp", "tensor")),
            P("dp", "tensor"),
            P("dp", "tensor"),
            P("tensor", "dp"),
        ),
        check_vma=False,
    )
```

```python
import math
from functools import partial

import jax
import jax.numpy as jnp
from jax import lax
from jax.experimental import pallas as pl
from jax.experimental.pallas import tpu as pltpu
from jax.sharding import PartitionSpec as P

HEAD_DIM = 64
EPSILON = 1e-05
ROPE_BASE = 130000.0
NEGATIVE = -1e30
VMEM_LIMIT = 63 * 1024 * 1024
BF = jnp.bfloat16
F32 = jnp.float32


def dot(left, right):
    return jnp.dot(left, right, preferred_element_type=F32)


def dot_rows(left, right):
    return lax.dot_general(left, right, (((1,), (1,)), ((), ())), preferred_element_type=F32)


def dot_cols(left, right):
    return lax.dot_general(left, right, (((0,), (0,)), ((), ())), preferred_element_type=F32)


def vmem():
    return pl.BlockSpec(memory_space=pltpu.VMEM)


def anyspace():
    return pl.BlockSpec(memory_space=pl.ANY)


def params():
    return pltpu.CompilerParams(vmem_limit_bytes=VMEM_LIMIT)


def cost(flops, nbytes):
    return pl.CostEstimate(flops=int(flops), bytes_accessed=int(nbytes), transcendentals=0)


def shape(dims, kind):
    return jax.ShapeDtypeStruct(dims, kind)


def place_copies(tags, pieces, target, sem, axis, width):
    own = lax.axis_index("dp")
    copies = []
    for slot, (tag, piece) in enumerate(zip(tags, pieces)):
        if tag is None:
            where = target
        else:
            start = pl.multiple_of((own ^ tag) * width, width)
            where = target.at[pl.ds(start, width), :] if axis == 0 else target.at[:, pl.ds(start, width)]
        copies.append(pltpu.make_async_copy(piece, where, sem.at[slot]))
    return copies


def row_copies(pieces, target, sem):
    copies = []
    for slot, piece in enumerate(pieces):
        rows = piece.shape[0]
        copies.append(pltpu.make_async_copy(piece, target.at[pl.ds(slot * rows, rows), :], sem.at[slot]))
    return copies


def start_all(copies):
    for copy in copies:
        copy.start()


def wait_all(copies):
    for copy in copies:
        copy.wait()


def turn(values, cosine, sine):
    width = values.shape[1]
    lane = lax.broadcasted_iota(jnp.int32, values.shape, 1)
    partner = jnp.where(
        lax.rem(lane, HEAD_DIM) < HEAD_DIM // 2,
        pltpu.roll(values, width - HEAD_DIM // 2, 1),
        pltpu.roll(values, HEAD_DIM // 2, 1),
    )
    return values * cosine + partner * sine


def norm_rows(source, target, inverses, gain, tile):
    @pl.loop(0, source.shape[0] // tile)
    def _(step):
        rows = pl.ds(pl.multiple_of(step * tile, tile), tile)
        values = source[rows, :].astype(F32)
        inverse = lax.rsqrt(jnp.mean(values * values, axis=-1, keepdims=True) + EPSILON)
        inverses[rows, :] = inverse
        target[rows, :] = (values * inverse * gain[...]).astype(BF)


def fill_bias(bias, first, last, key_index):
    keys = key_index[...]
    bias[...] = jnp.where((keys >= first[...]) & (keys <= last[...]), 0.0, NEGATIVE)


def head_lanes(width, half):
    lane = lax.broadcasted_iota(jnp.int32, (1, width), 1)
    return (lax.div(lane, HEAD_DIM) == half).astype(F32)


def probabilities(query, key, bias):
    scores = dot_rows(query, key) + bias
    weights = jnp.exp(scores - jnp.max(scores, axis=-1, keepdims=True))
    return weights * (1.0 / jnp.sum(weights, axis=-1, keepdims=True))


def attend(qkv, attended, bias, heads):
    @pl.loop(0, heads // 128)
    def _(pair):
        base = pl.multiple_of(pair * 128, 128)
        query = qkv[:, pl.ds(base, 128)]
        key = qkv[:, pl.ds(heads + base, 128)]
        value = qkv[:, pl.ds(2 * heads + base, 128)]
        total = None
        for half in range(2):
            lanes = head_lanes(128, half).astype(BF)
            probs = probabilities(query * (lanes * HEAD_DIM ** (-0.5)), key, bias[...])
            term = dot(probs.astype(BF), value * lanes)
            total = term if total is None else total + term
        attended[:, pl.ds(base, 128)] = total.astype(BF)


def attn_fwd_kernel(tags, width, nrow, *refs):
    npiece = len(tags)
    rows_in = refs[:nrow]
    gain, cosine, sine, first, last, key_index = refs[nrow : nrow + 6]
    rest = refs[nrow + 6 :]
    qkv_in, out_in = rest[:npiece], rest[npiece : 2 * npiece]
    rest = rest[2 * npiece :]
    normed, qkv, attended, inverses = rest[:4]
    parts = rest[4 : 4 + nrow]
    hidden, qkv_w, out_w, bias, sem_rows, sem_qkv, sem_out = rest[4 + nrow :]
    load_rows = row_copies(rows_in, hidden, sem_rows)
    load_qkv = place_copies(tags, qkv_in, qkv_w, sem_qkv, 0, width)
    load_out = place_copies(tags, out_in, out_w, sem_out, 1, width)
    start_all(load_rows + load_qkv + load_out)
    fill_bias(bias, first, last, key_index)
    wait_all(load_rows)
    norm_rows(hidden, normed, inverses, gain, 64)
    wait_all(load_qkv)
    heads = attended.shape[1]
    step_cols = 256

    @pl.loop(0, 2 * heads // step_cols)
    def _(step):
        cols = pl.ds(pl.multiple_of(step * step_cols, step_cols), step_cols)
        qkv[:, cols] = turn(dot(normed[...], qkv_w[:, cols]), cosine[...], sine[...]).astype(BF)

    @pl.loop(2 * heads // step_cols, 3 * heads // step_cols)
    def _(step):
        cols = pl.ds(pl.multiple_of(step * step_cols, step_cols), step_cols)
        qkv[:, cols] = dot(normed[...], qkv_w[:, cols]).astype(BF)

    attend(qkv, attended, bias, heads)
    wait_all(load_out)
    tile = parts[0].shape[0]

    @pl.loop(0, out_w.shape[1] // step_cols)
    def _(step):
        cols = pl.ds(pl.multiple_of(step * step_cols, step_cols), step_cols)
        product = dot(attended[...], out_w[:, cols])
        for slot, part in enumerate(parts):
            part[:, cols] = product[slot * tile : (slot + 1) * tile, :].astype(part.dtype)


def attn_fwd(rows, gain, tables, tags, width, qkv_pieces, out_pieces):
    nrow, (tile, dim) = len(rows), rows[0].shape
    tokens = nrow * tile
    heads = out_pieces[0].shape[0]
    npiece = len(tags)
    return pl.pallas_call(
        partial(attn_fwd_kernel, tags, width, nrow),
        out_shape=[
            shape((tokens, dim), BF),
            shape((tokens, 3 * heads), BF),
            shape((tokens, heads), BF),
            shape((tokens, 1), F32),
        ]
        + [shape((tile, dim), F32 if slot == 0 else BF) for slot in range(nrow)],
        in_specs=[anyspace()] * nrow + [vmem()] * 6 + [anyspace()] * (2 * npiece),
        out_specs=[vmem()] * (4 + nrow),
        scratch_shapes=[
            pltpu.VMEM((tokens, dim), BF),
            pltpu.VMEM((dim, 3 * heads), BF),
            pltpu.VMEM((heads, dim), BF),
            pltpu.VMEM((tokens, tokens), F32),
            pltpu.SemaphoreType.DMA((nrow,)),
            pltpu.SemaphoreType.DMA((npiece,)),
            pltpu.SemaphoreType.DMA((npiece,)),
        ],
        compiler_params=params(),
        cost_estimate=cost(2 * tokens * dim * 4 * heads * 3, 20e6),
        name="attn_fwd",
    )(*rows, gain, *tables, *qkv_pieces, *out_pieces)


def attend_back(qkv, d_attended, d_qkv, bias, cosine, sine, heads):
    score_scale = HEAD_DIM ** (-0.5)

    @pl.loop(0, heads // 128)
    def _(pair):
        base = pl.multiple_of(pair * 128, 128)
        query = qkv[:, pl.ds(base, 128)]
        key = qkv[:, pl.ds(heads + base, 128)]
        value = qkv[:, pl.ds(2 * heads + base, 128)]
        grad = d_attended[:, pl.ds(base, 128)]
        sums = [0.0, 0.0, 0.0]
        for half in range(2):
            lanes = head_lanes(128, half).astype(BF)
            own_query = query * (lanes * score_scale)
            own_grad = grad * lanes
            probs = probabilities(own_query, key, bias[...])
            d_value = dot_cols(probs.astype(BF), own_grad)
            d_probs = dot_rows(own_grad, value)
            delta = jnp.sum(probs * d_probs, axis=-1, keepdims=True)
            d_scores = (probs * (d_probs - delta)).astype(BF)
            d_query = dot(d_scores, key * lanes) * score_scale
            d_key = dot_cols(d_scores, own_query)
            sums = [sums[0] + d_query, sums[1] + d_key, sums[2] + d_value]
        back = -sine[:, :128]
        d_qkv[:, pl.ds(base, 128)] = turn(sums[0], cosine[:, :128], back).astype(BF)
        d_qkv[:, pl.ds(heads + base, 128)] = turn(sums[1], cosine[:, :128], back).astype(BF)
        d_qkv[:, pl.ds(2 * heads + base, 128)] = sums[2].astype(BF)


def attn_bwd_kernel(tags, width, nrow, npart, *refs):
    npiece = len(tags)
    nhid, nrow = nrow[1], nrow[0]
    rows_in, hidden_in = refs[:nrow], refs[nrow : nrow + nhid]
    refs = refs[nrow + nhid :]
    qkv, inverses, cosine, sine, first, last, key_index = refs[:7]
    rest = refs[7:]
    qkv_in, out_in = rest[:npiece], rest[npiece : 2 * npiece]
    rest = rest[2 * npiece :]
    branch, d_qkv, gain_grad = rest[:3]
    parts = rest[3 : 3 + npart]
    hidden, d_attended, qkv_w, out_w, bias, sem_rows, sem_x, sem_qkv, sem_out = rest[3 + npart :]
    load_rows = row_copies(rows_in, branch, sem_rows)
    load_x = row_copies(hidden_in, hidden, sem_x)
    load_out = place_copies(tags, out_in, out_w, sem_out, 1, width)
    load_qkv = place_copies(tags, qkv_in, qkv_w, sem_qkv, 0, width)
    start_all(load_rows + load_out + load_qkv + load_x)
    fill_bias(bias, first, last, key_index)
    wait_all(load_rows)
    wait_all(load_out)
    heads = out_w.shape[0]
    step_cols = 256

    @pl.loop(0, heads // step_cols)
    def _(step):
        cols = pl.ds(pl.multiple_of(step * step_cols, step_cols), step_cols)
        d_attended[:, cols] = dot_rows(branch[...], out_w[cols, :]).astype(BF)

    attend_back(qkv, d_attended, d_qkv, bias, cosine, sine, heads)
    wait_all(load_qkv)
    wait_all(load_x)
    tile = parts[0].shape[0]

    @pl.loop(0, qkv_w.shape[0] // step_cols)
    def _(step):
        cols = pl.ds(pl.multiple_of(step * step_cols, step_cols), step_cols)
        product = dot_rows(d_qkv[...], qkv_w[cols, :])
        gain_grad[:, cols] = jnp.sum(product * (hidden[:, cols].astype(F32) * inverses[...]), axis=0, keepdims=True)
        for slot, part in enumerate(parts):
            part[:, cols] = product[slot * tile : (slot + 1) * tile, :].astype(part.dtype)


def attn_bwd(rows, hidden, qkv, inverses, tables, tags, width, qkv_pieces, out_pieces, npart):
    nrow, nhid, dim = len(rows), len(hidden), rows[0].shape[1]
    tokens = qkv.shape[0]
    tile = tokens // npart
    heads = out_pieces[0].shape[0]
    npiece = len(tags)
    return pl.pallas_call(
        partial(attn_bwd_kernel, tags, width, (nrow, nhid), npart),
        out_shape=[shape((tokens, dim), BF), shape((tokens, 3 * heads), BF), shape((1, dim), F32)]
        + [shape((tile, dim), F32 if slot == 0 else BF) for slot in range(npart)],
        in_specs=[anyspace()] * (nrow + nhid) + [vmem()] * 7 + [anyspace()] * (2 * npiece),
        out_specs=[vmem()] * (3 + npart),
        scratch_shapes=[
            pltpu.VMEM((tokens, dim), BF),
            pltpu.VMEM((tokens, heads), BF),
            pltpu.VMEM((dim, 3 * heads), BF),
            pltpu.VMEM((heads, dim), BF),
            pltpu.VMEM((tokens, tokens), F32),
            pltpu.SemaphoreType.DMA((nrow,)),
            pltpu.SemaphoreType.DMA((nhid,)),
            pltpu.SemaphoreType.DMA((npiece,)),
            pltpu.SemaphoreType.DMA((npiece,)),
        ],
        compiler_params=params(),
        cost_estimate=cost(2 * tokens * dim * 4 * heads * 6, 30e6),
        name="attn_bwd",
    )(*rows, *hidden, qkv, inverses, *tables, *qkv_pieces, *out_pieces)


def mlp_kernel(tags, width, nrow, npart, *refs):
    npiece = len(tags)
    sent_in, cot_in = refs[:nrow], refs[nrow : 2 * nrow]
    gain = refs[2 * nrow]
    rest = refs[2 * nrow + 1 :]
    gate_in, up_in, down_in = rest[:npiece], rest[npiece : 2 * npiece], rest[2 * npiece : 3 * npiece]
    rest = rest[3 * npiece :]
    normed, hidden, d_gate, d_up, gain_grad = rest[:5]
    parts = rest[5 : 5 + npart]
    sent, cot, inverses, gate_w, up_w, down_w, sem_sent, sem_cot, sem_gate, sem_up, sem_down = rest[5 + npart :]
    load_sent = row_copies(sent_in, sent, sem_sent)
    load_cot = row_copies(cot_in, cot, sem_cot)
    load_gate = place_copies(tags, gate_in, gate_w, sem_gate, 0, width)
    load_up = place_copies(tags, up_in, up_w, sem_up, 0, width)
    load_down = place_copies(tags, down_in, down_w, sem_down, 1, width)
    start_all(load_sent + load_cot + load_gate + load_up + load_down)
    wait_all(load_sent)
    norm_rows(sent, normed, inverses, gain, 64)
    wait_all(load_cot)
    wait_all(load_gate)
    wait_all(load_up)
    wait_all(load_down)
    step_cols = 256

    @pl.loop(0, gate_w.shape[1] // step_cols)
    def _(step):
        cols = pl.ds(pl.multiple_of(step * step_cols, step_cols), step_cols)
        gate = dot(normed[...], gate_w[:, cols])
        up = dot(normed[...], up_w[:, cols])
        d_hidden = dot_rows(cot[...], down_w[cols, :])
        s = jax.nn.sigmoid(gate)
        activated = gate * s
        hidden[:, cols] = (activated * up).astype(BF)
        d_gate[:, cols] = (d_hidden * up * (s + activated * (1.0 - s))).astype(BF)
        d_up[:, cols] = (d_hidden * activated).astype(BF)

    tile = parts[0].shape[0]

    @pl.loop(0, gate_w.shape[0] // step_cols)
    def _(step):
        cols = pl.ds(pl.multiple_of(step * step_cols, step_cols), step_cols)
        product = dot_rows(d_gate[...], gate_w[cols, :]) + dot_rows(d_up[...], up_w[cols, :])
        gain_grad[:, cols] = jnp.sum(product * (sent[:, cols].astype(F32) * inverses[...]), axis=0, keepdims=True)
        for slot, part in enumerate(parts):
            part[:, cols] = product[slot * tile : (slot + 1) * tile, :].astype(part.dtype)


def mlp(sent, cot, gain, tags, width, gate_pieces, up_pieces, down_pieces, npart):
    nrow, dim = len(sent), sent[0].shape[1]
    tokens = nrow * sent[0].shape[0]
    tile = tokens // npart
    units = gate_pieces[0].shape[1]
    npiece = len(tags)
    return pl.pallas_call(
        partial(mlp_kernel, tags, width, nrow, npart),
        out_shape=[shape((tokens, dim), BF)]
        + [shape((tokens, units), BF)] * 3
        + [shape((1, dim), F32)]
        + [shape((tile, dim), F32 if slot == 0 else BF) for slot in range(npart)],
        in_specs=[anyspace()] * (2 * nrow) + [vmem()] + [anyspace()] * (3 * npiece),
        out_specs=[vmem()] * (5 + npart),
        scratch_shapes=[
            pltpu.VMEM((tokens, dim), BF),
            pltpu.VMEM((tokens, dim), BF),
            pltpu.VMEM((tokens, 1), F32),
            pltpu.VMEM((dim, units), BF),
            pltpu.VMEM((dim, units), BF),
            pltpu.VMEM((units, dim), BF),
            pltpu.SemaphoreType.DMA((nrow,)),
            pltpu.SemaphoreType.DMA((nrow,)),
            pltpu.SemaphoreType.DMA((npiece,)),
            pltpu.SemaphoreType.DMA((npiece,)),
            pltpu.SemaphoreType.DMA((npiece,)),
        ],
        compiler_params=params(),
        cost_estimate=cost(2 * tokens * dim * units * 5, 40e6),
        name="mlp",
    )(*sent, *cot, gain, *gate_pieces, *up_pieces, *down_pieces)


def mlp_out_kernel(tags, width, *refs):
    npiece = len(tags)
    hidden, down_in = refs[0], refs[1 : 1 + npiece]
    *parts, down_w, sem_down = refs[1 + npiece :]
    load_down = place_copies(tags, down_in, down_w, sem_down, 1, width)
    start_all(load_down)
    wait_all(load_down)
    tile, step_cols = parts[0].shape[0], 256

    @pl.loop(0, down_w.shape[1] // step_cols)
    def _(step):
        cols = pl.ds(pl.multiple_of(step * step_cols, step_cols), step_cols)
        product = dot(hidden[...], down_w[:, cols])
        for slot, part in enumerate(parts):
            part[:, cols] = product[slot * tile : (slot + 1) * tile, :].astype(part.dtype)


def mlp_out(hidden, nrow, dim, tags, width, down_pieces):
    tokens, units = hidden.shape
    tile, npiece = tokens // nrow, len(tags)
    return pl.pallas_call(
        partial(mlp_out_kernel, tags, width),
        out_shape=[shape((tile, dim), F32 if slot == 0 else BF) for slot in range(nrow)],
        in_specs=[vmem()] + [anyspace()] * npiece,
        out_specs=[vmem()] * nrow,
        scratch_shapes=[pltpu.VMEM((units, dim), BF), pltpu.SemaphoreType.DMA((npiece,))],
        compiler_params=params(),
        cost_estimate=cost(2 * tokens * dim * units, 14e6),
        name="mlp_out",
    )(hidden, *down_pieces)


def slice_of(slot, width, own):
    index = lax.axis_index("dp")
    owner = index ^ (2 * slot)
    return pl.ds(pl.multiple_of((owner if own else lax.div(owner, 2)) * width, width), width)

MESH = pl.DeviceIdType.MESH
NEAR = (2, 4, 6)
PARTS = 2
GROUPS = 4


def remote(source, target, send_sem, recv_sem, axis, peer):
    return pltpu.make_async_remote_copy(
        src_ref=source,
        dst_ref=target,
        send_sem=send_sem,
        recv_sem=recv_sem,
        device_id={axis: peer},
        device_id_type=MESH,
    )


def drain(ref, sem):
    pltpu.make_async_copy(ref, ref, sem).wait()


def meet():
    own, rank = lax.axis_index("dp"), lax.axis_index("tensor")
    barrier = pltpu.get_barrier_semaphore()
    for flip in range(1, 8):
        pl.semaphore_signal(barrier, inc=1, device_id={"dp": own ^ flip}, device_id_type=MESH)

    @pl.when(rank < 3)
    def _():
        pl.semaphore_signal(barrier, inc=1, device_id={"tensor": rank + 1}, device_id_type=MESH)

    @pl.when(rank > 0)
    def _():
        pl.semaphore_signal(barrier, inc=1, device_id={"tensor": rank - 1}, device_id_type=MESH)

    pl.semaphore_wait(barrier, 8 + lax.div(rank * (3 - rank), 2))


def at_cols(ref, index, width):
    return ref.at[:, pl.ds(pl.multiple_of(index * width, width), width)]


def at_rows(ref, index, width):
    return ref.at[pl.ds(pl.multiple_of(index * width, width), width), :]


def either(rank, *choices):
    result = rank == choices[0]
    for choice in choices[1:]:
        result = result | (rank == choice)
    return result


def ends(rank):
    return either(rank, 0, 3)


def inner(rank):
    return either(rank, 1, 2)


class RowGather:
    def __init__(self, rank, source, landing, part, size, send, recv):
        self.rank = rank

        def place(slot):
            return landing.at[pl.ds(pl.multiple_of((4 * part + slot) * size, size), size), :]

        def copy(origin, slot, peer):
            return remote(origin, place(slot), send.at[part], recv.at[part, slot - 1], "tensor", peer)

        def forward(slot, target, peer):
            return copy(place(slot), target, peer)

        outward, inward = (rank - 1) * 3, 3 - rank
        near, far = 5 - 2 * rank, 2 * rank - 1
        self.up, self.down = copy(source, 1, rank + 1), copy(source, 3, rank - 1)
        self.hops = [forward(near, 2, outward), forward(far, 2, inward), forward(2, far, outward)]
        self.slots = [near, far, 2]
        self.arrival = lambda slot: copy(source, slot, lax.rem(rank + 1, 4))
        self.sent = lambda count: drain(landing.at[pl.ds(0, count * size), :], send.at[part])

    def start(self):
        pl.when(self.rank < 3)(self.up.start)
        pl.when(self.rank > 0)(self.down.start)

    def hop(self, index):
        @pl.when(inner(self.rank))
        def _():
            self.arrival(self.slots[index]).wait_recv()
            self.hops[index].start()

    def wait(self):
        @pl.when(ends(self.rank))
        def _():
            for slot in (1, 2, 3):
                self.arrival(slot).wait_recv()

    def finish(self):
        pl.when(ends(self.rank))(lambda: self.sent(1))
        pl.when(inner(self.rank))(lambda: self.sent(5))


class RowScatter:
    def __init__(self, rank, source, landing, part, size, send, recv, staged=None, sem=None):
        self.rank, self.source, self.size, self.staged, self.sem = rank, source, size, staged, sem
        self.place = lambda k: pl.ds(pl.multiple_of((4 * part + k) * size, size), size)
        self.land = lambda slot: landing.at[pl.ds((5 * part + slot) * size, size), :]

        def copy(k, slot, peer):
            return remote(source.at[self.place(k), :], self.land(slot), send.at[part], recv.at[part, slot], "tensor", peer)

        end = lax.div(rank, 3)
        self.first = [copy(index + 1 + end * (2 - 2 * index), index, 1 + end) for index in range(3)]
        self.keys = [2, 5 - 2 * rank, 2 * rank - 1]
        self.later = [
            copy(self.keys[0], 3, 3 - rank),
            copy(self.keys[1], 4, 3 - rank),
            copy(self.keys[2], 4, (rank - 1) * 3),
        ]
        self.arrival = lambda slot: copy(1, slot, lax.rem(rank + 1, 4))
        self.finish = lambda: drain(source.at[pl.ds(0, 3 * size), :], send.at[part])

    def start(self, indices=(0, 1, 2)):
        @pl.when(ends(self.rank))
        def _():
            for index in indices:
                self.first[index].start()

    def hop(self, index):
        @pl.when(inner(self.rank))
        def _():
            slot = (0, 1, 3)[index]
            self.arrival(slot).wait_recv()
            other = self.land(slot)
            if self.staged is not None:
                load = pltpu.make_async_copy(other, self.staged, self.sem)
                load.start()
                load.wait()
                other = self.staged
            target = self.source.at[self.place(self.keys[index]), :]

            @pl.loop(0, self.size // 16)
            def _(step):
                rows = pl.ds(pl.multiple_of(step * 16, 16), 16)
                target[rows, :] = (target[rows, :].astype(F32) + other[rows, :].astype(F32)).astype(BF)

            self.later[index].start()

    def wait(self):
        pl.when(inner(self.rank))(self.arrival(2).wait_recv)
        self.arrival(4).wait_recv()


def fill_mask(bias, docs, size):
    rank = lax.axis_index("tensor")
    tokens = bias.shape[0]
    values = docs[...]
    starts = [jnp.sum(jnp.where(values < number, 1, 0), keepdims=True) for number in range(1, 8)]

    def document(position):
        return sum(jnp.where(position >= start, 1, 0) for start in starts)

    lane = lax.broadcasted_iota(jnp.int32, (1, tokens), 1)
    slot = lax.rem(lax.div(lane, size), 4)
    part = lax.div(lane, 4 * size)
    keys = lax.rem(rank - slot + 4, 4) * (2 * size) + part * size + lax.rem(lane, size)
    key_docs = document(keys)

    @pl.loop(0, tokens // size)
    def _(block):
        base = lax.rem(rank - lax.rem(block, 4) + 4, 4) * (2 * size) + lax.div(block, 4) * size
        queries = base + lax.broadcasted_iota(jnp.int32, (size, 1), 0)
        allowed = (document(queries) == key_docs) & (queries >= keys)
        bias[pl.ds(pl.multiple_of(block * size, size), size), :] = jnp.where(allowed, 0.0, NEGATIVE)


def fill_turns(cosine, sine, size):
    rank = lax.axis_index("tensor")
    half_size = HEAD_DIM // 2
    dims = (size, cosine.shape[1])
    lane = lax.broadcasted_iota(jnp.int32, dims, 1)
    row = lax.broadcasted_iota(jnp.int32, dims, 0)
    frequency = jnp.exp(lax.rem(lane, half_size).astype(F32) * (-math.log(ROPE_BASE) / half_size))
    sign = jnp.where(lax.rem(lane, HEAD_DIM) < half_size, -1.0, 1.0)

    @pl.loop(0, cosine.shape[0] // size)
    def _(block):
        start = (lax.rem(rank - lax.rem(block, 4) + 4, 4) * PARTS + lax.div(block, 4)) * size
        angles = (row + start).astype(F32) * frequency
        rows = pl.ds(pl.multiple_of(block * size, size), size)
        cosine[rows, :] = jnp.cos(angles)
        sine[rows, :] = jnp.sin(angles) * sign


def slice_of(slot, width, own):
    index = lax.axis_index("dp")
    owner = index ^ (2 * slot)
    return pl.ds(pl.multiple_of((owner if own else lax.div(owner, 2)) * width, width), width)


def layer_kernel(*refs):
    hidden_in, cot_in, *plain_gains = refs[:4]
    weights_in = refs[4:11]
    docs = refs[11]
    down_sum, gate_sum, up_sum, qkv_parts, out_parts = refs[12:17]
    down_parts, gate_parts, up_parts = refs[17:20]
    grad_merge = refs[20:25]
    pair_gate, pair_up, pair_qkv, pair_attended, pair_normed, pair_branch = refs[25:31]
    branch_rows, hidden_rows, normed_rows, mlp_recv, qkv_full, down_full = refs[31:37]
    out_ref, input_ref, gain_total = refs[37:40]
    gate_w, up_w, down_w, sent, cot, normed, hidden, d_gate, d_up = refs[40:49]
    two_half, cot_half, buffer_a, buffer_b, buffer_c, out_w = refs[49:55]
    qkv, attended, d_attended, bias, cosine, sine = refs[55:61]
    inverses_one, inverses, middle, grad_middle, send_part, recv_part = refs[61:67]
    gains_in, gains, gain_part, gain_recv, gain_z, layer_out, input_grad = refs[67:74]
    a_send, a_recv, f_send, f_recv, h_send, h_recv, z_send, z_recv, r_send, r_recv = refs[74:84]
    w_send, w_recv, d_send, d_recv, g_send, g_recv, y_send, y_recv, load, keep, down_load, s_recv, n_recv = refs[84:]

    own, rank = lax.axis_index("dp"), lax.axis_index("tensor")
    core = lax.rem(own, 2)
    tokens, dim = sent.shape
    units = gate_w.shape[1]
    tile = hidden_in.shape[0]
    size = tile // PARTS
    span = 4 * size
    heads = attended.shape[1]
    width = weights_in[0].shape[0]
    half = dim // (2 * width)
    d_qkv = cot.at[:, pl.ds(heads, 3 * heads)]
    group = units // GROUPS
    step_cols = 256
    count = dim // step_cols

    def cols_of(step, length=step_cols):
        return pl.ds(pl.multiple_of(step * length, length), length)

    def local(source, target, sem):
        return pltpu.make_async_copy(source, target, sem)

    def own_rows(part):
        return pl.ds(part * span, size)

    def part_rows(part):
        return pl.ds(part * size, size)

    def source_of(item):
        if item < 4:
            return weights_in[item]
        which, start = (item - 4) % 3, ((item - 4) // 3) * group
        if which == 2:
            return weights_in[4].at[pl.ds(start, group), :]
        return weights_in[5 + which].at[:, pl.ds(start, group)]

    def view(item, owner, part=None):
        rows = heads if item == 3 else group if item > 3 and (item - 4) % 3 == 2 else width
        length = rows if part is None else rows // 2
        start = 0 if part is None else part * length
        if item < 3:
            place = pl.ds(pl.multiple_of(owner * width + start, length), length)
            return down_w.at[place, pl.ds(item * heads, heads)]
        if item == 3:
            return out_w.at[pl.ds(start, length), pl.ds(pl.multiple_of(owner * width, width), width)]
        which, offset = (item - 4) % 3, ((item - 4) // 3) * group
        if which == 2:
            return down_full.at[pl.ds(offset + start, length), pl.ds(pl.multiple_of(owner * width, width), width)]
        place = pl.ds(pl.multiple_of(owner * width + start, length), length)
        return (gate_w, up_w)[which].at[place, pl.ds(offset, group)]

    def phase_of(item):
        return 0 if item < 3 else 1 if item == 3 else 2 + (item - 4) // 3

    def lot_of(item):
        return item if item < 4 else 4 + (item - 4) // 3

    def send_weight(item, flip):
        sem = s_recv.at[phase_of(item)] if flip == 1 else a_recv.at[lot_of(item), flip // 2 - 1]
        return remote(source_of(item), view(item, own), a_send.at[phase_of(item)], sem, "dp", own ^ flip)

    def relay_weight(item, part):
        place = view(item, own ^ (4 - 2 * part), part)
        return remote(place, place, a_send.at[phase_of(item)], a_recv.at[lot_of(item), 2], "dp", own ^ (2 + 2 * part))

    def pass_weight(item, flip):
        place = view(item, own ^ flip)
        return remote(place, place, a_send.at[phase_of(item)], s_recv.at[phase_of(item)], "dp", own ^ 1)

    def send_weights(items):
        for item in items:
            for flip in (2, 4, 1):
                send_weight(item, flip).start()

    def lots(items):
        return [[item] for item in items] if items[0] < 4 else [items]

    def arrived_weights(lot, tag):
        drain(gate_w.at[pl.ds(0, len(lot) * width // 4), :], a_recv.at[lot_of(lot[0]), tag])

    def relay_weights(items):
        for lot in lots(items):
            arrived_weights(lot, 1)
            for item in lot:
                relay_weight(item, 0).start()
            arrived_weights(lot, 0)
            for item in lot:
                relay_weight(item, 1).start()
            for item in lot:
                pass_weight(item, 4).start()
                pass_weight(item, 2).start()

    def pass_weights(items):
        for lot in lots(items):
            arrived_weights(lot, 2)
            for item in lot:
                pass_weight(item, 6).start()

    def have_weights(phase):
        drain(gate_w.at[pl.ds(0, width if phase == 1 else 3 * width), :], s_recv.at[phase])

    def sent_weights(phase):
        length = 7 * width // 4
        drain(gate_w.at[pl.ds(0, length if phase == 1 else 3 * length), :], a_send.at[phase])

    def items_of(index):
        return list(range(4 + 3 * index, 7 + 3 * index))

    def send_gain(flip):
        return remote(gains_in, at_cols(gains, own, width), y_send.at[0], y_recv.at[0], "dp", own ^ flip)

    def gathers(kind, source, landing):
        return [
            RowGather(rank, source(part), landing, part, size, z_send.at[kind], z_recv.at[kind]) for part in range(PARTS)
        ]

    gather_hidden = gathers(0, lambda part: hidden_in.at[part_rows(part), :], buffer_b)
    gather_cot = gathers(1, lambda part: cot_in.at[part_rows(part), :], cot)
    gather_sent = gathers(0, lambda part: sent.at[own_rows(part), :], sent)
    gather_branch = gathers(0, lambda part: sent.at[own_rows(part), :], branch_rows)

    def scatters(kind, source, landing, staged=None, sem=None):
        return [
            RowScatter(rank, source, landing, part, size, r_send.at[kind], r_recv.at[kind], staged, sem)
            for part in range(PARTS)
        ]

    gate_stage = up_w.at[pl.ds(4 * width, size), :]
    out_scatter = scatters(0, send_part, recv_part)
    two_scatter = scatters(0, send_part, recv_part)
    mlp_scatter = scatters(1, sent, mlp_recv, gate_stage, load.at[3])
    one_scatter = scatters(0, send_part, recv_part)

    def arrived(part, slot):
        return pl.ds((5 * part + slot) * size, size)

    def clear(part):
        @pl.when(ends(rank))
        def _():
            recv_part[arrived(part, 2), :] = jnp.zeros((size, dim), BF)

    def received(part, start, length, base):
        total = base
        for slot in (2, 4):
            rows = pl.ds(pl.multiple_of((5 * part + slot) * size + start, length), length)
            total = total + recv_part[rows, :].astype(F32)
        return total

    def to_pair(source, target, row, slot):
        return remote(source, target, h_send.at[row], h_recv.at[row], "dp", own ^ 1)

    def halves(source, target, row):
        return [
            to_pair(at_cols(source, 2 * slot + 1 - core, width), at_cols(target, slot, width), row, slot)
            for slot in range(half)
        ]

    def send_ff(step, which):
        cols = cols_of(step)
        source = (hidden, d_gate, d_up)[which].at[:, cols]
        target = (buffer_a, pair_gate, pair_up)[which].at[:, cols]
        arrival = lax.div(step, group // step_cols) if which == 0 else GROUPS - 1 + which
        return remote(source, target, f_send.at[which], f_recv.at[arrival], "dp", own ^ 1)

    def piece(index, slot):
        if index < 3:
            return at_rows(gate_w, (index - 1) * 4 + slot, width)
        if index == 3:
            return (hidden, d_gate)[slot // 2].at[pl.ds((slot % 2) * width, width), pl.ds(0, 3 * heads)]
        return at_cols(d_up, slot, width)

    def landing_of(index, slot):
        ref = (down_parts, gate_parts, up_parts, qkv_parts, out_parts)[index]
        if index < 3:
            return at_rows(ref, slot - 1, width)
        return at_cols(ref, slot, width) if index == 4 else at_rows(ref, slot, width)

    def half_of(ref, index, part):
        rows, cols = ref.shape
        if index == 4:
            return ref.at[pl.ds(part * (rows // 2), rows // 2), :]
        return ref.at[:, pl.ds(part * (cols // 2), cols // 2)]

    def stage_of(index, part):
        if index == 4:
            return up_w.at[pl.ds(7 * width, heads // 2), pl.ds(part * width, width)]
        length = units // 2 if index < 3 else 3 * heads // 2
        return up_w.at[pl.ds((3 + index) * width, width), pl.ds(part * (units // 2), length)]

    def send_far(index, part):
        return remote(
            half_of(piece(index, 3), index, part),
            half_of(grad_merge[index], index, part),
            w_send.at[index - 1],
            w_recv.at[index - 1, part],
            "dp",
            own ^ (2 + 2 * part),
        )

    def send_near(index, slot, part):
        return remote(
            half_of(piece(index, slot), index, part),
            half_of(landing_of(index, slot), index, part),
            w_send.at[index - 1],
            n_recv.at[index - 1],
            "dp",
            own ^ (2 * slot),
        )

    def keep_grad(index):
        return local(piece(index, 0), landing_of(index, 0), keep.at[index])

    def merge_grads(index):
        loads = [local(half_of(grad_merge[index], index, part), stage_of(index, part), load.at[part]) for part in range(2)]
        for part in range(2):
            send_far(index, part).wait_recv()
            loads[part].start()
        for part in range(2):
            loads[part].wait()
            target, source = half_of(piece(index, 2 - part), index, part), stage_of(index, part)
            length = source.shape[0] // 4

            @pl.loop(0, 4)
            def _(step):
                rows = cols_of(step, length)
                target[rows, :] = (target[rows, :].astype(F32) + source[rows, :].astype(F32)).astype(BF)

            send_near(index, 2 - part, part).start()

    def row_grads(index, slot, left, left_pair, right, right_pair, columns):
        mine, theirs = slice_of(slot, width, True), slice_of(slot, width, False)
        turned, turned_pair = jnp.transpose(left[:, mine]), jnp.transpose(left_pair[:, theirs])
        target = piece(index, slot)

        @pl.loop(0, columns // 512)
        def _(step):
            cols = cols_of(step, 512)
            total = dot(turned, right[:, cols]) + dot(turned_pair, right_pair[:, cols])
            target[:, cols] = total.astype(BF)

        if slot == 3:
            send_far(index, 0).start()
            send_far(index, 1).start()
        elif slot:
            send_near(index, slot, slot - 1).start()
        elif index == 3:
            keep_grad(index).start()

    def out_grads():
        for part in range(2):
            rows = pl.ds(part * (heads // 2), heads // 2)
            turned, turned_pair = jnp.transpose(attended[:, rows]), jnp.transpose(cot[:, rows])
            for slot in range(4):
                mine, theirs = slice_of(slot, width, True), slice_of(slot, width, False)
                total = dot(turned, buffer_a[:, mine]) + dot(turned_pair, cot_half[:, theirs])
                piece(4, slot)[rows, :] = total.astype(BF)
            send_far(4, part).start()
            send_near(4, part + 1, part).start()
        keep_grad(4).start()

    def down_piece(slot, index, part=None):
        cols = pl.ds(((slot % 2) * GROUPS + index) * width, width)
        rows = pl.ds(0, group) if part is None else pl.ds(part * (group // 2), group // 2)
        return (buffer_b, buffer_c)[slot // 2].at[rows, cols]

    def down_rows(ref, index, slot, part=None):
        rows = pl.ds(index * group, group) if part is None else pl.ds(index * group + part * (group // 2), group // 2)
        return ref.at[rows, pl.ds(slot * width, width)]

    def send_down(kind, index, part):
        if kind == 0:
            target, source = down_rows(grad_merge[0], index, 0, part), down_piece(3, index, part)
            peer = own ^ (2 + 2 * part)
        else:
            target, source = down_rows(down_parts, index, kind - 1, part), down_piece(kind, index, part)
            peer = own ^ (2 * kind)
        return remote(source, target, d_send.at[0], d_recv.at[GROUPS if kind else index], "dp", peer)

    def down_grads(index):
        drain(buffer_a.at[:, pl.ds(index * group, group)], f_recv.at[index])

        @pl.loop(0, group // 256)
        def _(step):
            cols = pl.ds(pl.multiple_of(index * group + step * 256, 256), 256)
            rows = pl.ds(pl.multiple_of(step * 256, 256), 256)
            turned, turned_pair = jnp.transpose(hidden[:, cols]), jnp.transpose(buffer_a[:, cols])
            for slot in range(4):
                mine, theirs = slice_of(slot, width, True), slice_of(slot, width, False)
                total = dot(turned, cot[:, mine]) + dot(turned_pair, cot_half[:, theirs])
                down_piece(slot, index)[rows, :] = total.astype(BF)

        for part in range(2):
            send_down(0, index, part).start()
        for part in range(2):
            send_down(1 + part, index, part).start()

    def merge_down(indices):
        entries = [(index, part) for index in indices for part in range(2)]

        def stage(index, part):
            rows = pl.ds(part * (group // 2), group // 2)
            return d_attended.at[rows, pl.ds((index % 2) * width, width)]

        loads = [
            local(down_rows(grad_merge[0], index, 0, part), stage(index, part), load.at[2 * (index % 2) + part])
            for index, part in entries
        ]
        for index in indices:
            drain(down_rows(grad_merge[0], index, 0), d_recv.at[index])
        start_all(loads)
        for copy, (index, part) in zip(loads, entries):
            copy.wait()
            target, source = down_piece(2 - part, index, part), stage(index, part)

            @pl.loop(0, 2)
            def _(step):
                rows = cols_of(step, group // 4)
                target[rows, :] = (target[rows, :].astype(F32) + source[rows, :].astype(F32)).astype(BF)

            send_down(2 - part, index, part).start()

    def norm_back(total, values, gain):
        inverse = lax.rsqrt(jnp.mean(values * values, axis=-1, keepdims=True) + EPSILON)
        scaled = total * gain
        return inverse * (scaled - values * inverse * inverse * jnp.mean(scaled * values, axis=-1, keepdims=True))

    meet()
    for gather in gather_hidden:
        gather.start()
    gains_in[...] = jnp.zeros(gains_in.shape, F32)
    for index, plain in enumerate(plain_gains):
        gains_in[index : index + 1, :] = plain[...].astype(F32).reshape(1, width)
    send_weights(range(3))
    for flip in range(1, 8):
        send_gain(flip).start()
    stage_down = down_w.at[:, pl.ds(3 * heads, width)]
    stage_in = local(weights_in[4], stage_down, load.at[0])
    own_loads = [local(gains_in, at_cols(gains, own, width), load.at[1])]
    own_loads += [local(weights_in[item], view(item, own), load.at[2 + item]) for item in range(4)]
    own_loads += [local(weights_in[5], at_rows(gate_w, own, width), load.at[6])]
    own_loads += [local(weights_in[6], at_rows(up_w, own, width), load.at[7])]
    for part in range(PARTS):
        own_loads.append(local(hidden_in.at[part_rows(part), :], buffer_b.at[own_rows(part), :], load.at[8 + part]))
        own_loads.append(local(cot_in.at[part_rows(part), :], cot.at[own_rows(part), :], load.at[10 + part]))
    start_all([stage_in] + own_loads)
    fill_mask(bias, docs, size)
    fill_turns(cosine, sine, size)
    for part in range(PARTS):
        clear(part)
    relay_weights([0])
    gather_hidden[0].hop(0)
    gather_hidden[0].hop(1)
    relay_weights([1])
    gather_hidden[1].hop(0)
    gather_hidden[1].hop(1)
    gather_hidden[0].hop(2)
    relay_weights([2])
    send_weights([3, 4])
    gather_hidden[1].hop(2)
    for gather in gather_cot:
        gather.start()
    stage_in.wait()
    stage_out = local(stage_down, at_cols(down_full, own, width), keep.at[5])
    stage_out.start()
    wait_all(own_loads)
    drain(gain_recv.at[pl.ds(0, 56), :], y_recv.at[0])
    gather_cot[0].hop(1)
    gather_cot[0].hop(0)
    pass_weights(range(3))
    relay_weights([3])
    send_weights(range(5, 4 + 3 * GROUPS))
    for gather in gather_hidden:
        gather.wait()

    norm_rows(buffer_b, buffer_c, inverses_one, gains.at[pl.ds(0, 1), :], 64)
    keep_hidden = local(buffer_b, hidden_rows, keep.at[0])
    keep_normed = local(buffer_c, normed_rows, keep.at[1])
    start_all([keep_hidden, keep_normed])
    have_weights(0)
    qkv_w = down_w.at[:, pl.ds(0, 3 * heads)]
    keep_qkv = local(qkv_w, qkv_full, keep.at[2])
    keep_qkv.start()

    @pl.loop(0, 2 * heads // step_cols)
    def _(step):
        cols = cols_of(step)
        product = dot(buffer_c[...], down_w[:, cols])
        turns = [jnp.concatenate([table[...]] * (step_cols // 128), axis=1) for table in (cosine, sine)]
        qkv[:, cols] = turn(product, *turns).astype(BF)

    @pl.loop(2 * heads // step_cols, 3 * heads // step_cols)
    def _(step):
        cols = cols_of(step)
        qkv[:, cols] = dot(buffer_c[...], down_w[:, cols]).astype(BF)

    attend(qkv, attended, bias, heads)
    gather_cot[0].hop(2)
    gather_cot[1].hop(1)
    gather_cot[1].hop(0)
    pass_weights([3])
    have_weights(1)

    def make_out(part):
        @pl.loop(0, count)
        def _(step):
            cols = cols_of(step)
            product = dot(attended[part * span : (part + 1) * span, :], out_w[:, cols])
            middle[part_rows(part), cols] = product[:size, :]
            send_part[pl.ds(part * span + size, span - size), cols] = product[size:, :].astype(BF)

    make_out(0)
    out_scatter[0].start()
    make_out(1)
    out_scatter[1].start()
    gather_cot[1].hop(2)
    wait_all([keep_hidden, keep_normed, keep_qkv, stage_out])
    send_normed = halves(normed_rows, pair_normed, 1)
    send_attended = to_pair(attended, pair_attended, 2, 0)
    start_all(send_normed + [send_attended])
    for index in range(3):
        out_scatter[0].hop(index)
    relay_weights(items_of(0))

    def make_sent(part):
        out_scatter[part].wait()

        @pl.loop(0, size // 32)
        def _(step):
            rows = pl.ds(pl.multiple_of(part * size + step * 32, 32), 32)
            place = pl.ds(pl.multiple_of(part * span + step * 32, 32), 32)
            total = received(part, step * 32, 32, hidden_of(place) + middle[rows, :])
            middle[rows, :] = total
            sent[place, :] = total.astype(BF)

        gather_sent[part].start()

    def hidden_of(place):
        return buffer_b[place, :].astype(F32)

    for gather in gather_hidden:
        gather.finish()
    make_sent(0)
    out_scatter[1].hop(0)
    relay_weights(items_of(1))
    gather_sent[0].hop(0)
    out_scatter[1].hop(1)
    out_scatter[1].hop(2)
    make_sent(1)
    gather_sent[0].hop(1)
    relay_weights(items_of(2))
    gather_sent[1].hop(0)
    gather_sent[1].hop(1)
    gather_sent[0].hop(2)
    gather_sent[1].hop(2)
    relay_weights(items_of(3))

    def load_down(index):
        rows = pl.ds(index * group, group)
        return local(down_full.at[rows, :], down_w.at[rows, :], down_load.at[index])

    for gather in gather_cot:
        gather.wait()
    send_cot = halves(cot, cot_half, 0)
    start_all(send_cot)
    for gather in gather_sent:
        gather.wait()
    norm_rows(sent, normed, inverses, gains.at[pl.ds(1, 1), :], 64)
    pass_weights(items_of(0))
    send_two = halves(normed, two_half, 3)
    start_all(send_two)
    have_weights(2)
    for phase in range(2):
        sent_weights(phase)
    load_down(0).start()
    for index in range(GROUPS):
        load_down(index).wait()
        if index + 1 < GROUPS:
            pass_weights(items_of(index + 1))

        @pl.loop(index * group // step_cols, (index + 1) * group // step_cols)
        def _(step):
            cols = cols_of(step)
            gate = dot(normed[...], gate_w[:, cols])
            up = dot(normed[...], up_w[:, cols])
            d_hidden = dot_rows(cot[...], down_w[cols, :])
            s = jax.nn.sigmoid(gate)
            activated = gate * s
            hidden[:, cols] = (activated * up).astype(BF)
            d_gate[:, cols] = (d_hidden * up * (s + activated * (1.0 - s))).astype(BF)
            d_up[:, cols] = (d_hidden * activated).astype(BF)
            for which in range(3):
                send_ff(step, which).start()

        if index + 1 < GROUPS:
            have_weights(3 + index)
            load_down(index + 1).start()
        if index == 0:
            drain(cot_half, h_recv.at[0])
        else:
            down_grads(index - 1)

    gain_part[...] = jnp.zeros(gain_part.shape, F32)
    for part in range(PARTS):
        out_scatter[part].finish()

    def make_two(part):
        block = slice(part * span, (part + 1) * span)

        @pl.loop(0, count)
        def _(step):
            cols = cols_of(step)
            product = dot_rows(d_gate[block, :], gate_w[cols, :]) + dot_rows(d_up[block, :], up_w[cols, :])
            gain_part[pl.ds(1, 1), cols] += jnp.sum(
                product * (sent[block, cols].astype(F32) * inverses[block, :]), axis=0, keepdims=True
            )
            grad_middle[part_rows(part), cols] = product[:size, :]
            send_part[pl.ds(part * span + size, span - size), cols] = product[size:, :].astype(BF)

    make_two(0)
    two_scatter[0].start()
    down_grads(GROUPS - 1)
    merge_down((0, 1))
    make_two(1)
    two_scatter[0].hop(0)
    two_scatter[1].start()
    for phase in range(2, 2 + GROUPS):
        sent_weights(phase)
    for which in (1, 2):
        drain((d_gate, d_up)[which - 1], f_recv.at[GROUPS - 1 + which])
    gate_pair, up_pair = up_w.at[pl.ds(0, tokens), :], up_w.at[pl.ds(tokens, tokens), :]
    pair_loads = [local(pair_gate, gate_pair, load.at[0]), local(pair_up, up_pair, load.at[1])]
    start_all(pair_loads)
    drain(two_half, h_recv.at[3])
    wait_all(pair_loads)
    gate_grads = lambda slot: row_grads(1, slot, normed, two_half, d_gate, gate_pair, units)
    up_grads = lambda slot: row_grads(2, slot, normed, two_half, d_up, up_pair, units)
    gate_grads(3)
    merge_down((2, 3))
    two_scatter[0].hop(1)
    two_scatter[0].hop(2)
    for slot in (1, 2, 0):
        gate_grads(slot)

    def make_branch(part):
        two_scatter[part].wait()

        @pl.loop(0, size // 32)
        def _(step):
            rows = pl.ds(pl.multiple_of(part * size + step * 32, 32), 32)
            place = pl.ds(pl.multiple_of(part * span + step * 32, 32), 32)
            total = received(part, step * 32, 32, grad_middle[rows, :])
            result = cot[place, :].astype(F32) + norm_back(total, sent[place, :].astype(F32), gains[1:2, :])
            grad_middle[rows, :] = result
            sent[place, :] = result.astype(BF)

        gather_branch[part].start()
        keep_branch[part].start()

    keep_branch = [
        local(sent.at[own_rows(part), :], branch_rows.at[own_rows(part), :], keep.at[6 + part]) for part in range(PARTS)
    ]
    for part in range(PARTS):
        gather_sent[part].finish()
    make_branch(0)
    up_grads(3)
    two_scatter[1].hop(0)
    up_grads(1)
    gather_branch[0].hop(0)
    two_scatter[1].hop(1)
    two_scatter[1].hop(2)
    up_grads(2)
    up_grads(0)
    def project(first, last):
        @pl.loop(first, last)
        def _(step):
            cols = cols_of(step)
            product = dot(hidden[...], down_w[:, cols])
            for part in range(PARTS):
                start = part * span
                middle[part_rows(part), cols] = middle[part_rows(part), cols] + product[start : start + size, :]
                sent[pl.ds(start + size, span - size), cols] = product[start + size : start + span, :].astype(BF)

    pl.when(ends(rank))(lambda: project(0, count))
    mlp_scatter[0].start((0,))
    make_branch(1)
    mlp_scatter[0].start((1, 2))
    mlp_scatter[1].start()
    pl.when(inner(rank))(lambda: project(0, count // 4))
    gather_branch[0].hop(1)
    merge_grads(1)
    pl.when(inner(rank))(lambda: project(count // 4, count // 2))
    gather_branch[1].hop(0)
    pl.when(inner(rank))(lambda: project(count // 2, count))
    gather_branch[1].hop(1)
    gather_branch[0].hop(2)
    gather_branch[1].hop(2)
    load_weight = local(qkv_full, qkv_w, load.at[4])
    load_hidden = local(hidden_rows, gate_pair, load.at[5])
    load_normed = local(normed_rows, up_pair, load.at[6])
    start_all([load_hidden, load_normed])
    mlp_scatter[0].hop(0)
    merge_grads(2)
    for part in range(PARTS):
        two_scatter[part].finish()
        gather_branch[part].wait()
        keep_branch[part].wait()

    load_branch = local(branch_rows, buffer_a, load.at[7])
    load_branch.start()
    load_weight.start()
    send_half = halves(branch_rows, pair_branch, 4)
    start_all(send_half)
    mlp_scatter[0].hop(1)
    load_branch.wait()

    @pl.loop(0, heads // step_cols)
    def _(step):
        cols = cols_of(step)
        d_attended[:, cols] = dot_rows(buffer_a[...], out_w[cols, :]).astype(BF)

    drain(cot_half, h_send.at[0])
    for gather in gather_cot:
        gather.finish()
    drain(two_half, h_recv.at[1])
    send_attended.wait_recv()
    early_loads = [
        local(pair_attended, cot.at[:, pl.ds(0, heads)], load.at[8]),
        local(pair_normed, two_half, load.at[9]),
    ]
    start_all(early_loads)
    attend_back(qkv, d_attended, d_qkv, bias, cosine, sine, heads)
    send_qkv = to_pair(d_qkv, pair_qkv, 5, 0)
    send_qkv.start()
    for which in range(3):
        drain((hidden, d_gate, d_up)[which], f_send.at[which])

    drain(cot_half, h_recv.at[4])
    load_half = local(pair_branch, cot_half, load.at[10])
    load_half.start()
    mlp_scatter[0].hop(2)
    mlp_scatter[1].hop(0)
    wait_all([load_weight, load_hidden, load_normed])

    def make_one(part):
        block = slice(part * span, (part + 1) * span)

        @pl.loop(0, count)
        def _(step):
            cols = cols_of(step)
            product = dot_rows(d_qkv[block, :], down_w[cols, pl.ds(0, 3 * heads)])
            gain_part[pl.ds(0, 1), cols] += jnp.sum(
                product * (gate_pair[block, cols].astype(F32) * inverses_one[block, :]), axis=0, keepdims=True
            )
            input_grad[part_rows(part), cols] = product[:size, :]
            send_part[pl.ds(part * span + size, span - size), cols] = product[size:, :].astype(BF)

        one_scatter[part].start()

    def share_gain(flip):
        source = at_cols(gain_part, own ^ flip, width)
        return remote(source, at_rows(gain_recv, flip, 8), g_send.at[0], g_recv.at[0], "dp", own ^ flip)

    make_one(0)
    mlp_scatter[1].hop(1)

    send_qkv.wait_recv()
    drain(two_half, h_send.at[3])
    load_qkv = local(pair_qkv, normed.at[:, pl.ds(0, 3 * heads)], load.at[0])
    load_qkv.start()
    wait_all(early_loads + [load_half])
    out_grads()
    mlp_scatter[1].hop(2)
    load_qkv.wait()
    for slot in (3, 1, 2, 0):
        row_grads(3, slot, up_pair, two_half, d_qkv, normed, 3 * heads)
        if slot == 2:
            one_scatter[0].hop(0)
            make_one(1)
    for flip in range(1, 8):
        share_gain(flip).start()
    one_scatter[0].hop(1)
    one_scatter[0].hop(2)
    merge_grads(4)

    drain(gate_w.at[pl.ds(0, 2 * width), :], n_recv.at[0])
    drain(gate_w.at[pl.ds(0, 2 * width), :], n_recv.at[1])
    drain(gate_w.at[pl.ds(0, units // 4), :], d_recv.at[GROUPS])
    staged = [up_w.at[pl.ds(2 * index * width, 2 * width), :] for index in range(2)]
    sum_loads = [local(ref, staged[index], load.at[4 + index]) for index, ref in enumerate((gate_parts, up_parts))]
    for index in range(GROUPS):
        for slot in range(2):
            place = buffer_a.at[:, pl.ds((slot * GROUPS + index) * width, width)]
            sum_loads.append(local(down_rows(down_parts, index, slot), place, load.at[6]))
    start_all(sum_loads)

    def add_rows(index):
        total = piece(index, 0)
        sum_loads[index - 1].wait()

        @pl.loop(0, width // 32)
        def _(step):
            rows = cols_of(step, 32)
            near = pl.ds(pl.multiple_of(width + step * 32, 32), 32)
            terms = [total[rows, :], staged[index - 1][rows, :], staged[index - 1][near, :]]
            total[rows, :] = sum(term.astype(F32) for term in terms).astype(BF)

        local(total, (gate_sum, up_sum)[index - 1], keep.at[index]).start()

    def add_down():
        drain(buffer_a, load.at[6])

        @pl.loop(0, tokens // 64)
        def _(step):
            rows = cols_of(step, 64)
            for index in range(GROUPS):
                total = down_piece(0, index)
                terms = [total[rows, :]]
                terms += [buffer_a[rows, pl.ds((slot * GROUPS + index) * width, width)] for slot in range(2)]
                total[rows, :] = sum(term.astype(F32) for term in terms).astype(BF)

        for index in range(GROUPS):
            local(down_piece(0, index), down_rows(down_sum, index, 0), keep.at[8]).start()

    one_scatter[1].hop(0)
    add_rows(1)
    merge_grads(3)
    add_rows(2)
    one_scatter[1].hop(1)
    one_scatter[1].hop(2)
    add_down()

    drain(gain_recv.at[pl.ds(8, 56), :], g_recv.at[0])
    gain_sum = gain_part[:, pl.ds(pl.multiple_of(own * width, width), width)]
    for flip in range(1, 8):
        gain_sum = gain_sum + gain_recv[pl.ds(flip * 8, 8), :]
    gain_z[pl.ds(0, 8), :] = gain_sum

    def share_gain_z(k):
        target = gain_z.at[pl.ds(8 * k, 8), :]
        return remote(gain_z.at[pl.ds(0, 8), :], target, y_send.at[1], y_recv.at[1], "tensor", lax.rem(rank + k, 4))

    for k in (1, 2, 3):
        share_gain_z(k).start()

    load_own = [
        local(hidden_in.at[part_rows(part), :], sent.at[own_rows(part), :], load.at[4 + part]) for part in range(PARTS)
    ]
    for part in range(PARTS):
        gather_branch[part].finish()
    start_all(load_own)
    wait_all(load_own)
    for part in range(PARTS):
        one_scatter[part].wait()

        @pl.loop(0, size // 32)
        def _(step):
            rows = pl.ds(pl.multiple_of(part * size + step * 32, 32), 32)
            place = pl.ds(pl.multiple_of(part * span + step * 32, 32), 32)
            total = received(part, step * 32, 32, input_grad[rows, :])
            input_grad[rows, :] = grad_middle[rows, :] + norm_back(total, sent[place, :].astype(F32), gains[0:1, :])

    leave = [local(input_grad, input_ref, keep.at[6]), local(layer_out, out_ref, keep.at[7])]
    leave[0].start()

    for scatter in mlp_scatter:
        scatter.wait()
    load_mlp = [
        [local(mlp_recv.at[arrived(part, slot), :], recv_part.at[arrived(part, slot), :], load.at[2 * part + index])
         for index, slot in enumerate((4, 2))]
        for part in range(PARTS)
    ]
    for part in range(PARTS):
        load_mlp[part][0].start()
        pl.when(inner(rank))(load_mlp[part][1].start)
    for part in range(PARTS):
        load_mlp[part][0].wait()
        pl.when(inner(rank))(load_mlp[part][1].wait)

        @pl.loop(0, size // 32)
        def _(step):
            rows = pl.ds(pl.multiple_of(part * size + step * 32, 32), 32)
            layer_out[rows, :] = received(part, step * 32, 32, middle[rows, :]).astype(BF)

    leave[1].start()

    drain(gain_z.at[pl.ds(8, 24), :], y_recv.at[1])
    gain_all = gain_z[pl.ds(0, 8), :]
    for k in (1, 2, 3):
        gain_all = gain_all + gain_z[pl.ds(8 * k, 8), :]
    gain_total[...] = gain_all

    for scatter in mlp_scatter + one_scatter:
        scatter.finish()
    drain(gate_w.at[pl.ds(0, 3 * units // 8), :], d_send.at[0])
    drain(gain_recv.at[pl.ds(8, 56), :], y_send.at[0])
    drain(gain_recv.at[pl.ds(8, 56), :], g_send.at[0])
    drain(gain_z.at[pl.ds(8, 24), :], y_send.at[1])
    drain(two_half, h_send.at[1])
    drain(two_half, h_send.at[4])
    send_attended.wait_send()
    send_qkv.wait_send()
    def pieces(index, number):
        rows = number * width if index < 4 else number * heads * width // dim
        return gate_w.at[pl.ds(0, rows), pl.ds(0, 3 * heads if index == 3 else dim)]

    wait_all(leave)
    local(gate_w.at[pl.ds(0, width), :], gate_sum, keep.at[1]).wait()
    local(gate_w.at[pl.ds(0, width), :], up_sum, keep.at[2]).wait()
    drain(down_sum, keep.at[8])
    for index in range(1, 5):
        if index > 2:
            drain(pieces(index, 2), n_recv.at[index - 1])
            keep_grad(index).wait()
        drain(pieces(index, 3), w_send.at[index - 1])


def layer(hidden_in, cot, gains, weights, docs):
    tile, dim = hidden_in.shape
    tokens = 4 * tile
    width, heads = weights[0].shape
    units = weights[5].shape[1]
    dma = pltpu.SemaphoreType.DMA
    rows, narrow, ff = shape((tokens, dim), BF), shape((tokens, dim // 2), BF), shape((tokens, units), BF)
    weights_shape = [(units, width), (width, units), (width, units), (width, 3 * heads), (heads, width)]
    sums_shape = weights_shape[:3] + [(3 * width, 3 * heads), (heads, 3 * width)]
    parts_shape = [(units, 2 * width), (2 * width, units), (2 * width, units)]
    outs = [shape(dims, BF) for dims in sums_shape + parts_shape + weights_shape]
    outs += [ff] * 2 + [shape((tokens, 3 * heads), BF), shape((tokens, heads), BF), narrow, narrow]
    outs += [rows] * 3 + [shape((5 * tile, dim), BF), shape((dim, 3 * heads), BF), shape((units, dim), BF)]
    in_hbm = len(outs)
    outs += [shape((tile, dim), BF), shape((tile, dim), F32), shape((8, width), F32)]
    in_hbm += 2
    items = 4 + 3 * GROUPS
    scratch = [((dim, units), BF), ((dim, units), BF), ((units, dim), BF)]
    scratch += [((tokens, dim), BF)] * 3 + [((tokens, units), BF)] * 3
    scratch += [((tokens, dim // 2), BF)] * 2 + [((tokens, dim), BF)] * 3 + [((heads, dim), BF)]
    scratch += [((tokens, 3 * heads), BF)] + [((tokens, heads), BF)] * 2
    scratch += [((tokens, tokens), F32), ((tokens, 128), F32), ((tokens, 128), F32)]
    scratch += [((tokens, 1), F32), ((tokens, 1), F32), ((tile, dim), F32), ((tile, dim), F32)]
    scratch += [((tokens, dim), BF), ((5 * tile, dim), BF)]
    scratch += [((8, width), F32), ((8, dim), F32), ((8, dim), F32), ((64, width), F32), ((32, width), F32)]
    scratch += [((tile, dim), BF), ((tile, dim), F32)]
    sems = [(2 + GROUPS,), (4 + GROUPS, 3), (3,), (GROUPS + 2,), (6,), (6,)]
    sems += [(2, PARTS), (2, PARTS, 3), (2, PARTS), (2, PARTS, 5), (4,), (4, 2), (1,), (GROUPS + 1,)]
    sems += [(1,), (1,), (2,), (2,), (12,), (8 + GROUPS,), (GROUPS,), (2 + GROUPS,), (4,)]
    return pl.pallas_call(
        layer_kernel,
        out_shape=outs,
        in_specs=[anyspace()] * 2 + [vmem()] * 2 + [anyspace()] * 7 + [vmem()],
        out_specs=[anyspace()] * in_hbm + [vmem()],
        scratch_shapes=[pltpu.VMEM(*entry) for entry in scratch] + [dma(entry) for entry in sems],
        compiler_params=pltpu.CompilerParams(vmem_limit_bytes=67000000, collective_id=0, has_side_effects=True),
        cost_estimate=cost(2 * tokens * dim * units * 12, 100e6),
        name="layer",
    )(hidden_in, cot, *gains, *weights, docs)


def sum_kernel(counts, *refs):
    parts, plain_in, gain_total = refs[:5], refs[5:7], refs[7]
    down, gate, up, query, key, value, out, *plain_out = refs[8:17]
    gains = refs[17:19]
    staged, totals, plain, load, store = refs[19:24], refs[24:29], refs[29:31], refs[31], refs[32]
    loads = [pltpu.make_async_copy(parts[index], staged[index], load.at[index]) for index in range(5)]
    loads += [pltpu.make_async_copy(plain_in[index], plain[index], load.at[5 + index]) for index in range(2)]
    start_all(loads)
    heads = query.shape[1]
    stores = [pltpu.make_async_copy(totals[index], ref, store.at[index]) for index, ref in enumerate((down, gate, up))]
    qkv_stores = [
        pltpu.make_async_copy(totals[3].at[:, pl.ds(index * heads, heads)], ref, store.at[3 + index])
        for index, ref in enumerate((query, key, value))
    ]
    out_store = pltpu.make_async_copy(totals[4], out, store.at[6])
    plain_stores = [pltpu.make_async_copy(plain[index], plain_out[index], store.at[7 + index]) for index in range(2)]
    wide, share = gain_total.shape[1], gains[0].shape[0]
    turned = pltpu.roll(gain_total[...], lax.rem(wide - share * lax.axis_index("tensor"), wide), 1)
    for index in range(2):
        gains[index][...] = turned[index, :share]
    groups = [[stores[0]], [stores[1]], [stores[2]], qkv_stores, [out_store]]
    for index in range(5):
        loads[index].wait()
        rows_first = index in (1, 2, 3)
        rows, cols = totals[index].shape
        step_rows = 32 if rows_first else 256

        @pl.loop(0, rows // step_rows)
        def _(step):
            start = pl.multiple_of(step * step_rows, step_rows)
            total = None
            for slot in range(counts[index]):
                if rows_first:
                    term = staged[index][pl.ds(pl.multiple_of(start + slot * rows, step_rows), step_rows), :]
                else:
                    term = staged[index][pl.ds(start, step_rows), slot * cols : (slot + 1) * cols]
                term = term.astype(F32)
                total = term if total is None else total + term
            totals[index][pl.ds(start, step_rows), :] = total

        start_all(groups[index])
    for index in range(2):
        loads[5 + index].wait()
        plain_stores[index].start()
    for entry in groups + [plain_stores]:
        wait_all(entry)


def sum_grads(parts, plain, gain_total, heads, counts, ranks):
    dims = [part.shape for part in parts]
    sums = [
        (rows // counts[index], cols) if index in (1, 2, 3) else (rows, cols // counts[index])
        for index, (rows, cols) in enumerate(dims)
    ]
    outs = sums[:3] + [(sums[3][0], heads)] * 3 + [sums[4]]
    dma = pltpu.SemaphoreType.DMA
    return pl.pallas_call(
        partial(sum_kernel, counts),
        out_shape=[shape(dim, F32) for dim in outs]
        + [shape(entry.shape, entry.dtype) for entry in plain]
        + [shape((gain_total.shape[1] // ranks,), F32)] * 2,
        in_specs=[anyspace()] * 7 + [vmem()],
        out_specs=[anyspace()] * 9 + [vmem()] * 2,
        scratch_shapes=[pltpu.VMEM(dim, BF) for dim in dims]
        + [pltpu.VMEM(dim, F32) for dim in sums]
        + [pltpu.VMEM(entry.shape, entry.dtype) for entry in plain]
        + [dma((7,)), dma((9,))],
        compiler_params=params(),
        cost_estimate=cost(1e6, 22e6),
        name="sum_grads",
    )(*parts, *plain, gain_total)


def shift(values, step):
    size = lax.axis_size("tensor")
    return lax.ppermute(values, "tensor", [(index, (index + step) % size) for index in range(size)])


def gather_rows(values):
    return [values] + [shift(values, step) for step in range(1, lax.axis_size("tensor"))]


def scatter_rows(parts):
    total = parts[0].astype(F32)
    for step in range(1, len(parts)):
        total = total + shift(parts[step], -step).astype(F32)
    return total


def gather_weight(values, axis):
    return [None], [lax.all_gather(values, "dp", axis=axis, tiled=True)]


def scatter_full(left, right, axis):
    full = dot_cols(left, right).astype(BF)
    return lax.psum_scatter(full, "dp", scatter_dimension=axis, tiled=True).astype(F32)


def frequencies():
    half_size = HEAD_DIM // 2
    return ROPE_BASE ** (-jnp.arange(half_size, dtype=F32) / half_size)


def rotary(length):
    angles = jnp.arange(length).astype(F32)[:, None] * frequencies()[None, :]
    cosine, sine = jnp.cos(angles), jnp.sin(angles)
    cosine = jnp.tile(cosine, (1, 8))
    sine = jnp.tile(jnp.concatenate([-sine, sine], axis=1), (1, 4))
    return cosine, sine


def position_tables(doc_ids, ranks):
    length = doc_ids.shape[0]
    token_index = jnp.arange(length, dtype=jnp.int32)
    before = jnp.concatenate([doc_ids[:1] - 1, doc_ids[:-1]])
    doc_start = lax.cummax(jnp.where(doc_ids != before, token_index, 0), axis=0)
    order = (lax.axis_index("tensor") - jnp.arange(ranks)) % ranks
    last = token_index.reshape(ranks, -1)[order].reshape(length)
    first = doc_start.reshape(ranks, -1)[order].reshape(length)
    cosine, sine = (table.reshape(ranks, -1, 256)[order].reshape(length, 256) for table in rotary(length))
    return cosine, sine, first[:, None], last[:, None], last[None, :]


def rms_back(grad_rows_, values, gain):
    inverse = lax.rsqrt(jnp.mean(values * values, axis=-1, keepdims=True) + EPSILON)
    scaled = grad_rows_ * gain
    return inverse * (scaled - values * inverse * inverse * jnp.mean(scaled * values, axis=-1, keepdims=True))


def body(
    hidden_in,
    out_cotangent,
    doc_ids,
    attn_gain,
    query_weight,
    key_weight,
    value_weight,
    out_weight,
    mlp_gain,
    gate_weight,
    up_weight,
    down_weight,
):
    ranks, groups = lax.axis_size("tensor"), lax.axis_size("dp")
    paired = (groups, ranks) == (8, 4)
    width, heads = query_weight.shape
    dim = hidden_in.shape[1]

    if paired:
        weights = (query_weight, key_weight, value_weight, out_weight, down_weight, gate_weight, up_weight)
        outs = layer(hidden_in, out_cotangent, (attn_gain, mlp_gain), weights, doc_ids.reshape(ranks, -1))
        sums = sum_grads(outs[:5], outs[-3:-1], outs[-1], heads, (1, 1, 1, 3, 3), ranks)
        down_grad, gate_grad, up_grad, query_grad, key_grad, value_grad, out_proj_grad, layer_out, input_grad = sums[:9]
        gain_grads = sums[9:]
    else:
        tables = position_tables(doc_ids, ranks)
        input_local = hidden_in.astype(F32)
        hidden_rows = gather_rows(hidden_in)
        gains = lax.all_gather(jnp.stack([attn_gain, mlp_gain]), "dp", axis=1, tiled=True).astype(F32)
        attn_scale, mlp_scale = gains[:1], gains[1:]
        qkv_weight = jnp.concatenate([query_weight, key_weight, value_weight], axis=1)
        tags, qkv_pieces = gather_weight(qkv_weight, 0)
        tags, out_pieces = gather_weight(out_weight, 1)
        cot_rows = gather_rows(out_cotangent)
        tags, down_pieces = gather_weight(down_weight, 1)
        tags, gate_pieces = gather_weight(gate_weight, 0)
        tags, up_pieces = gather_weight(up_weight, 0)
        normed, qkv, attended, inverses, *branch_parts = attn_fwd(
            hidden_rows, attn_scale, tables, tags, width, qkv_pieces, out_pieces
        )
        middle = input_local + scatter_rows(branch_parts)
        sent = middle.astype(BF)
        sent_rows = gather_rows(sent)
        cot_full = jnp.concatenate(cot_rows, axis=0)
        normed_two, hidden, d_gate, d_up, mlp_gain_part, *two_parts = mlp(
            sent_rows, cot_rows, mlp_scale, tags, width, gate_pieces, up_pieces, down_pieces, ranks
        )
        grad_two_rows = scatter_rows(two_parts)
        grad_middle = out_cotangent.astype(F32) + rms_back(grad_two_rows, sent.astype(F32), mlp_scale)
        branch_rows = gather_rows(grad_middle.astype(BF))
        down_grad = scatter_full(hidden, cot_full, 1)
        gate_grad = scatter_full(normed_two, d_gate, 0)
        up_grad = scatter_full(normed_two, d_up, 0)
        mlp_rows = scatter_rows(mlp_out(hidden, ranks, dim, tags, width, down_pieces))
        layer_out = (middle + mlp_rows).astype(BF)
        branch_full, d_qkv, attn_gain_part, *one_parts = attn_bwd(
            branch_rows, hidden_rows, qkv, inverses, tables, tags, width, qkv_pieces, out_pieces, ranks
        )
        out_proj_grad = scatter_full(attended, branch_full, 1)
        query_grad, key_grad, value_grad = jnp.split(scatter_full(normed, d_qkv, 0), 3, axis=1)
        grad_one_rows = scatter_rows(one_parts)
        input_grad = grad_middle + rms_back(grad_one_rows, input_local, attn_scale)
        gain_parts = jnp.concatenate([attn_gain_part, mlp_gain_part], axis=0)
        gain_grads = lax.psum_scatter(gain_parts, ("dp", "tensor"), scatter_dimension=1, tiled=True)
    return (
        layer_out,
        input_grad,
        gain_grads[0],
        query_grad,
        key_grad,
        value_grad,
        out_proj_grad,
        gain_grads[1],
        gate_grad,
        up_grad,
        down_grad,
    )


def solution(mesh):
    return jax.shard_map(
        body,
        mesh=mesh,
        in_specs=(
            P(("dp", "tensor"), None),
            P(("dp", "tensor"), None),
            P("dp"),
            P("dp"),
            P("dp", "tensor"),
            P("dp", "tensor"),
            P("dp", "tensor"),
            P("tensor", "dp"),
            P("dp"),
            P("dp", "tensor"),
            P("dp", "tensor"),
            P("tensor", "dp"),
        ),
        out_specs=(
            P(("dp", "tensor"), None),
            P(("dp", "tensor"), None),
            P(("dp", "tensor")),
            P("dp", "tensor"),
            P("dp", "tensor"),
            P("dp", "tensor"),
            P("tensor", "dp"),
            P(("dp", "tensor")),
            P("dp", "tensor"),
            P("dp", "tensor"),
            P("tensor", "dp"),
        ),
        check_vma=False,
    )
```

```python
import math
from functools import partial

import jax
import jax.numpy as jnp
from jax import lax
from jax.experimental import pallas as pl
from jax.experimental.pallas import tpu as pltpu
from jax.sharding import PartitionSpec as P

HEAD_DIM = 64
EPSILON = 1e-05
ROPE_BASE = 130000.0
NEGATIVE = -1e30
VMEM_LIMIT = 63 * 1024 * 1024
BF = jnp.bfloat16
F32 = jnp.float32


def dot(left, right):
    return jnp.dot(left, right, preferred_element_type=F32)


def dot_rows(left, right):
    return lax.dot_general(left, right, (((1,), (1,)), ((), ())), preferred_element_type=F32)


def dot_cols(left, right):
    return lax.dot_general(left, right, (((0,), (0,)), ((), ())), preferred_element_type=F32)


def vmem():
    return pl.BlockSpec(memory_space=pltpu.VMEM)


def anyspace():
    return pl.BlockSpec(memory_space=pl.ANY)


def params():
    return pltpu.CompilerParams(vmem_limit_bytes=VMEM_LIMIT)


def cost(flops, nbytes):
    return pl.CostEstimate(flops=int(flops), bytes_accessed=int(nbytes), transcendentals=0)


def shape(dims, kind):
    return jax.ShapeDtypeStruct(dims, kind)


def place_copies(tags, pieces, target, sem, axis, width):
    own = lax.axis_index("dp")
    copies = []
    for slot, (tag, piece) in enumerate(zip(tags, pieces)):
        if tag is None:
            where = target
        else:
            start = pl.multiple_of((own ^ tag) * width, width)
            where = target.at[pl.ds(start, width), :] if axis == 0 else target.at[:, pl.ds(start, width)]
        copies.append(pltpu.make_async_copy(piece, where, sem.at[slot]))
    return copies


def row_copies(pieces, target, sem):
    copies = []
    for slot, piece in enumerate(pieces):
        rows = piece.shape[0]
        copies.append(pltpu.make_async_copy(piece, target.at[pl.ds(slot * rows, rows), :], sem.at[slot]))
    return copies


def start_all(copies):
    for copy in copies:
        copy.start()


def wait_all(copies):
    for copy in copies:
        copy.wait()


def turn(values, cosine, sine):
    width = values.shape[1]
    lane = lax.broadcasted_iota(jnp.int32, values.shape, 1)
    partner = jnp.where(
        lax.rem(lane, HEAD_DIM) < HEAD_DIM // 2,
        pltpu.roll(values, width - HEAD_DIM // 2, 1),
        pltpu.roll(values, HEAD_DIM // 2, 1),
    )
    return values * cosine + partner * sine


def norm_rows(source, target, inverses, gain, tile):
    @pl.loop(0, source.shape[0] // tile)
    def _(step):
        rows = pl.ds(pl.multiple_of(step * tile, tile), tile)
        values = source[rows, :].astype(F32)
        inverse = lax.rsqrt(jnp.mean(values * values, axis=-1, keepdims=True) + EPSILON)
        inverses[rows, :] = inverse
        target[rows, :] = (values * inverse * gain[...]).astype(BF)


def fill_bias(bias, first, last, key_index):
    keys = key_index[...]
    bias[...] = jnp.where((keys >= first[...]) & (keys <= last[...]), 0.0, NEGATIVE)


def head_lanes(width, half):
    lane = lax.broadcasted_iota(jnp.int32, (1, width), 1)
    return (lax.div(lane, HEAD_DIM) == half).astype(F32)


def probabilities(query, key, bias):
    scores = dot_rows(query, key) + bias
    weights = jnp.exp(scores - jnp.max(scores, axis=-1, keepdims=True))
    return weights * (1.0 / jnp.sum(weights, axis=-1, keepdims=True))


def attend(qkv, attended, bias, heads):
    @pl.loop(0, heads // 128)
    def _(pair):
        base = pl.multiple_of(pair * 128, 128)
        query = qkv[:, pl.ds(base, 128)]
        key = qkv[:, pl.ds(heads + base, 128)]
        value = qkv[:, pl.ds(2 * heads + base, 128)]
        total = None
        for half in range(2):
            lanes = head_lanes(128, half).astype(BF)
            probs = probabilities(query * (lanes * HEAD_DIM ** (-0.5)), key, bias[...])
            term = dot(probs.astype(BF), value * lanes)
            total = term if total is None else total + term
        attended[:, pl.ds(base, 128)] = total.astype(BF)


def attn_fwd_kernel(tags, width, nrow, *refs):
    npiece = len(tags)
    rows_in = refs[:nrow]
    gain, cosine, sine, first, last, key_index = refs[nrow : nrow + 6]
    rest = refs[nrow + 6 :]
    qkv_in, out_in = rest[:npiece], rest[npiece : 2 * npiece]
    rest = rest[2 * npiece :]
    normed, qkv, attended, inverses = rest[:4]
    parts = rest[4 : 4 + nrow]
    hidden, qkv_w, out_w, bias, sem_rows, sem_qkv, sem_out = rest[4 + nrow :]
    load_rows = row_copies(rows_in, hidden, sem_rows)
    load_qkv = place_copies(tags, qkv_in, qkv_w, sem_qkv, 0, width)
    load_out = place_copies(tags, out_in, out_w, sem_out, 1, width)
    start_all(load_rows + load_qkv + load_out)
    fill_bias(bias, first, last, key_index)
    wait_all(load_rows)
    norm_rows(hidden, normed, inverses, gain, 64)
    wait_all(load_qkv)
    heads = attended.shape[1]
    step_cols = 256

    @pl.loop(0, 2 * heads // step_cols)
    def _(step):
        cols = pl.ds(pl.multiple_of(step * step_cols, step_cols), step_cols)
        qkv[:, cols] = turn(dot(normed[...], qkv_w[:, cols]), cosine[...], sine[...]).astype(BF)

    @pl.loop(2 * heads // step_cols, 3 * heads // step_cols)
    def _(step):
        cols = pl.ds(pl.multiple_of(step * step_cols, step_cols), step_cols)
        qkv[:, cols] = dot(normed[...], qkv_w[:, cols]).astype(BF)

    attend(qkv, attended, bias, heads)
    wait_all(load_out)
    tile = parts[0].shape[0]

    @pl.loop(0, out_w.shape[1] // step_cols)
    def _(step):
        cols = pl.ds(pl.multiple_of(step * step_cols, step_cols), step_cols)
        product = dot(attended[...], out_w[:, cols])
        for slot, part in enumerate(parts):
            part[:, cols] = product[slot * tile : (slot + 1) * tile, :].astype(part.dtype)


def attn_fwd(rows, gain, tables, tags, width, qkv_pieces, out_pieces):
    nrow, (tile, dim) = len(rows), rows[0].shape
    tokens = nrow * tile
    heads = out_pieces[0].shape[0]
    npiece = len(tags)
    return pl.pallas_call(
        partial(attn_fwd_kernel, tags, width, nrow),
        out_shape=[
            shape((tokens, dim), BF),
            shape((tokens, 3 * heads), BF),
            shape((tokens, heads), BF),
            shape((tokens, 1), F32),
        ]
        + [shape((tile, dim), F32 if slot == 0 else BF) for slot in range(nrow)],
        in_specs=[anyspace()] * nrow + [vmem()] * 6 + [anyspace()] * (2 * npiece),
        out_specs=[vmem()] * (4 + nrow),
        scratch_shapes=[
            pltpu.VMEM((tokens, dim), BF),
            pltpu.VMEM((dim, 3 * heads), BF),
            pltpu.VMEM((heads, dim), BF),
            pltpu.VMEM((tokens, tokens), F32),
            pltpu.SemaphoreType.DMA((nrow,)),
            pltpu.SemaphoreType.DMA((npiece,)),
            pltpu.SemaphoreType.DMA((npiece,)),
        ],
        compiler_params=params(),
        cost_estimate=cost(2 * tokens * dim * 4 * heads * 3, 20e6),
        name="attn_fwd",
    )(*rows, gain, *tables, *qkv_pieces, *out_pieces)


def attend_back(qkv, d_attended, d_qkv, bias, cosine, sine, heads):
    score_scale = HEAD_DIM ** (-0.5)

    @pl.loop(0, heads // 128)
    def _(pair):
        base = pl.multiple_of(pair * 128, 128)
        query = qkv[:, pl.ds(base, 128)]
        key = qkv[:, pl.ds(heads + base, 128)]
        value = qkv[:, pl.ds(2 * heads + base, 128)]
        grad = d_attended[:, pl.ds(base, 128)]
        sums = [0.0, 0.0, 0.0]
        for half in range(2):
            lanes = head_lanes(128, half).astype(BF)
            own_query = query * (lanes * score_scale)
            own_grad = grad * lanes
            probs = probabilities(own_query, key, bias[...])
            d_value = dot_cols(probs.astype(BF), own_grad)
            d_probs = dot_rows(own_grad, value)
            delta = jnp.sum(probs * d_probs, axis=-1, keepdims=True)
            d_scores = (probs * (d_probs - delta)).astype(BF)
            d_query = dot(d_scores, key * lanes) * score_scale
            d_key = dot_cols(d_scores, own_query)
            sums = [sums[0] + d_query, sums[1] + d_key, sums[2] + d_value]
        back = -sine[:, :128]
        d_qkv[:, pl.ds(base, 128)] = turn(sums[0], cosine[:, :128], back).astype(BF)
        d_qkv[:, pl.ds(heads + base, 128)] = turn(sums[1], cosine[:, :128], back).astype(BF)
        d_qkv[:, pl.ds(2 * heads + base, 128)] = sums[2].astype(BF)


def attn_bwd_kernel(tags, width, nrow, npart, *refs):
    npiece = len(tags)
    nhid, nrow = nrow[1], nrow[0]
    rows_in, hidden_in = refs[:nrow], refs[nrow : nrow + nhid]
    refs = refs[nrow + nhid :]
    qkv, inverses, cosine, sine, first, last, key_index = refs[:7]
    rest = refs[7:]
    qkv_in, out_in = rest[:npiece], rest[npiece : 2 * npiece]
    rest = rest[2 * npiece :]
    branch, d_qkv, gain_grad = rest[:3]
    parts = rest[3 : 3 + npart]
    hidden, d_attended, qkv_w, out_w, bias, sem_rows, sem_x, sem_qkv, sem_out = rest[3 + npart :]
    load_rows = row_copies(rows_in, branch, sem_rows)
    load_x = row_copies(hidden_in, hidden, sem_x)
    load_out = place_copies(tags, out_in, out_w, sem_out, 1, width)
    load_qkv = place_copies(tags, qkv_in, qkv_w, sem_qkv, 0, width)
    start_all(load_rows + load_out + load_qkv + load_x)
    fill_bias(bias, first, last, key_index)
    wait_all(load_rows)
    wait_all(load_out)
    heads = out_w.shape[0]
    step_cols = 256

    @pl.loop(0, heads // step_cols)
    def _(step):
        cols = pl.ds(pl.multiple_of(step * step_cols, step_cols), step_cols)
        d_attended[:, cols] = dot_rows(branch[...], out_w[cols, :]).astype(BF)

    attend_back(qkv, d_attended, d_qkv, bias, cosine, sine, heads)
    wait_all(load_qkv)
    wait_all(load_x)
    tile = parts[0].shape[0]

    @pl.loop(0, qkv_w.shape[0] // step_cols)
    def _(step):
        cols = pl.ds(pl.multiple_of(step * step_cols, step_cols), step_cols)
        product = dot_rows(d_qkv[...], qkv_w[cols, :])
        gain_grad[:, cols] = jnp.sum(product * (hidden[:, cols].astype(F32) * inverses[...]), axis=0, keepdims=True)
        for slot, part in enumerate(parts):
            part[:, cols] = product[slot * tile : (slot + 1) * tile, :].astype(part.dtype)


def attn_bwd(rows, hidden, qkv, inverses, tables, tags, width, qkv_pieces, out_pieces, npart):
    nrow, nhid, dim = len(rows), len(hidden), rows[0].shape[1]
    tokens = qkv.shape[0]
    tile = tokens // npart
    heads = out_pieces[0].shape[0]
    npiece = len(tags)
    return pl.pallas_call(
        partial(attn_bwd_kernel, tags, width, (nrow, nhid), npart),
        out_shape=[shape((tokens, dim), BF), shape((tokens, 3 * heads), BF), shape((1, dim), F32)]
        + [shape((tile, dim), F32 if slot == 0 else BF) for slot in range(npart)],
        in_specs=[anyspace()] * (nrow + nhid) + [vmem()] * 7 + [anyspace()] * (2 * npiece),
        out_specs=[vmem()] * (3 + npart),
        scratch_shapes=[
            pltpu.VMEM((tokens, dim), BF),
            pltpu.VMEM((tokens, heads), BF),
            pltpu.VMEM((dim, 3 * heads), BF),
            pltpu.VMEM((heads, dim), BF),
            pltpu.VMEM((tokens, tokens), F32),
            pltpu.SemaphoreType.DMA((nrow,)),
            pltpu.SemaphoreType.DMA((nhid,)),
            pltpu.SemaphoreType.DMA((npiece,)),
            pltpu.SemaphoreType.DMA((npiece,)),
        ],
        compiler_params=params(),
        cost_estimate=cost(2 * tokens * dim * 4 * heads * 6, 30e6),
        name="attn_bwd",
    )(*rows, *hidden, qkv, inverses, *tables, *qkv_pieces, *out_pieces)


def mlp_kernel(tags, width, nrow, npart, *refs):
    npiece = len(tags)
    sent_in, cot_in = refs[:nrow], refs[nrow : 2 * nrow]
    gain = refs[2 * nrow]
    rest = refs[2 * nrow + 1 :]
    gate_in, up_in, down_in = rest[:npiece], rest[npiece : 2 * npiece], rest[2 * npiece : 3 * npiece]
    rest = rest[3 * npiece :]
    normed, hidden, d_gate, d_up, gain_grad = rest[:5]
    parts = rest[5 : 5 + npart]
    sent, cot, inverses, gate_w, up_w, down_w, sem_sent, sem_cot, sem_gate, sem_up, sem_down = rest[5 + npart :]
    load_sent = row_copies(sent_in, sent, sem_sent)
    load_cot = row_copies(cot_in, cot, sem_cot)
    load_gate = place_copies(tags, gate_in, gate_w, sem_gate, 0, width)
    load_up = place_copies(tags, up_in, up_w, sem_up, 0, width)
    load_down = place_copies(tags, down_in, down_w, sem_down, 1, width)
    start_all(load_sent + load_cot + load_gate + load_up + load_down)
    wait_all(load_sent)
    norm_rows(sent, normed, inverses, gain, 64)
    wait_all(load_cot)
    wait_all(load_gate)
    wait_all(load_up)
    wait_all(load_down)
    step_cols = 256

    @pl.loop(0, gate_w.shape[1] // step_cols)
    def _(step):
        cols = pl.ds(pl.multiple_of(step * step_cols, step_cols), step_cols)
        gate = dot(normed[...], gate_w[:, cols])
        up = dot(normed[...], up_w[:, cols])
        d_hidden = dot_rows(cot[...], down_w[cols, :])
        s = jax.nn.sigmoid(gate)
        activated = gate * s
        hidden[:, cols] = (activated * up).astype(BF)
        d_gate[:, cols] = (d_hidden * up * (s + activated * (1.0 - s))).astype(BF)
        d_up[:, cols] = (d_hidden * activated).astype(BF)

    tile = parts[0].shape[0]

    @pl.loop(0, gate_w.shape[0] // step_cols)
    def _(step):
        cols = pl.ds(pl.multiple_of(step * step_cols, step_cols), step_cols)
        product = dot_rows(d_gate[...], gate_w[cols, :]) + dot_rows(d_up[...], up_w[cols, :])
        gain_grad[:, cols] = jnp.sum(product * (sent[:, cols].astype(F32) * inverses[...]), axis=0, keepdims=True)
        for slot, part in enumerate(parts):
            part[:, cols] = product[slot * tile : (slot + 1) * tile, :].astype(part.dtype)


def mlp(sent, cot, gain, tags, width, gate_pieces, up_pieces, down_pieces, npart):
    nrow, dim = len(sent), sent[0].shape[1]
    tokens = nrow * sent[0].shape[0]
    tile = tokens // npart
    units = gate_pieces[0].shape[1]
    npiece = len(tags)
    return pl.pallas_call(
        partial(mlp_kernel, tags, width, nrow, npart),
        out_shape=[shape((tokens, dim), BF)]
        + [shape((tokens, units), BF)] * 3
        + [shape((1, dim), F32)]
        + [shape((tile, dim), F32 if slot == 0 else BF) for slot in range(npart)],
        in_specs=[anyspace()] * (2 * nrow) + [vmem()] + [anyspace()] * (3 * npiece),
        out_specs=[vmem()] * (5 + npart),
        scratch_shapes=[
            pltpu.VMEM((tokens, dim), BF),
            pltpu.VMEM((tokens, dim), BF),
            pltpu.VMEM((tokens, 1), F32),
            pltpu.VMEM((dim, units), BF),
            pltpu.VMEM((dim, units), BF),
            pltpu.VMEM((units, dim), BF),
            pltpu.SemaphoreType.DMA((nrow,)),
            pltpu.SemaphoreType.DMA((nrow,)),
            pltpu.SemaphoreType.DMA((npiece,)),
            pltpu.SemaphoreType.DMA((npiece,)),
            pltpu.SemaphoreType.DMA((npiece,)),
        ],
        compiler_params=params(),
        cost_estimate=cost(2 * tokens * dim * units * 5, 40e6),
        name="mlp",
    )(*sent, *cot, gain, *gate_pieces, *up_pieces, *down_pieces)


def mlp_out_kernel(tags, width, *refs):
    npiece = len(tags)
    hidden, down_in = refs[0], refs[1 : 1 + npiece]
    *parts, down_w, sem_down = refs[1 + npiece :]
    load_down = place_copies(tags, down_in, down_w, sem_down, 1, width)
    start_all(load_down)
    wait_all(load_down)
    tile, step_cols = parts[0].shape[0], 256

    @pl.loop(0, down_w.shape[1] // step_cols)
    def _(step):
        cols = pl.ds(pl.multiple_of(step * step_cols, step_cols), step_cols)
        product = dot(hidden[...], down_w[:, cols])
        for slot, part in enumerate(parts):
            part[:, cols] = product[slot * tile : (slot + 1) * tile, :].astype(part.dtype)


def mlp_out(hidden, nrow, dim, tags, width, down_pieces):
    tokens, units = hidden.shape
    tile, npiece = tokens // nrow, len(tags)
    return pl.pallas_call(
        partial(mlp_out_kernel, tags, width),
        out_shape=[shape((tile, dim), F32 if slot == 0 else BF) for slot in range(nrow)],
        in_specs=[vmem()] + [anyspace()] * npiece,
        out_specs=[vmem()] * nrow,
        scratch_shapes=[pltpu.VMEM((units, dim), BF), pltpu.SemaphoreType.DMA((npiece,))],
        compiler_params=params(),
        cost_estimate=cost(2 * tokens * dim * units, 14e6),
        name="mlp_out",
    )(hidden, *down_pieces)


def slice_of(slot, width, own):
    index = lax.axis_index("dp")
    owner = index ^ (2 * slot)
    return pl.ds(pl.multiple_of((owner if own else lax.div(owner, 2)) * width, width), width)

MESH = pl.DeviceIdType.MESH
NEAR = (2, 4, 6)
PARTS = 2
GROUPS = 4


def remote(source, target, send_sem, recv_sem, axis, peer):
    return pltpu.make_async_remote_copy(
        src_ref=source,
        dst_ref=target,
        send_sem=send_sem,
        recv_sem=recv_sem,
        device_id={axis: peer},
        device_id_type=MESH,
    )


def drain(ref, sem):
    pltpu.make_async_copy(ref, ref, sem).wait()


def meet():
    own, rank = lax.axis_index("dp"), lax.axis_index("tensor")
    barrier = pltpu.get_barrier_semaphore()
    for flip in range(1, 8):
        pl.semaphore_signal(barrier, inc=1, device_id={"dp": own ^ flip}, device_id_type=MESH)

    @pl.when(rank < 3)
    def _():
        pl.semaphore_signal(barrier, inc=1, device_id={"tensor": rank + 1}, device_id_type=MESH)

    @pl.when(rank > 0)
    def _():
        pl.semaphore_signal(barrier, inc=1, device_id={"tensor": rank - 1}, device_id_type=MESH)

    pl.semaphore_wait(barrier, 8 + lax.div(rank * (3 - rank), 2))


def at_cols(ref, index, width):
    return ref.at[:, pl.ds(pl.multiple_of(index * width, width), width)]


def at_rows(ref, index, width):
    return ref.at[pl.ds(pl.multiple_of(index * width, width), width), :]


def either(rank, *choices):
    result = rank == choices[0]
    for choice in choices[1:]:
        result = result | (rank == choice)
    return result


def ends(rank):
    return either(rank, 0, 3)


def inner(rank):
    return either(rank, 1, 2)


class RowGather:
    def __init__(self, rank, source, landing, part, size, send, recv):
        self.rank = rank

        def place(slot):
            return landing.at[pl.ds(pl.multiple_of((4 * part + slot) * size, size), size), :]

        def copy(origin, slot, peer):
            return remote(origin, place(slot), send.at[part], recv.at[part, slot - 1], "tensor", peer)

        def forward(slot, target, peer):
            return copy(place(slot), target, peer)

        outward, inward = (rank - 1) * 3, 3 - rank
        near, far = 5 - 2 * rank, 2 * rank - 1
        self.up, self.down = copy(source, 1, rank + 1), copy(source, 3, rank - 1)
        self.hops = [forward(near, 2, outward), forward(far, 2, inward), forward(2, far, outward)]
        self.slots = [near, far, 2]
        self.arrival = lambda slot: copy(source, slot, lax.rem(rank + 1, 4))
        self.sent = lambda count: drain(landing.at[pl.ds(0, count * size), :], send.at[part])

    def start(self):
        pl.when(self.rank < 3)(self.up.start)
        pl.when(self.rank > 0)(self.down.start)

    def hop(self, index):
        @pl.when(inner(self.rank))
        def _():
            self.arrival(self.slots[index]).wait_recv()
            self.hops[index].start()

    def wait(self):
        @pl.when(ends(self.rank))
        def _():
            for slot in (1, 2, 3):
                self.arrival(slot).wait_recv()

    def finish(self):
        pl.when(ends(self.rank))(lambda: self.sent(1))
        pl.when(inner(self.rank))(lambda: self.sent(5))


class RowScatter:
    def __init__(self, rank, source, landing, part, size, send, recv, staged=None, sem=None):
        self.rank, self.source, self.size, self.staged, self.sem = rank, source, size, staged, sem
        self.place = lambda k: pl.ds(pl.multiple_of((4 * part + k) * size, size), size)
        self.land = lambda slot: landing.at[pl.ds((5 * part + slot) * size, size), :]

        def copy(k, slot, peer):
            return remote(source.at[self.place(k), :], self.land(slot), send.at[part], recv.at[part, slot], "tensor", peer)

        end = lax.div(rank, 3)
        self.first = [copy(index + 1 + end * (2 - 2 * index), index, 1 + end) for index in range(3)]
        self.keys = [2, 5 - 2 * rank, 2 * rank - 1]
        self.later = [
            copy(self.keys[0], 3, 3 - rank),
            copy(self.keys[1], 4, 3 - rank),
            copy(self.keys[2], 4, (rank - 1) * 3),
        ]
        self.arrival = lambda slot: copy(1, slot, lax.rem(rank + 1, 4))
        self.finish = lambda: drain(source.at[pl.ds(0, 3 * size), :], send.at[part])

    def start(self, indices=(0, 1, 2)):
        @pl.when(ends(self.rank))
        def _():
            for index in indices:
                self.first[index].start()

    def hop(self, index):
        @pl.when(inner(self.rank))
        def _():
            slot = (0, 1, 3)[index]
            self.arrival(slot).wait_recv()
            other = self.land(slot)
            if self.staged is not None:
                load = pltpu.make_async_copy(other, self.staged, self.sem)
                load.start()
                load.wait()
                other = self.staged
            target = self.source.at[self.place(self.keys[index]), :]

            @pl.loop(0, self.size // 16)
            def _(step):
                rows = pl.ds(pl.multiple_of(step * 16, 16), 16)
                target[rows, :] = (target[rows, :].astype(F32) + other[rows, :].astype(F32)).astype(BF)

            self.later[index].start()

    def wait(self):
        pl.when(inner(self.rank))(self.arrival(2).wait_recv)
        self.arrival(4).wait_recv()


def fill_mask(bias, docs, size):
    rank = lax.axis_index("tensor")
    tokens = bias.shape[0]
    values = docs[...]
    starts = [jnp.sum(jnp.where(values < number, 1, 0), keepdims=True) for number in range(1, 8)]

    def document(position):
        return sum(jnp.where(position >= start, 1, 0) for start in starts)

    lane = lax.broadcasted_iota(jnp.int32, (1, tokens), 1)
    slot = lax.rem(lax.div(lane, size), 4)
    part = lax.div(lane, 4 * size)
    keys = lax.rem(rank - slot + 4, 4) * (2 * size) + part * size + lax.rem(lane, size)
    key_docs = document(keys)

    @pl.loop(0, tokens // size)
    def _(block):
        base = lax.rem(rank - lax.rem(block, 4) + 4, 4) * (2 * size) + lax.div(block, 4) * size
        queries = base + lax.broadcasted_iota(jnp.int32, (size, 1), 0)
        allowed = (document(queries) == key_docs) & (queries >= keys)
        bias[pl.ds(pl.multiple_of(block * size, size), size), :] = jnp.where(allowed, 0.0, NEGATIVE)


def fill_turns(cosine, sine, size):
    rank = lax.axis_index("tensor")
    half_size = HEAD_DIM // 2
    dims = (size, cosine.shape[1])
    lane = lax.broadcasted_iota(jnp.int32, dims, 1)
    row = lax.broadcasted_iota(jnp.int32, dims, 0)
    frequency = jnp.exp(lax.rem(lane, half_size).astype(F32) * (-math.log(ROPE_BASE) / half_size))
    sign = jnp.where(lax.rem(lane, HEAD_DIM) < half_size, -1.0, 1.0)

    @pl.loop(0, cosine.shape[0] // size)
    def _(block):
        start = (lax.rem(rank - lax.rem(block, 4) + 4, 4) * PARTS + lax.div(block, 4)) * size
        angles = (row + start).astype(F32) * frequency
        rows = pl.ds(pl.multiple_of(block * size, size), size)
        cosine[rows, :] = jnp.cos(angles)
        sine[rows, :] = jnp.sin(angles) * sign


def slice_of(slot, width, own):
    index = lax.axis_index("dp")
    owner = index ^ (2 * slot)
    return pl.ds(pl.multiple_of((owner if own else lax.div(owner, 2)) * width, width), width)


def layer_kernel(*refs):
    hidden_in, cot_in, *gains_hbm = refs[:4]
    weights_in = refs[4:11]
    docs_hbm = refs[11]
    down_sum, gate_sum, up_sum, qkv_parts, out_parts = refs[12:17]
    down_parts, gate_parts, up_parts = refs[17:20]
    grad_merge = refs[20:25]
    pair_gate, pair_up, pair_qkv, pair_attended, pair_normed, pair_branch = refs[25:31]
    branch_rows, hidden_rows, normed_rows, mlp_recv, qkv_full, down_full = refs[31:37]
    out_ref, input_ref, gain_out = refs[37:40]
    gate_w, up_w, down_w, sent, cot, normed, hidden, d_gate, d_up = refs[40:49]
    two_half, cot_half, buffer_a, buffer_b, buffer_c, out_w = refs[49:55]
    qkv, attended, d_attended, bias, cosine, sine = refs[55:61]
    inverses_one, inverses, middle, grad_middle, send_part, recv_part = refs[61:67]
    gains_in, gains, gain_part, gain_recv, gain_z, layer_out, input_grad, gain_total, docs, *plain_gains = refs[67:78]
    a_send, a_recv, f_send, f_recv, h_send, h_recv, z_send, z_recv, r_send, r_recv = refs[78:88]
    w_send, w_recv, d_send, d_recv, g_send, g_recv, y_send, y_recv, load, keep, down_load, s_recv, n_recv = refs[88:]

    own, rank = lax.axis_index("dp"), lax.axis_index("tensor")
    core = lax.rem(own, 2)
    tokens, dim = sent.shape
    units = gate_w.shape[1]
    tile = hidden_in.shape[0]
    size = tile // PARTS
    span = 4 * size
    heads = attended.shape[1]
    width = weights_in[0].shape[0]
    half = dim // (2 * width)
    d_qkv = cot.at[:, pl.ds(heads, 3 * heads)]
    group = units // GROUPS
    step_cols = 256
    count = dim // step_cols

    def cols_of(step, length=step_cols):
        return pl.ds(pl.multiple_of(step * length, length), length)

    def local(source, target, sem):
        return pltpu.make_async_copy(source, target, sem)

    def own_rows(part):
        return pl.ds(part * span, size)

    def part_rows(part):
        return pl.ds(part * size, size)

    def source_of(item):
        if item < 4:
            return weights_in[item]
        which, start = (item - 4) % 3, ((item - 4) // 3) * group
        if which == 2:
            return weights_in[4].at[pl.ds(start, group), :]
        return weights_in[5 + which].at[:, pl.ds(start, group)]

    def view(item, owner, part=None):
        rows = heads if item == 3 else group if item > 3 and (item - 4) % 3 == 2 else width
        length = rows if part is None else rows // 2
        start = 0 if part is None else part * length
        if item < 3:
            place = pl.ds(pl.multiple_of(owner * width + start, length), length)
            return down_w.at[place, pl.ds(item * heads, heads)]
        if item == 3:
            return out_w.at[pl.ds(start, length), pl.ds(pl.multiple_of(owner * width, width), width)]
        which, offset = (item - 4) % 3, ((item - 4) // 3) * group
        if which == 2:
            return down_full.at[pl.ds(offset + start, length), pl.ds(pl.multiple_of(owner * width, width), width)]
        place = pl.ds(pl.multiple_of(owner * width + start, length), length)
        return (gate_w, up_w)[which].at[place, pl.ds(offset, group)]

    def phase_of(item):
        return 0 if item < 3 else 1 if item == 3 else 2 + (item - 4) // 3

    def lot_of(item):
        return item if item < 4 else 4 + (item - 4) // 3

    def send_weight(item, flip):
        sem = s_recv.at[phase_of(item)] if flip == 1 else a_recv.at[lot_of(item), flip // 2 - 1]
        return remote(source_of(item), view(item, own), a_send.at[phase_of(item)], sem, "dp", own ^ flip)

    def relay_weight(item, part):
        place = view(item, own ^ (4 - 2 * part), part)
        return remote(place, place, a_send.at[phase_of(item)], a_recv.at[lot_of(item), 2], "dp", own ^ (2 + 2 * part))

    def pass_weight(item, flip):
        place = view(item, own ^ flip)
        return remote(place, place, a_send.at[phase_of(item)], s_recv.at[phase_of(item)], "dp", own ^ 1)

    def send_weights(items):
        for item in items:
            for flip in (2, 4, 1):
                send_weight(item, flip).start()

    def lots(items):
        return [[item] for item in items] if items[0] < 4 else [items]

    def arrived_weights(lot, tag):
        drain(gate_w.at[pl.ds(0, len(lot) * width // 4), :], a_recv.at[lot_of(lot[0]), tag])

    def relay_weights(items):
        for lot in lots(items):
            arrived_weights(lot, 1)
            for item in lot:
                relay_weight(item, 0).start()
            arrived_weights(lot, 0)
            for item in lot:
                relay_weight(item, 1).start()
            for item in lot:
                pass_weight(item, 4).start()
                pass_weight(item, 2).start()

    def pass_weights(items):
        for lot in lots(items):
            arrived_weights(lot, 2)
            for item in lot:
                pass_weight(item, 6).start()

    def have_weights(phase):
        drain(gate_w.at[pl.ds(0, width if phase == 1 else 3 * width), :], s_recv.at[phase])

    def sent_weights(phase):
        length = 7 * width // 4
        drain(gate_w.at[pl.ds(0, length if phase == 1 else 3 * length), :], a_send.at[phase])

    def items_of(index):
        return list(range(4 + 3 * index, 7 + 3 * index))

    def send_gain(flip):
        return remote(gains_in, at_cols(gains, own, width), y_send.at[0], y_recv.at[0], "dp", own ^ flip)

    def gathers(kind, source, landing):
        return [
            RowGather(rank, source(part), landing, part, size, z_send.at[kind], z_recv.at[kind]) for part in range(PARTS)
        ]

    gather_hidden = gathers(0, lambda part: hidden_in.at[part_rows(part), :], buffer_b)
    gather_cot = gathers(1, lambda part: cot_in.at[part_rows(part), :], cot)
    gather_sent = gathers(0, lambda part: sent.at[own_rows(part), :], sent)
    gather_branch = gathers(0, lambda part: sent.at[own_rows(part), :], branch_rows)

    def scatters(kind, source, landing, staged=None, sem=None):
        return [
            RowScatter(rank, source, landing, part, size, r_send.at[kind], r_recv.at[kind], staged, sem)
            for part in range(PARTS)
        ]

    gate_stage = up_w.at[pl.ds(4 * width, size), :]
    out_scatter = scatters(0, send_part, recv_part)
    two_scatter = scatters(0, send_part, recv_part)
    mlp_scatter = scatters(1, sent, mlp_recv, gate_stage, load.at[3])
    one_scatter = scatters(0, send_part, recv_part)

    def arrived(part, slot):
        return pl.ds((5 * part + slot) * size, size)

    def clear(part):
        @pl.when(ends(rank))
        def _():
            recv_part[arrived(part, 2), :] = jnp.zeros((size, dim), BF)

    def received(part, start, length, base):
        total = base
        for slot in (2, 4):
            rows = pl.ds(pl.multiple_of((5 * part + slot) * size + start, length), length)
            total = total + recv_part[rows, :].astype(F32)
        return total

    def to_pair(source, target, row, slot):
        return remote(source, target, h_send.at[row], h_recv.at[row], "dp", own ^ 1)

    def halves(source, target, row):
        return [
            to_pair(at_cols(source, 2 * slot + 1 - core, width), at_cols(target, slot, width), row, slot)
            for slot in range(half)
        ]

    def send_ff(step, which):
        cols = cols_of(step)
        source = (hidden, d_gate, d_up)[which].at[:, cols]
        target = (buffer_a, pair_gate, pair_up)[which].at[:, cols]
        arrival = lax.div(step, group // step_cols) if which == 0 else GROUPS - 1 + which
        return remote(source, target, f_send.at[which], f_recv.at[arrival], "dp", own ^ 1)

    def piece(index, slot):
        if index < 3:
            return at_rows(gate_w, (index - 1) * 4 + slot, width)
        if index == 3:
            return (hidden, d_gate)[slot // 2].at[pl.ds((slot % 2) * width, width), pl.ds(0, 3 * heads)]
        return at_cols(d_up, slot, width)

    def landing_of(index, slot):
        ref = (down_parts, gate_parts, up_parts, qkv_parts, out_parts)[index]
        if index < 3:
            return at_rows(ref, slot - 1, width)
        return at_cols(ref, slot, width) if index == 4 else at_rows(ref, slot, width)

    def half_of(ref, index, part):
        rows, cols = ref.shape
        if index == 4:
            return ref.at[pl.ds(part * (rows // 2), rows // 2), :]
        return ref.at[:, pl.ds(part * (cols // 2), cols // 2)]

    def stage_of(index, part):
        if index == 4:
            return up_w.at[pl.ds(7 * width, heads // 2), pl.ds(part * width, width)]
        length = units // 2 if index < 3 else 3 * heads // 2
        return up_w.at[pl.ds((3 + index) * width, width), pl.ds(part * (units // 2), length)]

    def send_far(index, part):
        return remote(
            half_of(piece(index, 3), index, part),
            half_of(grad_merge[index], index, part),
            w_send.at[index - 1],
            w_recv.at[index - 1, part],
            "dp",
            own ^ (2 + 2 * part),
        )

    def send_near(index, slot, part):
        return remote(
            half_of(piece(index, slot), index, part),
            half_of(landing_of(index, slot), index, part),
            w_send.at[index - 1],
            n_recv.at[index - 1],
            "dp",
            own ^ (2 * slot),
        )

    def keep_grad(index):
        return local(piece(index, 0), landing_of(index, 0), keep.at[index])

    def merge_grads(index):
        loads = [local(half_of(grad_merge[index], index, part), stage_of(index, part), load.at[part]) for part in range(2)]
        for part in range(2):
            send_far(index, part).wait_recv()
            loads[part].start()
        for part in range(2):
            loads[part].wait()
            target, source = half_of(piece(index, 2 - part), index, part), stage_of(index, part)
            length = source.shape[0] // 4

            @pl.loop(0, 4)
            def _(step):
                rows = cols_of(step, length)
                target[rows, :] = (target[rows, :].astype(F32) + source[rows, :].astype(F32)).astype(BF)

            send_near(index, 2 - part, part).start()

    def row_grads(index, slot, left, left_pair, right, right_pair, columns):
        mine, theirs = slice_of(slot, width, True), slice_of(slot, width, False)
        turned, turned_pair = jnp.transpose(left[:, mine]), jnp.transpose(left_pair[:, theirs])
        target = piece(index, slot)

        @pl.loop(0, columns // 512)
        def _(step):
            cols = cols_of(step, 512)
            total = dot(turned, right[:, cols]) + dot(turned_pair, right_pair[:, cols])
            target[:, cols] = total.astype(BF)

        if slot == 3:
            send_far(index, 0).start()
            send_far(index, 1).start()
        elif slot:
            send_near(index, slot, slot - 1).start()
        elif index == 3:
            keep_grad(index).start()

    def out_grads():
        for part in range(2):
            rows = pl.ds(part * (heads // 2), heads // 2)
            turned, turned_pair = jnp.transpose(attended[:, rows]), jnp.transpose(cot[:, rows])
            for slot in range(4):
                mine, theirs = slice_of(slot, width, True), slice_of(slot, width, False)
                total = dot(turned, buffer_a[:, mine]) + dot(turned_pair, cot_half[:, theirs])
                piece(4, slot)[rows, :] = total.astype(BF)
            send_far(4, part).start()
            send_near(4, part + 1, part).start()
        keep_grad(4).start()

    def down_piece(slot, index, part=None):
        cols = pl.ds(((slot % 2) * GROUPS + index) * width, width)
        rows = pl.ds(0, group) if part is None else pl.ds(part * (group // 2), group // 2)
        return (buffer_b, buffer_c)[slot // 2].at[rows, cols]

    def down_rows(ref, index, slot, part=None):
        rows = pl.ds(index * group, group) if part is None else pl.ds(index * group + part * (group // 2), group // 2)
        return ref.at[rows, pl.ds(slot * width, width)]

    def send_down(kind, index, part):
        if kind == 0:
            target, source = down_rows(grad_merge[0], index, 0, part), down_piece(3, index, part)
            peer = own ^ (2 + 2 * part)
        else:
            target, source = down_rows(down_parts, index, kind - 1, part), down_piece(kind, index, part)
            peer = own ^ (2 * kind)
        return remote(source, target, d_send.at[0], d_recv.at[GROUPS if kind else index], "dp", peer)

    def down_grads(index):
        drain(buffer_a.at[:, pl.ds(index * group, group)], f_recv.at[index])

        @pl.loop(0, group // 256)
        def _(step):
            cols = pl.ds(pl.multiple_of(index * group + step * 256, 256), 256)
            rows = pl.ds(pl.multiple_of(step * 256, 256), 256)
            turned, turned_pair = jnp.transpose(hidden[:, cols]), jnp.transpose(buffer_a[:, cols])
            for slot in range(4):
                mine, theirs = slice_of(slot, width, True), slice_of(slot, width, False)
                total = dot(turned, cot[:, mine]) + dot(turned_pair, cot_half[:, theirs])
                down_piece(slot, index)[rows, :] = total.astype(BF)

        for part in range(2):
            send_down(0, index, part).start()
        for part in range(2):
            send_down(1 + part, index, part).start()

    def merge_down(indices):
        entries = [(index, part) for index in indices for part in range(2)]

        def stage(index, part):
            rows = pl.ds(part * (group // 2), group // 2)
            return d_attended.at[rows, pl.ds((index % 2) * width, width)]

        loads = [
            local(down_rows(grad_merge[0], index, 0, part), stage(index, part), load.at[2 * (index % 2) + part])
            for index, part in entries
        ]
        for index in indices:
            drain(down_rows(grad_merge[0], index, 0), d_recv.at[index])
        start_all(loads)
        for copy, (index, part) in zip(loads, entries):
            copy.wait()
            target, source = down_piece(2 - part, index, part), stage(index, part)

            @pl.loop(0, 2)
            def _(step):
                rows = cols_of(step, group // 4)
                target[rows, :] = (target[rows, :].astype(F32) + source[rows, :].astype(F32)).astype(BF)

            send_down(2 - part, index, part).start()

    def norm_back(total, values, gain):
        inverse = lax.rsqrt(jnp.mean(values * values, axis=-1, keepdims=True) + EPSILON)
        scaled = total * gain
        return inverse * (scaled - values * inverse * inverse * jnp.mean(scaled * values, axis=-1, keepdims=True))

    first_loads = [local(source, target, load.at[12 + index]) for index, (source, target) in enumerate(
        zip((docs_hbm, *gains_hbm), (docs, *plain_gains))
    )]
    meet()
    start_all(first_loads)
    send_weights(range(3))
    for gather in gather_hidden:
        gather.start()
    wait_all(first_loads)
    gains_in[...] = jnp.zeros(gains_in.shape, F32)
    for index, plain in enumerate(plain_gains):
        gains_in[index : index + 1, :] = plain[...].astype(F32).reshape(1, width)
    for flip in range(1, 8):
        send_gain(flip).start()
    stage_down = down_w.at[:, pl.ds(3 * heads, width)]
    stage_in = local(weights_in[4], stage_down, load.at[0])
    own_loads = [local(gains_in, at_cols(gains, own, width), load.at[1])]
    own_loads += [local(weights_in[item], view(item, own), load.at[2 + item]) for item in range(4)]
    own_loads += [local(weights_in[5], at_rows(gate_w, own, width), load.at[6])]
    own_loads += [local(weights_in[6], at_rows(up_w, own, width), load.at[7])]
    for part in range(PARTS):
        own_loads.append(local(hidden_in.at[part_rows(part), :], buffer_b.at[own_rows(part), :], load.at[8 + part]))
        own_loads.append(local(cot_in.at[part_rows(part), :], cot.at[own_rows(part), :], load.at[10 + part]))
    start_all([stage_in] + own_loads)
    fill_mask(bias, docs, size)
    fill_turns(cosine, sine, size)
    for part in range(PARTS):
        clear(part)
    relay_weights([0])
    gather_hidden[0].hop(0)
    gather_hidden[0].hop(1)
    relay_weights([1])
    gather_hidden[1].hop(0)
    gather_hidden[1].hop(1)
    gather_hidden[0].hop(2)
    relay_weights([2])
    send_weights([3, 4])
    gather_hidden[1].hop(2)
    for gather in gather_cot:
        gather.start()
    stage_in.wait()
    stage_out = local(stage_down, at_cols(down_full, own, width), keep.at[5])
    stage_out.start()
    wait_all(own_loads)
    drain(gain_recv.at[pl.ds(0, 56), :], y_recv.at[0])
    gather_cot[0].hop(1)
    gather_cot[0].hop(0)
    pass_weights(range(3))
    relay_weights([3])
    send_weights(range(5, 4 + 3 * GROUPS))
    for gather in gather_hidden:
        gather.wait()

    norm_rows(buffer_b, buffer_c, inverses_one, gains.at[pl.ds(0, 1), :], 64)
    keep_hidden = local(buffer_b, hidden_rows, keep.at[0])
    keep_normed = local(buffer_c, normed_rows, keep.at[1])
    start_all([keep_hidden, keep_normed])
    have_weights(0)
    qkv_w = down_w.at[:, pl.ds(0, 3 * heads)]
    keep_qkv = local(qkv_w, qkv_full, keep.at[2])
    keep_qkv.start()

    @pl.loop(0, 2 * heads // step_cols)
    def _(step):
        cols = cols_of(step)
        product = dot(buffer_c[...], down_w[:, cols])
        turns = [jnp.concatenate([table[...]] * (step_cols // 128), axis=1) for table in (cosine, sine)]
        qkv[:, cols] = turn(product, *turns).astype(BF)

    @pl.loop(2 * heads // step_cols, 3 * heads // step_cols)
    def _(step):
        cols = cols_of(step)
        qkv[:, cols] = dot(buffer_c[...], down_w[:, cols]).astype(BF)

    attend(qkv, attended, bias, heads)
    gather_cot[0].hop(2)
    gather_cot[1].hop(1)
    gather_cot[1].hop(0)
    pass_weights([3])
    have_weights(1)

    def make_out(part):
        @pl.loop(0, count)
        def _(step):
            cols = cols_of(step)
            product = dot(attended[part * span : (part + 1) * span, :], out_w[:, cols])
            middle[part_rows(part), cols] = product[:size, :]
            send_part[pl.ds(part * span + size, span - size), cols] = product[size:, :].astype(BF)

    make_out(0)
    out_scatter[0].start()
    make_out(1)
    out_scatter[1].start()
    gather_cot[1].hop(2)
    wait_all([keep_hidden, keep_normed, keep_qkv, stage_out])
    send_normed = halves(normed_rows, pair_normed, 1)
    send_attended = to_pair(attended, pair_attended, 2, 0)
    start_all(send_normed + [send_attended])
    for index in range(3):
        out_scatter[0].hop(index)
    relay_weights(items_of(0))

    def make_sent(part):
        out_scatter[part].wait()

        @pl.loop(0, size // 32)
        def _(step):
            rows = pl.ds(pl.multiple_of(part * size + step * 32, 32), 32)
            place = pl.ds(pl.multiple_of(part * span + step * 32, 32), 32)
            total = received(part, step * 32, 32, hidden_of(place) + middle[rows, :])
            middle[rows, :] = total
            sent[place, :] = total.astype(BF)

        gather_sent[part].start()

    def hidden_of(place):
        return buffer_b[place, :].astype(F32)

    for gather in gather_hidden:
        gather.finish()
    make_sent(0)
    out_scatter[1].hop(0)
    relay_weights(items_of(1))
    gather_sent[0].hop(0)
    out_scatter[1].hop(1)
    out_scatter[1].hop(2)
    make_sent(1)
    gather_sent[0].hop(1)
    relay_weights(items_of(2))
    gather_sent[1].hop(0)
    gather_sent[1].hop(1)
    gather_sent[0].hop(2)
    gather_sent[1].hop(2)
    relay_weights(items_of(3))

    def load_down(index):
        rows = pl.ds(index * group, group)
        return local(down_full.at[rows, :], down_w.at[rows, :], down_load.at[index])

    for gather in gather_cot:
        gather.wait()
    send_cot = halves(cot, cot_half, 0)
    start_all(send_cot)
    for gather in gather_sent:
        gather.wait()
    norm_rows(sent, normed, inverses, gains.at[pl.ds(1, 1), :], 64)
    pass_weights(items_of(0))
    send_two = halves(normed, two_half, 3)
    start_all(send_two)
    have_weights(2)
    for phase in range(2):
        sent_weights(phase)
    load_down(0).start()
    for index in range(GROUPS):
        load_down(index).wait()
        if index + 1 < GROUPS:
            pass_weights(items_of(index + 1))

        @pl.loop(index * group // step_cols, (index + 1) * group // step_cols)
        def _(step):
            cols = cols_of(step)
            gate = dot(normed[...], gate_w[:, cols])
            up = dot(normed[...], up_w[:, cols])
            d_hidden = dot_rows(cot[...], down_w[cols, :])
            s = jax.nn.sigmoid(gate)
            activated = gate * s
            hidden[:, cols] = (activated * up).astype(BF)
            d_gate[:, cols] = (d_hidden * up * (s + activated * (1.0 - s))).astype(BF)
            d_up[:, cols] = (d_hidden * activated).astype(BF)
            for which in range(3):
                send_ff(step, which).start()

        if index + 1 < GROUPS:
            have_weights(3 + index)
            load_down(index + 1).start()
        if index == 0:
            drain(cot_half, h_recv.at[0])
        else:
            down_grads(index - 1)

    gain_part[...] = jnp.zeros(gain_part.shape, F32)
    for part in range(PARTS):
        out_scatter[part].finish()

    def make_two(part):
        block = slice(part * span, (part + 1) * span)

        @pl.loop(0, count)
        def _(step):
            cols = cols_of(step)
            product = dot_rows(d_gate[block, :], gate_w[cols, :]) + dot_rows(d_up[block, :], up_w[cols, :])
            gain_part[pl.ds(1, 1), cols] += jnp.sum(
                product * (sent[block, cols].astype(F32) * inverses[block, :]), axis=0, keepdims=True
            )
            grad_middle[part_rows(part), cols] = product[:size, :]
            send_part[pl.ds(part * span + size, span - size), cols] = product[size:, :].astype(BF)

    make_two(0)
    two_scatter[0].start()
    down_grads(GROUPS - 1)
    merge_down((0, 1))
    make_two(1)
    two_scatter[0].hop(0)
    two_scatter[1].start()
    for phase in range(2, 2 + GROUPS):
        sent_weights(phase)
    for which in (1, 2):
        drain((d_gate, d_up)[which - 1], f_recv.at[GROUPS - 1 + which])
    gate_pair, up_pair = up_w.at[pl.ds(0, tokens), :], up_w.at[pl.ds(tokens, tokens), :]
    pair_loads = [local(pair_gate, gate_pair, load.at[0]), local(pair_up, up_pair, load.at[1])]
    start_all(pair_loads)
    drain(two_half, h_recv.at[3])
    wait_all(pair_loads)
    gate_grads = lambda slot: row_grads(1, slot, normed, two_half, d_gate, gate_pair, units)
    up_grads = lambda slot: row_grads(2, slot, normed, two_half, d_up, up_pair, units)
    gate_grads(3)
    merge_down((2, 3))
    two_scatter[0].hop(1)
    two_scatter[0].hop(2)
    for slot in (1, 2, 0):
        gate_grads(slot)

    def make_branch(part):
        two_scatter[part].wait()

        @pl.loop(0, size // 32)
        def _(step):
            rows = pl.ds(pl.multiple_of(part * size + step * 32, 32), 32)
            place = pl.ds(pl.multiple_of(part * span + step * 32, 32), 32)
            total = received(part, step * 32, 32, grad_middle[rows, :])
            result = cot[place, :].astype(F32) + norm_back(total, sent[place, :].astype(F32), gains[1:2, :])
            grad_middle[rows, :] = result
            sent[place, :] = result.astype(BF)

        gather_branch[part].start()
        keep_branch[part].start()

    keep_branch = [
        local(sent.at[own_rows(part), :], branch_rows.at[own_rows(part), :], keep.at[6 + part]) for part in range(PARTS)
    ]
    for part in range(PARTS):
        gather_sent[part].finish()
    make_branch(0)
    up_grads(3)
    two_scatter[1].hop(0)
    up_grads(1)
    gather_branch[0].hop(0)
    two_scatter[1].hop(1)
    two_scatter[1].hop(2)
    up_grads(2)
    up_grads(0)
    def project(first, last):
        @pl.loop(first, last)
        def _(step):
            cols = cols_of(step)
            product = dot(hidden[...], down_w[:, cols])
            for part in range(PARTS):
                start = part * span
                middle[part_rows(part), cols] = middle[part_rows(part), cols] + product[start : start + size, :]
                sent[pl.ds(start + size, span - size), cols] = product[start + size : start + span, :].astype(BF)

    pl.when(ends(rank))(lambda: project(0, count))
    mlp_scatter[0].start((0,))
    make_branch(1)
    mlp_scatter[0].start((1, 2))
    mlp_scatter[1].start()
    pl.when(inner(rank))(lambda: project(0, count // 4))
    gather_branch[0].hop(1)
    merge_grads(1)
    pl.when(inner(rank))(lambda: project(count // 4, count // 2))
    gather_branch[1].hop(0)
    pl.when(inner(rank))(lambda: project(count // 2, count))
    gather_branch[1].hop(1)
    gather_branch[0].hop(2)
    gather_branch[1].hop(2)
    load_weight = local(qkv_full, qkv_w, load.at[4])
    load_hidden = local(hidden_rows, gate_pair, load.at[5])
    load_normed = local(normed_rows, up_pair, load.at[6])
    start_all([load_hidden, load_normed])
    mlp_scatter[0].hop(0)
    merge_grads(2)
    for part in range(PARTS):
        two_scatter[part].finish()
        gather_branch[part].wait()
        keep_branch[part].wait()

    load_branch = local(branch_rows, buffer_a, load.at[7])
    load_branch.start()
    load_weight.start()
    send_half = halves(branch_rows, pair_branch, 4)
    start_all(send_half)
    mlp_scatter[0].hop(1)
    load_branch.wait()

    @pl.loop(0, heads // step_cols)
    def _(step):
        cols = cols_of(step)
        d_attended[:, cols] = dot_rows(buffer_a[...], out_w[cols, :]).astype(BF)

    drain(cot_half, h_send.at[0])
    for gather in gather_cot:
        gather.finish()
    drain(two_half, h_recv.at[1])
    send_attended.wait_recv()
    early_loads = [
        local(pair_attended, cot.at[:, pl.ds(0, heads)], load.at[8]),
        local(pair_normed, two_half, load.at[9]),
    ]
    start_all(early_loads)
    attend_back(qkv, d_attended, d_qkv, bias, cosine, sine, heads)
    send_qkv = to_pair(d_qkv, pair_qkv, 5, 0)
    send_qkv.start()
    for which in range(3):
        drain((hidden, d_gate, d_up)[which], f_send.at[which])

    drain(cot_half, h_recv.at[4])
    load_half = local(pair_branch, cot_half, load.at[10])
    load_half.start()
    mlp_scatter[0].hop(2)
    mlp_scatter[1].hop(0)
    wait_all([load_weight, load_hidden, load_normed])

    def make_one(part):
        block = slice(part * span, (part + 1) * span)

        @pl.loop(0, count)
        def _(step):
            cols = cols_of(step)
            product = dot_rows(d_qkv[block, :], down_w[cols, pl.ds(0, 3 * heads)])
            gain_part[pl.ds(0, 1), cols] += jnp.sum(
                product * (gate_pair[block, cols].astype(F32) * inverses_one[block, :]), axis=0, keepdims=True
            )
            input_grad[part_rows(part), cols] = product[:size, :]
            send_part[pl.ds(part * span + size, span - size), cols] = product[size:, :].astype(BF)

        one_scatter[part].start()

    def share_gain(flip):
        source = at_cols(gain_part, own ^ flip, width)
        return remote(source, at_rows(gain_recv, flip, 8), g_send.at[0], g_recv.at[0], "dp", own ^ flip)

    make_one(0)
    mlp_scatter[1].hop(1)

    send_qkv.wait_recv()
    drain(two_half, h_send.at[3])
    load_qkv = local(pair_qkv, normed.at[:, pl.ds(0, 3 * heads)], load.at[0])
    load_qkv.start()
    wait_all(early_loads + [load_half])
    out_grads()
    mlp_scatter[1].hop(2)
    load_qkv.wait()
    for slot in (3, 1, 2, 0):
        row_grads(3, slot, up_pair, two_half, d_qkv, normed, 3 * heads)
        if slot == 2:
            one_scatter[0].hop(0)
            make_one(1)
    for flip in range(1, 8):
        share_gain(flip).start()
    one_scatter[0].hop(1)
    one_scatter[0].hop(2)
    merge_grads(4)

    drain(gate_w.at[pl.ds(0, 2 * width), :], n_recv.at[0])
    drain(gate_w.at[pl.ds(0, 2 * width), :], n_recv.at[1])
    drain(gate_w.at[pl.ds(0, units // 4), :], d_recv.at[GROUPS])
    staged = [up_w.at[pl.ds(2 * index * width, 2 * width), :] for index in range(2)]
    sum_loads = [local(ref, staged[index], load.at[4 + index]) for index, ref in enumerate((gate_parts, up_parts))]
    for index in range(GROUPS):
        for slot in range(2):
            place = buffer_a.at[:, pl.ds((slot * GROUPS + index) * width, width)]
            sum_loads.append(local(down_rows(down_parts, index, slot), place, load.at[6]))
    start_all(sum_loads)

    def add_rows(index):
        total = piece(index, 0)
        sum_loads[index - 1].wait()

        @pl.loop(0, width // 32)
        def _(step):
            rows = cols_of(step, 32)
            near = pl.ds(pl.multiple_of(width + step * 32, 32), 32)
            terms = [total[rows, :], staged[index - 1][rows, :], staged[index - 1][near, :]]
            total[rows, :] = sum(term.astype(F32) for term in terms).astype(BF)

        local(total, (gate_sum, up_sum)[index - 1], keep.at[index]).start()

    def add_down():
        drain(buffer_a, load.at[6])

        @pl.loop(0, tokens // 64)
        def _(step):
            rows = cols_of(step, 64)
            for index in range(GROUPS):
                total = down_piece(0, index)
                terms = [total[rows, :]]
                terms += [buffer_a[rows, pl.ds((slot * GROUPS + index) * width, width)] for slot in range(2)]
                total[rows, :] = sum(term.astype(F32) for term in terms).astype(BF)

        for index in range(GROUPS):
            local(down_piece(0, index), down_rows(down_sum, index, 0), keep.at[8]).start()

    one_scatter[1].hop(0)
    add_rows(1)
    merge_grads(3)
    add_rows(2)
    one_scatter[1].hop(1)
    one_scatter[1].hop(2)
    add_down()

    drain(gain_recv.at[pl.ds(8, 56), :], g_recv.at[0])
    gain_sum = gain_part[:, pl.ds(pl.multiple_of(own * width, width), width)]
    for flip in range(1, 8):
        gain_sum = gain_sum + gain_recv[pl.ds(flip * 8, 8), :]
    gain_z[pl.ds(0, 8), :] = gain_sum

    def share_gain_z(k):
        target = gain_z.at[pl.ds(8 * k, 8), :]
        return remote(gain_z.at[pl.ds(0, 8), :], target, y_send.at[1], y_recv.at[1], "tensor", lax.rem(rank + k, 4))

    for k in (1, 2, 3):
        share_gain_z(k).start()

    load_own = [
        local(hidden_in.at[part_rows(part), :], sent.at[own_rows(part), :], load.at[4 + part]) for part in range(PARTS)
    ]
    for part in range(PARTS):
        gather_branch[part].finish()
    start_all(load_own)
    wait_all(load_own)
    for part in range(PARTS):
        one_scatter[part].wait()

        @pl.loop(0, size // 32)
        def _(step):
            rows = pl.ds(pl.multiple_of(part * size + step * 32, 32), 32)
            place = pl.ds(pl.multiple_of(part * span + step * 32, 32), 32)
            total = received(part, step * 32, 32, input_grad[rows, :])
            input_grad[rows, :] = grad_middle[rows, :] + norm_back(total, sent[place, :].astype(F32), gains[0:1, :])

    leave = [local(input_grad, input_ref, keep.at[6]), local(layer_out, out_ref, keep.at[7])]
    leave[0].start()

    for scatter in mlp_scatter:
        scatter.wait()
    load_mlp = [
        [local(mlp_recv.at[arrived(part, slot), :], recv_part.at[arrived(part, slot), :], load.at[2 * part + index])
         for index, slot in enumerate((4, 2))]
        for part in range(PARTS)
    ]
    for part in range(PARTS):
        load_mlp[part][0].start()
        pl.when(inner(rank))(load_mlp[part][1].start)
    for part in range(PARTS):
        load_mlp[part][0].wait()
        pl.when(inner(rank))(load_mlp[part][1].wait)

        @pl.loop(0, size // 32)
        def _(step):
            rows = pl.ds(pl.multiple_of(part * size + step * 32, 32), 32)
            layer_out[rows, :] = received(part, step * 32, 32, middle[rows, :]).astype(BF)

    leave[1].start()

    drain(gain_z.at[pl.ds(8, 24), :], y_recv.at[1])
    gain_all = gain_z[pl.ds(0, 8), :]
    for k in (1, 2, 3):
        gain_all = gain_all + gain_z[pl.ds(8 * k, 8), :]
    gain_total[...] = gain_all
    leave.append(local(gain_total, gain_out, keep.at[5]))
    leave[2].start()

    for scatter in mlp_scatter + one_scatter:
        scatter.finish()
    drain(gate_w.at[pl.ds(0, 3 * units // 8), :], d_send.at[0])
    drain(gain_recv.at[pl.ds(8, 56), :], y_send.at[0])
    drain(gain_recv.at[pl.ds(8, 56), :], g_send.at[0])
    drain(gain_z.at[pl.ds(8, 24), :], y_send.at[1])
    drain(two_half, h_send.at[1])
    drain(two_half, h_send.at[4])
    send_attended.wait_send()
    send_qkv.wait_send()
    def pieces(index, number):
        rows = number * width if index < 4 else number * heads * width // dim
        return gate_w.at[pl.ds(0, rows), pl.ds(0, 3 * heads if index == 3 else dim)]

    wait_all(leave)
    local(gate_w.at[pl.ds(0, width), :], gate_sum, keep.at[1]).wait()
    local(gate_w.at[pl.ds(0, width), :], up_sum, keep.at[2]).wait()
    drain(down_sum, keep.at[8])
    for index in range(1, 5):
        if index > 2:
            drain(pieces(index, 2), n_recv.at[index - 1])
            keep_grad(index).wait()
        drain(pieces(index, 3), w_send.at[index - 1])


def layer(hidden_in, cot, gains, weights, docs):
    tile, dim = hidden_in.shape
    tokens = 4 * tile
    width, heads = weights[0].shape
    units = weights[5].shape[1]
    dma = pltpu.SemaphoreType.DMA
    rows, narrow, ff = shape((tokens, dim), BF), shape((tokens, dim // 2), BF), shape((tokens, units), BF)
    weights_shape = [(units, width), (width, units), (width, units), (width, 3 * heads), (heads, width)]
    sums_shape = weights_shape[:3] + [(3 * width, 3 * heads), (heads, 3 * width)]
    parts_shape = [(units, 2 * width), (2 * width, units), (2 * width, units)]
    outs = [shape(dims, BF) for dims in sums_shape + parts_shape + weights_shape]
    outs += [ff] * 2 + [shape((tokens, 3 * heads), BF), shape((tokens, heads), BF), narrow, narrow]
    outs += [rows] * 3 + [shape((5 * tile, dim), BF), shape((dim, 3 * heads), BF), shape((units, dim), BF)]
    in_hbm = len(outs)
    outs += [shape((tile, dim), BF), shape((tile, dim), F32), shape((8, width), F32)]
    in_hbm += 3
    items = 4 + 3 * GROUPS
    scratch = [((dim, units), BF), ((dim, units), BF), ((units, dim), BF)]
    scratch += [((tokens, dim), BF)] * 3 + [((tokens, units), BF)] * 3
    scratch += [((tokens, dim // 2), BF)] * 2 + [((tokens, dim), BF)] * 3 + [((heads, dim), BF)]
    scratch += [((tokens, 3 * heads), BF)] + [((tokens, heads), BF)] * 2
    scratch += [((tokens, tokens), F32), ((tokens, 128), F32), ((tokens, 128), F32)]
    scratch += [((tokens, 1), F32), ((tokens, 1), F32), ((tile, dim), F32), ((tile, dim), F32)]
    scratch += [((tokens, dim), BF), ((5 * tile, dim), BF)]
    scratch += [((8, width), F32), ((8, dim), F32), ((8, dim), F32), ((64, width), F32), ((32, width), F32)]
    scratch += [((tile, dim), BF), ((tile, dim), F32), ((8, width), F32), (docs.shape, jnp.int32)]
    scratch += [((width,), BF)] * 2
    sems = [(2 + GROUPS,), (4 + GROUPS, 3), (3,), (GROUPS + 2,), (6,), (6,)]
    sems += [(2, PARTS), (2, PARTS, 3), (2, PARTS), (2, PARTS, 5), (4,), (4, 2), (1,), (GROUPS + 1,)]
    sems += [(1,), (1,), (2,), (2,), (15,), (8 + GROUPS,), (GROUPS,), (2 + GROUPS,), (4,)]
    return pl.pallas_call(
        layer_kernel,
        out_shape=outs,
        in_specs=[anyspace()] * 12,
        out_specs=[anyspace()] * in_hbm,
        scratch_shapes=[pltpu.VMEM(*entry) for entry in scratch] + [dma(entry) for entry in sems],
        compiler_params=pltpu.CompilerParams(vmem_limit_bytes=67000000, collective_id=0, has_side_effects=True),
        cost_estimate=cost(2 * tokens * dim * units * 12, 100e6),
        name="layer",
    )(hidden_in, cot, *gains, *weights, docs)


def sum_kernel(counts, *refs):
    parts, plain_in = refs[:5], refs[5:7]
    down, gate, up, query, key, value, out, *plain_out = refs[7:16]
    staged, totals, plain, load, store = refs[16:21], refs[21:26], refs[26:28], refs[28], refs[29]
    loads = [pltpu.make_async_copy(parts[index], staged[index], load.at[index]) for index in range(5)]
    loads += [pltpu.make_async_copy(plain_in[index], plain[index], load.at[5 + index]) for index in range(2)]
    start_all(loads)
    heads = query.shape[1]
    stores = [pltpu.make_async_copy(totals[index], ref, store.at[index]) for index, ref in enumerate((down, gate, up))]
    qkv_stores = [
        pltpu.make_async_copy(totals[3].at[:, pl.ds(index * heads, heads)], ref, store.at[3 + index])
        for index, ref in enumerate((query, key, value))
    ]
    out_store = pltpu.make_async_copy(totals[4], out, store.at[6])
    plain_stores = [pltpu.make_async_copy(plain[index], plain_out[index], store.at[7 + index]) for index in range(2)]
    groups = [[stores[0]], [stores[1]], [stores[2]], qkv_stores, [out_store]]
    for index in range(5):
        loads[index].wait()
        rows_first = index in (1, 2, 3)
        rows, cols = totals[index].shape
        step_rows = 32 if rows_first else 256

        @pl.loop(0, rows // step_rows)
        def _(step):
            start = pl.multiple_of(step * step_rows, step_rows)
            total = None
            for slot in range(counts[index]):
                if rows_first:
                    term = staged[index][pl.ds(pl.multiple_of(start + slot * rows, step_rows), step_rows), :]
                else:
                    term = staged[index][pl.ds(start, step_rows), slot * cols : (slot + 1) * cols]
                term = term.astype(F32)
                total = term if total is None else total + term
            totals[index][pl.ds(start, step_rows), :] = total

        start_all(groups[index])
    for index in range(2):
        loads[5 + index].wait()
        plain_stores[index].start()
    for entry in groups + [plain_stores]:
        wait_all(entry)


def sum_grads(parts, plain, heads, counts):
    dims = [part.shape for part in parts]
    sums = [
        (rows // counts[index], cols) if index in (1, 2, 3) else (rows, cols // counts[index])
        for index, (rows, cols) in enumerate(dims)
    ]
    outs = sums[:3] + [(sums[3][0], heads)] * 3 + [sums[4]]
    dma = pltpu.SemaphoreType.DMA
    return pl.pallas_call(
        partial(sum_kernel, counts),
        out_shape=[shape(dim, F32) for dim in outs] + [shape(entry.shape, entry.dtype) for entry in plain],
        in_specs=[anyspace()] * 7,
        out_specs=[anyspace()] * 9,
        scratch_shapes=[pltpu.VMEM(dim, BF) for dim in dims]
        + [pltpu.VMEM(dim, F32) for dim in sums]
        + [pltpu.VMEM(entry.shape, entry.dtype) for entry in plain]
        + [dma((7,)), dma((9,))],
        compiler_params=params(),
        cost_estimate=cost(1e6, 22e6),
        name="sum_grads",
    )(*parts, *plain)


def shift(values, step):
    size = lax.axis_size("tensor")
    return lax.ppermute(values, "tensor", [(index, (index + step) % size) for index in range(size)])


def gather_rows(values):
    return [values] + [shift(values, step) for step in range(1, lax.axis_size("tensor"))]


def scatter_rows(parts):
    total = parts[0].astype(F32)
    for step in range(1, len(parts)):
        total = total + shift(parts[step], -step).astype(F32)
    return total


def gather_weight(values, axis):
    return [None], [lax.all_gather(values, "dp", axis=axis, tiled=True)]


def scatter_full(left, right, axis):
    full = dot_cols(left, right).astype(BF)
    return lax.psum_scatter(full, "dp", scatter_dimension=axis, tiled=True).astype(F32)


def frequencies():
    half_size = HEAD_DIM // 2
    return ROPE_BASE ** (-jnp.arange(half_size, dtype=F32) / half_size)


def rotary(length):
    angles = jnp.arange(length).astype(F32)[:, None] * frequencies()[None, :]
    cosine, sine = jnp.cos(angles), jnp.sin(angles)
    cosine = jnp.tile(cosine, (1, 8))
    sine = jnp.tile(jnp.concatenate([-sine, sine], axis=1), (1, 4))
    return cosine, sine


def position_tables(doc_ids, ranks):
    length = doc_ids.shape[0]
    token_index = jnp.arange(length, dtype=jnp.int32)
    before = jnp.concatenate([doc_ids[:1] - 1, doc_ids[:-1]])
    doc_start = lax.cummax(jnp.where(doc_ids != before, token_index, 0), axis=0)
    order = (lax.axis_index("tensor") - jnp.arange(ranks)) % ranks
    last = token_index.reshape(ranks, -1)[order].reshape(length)
    first = doc_start.reshape(ranks, -1)[order].reshape(length)
    cosine, sine = (table.reshape(ranks, -1, 256)[order].reshape(length, 256) for table in rotary(length))
    return cosine, sine, first[:, None], last[:, None], last[None, :]


def rms_back(grad_rows_, values, gain):
    inverse = lax.rsqrt(jnp.mean(values * values, axis=-1, keepdims=True) + EPSILON)
    scaled = grad_rows_ * gain
    return inverse * (scaled - values * inverse * inverse * jnp.mean(scaled * values, axis=-1, keepdims=True))


def body(
    hidden_in,
    out_cotangent,
    doc_ids,
    attn_gain,
    query_weight,
    key_weight,
    value_weight,
    out_weight,
    mlp_gain,
    gate_weight,
    up_weight,
    down_weight,
):
    ranks, groups = lax.axis_size("tensor"), lax.axis_size("dp")
    paired = (groups, ranks) == (8, 4)
    width, heads = query_weight.shape
    dim = hidden_in.shape[1]

    if paired:
        weights = (query_weight, key_weight, value_weight, out_weight, down_weight, gate_weight, up_weight)
        outs = layer(hidden_in, out_cotangent, (attn_gain, mlp_gain), weights, doc_ids.reshape(ranks, -1))
        sums = sum_grads(outs[:5], outs[-3:-1], heads, (1, 1, 1, 3, 3))
        down_grad, gate_grad, up_grad, query_grad, key_grad, value_grad, out_proj_grad, layer_out, input_grad = sums
        gain_total = outs[-1]
        share = width // ranks
        gain_grads = lax.dynamic_slice_in_dim(gain_total, lax.axis_index("tensor") * share, share, axis=1)
    else:
        tables = position_tables(doc_ids, ranks)
        input_local = hidden_in.astype(F32)
        hidden_rows = gather_rows(hidden_in)
        gains = lax.all_gather(jnp.stack([attn_gain, mlp_gain]), "dp", axis=1, tiled=True).astype(F32)
        attn_scale, mlp_scale = gains[:1], gains[1:]
        qkv_weight = jnp.concatenate([query_weight, key_weight, value_weight], axis=1)
        tags, qkv_pieces = gather_weight(qkv_weight, 0)
        tags, out_pieces = gather_weight(out_weight, 1)
        cot_rows = gather_rows(out_cotangent)
        tags, down_pieces = gather_weight(down_weight, 1)
        tags, gate_pieces = gather_weight(gate_weight, 0)
        tags, up_pieces = gather_weight(up_weight, 0)
        normed, qkv, attended, inverses, *branch_parts = attn_fwd(
            hidden_rows, attn_scale, tables, tags, width, qkv_pieces, out_pieces
        )
        middle = input_local + scatter_rows(branch_parts)
        sent = middle.astype(BF)
        sent_rows = gather_rows(sent)
        cot_full = jnp.concatenate(cot_rows, axis=0)
        normed_two, hidden, d_gate, d_up, mlp_gain_part, *two_parts = mlp(
            sent_rows, cot_rows, mlp_scale, tags, width, gate_pieces, up_pieces, down_pieces, ranks
        )
        grad_two_rows = scatter_rows(two_parts)
        grad_middle = out_cotangent.astype(F32) + rms_back(grad_two_rows, sent.astype(F32), mlp_scale)
        branch_rows = gather_rows(grad_middle.astype(BF))
        down_grad = scatter_full(hidden, cot_full, 1)
        gate_grad = scatter_full(normed_two, d_gate, 0)
        up_grad = scatter_full(normed_two, d_up, 0)
        mlp_rows = scatter_rows(mlp_out(hidden, ranks, dim, tags, width, down_pieces))
        layer_out = (middle + mlp_rows).astype(BF)
        branch_full, d_qkv, attn_gain_part, *one_parts = attn_bwd(
            branch_rows, hidden_rows, qkv, inverses, tables, tags, width, qkv_pieces, out_pieces, ranks
        )
        out_proj_grad = scatter_full(attended, branch_full, 1)
        query_grad, key_grad, value_grad = jnp.split(scatter_full(normed, d_qkv, 0), 3, axis=1)
        grad_one_rows = scatter_rows(one_parts)
        input_grad = grad_middle + rms_back(grad_one_rows, input_local, attn_scale)
        gain_parts = jnp.concatenate([attn_gain_part, mlp_gain_part], axis=0)
        gain_grads = lax.psum_scatter(gain_parts, ("dp", "tensor"), scatter_dimension=1, tiled=True)
    return (
        layer_out,
        input_grad,
        gain_grads[0],
        query_grad,
        key_grad,
        value_grad,
        out_proj_grad,
        gain_grads[1],
        gate_grad,
        up_grad,
        down_grad,
    )


def solution(mesh):
    return jax.shard_map(
        body,
        mesh=mesh,
        in_specs=(
            P(("dp", "tensor"), None),
            P(("dp", "tensor"), None),
            P("dp"),
            P("dp"),
            P("dp", "tensor"),
            P("dp", "tensor"),
            P("dp", "tensor"),
            P("tensor", "dp"),
            P("dp"),
            P("dp", "tensor"),
            P("dp", "tensor"),
            P("tensor", "dp"),
        ),
        out_specs=(
            P(("dp", "tensor"), None),
            P(("dp", "tensor"), None),
            P(("dp", "tensor")),
            P("dp", "tensor"),
            P("dp", "tensor"),
            P("dp", "tensor"),
            P("tensor", "dp"),
            P(("dp", "tensor")),
            P("dp", "tensor"),
            P("dp", "tensor"),
            P("tensor", "dp"),
        ),
        check_vma=False,
    )
```

```python
import math
from functools import partial

import jax
import jax.numpy as jnp
from jax import lax
from jax.experimental import pallas as pl
from jax.experimental.pallas import tpu as pltpu
from jax.sharding import PartitionSpec as P

HEAD_DIM = 64
EPSILON = 1e-05
ROPE_BASE = 130000.0
NEGATIVE = -1e30
VMEM_LIMIT = 63 * 1024 * 1024
BF = jnp.bfloat16
F32 = jnp.float32


def dot(left, right):
    return jnp.dot(left, right, preferred_element_type=F32)


def dot_rows(left, right):
    return lax.dot_general(left, right, (((1,), (1,)), ((), ())), preferred_element_type=F32)


def dot_cols(left, right):
    return lax.dot_general(left, right, (((0,), (0,)), ((), ())), preferred_element_type=F32)


def vmem():
    return pl.BlockSpec(memory_space=pltpu.VMEM)


def anyspace():
    return pl.BlockSpec(memory_space=pl.ANY)


def params():
    return pltpu.CompilerParams(vmem_limit_bytes=VMEM_LIMIT)


def cost(flops, nbytes):
    return pl.CostEstimate(flops=int(flops), bytes_accessed=int(nbytes), transcendentals=0)


def shape(dims, kind):
    return jax.ShapeDtypeStruct(dims, kind)


def place_copies(tags, pieces, target, sem, axis, width):
    own = lax.axis_index("dp")
    copies = []
    for slot, (tag, piece) in enumerate(zip(tags, pieces)):
        if tag is None:
            where = target
        else:
            start = pl.multiple_of((own ^ tag) * width, width)
            where = target.at[pl.ds(start, width), :] if axis == 0 else target.at[:, pl.ds(start, width)]
        copies.append(pltpu.make_async_copy(piece, where, sem.at[slot]))
    return copies


def row_copies(pieces, target, sem):
    copies = []
    for slot, piece in enumerate(pieces):
        rows = piece.shape[0]
        copies.append(pltpu.make_async_copy(piece, target.at[pl.ds(slot * rows, rows), :], sem.at[slot]))
    return copies


def start_all(copies):
    for copy in copies:
        copy.start()


def wait_all(copies):
    for copy in copies:
        copy.wait()


def turn(values, cosine, sine):
    width = values.shape[1]
    lane = lax.broadcasted_iota(jnp.int32, values.shape, 1)
    partner = jnp.where(
        lax.rem(lane, HEAD_DIM) < HEAD_DIM // 2,
        pltpu.roll(values, width - HEAD_DIM // 2, 1),
        pltpu.roll(values, HEAD_DIM // 2, 1),
    )
    return values * cosine + partner * sine


def norm_rows(source, target, inverses, gain, tile):
    @pl.loop(0, source.shape[0] // tile)
    def _(step):
        rows = pl.ds(pl.multiple_of(step * tile, tile), tile)
        values = source[rows, :].astype(F32)
        inverse = lax.rsqrt(jnp.mean(values * values, axis=-1, keepdims=True) + EPSILON)
        inverses[rows, :] = inverse
        target[rows, :] = (values * inverse * gain[...]).astype(BF)


def fill_bias(bias, first, last, key_index):
    keys = key_index[...]
    bias[...] = jnp.where((keys >= first[...]) & (keys <= last[...]), 0.0, NEGATIVE)


def head_lanes(width, half):
    lane = lax.broadcasted_iota(jnp.int32, (1, width), 1)
    return (lax.div(lane, HEAD_DIM) == half).astype(F32)


def probabilities(query, key, bias):
    scores = dot_rows(query, key) + bias
    weights = jnp.exp(scores - jnp.max(scores, axis=-1, keepdims=True))
    return weights * (1.0 / jnp.sum(weights, axis=-1, keepdims=True))


def attend(qkv, attended, bias, heads):
    @pl.loop(0, heads // 128)
    def _(pair):
        base = pl.multiple_of(pair * 128, 128)
        query = qkv[:, pl.ds(base, 128)]
        key = qkv[:, pl.ds(heads + base, 128)]
        value = qkv[:, pl.ds(2 * heads + base, 128)]
        total = None
        for half in range(2):
            lanes = head_lanes(128, half).astype(BF)
            probs = probabilities(query * (lanes * HEAD_DIM ** (-0.5)), key, bias[...])
            term = dot(probs.astype(BF), value * lanes)
            total = term if total is None else total + term
        attended[:, pl.ds(base, 128)] = total.astype(BF)


def attn_fwd_kernel(tags, width, nrow, *refs):
    npiece = len(tags)
    rows_in = refs[:nrow]
    gain, cosine, sine, first, last, key_index = refs[nrow : nrow + 6]
    rest = refs[nrow + 6 :]
    qkv_in, out_in = rest[:npiece], rest[npiece : 2 * npiece]
    rest = rest[2 * npiece :]
    normed, qkv, attended, inverses = rest[:4]
    parts = rest[4 : 4 + nrow]
    hidden, qkv_w, out_w, bias, sem_rows, sem_qkv, sem_out = rest[4 + nrow :]
    load_rows = row_copies(rows_in, hidden, sem_rows)
    load_qkv = place_copies(tags, qkv_in, qkv_w, sem_qkv, 0, width)
    load_out = place_copies(tags, out_in, out_w, sem_out, 1, width)
    start_all(load_rows + load_qkv + load_out)
    fill_bias(bias, first, last, key_index)
    wait_all(load_rows)
    norm_rows(hidden, normed, inverses, gain, 64)
    wait_all(load_qkv)
    heads = attended.shape[1]
    step_cols = 256

    @pl.loop(0, 2 * heads // step_cols)
    def _(step):
        cols = pl.ds(pl.multiple_of(step * step_cols, step_cols), step_cols)
        qkv[:, cols] = turn(dot(normed[...], qkv_w[:, cols]), cosine[...], sine[...]).astype(BF)

    @pl.loop(2 * heads // step_cols, 3 * heads // step_cols)
    def _(step):
        cols = pl.ds(pl.multiple_of(step * step_cols, step_cols), step_cols)
        qkv[:, cols] = dot(normed[...], qkv_w[:, cols]).astype(BF)

    attend(qkv, attended, bias, heads)
    wait_all(load_out)
    tile = parts[0].shape[0]

    @pl.loop(0, out_w.shape[1] // step_cols)
    def _(step):
        cols = pl.ds(pl.multiple_of(step * step_cols, step_cols), step_cols)
        product = dot(attended[...], out_w[:, cols])
        for slot, part in enumerate(parts):
            part[:, cols] = product[slot * tile : (slot + 1) * tile, :].astype(part.dtype)


def attn_fwd(rows, gain, tables, tags, width, qkv_pieces, out_pieces):
    nrow, (tile, dim) = len(rows), rows[0].shape
    tokens = nrow * tile
    heads = out_pieces[0].shape[0]
    npiece = len(tags)
    return pl.pallas_call(
        partial(attn_fwd_kernel, tags, width, nrow),
        out_shape=[
            shape((tokens, dim), BF),
            shape((tokens, 3 * heads), BF),
            shape((tokens, heads), BF),
            shape((tokens, 1), F32),
        ]
        + [shape((tile, dim), F32 if slot == 0 else BF) for slot in range(nrow)],
        in_specs=[anyspace()] * nrow + [vmem()] * 6 + [anyspace()] * (2 * npiece),
        out_specs=[vmem()] * (4 + nrow),
        scratch_shapes=[
            pltpu.VMEM((tokens, dim), BF),
            pltpu.VMEM((dim, 3 * heads), BF),
            pltpu.VMEM((heads, dim), BF),
            pltpu.VMEM((tokens, tokens), F32),
            pltpu.SemaphoreType.DMA((nrow,)),
            pltpu.SemaphoreType.DMA((npiece,)),
            pltpu.SemaphoreType.DMA((npiece,)),
        ],
        compiler_params=params(),
        cost_estimate=cost(2 * tokens * dim * 4 * heads * 3, 20e6),
        name="attn_fwd",
    )(*rows, gain, *tables, *qkv_pieces, *out_pieces)


def attend_back(qkv, d_attended, d_qkv, bias, cosine, sine, heads):
    score_scale = HEAD_DIM ** (-0.5)

    @pl.loop(0, heads // 128)
    def _(pair):
        base = pl.multiple_of(pair * 128, 128)
        query = qkv[:, pl.ds(base, 128)]
        key = qkv[:, pl.ds(heads + base, 128)]
        value = qkv[:, pl.ds(2 * heads + base, 128)]
        grad = d_attended[:, pl.ds(base, 128)]
        sums = [0.0, 0.0, 0.0]
        for half in range(2):
            lanes = head_lanes(128, half).astype(BF)
            own_query = query * (lanes * score_scale)
            own_grad = grad * lanes
            probs = probabilities(own_query, key, bias[...])
            d_value = dot_cols(probs.astype(BF), own_grad)
            d_probs = dot_rows(own_grad, value)
            delta = jnp.sum(probs * d_probs, axis=-1, keepdims=True)
            d_scores = (probs * (d_probs - delta)).astype(BF)
            d_query = dot(d_scores, key * lanes) * score_scale
            d_key = dot_cols(d_scores, own_query)
            sums = [sums[0] + d_query, sums[1] + d_key, sums[2] + d_value]
        back = -sine[:, :128]
        d_qkv[:, pl.ds(base, 128)] = turn(sums[0], cosine[:, :128], back).astype(BF)
        d_qkv[:, pl.ds(heads + base, 128)] = turn(sums[1], cosine[:, :128], back).astype(BF)
        d_qkv[:, pl.ds(2 * heads + base, 128)] = sums[2].astype(BF)


def attn_bwd_kernel(tags, width, nrow, npart, *refs):
    npiece = len(tags)
    nhid, nrow = nrow[1], nrow[0]
    rows_in, hidden_in = refs[:nrow], refs[nrow : nrow + nhid]
    refs = refs[nrow + nhid :]
    qkv, inverses, cosine, sine, first, last, key_index = refs[:7]
    rest = refs[7:]
    qkv_in, out_in = rest[:npiece], rest[npiece : 2 * npiece]
    rest = rest[2 * npiece :]
    branch, d_qkv, gain_grad = rest[:3]
    parts = rest[3 : 3 + npart]
    hidden, d_attended, qkv_w, out_w, bias, sem_rows, sem_x, sem_qkv, sem_out = rest[3 + npart :]
    load_rows = row_copies(rows_in, branch, sem_rows)
    load_x = row_copies(hidden_in, hidden, sem_x)
    load_out = place_copies(tags, out_in, out_w, sem_out, 1, width)
    load_qkv = place_copies(tags, qkv_in, qkv_w, sem_qkv, 0, width)
    start_all(load_rows + load_out + load_qkv + load_x)
    fill_bias(bias, first, last, key_index)
    wait_all(load_rows)
    wait_all(load_out)
    heads = out_w.shape[0]
    step_cols = 256

    @pl.loop(0, heads // step_cols)
    def _(step):
        cols = pl.ds(pl.multiple_of(step * step_cols, step_cols), step_cols)
        d_attended[:, cols] = dot_rows(branch[...], out_w[cols, :]).astype(BF)

    attend_back(qkv, d_attended, d_qkv, bias, cosine, sine, heads)
    wait_all(load_qkv)
    wait_all(load_x)
    tile = parts[0].shape[0]

    @pl.loop(0, qkv_w.shape[0] // step_cols)
    def _(step):
        cols = pl.ds(pl.multiple_of(step * step_cols, step_cols), step_cols)
        product = dot_rows(d_qkv[...], qkv_w[cols, :])
        gain_grad[:, cols] = jnp.sum(product * (hidden[:, cols].astype(F32) * inverses[...]), axis=0, keepdims=True)
        for slot, part in enumerate(parts):
            part[:, cols] = product[slot * tile : (slot + 1) * tile, :].astype(part.dtype)


def attn_bwd(rows, hidden, qkv, inverses, tables, tags, width, qkv_pieces, out_pieces, npart):
    nrow, nhid, dim = len(rows), len(hidden), rows[0].shape[1]
    tokens = qkv.shape[0]
    tile = tokens // npart
    heads = out_pieces[0].shape[0]
    npiece = len(tags)
    return pl.pallas_call(
        partial(attn_bwd_kernel, tags, width, (nrow, nhid), npart),
        out_shape=[shape((tokens, dim), BF), shape((tokens, 3 * heads), BF), shape((1, dim), F32)]
        + [shape((tile, dim), F32 if slot == 0 else BF) for slot in range(npart)],
        in_specs=[anyspace()] * (nrow + nhid) + [vmem()] * 7 + [anyspace()] * (2 * npiece),
        out_specs=[vmem()] * (3 + npart),
        scratch_shapes=[
            pltpu.VMEM((tokens, dim), BF),
            pltpu.VMEM((tokens, heads), BF),
            pltpu.VMEM((dim, 3 * heads), BF),
            pltpu.VMEM((heads, dim), BF),
            pltpu.VMEM((tokens, tokens), F32),
            pltpu.SemaphoreType.DMA((nrow,)),
            pltpu.SemaphoreType.DMA((nhid,)),
            pltpu.SemaphoreType.DMA((npiece,)),
            pltpu.SemaphoreType.DMA((npiece,)),
        ],
        compiler_params=params(),
        cost_estimate=cost(2 * tokens * dim * 4 * heads * 6, 30e6),
        name="attn_bwd",
    )(*rows, *hidden, qkv, inverses, *tables, *qkv_pieces, *out_pieces)


def mlp_kernel(tags, width, nrow, npart, *refs):
    npiece = len(tags)
    sent_in, cot_in = refs[:nrow], refs[nrow : 2 * nrow]
    gain = refs[2 * nrow]
    rest = refs[2 * nrow + 1 :]
    gate_in, up_in, down_in = rest[:npiece], rest[npiece : 2 * npiece], rest[2 * npiece : 3 * npiece]
    rest = rest[3 * npiece :]
    normed, hidden, d_gate, d_up, gain_grad = rest[:5]
    parts = rest[5 : 5 + npart]
    sent, cot, inverses, gate_w, up_w, down_w, sem_sent, sem_cot, sem_gate, sem_up, sem_down = rest[5 + npart :]
    load_sent = row_copies(sent_in, sent, sem_sent)
    load_cot = row_copies(cot_in, cot, sem_cot)
    load_gate = place_copies(tags, gate_in, gate_w, sem_gate, 0, width)
    load_up = place_copies(tags, up_in, up_w, sem_up, 0, width)
    load_down = place_copies(tags, down_in, down_w, sem_down, 1, width)
    start_all(load_sent + load_cot + load_gate + load_up + load_down)
    wait_all(load_sent)
    norm_rows(sent, normed, inverses, gain, 64)
    wait_all(load_cot)
    wait_all(load_gate)
    wait_all(load_up)
    wait_all(load_down)
    step_cols = 256

    @pl.loop(0, gate_w.shape[1] // step_cols)
    def _(step):
        cols = pl.ds(pl.multiple_of(step * step_cols, step_cols), step_cols)
        gate = dot(normed[...], gate_w[:, cols])
        up = dot(normed[...], up_w[:, cols])
        d_hidden = dot_rows(cot[...], down_w[cols, :])
        s = jax.nn.sigmoid(gate)
        activated = gate * s
        hidden[:, cols] = (activated * up).astype(BF)
        d_gate[:, cols] = (d_hidden * up * (s + activated * (1.0 - s))).astype(BF)
        d_up[:, cols] = (d_hidden * activated).astype(BF)

    tile = parts[0].shape[0]

    @pl.loop(0, gate_w.shape[0] // step_cols)
    def _(step):
        cols = pl.ds(pl.multiple_of(step * step_cols, step_cols), step_cols)
        product = dot_rows(d_gate[...], gate_w[cols, :]) + dot_rows(d_up[...], up_w[cols, :])
        gain_grad[:, cols] = jnp.sum(product * (sent[:, cols].astype(F32) * inverses[...]), axis=0, keepdims=True)
        for slot, part in enumerate(parts):
            part[:, cols] = product[slot * tile : (slot + 1) * tile, :].astype(part.dtype)


def mlp(sent, cot, gain, tags, width, gate_pieces, up_pieces, down_pieces, npart):
    nrow, dim = len(sent), sent[0].shape[1]
    tokens = nrow * sent[0].shape[0]
    tile = tokens // npart
    units = gate_pieces[0].shape[1]
    npiece = len(tags)
    return pl.pallas_call(
        partial(mlp_kernel, tags, width, nrow, npart),
        out_shape=[shape((tokens, dim), BF)]
        + [shape((tokens, units), BF)] * 3
        + [shape((1, dim), F32)]
        + [shape((tile, dim), F32 if slot == 0 else BF) for slot in range(npart)],
        in_specs=[anyspace()] * (2 * nrow) + [vmem()] + [anyspace()] * (3 * npiece),
        out_specs=[vmem()] * (5 + npart),
        scratch_shapes=[
            pltpu.VMEM((tokens, dim), BF),
            pltpu.VMEM((tokens, dim), BF),
            pltpu.VMEM((tokens, 1), F32),
            pltpu.VMEM((dim, units), BF),
            pltpu.VMEM((dim, units), BF),
            pltpu.VMEM((units, dim), BF),
            pltpu.SemaphoreType.DMA((nrow,)),
            pltpu.SemaphoreType.DMA((nrow,)),
            pltpu.SemaphoreType.DMA((npiece,)),
            pltpu.SemaphoreType.DMA((npiece,)),
            pltpu.SemaphoreType.DMA((npiece,)),
        ],
        compiler_params=params(),
        cost_estimate=cost(2 * tokens * dim * units * 5, 40e6),
        name="mlp",
    )(*sent, *cot, gain, *gate_pieces, *up_pieces, *down_pieces)


def mlp_out_kernel(tags, width, *refs):
    npiece = len(tags)
    hidden, down_in = refs[0], refs[1 : 1 + npiece]
    *parts, down_w, sem_down = refs[1 + npiece :]
    load_down = place_copies(tags, down_in, down_w, sem_down, 1, width)
    start_all(load_down)
    wait_all(load_down)
    tile, step_cols = parts[0].shape[0], 256

    @pl.loop(0, down_w.shape[1] // step_cols)
    def _(step):
        cols = pl.ds(pl.multiple_of(step * step_cols, step_cols), step_cols)
        product = dot(hidden[...], down_w[:, cols])
        for slot, part in enumerate(parts):
            part[:, cols] = product[slot * tile : (slot + 1) * tile, :].astype(part.dtype)


def mlp_out(hidden, nrow, dim, tags, width, down_pieces):
    tokens, units = hidden.shape
    tile, npiece = tokens // nrow, len(tags)
    return pl.pallas_call(
        partial(mlp_out_kernel, tags, width),
        out_shape=[shape((tile, dim), F32 if slot == 0 else BF) for slot in range(nrow)],
        in_specs=[vmem()] + [anyspace()] * npiece,
        out_specs=[vmem()] * nrow,
        scratch_shapes=[pltpu.VMEM((units, dim), BF), pltpu.SemaphoreType.DMA((npiece,))],
        compiler_params=params(),
        cost_estimate=cost(2 * tokens * dim * units, 14e6),
        name="mlp_out",
    )(hidden, *down_pieces)


def slice_of(slot, width, own):
    index = lax.axis_index("dp")
    owner = index ^ (2 * slot)
    return pl.ds(pl.multiple_of((owner if own else lax.div(owner, 2)) * width, width), width)

MESH = pl.DeviceIdType.MESH
NEAR = (2, 4, 6)
PARTS = 2
GROUPS = 4


def remote(source, target, send_sem, recv_sem, axis, peer):
    return pltpu.make_async_remote_copy(
        src_ref=source,
        dst_ref=target,
        send_sem=send_sem,
        recv_sem=recv_sem,
        device_id={axis: peer},
        device_id_type=MESH,
    )


def drain(ref, sem):
    pltpu.make_async_copy(ref, ref, sem).wait()


def meet():
    own, rank = lax.axis_index("dp"), lax.axis_index("tensor")
    barrier = pltpu.get_barrier_semaphore()
    for flip in range(1, 8):
        pl.semaphore_signal(barrier, inc=1, device_id={"dp": own ^ flip}, device_id_type=MESH)

    @pl.when(rank < 3)
    def _():
        pl.semaphore_signal(barrier, inc=1, device_id={"tensor": rank + 1}, device_id_type=MESH)

    @pl.when(rank > 0)
    def _():
        pl.semaphore_signal(barrier, inc=1, device_id={"tensor": rank - 1}, device_id_type=MESH)

    pl.semaphore_wait(barrier, 8 + lax.div(rank * (3 - rank), 2))


def at_cols(ref, index, width):
    return ref.at[:, pl.ds(pl.multiple_of(index * width, width), width)]


def at_rows(ref, index, width):
    return ref.at[pl.ds(pl.multiple_of(index * width, width), width), :]


def either(rank, *choices):
    result = rank == choices[0]
    for choice in choices[1:]:
        result = result | (rank == choice)
    return result


def ends(rank):
    return either(rank, 0, 3)


def inner(rank):
    return either(rank, 1, 2)


class RowGather:
    def __init__(self, rank, source, landing, part, size, send, recv):
        self.rank = rank

        def place(slot):
            return landing.at[pl.ds(pl.multiple_of((4 * part + slot) * size, size), size), :]

        def copy(origin, slot, peer):
            return remote(origin, place(slot), send.at[part], recv.at[part, slot - 1], "tensor", peer)

        def forward(slot, target, peer):
            return copy(place(slot), target, peer)

        outward, inward = (rank - 1) * 3, 3 - rank
        near, far = 5 - 2 * rank, 2 * rank - 1
        self.up, self.down = copy(source, 1, rank + 1), copy(source, 3, rank - 1)
        self.hops = [forward(near, 2, outward), forward(far, 2, inward), forward(2, far, outward)]
        self.slots = [near, far, 2]
        self.arrival = lambda slot: copy(source, slot, lax.rem(rank + 1, 4))
        self.sent = lambda count: drain(landing.at[pl.ds(0, count * size), :], send.at[part])

    def start(self):
        pl.when(self.rank < 3)(self.up.start)
        pl.when(self.rank > 0)(self.down.start)

    def hop(self, index):
        @pl.when(inner(self.rank))
        def _():
            self.arrival(self.slots[index]).wait_recv()
            self.hops[index].start()

    def wait(self):
        @pl.when(ends(self.rank))
        def _():
            for slot in (1, 2, 3):
                self.arrival(slot).wait_recv()

    def finish(self):
        pl.when(ends(self.rank))(lambda: self.sent(1))
        pl.when(inner(self.rank))(lambda: self.sent(5))


class RowScatter:
    def __init__(self, rank, source, landing, part, size, send, recv, staged=None, sem=None):
        self.rank, self.source, self.size, self.staged, self.sem = rank, source, size, staged, sem
        self.place = lambda k: pl.ds(pl.multiple_of((4 * part + k) * size, size), size)
        self.land = lambda slot: landing.at[pl.ds((5 * part + slot) * size, size), :]

        def copy(k, slot, peer):
            return remote(source.at[self.place(k), :], self.land(slot), send.at[part], recv.at[part, slot], "tensor", peer)

        end = lax.div(rank, 3)
        self.first = [copy(index + 1 + end * (2 - 2 * index), index, 1 + end) for index in range(3)]
        self.keys = [2, 5 - 2 * rank, 2 * rank - 1]
        self.later = [
            copy(self.keys[0], 3, 3 - rank),
            copy(self.keys[1], 4, 3 - rank),
            copy(self.keys[2], 4, (rank - 1) * 3),
        ]
        self.arrival = lambda slot: copy(1, slot, lax.rem(rank + 1, 4))
        self.finish = lambda: drain(source.at[pl.ds(0, 3 * size), :], send.at[part])

    def start(self, indices=(0, 1, 2)):
        @pl.when(ends(self.rank))
        def _():
            for index in indices:
                self.first[index].start()

    def hop(self, index):
        @pl.when(inner(self.rank))
        def _():
            slot = (0, 1, 3)[index]
            self.arrival(slot).wait_recv()
            other = self.land(slot)
            if self.staged is not None:
                load = pltpu.make_async_copy(other, self.staged, self.sem)
                load.start()
                load.wait()
                other = self.staged
            target = self.source.at[self.place(self.keys[index]), :]

            @pl.loop(0, self.size // 16)
            def _(step):
                rows = pl.ds(pl.multiple_of(step * 16, 16), 16)
                target[rows, :] = (target[rows, :].astype(F32) + other[rows, :].astype(F32)).astype(BF)

            self.later[index].start()

    def wait(self):
        pl.when(inner(self.rank))(self.arrival(2).wait_recv)
        self.arrival(4).wait_recv()


def fill_mask(bias, docs, size):
    rank = lax.axis_index("tensor")
    tokens = bias.shape[0]
    values = docs[...]
    starts = [jnp.sum(jnp.where(values < number, 1, 0), keepdims=True) for number in range(1, 8)]

    def document(position):
        return sum(jnp.where(position >= start, 1, 0) for start in starts)

    lane = lax.broadcasted_iota(jnp.int32, (1, tokens), 1)
    slot = lax.rem(lax.div(lane, size), 4)
    part = lax.div(lane, 4 * size)
    keys = lax.rem(rank - slot + 4, 4) * (2 * size) + part * size + lax.rem(lane, size)
    key_docs = document(keys)

    @pl.loop(0, tokens // size)
    def _(block):
        base = lax.rem(rank - lax.rem(block, 4) + 4, 4) * (2 * size) + lax.div(block, 4) * size
        queries = base + lax.broadcasted_iota(jnp.int32, (size, 1), 0)
        allowed = (document(queries) == key_docs) & (queries >= keys)
        bias[pl.ds(pl.multiple_of(block * size, size), size), :] = jnp.where(allowed, 0.0, NEGATIVE)


def fill_turns(cosine, sine, size):
    rank = lax.axis_index("tensor")
    half_size = HEAD_DIM // 2
    dims = (size, cosine.shape[1])
    lane = lax.broadcasted_iota(jnp.int32, dims, 1)
    row = lax.broadcasted_iota(jnp.int32, dims, 0)
    frequency = jnp.exp(lax.rem(lane, half_size).astype(F32) * (-math.log(ROPE_BASE) / half_size))
    sign = jnp.where(lax.rem(lane, HEAD_DIM) < half_size, -1.0, 1.0)

    @pl.loop(0, cosine.shape[0] // size)
    def _(block):
        start = (lax.rem(rank - lax.rem(block, 4) + 4, 4) * PARTS + lax.div(block, 4)) * size
        angles = (row + start).astype(F32) * frequency
        rows = pl.ds(pl.multiple_of(block * size, size), size)
        cosine[rows, :] = jnp.cos(angles)
        sine[rows, :] = jnp.sin(angles) * sign


def slice_of(slot, width, own):
    index = lax.axis_index("dp")
    owner = index ^ (2 * slot)
    return pl.ds(pl.multiple_of((owner if own else lax.div(owner, 2)) * width, width), width)


def layer_kernel(*refs):
    hidden_in, cot_in, *gains_hbm = refs[:4]
    weights_in = refs[4:11]
    docs_hbm = refs[11]
    down_sum, gate_sum, up_sum, qkv_parts, out_parts = refs[12:17]
    down_parts, gate_parts, up_parts = refs[17:20]
    grad_merge = refs[20:25]
    pair_gate, pair_up, pair_qkv, pair_attended, pair_normed, pair_branch = refs[25:31]
    branch_rows, hidden_rows, normed_rows, mlp_recv, qkv_full, down_full = refs[31:37]
    out_ref, input_ref, gain_out = refs[37:40]
    gate_w, up_w, down_w, sent, cot, normed, hidden, d_gate, d_up = refs[40:49]
    two_half, cot_half, buffer_a, buffer_b, buffer_c, out_w = refs[49:55]
    qkv, attended, d_attended, bias, cosine, sine = refs[55:61]
    inverses_one, inverses, middle, grad_middle, send_part, recv_part = refs[61:67]
    gains_in, gains, gain_part, gain_recv, gain_z, layer_out, input_grad, gain_total, docs, *plain_gains = refs[67:78]
    a_send, a_recv, f_send, f_recv, h_send, h_recv, z_send, z_recv, r_send, r_recv = refs[78:88]
    w_send, w_recv, d_send, d_recv, g_send, g_recv, y_send, y_recv, load, keep, down_load, s_recv, n_recv = refs[88:]

    own, rank = lax.axis_index("dp"), lax.axis_index("tensor")
    core = lax.rem(own, 2)
    tokens, dim = sent.shape
    units = gate_w.shape[1]
    tile = hidden_in.shape[0]
    size = tile // PARTS
    span = 4 * size
    heads = attended.shape[1]
    width = weights_in[0].shape[0]
    half = dim // (2 * width)
    d_qkv = cot.at[:, pl.ds(heads, 3 * heads)]
    group = units // GROUPS
    step_cols = 256
    count = dim // step_cols

    def cols_of(step, length=step_cols):
        return pl.ds(pl.multiple_of(step * length, length), length)

    def local(source, target, sem):
        return pltpu.make_async_copy(source, target, sem)

    def own_rows(part):
        return pl.ds(part * span, size)

    def part_rows(part):
        return pl.ds(part * size, size)

    def source_of(item):
        if item < 4:
            return weights_in[item]
        which, start = (item - 4) % 3, ((item - 4) // 3) * group
        if which == 2:
            return weights_in[4].at[pl.ds(start, group), :]
        return weights_in[5 + which].at[:, pl.ds(start, group)]

    def view(item, owner, part=None):
        rows = heads if item == 3 else group if item > 3 and (item - 4) % 3 == 2 else width
        length = rows if part is None else rows // 2
        start = 0 if part is None else part * length
        if item < 3:
            place = pl.ds(pl.multiple_of(owner * width + start, length), length)
            return down_w.at[place, pl.ds(item * heads, heads)]
        if item == 3:
            return out_w.at[pl.ds(start, length), pl.ds(pl.multiple_of(owner * width, width), width)]
        which, offset = (item - 4) % 3, ((item - 4) // 3) * group
        if which == 2:
            return down_full.at[pl.ds(offset + start, length), pl.ds(pl.multiple_of(owner * width, width), width)]
        place = pl.ds(pl.multiple_of(owner * width + start, length), length)
        return (gate_w, up_w)[which].at[place, pl.ds(offset, group)]

    def phase_of(item):
        return 0 if item < 3 else 1 if item == 3 else 2 + (item - 4) // 3

    def lot_of(item):
        return item if item < 4 else 4 + (item - 4) // 3

    def send_weight(item, flip):
        sem = s_recv.at[phase_of(item)] if flip == 1 else a_recv.at[lot_of(item), flip // 2 - 1]
        return remote(source_of(item), view(item, own), a_send.at[phase_of(item)], sem, "dp", own ^ flip)

    def relay_weight(item, part):
        place = view(item, own ^ (4 - 2 * part), part)
        return remote(place, place, a_send.at[phase_of(item)], a_recv.at[lot_of(item), 2], "dp", own ^ (2 + 2 * part))

    def pass_weight(item, flip):
        place = view(item, own ^ flip)
        return remote(place, place, a_send.at[phase_of(item)], s_recv.at[phase_of(item)], "dp", own ^ 1)

    def send_weights(items):
        for item in items:
            for flip in (2, 4, 1):
                send_weight(item, flip).start()

    def lots(items):
        return [[item] for item in items] if items[0] < 4 else [items]

    def arrived_weights(lot, tag):
        drain(gate_w.at[pl.ds(0, len(lot) * width // 4), :], a_recv.at[lot_of(lot[0]), tag])

    def relay_weights(items):
        for lot in lots(items):
            arrived_weights(lot, 1)
            for item in lot:
                relay_weight(item, 0).start()
            arrived_weights(lot, 0)
            for item in lot:
                relay_weight(item, 1).start()
            for item in lot:
                pass_weight(item, 4).start()
                pass_weight(item, 2).start()

    def pass_weights(items):
        for lot in lots(items):
            arrived_weights(lot, 2)
            for item in lot:
                pass_weight(item, 6).start()

    def have_weights(phase):
        drain(gate_w.at[pl.ds(0, width if phase == 1 else 3 * width), :], s_recv.at[phase])

    def sent_weights(phase):
        length = 7 * width // 4
        drain(gate_w.at[pl.ds(0, length if phase == 1 else 3 * length), :], a_send.at[phase])

    def items_of(index):
        return list(range(4 + 3 * index, 7 + 3 * index))

    def send_gain(flip):
        return remote(gains_in, at_cols(gains, own, width), y_send.at[0], y_recv.at[0], "dp", own ^ flip)

    def gathers(kind, source, landing):
        return [
            RowGather(rank, source(part), landing, part, size, z_send.at[kind], z_recv.at[kind]) for part in range(PARTS)
        ]

    gather_hidden = gathers(0, lambda part: hidden_in.at[part_rows(part), :], buffer_b)
    gather_cot = gathers(1, lambda part: cot_in.at[part_rows(part), :], cot)
    gather_sent = gathers(0, lambda part: sent.at[own_rows(part), :], sent)
    gather_branch = gathers(0, lambda part: sent.at[own_rows(part), :], branch_rows)

    def scatters(kind, source, landing, staged=None, sem=None):
        return [
            RowScatter(rank, source, landing, part, size, r_send.at[kind], r_recv.at[kind], staged, sem)
            for part in range(PARTS)
        ]

    gate_stage = up_w.at[pl.ds(4 * width, size), :]
    out_scatter = scatters(0, send_part, recv_part)
    two_scatter = scatters(0, send_part, recv_part)
    mlp_scatter = scatters(1, sent, mlp_recv, gate_stage, load.at[3])
    one_scatter = scatters(0, send_part, recv_part)

    def arrived(part, slot):
        return pl.ds((5 * part + slot) * size, size)

    def clear(part):
        @pl.when(ends(rank))
        def _():
            recv_part[arrived(part, 2), :] = jnp.zeros((size, dim), BF)

    def received(part, start, length, base):
        total = base
        for slot in (2, 4):
            rows = pl.ds(pl.multiple_of((5 * part + slot) * size + start, length), length)
            total = total + recv_part[rows, :].astype(F32)
        return total

    def to_pair(source, target, row, slot):
        return remote(source, target, h_send.at[row], h_recv.at[row], "dp", own ^ 1)

    def halves(source, target, row):
        return [
            to_pair(at_cols(source, 2 * slot + 1 - core, width), at_cols(target, slot, width), row, slot)
            for slot in range(half)
        ]

    def send_ff(step, which):
        cols = cols_of(step)
        source = (hidden, d_gate, d_up)[which].at[:, cols]
        target = (buffer_a, pair_gate, pair_up)[which].at[:, cols]
        arrival = lax.div(step, group // step_cols) if which == 0 else GROUPS - 1 + which
        return remote(source, target, f_send.at[which], f_recv.at[arrival], "dp", own ^ 1)

    def piece(index, slot):
        if index < 3:
            return at_rows(gate_w, (index - 1) * 4 + slot, width)
        if index == 3:
            return (hidden, d_gate)[slot // 2].at[pl.ds((slot % 2) * width, width), pl.ds(0, 3 * heads)]
        return at_cols(d_up, slot, width)

    def landing_of(index, slot):
        ref = (down_parts, gate_parts, up_parts, qkv_parts, out_parts)[index]
        if index < 3:
            return at_rows(ref, slot - 1, width)
        return at_cols(ref, slot, width) if index == 4 else at_rows(ref, slot, width)

    def half_of(ref, index, part):
        rows, cols = ref.shape
        if index == 4:
            return ref.at[pl.ds(part * (rows // 2), rows // 2), :]
        return ref.at[:, pl.ds(part * (cols // 2), cols // 2)]

    def stage_of(index, part):
        if index == 4:
            return up_w.at[pl.ds(7 * width, heads // 2), pl.ds(part * width, width)]
        length = units // 2 if index < 3 else 3 * heads // 2
        return up_w.at[pl.ds((3 + index) * width, width), pl.ds(part * (units // 2), length)]

    def send_far(index, part):
        return remote(
            half_of(piece(index, 3), index, part),
            half_of(grad_merge[index], index, part),
            w_send.at[index - 1],
            w_recv.at[index - 1, part],
            "dp",
            own ^ (2 + 2 * part),
        )

    def send_near(index, slot, part):
        return remote(
            half_of(piece(index, slot), index, part),
            half_of(landing_of(index, slot), index, part),
            w_send.at[index - 1],
            n_recv.at[index - 1],
            "dp",
            own ^ (2 * slot),
        )

    def keep_grad(index):
        return local(piece(index, 0), landing_of(index, 0), keep.at[index])

    def merge_grads(index):
        loads = [local(half_of(grad_merge[index], index, part), stage_of(index, part), load.at[part]) for part in range(2)]
        for part in range(2):
            send_far(index, part).wait_recv()
            loads[part].start()
        for part in range(2):
            loads[part].wait()
            target, source = half_of(piece(index, 2 - part), index, part), stage_of(index, part)
            length = source.shape[0] // 4

            @pl.loop(0, 4)
            def _(step):
                rows = cols_of(step, length)
                target[rows, :] = (target[rows, :].astype(F32) + source[rows, :].astype(F32)).astype(BF)

            send_near(index, 2 - part, part).start()

    def row_grads(index, slot, left, left_pair, right, right_pair, columns):
        mine, theirs = slice_of(slot, width, True), slice_of(slot, width, False)
        turned, turned_pair = jnp.transpose(left[:, mine]), jnp.transpose(left_pair[:, theirs])
        target = piece(index, slot)

        @pl.loop(0, columns // 512)
        def _(step):
            cols = cols_of(step, 512)
            total = dot(turned, right[:, cols]) + dot(turned_pair, right_pair[:, cols])
            target[:, cols] = total.astype(BF)

        if slot == 3:
            send_far(index, 0).start()
            send_far(index, 1).start()
        elif slot:
            send_near(index, slot, slot - 1).start()
        elif index == 3:
            keep_grad(index).start()

    def out_grads():
        for part in range(2):
            rows = pl.ds(part * (heads // 2), heads // 2)
            turned, turned_pair = jnp.transpose(attended[:, rows]), jnp.transpose(cot[:, rows])
            for slot in range(4):
                mine, theirs = slice_of(slot, width, True), slice_of(slot, width, False)
                total = dot(turned, buffer_a[:, mine]) + dot(turned_pair, cot_half[:, theirs])
                piece(4, slot)[rows, :] = total.astype(BF)
            send_far(4, part).start()
            send_near(4, part + 1, part).start()
        keep_grad(4).start()

    def down_piece(slot, index, part=None):
        cols = pl.ds(((slot % 2) * GROUPS + index) * width, width)
        rows = pl.ds(0, group) if part is None else pl.ds(part * (group // 2), group // 2)
        return (buffer_b, buffer_c)[slot // 2].at[rows, cols]

    def down_rows(ref, index, slot, part=None):
        rows = pl.ds(index * group, group) if part is None else pl.ds(index * group + part * (group // 2), group // 2)
        return ref.at[rows, pl.ds(slot * width, width)]

    def send_down(kind, index, part):
        if kind == 0:
            target, source = down_rows(grad_merge[0], index, 0, part), down_piece(3, index, part)
            peer = own ^ (2 + 2 * part)
        else:
            target, source = down_rows(down_parts, index, kind - 1, part), down_piece(kind, index, part)
            peer = own ^ (2 * kind)
        return remote(source, target, d_send.at[0], d_recv.at[GROUPS if kind else index], "dp", peer)

    def down_grads(index):
        drain(buffer_a.at[:, pl.ds(index * group, group)], f_recv.at[index])

        @pl.loop(0, group // 256)
        def _(step):
            cols = pl.ds(pl.multiple_of(index * group + step * 256, 256), 256)
            rows = pl.ds(pl.multiple_of(step * 256, 256), 256)
            turned, turned_pair = jnp.transpose(hidden[:, cols]), jnp.transpose(buffer_a[:, cols])
            for slot in range(4):
                mine, theirs = slice_of(slot, width, True), slice_of(slot, width, False)
                total = dot(turned, cot[:, mine]) + dot(turned_pair, cot_half[:, theirs])
                down_piece(slot, index)[rows, :] = total.astype(BF)

        for part in range(2):
            send_down(0, index, part).start()
        for part in range(2):
            send_down(1 + part, index, part).start()

    def merge_down(indices):
        entries = [(index, part) for index in indices for part in range(2)]

        def stage(index, part):
            rows = pl.ds(part * (group // 2), group // 2)
            return d_attended.at[rows, pl.ds((index % 2) * width, width)]

        loads = [
            local(down_rows(grad_merge[0], index, 0, part), stage(index, part), load.at[2 * (index % 2) + part])
            for index, part in entries
        ]
        for index in indices:
            drain(down_rows(grad_merge[0], index, 0), d_recv.at[index])
        start_all(loads)
        for copy, (index, part) in zip(loads, entries):
            copy.wait()
            target, source = down_piece(2 - part, index, part), stage(index, part)

            @pl.loop(0, 2)
            def _(step):
                rows = cols_of(step, group // 4)
                target[rows, :] = (target[rows, :].astype(F32) + source[rows, :].astype(F32)).astype(BF)

            send_down(2 - part, index, part).start()

    def norm_back(total, values, gain):
        inverse = lax.rsqrt(jnp.mean(values * values, axis=-1, keepdims=True) + EPSILON)
        scaled = total * gain
        return inverse * (scaled - values * inverse * inverse * jnp.mean(scaled * values, axis=-1, keepdims=True))

    first_loads = [local(source, target, load.at[12 + index]) for index, (source, target) in enumerate(
        zip((docs_hbm, *gains_hbm), (docs, *plain_gains))
    )]
    meet()
    start_all(first_loads)
    send_weights(range(3))
    for gather in gather_hidden:
        gather.start()
    wait_all(first_loads)
    gains_in[...] = jnp.zeros(gains_in.shape, F32)
    for index, plain in enumerate(plain_gains):
        gains_in[index : index + 1, :] = plain[...].astype(F32).reshape(1, width)
    for flip in range(1, 8):
        send_gain(flip).start()
    stage_down = down_w.at[:, pl.ds(3 * heads, width)]
    stage_in = local(weights_in[4], stage_down, load.at[0])
    own_loads = [local(gains_in, at_cols(gains, own, width), load.at[1])]
    own_loads += [local(weights_in[item], view(item, own), load.at[2 + item]) for item in range(4)]
    own_loads += [local(weights_in[5], at_rows(gate_w, own, width), load.at[6])]
    own_loads += [local(weights_in[6], at_rows(up_w, own, width), load.at[7])]
    for part in range(PARTS):
        own_loads.append(local(hidden_in.at[part_rows(part), :], buffer_b.at[own_rows(part), :], load.at[8 + part]))
        own_loads.append(local(cot_in.at[part_rows(part), :], cot.at[own_rows(part), :], load.at[10 + part]))
    start_all([stage_in] + own_loads)
    fill_mask(bias, docs, size)
    fill_turns(cosine, sine, size)
    for part in range(PARTS):
        clear(part)
    relay_weights([0])
    gather_hidden[0].hop(0)
    gather_hidden[0].hop(1)
    relay_weights([1])
    gather_hidden[1].hop(0)
    gather_hidden[1].hop(1)
    gather_hidden[0].hop(2)
    relay_weights([2])
    send_weights([3, 4])
    gather_hidden[1].hop(2)
    for gather in gather_cot:
        gather.start()
    stage_in.wait()
    stage_out = local(stage_down, at_cols(down_full, own, width), keep.at[5])
    stage_out.start()
    wait_all(own_loads)
    drain(gain_recv.at[pl.ds(0, 56), :], y_recv.at[0])
    gather_cot[0].hop(1)
    gather_cot[0].hop(0)
    pass_weights(range(3))
    relay_weights([3])
    send_weights(range(5, 4 + 3 * GROUPS))
    for gather in gather_hidden:
        gather.wait()

    norm_rows(buffer_b, buffer_c, inverses_one, gains.at[pl.ds(0, 1), :], 64)
    keep_hidden = local(buffer_b, hidden_rows, keep.at[0])
    keep_normed = local(buffer_c, normed_rows, keep.at[1])
    start_all([keep_hidden, keep_normed])
    have_weights(0)
    qkv_w = down_w.at[:, pl.ds(0, 3 * heads)]
    keep_qkv = local(qkv_w, qkv_full, keep.at[2])
    keep_qkv.start()

    @pl.loop(0, 2 * heads // step_cols)
    def _(step):
        cols = cols_of(step)
        product = dot(buffer_c[...], down_w[:, cols])
        turns = [jnp.concatenate([table[...]] * (step_cols // 128), axis=1) for table in (cosine, sine)]
        qkv[:, cols] = turn(product, *turns).astype(BF)

    @pl.loop(2 * heads // step_cols, 3 * heads // step_cols)
    def _(step):
        cols = cols_of(step)
        qkv[:, cols] = dot(buffer_c[...], down_w[:, cols]).astype(BF)

    attend(qkv, attended, bias, heads)
    gather_cot[0].hop(2)
    gather_cot[1].hop(1)
    gather_cot[1].hop(0)
    pass_weights([3])
    have_weights(1)

    def make_out(part):
        @pl.loop(0, count)
        def _(step):
            cols = cols_of(step)
            product = dot(attended[part * span : (part + 1) * span, :], out_w[:, cols])
            middle[part_rows(part), cols] = product[:size, :]
            send_part[pl.ds(part * span + size, span - size), cols] = product[size:, :].astype(BF)

    make_out(0)
    out_scatter[0].start()
    make_out(1)
    out_scatter[1].start()
    gather_cot[1].hop(2)
    wait_all([keep_hidden, keep_normed, keep_qkv, stage_out])
    send_normed = halves(normed_rows, pair_normed, 1)
    send_attended = to_pair(attended, pair_attended, 2, 0)
    start_all(send_normed + [send_attended])
    for index in range(3):
        out_scatter[0].hop(index)
    relay_weights(items_of(0))

    def make_sent(part):
        out_scatter[part].wait()

        @pl.loop(0, size // 32)
        def _(step):
            rows = pl.ds(pl.multiple_of(part * size + step * 32, 32), 32)
            place = pl.ds(pl.multiple_of(part * span + step * 32, 32), 32)
            total = received(part, step * 32, 32, hidden_of(place) + middle[rows, :])
            middle[rows, :] = total
            sent[place, :] = total.astype(BF)

        gather_sent[part].start()

    def hidden_of(place):
        return buffer_b[place, :].astype(F32)

    for gather in gather_hidden:
        gather.finish()
    make_sent(0)
    out_scatter[1].hop(0)
    relay_weights(items_of(1))
    gather_sent[0].hop(0)
    out_scatter[1].hop(1)
    out_scatter[1].hop(2)
    make_sent(1)
    gather_sent[0].hop(1)
    relay_weights(items_of(2))
    gather_sent[1].hop(0)
    gather_sent[1].hop(1)
    gather_sent[0].hop(2)
    gather_sent[1].hop(2)
    relay_weights(items_of(3))

    def load_down(index):
        rows = pl.ds(index * group, group)
        return local(down_full.at[rows, :], down_w.at[rows, :], down_load.at[index])

    for gather in gather_cot:
        gather.wait()
    send_cot = halves(cot, cot_half, 0)
    start_all(send_cot)
    for gather in gather_sent:
        gather.wait()
    norm_rows(sent, normed, inverses, gains.at[pl.ds(1, 1), :], 64)
    pass_weights(items_of(0))
    send_two = halves(normed, two_half, 3)
    start_all(send_two)
    have_weights(2)
    for phase in range(2):
        sent_weights(phase)
    load_down(0).start()
    for index in range(GROUPS):
        load_down(index).wait()
        if index + 1 < GROUPS:
            pass_weights(items_of(index + 1))

        @pl.loop(index * group // step_cols, (index + 1) * group // step_cols)
        def _(step):
            cols = cols_of(step)
            gate = dot(normed[...], gate_w[:, cols])
            up = dot(normed[...], up_w[:, cols])
            d_hidden = dot_rows(cot[...], down_w[cols, :])
            s = jax.nn.sigmoid(gate)
            activated = gate * s
            hidden[:, cols] = (activated * up).astype(BF)
            d_gate[:, cols] = (d_hidden * up * (s + activated * (1.0 - s))).astype(BF)
            d_up[:, cols] = (d_hidden * activated).astype(BF)
            for which in range(3):
                send_ff(step, which).start()

        if index + 1 < GROUPS:
            have_weights(3 + index)
            load_down(index + 1).start()
        if index == 0:
            drain(cot_half, h_recv.at[0])
        else:
            down_grads(index - 1)

    gain_part[...] = jnp.zeros(gain_part.shape, F32)
    for part in range(PARTS):
        out_scatter[part].finish()

    def make_two(part):
        block = slice(part * span, (part + 1) * span)

        @pl.loop(0, count)
        def _(step):
            cols = cols_of(step)
            product = dot_rows(d_gate[block, :], gate_w[cols, :]) + dot_rows(d_up[block, :], up_w[cols, :])
            gain_part[pl.ds(1, 1), cols] += jnp.sum(
                product * (sent[block, cols].astype(F32) * inverses[block, :]), axis=0, keepdims=True
            )
            grad_middle[part_rows(part), cols] = product[:size, :]
            send_part[pl.ds(part * span + size, span - size), cols] = product[size:, :].astype(BF)

    make_two(0)
    two_scatter[0].start()
    down_grads(GROUPS - 1)
    merge_down((0, 1))
    make_two(1)
    two_scatter[0].hop(0)
    two_scatter[1].start()
    for phase in range(2, 2 + GROUPS):
        sent_weights(phase)
    for which in (1, 2):
        drain((d_gate, d_up)[which - 1], f_recv.at[GROUPS - 1 + which])
    gate_pair, up_pair = up_w.at[pl.ds(0, tokens), :], up_w.at[pl.ds(tokens, tokens), :]
    pair_loads = [local(pair_gate, gate_pair, load.at[0]), local(pair_up, up_pair, load.at[1])]
    start_all(pair_loads)
    drain(two_half, h_recv.at[3])
    wait_all(pair_loads)
    gate_grads = lambda slot: row_grads(1, slot, normed, two_half, d_gate, gate_pair, units)
    up_grads = lambda slot: row_grads(2, slot, normed, two_half, d_up, up_pair, units)
    gate_grads(3)
    merge_down((2, 3))
    two_scatter[0].hop(1)
    two_scatter[0].hop(2)
    for slot in (1, 2, 0):
        gate_grads(slot)

    def make_branch(part):
        two_scatter[part].wait()

        @pl.loop(0, size // 32)
        def _(step):
            rows = pl.ds(pl.multiple_of(part * size + step * 32, 32), 32)
            place = pl.ds(pl.multiple_of(part * span + step * 32, 32), 32)
            total = received(part, step * 32, 32, grad_middle[rows, :])
            result = cot[place, :].astype(F32) + norm_back(total, sent[place, :].astype(F32), gains[1:2, :])
            grad_middle[rows, :] = result
            sent[place, :] = result.astype(BF)

        gather_branch[part].start()
        keep_branch[part].start()

    keep_branch = [
        local(sent.at[own_rows(part), :], branch_rows.at[own_rows(part), :], keep.at[6 + part]) for part in range(PARTS)
    ]
    for part in range(PARTS):
        gather_sent[part].finish()
    make_branch(0)
    up_grads(3)
    two_scatter[1].hop(0)
    up_grads(1)
    gather_branch[0].hop(0)
    two_scatter[1].hop(1)
    two_scatter[1].hop(2)
    up_grads(2)
    up_grads(0)
    def project(first, last):
        @pl.loop(first, last)
        def _(step):
            cols = cols_of(step)
            product = dot(hidden[...], down_w[:, cols])
            for part in range(PARTS):
                start = part * span
                middle[part_rows(part), cols] = middle[part_rows(part), cols] + product[start : start + size, :]
                sent[pl.ds(start + size, span - size), cols] = product[start + size : start + span, :].astype(BF)

    pl.when(ends(rank))(lambda: project(0, count))
    mlp_scatter[0].start((0,))
    make_branch(1)
    mlp_scatter[0].start((1, 2))
    mlp_scatter[1].start()
    pl.when(inner(rank))(lambda: project(0, count // 4))
    gather_branch[0].hop(1)
    merge_grads(1)
    pl.when(inner(rank))(lambda: project(count // 4, count // 2))
    gather_branch[1].hop(0)
    pl.when(inner(rank))(lambda: project(count // 2, count))
    gather_branch[1].hop(1)
    gather_branch[0].hop(2)
    gather_branch[1].hop(2)
    load_weight = local(qkv_full, qkv_w, load.at[4])
    load_hidden = local(hidden_rows, gate_pair, load.at[5])
    load_normed = local(normed_rows, up_pair, load.at[6])
    start_all([load_hidden, load_normed])
    mlp_scatter[0].hop(0)
    merge_grads(2)
    for part in range(PARTS):
        two_scatter[part].finish()
        gather_branch[part].wait()
        keep_branch[part].wait()

    load_branch = local(branch_rows, buffer_a, load.at[7])
    load_branch.start()
    load_weight.start()
    send_half = halves(branch_rows, pair_branch, 4)
    start_all(send_half)
    mlp_scatter[0].hop(1)
    load_branch.wait()

    @pl.loop(0, heads // step_cols)
    def _(step):
        cols = cols_of(step)
        d_attended[:, cols] = dot_rows(buffer_a[...], out_w[cols, :]).astype(BF)

    drain(cot_half, h_send.at[0])
    for gather in gather_cot:
        gather.finish()
    drain(two_half, h_recv.at[1])
    send_attended.wait_recv()
    early_loads = [
        local(pair_attended, cot.at[:, pl.ds(0, heads)], load.at[8]),
        local(pair_normed, two_half, load.at[9]),
    ]
    start_all(early_loads)
    attend_back(qkv, d_attended, d_qkv, bias, cosine, sine, heads)
    send_qkv = to_pair(d_qkv, pair_qkv, 5, 0)
    send_qkv.start()
    for which in range(3):
        drain((hidden, d_gate, d_up)[which], f_send.at[which])

    drain(cot_half, h_recv.at[4])
    load_half = local(pair_branch, cot_half, load.at[10])
    load_half.start()
    mlp_scatter[0].hop(2)
    mlp_scatter[1].hop(0)
    wait_all([load_weight, load_hidden, load_normed])

    def make_one(part):
        block = slice(part * span, (part + 1) * span)

        @pl.loop(0, count)
        def _(step):
            cols = cols_of(step)
            product = dot_rows(d_qkv[block, :], down_w[cols, pl.ds(0, 3 * heads)])
            gain_part[pl.ds(0, 1), cols] += jnp.sum(
                product * (gate_pair[block, cols].astype(F32) * inverses_one[block, :]), axis=0, keepdims=True
            )
            input_grad[part_rows(part), cols] = product[:size, :]
            send_part[pl.ds(part * span + size, span - size), cols] = product[size:, :].astype(BF)

        one_scatter[part].start()

    def share_gain(flip):
        source = at_cols(gain_part, own ^ flip, width)
        return remote(source, at_rows(gain_recv, flip, 8), g_send.at[0], g_recv.at[0], "dp", own ^ flip)

    make_one(0)
    mlp_scatter[1].hop(1)

    send_qkv.wait_recv()
    drain(two_half, h_send.at[3])
    load_qkv = local(pair_qkv, normed.at[:, pl.ds(0, 3 * heads)], load.at[0])
    load_qkv.start()
    wait_all(early_loads + [load_half])
    out_grads()
    mlp_scatter[1].hop(2)
    load_qkv.wait()
    for slot in (3, 1, 2, 0):
        row_grads(3, slot, up_pair, two_half, d_qkv, normed, 3 * heads)
        if slot == 2:
            one_scatter[0].hop(0)
            make_one(1)
    for flip in range(1, 8):
        share_gain(flip).start()
    one_scatter[0].hop(1)
    one_scatter[0].hop(2)
    merge_grads(4)

    drain(gate_w.at[pl.ds(0, 2 * width), :], n_recv.at[0])
    drain(gate_w.at[pl.ds(0, 2 * width), :], n_recv.at[1])
    drain(gate_w.at[pl.ds(0, units // 4), :], d_recv.at[GROUPS])
    staged = [up_w.at[pl.ds(2 * index * width, 2 * width), :] for index in range(2)]
    sum_loads = [local(ref, staged[index], load.at[4 + index]) for index, ref in enumerate((gate_parts, up_parts))]
    for index in range(GROUPS):
        for slot in range(2):
            place = buffer_a.at[:, pl.ds((slot * GROUPS + index) * width, width)]
            sum_loads.append(local(down_rows(down_parts, index, slot), place, load.at[6]))
    start_all(sum_loads)

    def add_rows(index):
        total = piece(index, 0)
        sum_loads[index - 1].wait()

        @pl.loop(0, width // 32)
        def _(step):
            rows = cols_of(step, 32)
            near = pl.ds(pl.multiple_of(width + step * 32, 32), 32)
            terms = [total[rows, :], staged[index - 1][rows, :], staged[index - 1][near, :]]
            total[rows, :] = sum(term.astype(F32) for term in terms).astype(BF)

        local(total, (gate_sum, up_sum)[index - 1], keep.at[index]).start()

    def add_down():
        drain(buffer_a, load.at[6])

        @pl.loop(0, tokens // 64)
        def _(step):
            rows = cols_of(step, 64)
            for index in range(GROUPS):
                total = down_piece(0, index)
                terms = [total[rows, :]]
                terms += [buffer_a[rows, pl.ds((slot * GROUPS + index) * width, width)] for slot in range(2)]
                total[rows, :] = sum(term.astype(F32) for term in terms).astype(BF)

        for index in range(GROUPS):
            local(down_piece(0, index), down_rows(down_sum, index, 0), keep.at[8]).start()

    one_scatter[1].hop(0)
    add_rows(1)
    merge_grads(3)
    add_rows(2)
    one_scatter[1].hop(1)
    one_scatter[1].hop(2)
    add_down()

    drain(gain_recv.at[pl.ds(8, 56), :], g_recv.at[0])
    gain_sum = gain_part[:, pl.ds(pl.multiple_of(own * width, width), width)]
    for flip in range(1, 8):
        gain_sum = gain_sum + gain_recv[pl.ds(flip * 8, 8), :]
    gain_z[pl.ds(0, 8), :] = gain_sum

    def share_gain_z(k):
        target = gain_z.at[pl.ds(8 * k, 8), :]
        return remote(gain_z.at[pl.ds(0, 8), :], target, y_send.at[1], y_recv.at[1], "tensor", lax.rem(rank + k, 4))

    for k in (1, 2, 3):
        share_gain_z(k).start()

    load_own = [
        local(hidden_in.at[part_rows(part), :], sent.at[own_rows(part), :], load.at[4 + part]) for part in range(PARTS)
    ]
    for part in range(PARTS):
        gather_branch[part].finish()
    start_all(load_own)
    wait_all(load_own)
    leave = [local(input_grad, input_ref, keep.at[6]), local(layer_out, out_ref, keep.at[7])]
    for scatter in mlp_scatter:
        scatter.wait()

    def mlp_term(part, index):
        return up_w.at[pl.ds((2 * part + index) * size, size), :]

    load_mlp = [
        [local(mlp_recv.at[arrived(part, slot), :], mlp_term(part, index), load.at[2 * part + index])
         for index, slot in enumerate((4, 2))]
        for part in range(PARTS)
    ]
    for part in range(PARTS):
        load_mlp[part][0].start()
        pl.when(inner(rank))(load_mlp[part][1].start)

        @pl.when(ends(rank))
        def _():
            mlp_term(part, 1)[...] = jnp.zeros((size, dim), BF)

    for part in range(PARTS):
        load_mlp[part][0].wait()
        pl.when(inner(rank))(load_mlp[part][1].wait)
        terms = [mlp_term(part, index) for index in range(2)]

        @pl.loop(0, size // 32)
        def _(step):
            rows = pl.ds(pl.multiple_of(part * size + step * 32, 32), 32)
            place = cols_of(step, 32)
            total = middle[rows, :]
            for term in terms:
                total = total + term[place, :].astype(F32)
            layer_out[rows, :] = total.astype(BF)

    leave[1].start()
    for part in range(PARTS):
        one_scatter[part].wait()

        @pl.loop(0, size // 32)
        def _(step):
            rows = pl.ds(pl.multiple_of(part * size + step * 32, 32), 32)
            place = pl.ds(pl.multiple_of(part * span + step * 32, 32), 32)
            total = received(part, step * 32, 32, input_grad[rows, :])
            input_grad[rows, :] = grad_middle[rows, :] + norm_back(total, sent[place, :].astype(F32), gains[0:1, :])

    leave[0].start()

    drain(gain_z.at[pl.ds(8, 24), :], y_recv.at[1])
    gain_all = gain_z[pl.ds(0, 8), :]
    for k in (1, 2, 3):
        gain_all = gain_all + gain_z[pl.ds(8 * k, 8), :]
    gain_total[...] = gain_all
    leave.append(local(gain_total, gain_out, keep.at[5]))
    leave[2].start()

    for scatter in mlp_scatter + one_scatter:
        scatter.finish()
    drain(gate_w.at[pl.ds(0, 3 * units // 8), :], d_send.at[0])
    drain(gain_recv.at[pl.ds(8, 56), :], y_send.at[0])
    drain(gain_recv.at[pl.ds(8, 56), :], g_send.at[0])
    drain(gain_z.at[pl.ds(8, 24), :], y_send.at[1])
    drain(two_half, h_send.at[1])
    drain(two_half, h_send.at[4])
    send_attended.wait_send()
    send_qkv.wait_send()
    def pieces(index, number):
        rows = number * width if index < 4 else number * heads * width // dim
        return gate_w.at[pl.ds(0, rows), pl.ds(0, 3 * heads if index == 3 else dim)]

    wait_all(leave)
    local(gate_w.at[pl.ds(0, width), :], gate_sum, keep.at[1]).wait()
    local(gate_w.at[pl.ds(0, width), :], up_sum, keep.at[2]).wait()
    drain(down_sum, keep.at[8])
    for index in range(1, 5):
        if index > 2:
            drain(pieces(index, 2), n_recv.at[index - 1])
            keep_grad(index).wait()
        drain(pieces(index, 3), w_send.at[index - 1])


def layer(hidden_in, cot, gains, weights, docs):
    tile, dim = hidden_in.shape
    tokens = 4 * tile
    width, heads = weights[0].shape
    units = weights[5].shape[1]
    dma = pltpu.SemaphoreType.DMA
    rows, narrow, ff = shape((tokens, dim), BF), shape((tokens, dim // 2), BF), shape((tokens, units), BF)
    weights_shape = [(units, width), (width, units), (width, units), (width, 3 * heads), (heads, width)]
    sums_shape = weights_shape[:3] + [(3 * width, 3 * heads), (heads, 3 * width)]
    parts_shape = [(units, 2 * width), (2 * width, units), (2 * width, units)]
    outs = [shape(dims, BF) for dims in sums_shape + parts_shape + weights_shape]
    outs += [ff] * 2 + [shape((tokens, 3 * heads), BF), shape((tokens, heads), BF), narrow, narrow]
    outs += [rows] * 3 + [shape((5 * tile, dim), BF), shape((dim, 3 * heads), BF), shape((units, dim), BF)]
    in_hbm = len(outs)
    outs += [shape((tile, dim), BF), shape((tile, dim), F32), shape((8, width), F32)]
    in_hbm += 3
    items = 4 + 3 * GROUPS
    scratch = [((dim, units), BF), ((dim, units), BF), ((units, dim), BF)]
    scratch += [((tokens, dim), BF)] * 3 + [((tokens, units), BF)] * 3
    scratch += [((tokens, dim // 2), BF)] * 2 + [((tokens, dim), BF)] * 3 + [((heads, dim), BF)]
    scratch += [((tokens, 3 * heads), BF)] + [((tokens, heads), BF)] * 2
    scratch += [((tokens, tokens), F32), ((tokens, 128), F32), ((tokens, 128), F32)]
    scratch += [((tokens, 1), F32), ((tokens, 1), F32), ((tile, dim), F32), ((tile, dim), F32)]
    scratch += [((tokens, dim), BF), ((5 * tile, dim), BF)]
    scratch += [((8, width), F32), ((8, dim), F32), ((8, dim), F32), ((64, width), F32), ((32, width), F32)]
    scratch += [((tile, dim), BF), ((tile, dim), F32), ((8, width), F32), (docs.shape, jnp.int32)]
    scratch += [((width,), BF)] * 2
    sems = [(2 + GROUPS,), (4 + GROUPS, 3), (3,), (GROUPS + 2,), (6,), (6,)]
    sems += [(2, PARTS), (2, PARTS, 3), (2, PARTS), (2, PARTS, 5), (4,), (4, 2), (1,), (GROUPS + 1,)]
    sems += [(1,), (1,), (2,), (2,), (15,), (8 + GROUPS,), (GROUPS,), (2 + GROUPS,), (4,)]
    return pl.pallas_call(
        layer_kernel,
        out_shape=outs,
        in_specs=[anyspace()] * 12,
        out_specs=[anyspace()] * in_hbm,
        scratch_shapes=[pltpu.VMEM(*entry) for entry in scratch] + [dma(entry) for entry in sems],
        compiler_params=pltpu.CompilerParams(vmem_limit_bytes=67000000, collective_id=0, has_side_effects=True),
        cost_estimate=cost(2 * tokens * dim * units * 12, 100e6),
        name="layer",
    )(hidden_in, cot, *gains, *weights, docs)


def sum_kernel(counts, *refs):
    parts, plain_in = refs[:5], refs[5:7]
    down, gate, up, query, key, value, out, *plain_out = refs[7:16]
    staged, totals, plain, load, store = refs[16:21], refs[21:26], refs[26:28], refs[28], refs[29]
    loads = [pltpu.make_async_copy(parts[index], staged[index], load.at[index]) for index in range(5)]
    loads += [pltpu.make_async_copy(plain_in[index], plain[index], load.at[5 + index]) for index in range(2)]
    start_all(loads)
    heads = query.shape[1]
    stores = [pltpu.make_async_copy(totals[index], ref, store.at[index]) for index, ref in enumerate((down, gate, up))]
    qkv_stores = [
        pltpu.make_async_copy(totals[3].at[:, pl.ds(index * heads, heads)], ref, store.at[3 + index])
        for index, ref in enumerate((query, key, value))
    ]
    out_store = pltpu.make_async_copy(totals[4], out, store.at[6])
    plain_stores = [pltpu.make_async_copy(plain[index], plain_out[index], store.at[7 + index]) for index in range(2)]
    groups = [[stores[0]], [stores[1]], [stores[2]], qkv_stores, [out_store]]
    for index in range(5):
        loads[index].wait()
        rows_first = index in (1, 2, 3)
        rows, cols = totals[index].shape
        step_rows = 32 if rows_first else 256

        @pl.loop(0, rows // step_rows)
        def _(step):
            start = pl.multiple_of(step * step_rows, step_rows)
            total = None
            for slot in range(counts[index]):
                if rows_first:
                    term = staged[index][pl.ds(pl.multiple_of(start + slot * rows, step_rows), step_rows), :]
                else:
                    term = staged[index][pl.ds(start, step_rows), slot * cols : (slot + 1) * cols]
                term = term.astype(F32)
                total = term if total is None else total + term
            totals[index][pl.ds(start, step_rows), :] = total

        start_all(groups[index])
    for index in range(2):
        loads[5 + index].wait()
        plain_stores[index].start()
    for entry in groups + [plain_stores]:
        wait_all(entry)


def sum_grads(parts, plain, heads, counts):
    dims = [part.shape for part in parts]
    sums = [
        (rows // counts[index], cols) if index in (1, 2, 3) else (rows, cols // counts[index])
        for index, (rows, cols) in enumerate(dims)
    ]
    outs = sums[:3] + [(sums[3][0], heads)] * 3 + [sums[4]]
    dma = pltpu.SemaphoreType.DMA
    return pl.pallas_call(
        partial(sum_kernel, counts),
        out_shape=[shape(dim, F32) for dim in outs] + [shape(entry.shape, entry.dtype) for entry in plain],
        in_specs=[anyspace()] * 7,
        out_specs=[anyspace()] * 9,
        scratch_shapes=[pltpu.VMEM(dim, BF) for dim in dims]
        + [pltpu.VMEM(dim, F32) for dim in sums]
        + [pltpu.VMEM(entry.shape, entry.dtype) for entry in plain]
        + [dma((7,)), dma((9,))],
        compiler_params=params(),
        cost_estimate=cost(1e6, 22e6),
        name="sum_grads",
    )(*parts, *plain)


def shift(values, step):
    size = lax.axis_size("tensor")
    return lax.ppermute(values, "tensor", [(index, (index + step) % size) for index in range(size)])


def gather_rows(values):
    return [values] + [shift(values, step) for step in range(1, lax.axis_size("tensor"))]


def scatter_rows(parts):
    total = parts[0].astype(F32)
    for step in range(1, len(parts)):
        total = total + shift(parts[step], -step).astype(F32)
    return total


def gather_weight(values, axis):
    return [None], [lax.all_gather(values, "dp", axis=axis, tiled=True)]


def scatter_full(left, right, axis):
    full = dot_cols(left, right).astype(BF)
    return lax.psum_scatter(full, "dp", scatter_dimension=axis, tiled=True).astype(F32)


def frequencies():
    half_size = HEAD_DIM // 2
    return ROPE_BASE ** (-jnp.arange(half_size, dtype=F32) / half_size)


def rotary(length):
    angles = jnp.arange(length).astype(F32)[:, None] * frequencies()[None, :]
    cosine, sine = jnp.cos(angles), jnp.sin(angles)
    cosine = jnp.tile(cosine, (1, 8))
    sine = jnp.tile(jnp.concatenate([-sine, sine], axis=1), (1, 4))
    return cosine, sine


def position_tables(doc_ids, ranks):
    length = doc_ids.shape[0]
    token_index = jnp.arange(length, dtype=jnp.int32)
    before = jnp.concatenate([doc_ids[:1] - 1, doc_ids[:-1]])
    doc_start = lax.cummax(jnp.where(doc_ids != before, token_index, 0), axis=0)
    order = (lax.axis_index("tensor") - jnp.arange(ranks)) % ranks
    last = token_index.reshape(ranks, -1)[order].reshape(length)
    first = doc_start.reshape(ranks, -1)[order].reshape(length)
    cosine, sine = (table.reshape(ranks, -1, 256)[order].reshape(length, 256) for table in rotary(length))
    return cosine, sine, first[:, None], last[:, None], last[None, :]


def rms_back(grad_rows_, values, gain):
    inverse = lax.rsqrt(jnp.mean(values * values, axis=-1, keepdims=True) + EPSILON)
    scaled = grad_rows_ * gain
    return inverse * (scaled - values * inverse * inverse * jnp.mean(scaled * values, axis=-1, keepdims=True))


def body(
    hidden_in,
    out_cotangent,
    doc_ids,
    attn_gain,
    query_weight,
    key_weight,
    value_weight,
    out_weight,
    mlp_gain,
    gate_weight,
    up_weight,
    down_weight,
):
    ranks, groups = lax.axis_size("tensor"), lax.axis_size("dp")
    paired = (groups, ranks) == (8, 4)
    width, heads = query_weight.shape
    dim = hidden_in.shape[1]

    if paired:
        weights = (query_weight, key_weight, value_weight, out_weight, down_weight, gate_weight, up_weight)
        outs = layer(hidden_in, out_cotangent, (attn_gain, mlp_gain), weights, doc_ids.reshape(ranks, -1))
        sums = sum_grads(outs[:5], outs[-3:-1], heads, (1, 1, 1, 3, 3))
        down_grad, gate_grad, up_grad, query_grad, key_grad, value_grad, out_proj_grad, layer_out, input_grad = sums
        gain_total = outs[-1]
        share = width // ranks
        gain_grads = lax.dynamic_slice_in_dim(gain_total, lax.axis_index("tensor") * share, share, axis=1)
    else:
        tables = position_tables(doc_ids, ranks)
        input_local = hidden_in.astype(F32)
        hidden_rows = gather_rows(hidden_in)
        gains = lax.all_gather(jnp.stack([attn_gain, mlp_gain]), "dp", axis=1, tiled=True).astype(F32)
        attn_scale, mlp_scale = gains[:1], gains[1:]
        qkv_weight = jnp.concatenate([query_weight, key_weight, value_weight], axis=1)
        tags, qkv_pieces = gather_weight(qkv_weight, 0)
        tags, out_pieces = gather_weight(out_weight, 1)
        cot_rows = gather_rows(out_cotangent)
        tags, down_pieces = gather_weight(down_weight, 1)
        tags, gate_pieces = gather_weight(gate_weight, 0)
        tags, up_pieces = gather_weight(up_weight, 0)
        normed, qkv, attended, inverses, *branch_parts = attn_fwd(
            hidden_rows, attn_scale, tables, tags, width, qkv_pieces, out_pieces
        )
        middle = input_local + scatter_rows(branch_parts)
        sent = middle.astype(BF)
        sent_rows = gather_rows(sent)
        cot_full = jnp.concatenate(cot_rows, axis=0)
        normed_two, hidden, d_gate, d_up, mlp_gain_part, *two_parts = mlp(
            sent_rows, cot_rows, mlp_scale, tags, width, gate_pieces, up_pieces, down_pieces, ranks
        )
        grad_two_rows = scatter_rows(two_parts)
        grad_middle = out_cotangent.astype(F32) + rms_back(grad_two_rows, sent.astype(F32), mlp_scale)
        branch_rows = gather_rows(grad_middle.astype(BF))
        down_grad = scatter_full(hidden, cot_full, 1)
        gate_grad = scatter_full(normed_two, d_gate, 0)
        up_grad = scatter_full(normed_two, d_up, 0)
        mlp_rows = scatter_rows(mlp_out(hidden, ranks, dim, tags, width, down_pieces))
        layer_out = (middle + mlp_rows).astype(BF)
        branch_full, d_qkv, attn_gain_part, *one_parts = attn_bwd(
            branch_rows, hidden_rows, qkv, inverses, tables, tags, width, qkv_pieces, out_pieces, ranks
        )
        out_proj_grad = scatter_full(attended, branch_full, 1)
        query_grad, key_grad, value_grad = jnp.split(scatter_full(normed, d_qkv, 0), 3, axis=1)
        grad_one_rows = scatter_rows(one_parts)
        input_grad = grad_middle + rms_back(grad_one_rows, input_local, attn_scale)
        gain_parts = jnp.concatenate([attn_gain_part, mlp_gain_part], axis=0)
        gain_grads = lax.psum_scatter(gain_parts, ("dp", "tensor"), scatter_dimension=1, tiled=True)
    return (
        layer_out,
        input_grad,
        gain_grads[0],
        query_grad,
        key_grad,
        value_grad,
        out_proj_grad,
        gain_grads[1],
        gate_grad,
        up_grad,
        down_grad,
    )


def solution(mesh):
    return jax.shard_map(
        body,
        mesh=mesh,
        in_specs=(
            P(("dp", "tensor"), None),
            P(("dp", "tensor"), None),
            P("dp"),
            P("dp"),
            P("dp", "tensor"),
            P("dp", "tensor"),
            P("dp", "tensor"),
            P("tensor", "dp"),
            P("dp"),
            P("dp", "tensor"),
            P("dp", "tensor"),
            P("tensor", "dp"),
        ),
        out_specs=(
            P(("dp", "tensor"), None),
            P(("dp", "tensor"), None),
            P(("dp", "tensor")),
            P("dp", "tensor"),
            P("dp", "tensor"),
            P("dp", "tensor"),
            P("tensor", "dp"),
            P(("dp", "tensor")),
            P("dp", "tensor"),
            P("dp", "tensor"),
            P("tensor", "dp"),
        ),
        check_vma=False,
    )
```

```python
import math
from functools import partial

import jax
import jax.numpy as jnp
from jax import lax
from jax.experimental import pallas as pl
from jax.experimental.pallas import tpu as pltpu
from jax.sharding import PartitionSpec as P

HEAD_DIM = 64
EPSILON = 1e-05
ROPE_BASE = 130000.0
NEGATIVE = -1e30
VMEM_LIMIT = 63 * 1024 * 1024
BF = jnp.bfloat16
F32 = jnp.float32


def dot(left, right):
    return jnp.dot(left, right, preferred_element_type=F32)


def dot_rows(left, right):
    return lax.dot_general(left, right, (((1,), (1,)), ((), ())), preferred_element_type=F32)


def dot_cols(left, right):
    return lax.dot_general(left, right, (((0,), (0,)), ((), ())), preferred_element_type=F32)


def vmem():
    return pl.BlockSpec(memory_space=pltpu.VMEM)


def anyspace():
    return pl.BlockSpec(memory_space=pl.ANY)


def params():
    return pltpu.CompilerParams(vmem_limit_bytes=VMEM_LIMIT)


def cost(flops, nbytes):
    return pl.CostEstimate(flops=int(flops), bytes_accessed=int(nbytes), transcendentals=0)


def shape(dims, kind):
    return jax.ShapeDtypeStruct(dims, kind)


def place_copies(tags, pieces, target, sem, axis, width):
    own = lax.axis_index("dp")
    copies = []
    for slot, (tag, piece) in enumerate(zip(tags, pieces)):
        if tag is None:
            where = target
        else:
            start = pl.multiple_of((own ^ tag) * width, width)
            where = target.at[pl.ds(start, width), :] if axis == 0 else target.at[:, pl.ds(start, width)]
        copies.append(pltpu.make_async_copy(piece, where, sem.at[slot]))
    return copies


def row_copies(pieces, target, sem):
    copies = []
    for slot, piece in enumerate(pieces):
        rows = piece.shape[0]
        copies.append(pltpu.make_async_copy(piece, target.at[pl.ds(slot * rows, rows), :], sem.at[slot]))
    return copies


def start_all(copies):
    for copy in copies:
        copy.start()


def wait_all(copies):
    for copy in copies:
        copy.wait()


def turn(values, cosine, sine):
    width = values.shape[1]
    lane = lax.broadcasted_iota(jnp.int32, values.shape, 1)
    partner = jnp.where(
        lax.rem(lane, HEAD_DIM) < HEAD_DIM // 2,
        pltpu.roll(values, width - HEAD_DIM // 2, 1),
        pltpu.roll(values, HEAD_DIM // 2, 1),
    )
    return values * cosine + partner * sine


def norm_rows(source, target, inverses, gain, tile):
    @pl.loop(0, source.shape[0] // tile)
    def _(step):
        rows = pl.ds(pl.multiple_of(step * tile, tile), tile)
        values = source[rows, :].astype(F32)
        inverse = lax.rsqrt(jnp.mean(values * values, axis=-1, keepdims=True) + EPSILON)
        inverses[rows, :] = inverse
        target[rows, :] = (values * inverse * gain[...]).astype(BF)


def fill_bias(bias, first, last, key_index):
    keys = key_index[...]
    bias[...] = jnp.where((keys >= first[...]) & (keys <= last[...]), 0.0, NEGATIVE)


def head_lanes(width, half):
    lane = lax.broadcasted_iota(jnp.int32, (1, width), 1)
    return (lax.div(lane, HEAD_DIM) == half).astype(F32)


def probabilities(query, key, bias):
    scores = dot_rows(query, key) + bias
    weights = jnp.exp(scores - jnp.max(scores, axis=-1, keepdims=True))
    return weights * (1.0 / jnp.sum(weights, axis=-1, keepdims=True))


def attend(qkv, attended, bias, heads):
    @pl.loop(0, heads // 128)
    def _(pair):
        base = pl.multiple_of(pair * 128, 128)
        query = qkv[:, pl.ds(base, 128)]
        key = qkv[:, pl.ds(heads + base, 128)]
        value = qkv[:, pl.ds(2 * heads + base, 128)]
        total = None
        for half in range(2):
            lanes = head_lanes(128, half).astype(BF)
            probs = probabilities(query * (lanes * HEAD_DIM ** (-0.5)), key, bias[...])
            term = dot(probs.astype(BF), value * lanes)
            total = term if total is None else total + term
        attended[:, pl.ds(base, 128)] = total.astype(BF)


def attn_fwd_kernel(tags, width, nrow, *refs):
    npiece = len(tags)
    rows_in = refs[:nrow]
    gain, cosine, sine, first, last, key_index = refs[nrow : nrow + 6]
    rest = refs[nrow + 6 :]
    qkv_in, out_in = rest[:npiece], rest[npiece : 2 * npiece]
    rest = rest[2 * npiece :]
    normed, qkv, attended, inverses = rest[:4]
    parts = rest[4 : 4 + nrow]
    hidden, qkv_w, out_w, bias, sem_rows, sem_qkv, sem_out = rest[4 + nrow :]
    load_rows = row_copies(rows_in, hidden, sem_rows)
    load_qkv = place_copies(tags, qkv_in, qkv_w, sem_qkv, 0, width)
    load_out = place_copies(tags, out_in, out_w, sem_out, 1, width)
    start_all(load_rows + load_qkv + load_out)
    fill_bias(bias, first, last, key_index)
    wait_all(load_rows)
    norm_rows(hidden, normed, inverses, gain, 64)
    wait_all(load_qkv)
    heads = attended.shape[1]
    step_cols = 256

    @pl.loop(0, 2 * heads // step_cols)
    def _(step):
        cols = pl.ds(pl.multiple_of(step * step_cols, step_cols), step_cols)
        qkv[:, cols] = turn(dot(normed[...], qkv_w[:, cols]), cosine[...], sine[...]).astype(BF)

    @pl.loop(2 * heads // step_cols, 3 * heads // step_cols)
    def _(step):
        cols = pl.ds(pl.multiple_of(step * step_cols, step_cols), step_cols)
        qkv[:, cols] = dot(normed[...], qkv_w[:, cols]).astype(BF)

    attend(qkv, attended, bias, heads)
    wait_all(load_out)
    tile = parts[0].shape[0]

    @pl.loop(0, out_w.shape[1] // step_cols)
    def _(step):
        cols = pl.ds(pl.multiple_of(step * step_cols, step_cols), step_cols)
        product = dot(attended[...], out_w[:, cols])
        for slot, part in enumerate(parts):
            part[:, cols] = product[slot * tile : (slot + 1) * tile, :].astype(part.dtype)


def attn_fwd(rows, gain, tables, tags, width, qkv_pieces, out_pieces):
    nrow, (tile, dim) = len(rows), rows[0].shape
    tokens = nrow * tile
    heads = out_pieces[0].shape[0]
    npiece = len(tags)
    return pl.pallas_call(
        partial(attn_fwd_kernel, tags, width, nrow),
        out_shape=[
            shape((tokens, dim), BF),
            shape((tokens, 3 * heads), BF),
            shape((tokens, heads), BF),
            shape((tokens, 1), F32),
        ]
        + [shape((tile, dim), F32 if slot == 0 else BF) for slot in range(nrow)],
        in_specs=[anyspace()] * nrow + [vmem()] * 6 + [anyspace()] * (2 * npiece),
        out_specs=[vmem()] * (4 + nrow),
        scratch_shapes=[
            pltpu.VMEM((tokens, dim), BF),
            pltpu.VMEM((dim, 3 * heads), BF),
            pltpu.VMEM((heads, dim), BF),
            pltpu.VMEM((tokens, tokens), F32),
            pltpu.SemaphoreType.DMA((nrow,)),
            pltpu.SemaphoreType.DMA((npiece,)),
            pltpu.SemaphoreType.DMA((npiece,)),
        ],
        compiler_params=params(),
        cost_estimate=cost(2 * tokens * dim * 4 * heads * 3, 20e6),
        name="attn_fwd",
    )(*rows, gain, *tables, *qkv_pieces, *out_pieces)


def attend_back(qkv, d_attended, d_qkv, bias, cosine, sine, heads):
    score_scale = HEAD_DIM ** (-0.5)

    @pl.loop(0, heads // 128)
    def _(pair):
        base = pl.multiple_of(pair * 128, 128)
        query = qkv[:, pl.ds(base, 128)]
        key = qkv[:, pl.ds(heads + base, 128)]
        value = qkv[:, pl.ds(2 * heads + base, 128)]
        grad = d_attended[:, pl.ds(base, 128)]
        sums = [0.0, 0.0, 0.0]
        for half in range(2):
            lanes = head_lanes(128, half).astype(BF)
            own_query = query * (lanes * score_scale)
            own_grad = grad * lanes
            probs = probabilities(own_query, key, bias[...])
            d_value = dot_cols(probs.astype(BF), own_grad)
            d_probs = dot_rows(own_grad, value)
            delta = jnp.sum(probs * d_probs, axis=-1, keepdims=True)
            d_scores = (probs * (d_probs - delta)).astype(BF)
            d_query = dot(d_scores, key * lanes) * score_scale
            d_key = dot_cols(d_scores, own_query)
            sums = [sums[0] + d_query, sums[1] + d_key, sums[2] + d_value]
        back = -sine[:, :128]
        d_qkv[:, pl.ds(base, 128)] = turn(sums[0], cosine[:, :128], back).astype(BF)
        d_qkv[:, pl.ds(heads + base, 128)] = turn(sums[1], cosine[:, :128], back).astype(BF)
        d_qkv[:, pl.ds(2 * heads + base, 128)] = sums[2].astype(BF)


def attn_bwd_kernel(tags, width, nrow, npart, *refs):
    npiece = len(tags)
    nhid, nrow = nrow[1], nrow[0]
    rows_in, hidden_in = refs[:nrow], refs[nrow : nrow + nhid]
    refs = refs[nrow + nhid :]
    qkv, inverses, cosine, sine, first, last, key_index = refs[:7]
    rest = refs[7:]
    qkv_in, out_in = rest[:npiece], rest[npiece : 2 * npiece]
    rest = rest[2 * npiece :]
    branch, d_qkv, gain_grad = rest[:3]
    parts = rest[3 : 3 + npart]
    hidden, d_attended, qkv_w, out_w, bias, sem_rows, sem_x, sem_qkv, sem_out = rest[3 + npart :]
    load_rows = row_copies(rows_in, branch, sem_rows)
    load_x = row_copies(hidden_in, hidden, sem_x)
    load_out = place_copies(tags, out_in, out_w, sem_out, 1, width)
    load_qkv = place_copies(tags, qkv_in, qkv_w, sem_qkv, 0, width)
    start_all(load_rows + load_out + load_qkv + load_x)
    fill_bias(bias, first, last, key_index)
    wait_all(load_rows)
    wait_all(load_out)
    heads = out_w.shape[0]
    step_cols = 256

    @pl.loop(0, heads // step_cols)
    def _(step):
        cols = pl.ds(pl.multiple_of(step * step_cols, step_cols), step_cols)
        d_attended[:, cols] = dot_rows(branch[...], out_w[cols, :]).astype(BF)

    attend_back(qkv, d_attended, d_qkv, bias, cosine, sine, heads)
    wait_all(load_qkv)
    wait_all(load_x)
    tile = parts[0].shape[0]

    @pl.loop(0, qkv_w.shape[0] // step_cols)
    def _(step):
        cols = pl.ds(pl.multiple_of(step * step_cols, step_cols), step_cols)
        product = dot_rows(d_qkv[...], qkv_w[cols, :])
        gain_grad[:, cols] = jnp.sum(product * (hidden[:, cols].astype(F32) * inverses[...]), axis=0, keepdims=True)
        for slot, part in enumerate(parts):
            part[:, cols] = product[slot * tile : (slot + 1) * tile, :].astype(part.dtype)


def attn_bwd(rows, hidden, qkv, inverses, tables, tags, width, qkv_pieces, out_pieces, npart):
    nrow, nhid, dim = len(rows), len(hidden), rows[0].shape[1]
    tokens = qkv.shape[0]
    tile = tokens // npart
    heads = out_pieces[0].shape[0]
    npiece = len(tags)
    return pl.pallas_call(
        partial(attn_bwd_kernel, tags, width, (nrow, nhid), npart),
        out_shape=[shape((tokens, dim), BF), shape((tokens, 3 * heads), BF), shape((1, dim), F32)]
        + [shape((tile, dim), F32 if slot == 0 else BF) for slot in range(npart)],
        in_specs=[anyspace()] * (nrow + nhid) + [vmem()] * 7 + [anyspace()] * (2 * npiece),
        out_specs=[vmem()] * (3 + npart),
        scratch_shapes=[
            pltpu.VMEM((tokens, dim), BF),
            pltpu.VMEM((tokens, heads), BF),
            pltpu.VMEM((dim, 3 * heads), BF),
            pltpu.VMEM((heads, dim), BF),
            pltpu.VMEM((tokens, tokens), F32),
            pltpu.SemaphoreType.DMA((nrow,)),
            pltpu.SemaphoreType.DMA((nhid,)),
            pltpu.SemaphoreType.DMA((npiece,)),
            pltpu.SemaphoreType.DMA((npiece,)),
        ],
        compiler_params=params(),
        cost_estimate=cost(2 * tokens * dim * 4 * heads * 6, 30e6),
        name="attn_bwd",
    )(*rows, *hidden, qkv, inverses, *tables, *qkv_pieces, *out_pieces)


def mlp_kernel(tags, width, nrow, npart, *refs):
    npiece = len(tags)
    sent_in, cot_in = refs[:nrow], refs[nrow : 2 * nrow]
    gain = refs[2 * nrow]
    rest = refs[2 * nrow + 1 :]
    gate_in, up_in, down_in = rest[:npiece], rest[npiece : 2 * npiece], rest[2 * npiece : 3 * npiece]
    rest = rest[3 * npiece :]
    normed, hidden, d_gate, d_up, gain_grad = rest[:5]
    parts = rest[5 : 5 + npart]
    sent, cot, inverses, gate_w, up_w, down_w, sem_sent, sem_cot, sem_gate, sem_up, sem_down = rest[5 + npart :]
    load_sent = row_copies(sent_in, sent, sem_sent)
    load_cot = row_copies(cot_in, cot, sem_cot)
    load_gate = place_copies(tags, gate_in, gate_w, sem_gate, 0, width)
    load_up = place_copies(tags, up_in, up_w, sem_up, 0, width)
    load_down = place_copies(tags, down_in, down_w, sem_down, 1, width)
    start_all(load_sent + load_cot + load_gate + load_up + load_down)
    wait_all(load_sent)
    norm_rows(sent, normed, inverses, gain, 64)
    wait_all(load_cot)
    wait_all(load_gate)
    wait_all(load_up)
    wait_all(load_down)
    step_cols = 256

    @pl.loop(0, gate_w.shape[1] // step_cols)
    def _(step):
        cols = pl.ds(pl.multiple_of(step * step_cols, step_cols), step_cols)
        gate = dot(normed[...], gate_w[:, cols])
        up = dot(normed[...], up_w[:, cols])
        d_hidden = dot_rows(cot[...], down_w[cols, :])
        s = jax.nn.sigmoid(gate)
        activated = gate * s
        hidden[:, cols] = (activated * up).astype(BF)
        d_gate[:, cols] = (d_hidden * up * (s + activated * (1.0 - s))).astype(BF)
        d_up[:, cols] = (d_hidden * activated).astype(BF)

    tile = parts[0].shape[0]

    @pl.loop(0, gate_w.shape[0] // step_cols)
    def _(step):
        cols = pl.ds(pl.multiple_of(step * step_cols, step_cols), step_cols)
        product = dot_rows(d_gate[...], gate_w[cols, :]) + dot_rows(d_up[...], up_w[cols, :])
        gain_grad[:, cols] = jnp.sum(product * (sent[:, cols].astype(F32) * inverses[...]), axis=0, keepdims=True)
        for slot, part in enumerate(parts):
            part[:, cols] = product[slot * tile : (slot + 1) * tile, :].astype(part.dtype)


def mlp(sent, cot, gain, tags, width, gate_pieces, up_pieces, down_pieces, npart):
    nrow, dim = len(sent), sent[0].shape[1]
    tokens = nrow * sent[0].shape[0]
    tile = tokens // npart
    units = gate_pieces[0].shape[1]
    npiece = len(tags)
    return pl.pallas_call(
        partial(mlp_kernel, tags, width, nrow, npart),
        out_shape=[shape((tokens, dim), BF)]
        + [shape((tokens, units), BF)] * 3
        + [shape((1, dim), F32)]
        + [shape((tile, dim), F32 if slot == 0 else BF) for slot in range(npart)],
        in_specs=[anyspace()] * (2 * nrow) + [vmem()] + [anyspace()] * (3 * npiece),
        out_specs=[vmem()] * (5 + npart),
        scratch_shapes=[
            pltpu.VMEM((tokens, dim), BF),
            pltpu.VMEM((tokens, dim), BF),
            pltpu.VMEM((tokens, 1), F32),
            pltpu.VMEM((dim, units), BF),
            pltpu.VMEM((dim, units), BF),
            pltpu.VMEM((units, dim), BF),
            pltpu.SemaphoreType.DMA((nrow,)),
            pltpu.SemaphoreType.DMA((nrow,)),
            pltpu.SemaphoreType.DMA((npiece,)),
            pltpu.SemaphoreType.DMA((npiece,)),
            pltpu.SemaphoreType.DMA((npiece,)),
        ],
        compiler_params=params(),
        cost_estimate=cost(2 * tokens * dim * units * 5, 40e6),
        name="mlp",
    )(*sent, *cot, gain, *gate_pieces, *up_pieces, *down_pieces)


def mlp_out_kernel(tags, width, *refs):
    npiece = len(tags)
    hidden, down_in = refs[0], refs[1 : 1 + npiece]
    *parts, down_w, sem_down = refs[1 + npiece :]
    load_down = place_copies(tags, down_in, down_w, sem_down, 1, width)
    start_all(load_down)
    wait_all(load_down)
    tile, step_cols = parts[0].shape[0], 256

    @pl.loop(0, down_w.shape[1] // step_cols)
    def _(step):
        cols = pl.ds(pl.multiple_of(step * step_cols, step_cols), step_cols)
        product = dot(hidden[...], down_w[:, cols])
        for slot, part in enumerate(parts):
            part[:, cols] = product[slot * tile : (slot + 1) * tile, :].astype(part.dtype)


def mlp_out(hidden, nrow, dim, tags, width, down_pieces):
    tokens, units = hidden.shape
    tile, npiece = tokens // nrow, len(tags)
    return pl.pallas_call(
        partial(mlp_out_kernel, tags, width),
        out_shape=[shape((tile, dim), F32 if slot == 0 else BF) for slot in range(nrow)],
        in_specs=[vmem()] + [anyspace()] * npiece,
        out_specs=[vmem()] * nrow,
        scratch_shapes=[pltpu.VMEM((units, dim), BF), pltpu.SemaphoreType.DMA((npiece,))],
        compiler_params=params(),
        cost_estimate=cost(2 * tokens * dim * units, 14e6),
        name="mlp_out",
    )(hidden, *down_pieces)


def slice_of(slot, width, own):
    index = lax.axis_index("dp")
    owner = index ^ (2 * slot)
    return pl.ds(pl.multiple_of((owner if own else lax.div(owner, 2)) * width, width), width)

MESH = pl.DeviceIdType.MESH
NEAR = (2, 4, 6)
PARTS = 2
GROUPS = 4


def remote(source, target, send_sem, recv_sem, axis, peer):
    return pltpu.make_async_remote_copy(
        src_ref=source,
        dst_ref=target,
        send_sem=send_sem,
        recv_sem=recv_sem,
        device_id={axis: peer},
        device_id_type=MESH,
    )


def drain(ref, sem):
    pltpu.make_async_copy(ref, ref, sem).wait()


def meet():
    own, rank = lax.axis_index("dp"), lax.axis_index("tensor")
    barrier = pltpu.get_barrier_semaphore()
    for flip in range(1, 8):
        pl.semaphore_signal(barrier, inc=1, device_id={"dp": own ^ flip}, device_id_type=MESH)

    @pl.when(rank < 3)
    def _():
        pl.semaphore_signal(barrier, inc=1, device_id={"tensor": rank + 1}, device_id_type=MESH)

    @pl.when(rank > 0)
    def _():
        pl.semaphore_signal(barrier, inc=1, device_id={"tensor": rank - 1}, device_id_type=MESH)

    pl.semaphore_wait(barrier, 8 + lax.div(rank * (3 - rank), 2))


def at_cols(ref, index, width):
    return ref.at[:, pl.ds(pl.multiple_of(index * width, width), width)]


def at_rows(ref, index, width):
    return ref.at[pl.ds(pl.multiple_of(index * width, width), width), :]


def either(rank, *choices):
    result = rank == choices[0]
    for choice in choices[1:]:
        result = result | (rank == choice)
    return result


def ends(rank):
    return either(rank, 0, 3)


def inner(rank):
    return either(rank, 1, 2)


class RowGather:
    def __init__(self, rank, source, landing, part, size, send, recv):
        self.rank = rank

        def place(slot):
            return landing.at[pl.ds(pl.multiple_of((4 * part + slot) * size, size), size), :]

        def copy(origin, slot, peer):
            return remote(origin, place(slot), send.at[part], recv.at[part, slot - 1], "tensor", peer)

        def forward(slot, target, peer):
            return copy(place(slot), target, peer)

        outward, inward = (rank - 1) * 3, 3 - rank
        near, far = 5 - 2 * rank, 2 * rank - 1
        self.up, self.down = copy(source, 1, rank + 1), copy(source, 3, rank - 1)
        self.hops = [forward(near, 2, outward), forward(far, 2, inward), forward(2, far, outward)]
        self.slots = [near, far, 2]
        self.arrival = lambda slot: copy(source, slot, lax.rem(rank + 1, 4))
        self.sent = lambda count: drain(landing.at[pl.ds(0, count * size), :], send.at[part])

    def start(self):
        pl.when(self.rank < 3)(self.up.start)
        pl.when(self.rank > 0)(self.down.start)

    def hop(self, index):
        @pl.when(inner(self.rank))
        def _():
            self.arrival(self.slots[index]).wait_recv()
            self.hops[index].start()

    def wait(self):
        @pl.when(ends(self.rank))
        def _():
            for slot in (1, 2, 3):
                self.arrival(slot).wait_recv()

    def finish(self):
        pl.when(ends(self.rank))(lambda: self.sent(1))
        pl.when(inner(self.rank))(lambda: self.sent(5))


class RowScatter:
    def __init__(self, rank, source, landing, part, size, send, recv, staged=None, sem=None):
        self.rank, self.source, self.size, self.staged, self.sem = rank, source, size, staged, sem
        self.place = lambda k: pl.ds(pl.multiple_of((4 * part + k) * size, size), size)
        self.land = lambda slot: landing.at[pl.ds((5 * part + slot) * size, size), :]

        def copy(k, slot, peer):
            return remote(source.at[self.place(k), :], self.land(slot), send.at[part], recv.at[part, slot], "tensor", peer)

        end = lax.div(rank, 3)
        self.first = [copy(index + 1 + end * (2 - 2 * index), index, 1 + end) for index in range(3)]
        self.keys = [2, 5 - 2 * rank, 2 * rank - 1]
        self.later = [
            copy(self.keys[0], 3, 3 - rank),
            copy(self.keys[1], 4, 3 - rank),
            copy(self.keys[2], 4, (rank - 1) * 3),
        ]
        self.arrival = lambda slot: copy(1, slot, lax.rem(rank + 1, 4))
        self.finish = lambda: drain(source.at[pl.ds(0, 3 * size), :], send.at[part])

    def start(self, indices=(0, 1, 2)):
        @pl.when(ends(self.rank))
        def _():
            for index in indices:
                self.first[index].start()

    def hop(self, index):
        @pl.when(inner(self.rank))
        def _():
            slot = (0, 1, 3)[index]
            self.arrival(slot).wait_recv()
            other = self.land(slot)
            if self.staged is not None:
                load = pltpu.make_async_copy(other, self.staged, self.sem)
                load.start()
                load.wait()
                other = self.staged
            target = self.source.at[self.place(self.keys[index]), :]

            @pl.loop(0, self.size // 16)
            def _(step):
                rows = pl.ds(pl.multiple_of(step * 16, 16), 16)
                target[rows, :] = (target[rows, :].astype(F32) + other[rows, :].astype(F32)).astype(BF)

            self.later[index].start()

    def wait(self):
        pl.when(inner(self.rank))(self.arrival(2).wait_recv)
        self.arrival(4).wait_recv()


def fill_mask(bias, docs, size):
    rank = lax.axis_index("tensor")
    tokens = bias.shape[0]
    values = docs[...]
    starts = [jnp.sum(jnp.where(values < number, 1, 0), keepdims=True) for number in range(1, 8)]

    def document(position):
        return sum(jnp.where(position >= start, 1, 0) for start in starts)

    lane = lax.broadcasted_iota(jnp.int32, (1, tokens), 1)
    slot = lax.rem(lax.div(lane, size), 4)
    part = lax.div(lane, 4 * size)
    keys = lax.rem(rank - slot + 4, 4) * (2 * size) + part * size + lax.rem(lane, size)
    key_docs = document(keys)

    @pl.loop(0, tokens // size)
    def _(block):
        base = lax.rem(rank - lax.rem(block, 4) + 4, 4) * (2 * size) + lax.div(block, 4) * size
        queries = base + lax.broadcasted_iota(jnp.int32, (size, 1), 0)
        allowed = (document(queries) == key_docs) & (queries >= keys)
        bias[pl.ds(pl.multiple_of(block * size, size), size), :] = jnp.where(allowed, 0.0, NEGATIVE)


def fill_turns(cosine, sine, size):
    rank = lax.axis_index("tensor")
    half_size = HEAD_DIM // 2
    dims = (size, cosine.shape[1])
    lane = lax.broadcasted_iota(jnp.int32, dims, 1)
    row = lax.broadcasted_iota(jnp.int32, dims, 0)
    frequency = jnp.exp(lax.rem(lane, half_size).astype(F32) * (-math.log(ROPE_BASE) / half_size))
    sign = jnp.where(lax.rem(lane, HEAD_DIM) < half_size, -1.0, 1.0)

    @pl.loop(0, cosine.shape[0] // size)
    def _(block):
        start = (lax.rem(rank - lax.rem(block, 4) + 4, 4) * PARTS + lax.div(block, 4)) * size
        angles = (row + start).astype(F32) * frequency
        rows = pl.ds(pl.multiple_of(block * size, size), size)
        cosine[rows, :] = jnp.cos(angles)
        sine[rows, :] = jnp.sin(angles) * sign


def slice_of(slot, width, own):
    index = lax.axis_index("dp")
    owner = index ^ (2 * slot)
    return pl.ds(pl.multiple_of((owner if own else lax.div(owner, 2)) * width, width), width)


def layer_kernel(*refs):
    hidden_in, cot_in, *gains_hbm = refs[:4]
    weights_in = refs[4:11]
    docs_hbm = refs[11]
    down_sum, gate_sum, up_sum, qkv_parts, out_parts = refs[12:17]
    down_parts, gate_parts, up_parts = refs[17:20]
    grad_merge = refs[20:25]
    pair_gate, pair_up, pair_qkv, pair_attended, pair_normed, pair_branch = refs[25:31]
    branch_rows, hidden_rows, normed_rows, mlp_recv, qkv_full, down_full = refs[31:37]
    out_ref, input_ref, gain_out = refs[37:40]
    gate_w, up_w, down_w, sent, cot, normed, hidden, d_gate, d_up = refs[40:49]
    two_half, cot_half, buffer_a, buffer_b, buffer_c, out_w = refs[49:55]
    qkv, attended, d_attended, bias, cosine, sine = refs[55:61]
    inverses_one, inverses, middle, grad_middle, send_part, recv_part = refs[61:67]
    gains_in, gains, gain_part, gain_recv, gain_z, layer_out, input_grad, gain_total, docs, *plain_gains = refs[67:78]
    a_send, a_recv, f_send, f_recv, h_send, h_recv, z_send, z_recv, r_send, r_recv = refs[78:88]
    w_send, w_recv, d_send, d_recv, g_send, g_recv, y_send, y_recv, load, keep, down_load, s_recv, n_recv = refs[88:]

    own, rank = lax.axis_index("dp"), lax.axis_index("tensor")
    core = lax.rem(own, 2)
    tokens, dim = sent.shape
    units = gate_w.shape[1]
    tile = hidden_in.shape[0]
    size = tile // PARTS
    span = 4 * size
    heads = attended.shape[1]
    width = weights_in[0].shape[0]
    half = dim // (2 * width)
    d_qkv = cot.at[:, pl.ds(heads, 3 * heads)]
    group = units // GROUPS
    step_cols = 256
    count = dim // step_cols

    def cols_of(step, length=step_cols):
        return pl.ds(pl.multiple_of(step * length, length), length)

    def local(source, target, sem):
        return pltpu.make_async_copy(source, target, sem)

    def own_rows(part):
        return pl.ds(part * span, size)

    def part_rows(part):
        return pl.ds(part * size, size)

    def source_of(item):
        if item < 4:
            return weights_in[item]
        which, start = (item - 4) % 3, ((item - 4) // 3) * group
        if which == 2:
            return weights_in[4].at[pl.ds(start, group), :]
        return weights_in[5 + which].at[:, pl.ds(start, group)]

    def view(item, owner, part=None):
        rows = heads if item == 3 else group if item > 3 and (item - 4) % 3 == 2 else width
        length = rows if part is None else rows // 2
        start = 0 if part is None else part * length
        if item < 3:
            place = pl.ds(pl.multiple_of(owner * width + start, length), length)
            return down_w.at[place, pl.ds(item * heads, heads)]
        if item == 3:
            return out_w.at[pl.ds(start, length), pl.ds(pl.multiple_of(owner * width, width), width)]
        which, offset = (item - 4) % 3, ((item - 4) // 3) * group
        if which == 2:
            return down_full.at[pl.ds(offset + start, length), pl.ds(pl.multiple_of(owner * width, width), width)]
        place = pl.ds(pl.multiple_of(owner * width + start, length), length)
        return (gate_w, up_w)[which].at[place, pl.ds(offset, group)]

    def phase_of(item):
        return 0 if item < 3 else 1 if item == 3 else 2 + (item - 4) // 3

    def lot_of(item):
        return item if item < 4 else 4 + (item - 4) // 3

    def send_weight(item, flip):
        sem = s_recv.at[phase_of(item)] if flip == 1 else a_recv.at[lot_of(item), flip // 2 - 1]
        return remote(source_of(item), view(item, own), a_send.at[phase_of(item)], sem, "dp", own ^ flip)

    def relay_weight(item, part):
        place = view(item, own ^ (4 - 2 * part), part)
        return remote(place, place, a_send.at[phase_of(item)], a_recv.at[lot_of(item), 2], "dp", own ^ (2 + 2 * part))

    def pass_weight(item, flip):
        place = view(item, own ^ flip)
        return remote(place, place, a_send.at[phase_of(item)], s_recv.at[phase_of(item)], "dp", own ^ 1)

    def send_weights(items):
        for item in items:
            for flip in (2, 4, 1):
                send_weight(item, flip).start()

    def lots(items):
        return [[item] for item in items] if items[0] < 4 else [items]

    def arrived_weights(lot, tag):
        drain(gate_w.at[pl.ds(0, len(lot) * width // 4), :], a_recv.at[lot_of(lot[0]), tag])

    def relay_weights(items):
        for lot in lots(items):
            arrived_weights(lot, 1)
            for item in lot:
                relay_weight(item, 0).start()
            arrived_weights(lot, 0)
            for item in lot:
                relay_weight(item, 1).start()
            for item in lot:
                pass_weight(item, 4).start()
                pass_weight(item, 2).start()

    def pass_weights(items):
        for lot in lots(items):
            arrived_weights(lot, 2)
            for item in lot:
                pass_weight(item, 6).start()

    def have_weights(phase):
        drain(gate_w.at[pl.ds(0, width if phase == 1 else 3 * width), :], s_recv.at[phase])

    def sent_weights(phase):
        length = 7 * width // 4
        drain(gate_w.at[pl.ds(0, length if phase == 1 else 3 * length), :], a_send.at[phase])

    def items_of(index):
        return list(range(4 + 3 * index, 7 + 3 * index))

    def send_gain(flip):
        return remote(gains_in, at_cols(gains, own, width), y_send.at[0], y_recv.at[0], "dp", own ^ flip)

    def gathers(kind, source, landing):
        return [
            RowGather(rank, source(part), landing, part, size, z_send.at[kind], z_recv.at[kind]) for part in range(PARTS)
        ]

    gather_hidden = gathers(0, lambda part: hidden_in.at[part_rows(part), :], buffer_b)
    gather_cot = gathers(1, lambda part: cot_in.at[part_rows(part), :], cot)
    gather_sent = gathers(0, lambda part: sent.at[own_rows(part), :], sent)
    gather_branch = gathers(0, lambda part: sent.at[own_rows(part), :], branch_rows)

    def scatters(kind, source, landing, staged=None, sem=None):
        return [
            RowScatter(rank, source, landing, part, size, r_send.at[kind], r_recv.at[kind], staged, sem)
            for part in range(PARTS)
        ]

    gate_stage = up_w.at[pl.ds(4 * width, size), :]
    out_scatter = scatters(0, send_part, recv_part)
    two_scatter = scatters(0, send_part, recv_part)
    mlp_scatter = scatters(1, sent, mlp_recv, gate_stage, load.at[3])
    one_scatter = scatters(0, send_part, recv_part)

    def arrived(part, slot):
        return pl.ds((5 * part + slot) * size, size)

    def clear(part):
        @pl.when(ends(rank))
        def _():
            recv_part[arrived(part, 2), :] = jnp.zeros((size, dim), BF)

    def received(part, start, length, base):
        total = base
        for slot in (2, 4):
            rows = pl.ds(pl.multiple_of((5 * part + slot) * size + start, length), length)
            total = total + recv_part[rows, :].astype(F32)
        return total

    def to_pair(source, target, row, slot):
        return remote(source, target, h_send.at[row], h_recv.at[row], "dp", own ^ 1)

    def halves(source, target, row):
        return [
            to_pair(at_cols(source, 2 * slot + 1 - core, width), at_cols(target, slot, width), row, slot)
            for slot in range(half)
        ]

    def send_ff(step, which):
        cols = cols_of(step)
        source = (hidden, d_gate, d_up)[which].at[:, cols]
        target = (buffer_a, pair_gate, pair_up)[which].at[:, cols]
        arrival = lax.div(step, group // step_cols) if which == 0 else GROUPS - 1 + which
        return remote(source, target, f_send.at[which], f_recv.at[arrival], "dp", own ^ 1)

    def piece(index, slot):
        if index < 3:
            return at_rows(gate_w, (index - 1) * 4 + slot, width)
        if index == 3:
            return (hidden, d_gate)[slot // 2].at[pl.ds((slot % 2) * width, width), pl.ds(0, 3 * heads)]
        return at_cols(d_up, slot, width)

    def landing_of(index, slot):
        ref = (down_parts, gate_parts, up_parts, qkv_parts, out_parts)[index]
        if index < 3:
            return at_rows(ref, slot - 1, width)
        return at_cols(ref, slot, width) if index == 4 else at_rows(ref, slot, width)

    def half_of(ref, index, part):
        rows, cols = ref.shape
        if index == 4:
            return ref.at[pl.ds(part * (rows // 2), rows // 2), :]
        return ref.at[:, pl.ds(part * (cols // 2), cols // 2)]

    def stage_of(index, part):
        if index == 4:
            return up_w.at[pl.ds(7 * width, heads // 2), pl.ds(part * width, width)]
        length = units // 2 if index < 3 else 3 * heads // 2
        return up_w.at[pl.ds((3 + index) * width, width), pl.ds(part * (units // 2), length)]

    def send_far(index, part):
        return remote(
            half_of(piece(index, 3), index, part),
            half_of(grad_merge[index], index, part),
            w_send.at[index - 1],
            w_recv.at[index - 1, part],
            "dp",
            own ^ (2 + 2 * part),
        )

    def send_near(index, slot, part):
        return remote(
            half_of(piece(index, slot), index, part),
            half_of(landing_of(index, slot), index, part),
            w_send.at[index - 1],
            n_recv.at[index - 1],
            "dp",
            own ^ (2 * slot),
        )

    def keep_grad(index):
        return local(piece(index, 0), landing_of(index, 0), keep.at[index])

    def merge_grads(index):
        loads = [local(half_of(grad_merge[index], index, part), stage_of(index, part), load.at[part]) for part in range(2)]
        for part in range(2):
            send_far(index, part).wait_recv()
            loads[part].start()
        for part in range(2):
            loads[part].wait()
            target, source = half_of(piece(index, 2 - part), index, part), stage_of(index, part)
            length = source.shape[0] // 4

            @pl.loop(0, 4)
            def _(step):
                rows = cols_of(step, length)
                target[rows, :] = (target[rows, :].astype(F32) + source[rows, :].astype(F32)).astype(BF)

            send_near(index, 2 - part, part).start()

    def row_grads(index, slot, left, left_pair, right, right_pair, columns):
        mine, theirs = slice_of(slot, width, True), slice_of(slot, width, False)
        turned, turned_pair = jnp.transpose(left[:, mine]), jnp.transpose(left_pair[:, theirs])
        target = piece(index, slot)

        @pl.loop(0, columns // 512)
        def _(step):
            cols = cols_of(step, 512)
            total = dot(turned, right[:, cols]) + dot(turned_pair, right_pair[:, cols])
            target[:, cols] = total.astype(BF)

        if slot == 3:
            send_far(index, 0).start()
            send_far(index, 1).start()
        elif slot:
            send_near(index, slot, slot - 1).start()
        elif index == 3:
            keep_grad(index).start()

    def out_grads():
        for part in range(2):
            rows = pl.ds(part * (heads // 2), heads // 2)
            turned, turned_pair = jnp.transpose(attended[:, rows]), jnp.transpose(cot[:, rows])
            for slot in range(4):
                mine, theirs = slice_of(slot, width, True), slice_of(slot, width, False)
                total = dot(turned, buffer_a[:, mine]) + dot(turned_pair, cot_half[:, theirs])
                piece(4, slot)[rows, :] = total.astype(BF)
            send_far(4, part).start()
            send_near(4, part + 1, part).start()
        keep_grad(4).start()

    def down_piece(slot, index, part=None):
        cols = pl.ds(((slot % 2) * GROUPS + index) * width, width)
        rows = pl.ds(0, group) if part is None else pl.ds(part * (group // 2), group // 2)
        return (buffer_b, buffer_c)[slot // 2].at[rows, cols]

    def down_rows(ref, index, slot, part=None):
        rows = pl.ds(index * group, group) if part is None else pl.ds(index * group + part * (group // 2), group // 2)
        return ref.at[rows, pl.ds(slot * width, width)]

    def send_down(kind, index, part):
        if kind == 0:
            target, source = down_rows(grad_merge[0], index, 0, part), down_piece(3, index, part)
            peer = own ^ (2 + 2 * part)
        else:
            target, source = down_rows(down_parts, index, kind - 1, part), down_piece(kind, index, part)
            peer = own ^ (2 * kind)
        return remote(source, target, d_send.at[0], d_recv.at[GROUPS if kind else index], "dp", peer)

    def down_grads(index):
        drain(buffer_a.at[:, pl.ds(index * group, group)], f_recv.at[index])

        @pl.loop(0, group // 256)
        def _(step):
            cols = pl.ds(pl.multiple_of(index * group + step * 256, 256), 256)
            rows = pl.ds(pl.multiple_of(step * 256, 256), 256)
            turned, turned_pair = jnp.transpose(hidden[:, cols]), jnp.transpose(buffer_a[:, cols])
            for slot in range(4):
                mine, theirs = slice_of(slot, width, True), slice_of(slot, width, False)
                total = dot(turned, cot[:, mine]) + dot(turned_pair, cot_half[:, theirs])
                down_piece(slot, index)[rows, :] = total.astype(BF)

        for part in range(2):
            send_down(0, index, part).start()
        for part in range(2):
            send_down(1 + part, index, part).start()

    def merge_down(indices):
        entries = [(index, part) for index in indices for part in range(2)]

        def stage(index, part):
            rows = pl.ds(part * (group // 2), group // 2)
            return d_attended.at[rows, pl.ds((index % 2) * width, width)]

        loads = [
            local(down_rows(grad_merge[0], index, 0, part), stage(index, part), load.at[2 * (index % 2) + part])
            for index, part in entries
        ]
        for index in indices:
            drain(down_rows(grad_merge[0], index, 0), d_recv.at[index])
        start_all(loads)
        for copy, (index, part) in zip(loads, entries):
            copy.wait()
            target, source = down_piece(2 - part, index, part), stage(index, part)

            @pl.loop(0, 2)
            def _(step):
                rows = cols_of(step, group // 4)
                target[rows, :] = (target[rows, :].astype(F32) + source[rows, :].astype(F32)).astype(BF)

            send_down(2 - part, index, part).start()

    def norm_back(total, values, gain):
        inverse = lax.rsqrt(jnp.mean(values * values, axis=-1, keepdims=True) + EPSILON)
        scaled = total * gain
        return inverse * (scaled - values * inverse * inverse * jnp.mean(scaled * values, axis=-1, keepdims=True))

    first_loads = [local(source, target, load.at[12 + index]) for index, (source, target) in enumerate(
        zip((docs_hbm, *gains_hbm), (docs, *plain_gains))
    )]
    meet()
    start_all(first_loads)
    send_weights(range(3))
    for gather in gather_hidden:
        gather.start()
    wait_all(first_loads)
    gains_in[...] = jnp.zeros(gains_in.shape, F32)
    for index, plain in enumerate(plain_gains):
        gains_in[index : index + 1, :] = plain[...].astype(F32).reshape(1, width)
    for flip in range(1, 8):
        send_gain(flip).start()
    stage_down = down_w.at[:, pl.ds(3 * heads, width)]
    stage_in = local(weights_in[4], stage_down, load.at[0])
    own_loads = [local(gains_in, at_cols(gains, own, width), load.at[1])]
    own_loads += [local(weights_in[item], view(item, own), load.at[2 + item]) for item in range(4)]
    own_loads += [local(weights_in[5], at_rows(gate_w, own, width), load.at[6])]
    own_loads += [local(weights_in[6], at_rows(up_w, own, width), load.at[7])]
    for part in range(PARTS):
        own_loads.append(local(hidden_in.at[part_rows(part), :], buffer_b.at[own_rows(part), :], load.at[8 + part]))
        own_loads.append(local(cot_in.at[part_rows(part), :], cot.at[own_rows(part), :], load.at[10 + part]))
    start_all([stage_in] + own_loads)
    fill_mask(bias, docs, size)
    fill_turns(cosine, sine, size)
    for part in range(PARTS):
        clear(part)
    relay_weights([0])
    gather_hidden[0].hop(0)
    gather_hidden[0].hop(1)
    relay_weights([1])
    gather_hidden[1].hop(0)
    gather_hidden[1].hop(1)
    gather_hidden[0].hop(2)
    relay_weights([2])
    send_weights([3, 4])
    gather_hidden[1].hop(2)
    for gather in gather_cot:
        gather.start()
    stage_in.wait()
    stage_out = local(stage_down, at_cols(down_full, own, width), keep.at[5])
    stage_out.start()
    wait_all(own_loads)
    drain(gain_recv.at[pl.ds(0, 56), :], y_recv.at[0])
    gather_cot[0].hop(1)
    gather_cot[0].hop(0)
    pass_weights(range(3))
    relay_weights([3])
    send_weights(range(5, 4 + 3 * GROUPS))
    for gather in gather_hidden:
        gather.wait()

    norm_rows(buffer_b, buffer_c, inverses_one, gains.at[pl.ds(0, 1), :], 64)
    keep_hidden = local(buffer_b, hidden_rows, keep.at[0])
    keep_normed = local(buffer_c, normed_rows, keep.at[1])
    start_all([keep_hidden, keep_normed])
    have_weights(0)
    qkv_w = down_w.at[:, pl.ds(0, 3 * heads)]
    keep_qkv = local(qkv_w, qkv_full, keep.at[2])
    keep_qkv.start()

    @pl.loop(0, 2 * heads // step_cols)
    def _(step):
        cols = cols_of(step)
        product = dot(buffer_c[...], down_w[:, cols])
        turns = [jnp.concatenate([table[...]] * (step_cols // 128), axis=1) for table in (cosine, sine)]
        qkv[:, cols] = turn(product, *turns).astype(BF)

    @pl.loop(2 * heads // step_cols, 3 * heads // step_cols)
    def _(step):
        cols = cols_of(step)
        qkv[:, cols] = dot(buffer_c[...], down_w[:, cols]).astype(BF)

    attend(qkv, attended, bias, heads)
    gather_cot[0].hop(2)
    gather_cot[1].hop(1)
    gather_cot[1].hop(0)
    pass_weights([3])
    have_weights(1)

    def make_out(part):
        @pl.loop(0, count)
        def _(step):
            cols = cols_of(step)
            product = dot(attended[part * span : (part + 1) * span, :], out_w[:, cols])
            middle[part_rows(part), cols] = product[:size, :]
            send_part[pl.ds(part * span + size, span - size), cols] = product[size:, :].astype(BF)

    make_out(0)
    out_scatter[0].start()
    make_out(1)
    out_scatter[1].start()
    gather_cot[1].hop(2)
    wait_all([keep_hidden, keep_normed, keep_qkv, stage_out])
    send_normed = halves(normed_rows, pair_normed, 1)
    send_attended = to_pair(attended, pair_attended, 2, 0)
    start_all(send_normed + [send_attended])
    for index in range(3):
        out_scatter[0].hop(index)
    relay_weights(items_of(0))

    def make_sent(part):
        out_scatter[part].wait()

        @pl.loop(0, size // 32)
        def _(step):
            rows = pl.ds(pl.multiple_of(part * size + step * 32, 32), 32)
            place = pl.ds(pl.multiple_of(part * span + step * 32, 32), 32)
            total = received(part, step * 32, 32, hidden_of(place) + middle[rows, :])
            middle[rows, :] = total
            sent[place, :] = total.astype(BF)

        gather_sent[part].start()

    def hidden_of(place):
        return buffer_b[place, :].astype(F32)

    for gather in gather_hidden:
        gather.finish()
    make_sent(0)
    out_scatter[1].hop(0)
    relay_weights(items_of(1))
    gather_sent[0].hop(0)
    out_scatter[1].hop(1)
    out_scatter[1].hop(2)
    make_sent(1)
    gather_sent[0].hop(1)
    relay_weights(items_of(2))
    gather_sent[1].hop(0)
    gather_sent[1].hop(1)
    gather_sent[0].hop(2)
    gather_sent[1].hop(2)
    relay_weights(items_of(3))

    def load_down(index):
        rows = pl.ds(index * group, group)
        return local(down_full.at[rows, :], down_w.at[rows, :], down_load.at[index])

    for gather in gather_cot:
        gather.wait()
    send_cot = halves(cot, cot_half, 0)
    start_all(send_cot)
    for gather in gather_sent:
        gather.wait()
    norm_rows(sent, normed, inverses, gains.at[pl.ds(1, 1), :], 64)
    pass_weights(items_of(0))
    send_two = halves(normed, two_half, 3)
    start_all(send_two)
    have_weights(2)
    for phase in range(2):
        sent_weights(phase)
    load_down(0).start()
    for index in range(GROUPS):
        load_down(index).wait()
        if index + 1 < GROUPS:
            pass_weights(items_of(index + 1))

        @pl.loop(index * group // step_cols, (index + 1) * group // step_cols)
        def _(step):
            cols = cols_of(step)
            gate = dot(normed[...], gate_w[:, cols])
            up = dot(normed[...], up_w[:, cols])
            d_hidden = dot_rows(cot[...], down_w[cols, :])
            s = jax.nn.sigmoid(gate)
            activated = gate * s
            hidden[:, cols] = (activated * up).astype(BF)
            d_gate[:, cols] = (d_hidden * up * (s + activated * (1.0 - s))).astype(BF)
            d_up[:, cols] = (d_hidden * activated).astype(BF)
            for which in range(3):
                send_ff(step, which).start()

        if index + 1 < GROUPS:
            have_weights(3 + index)
            load_down(index + 1).start()
        if index == 0:
            drain(cot_half, h_recv.at[0])
        else:
            down_grads(index - 1)

    gain_part[...] = jnp.zeros(gain_part.shape, F32)
    for part in range(PARTS):
        out_scatter[part].finish()

    def make_two(part):
        block = slice(part * span, (part + 1) * span)

        @pl.loop(0, count)
        def _(step):
            cols = cols_of(step)
            product = dot_rows(d_gate[block, :], gate_w[cols, :]) + dot_rows(d_up[block, :], up_w[cols, :])
            gain_part[pl.ds(1, 1), cols] += jnp.sum(
                product * (sent[block, cols].astype(F32) * inverses[block, :]), axis=0, keepdims=True
            )
            grad_middle[part_rows(part), cols] = product[:size, :]
            send_part[pl.ds(part * span + size, span - size), cols] = product[size:, :].astype(BF)

    make_two(0)
    two_scatter[0].start()
    down_grads(GROUPS - 1)
    merge_down((0, 1))
    make_two(1)
    two_scatter[0].hop(0)
    two_scatter[1].start()
    for phase in range(2, 2 + GROUPS):
        sent_weights(phase)
    for which in (1, 2):
        drain((d_gate, d_up)[which - 1], f_recv.at[GROUPS - 1 + which])
    gate_pair, up_pair = up_w.at[pl.ds(0, tokens), :], up_w.at[pl.ds(tokens, tokens), :]
    pair_loads = [local(pair_gate, gate_pair, load.at[0]), local(pair_up, up_pair, load.at[1])]
    start_all(pair_loads)
    drain(two_half, h_recv.at[3])
    wait_all(pair_loads)
    gate_grads = lambda slot: row_grads(1, slot, normed, two_half, d_gate, gate_pair, units)
    up_grads = lambda slot: row_grads(2, slot, normed, two_half, d_up, up_pair, units)
    gate_grads(3)
    merge_down((2, 3))
    two_scatter[0].hop(1)
    two_scatter[0].hop(2)
    for slot in (1, 2, 0):
        gate_grads(slot)

    def make_branch(part):
        two_scatter[part].wait()

        @pl.loop(0, size // 32)
        def _(step):
            rows = pl.ds(pl.multiple_of(part * size + step * 32, 32), 32)
            place = pl.ds(pl.multiple_of(part * span + step * 32, 32), 32)
            total = received(part, step * 32, 32, grad_middle[rows, :])
            result = cot[place, :].astype(F32) + norm_back(total, sent[place, :].astype(F32), gains[1:2, :])
            grad_middle[rows, :] = result
            sent[place, :] = result.astype(BF)

        gather_branch[part].start()
        keep_branch[part].start()

    keep_branch = [
        local(sent.at[own_rows(part), :], branch_rows.at[own_rows(part), :], keep.at[6 + part]) for part in range(PARTS)
    ]
    for part in range(PARTS):
        gather_sent[part].finish()
    make_branch(0)
    up_grads(3)
    two_scatter[1].hop(0)
    up_grads(1)
    gather_branch[0].hop(0)
    two_scatter[1].hop(1)
    two_scatter[1].hop(2)
    up_grads(2)
    up_grads(0)
    def project(first, last):
        @pl.loop(first, last)
        def _(step):
            cols = cols_of(step)
            product = dot(hidden[...], down_w[:, cols])
            for part in range(PARTS):
                start = part * span
                middle[part_rows(part), cols] = middle[part_rows(part), cols] + product[start : start + size, :]
                sent[pl.ds(start + size, span - size), cols] = product[start + size : start + span, :].astype(BF)

    pl.when(ends(rank))(lambda: project(0, count))
    mlp_scatter[0].start((0,))
    make_branch(1)
    mlp_scatter[0].start((1, 2))
    mlp_scatter[1].start()
    pl.when(inner(rank))(lambda: project(0, count // 4))
    gather_branch[0].hop(1)
    merge_grads(1)
    pl.when(inner(rank))(lambda: project(count // 4, count // 2))
    gather_branch[1].hop(0)
    pl.when(inner(rank))(lambda: project(count // 2, count))
    gather_branch[1].hop(1)
    gather_branch[0].hop(2)
    gather_branch[1].hop(2)
    load_weight = local(qkv_full, qkv_w, load.at[4])
    load_hidden = local(hidden_rows, gate_pair, load.at[5])
    load_normed = local(normed_rows, up_pair, load.at[6])
    start_all([load_hidden, load_normed])
    mlp_scatter[0].hop(0)
    merge_grads(2)
    for part in range(PARTS):
        two_scatter[part].finish()
        gather_branch[part].wait()
        keep_branch[part].wait()

    load_branch = local(branch_rows, buffer_a, load.at[7])
    load_branch.start()
    load_weight.start()
    send_half = halves(branch_rows, pair_branch, 4)
    start_all(send_half)
    mlp_scatter[0].hop(1)
    load_branch.wait()

    @pl.loop(0, heads // step_cols)
    def _(step):
        cols = cols_of(step)
        d_attended[:, cols] = dot_rows(buffer_a[...], out_w[cols, :]).astype(BF)

    drain(cot_half, h_send.at[0])
    for gather in gather_cot:
        gather.finish()
    drain(two_half, h_recv.at[1])
    send_attended.wait_recv()
    early_loads = [
        local(pair_attended, cot.at[:, pl.ds(0, heads)], load.at[8]),
        local(pair_normed, two_half, load.at[9]),
    ]
    start_all(early_loads)
    attend_back(qkv, d_attended, d_qkv, bias, cosine, sine, heads)
    send_qkv = to_pair(d_qkv, pair_qkv, 5, 0)
    send_qkv.start()
    for which in range(3):
        drain((hidden, d_gate, d_up)[which], f_send.at[which])

    drain(cot_half, h_recv.at[4])
    load_half = local(pair_branch, cot_half, load.at[10])
    load_half.start()
    mlp_scatter[0].hop(2)
    mlp_scatter[1].hop(0)
    wait_all([load_weight, load_hidden, load_normed])

    def make_one(part):
        block = slice(part * span, (part + 1) * span)

        @pl.loop(0, count)
        def _(step):
            cols = cols_of(step)
            product = dot_rows(d_qkv[block, :], down_w[cols, pl.ds(0, 3 * heads)])
            gain_part[pl.ds(0, 1), cols] += jnp.sum(
                product * (gate_pair[block, cols].astype(F32) * inverses_one[block, :]), axis=0, keepdims=True
            )
            input_grad[part_rows(part), cols] = product[:size, :]
            send_part[pl.ds(part * span + size, span - size), cols] = product[size:, :].astype(BF)

        one_scatter[part].start()

    def share_gain(flip):
        source = at_cols(gain_part, own ^ flip, width)
        return remote(source, at_rows(gain_recv, flip, 8), g_send.at[0], g_recv.at[0], "dp", own ^ flip)

    make_one(0)
    mlp_scatter[1].hop(1)

    send_qkv.wait_recv()
    drain(two_half, h_send.at[3])
    load_qkv = local(pair_qkv, normed.at[:, pl.ds(0, 3 * heads)], load.at[0])
    load_qkv.start()
    wait_all(early_loads + [load_half])
    out_grads()
    mlp_scatter[1].hop(2)
    load_qkv.wait()
    for slot in (3, 1, 2, 0):
        row_grads(3, slot, up_pair, two_half, d_qkv, normed, 3 * heads)
        if slot == 2:
            one_scatter[0].hop(0)
            make_one(1)
    for flip in range(1, 8):
        share_gain(flip).start()
    one_scatter[0].hop(1)
    one_scatter[0].hop(2)
    merge_grads(4)

    drain(gate_w.at[pl.ds(0, 2 * width), :], n_recv.at[0])
    drain(gate_w.at[pl.ds(0, 2 * width), :], n_recv.at[1])
    drain(gate_w.at[pl.ds(0, units // 4), :], d_recv.at[GROUPS])
    staged = [up_w.at[pl.ds(2 * index * width, 2 * width), :] for index in range(2)]
    sum_loads = [local(ref, staged[index], load.at[4 + index]) for index, ref in enumerate((gate_parts, up_parts))]
    for index in range(GROUPS):
        for slot in range(2):
            place = buffer_a.at[:, pl.ds((slot * GROUPS + index) * width, width)]
            sum_loads.append(local(down_rows(down_parts, index, slot), place, load.at[6]))
    start_all(sum_loads)

    def add_rows(index):
        total = piece(index, 0)
        sum_loads[index - 1].wait()

        @pl.loop(0, width // 32)
        def _(step):
            rows = cols_of(step, 32)
            near = pl.ds(pl.multiple_of(width + step * 32, 32), 32)
            terms = [total[rows, :], staged[index - 1][rows, :], staged[index - 1][near, :]]
            total[rows, :] = sum(term.astype(F32) for term in terms).astype(BF)

        local(total, (gate_sum, up_sum)[index - 1], keep.at[index]).start()

    def add_down():
        drain(buffer_a, load.at[6])

        @pl.loop(0, tokens // 64)
        def _(step):
            rows = cols_of(step, 64)
            for index in range(GROUPS):
                total = down_piece(0, index)
                terms = [total[rows, :]]
                terms += [buffer_a[rows, pl.ds((slot * GROUPS + index) * width, width)] for slot in range(2)]
                total[rows, :] = sum(term.astype(F32) for term in terms).astype(BF)

        for index in range(GROUPS):
            local(down_piece(0, index), down_rows(down_sum, index, 0), keep.at[8]).start()

    one_scatter[1].hop(0)
    add_rows(1)
    merge_grads(3)
    add_rows(2)
    one_scatter[1].hop(1)
    one_scatter[1].hop(2)
    add_down()

    drain(gain_recv.at[pl.ds(8, 56), :], g_recv.at[0])
    gain_sum = gain_part[:, pl.ds(pl.multiple_of(own * width, width), width)]
    for flip in range(1, 8):
        gain_sum = gain_sum + gain_recv[pl.ds(flip * 8, 8), :]
    gain_z[pl.ds(0, 8), :] = gain_sum

    def share_gain_z(k):
        target = gain_z.at[pl.ds(8 * k, 8), :]
        return remote(gain_z.at[pl.ds(0, 8), :], target, y_send.at[1], y_recv.at[1], "tensor", lax.rem(rank + k, 4))

    for k in (1, 2, 3):
        share_gain_z(k).start()

    load_own = [
        local(hidden_in.at[part_rows(part), :], sent.at[own_rows(part), :], load.at[4 + part]) for part in range(PARTS)
    ]
    for part in range(PARTS):
        gather_branch[part].finish()
    start_all(load_own)
    wait_all(load_own)
    leave = [local(input_grad, input_ref, keep.at[6]), local(layer_out, out_ref, keep.at[7])]
    for scatter in mlp_scatter:
        scatter.wait()

    def mlp_term(part, index):
        return up_w.at[pl.ds((2 * part + index) * size, size), :]

    load_mlp = [
        [local(mlp_recv.at[arrived(part, slot), :], mlp_term(part, index), load.at[2 * part + index])
         for index, slot in enumerate((4, 2))]
        for part in range(PARTS)
    ]
    for part in range(PARTS):
        load_mlp[part][0].start()
        pl.when(inner(rank))(load_mlp[part][1].start)

        @pl.when(ends(rank))
        def _():
            mlp_term(part, 1)[...] = jnp.zeros((size, dim), BF)

    for part in range(PARTS):
        load_mlp[part][0].wait()
        pl.when(inner(rank))(load_mlp[part][1].wait)
        terms = [mlp_term(part, index) for index in range(2)]

        @pl.loop(0, size // 32)
        def _(step):
            rows = pl.ds(pl.multiple_of(part * size + step * 32, 32), 32)
            place = cols_of(step, 32)
            total = middle[rows, :]
            for term in terms:
                total = total + term[place, :].astype(F32)
            layer_out[rows, :] = total.astype(BF)

    leave[1].start()
    for part in range(PARTS):
        one_scatter[part].wait()

        @pl.loop(0, size // 32)
        def _(step):
            rows = pl.ds(pl.multiple_of(part * size + step * 32, 32), 32)
            place = pl.ds(pl.multiple_of(part * span + step * 32, 32), 32)
            total = received(part, step * 32, 32, input_grad[rows, :])
            input_grad[rows, :] = grad_middle[rows, :] + norm_back(total, sent[place, :].astype(F32), gains[0:1, :])

    leave[0].start()

    drain(gain_z.at[pl.ds(8, 24), :], y_recv.at[1])
    gain_all = gain_z[pl.ds(0, 8), :]
    for k in (1, 2, 3):
        gain_all = gain_all + gain_z[pl.ds(8 * k, 8), :]
    gain_total[...] = gain_all
    leave.append(local(gain_total, gain_out, keep.at[5]))
    leave[2].start()

    for scatter in mlp_scatter + one_scatter:
        scatter.finish()
    drain(gate_w.at[pl.ds(0, 3 * units // 8), :], d_send.at[0])
    drain(gain_recv.at[pl.ds(8, 56), :], y_send.at[0])
    drain(gain_recv.at[pl.ds(8, 56), :], g_send.at[0])
    drain(gain_z.at[pl.ds(8, 24), :], y_send.at[1])
    drain(two_half, h_send.at[1])
    drain(two_half, h_send.at[4])
    send_attended.wait_send()
    send_qkv.wait_send()
    def pieces(index, number):
        rows = number * width if index < 4 else number * heads * width // dim
        return gate_w.at[pl.ds(0, rows), pl.ds(0, 3 * heads if index == 3 else dim)]

    wait_all(leave)
    local(gate_w.at[pl.ds(0, width), :], gate_sum, keep.at[1]).wait()
    local(gate_w.at[pl.ds(0, width), :], up_sum, keep.at[2]).wait()
    drain(down_sum, keep.at[8])
    for index in range(1, 5):
        if index > 2:
            drain(pieces(index, 2), n_recv.at[index - 1])
            keep_grad(index).wait()
        drain(pieces(index, 3), w_send.at[index - 1])


def layer(hidden_in, cot, gains, weights, docs):
    tile, dim = hidden_in.shape
    tokens = 4 * tile
    width, heads = weights[0].shape
    units = weights[5].shape[1]
    dma = pltpu.SemaphoreType.DMA
    rows, narrow, ff = shape((tokens, dim), BF), shape((tokens, dim // 2), BF), shape((tokens, units), BF)
    weights_shape = [(units, width), (width, units), (width, units), (width, 3 * heads), (heads, width)]
    sums_shape = weights_shape[:3] + [(3 * width, 3 * heads), (heads, 3 * width)]
    parts_shape = [(units, 2 * width), (2 * width, units), (2 * width, units)]
    outs = [shape(dims, BF) for dims in sums_shape + parts_shape + weights_shape]
    outs += [ff] * 2 + [shape((tokens, 3 * heads), BF), shape((tokens, heads), BF), narrow, narrow]
    outs += [rows] * 3 + [shape((5 * tile, dim), BF), shape((dim, 3 * heads), BF), shape((units, dim), BF)]
    in_hbm = len(outs)
    outs += [shape((tile, dim), BF), shape((tile, dim), F32), shape((8, width), F32)]
    in_hbm += 3
    items = 4 + 3 * GROUPS
    scratch = [((dim, units), BF), ((dim, units), BF), ((units, dim), BF)]
    scratch += [((tokens, dim), BF)] * 3 + [((tokens, units), BF)] * 3
    scratch += [((tokens, dim // 2), BF)] * 2 + [((tokens, dim), BF)] * 3 + [((heads, dim), BF)]
    scratch += [((tokens, 3 * heads), BF)] + [((tokens, heads), BF)] * 2
    scratch += [((tokens, tokens), F32), ((tokens, 128), F32), ((tokens, 128), F32)]
    scratch += [((tokens, 1), F32), ((tokens, 1), F32), ((tile, dim), F32), ((tile, dim), F32)]
    scratch += [((tokens, dim), BF), ((5 * tile, dim), BF)]
    scratch += [((8, width), F32), ((8, dim), F32), ((8, dim), F32), ((64, width), F32), ((32, width), F32)]
    scratch += [((tile, dim), BF), ((tile, dim), F32), ((8, width), F32), (docs.shape, jnp.int32)]
    scratch += [((width,), BF)] * 2
    sems = [(2 + GROUPS,), (4 + GROUPS, 3), (3,), (GROUPS + 2,), (6,), (6,)]
    sems += [(2, PARTS), (2, PARTS, 3), (2, PARTS), (2, PARTS, 5), (4,), (4, 2), (1,), (GROUPS + 1,)]
    sems += [(1,), (1,), (2,), (2,), (15,), (8 + GROUPS,), (GROUPS,), (2 + GROUPS,), (4,)]
    return pl.pallas_call(
        layer_kernel,
        out_shape=outs,
        in_specs=[anyspace()] * 12,
        out_specs=[anyspace()] * in_hbm,
        scratch_shapes=[pltpu.VMEM(*entry) for entry in scratch] + [dma(entry) for entry in sems],
        compiler_params=pltpu.CompilerParams(vmem_limit_bytes=67000000, collective_id=0, has_side_effects=True),
        cost_estimate=cost(2 * tokens * dim * units * 12, 100e6),
        name="layer",
    )(hidden_in, cot, *gains, *weights, docs)


def sum_kernel(counts, *refs):
    parts, plain_in = refs[:5], refs[5:7]
    down, gate, up, query, key, value, out, *plain_out = refs[7:16]
    staged, totals, plain, load, store = refs[16:21], refs[21:26], refs[26:28], refs[28], refs[29]
    loads = [pltpu.make_async_copy(parts[index], staged[index], load.at[index]) for index in range(5)]
    loads += [pltpu.make_async_copy(plain_in[index], plain[index], load.at[5 + index]) for index in range(2)]
    start_all(loads)
    heads = query.shape[1]
    plain_stores = [pltpu.make_async_copy(plain[index], plain_out[index], store.at[14 + index]) for index in range(2)]
    targets = [[down], [gate], [up], [query, key, value], [out]]

    def stores(index, part):
        half = totals[index].shape[0] // 2
        rows = pl.ds(part * half, half)
        first = 2 * (index if index < 4 else 6) + part
        return [
            pltpu.make_async_copy(
                totals[index].at[rows, pl.ds(place * ref.shape[1], ref.shape[1])], ref.at[rows, :], store.at[first + 2 * place]
            )
            for place, ref in enumerate(targets[index])
        ]

    for index in range(5):
        loads[index].wait()
        rows_first = index in (1, 2, 3)
        rows, cols = totals[index].shape
        step_rows = 32 if rows_first else 256
        for part in range(2):

            @pl.loop(part * (rows // step_rows) // 2, (part + 1) * (rows // step_rows) // 2)
            def _(step):
                start = pl.multiple_of(step * step_rows, step_rows)
                total = None
                for slot in range(counts[index]):
                    if rows_first:
                        term = staged[index][pl.ds(pl.multiple_of(start + slot * rows, step_rows), step_rows), :]
                    else:
                        term = staged[index][pl.ds(start, step_rows), slot * cols : (slot + 1) * cols]
                    term = term.astype(F32)
                    total = term if total is None else total + term
                totals[index][pl.ds(start, step_rows), :] = total

            start_all(stores(index, part))
    for index in range(2):
        loads[5 + index].wait()
        plain_stores[index].start()
    for index in range(5):
        for part in range(2):
            wait_all(stores(index, part))
    wait_all(plain_stores)


def sum_grads(parts, plain, heads, counts):
    dims = [part.shape for part in parts]
    sums = [
        (rows // counts[index], cols) if index in (1, 2, 3) else (rows, cols // counts[index])
        for index, (rows, cols) in enumerate(dims)
    ]
    outs = sums[:3] + [(sums[3][0], heads)] * 3 + [sums[4]]
    dma = pltpu.SemaphoreType.DMA
    return pl.pallas_call(
        partial(sum_kernel, counts),
        out_shape=[shape(dim, F32) for dim in outs] + [shape(entry.shape, entry.dtype) for entry in plain],
        in_specs=[anyspace()] * 7,
        out_specs=[anyspace()] * 9,
        scratch_shapes=[pltpu.VMEM(dim, BF) for dim in dims]
        + [pltpu.VMEM(dim, F32) for dim in sums]
        + [pltpu.VMEM(entry.shape, entry.dtype) for entry in plain]
        + [dma((7,)), dma((16,))],
        compiler_params=params(),
        cost_estimate=cost(1e6, 22e6),
        name="sum_grads",
    )(*parts, *plain)


def shift(values, step):
    size = lax.axis_size("tensor")
    return lax.ppermute(values, "tensor", [(index, (index + step) % size) for index in range(size)])


def gather_rows(values):
    return [values] + [shift(values, step) for step in range(1, lax.axis_size("tensor"))]


def scatter_rows(parts):
    total = parts[0].astype(F32)
    for step in range(1, len(parts)):
        total = total + shift(parts[step], -step).astype(F32)
    return total


def gather_weight(values, axis):
    return [None], [lax.all_gather(values, "dp", axis=axis, tiled=True)]


def scatter_full(left, right, axis):
    full = dot_cols(left, right).astype(BF)
    return lax.psum_scatter(full, "dp", scatter_dimension=axis, tiled=True).astype(F32)


def frequencies():
    half_size = HEAD_DIM // 2
    return ROPE_BASE ** (-jnp.arange(half_size, dtype=F32) / half_size)


def rotary(length):
    angles = jnp.arange(length).astype(F32)[:, None] * frequencies()[None, :]
    cosine, sine = jnp.cos(angles), jnp.sin(angles)
    cosine = jnp.tile(cosine, (1, 8))
    sine = jnp.tile(jnp.concatenate([-sine, sine], axis=1), (1, 4))
    return cosine, sine


def position_tables(doc_ids, ranks):
    length = doc_ids.shape[0]
    token_index = jnp.arange(length, dtype=jnp.int32)
    before = jnp.concatenate([doc_ids[:1] - 1, doc_ids[:-1]])
    doc_start = lax.cummax(jnp.where(doc_ids != before, token_index, 0), axis=0)
    order = (lax.axis_index("tensor") - jnp.arange(ranks)) % ranks
    last = token_index.reshape(ranks, -1)[order].reshape(length)
    first = doc_start.reshape(ranks, -1)[order].reshape(length)
    cosine, sine = (table.reshape(ranks, -1, 256)[order].reshape(length, 256) for table in rotary(length))
    return cosine, sine, first[:, None], last[:, None], last[None, :]


def rms_back(grad_rows_, values, gain):
    inverse = lax.rsqrt(jnp.mean(values * values, axis=-1, keepdims=True) + EPSILON)
    scaled = grad_rows_ * gain
    return inverse * (scaled - values * inverse * inverse * jnp.mean(scaled * values, axis=-1, keepdims=True))


def body(
    hidden_in,
    out_cotangent,
    doc_ids,
    attn_gain,
    query_weight,
    key_weight,
    value_weight,
    out_weight,
    mlp_gain,
    gate_weight,
    up_weight,
    down_weight,
):
    ranks, groups = lax.axis_size("tensor"), lax.axis_size("dp")
    paired = (groups, ranks) == (8, 4)
    width, heads = query_weight.shape
    dim = hidden_in.shape[1]

    if paired:
        weights = (query_weight, key_weight, value_weight, out_weight, down_weight, gate_weight, up_weight)
        outs = layer(hidden_in, out_cotangent, (attn_gain, mlp_gain), weights, doc_ids.reshape(ranks, -1))
        sums = sum_grads(outs[:5], outs[-3:-1], heads, (1, 1, 1, 3, 3))
        down_grad, gate_grad, up_grad, query_grad, key_grad, value_grad, out_proj_grad, layer_out, input_grad = sums
        gain_total = outs[-1]
        share = width // ranks
        gain_grads = lax.dynamic_slice_in_dim(gain_total, lax.axis_index("tensor") * share, share, axis=1)
    else:
        tables = position_tables(doc_ids, ranks)
        input_local = hidden_in.astype(F32)
        hidden_rows = gather_rows(hidden_in)
        gains = lax.all_gather(jnp.stack([attn_gain, mlp_gain]), "dp", axis=1, tiled=True).astype(F32)
        attn_scale, mlp_scale = gains[:1], gains[1:]
        qkv_weight = jnp.concatenate([query_weight, key_weight, value_weight], axis=1)
        tags, qkv_pieces = gather_weight(qkv_weight, 0)
        tags, out_pieces = gather_weight(out_weight, 1)
        cot_rows = gather_rows(out_cotangent)
        tags, down_pieces = gather_weight(down_weight, 1)
        tags, gate_pieces = gather_weight(gate_weight, 0)
        tags, up_pieces = gather_weight(up_weight, 0)
        normed, qkv, attended, inverses, *branch_parts = attn_fwd(
            hidden_rows, attn_scale, tables, tags, width, qkv_pieces, out_pieces
        )
        middle = input_local + scatter_rows(branch_parts)
        sent = middle.astype(BF)
        sent_rows = gather_rows(sent)
        cot_full = jnp.concatenate(cot_rows, axis=0)
        normed_two, hidden, d_gate, d_up, mlp_gain_part, *two_parts = mlp(
            sent_rows, cot_rows, mlp_scale, tags, width, gate_pieces, up_pieces, down_pieces, ranks
        )
        grad_two_rows = scatter_rows(two_parts)
        grad_middle = out_cotangent.astype(F32) + rms_back(grad_two_rows, sent.astype(F32), mlp_scale)
        branch_rows = gather_rows(grad_middle.astype(BF))
        down_grad = scatter_full(hidden, cot_full, 1)
        gate_grad = scatter_full(normed_two, d_gate, 0)
        up_grad = scatter_full(normed_two, d_up, 0)
        mlp_rows = scatter_rows(mlp_out(hidden, ranks, dim, tags, width, down_pieces))
        layer_out = (middle + mlp_rows).astype(BF)
        branch_full, d_qkv, attn_gain_part, *one_parts = attn_bwd(
            branch_rows, hidden_rows, qkv, inverses, tables, tags, width, qkv_pieces, out_pieces, ranks
        )
        out_proj_grad = scatter_full(attended, branch_full, 1)
        query_grad, key_grad, value_grad = jnp.split(scatter_full(normed, d_qkv, 0), 3, axis=1)
        grad_one_rows = scatter_rows(one_parts)
        input_grad = grad_middle + rms_back(grad_one_rows, input_local, attn_scale)
        gain_parts = jnp.concatenate([attn_gain_part, mlp_gain_part], axis=0)
        gain_grads = lax.psum_scatter(gain_parts, ("dp", "tensor"), scatter_dimension=1, tiled=True)
    return (
        layer_out,
        input_grad,
        gain_grads[0],
        query_grad,
        key_grad,
        value_grad,
        out_proj_grad,
        gain_grads[1],
        gate_grad,
        up_grad,
        down_grad,
    )


def solution(mesh):
    return jax.shard_map(
        body,
        mesh=mesh,
        in_specs=(
            P(("dp", "tensor"), None),
            P(("dp", "tensor"), None),
            P("dp"),
            P("dp"),
            P("dp", "tensor"),
            P("dp", "tensor"),
            P("dp", "tensor"),
            P("tensor", "dp"),
            P("dp"),
            P("dp", "tensor"),
            P("dp", "tensor"),
            P("tensor", "dp"),
        ),
        out_specs=(
            P(("dp", "tensor"), None),
            P(("dp", "tensor"), None),
            P(("dp", "tensor")),
            P("dp", "tensor"),
            P("dp", "tensor"),
            P("dp", "tensor"),
            P("tensor", "dp"),
            P(("dp", "tensor")),
            P("dp", "tensor"),
            P("dp", "tensor"),
            P("tensor", "dp"),
        ),
        check_vma=False,
    )
```
